128 devices in a mesh: node: 16 (over z, y), local: 8 (over x, core).
Axes of the slice: x: 4, y: 4, z: 4, core: 2. Of those that a mesh axis runs over, the one named last changes fastest.
Arguments:
- x: bfloat16 [128, 384, 1024], P(('node', 'local'))
- y_cot: bfloat16 [128, 384, 1024], P(('node', 'local'))
- ln1_gain: bfloat16 [2, 1024], P(None, ('node', 'local'))
- ln1_bias: bfloat16 [2, 1024], P(None, ('node', 'local'))
- qkv_weight: bfloat16 [2, 1024, 16, 192], P(None, ('node', 'local'))
- qkv_bias: bfloat16 [2, 3072], P(None, ('node', 'local'))
- out_weight: bfloat16 [2, 1024, 1024], P(None, ('node', 'local'))
- out_bias: bfloat16 [2, 1024], P(None, ('node', 'local'))
- ln2_gain: bfloat16 [2, 1024], P(None, ('node', 'local'))
- ln2_bias: bfloat16 [2, 1024], P(None, ('node', 'local'))
- up_weight: bfloat16 [2, 1024, 4096], P(None, ('node', 'local'))
- up_bias: bfloat16 [2, 4096], P(None, ('node', 'local'))
- down_weight: bfloat16 [2, 4096, 1024], P(None, ('node', 'local'))
- down_bias: bfloat16 [2, 1024], P(None, ('node', 'local'))
Outputs:
- output 1: bfloat16 [128, 384, 1024], P(('node', 'local'))
- output 2: bfloat16 [128, 384, 1024], P(('node', 'local'))
- output 3: bfloat16 [2, 1024], P(None, ('node', 'local'))
- output 4: bfloat16 [2, 1024], P(None, ('node', 'local'))
- output 5: bfloat16 [2, 1024, 16, 192], P(None, ('node', 'local'))
- output 6: bfloat16 [2, 3072], P(None, ('node', 'local'))
- output 7: bfloat16 [2, 1024, 1024], P(None, ('node', 'local'))
- output 8: bfloat16 [2, 1024], P(None, ('node', 'local'))
- output 9: bfloat16 [2, 1024], P(None, ('node', 'local'))
- output 10: bfloat16 [2, 1024], P(None, ('node', 'local'))
- output 11: bfloat16 [2, 1024, 4096], P(None, ('node', 'local'))
- output 12: bfloat16 [2, 4096], P(None, ('node', 'local'))
- output 13: bfloat16 [2, 4096, 1024], P(None, ('node', 'local'))
- output 14: bfloat16 [2, 1024], P(None, ('node', 'local'))
All inputs are finite; a program needn't handle non-finite values.
Results may differ from the reference program's by a relative error of at most 0.018346.
Values are sent between devices in bfloat16 or wider.
A program may use at most 1 GiB of HBM per device.

```python
import jax
import jax.numpy as jnp
from jax import lax

D_MODEL = 1024
HEADS = 16
SEQ_LEN = 384
BATCH = 128
LAYERS = 2
HEAD_DIM = D_MODEL // HEADS
ROT_DIM = HEAD_DIM // 4
FF_DIM = 4 * D_MODEL
EPSILON = 1e-5


def slow_waves(rng_key, frequencies):
    amp_key, phase_key = jax.random.split(rng_key)
    positions = jnp.arange(SEQ_LEN, dtype=jnp.float32)[None, :, None] / SEQ_LEN
    wave_sum = jnp.zeros((BATCH, SEQ_LEN, D_MODEL), jnp.float32)
    for wave_idx, frequency in enumerate(frequencies):
        amplitude = jax.random.normal(jax.random.fold_in(amp_key, wave_idx), (BATCH, 1, D_MODEL), jnp.float32)
        phase_off = jax.random.uniform(jax.random.fold_in(phase_key, wave_idx), (BATCH, 1, D_MODEL), jnp.float32, 0.0, 6.283185307179586)
        wave_sum = wave_sum + amplitude * jnp.cos(6.283185307179586 * frequency * positions + phase_off)
    return wave_sum * (2.0 / len(frequencies)) ** 0.5


def normal_draw(rng_key, out_shape, spread, offset=0.0):
    return (offset + spread * jax.random.normal(rng_key, out_shape, jnp.float32)).astype(jnp.bfloat16)


def setup_inputs(seed: int = 0) -> dict:
    sub_keys = jax.random.split(jax.random.key(seed), 16)
    white_noise = jax.random.normal(sub_keys[0], (BATCH, SEQ_LEN, D_MODEL), jnp.float32)
    x = (0.8 * slow_waves(sub_keys[1], (0.5, 1.0, 2.0, 3.0)) + 0.6 * white_noise).astype(jnp.bfloat16)
    y_cot = normal_draw(sub_keys[2], (BATCH, SEQ_LEN, D_MODEL), (BATCH * SEQ_LEN) ** -0.25)
    width_scale = D_MODEL ** -0.5
    return {
        'x': x,
        'y_cot': y_cot,
        'ln1_gain': normal_draw(sub_keys[3], (LAYERS, D_MODEL), 0.25, 1.0),
        'ln1_bias': normal_draw(sub_keys[4], (LAYERS, D_MODEL), 0.25),
        'qkv_weight': normal_draw(sub_keys[5], (LAYERS, D_MODEL, HEADS, 3 * HEAD_DIM), width_scale),
        'qkv_bias': normal_draw(sub_keys[6], (LAYERS, 3 * D_MODEL), 0.3),
        'out_weight': normal_draw(sub_keys[7], (LAYERS, D_MODEL, D_MODEL), 1.5 * width_scale),
        'out_bias': normal_draw(sub_keys[8], (LAYERS, D_MODEL), 0.3),
        'ln2_gain': normal_draw(sub_keys[9], (LAYERS, D_MODEL), 0.25, 1.0),
        'ln2_bias': normal_draw(sub_keys[10], (LAYERS, D_MODEL), 0.25),
        'up_weight': normal_draw(sub_keys[11], (LAYERS, D_MODEL, FF_DIM), width_scale),
        'up_bias': normal_draw(sub_keys[12], (LAYERS, FF_DIM), 0.3),
        'down_weight': normal_draw(sub_keys[13], (LAYERS, FF_DIM, D_MODEL), FF_DIM ** -0.5),
        'down_bias': normal_draw(sub_keys[14], (LAYERS, D_MODEL), 0.3),
    }


def to_bf16(values):
    return values.astype(jnp.bfloat16).astype(jnp.float32)


def rope_tables():
    inv_freq = 1.0 / (10000.0 ** (jnp.arange(0, ROT_DIM, 2, dtype=jnp.float32) / ROT_DIM))
    angles = jnp.arange(SEQ_LEN, dtype=jnp.float32)[:, None] * inv_freq[None, :]
    angles = jnp.concatenate([angles, angles], axis=-1)
    return jnp.cos(angles), jnp.sin(angles)


def apply_rotary(vectors, cos_tab, sin_tab):
    half_dim = ROT_DIM // 2
    rot_part = vectors[..., :ROT_DIM]
    pass_part = vectors[..., ROT_DIM:]
    turned = jnp.concatenate([-rot_part[..., half_dim:], rot_part[..., :half_dim]], axis=-1)
    rot_part = rot_part * cos_tab[:, None, :] + turned * sin_tab[:, None, :]
    return jnp.concatenate([rot_part, pass_part], axis=-1)


def layer_norm(hidden, ln_gain, ln_bias):
    center = hidden - jnp.mean(hidden, axis=-1, keepdims=True)
    variance = jnp.mean(center * center, axis=-1, keepdims=True)
    return center * lax.rsqrt(variance + EPSILON) * ln_gain + ln_bias


def layer_forward(hidden, weights, cos_tab, sin_tab):
    (ln1_gain, ln1_bias, qkv_weight, qkv_bias, out_weight, out_bias,
     ln2_gain, ln2_bias, up_weight, up_bias, down_weight, down_bias) = weights
    normed_attn = to_bf16(layer_norm(hidden, ln1_gain, ln1_bias))
    normed_mlp = to_bf16(layer_norm(hidden, ln2_gain, ln2_bias))
    qkv_all = jnp.einsum('sd,dhe->she', normed_attn, qkv_weight) + qkv_bias.reshape(HEADS, 3 * HEAD_DIM)
    query_rot = to_bf16(apply_rotary(qkv_all[..., :HEAD_DIM], cos_tab, sin_tab))
    key_rot = to_bf16(apply_rotary(qkv_all[..., HEAD_DIM:2 * HEAD_DIM], cos_tab, sin_tab))
    values = to_bf16(qkv_all[..., 2 * HEAD_DIM:])
    scores = jnp.einsum('qhd,khd->hqk', query_rot, key_rot) * HEAD_DIM ** -0.5
    causal = jnp.arange(SEQ_LEN)[:, None] >= jnp.arange(SEQ_LEN)[None, :]
    scores = jnp.where(causal[None], scores, -1e30)
    attn_probs = to_bf16(jax.nn.softmax(scores, axis=-1))
    context = to_bf16(jnp.einsum('hqk,khd->qhd', attn_probs, values))
    attn_out = jnp.einsum('qhd,hde->qe', context, out_weight.reshape(HEADS, HEAD_DIM, D_MODEL)) + out_bias
    mlp_act = to_bf16(jax.nn.gelu(jnp.dot(normed_mlp, up_weight) + up_bias, approximate=False))
    mlp_out = jnp.dot(mlp_act, down_weight) + down_bias
    return hidden + attn_out + mlp_out


def reference(x, y_cot, ln1_gain, ln1_bias, qkv_weight, qkv_bias, out_weight, out_bias,
              ln2_gain, ln2_bias, up_weight, up_bias, down_weight, down_bias):
    stacked = tuple(tensor.astype(jnp.float32) for tensor in (
        ln1_gain, ln1_bias, qkv_weight, qkv_bias, out_weight, out_bias,
        ln2_gain, ln2_bias, up_weight, up_bias, down_weight, down_bias))
    cos_tab, sin_tab = rope_tables()

    def both_layers(x_seq, params):
        hidden = x_seq
        for layer_idx in range(LAYERS):
            hidden = to_bf16(layer_forward(hidden, [tensor[layer_idx] for tensor in params], cos_tab, sin_tab))
        return hidden

    def seq_step(grad_sums, seq_pair):
        x_seq, cot_seq = seq_pair
        seq_out, pullback = jax.vjp(both_layers, x_seq.astype(jnp.float32), stacked)
        x_bar, param_bars = pullback(cot_seq.astype(jnp.float32))
        grad_sums = tuple(grad_sum + part_grad for grad_sum, part_grad in zip(grad_sums, param_bars))
        return grad_sums, (seq_out.astype(jnp.bfloat16), x_bar.astype(jnp.bfloat16))

    zero_sums = tuple(jnp.zeros_like(tensor) for tensor in stacked)
    grad_sums, (y_out, x_grad) = lax.scan(seq_step, zero_sums, (x, y_cot))
    grad_list = [grad_sum.astype(jnp.bfloat16) for grad_sum in grad_sums]
    return (y_out, x_grad, grad_list[0], grad_list[1], grad_list[2], grad_list[3], grad_list[4], grad_list[5],
            grad_list[6], grad_list[7], grad_list[8], grad_list[9], grad_list[10], grad_list[11])
```

```python
import functools
import jax
import jax.numpy as jnp
from jax import lax
from jax.experimental import pallas as pl
from jax.experimental.pallas import tpu as pltpu
from jax.sharding import PartitionSpec as P

EPSILON = 1e-5
MESH = pl.DeviceIdType.MESH
ANY = pl.BlockSpec(memory_space=pl.ANY)
IN_VMEM = pl.BlockSpec(memory_space=pltpu.VMEM)
ORDERS = ((2, 1, 0), (1, 0, 2), (0, 2, 1))
VMEM_LIMIT = 60 * 2**20


def flip(index, mask):
    if mask == 1:
        return index + 1 - 2 * lax.rem(index, 2)
    if mask == 3:
        return 3 - index
    return lax.rem(index + 2, 4)


def place():
    node = lax.axis_index('node')
    local = lax.axis_index('local')
    return (node // 4, lax.rem(node, 4), local // 2), lax.rem(local, 2)


def device_at(chip, core):
    return (chip[0] * 4 + chip[1], chip[2] * 2 + core)


def moved(chip, axis, mask):
    return tuple(flip(v, mask) if k == axis else v for k, v in enumerate(chip))


def colour_plan(colour):
    return ORDERS[colour // 2], ((1, 3) if colour % 2 == 0 else (3, 1))


def entry_barrier(chip, core):
    barrier = pltpu.get_barrier_semaphore()
    for axis in range(3):
        for mask in (1, 3):
            pl.semaphore_signal(barrier, inc=1, device_id=device_at(moved(chip, axis, mask), core), device_id_type=MESH)
    pl.semaphore_signal(barrier, inc=1, device_id=device_at(chip, 1 - core), device_id_type=MESH)
    pl.semaphore_wait(barrier, 7)


GATHER_PARTS = ((0, 0, 2048, 0), (0, 2048, 2048, 1), (1, 0, 512, 2), (1, 512, 512, 3),
                (2, 0, 2048, 4), (2, 2048, 1024, 5), (3, 0, 1024, 5))


def gather_kernel(n_layers, *refs):
    shards, refs = refs[:5], refs[5:]
    fulls, refs = refs[:4 * n_layers + 1], refs[4 * n_layers + 1:]
    send_sem, recv_sem, pass_send, pass_recv, own_sem = refs
    chip, core = place()
    entry_barrier(chip, core)
    every = pl.ds(0, 4)
    copies = []

    parts = []
    for layer in range(n_layers):
        for arr, col, width, colour in GATHER_PARTS:
            parts.append((fulls[4 * layer + arr], shards[arr].at[layer, :, pl.ds(col, width)], col, width, colour))
    parts.append((fulls[-1], shards[4], 0, 128, 4))

    def box(part, where):
        full, _, col, width, _ = part
        return full.at[where[0], where[1], where[2], core, :, pl.ds(col, width)]

    def reach(n, slot, where, target, own):
        part = parts[n]
        copy = pltpu.make_async_remote_copy(
            src_ref=part[1] if own else box(part, where), dst_ref=box(part, where),
            send_sem=send_sem.at[n, slot], recv_sem=recv_sem.at[n, slot],
            device_id=device_at(target, core), device_id_type=MESH)
        copy.start()
        copies.append(copy)
        return copy

    def pass_on(n, slot, where, own):
        part = parts[n]
        copy = pltpu.make_async_remote_copy(
            src_ref=part[1] if own else box(part, where), dst_ref=box(part, where),
            send_sem=pass_send.at[n, slot], recv_sem=pass_recv.at[n, slot],
            device_id=device_at(chip, 1 - core), device_id_type=MESH)
        copy.start()
        copies.append(copy)
        return copy

    def span(order, stage, value):
        where = list(chip)
        for axis in order[:stage]:
            where[axis] = every
        where[order[stage]] = value
        return where

    own = []
    for layer in range(n_layers):
        for arr in range(4):
            own.append(pltpu.make_async_copy(
                shards[arr].at[layer], fulls[4 * layer + arr].at[chip[0], chip[1], chip[2], core], own_sem.at[4 * layer + arr]))
    own.append(pltpu.make_async_copy(shards[4], fulls[-1].at[chip[0], chip[1], chip[2], core], own_sem.at[4 * n_layers]))
    for copy in own:
        copy.start()

    passed = []
    first = {}
    for stage in range(3):
        for turn in range(2):
            for n, part in enumerate(parts):
                order, masks = colour_plan(part[4])
                axis = order[stage]
                target = moved(chip, axis, masks[turn])
                first[n, turn] = reach(n, 3 * stage + turn, span(order, stage, chip[axis]), target, stage == 0)
        if stage == 0:
            for n, part in enumerate(parts):
                passed.append(pass_on(n, 9, list(chip), True))
            for copy in own:
                copy.wait()
        second = {}
        for n, part in enumerate(parts):
            order, masks = colour_plan(part[4])
            axis = order[stage]
            first[n, 0].wait_recv()
            where = span(order, stage, flip(chip[axis], masks[0]))
            second[n] = reach(n, 3 * stage + 2, where, moved(chip, axis, masks[1]), False)
            passed.append(pass_on(n, 3 * stage, where, False))
        for n, part in enumerate(parts):
            order, masks = colour_plan(part[4])
            axis = order[stage]
            first[n, 1].wait_recv()
            passed.append(pass_on(n, 3 * stage + 1, span(order, stage, flip(chip[axis], masks[1])), False))
            second[n].wait_recv()
            passed.append(pass_on(n, 3 * stage + 2, span(order, stage, flip(chip[axis], 2)), False))
    for copy in passed:
        copy.wait_recv()
    for copy in copies:
        copy.wait_send()


def gather_all(up, down, qkv, out, small):
    n_layers = up.shape[0]
    shards = (up, down, qkv, out, small)
    n_parts = len(GATHER_PARTS) * n_layers + 1
    shapes = [jax.ShapeDtypeStruct((4, 4, 4, 2) + tensor.shape[1:], tensor.dtype) for _ in range(n_layers) for tensor in shards[:4]]
    shapes.append(jax.ShapeDtypeStruct((4, 4, 4, 2) + small.shape, small.dtype))
    fulls = pl.pallas_call(
        functools.partial(gather_kernel, n_layers),
        out_shape=shapes,
        in_specs=[IN_VMEM] * 5,
        out_specs=[ANY] * len(shapes),
        scratch_shapes=[pltpu.SemaphoreType.DMA((n_parts, 9)), pltpu.SemaphoreType.DMA((n_parts, 9)),
                        pltpu.SemaphoreType.DMA((n_parts, 10)), pltpu.SemaphoreType.DMA((n_parts, 10)),
                        pltpu.SemaphoreType.DMA((4 * n_layers + 1,))],
        compiler_params=pltpu.CompilerParams(collective_id=0, has_side_effects=True),
        name='gather_weights',
    )(*shards)
    layers = []
    for layer in range(n_layers):
        layers.append([full.reshape((-1, full.shape[-1])) for full in fulls[4 * layer:4 * layer + 4]])
    return layers, fulls[-1].reshape((128,) + small.shape)


REDUCE_PARTS = ((0, 0, 1024, 0), (0, 1024, 1024, 1), (1, 0, 256, 2), (1, 256, 256, 3),
                (2, 0, 1024, 4), (2, 1024, 512, 5), (3, 0, 512, 5), (4, 0, 128, 4))


def reduce_kernel(*refs):
    grads, sums, refs = refs[:5], refs[5:10], refs[10:]
    n_parts = len(REDUCE_PARTS)
    kept, refs = refs[:n_parts], refs[n_parts:]
    came, refs = [refs[6 * n:6 * n + 6] for n in range(n_parts)], refs[6 * n_parts:]
    send_sem, recv_sem, load_sem, tile = refs
    chip, core = place()
    entry_barrier(chip, core)
    copies = []
    started = {}

    def reach(n, slot, src, dst, target, to_core=core):
        copy = pltpu.make_async_remote_copy(
            src_ref=src, dst_ref=dst, send_sem=send_sem.at[n, slot], recv_sem=recv_sem.at[n, slot],
            device_id=device_at(target, to_core), device_id_type=MESH)
        copy.start()
        copies.append(copy)
        started[n, slot] = copy

    def at_axis(ref, axis, value, n_axes, lead=()):
        every = [pl.ds(0, 4)] * n_axes
        every[axis] = value
        return ref.at[tuple(lead) + tuple(every)]

    def add_into(dst, src, n_axes):
        if n_axes == 0:
            dst[...] += src[...]
            return
        rows, cols = dst.shape[-2:]

        @pl.loop(0, 4 ** n_axes)
        def _(k):
            index = (k,) if n_axes == 1 else (k // 4, lax.rem(k, 4))
            dst[index] += src[index]

    plans = [colour_plan(part[3]) for part in REDUCE_PARTS]

    loads = {}
    for slot in (1, 0):
        for n, (arr, col, width, colour) in enumerate(REDUCE_PARTS):
            order, (one, two) = plans[n]
            axis = order[0]
            mine = chip[axis]
            target = moved(chip, axis, one)
            theirs = flip(mine, one) if slot == 0 else flip(mine, 2)
            cols = grads[arr].at[:, :, :, :, pl.ds(col, width)]
            reach(n, slot, at_axis(cols, axis, theirs, 3), came[n][0].at[slot], target)
    for slot in (1, 0):
        for n, (arr, col, width, colour) in enumerate(REDUCE_PARTS):
            order, (one, two) = plans[n]
            axis = order[0]
            keep = chip[axis] if slot == 0 else flip(chip[axis], two)
            cols = grads[arr].at[:, :, :, :, pl.ds(col, width)]
            loads[n, slot] = pltpu.make_async_copy(at_axis(cols, axis, keep, 3), kept[n].at[slot], load_sem.at[n, slot])
            loads[n, slot].start()

    def remaining(order, stage):
        return [axis for axis in range(3) if axis not in order[:stage]]

    for n in range(n_parts):
        order, (one, two) = plans[n]
        loads[n, 1].wait()
        started[n, 1].wait_recv()
        add_into(kept[n].at[1], came[n][0].at[1], 2)
        reach(n, 2, kept[n].at[1], came[n][1], moved(chip, order[0], two))
    for n in range(n_parts):
        loads[n, 0].wait()
        started[n, 0].wait_recv()
        add_into(kept[n].at[0], came[n][0].at[0], 2)

    def held(n, stage):
        order, _ = plans[n]
        axes = remaining(order, 1)
        ref = kept[n].at[0]
        if stage == 1:
            return ref, axes.index(order[1]), 2
        fixed = axes.index(order[1])
        return at_axis(ref, fixed, chip[order[1]], 2), 0, 1

    for stage in (1, 2):
        base = 3 * stage
        for n in range(n_parts):
            order, (one, two) = plans[n]
            ref, spot, n_axes = held(n, stage)
            mine = chip[order[stage]]
            started[n, base - 1].wait_recv()
            arrived = came[n][2 * stage - 1]
            for slot in (1, 0):
                theirs = flip(mine, one) if slot == 0 else flip(mine, 2)
                view = at_axis(ref, spot, theirs, n_axes)
                add_into(view, at_axis(arrived, spot, theirs, n_axes), n_axes - 1)
                reach(n, base + slot, view, came[n][2 * stage].at[slot], moved(chip, order[stage], one))
            for keep in (flip(mine, two), mine):
                add_into(at_axis(ref, spot, keep, n_axes), at_axis(arrived, spot, keep, n_axes), n_axes - 1)
        for n in range(n_parts):
            order, (one, two) = plans[n]
            ref, spot, n_axes = held(n, stage)
            mine = chip[order[stage]]
            started[n, base + 1].wait_recv()
            view = at_axis(ref, spot, flip(mine, two), n_axes)
            add_into(view, came[n][2 * stage].at[1], n_axes - 1)
            reach(n, base + 2, view, came[n][2 * stage + 1], moved(chip, order[stage], two))
        for n in range(n_parts):
            order, _ = plans[n]
            ref, spot, n_axes = held(n, stage)
            started[n, base].wait_recv()
            add_into(at_axis(ref, spot, chip[order[stage]], n_axes), came[n][2 * stage].at[0], n_axes - 1)

    for n, (arr, col, width, colour) in enumerate(REDUCE_PARTS):
        order, _ = plans[n]
        ref, _, _ = held(n, 2)
        box = ref.at[chip[order[2]]]
        started[n, 8].wait_recv()
        add_into(box, came[n][5], 0)
        if arr == 4:
            reach(n, 9, box, tile, chip, 1 - core)
            continue
        rows = box.shape[0] // 2
        theirs = box.at[pl.ds(pl.multiple_of((1 - core) * rows, rows), rows)]
        reach(n, 9, theirs, sums[arr].at[core, :, pl.ds(col, width)], chip, 1 - core)
    for n, (arr, col, width, colour) in enumerate(REDUCE_PARTS):
        order, _ = plans[n]
        ref, _, _ = held(n, 2)
        box = ref.at[chip[order[2]]]
        started[n, 9].wait_recv()
        if arr == 4:
            sums[4][...] = box[...] + tile[...]
            continue
        rows = box.shape[0] // 2
        sums[arr][core, :, pl.ds(col, width)] = box[pl.ds(pl.multiple_of(core * rows, rows), rows), :]
    for copy in copies:
        copy.wait_send()


def reduce_all(up, down, qkv, out, small):
    grads = [tensor.reshape((4, 4, 4, -1, tensor.shape[-1])) for tensor in (up, down, qkv, out, small)]
    shapes = [jax.ShapeDtypeStruct((2, g.shape[3] // 2, g.shape[4]), jnp.float32) for g in grads[:4]]
    shapes.append(jax.ShapeDtypeStruct((8, 128), jnp.float32))
    kept, came = [], []
    for arr, col, width, colour in REDUCE_PARTS:
        block = (grads[arr].shape[3], width)
        kept.append(pltpu.VMEM((2, 4, 4) + block, jnp.float32))
        for lead in ((2, 4, 4), (4, 4), (2, 4), (4,), (2,), ()):
            came.append(pltpu.VMEM(lead + block, jnp.float32))
    n_parts = len(REDUCE_PARTS)
    return pl.pallas_call(
        reduce_kernel,
        out_shape=shapes,
        in_specs=[ANY] * 5,
        out_specs=[IN_VMEM] * 5,
        scratch_shapes=kept + came + [pltpu.SemaphoreType.DMA((n_parts, 10)), pltpu.SemaphoreType.DMA((n_parts, 10)),
                                      pltpu.SemaphoreType.DMA((n_parts, 2)), pltpu.VMEM((8, 128), jnp.float32)],
        compiler_params=pltpu.CompilerParams(collective_id=1, has_side_effects=True, vmem_limit_bytes=VMEM_LIMIT),
        name='reduce_gradients',
    )(*grads)


def product(einsum_form, first_op, second_op):
    return jnp.einsum(einsum_form, first_op, second_op, preferred_element_type=jnp.float32)


def rope_tables(seq_len, rot_dim):
    inv_freq = 1.0 / (10000.0 ** (jnp.arange(0, rot_dim, 2, dtype=jnp.float32) / rot_dim))
    angles = jnp.arange(seq_len, dtype=jnp.float32)[:, None] * inv_freq[None, :]
    angles = jnp.concatenate([angles, angles], axis=-1)
    return jnp.cos(angles), jnp.sin(angles)


def norm_pair(hidden32, gain_attn, bias_attn, gain_mlp, bias_mlp):
    center = hidden32 - jnp.mean(hidden32, axis=-1, keepdims=True)
    scaled = center * lax.rsqrt(jnp.mean(center * center, axis=-1, keepdims=True) + EPSILON)
    return ((scaled * gain_attn + bias_attn).astype(jnp.bfloat16),
            (scaled * gain_mlp + bias_mlp).astype(jnp.bfloat16))


def rotary_split(qkv_all, cos_tab, sin_tab):
    head_dim = qkv_all.shape[-1] // 3
    rot_dim = head_dim // 4
    half_dim = rot_dim // 2
    cos_b = cos_tab[:, None, :]
    sin_b = sin_tab[:, None, :]

    def rotate_vec(vectors):
        rot_part = vectors[..., :rot_dim]
        turned = jnp.concatenate([-rot_part[..., half_dim:], rot_part[..., :half_dim]], axis=-1)
        return jnp.concatenate([rot_part * cos_b + turned * sin_b, vectors[..., rot_dim:]], axis=-1)

    query_rot = rotate_vec(qkv_all[..., :head_dim]).astype(jnp.bfloat16)
    key_rot = rotate_vec(qkv_all[..., head_dim:2 * head_dim]).astype(jnp.bfloat16)
    return query_rot, key_rot, qkv_all[..., 2 * head_dim:].astype(jnp.bfloat16)


def gelu_bf16(pre_act):
    return jax.nn.gelu(pre_act, approximate=False).astype(jnp.bfloat16)


def layer_forward(hidden, weights, vectors, cos_tab, sin_tab):
    up_weight, down_weight, qkv_weight, out_weight = weights
    ln1_gain, ln1_bias, ln2_gain, ln2_bias, qkv_bias, out_bias, up_bias, down_bias = vectors
    seq_len, d_model = hidden.shape
    num_heads = 16
    head_dim = d_model // num_heads
    hidden32 = hidden.astype(jnp.float32)
    (normed_attn, normed_mlp), norm_pull = jax.vjp(norm_pair, hidden32, ln1_gain, ln1_bias, ln2_gain, ln2_bias)
    qkv_all = (product('sd,de->se', normed_attn, qkv_weight) + qkv_bias).reshape(seq_len, num_heads, 3 * head_dim)
    (query_rot, key_rot, values), rotary_pull = jax.vjp(
        functools.partial(rotary_split, cos_tab=cos_tab, sin_tab=sin_tab), qkv_all)
    scores = product('qhd,khd->hqk', query_rot, key_rot) * head_dim ** -0.5
    causal = lax.broadcasted_iota(jnp.int32, (seq_len, seq_len), 0) >= lax.broadcasted_iota(jnp.int32, (seq_len, seq_len), 1)
    attn_probs = jax.nn.softmax(jnp.where(causal, scores, -1e30), axis=-1)
    probs_bf = attn_probs.astype(jnp.bfloat16)
    context = product('hqk,khd->qhd', probs_bf, values).astype(jnp.bfloat16).reshape(seq_len, d_model)
    attn_out = product('qe,ed->qd', context, out_weight) + out_bias
    pre_act = product('sd,df->sf', normed_mlp, up_weight) + up_bias
    mlp_act, gelu_pull = jax.vjp(gelu_bf16, pre_act)
    mlp_out = product('sf,fd->sd', mlp_act, down_weight) + down_bias
    layer_out = (hidden32 + attn_out + mlp_out).astype(jnp.bfloat16)
    saved_state = (norm_pull, normed_attn, normed_mlp, rotary_pull, query_rot, key_rot, values,
                   attn_probs, probs_bf, context, gelu_pull, mlp_act)
    return layer_out, saved_state


def layer_backward(d_out, weights, saved_state, with_partner, half_of):
    up_weight, down_weight, qkv_weight, out_weight = weights
    (norm_pull, normed_attn, normed_mlp, rotary_pull, query_rot, key_rot, values,
     attn_probs, probs_bf, context, gelu_pull, mlp_act) = saved_state
    seq_len, d_model = d_out.shape
    num_heads = 16
    head_dim = d_model // num_heads
    d_out32 = d_out.astype(jnp.float32)
    out_sum_grad = jnp.sum(d_out32, axis=0)

    def both(left, right):
        mine, other = half_of(right)
        return left, mine, with_partner(other)

    d_act = product('sd,fd->sf', d_out, down_weight).astype(jnp.bfloat16)
    (d_pre,) = gelu_pull(d_act)
    up_bias_grad = jnp.sum(d_pre, axis=0)
    d_pre_bf = d_pre.astype(jnp.bfloat16)
    d_normed_mlp = product('sf,df->sd', d_pre_bf, up_weight).astype(jnp.bfloat16)
    d_context = product('qd,ed->qe', d_out, out_weight).astype(jnp.bfloat16).reshape(seq_len, num_heads, head_dim)
    d_probs = product('qhd,khd->hqk', d_context, values).astype(jnp.bfloat16).astype(jnp.float32)
    d_values = product('hqk,qhd->khd', probs_bf, d_context).astype(jnp.bfloat16)
    d_scores = (attn_probs * (d_probs - jnp.sum(d_probs * attn_probs, axis=-1, keepdims=True)) * head_dim ** -0.5).astype(jnp.bfloat16)
    d_query = product('hqk,khd->qhd', d_scores, key_rot).astype(jnp.bfloat16)
    d_key = product('hqk,qhd->khd', d_scores, query_rot).astype(jnp.bfloat16)
    (d_qkv,) = rotary_pull((d_query, d_key, d_values))
    d_qkv = d_qkv.reshape(seq_len, 3 * d_model)
    qkv_bias_grad = jnp.sum(d_qkv, axis=0)
    d_qkv_bf = d_qkv.astype(jnp.bfloat16)
    d_normed_attn = product('se,de->sd', d_qkv_bf, qkv_weight).astype(jnp.bfloat16)
    d_hidden32, gain1_grad, bias1_grad, gain2_grad, bias2_grad = norm_pull((d_normed_attn, d_normed_mlp))
    d_hidden = (d_out32 + d_hidden32).astype(jnp.bfloat16)

    def weight_grad(left, left_other, right):
        mine, other = half_of(right)
        rows = jnp.concatenate([left, left_other], axis=0)
        cols = jnp.concatenate([mine, with_partner(other)], axis=0)
        return product('sd,se->de', rows, cols)

    out_half = half_of(d_out)
    d_out_cols = jnp.concatenate([out_half[0], with_partner(out_half[1])], axis=0)

    def on_d_out(left):
        return product('sd,se->de', jnp.concatenate([left, with_partner(left)], axis=0), d_out_cols)

    down_grad = on_d_out(mlp_act)
    out_grad = on_d_out(context)
    up_grad = weight_grad(normed_mlp, with_partner(normed_mlp), d_pre_bf)
    qkv_grad = weight_grad(normed_attn, with_partner(normed_attn), d_qkv_bf)
    vectors = (gain1_grad, bias1_grad, gain2_grad, bias2_grad, qkv_bias_grad, out_sum_grad, up_bias_grad, out_sum_grad)
    return d_hidden, (up_grad, down_grad, qkv_grad, out_grad), vectors


def pack_vectors(vectors):
    packed = jnp.concatenate(vectors, axis=-1)
    return jnp.pad(packed, ((0, 0), (0, 128 - packed.shape[-1])))


def solution(mesh):
    shard_axes = ('node', 'local')
    act_spec = P(shard_axes)
    param_spec = P(None, shard_axes)
    n_local = mesh.shape['local']
    pairs = [(i, i + 1 - 2 * (i % 2)) for i in range(n_local)]

    def with_partner(tensor):
        return lax.ppermute(tensor, 'local', pairs)

    def device_step(x, y_cot, ln1_gain, ln1_bias, qkv_weight, qkv_bias, out_weight, out_bias,
                    ln2_gain, ln2_bias, up_weight, up_bias, down_weight, down_bias):
        num_layers = ln1_gain.shape[0]
        core = lax.rem(lax.axis_index('local'), 2)
        cos_tab, sin_tab = rope_tables(x.shape[1], qkv_weight.shape[3] // 12)

        def half_of(tensor):
            width = tensor.shape[1] // 2
            return (lax.dynamic_slice_in_dim(tensor, core * width, width, 1),
                    lax.dynamic_slice_in_dim(tensor, (1 - core) * width, width, 1))

        small = (ln1_gain, ln1_bias, ln2_gain, ln2_bias, qkv_bias, out_bias, up_bias, down_bias)
        widths = [tensor.shape[1] for tensor in small]
        small_tile = jnp.pad(pack_vectors(small), ((0, 8 - num_layers), (0, 0)))
        layers, small_full = gather_all(up_weight, down_weight, qkv_weight.reshape(num_layers, -1, 3 * x.shape[2]),
                                        out_weight, small_tile)

        def vectors_of(layer):
            found, start = [], 0
            for width in widths:
                found.append(small_full[:, layer, start:start + width].reshape(-1).astype(jnp.float32))
                start += width
            return found

        hidden = x[0]
        states = []
        for layer in range(num_layers):
            hidden, state = layer_forward(hidden, layers[layer], vectors_of(layer), cos_tab, sin_tab)
            states.append(state)
        y_out = hidden
        d_hidden = y_cot[0]
        sums = [None] * num_layers
        for layer in reversed(range(num_layers)):
            d_hidden, weight_grads, vector_grads = layer_backward(d_hidden, layers[layer], states[layer], with_partner, half_of)
            rows = pack_vectors([grad.reshape(128, -1) for grad in vector_grads])
            tiles = jnp.pad(rows.reshape(64, 2, 128), ((0, 0), (0, 6), (0, 0)))
            sums[layer] = reduce_all(*weight_grads, tiles)

        def joined(arr, shape):
            return jnp.stack([s[arr].swapaxes(0, 1).reshape(shape[1:]).astype(jnp.bfloat16) for s in sums])

        small_sums = jnp.stack([lax.dynamic_index_in_dim(s[4], core, 0, False) for s in sums]).astype(jnp.bfloat16)
        small_grads, start = [], 0
        for width in widths:
            small_grads.append(small_sums[:, start:start + width])
            start += width
        g1, b1, g2, b2, qb, ob, ub, db = small_grads
        return (y_out[None], d_hidden[None], g1, b1, joined(2, qkv_weight.shape), qb, joined(3, out_weight.shape), ob,
                g2, b2, joined(0, up_weight.shape), ub, joined(1, down_weight.shape), db)

    return jax.shard_map(device_step, mesh=mesh,
                         in_specs=(act_spec, act_spec) + (param_spec,) * 12,
                         out_specs=(act_spec, act_spec) + (param_spec,) * 12,
                         check_vma=False)
```

```python
import functools
import jax
import jax.numpy as jnp
from jax import lax
from jax.experimental import pallas as pl
from jax.experimental.pallas import tpu as pltpu
from jax.sharding import PartitionSpec as P

EPSILON = 1e-5
MESH = pl.DeviceIdType.MESH
ANY = pl.BlockSpec(memory_space=pl.ANY)
IN_VMEM = pl.BlockSpec(memory_space=pltpu.VMEM)
ORDERS = ((2, 1, 0), (1, 0, 2), (0, 2, 1))
VMEM_LIMIT = 60 * 2**20


def flip(index, mask):
    if mask == 1:
        return index + 1 - 2 * lax.rem(index, 2)
    if mask == 3:
        return 3 - index
    return lax.rem(index + 2, 4)


def place():
    node = lax.axis_index('node')
    local = lax.axis_index('local')
    return (node // 4, lax.rem(node, 4), local // 2), lax.rem(local, 2)


def device_at(chip, core):
    return (chip[0] * 4 + chip[1], chip[2] * 2 + core)


def moved(chip, axis, mask):
    return tuple(flip(v, mask) if k == axis else v for k, v in enumerate(chip))


def colour_plan(colour):
    return ORDERS[colour // 2], ((1, 3) if colour % 2 == 0 else (3, 1))


def entry_barrier(chip, core):
    barrier = pltpu.get_barrier_semaphore()
    for axis in range(3):
        for mask in (1, 3):
            pl.semaphore_signal(barrier, inc=1, device_id=device_at(moved(chip, axis, mask), core), device_id_type=MESH)
    pl.semaphore_signal(barrier, inc=1, device_id=device_at(chip, 1 - core), device_id_type=MESH)
    pl.semaphore_wait(barrier, 7)


GATHER_PARTS = ((0, 0, 2048, 0), (0, 2048, 2048, 1), (1, 0, 512, 2), (1, 512, 512, 3),
                (2, 0, 2048, 4), (2, 2048, 1024, 5), (3, 0, 1024, 5))


def gather_kernel(n_layers, *refs):
    shards, refs = refs[:5], refs[5:]
    fulls, refs = refs[:4 * n_layers + 1], refs[4 * n_layers + 1:]
    send_sem, recv_sem, pass_send, pass_recv, own_sem = refs
    chip, core = place()
    entry_barrier(chip, core)
    every = pl.ds(0, 4)
    copies = []

    parts = []
    for layer in range(n_layers):
        for arr, col, width, colour in GATHER_PARTS:
            parts.append((fulls[4 * layer + arr], shards[arr].at[layer, :, pl.ds(col, width)], col, width, colour))
    parts.append((fulls[-1], shards[4], 0, 128, 4))

    def box(part, where):
        full, _, col, width, _ = part
        return full.at[where[0], where[1], where[2], core, :, pl.ds(col, width)]

    def reach(n, slot, where, target, own):
        part = parts[n]
        copy = pltpu.make_async_remote_copy(
            src_ref=part[1] if own else box(part, where), dst_ref=box(part, where),
            send_sem=send_sem.at[n, slot], recv_sem=recv_sem.at[n, slot],
            device_id=device_at(target, core), device_id_type=MESH)
        copy.start()
        copies.append(copy)
        return copy

    def pass_on(n, slot, where, own):
        part = parts[n]
        copy = pltpu.make_async_remote_copy(
            src_ref=part[1] if own else box(part, where), dst_ref=box(part, where),
            send_sem=pass_send.at[n, slot], recv_sem=pass_recv.at[n, slot],
            device_id=device_at(chip, 1 - core), device_id_type=MESH)
        copy.start()
        copies.append(copy)
        return copy

    def span(order, stage, value):
        where = list(chip)
        for axis in order[:stage]:
            where[axis] = every
        where[order[stage]] = value
        return where

    own = []
    for layer in range(n_layers):
        for arr in range(4):
            own.append(pltpu.make_async_copy(
                shards[arr].at[layer], fulls[4 * layer + arr].at[chip[0], chip[1], chip[2], core], own_sem.at[4 * layer + arr]))
    own.append(pltpu.make_async_copy(shards[4], fulls[-1].at[chip[0], chip[1], chip[2], core], own_sem.at[4 * n_layers]))
    for copy in own:
        copy.start()

    passed = []
    first = {}
    for stage in range(3):
        for turn in range(2):
            for n, part in enumerate(parts):
                order, masks = colour_plan(part[4])
                axis = order[stage]
                target = moved(chip, axis, masks[turn])
                first[n, turn] = reach(n, 3 * stage + turn, span(order, stage, chip[axis]), target, stage == 0)
        if stage == 0:
            for n, part in enumerate(parts):
                passed.append(pass_on(n, 9, list(chip), True))
            for copy in own:
                copy.wait()
        second = {}
        for n, part in enumerate(parts):
            order, masks = colour_plan(part[4])
            axis = order[stage]
            first[n, 0].wait_recv()
            where = span(order, stage, flip(chip[axis], masks[0]))
            second[n] = reach(n, 3 * stage + 2, where, moved(chip, axis, masks[1]), False)
            passed.append(pass_on(n, 3 * stage, where, False))
        for n, part in enumerate(parts):
            order, masks = colour_plan(part[4])
            axis = order[stage]
            first[n, 1].wait_recv()
            passed.append(pass_on(n, 3 * stage + 1, span(order, stage, flip(chip[axis], masks[1])), False))
            second[n].wait_recv()
            passed.append(pass_on(n, 3 * stage + 2, span(order, stage, flip(chip[axis], 2)), False))
    for copy in passed:
        copy.wait_recv()
    for copy in copies:
        copy.wait_send()


def gather_all(up, down, qkv, out, small):
    n_layers = up.shape[0]
    shards = (up, down, qkv, out, small)
    n_parts = len(GATHER_PARTS) * n_layers + 1
    shapes = [jax.ShapeDtypeStruct((4, 4, 4, 2) + tensor.shape[1:], tensor.dtype) for _ in range(n_layers) for tensor in shards[:4]]
    shapes.append(jax.ShapeDtypeStruct((4, 4, 4, 2) + small.shape, small.dtype))
    fulls = pl.pallas_call(
        functools.partial(gather_kernel, n_layers),
        out_shape=shapes,
        in_specs=[IN_VMEM] * 5,
        out_specs=[ANY] * len(shapes),
        scratch_shapes=[pltpu.SemaphoreType.DMA((n_parts, 9)), pltpu.SemaphoreType.DMA((n_parts, 9)),
                        pltpu.SemaphoreType.DMA((n_parts, 10)), pltpu.SemaphoreType.DMA((n_parts, 10)),
                        pltpu.SemaphoreType.DMA((4 * n_layers + 1,))],
        compiler_params=pltpu.CompilerParams(collective_id=0, has_side_effects=True),
        name='gather_weights',
    )(*shards)
    layers = []
    for layer in range(n_layers):
        layers.append([full.reshape((-1, full.shape[-1])) for full in fulls[4 * layer:4 * layer + 4]])
    return layers, fulls[-1].reshape((128,) + small.shape)


REDUCE_PARTS = ((0, 0, 1024, 0), (0, 1024, 1024, 1), (1, 0, 256, 2), (1, 256, 256, 3),
                (2, 0, 1024, 4), (2, 1024, 512, 5), (3, 0, 512, 5), (4, 0, 128, 4))


def reduce_kernel(*refs):
    grads, sums, refs = refs[:5], refs[5:10], refs[10:]
    n_parts = len(REDUCE_PARTS)
    kept, refs = refs[:n_parts], refs[n_parts:]
    came, refs = [refs[6 * n:6 * n + 6] for n in range(n_parts)], refs[6 * n_parts:]
    send_sem, recv_sem, load_sem, tile = refs
    chip, core = place()
    entry_barrier(chip, core)
    copies = []
    started = {}

    def reach(n, slot, src, dst, target, to_core=core):
        copy = pltpu.make_async_remote_copy(
            src_ref=src, dst_ref=dst, send_sem=send_sem.at[n, slot], recv_sem=recv_sem.at[n, slot],
            device_id=device_at(target, to_core), device_id_type=MESH)
        copy.start()
        copies.append(copy)
        started[n, slot] = copy

    def at_axis(ref, axis, value, n_axes, lead=()):
        every = [pl.ds(0, 4)] * n_axes
        every[axis] = value
        return ref.at[tuple(lead) + tuple(every)]

    def add_into(dst, src, n_axes):
        if n_axes == 0:
            dst[...] += src[...]
            return
        rows, cols = dst.shape[-2:]

        @pl.loop(0, 4 ** n_axes)
        def _(k):
            index = (k,) if n_axes == 1 else (k // 4, lax.rem(k, 4))
            dst[index] += src[index]

    plans = [colour_plan(part[3]) for part in REDUCE_PARTS]

    loads = {}
    for slot in (1, 0):
        for n, (arr, col, width, colour) in enumerate(REDUCE_PARTS):
            order, (one, two) = plans[n]
            axis = order[0]
            mine = chip[axis]
            target = moved(chip, axis, one)
            theirs = flip(mine, one) if slot == 0 else flip(mine, 2)
            cols = grads[arr].at[:, :, :, :, pl.ds(col, width)]
            reach(n, slot, at_axis(cols, axis, theirs, 3), came[n][0].at[slot], target)
    for slot in (1, 0):
        for n, (arr, col, width, colour) in enumerate(REDUCE_PARTS):
            order, (one, two) = plans[n]
            axis = order[0]
            keep = chip[axis] if slot == 0 else flip(chip[axis], two)
            cols = grads[arr].at[:, :, :, :, pl.ds(col, width)]
            loads[n, slot] = pltpu.make_async_copy(at_axis(cols, axis, keep, 3), kept[n].at[slot], load_sem.at[n, slot])
            loads[n, slot].start()

    def remaining(order, stage):
        return [axis for axis in range(3) if axis not in order[:stage]]

    for n in range(n_parts):
        order, (one, two) = plans[n]
        loads[n, 1].wait()
        started[n, 1].wait_recv()
        add_into(kept[n].at[1], came[n][0].at[1], 2)
        reach(n, 2, kept[n].at[1], came[n][1], moved(chip, order[0], two))
    for n in range(n_parts):
        loads[n, 0].wait()
        started[n, 0].wait_recv()
        add_into(kept[n].at[0], came[n][0].at[0], 2)

    def held(n, stage):
        order, _ = plans[n]
        axes = remaining(order, 1)
        ref = kept[n].at[0]
        if stage == 1:
            return ref, axes.index(order[1]), 2
        fixed = axes.index(order[1])
        return at_axis(ref, fixed, chip[order[1]], 2), 0, 1

    for stage in (1, 2):
        base = 3 * stage
        for n in range(n_parts):
            order, (one, two) = plans[n]
            ref, spot, n_axes = held(n, stage)
            mine = chip[order[stage]]
            started[n, base - 1].wait_recv()
            arrived = came[n][2 * stage - 1]
            for slot in (1, 0):
                theirs = flip(mine, one) if slot == 0 else flip(mine, 2)
                view = at_axis(ref, spot, theirs, n_axes)
                add_into(view, at_axis(arrived, spot, theirs, n_axes), n_axes - 1)
                reach(n, base + slot, view, came[n][2 * stage].at[slot], moved(chip, order[stage], one))
            for keep in (flip(mine, two), mine):
                add_into(at_axis(ref, spot, keep, n_axes), at_axis(arrived, spot, keep, n_axes), n_axes - 1)
        for n in range(n_parts):
            order, (one, two) = plans[n]
            ref, spot, n_axes = held(n, stage)
            mine = chip[order[stage]]
            started[n, base + 1].wait_recv()
            view = at_axis(ref, spot, flip(mine, two), n_axes)
            add_into(view, came[n][2 * stage].at[1], n_axes - 1)
            reach(n, base + 2, view, came[n][2 * stage + 1], moved(chip, order[stage], two))
        for n in range(n_parts):
            order, _ = plans[n]
            ref, spot, n_axes = held(n, stage)
            started[n, base].wait_recv()
            add_into(at_axis(ref, spot, chip[order[stage]], n_axes), came[n][2 * stage].at[0], n_axes - 1)

    for n, (arr, col, width, colour) in enumerate(REDUCE_PARTS):
        order, _ = plans[n]
        ref, _, _ = held(n, 2)
        box = ref.at[chip[order[2]]]
        started[n, 8].wait_recv()
        add_into(box, came[n][5], 0)
        if arr == 4:
            reach(n, 9, box, tile, chip, 1 - core)
            continue
        rows = box.shape[0] // 2
        theirs = box.at[pl.ds(pl.multiple_of((1 - core) * rows, rows), rows)]
        reach(n, 9, theirs, sums[arr].at[core, :, pl.ds(col, width)], chip, 1 - core)
    for n, (arr, col, width, colour) in enumerate(REDUCE_PARTS):
        order, _ = plans[n]
        ref, _, _ = held(n, 2)
        box = ref.at[chip[order[2]]]
        started[n, 9].wait_recv()
        if arr == 4:
            sums[4][...] = box[...] + tile[...]
            continue
        rows = box.shape[0] // 2
        sums[arr][core, :, pl.ds(col, width)] = box[pl.ds(pl.multiple_of(core * rows, rows), rows), :]
    for copy in copies:
        copy.wait_send()


def reduce_all(up, down, qkv, out, small):
    grads = [tensor.reshape((4, 4, 4, -1, tensor.shape[-1])) for tensor in (up, down, qkv, out, small)]
    shapes = [jax.ShapeDtypeStruct((2, g.shape[3] // 2, g.shape[4]), jnp.float32) for g in grads[:4]]
    shapes.append(jax.ShapeDtypeStruct((8, 128), jnp.float32))
    kept, came = [], []
    for arr, col, width, colour in REDUCE_PARTS:
        block = (grads[arr].shape[3], width)
        kept.append(pltpu.VMEM((2, 4, 4) + block, jnp.float32))
        for lead in ((2, 4, 4), (4, 4), (2, 4), (4,), (2,), ()):
            came.append(pltpu.VMEM(lead + block, jnp.float32))
    n_parts = len(REDUCE_PARTS)
    return pl.pallas_call(
        reduce_kernel,
        out_shape=shapes,
        in_specs=[ANY] * 5,
        out_specs=[IN_VMEM] * 5,
        scratch_shapes=kept + came + [pltpu.SemaphoreType.DMA((n_parts, 10)), pltpu.SemaphoreType.DMA((n_parts, 10)),
                                      pltpu.SemaphoreType.DMA((n_parts, 2)), pltpu.VMEM((8, 128), jnp.float32)],
        compiler_params=pltpu.CompilerParams(collective_id=1, has_side_effects=True, vmem_limit_bytes=VMEM_LIMIT),
        name='reduce_gradients',
    )(*grads)


SEQ, WIDTH, HIDDEN, TILE = 384, 1024, 4096, 512
N_TILES = HIDDEN // TILE
PAIR = 128
INV_SQRT2 = 0.7071067811865476
INV_SQRT2PI = 0.3989422804014327
SCALE = 0.125


def dot(a, b):
    return lax.dot_general(a, b, (((1,), (0,)), ((), ())), preferred_element_type=jnp.float32)


def dot_t(a, b):
    return lax.dot_general(a, b, (((1,), (1,)), ((), ())), preferred_element_type=jnp.float32)


def lanes(start, width=PAIR):
    return pl.ds(pl.multiple_of(start, PAIR), width)


def turn(x, cos, sin_a, sin_b):
    return x * cos + pltpu.roll(x, PAIR - 8, 1) * sin_a + pltpu.roll(x, 8, 1) * sin_b


def turn_back(d, cos, sin_a, sin_b):
    return d * cos + pltpu.roll(d * sin_a, 8, 1) + pltpu.roll(d * sin_b, PAIR - 8, 1)


def split_heads(x):
    first = lax.broadcasted_iota(jnp.int32, (PAIR, PAIR), 1) < PAIR // 2
    rows = []
    for j in range(SEQ // PAIR):
        block = x[j * PAIR:(j + 1) * PAIR]
        rows += [jnp.where(first, block, jnp.zeros_like(block)), jnp.where(first, jnp.zeros_like(block), block)]
    return jnp.concatenate(rows, axis=0)


def probabilities(q_block, keys, i):
    scores = dot_t(q_block, keys)
    causal = (lax.broadcasted_iota(jnp.int32, (PAIR, PAIR), 0) >= lax.broadcasted_iota(jnp.int32, (PAIR, PAIR), 1))
    probs = [None] * (2 * i + 2)
    for head in range(2):
        chunks = [scores[:, (2 * j + head) * PAIR:(2 * j + head + 1) * PAIR] * SCALE for j in range(i + 1)]
        chunks[i] = jnp.where(causal, chunks[i], -1e30)
        top = chunks[0]
        for chunk in chunks[1:]:
            top = jnp.maximum(top, chunk)
        top = jnp.max(top, axis=1, keepdims=True)
        chunks = [jnp.exp(chunk - top) for chunk in chunks]
        total = chunks[0]
        for chunk in chunks[1:]:
            total = total + chunk
        inverse = 1.0 / jnp.sum(total, axis=1, keepdims=True)
        for j in range(i + 1):
            probs[2 * j + head] = chunks[j] * inverse
    return probs


def normalised(h):
    center = h - jnp.mean(h, axis=1, keepdims=True)
    inverse = lax.rsqrt(jnp.mean(center * center, axis=1, keepdims=True) + EPSILON)
    return center * inverse, inverse


LN_ROWS = 64


def forward_kernel(h_ref, g1_ref, b1_ref, g2_ref, b2_ref, qkvb_ref, outb_ref, upb_ref, cos_ref, sina_ref, sinb_ref,
                   wqkv, wout, wup, wdown, y_ref, n1_ref, n2_ref, qkv_ref, ctx_ref, act_ref, pre_hbm,
                   wqkv_v, wout_v, wup_v, wdown_v, acc, pre_v, sems, pre_sems):
    loads = []
    for k in range(6):
        loads.append(pltpu.make_async_copy(wqkv.at[:, pl.ds(k * 512, 512)], wqkv_v.at[:, pl.ds(k * 512, 512)], sems.at[k]))
    loads.append(pltpu.make_async_copy(wout, wout_v, sems.at[6]))
    for t in range(N_TILES):
        loads.append(pltpu.make_async_copy(wup.at[:, pl.ds(t * TILE, TILE)], wup_v.at[:, pl.ds(t * TILE, TILE)], sems.at[7 + 2 * t]))
        loads.append(pltpu.make_async_copy(wdown.at[pl.ds(t * TILE, TILE)], wdown_v.at[pl.ds(t * TILE, TILE)], sems.at[8 + 2 * t]))
    for load in loads:
        load.start()

    @pl.loop(0, SEQ // LN_ROWS)
    def _(r):
        rows = pl.ds(pl.multiple_of(r * LN_ROWS, LN_ROWS), LN_ROWS)
        scaled, _ = normalised(h_ref[rows, :].astype(jnp.float32))
        n1_ref[rows, :] = (scaled * g1_ref[...] + b1_ref[...]).astype(jnp.bfloat16)
        n2_ref[rows, :] = (scaled * g2_ref[...] + b2_ref[...]).astype(jnp.bfloat16)

    for k in range(6):
        loads[k].wait()
        x = dot(n1_ref[...], wqkv_v[:, k * 512:(k + 1) * 512]) + qkvb_ref[:, k * 512:(k + 1) * 512]
        for c in range(4):
            block = x[:, c * PAIR:(c + 1) * PAIR]
            if k < 4:
                block = turn(block, cos_ref[...], sina_ref[...], sinb_ref[...])
            qkv_ref[:, k * 512 + c * PAIR:k * 512 + (c + 1) * PAIR] = block.astype(jnp.bfloat16)

    @pl.loop(0, WIDTH // PAIR)
    def _(pair):
        keys = split_heads(qkv_ref[:, lanes(WIDTH + pair * PAIR)])
        values = split_heads(qkv_ref[:, lanes(2 * WIDTH + pair * PAIR)])
        for i in range(SEQ // PAIR):
            n = (i + 1) * 2 * PAIR
            probs = probabilities(qkv_ref[i * PAIR:(i + 1) * PAIR, lanes(pair * PAIR)], keys[:n], i)
            probs = jnp.concatenate([p.astype(jnp.bfloat16) for p in probs], axis=1)
            ctx_ref[i * PAIR:(i + 1) * PAIR, lanes(pair * PAIR)] = dot(probs, values[:n]).astype(jnp.bfloat16)

    loads[6].wait()
    for k in range(2):
        cols = slice(k * 512, (k + 1) * 512)
        acc[:, cols] = h_ref[:, cols].astype(jnp.float32) + dot(ctx_ref[...], wout_v[:, cols]) + outb_ref[:, cols]
    stores = []
    for t in range(N_TILES):
        cols = slice(t * TILE, (t + 1) * TILE)
        loads[7 + 2 * t].wait()
        pre = dot(n2_ref[...], wup_v[:, cols]) + upb_ref[:, cols]
        pre_v[t] = pre
        stores.append(pltpu.make_async_copy(pre_v.at[t], pre_hbm.at[t], pre_sems.at[t]))
        stores[-1].start()
        act_ref[:, cols] = (0.5 * pre * (1.0 + lax.erf(pre * INV_SQRT2))).astype(jnp.bfloat16)
        loads[8 + 2 * t].wait()
        acc[...] += dot(act_ref[:, cols], wdown_v[cols, :])
    y_ref[...] = acc[...].astype(jnp.bfloat16)
    for store in stores:
        store.wait()


def forward_layer(hidden, weights, vectors, tables):
    up_weight, down_weight, qkv_weight, out_weight = weights
    g1, b1, g2, b2, qkv_bias, out_bias, up_bias, down_bias = [v.reshape(1, -1) for v in vectors]
    bf16 = jnp.bfloat16
    shapes = [((SEQ, WIDTH), bf16)] * 3 + [((SEQ, 3 * WIDTH), bf16), ((SEQ, WIDTH), bf16), ((SEQ, HIDDEN), bf16),
                                           ((N_TILES, SEQ, TILE), jnp.float32)]
    return pl.pallas_call(
        forward_kernel,
        out_shape=[jax.ShapeDtypeStruct(s, d) for s, d in shapes],
        in_specs=[IN_VMEM] * 11 + [ANY] * 4,
        out_specs=[IN_VMEM] * 6 + [ANY],
        scratch_shapes=[pltpu.VMEM((WIDTH, 3 * WIDTH), bf16), pltpu.VMEM((WIDTH, WIDTH), bf16), pltpu.VMEM((WIDTH, HIDDEN), bf16),
                        pltpu.VMEM((HIDDEN, WIDTH), bf16), pltpu.VMEM((SEQ, WIDTH), jnp.float32),
                        pltpu.VMEM((N_TILES, SEQ, TILE), jnp.float32), pltpu.SemaphoreType.DMA((23,)), pltpu.SemaphoreType.DMA((N_TILES,))],
        compiler_params=pltpu.CompilerParams(vmem_limit_bytes=VMEM_LIMIT),
        cost_estimate=pl.CostEstimate(flops=10 * 10**9, bytes_accessed=45 * 10**6, transcendentals=4 * 10**6),
        name='forward_layer',
    )(hidden, g1, b1, g2, b2, qkv_bias, out_bias + down_bias, up_bias, *tables, qkv_weight, out_weight, up_weight, down_weight)


def backward_kernel(dout_ref, h_ref, g1_ref, g2_ref, cos_ref, sina_ref, sinb_ref, qkv_ref, pre_hbm, wqkv, wout, wup, wdown,
                    dh_ref, dpre_ref, dqkv_ref, dg1_ref, db1_ref, dg2_ref, db2_ref, dqkvb_ref, dupb_ref, dsum_ref,
                    wqkv_v, wout_v, wup_v, wdown_v, pre_v, dn2, dn1, dctx, dk_acc, dv_acc, tile_sems, wout_sem, qkv_sems):
    def tile_loads(t, slot):
        start = pl.multiple_of(t * TILE, TILE)
        return (pltpu.make_async_copy(wdown.at[pl.ds(start, TILE)], wdown_v.at[slot], tile_sems.at[slot, 0]),
                pltpu.make_async_copy(pre_hbm.at[t], pre_v.at[slot], tile_sems.at[slot, 1]),
                pltpu.make_async_copy(wup.at[:, pl.ds(start, TILE)], wup_v.at[slot], tile_sems.at[slot, 2]))

    def qkv_load(k):
        return pltpu.make_async_copy(wqkv.at[:, pl.ds(k * WIDTH, WIDTH)], wqkv_v.at[k % 2], qkv_sems.at[k % 2])

    for t in range(2):
        for load in tile_loads(t, t):
            load.start()
    load_out = pltpu.make_async_copy(wout, wout_v, wout_sem)
    load_out.start()
    for k in range(2):
        qkv_load(k).start()
    dsum_ref[...] = jnp.sum(dout_ref[...].astype(jnp.float32), axis=0, keepdims=True)
    dn2[...] = jnp.zeros_like(dn2)

    @pl.loop(0, N_TILES)
    def _(t):
        slot = lax.rem(t, 2)
        cols = pl.ds(pl.multiple_of(t * TILE, TILE), TILE)
        for load in tile_loads(t, slot):
            load.wait()
        d_act = dot_t(dout_ref[...], wdown_v[slot]).astype(jnp.bfloat16).astype(jnp.float32)
        pre = pre_v[slot]
        slope = 0.5 * (1.0 + lax.erf(pre * INV_SQRT2)) + pre * (INV_SQRT2PI * jnp.exp(-0.5 * pre * pre))
        d_pre = d_act * slope
        dupb_ref[:, cols] = jnp.sum(d_pre, axis=0, keepdims=True)
        d_pre = d_pre.astype(jnp.bfloat16)
        dpre_ref[:, cols] = d_pre
        dn2[...] += dot_t(d_pre, wup_v[slot])

        @pl.when(t + 2 < N_TILES)
        def _():
            for load in tile_loads(t + 2, slot):
                load.start()

    load_out.wait()
    for k in range(2):
        rows = slice(k * 512, (k + 1) * 512)
        dctx[:, rows] = dot_t(dout_ref[...], wout_v[rows, :]).astype(jnp.bfloat16)

    @pl.loop(0, WIDTH // PAIR)
    def _(pair):
        at = lanes(pair * PAIR)
        keys = split_heads(qkv_ref[:, lanes(WIDTH + pair * PAIR)])
        values = split_heads(qkv_ref[:, lanes(2 * WIDTH + pair * PAIR)])
        q_t = qkv_ref[:, at].T
        dc_t = dctx[:, at].T
        dbq = jnp.zeros((1, PAIR), jnp.float32)
        for i in range(SEQ // PAIR):
            n = (i + 1) * 2 * PAIR
            rows = slice(i * PAIR, (i + 1) * PAIR)
            probs = probabilities(qkv_ref[rows, at], keys[:n], i)
            d_all = dot_t(dctx[rows, at], values[:n]).astype(jnp.bfloat16).astype(jnp.float32)
            d_probs = [d_all[:, j * PAIR:(j + 1) * PAIR] for j in range(2 * i + 2)]
            d_scores = [None] * (2 * i + 2)
            for head in range(2):
                mean = probs[head] * d_probs[head]
                for j in range(1, i + 1):
                    mean = mean + probs[2 * j + head] * d_probs[2 * j + head]
                mean = jnp.sum(mean, axis=1, keepdims=True)
                for j in range(head, 2 * i + 2, 2):
                    d_scores[j] = (probs[j] * (d_probs[j] - mean) * SCALE).astype(jnp.bfloat16)
            d_scores = jnp.concatenate(d_scores, axis=1)
            probs = jnp.concatenate([p.astype(jnp.bfloat16) for p in probs], axis=1)
            d_query = dot(d_scores, keys[:n]).astype(jnp.bfloat16).astype(jnp.float32)
            d_query = turn_back(d_query, cos_ref[rows, :], sina_ref[rows, :], sinb_ref[rows, :])
            dbq = dbq + jnp.sum(d_query, axis=0, keepdims=True)
            dqkv_ref[rows, at] = d_query.astype(jnp.bfloat16)
            d_keys = dot(q_t[:, rows], d_scores)
            d_values = dot(dc_t[:, rows], probs)
            old = 2 * i * PAIR
            if i:
                dk_acc[:, :old] += d_keys[:, :old]
                dv_acc[:, :old] += d_values[:, :old]
            dk_acc[:, old:n] = d_keys[:, old:]
            dv_acc[:, old:n] = d_values[:, old:]
        dqkvb_ref[:, at] = dbq
        first = lax.broadcasted_iota(jnp.int32, (PAIR, PAIR), 0) < PAIR // 2
        dbk = jnp.zeros((1, PAIR), jnp.float32)
        dbv = jnp.zeros((1, PAIR), jnp.float32)
        for j in range(SEQ // PAIR):
            rows = slice(j * PAIR, (j + 1) * PAIR)
            left, right = slice(2 * j * PAIR, (2 * j + 1) * PAIR), slice((2 * j + 1) * PAIR, (2 * j + 2) * PAIR)
            d_key = jnp.where(first, dk_acc[:, left], dk_acc[:, right]).T.astype(jnp.bfloat16).astype(jnp.float32)
            d_key = turn_back(d_key, cos_ref[rows, :], sina_ref[rows, :], sinb_ref[rows, :])
            dbk = dbk + jnp.sum(d_key, axis=0, keepdims=True)
            dqkv_ref[rows, lanes(WIDTH + pair * PAIR)] = d_key.astype(jnp.bfloat16)
            d_value = jnp.where(first, dv_acc[:, left], dv_acc[:, right]).T.astype(jnp.bfloat16)
            dbv = dbv + jnp.sum(d_value.astype(jnp.float32), axis=0, keepdims=True)
            dqkv_ref[rows, lanes(2 * WIDTH + pair * PAIR)] = d_value
        dqkvb_ref[:, lanes(WIDTH + pair * PAIR)] = dbk
        dqkvb_ref[:, lanes(2 * WIDTH + pair * PAIR)] = dbv

    for k in range(3):
        qkv_load(k).wait()
        part = dot_t(dqkv_ref[:, k * WIDTH:(k + 1) * WIDTH], wqkv_v[k % 2])
        if k == 0:
            dn1[...] = part
            qkv_load(2).start()
        else:
            dn1[...] += part

    for ref in (dg1_ref, db1_ref, dg2_ref, db2_ref):
        ref[...] = jnp.zeros_like(ref)

    @pl.loop(0, SEQ // LN_ROWS)
    def _(r):
        rows = pl.ds(pl.multiple_of(r * LN_ROWS, LN_ROWS), LN_ROWS)
        scaled, inverse = normalised(h_ref[rows, :].astype(jnp.float32))
        d1 = dn1[rows, :].astype(jnp.bfloat16).astype(jnp.float32)
        d2 = dn2[rows, :].astype(jnp.bfloat16).astype(jnp.float32)
        dg1_ref[...] += jnp.sum(d1 * scaled, axis=0, keepdims=True)
        db1_ref[...] += jnp.sum(d1, axis=0, keepdims=True)
        dg2_ref[...] += jnp.sum(d2 * scaled, axis=0, keepdims=True)
        db2_ref[...] += jnp.sum(d2, axis=0, keepdims=True)
        d_scaled = d1 * g1_ref[...] + d2 * g2_ref[...]
        d_h = inverse * (d_scaled - jnp.mean(d_scaled, axis=1, keepdims=True)
                         - scaled * jnp.mean(d_scaled * scaled, axis=1, keepdims=True))
        dh_ref[rows, :] = (dout_ref[rows, :].astype(jnp.float32) + d_h).astype(jnp.bfloat16)


def backward_layer(d_out, hidden, weights, vectors, tables, qkv, pre):
    up_weight, down_weight, qkv_weight, out_weight = weights
    g1, g2 = vectors[0].reshape(1, -1), vectors[2].reshape(1, -1)
    bf16, f32 = jnp.bfloat16, jnp.float32
    shapes = [((SEQ, WIDTH), bf16), ((SEQ, HIDDEN), bf16), ((SEQ, 3 * WIDTH), bf16)] + [((1, WIDTH), f32)] * 4
    shapes += [((1, 3 * WIDTH), f32), ((1, HIDDEN), f32), ((1, WIDTH), f32)]
    return pl.pallas_call(
        backward_kernel,
        out_shape=[jax.ShapeDtypeStruct(s, d) for s, d in shapes],
        in_specs=[IN_VMEM] * 8 + [ANY] * 5,
        out_specs=[IN_VMEM] * 10,
        scratch_shapes=[pltpu.VMEM((2, WIDTH, WIDTH), bf16), pltpu.VMEM((WIDTH, WIDTH), bf16), pltpu.VMEM((2, WIDTH, TILE), bf16),
                        pltpu.VMEM((2, TILE, WIDTH), bf16), pltpu.VMEM((2, SEQ, TILE), f32), pltpu.VMEM((SEQ, WIDTH), f32),
                        pltpu.VMEM((SEQ, WIDTH), f32), pltpu.VMEM((SEQ, WIDTH), bf16), pltpu.VMEM((PAIR, 2 * SEQ), f32),
                        pltpu.VMEM((PAIR, 2 * SEQ), f32), pltpu.SemaphoreType.DMA((2, 3)), pltpu.SemaphoreType.DMA,
                        pltpu.SemaphoreType.DMA((2,))],
        compiler_params=pltpu.CompilerParams(vmem_limit_bytes=VMEM_LIMIT),
        cost_estimate=pl.CostEstimate(flops=13 * 10**9, bytes_accessed=45 * 10**6, transcendentals=6 * 10**6),
        name='backward_layer',
    )(d_out, hidden, g1, g2, *tables, qkv, pre, qkv_weight, out_weight, up_weight, down_weight)


def product(einsum_form, first_op, second_op):
    return jnp.einsum(einsum_form, first_op, second_op, preferred_element_type=jnp.float32)


def rope_tables(seq_len, head_dim):
    rot_dim = head_dim // 4
    inv_freq = 1.0 / (10000.0 ** (jnp.arange(0, rot_dim, 2, dtype=jnp.float32) / rot_dim))
    angles = jnp.arange(seq_len, dtype=jnp.float32)[:, None] * inv_freq[None, :]
    cos, sin = jnp.cos(angles), jnp.sin(angles)
    zero = jnp.zeros_like(sin)
    rest = jnp.zeros((seq_len, head_dim - rot_dim), jnp.float32)
    tables = ([cos, cos, rest + 1.0], [-sin, zero, rest], [zero, sin, rest])
    return [jnp.tile(jnp.concatenate(table, axis=1), (1, 2)) for table in tables]


def pack_vectors(vectors):
    packed = jnp.concatenate(vectors, axis=-1)
    return jnp.pad(packed, ((0, 0), (0, 128 - packed.shape[-1])))


def heads_last(tensor):
    lead = tensor.shape[:-2]
    return jnp.swapaxes(tensor.reshape(lead + (16, 3, 64)), -3, -2).reshape(lead + (3072,))


def heads_first(tensor):
    lead = tensor.shape[:-1]
    return jnp.swapaxes(tensor.reshape(lead + (3, 16, 64)), -3, -2).reshape(lead + (16, 192))


def solution(mesh):
    shard_axes = ('node', 'local')
    act_spec = P(shard_axes)
    param_spec = P(None, shard_axes)
    n_local = mesh.shape['local']
    pairs = [(i, i + 1 - 2 * (i % 2)) for i in range(n_local)]

    def with_partner(tensor):
        return lax.ppermute(tensor, 'local', pairs)

    def device_step(x, y_cot, ln1_gain, ln1_bias, qkv_weight, qkv_bias, out_weight, out_bias,
                    ln2_gain, ln2_bias, up_weight, up_bias, down_weight, down_bias):
        num_layers = ln1_gain.shape[0]
        core = lax.rem(lax.axis_index('local'), 2)
        tables = rope_tables(x.shape[1], qkv_weight.shape[3] // 3)

        def half_of(tensor):
            width = tensor.shape[1] // 2
            return (lax.dynamic_slice_in_dim(tensor, core * width, width, 1),
                    lax.dynamic_slice_in_dim(tensor, (1 - core) * width, width, 1))

        def columns(tensor):
            mine, other = half_of(tensor)
            return jnp.concatenate([mine, with_partner(other)], axis=0)

        def rows(tensor):
            return jnp.concatenate([tensor, with_partner(tensor)], axis=0)

        small = (ln1_gain, ln1_bias, ln2_gain, ln2_bias, qkv_bias, out_bias, up_bias, down_bias)
        widths = [tensor.shape[1] for tensor in small]
        small_tile = jnp.pad(pack_vectors(small), ((0, 8 - num_layers), (0, 0)))
        layers, small_full = gather_all(up_weight, down_weight, heads_last(qkv_weight), out_weight, small_tile)

        def vectors_of(layer):
            found, start = [], 0
            for width in widths:
                found.append(small_full[:, layer, start:start + width].reshape(-1).astype(jnp.float32))
                start += width
            found[4] = heads_last(found[4].reshape(16, 192))
            return found

        hidden = x[0]
        inputs, states, vectors = [], [], []
        for layer in range(num_layers):
            inputs.append(hidden)
            vectors.append(vectors_of(layer))
            hidden, *state = forward_layer(hidden, layers[layer], vectors[layer], tables)
            states.append(state)
        y_out = hidden
        d_hidden = y_cot[0]
        sums = [None] * num_layers
        for layer in reversed(range(num_layers)):
            normed_attn, normed_mlp, qkv, context, act, pre = states[layer]
            d_out = d_hidden
            d_hidden, d_pre, d_qkv, dg1, db1, dg2, db2, dqkvb, dupb, dsum = backward_layer(
                d_out, inputs[layer], layers[layer], vectors[layer], tables, qkv, pre)
            d_out_cols = columns(d_out)
            down_grad = product('sd,se->de', rows(act), d_out_cols)
            out_grad = product('sd,se->de', rows(context), d_out_cols)
            up_grad = product('sd,se->de', rows(normed_mlp), columns(d_pre))
            qkv_grad = product('sd,se->de', rows(normed_attn), columns(d_qkv))
            vector_grads = (dg1, db1, dg2, db2, heads_first(dqkvb), dsum, dupb, dsum)
            packed = pack_vectors([grad.reshape(128, -1) for grad in vector_grads])
            tiles = jnp.pad(packed.reshape(64, 2, 128), ((0, 0), (0, 6), (0, 0)))
            sums[layer] = reduce_all(up_grad, down_grad, qkv_grad, out_grad, tiles)

        def joined(arr):
            return jnp.stack([jnp.concatenate([s[arr][0], s[arr][1]], axis=1) for s in sums]).astype(jnp.bfloat16)

        small_sums = jnp.stack([lax.dynamic_index_in_dim(s[4], core, 0, False) for s in sums]).astype(jnp.bfloat16)
        small_grads, start = [], 0
        for width in widths:
            small_grads.append(small_sums[:, start:start + width])
            start += width
        g1, b1, g2, b2, qb, ob, ub, db = small_grads
        return (y_out[None], d_hidden[None], g1, b1, heads_first(joined(2)), qb, joined(3), ob,
                g2, b2, joined(0), ub, joined(1), db)

    return jax.shard_map(device_step, mesh=mesh,
                         in_specs=(act_spec, act_spec) + (param_spec,) * 12,
                         out_specs=(act_spec, act_spec) + (param_spec,) * 12,
                         check_vma=False)
```

```python
import functools
import jax
import jax.numpy as jnp
import numpy as np
from jax import lax
from jax.experimental import pallas as pl
from jax.experimental.pallas import tpu as pltpu
from jax.sharding import PartitionSpec as P

EPSILON = 1e-5
MESH = pl.DeviceIdType.MESH
ANY = pl.BlockSpec(memory_space=pl.ANY)
IN_VMEM = pl.BlockSpec(memory_space=pltpu.VMEM)
ORDERS = ((2, 1, 0), (1, 0, 2), (0, 2, 1))
VMEM_LIMIT = 60 * 2**20


def flip(index, mask):
    if mask == 1:
        return index + 1 - 2 * lax.rem(index, 2)
    if mask == 3:
        return 3 - index
    return lax.rem(index + 2, 4)


def place():
    node = lax.axis_index('node')
    local = lax.axis_index('local')
    return (node // 4, lax.rem(node, 4), local // 2), lax.rem(local, 2)


def device_at(chip, core):
    return (chip[0] * 4 + chip[1], chip[2] * 2 + core)


def moved(chip, axis, mask):
    return tuple(flip(v, mask) if k == axis else v for k, v in enumerate(chip))


def colour_plan(colour):
    return ORDERS[colour // 2], ((1, 3) if colour % 2 == 0 else (3, 1))


def entry_barrier(chip, core):
    barrier = pltpu.get_barrier_semaphore()
    for axis in range(3):
        for mask in (1, 3):
            pl.semaphore_signal(barrier, inc=1, device_id=device_at(moved(chip, axis, mask), core), device_id_type=MESH)
    pl.semaphore_signal(barrier, inc=1, device_id=device_at(chip, 1 - core), device_id_type=MESH)
    pl.semaphore_wait(barrier, 7)


SHARES = (8, 8, 8, 8, 24, 8, 32, 8)
SIZES = tuple(128 * share for share in SHARES)
OFFSETS = tuple(sum(SIZES[:k]) for k in range(len(SIZES)))
N_VEC = sum(SIZES)


SEQ, WIDTH, HIDDEN, TILE = 384, 1024, 4096, 512
N_TILES = HIDDEN // TILE
PAIR = 128
INV_SQRT2 = 0.7071067811865476
INV_SQRT2PI = 0.3989422804014327
SCALE = 0.125


def dot(a, b):
    return lax.dot_general(a, b, (((1,), (0,)), ((), ())), preferred_element_type=jnp.float32)


def dot_t(a, b):
    return lax.dot_general(a, b, (((1,), (1,)), ((), ())), preferred_element_type=jnp.float32)


def lanes(start, width=PAIR):
    return pl.ds(pl.multiple_of(start, PAIR), width)


def turn(x, cos, sin_a, sin_b):
    return x * cos + pltpu.roll(x, PAIR - 8, 1) * sin_a + pltpu.roll(x, 8, 1) * sin_b


def turn_back(d, cos, sin_a, sin_b):
    return d * cos + pltpu.roll(d * sin_a, 8, 1) + pltpu.roll(d * sin_b, PAIR - 8, 1)


def split_heads(x):
    first = lax.broadcasted_iota(jnp.int32, (PAIR, PAIR), 1) < PAIR // 2
    rows = []
    for j in range(SEQ // PAIR):
        block = x[j * PAIR:(j + 1) * PAIR]
        rows += [jnp.where(first, block, jnp.zeros_like(block)), jnp.where(first, jnp.zeros_like(block), block)]
    return jnp.concatenate(rows, axis=0)


def probabilities(q_block, keys, i):
    scores = dot_t(q_block, keys)
    causal = (lax.broadcasted_iota(jnp.int32, (PAIR, PAIR), 0) >= lax.broadcasted_iota(jnp.int32, (PAIR, PAIR), 1))
    probs = [None] * (2 * i + 2)
    for head in range(2):
        chunks = [scores[:, (2 * j + head) * PAIR:(2 * j + head + 1) * PAIR] * SCALE for j in range(i + 1)]
        chunks[i] = jnp.where(causal, chunks[i], -1e30)
        top = chunks[0]
        for chunk in chunks[1:]:
            top = jnp.maximum(top, chunk)
        top = jnp.max(top, axis=1, keepdims=True)
        chunks = [jnp.exp(chunk - top) for chunk in chunks]
        total = chunks[0]
        for chunk in chunks[1:]:
            total = total + chunk
        inverse = 1.0 / jnp.sum(total, axis=1, keepdims=True)
        for j in range(i + 1):
            probs[2 * j + head] = chunks[j] * inverse
    return probs


def normalised(h):
    center = h - jnp.mean(h, axis=1, keepdims=True)
    inverse = lax.rsqrt(jnp.mean(center * center, axis=1, keepdims=True) + EPSILON)
    return center * inverse, inverse


LN_ROWS = 64


GATHER_PARTS = ((0, 0, 2048, 0), (0, 2048, 2048, 1), (1, 0, 512, 2), (1, 512, 512, 3),
                (2, 0, 2048, 4), (2, 2048, 1024, 5), (3, 0, 1024, 5))


class Gather:
    def __init__(self, chip, core, parts, sems):
        self.chip, self.core, self.parts = chip, core, parts
        self.send_sem, self.recv_sem, self.pass_send, self.pass_recv = sems
        self.copies, self.passed, self.first, self.second = [], {}, {}, {}

    def copy(self, sems, n, slot, where, own, device):
        full, shard, cols, _ = self.parts[n]
        box = full.at[where[0], where[1], where[2], self.core, :, cols]
        copy = pltpu.make_async_remote_copy(
            src_ref=shard if own else box, dst_ref=box, send_sem=sems[0].at[n, slot], recv_sem=sems[1].at[n, slot],
            device_id=device, device_id_type=MESH)
        copy.start()
        self.copies.append(copy)
        return copy

    def reach(self, n, slot, where, own, axis, mask):
        return self.copy((self.send_sem, self.recv_sem), n, slot, where, own, device_at(moved(self.chip, axis, mask), self.core))

    def pass_on(self, n, slot, where, own=False):
        copy = self.copy((self.pass_send, self.pass_recv), n, slot, where, own, device_at(self.chip, 1 - self.core))
        self.passed.setdefault(n, []).append(copy)

    def span(self, n, stage, mask):
        order, masks = colour_plan(self.parts[n][3])
        where = list(self.chip)
        for axis in order[:stage]:
            where[axis] = pl.ds(0, 4)
        where[order[stage]] = flip(self.chip[order[stage]], mask) if mask else self.chip[order[stage]]
        return where, order[stage], masks

    def start(self, ns, stage):
        for turn in range(2):
            for n in ns:
                where, axis, masks = self.span(n, stage, 0)
                self.first[n, turn] = self.reach(n, 3 * stage + turn, where, stage == 0, axis, masks[turn])

    def pass_own(self, ns):
        for n in ns:
            self.pass_on(n, 9, list(self.chip), True)

    def middle(self, ns, stage):
        for n in ns:
            order, masks = colour_plan(self.parts[n][3])
            self.first[n, 0].wait_recv()
            where, axis, masks = self.span(n, stage, masks[0])
            self.second[n] = self.reach(n, 3 * stage + 2, where, False, axis, masks[1])
            self.pass_on(n, 3 * stage, where)

    def late(self, ns, stage):
        for n in ns:
            _, masks = colour_plan(self.parts[n][3])
            self.first[n, 1].wait_recv()
            self.pass_on(n, 3 * stage + 1, self.span(n, stage, masks[1])[0])

    def end(self, ns, stage):
        for n in ns:
            self.second[n].wait_recv()
            self.pass_on(n, 3 * stage + 2, self.span(n, stage, 2)[0])

    def arrived(self, ns):
        for n in ns:
            for copy in self.passed.pop(n):
                copy.wait_recv()


def unpack_vectors(small_v, layer, sel_shard, sel_lane, vec_ref):
    tiles = small_v[...].astype(jnp.float32).reshape((PAIR,) + small_v.shape[-2:])
    held = jnp.where(lax.broadcasted_iota(jnp.int32, tiles.shape, 1) == layer, tiles, 0.0)
    held = jnp.sum(held, axis=1).astype(jnp.bfloat16)
    for k in range(N_VEC // WIDTH):
        cols = slice(k * WIDTH, (k + 1) * WIDTH)
        number = lax.broadcasted_iota(jnp.int32, (PAIR, WIDTH), 0)
        pick = (number == sel_lane[:, cols]).astype(jnp.float32).astype(jnp.bfloat16)
        spread = jnp.where(number == sel_shard[:, cols], dot(held, pick), 0.0)
        vec_ref[layer:layer + 1, cols] = jnp.sum(spread, axis=0, keepdims=True)


def forward_kernel(n_layers, *refs):
    x_ref, cos_ref, sina_ref, sinb_ref, sel_shard, sel_lane = refs[:6]
    shards, refs = refs[6:11], refs[11:]
    fulls, refs = refs[:4 * n_layers + 1], refs[4 * n_layers + 1:]
    vec_ref, refs = refs[0], refs[1:]
    saved, refs = refs[:7 * n_layers], refs[7 * n_layers:]
    (wup_v, wdown_v, wqkv_v, wout_v, small_v, acc, pre_v, n1_v, n2_v, qkv_v, ctx_v, act_v, y_v,
     send_sem, recv_sem, pass_send, pass_recv, own_sem, load_sem, save_sem, share_send, share_recv) = refs
    chip, core = place()
    entry_barrier(chip, core)

    parts = []
    for layer in range(n_layers):
        for arr, col, width, colour in GATHER_PARTS:
            cols = pl.ds(col, width)
            parts.append((fulls[4 * layer + arr], shards[arr].at[layer, :, cols], cols, colour))
    parts.append((fulls[-1], shards[4], pl.ds(0, PAIR), 4))
    gather = Gather(chip, core, parts, (send_sem, recv_sem, pass_send, pass_recv))
    per = len(GATHER_PARTS)
    now = list(range(per)) + [len(parts) - 1]
    nxt = list(range(per, 2 * per))

    own = []
    for layer in range(n_layers):
        for arr in range(4):
            own.append((shards[arr].at[layer], fulls[4 * layer + arr]))
    own.append((shards[4], fulls[-1]))
    own = [pltpu.make_async_copy(src, dst.at[chip[0], chip[1], chip[2], core], own_sem.at[k]) for k, (src, dst) in enumerate(own)]
    gather.start(now, 0)
    for copy in own:
        copy.start()
    gather.start(nxt, 0)
    gather.pass_own(now + nxt)
    for copy in own:
        copy.wait()
    for stage in range(3):
        gather.middle(now, stage)
        if stage:
            gather.start(nxt, stage)
        gather.late(now, stage)
        gather.end(now, stage)
        if stage < 2:
            gather.start(now, stage + 1)
            gather.middle(nxt, stage)
            gather.late(nxt, stage)
            gather.end(nxt, stage)

    saves, shares = [], []

    def save(src, dst):
        copy = pltpu.make_async_copy(src, dst, save_sem.at[len(saves)])
        copy.start()
        saves.append(copy)

    def share(src, dst):
        save(src, dst.at[core])
        copy = pltpu.make_async_remote_copy(
            src_ref=src, dst_ref=dst.at[core], send_sem=share_send.at[len(shares)], recv_sem=share_recv.at[len(shares)],
            device_id=device_at(chip, 1 - core), device_id_type=MESH)
        copy.start()
        shares.append(copy)

    def load(layer, arr, k, width=None):
        full, held = fulls[4 * layer + arr].at[:, :, :, :, :, :], (wup_v, wdown_v, wqkv_v, wout_v)[arr]
        if width:
            cols = pl.ds(k * width, width)
            full, held = full.at[:, :, :, :, :, cols], held.at[:, :, :, :, :, cols]
        copy = pltpu.make_async_copy(full, held, load_sem.at[arr, k])
        copy.start()
        return copy

    def matrix(held, cols=slice(None)):
        return held[:, :, :, :, :, cols].reshape((-1, held.shape[-1] if cols == slice(None) else cols.stop - cols.start))

    def have(layer, arrs):
        gather.arrived([n for n in (now if layer == 0 else nxt) if n in gather.passed
                        and (parts[n][0] is fulls[-1] or any(parts[n][0] is fulls[4 * layer + arr] for arr in arrs))])

    for layer in range(n_layers):
        h_ref = y_v if layer else x_ref
        y_hbm, n1_hbm, n2_hbm, ctx_hbm, act_hbm, qkv_hbm, pre_hbm = saved[7 * layer:7 * layer + 7]
        have(layer, [2])
        loads = [load(layer, 2, k, TILE) for k in range(6)]
        if layer == 0:
            fetch = pltpu.make_async_copy(fulls[-1], small_v, load_sem.at[3, 1])
            fetch.start()
            fetch.wait()
            for k in range(n_layers):
                unpack_vectors(small_v, k, sel_shard, sel_lane, vec_ref)
        else:
            for copy in saves:
                copy.wait()
            for copy in shares:
                copy.wait_send()
            saves.clear()

        def vector(k, cols=slice(None)):
            at = OFFSETS[k]
            return vec_ref[layer:layer + 1, at:at + SIZES[k]] if cols == slice(None) else vec_ref[layer:layer + 1, at + cols.start:at + cols.stop]

        for r in range(SEQ // LN_ROWS):
            rows = slice(r * LN_ROWS, (r + 1) * LN_ROWS)
            scaled, _ = normalised(h_ref[rows, :].astype(jnp.float32))
            n1_v[rows, :] = (scaled * vector(0) + vector(1)).astype(jnp.bfloat16)
            n2_v[rows, :] = (scaled * vector(2) + vector(3)).astype(jnp.bfloat16)
        share(n1_v, n1_hbm)
        share(n2_v, n2_hbm)
        for k in range(6):
            cols = slice(k * TILE, (k + 1) * TILE)
            loads[k].wait()
            x = dot(n1_v[...], matrix(wqkv_v, cols)) + vector(4, cols)
            for c in range(TILE // PAIR):
                block = x[:, c * PAIR:(c + 1) * PAIR]
                if k < 4:
                    block = turn(block, cos_ref[...], sina_ref[...], sinb_ref[...])
                at = k * TILE + c * PAIR
                qkv_v[:, at:at + PAIR] = block.astype(jnp.bfloat16)
        save(qkv_v, qkv_hbm)
        have(layer, [0, 1, 3])
        out_load = load(layer, 3, 0)
        up_loads = [load(layer, 0, t, TILE) for t in range(N_TILES)]
        down_load = load(layer, 1, 0)

        @pl.loop(0, WIDTH // PAIR)
        def _(pair):
            keys = split_heads(qkv_v[:, lanes(WIDTH + pair * PAIR)])
            values = split_heads(qkv_v[:, lanes(2 * WIDTH + pair * PAIR)])
            for i in range(SEQ // PAIR):
                n = (i + 1) * 2 * PAIR
                rows = slice(i * PAIR, (i + 1) * PAIR)
                probs = probabilities(qkv_v[rows, lanes(pair * PAIR)], keys[:n], i)
                probs = jnp.concatenate([p.astype(jnp.bfloat16) for p in probs], axis=1)
                ctx_v[rows, lanes(pair * PAIR)] = dot(probs, values[:n]).astype(jnp.bfloat16)

        share(ctx_v, ctx_hbm)
        if layer == 0:
            gather.middle(nxt, 2)
        out_load.wait()
        for cols in (slice(0, TILE), slice(TILE, WIDTH)):
            acc[:, cols] = (h_ref[:, cols].astype(jnp.float32) + dot(ctx_v[...], matrix(wout_v, cols))
                            + (vector(5, cols) + vector(7, cols)))
        down_load.wait()
        for t in range(N_TILES):
            cols = slice(t * TILE, (t + 1) * TILE)
            up_loads[t].wait()
            pre = dot(n2_v[...], matrix(wup_v, cols)) + vector(6, cols)
            pre_v[t] = pre
            act_v[:, cols] = (0.5 * pre * (1.0 + lax.erf(pre * INV_SQRT2))).astype(jnp.bfloat16)
            acc[...] += dot(act_v[:, cols], wdown_v[t // 2, t % 2 * 2:t % 2 * 2 + 2].reshape((TILE, WIDTH)))
            if layer == 0 and t == N_TILES // 2:
                gather.late(nxt, 2)
        save(pre_v, pre_hbm)
        share(act_v, act_hbm)
        y_v[...] = acc[...].astype(jnp.bfloat16)
        save(y_v, y_hbm)
        if layer == 0:
            gather.end(nxt, 2)
    for copy in saves:
        copy.wait()
    per = len(shares) // n_layers
    for copy in shares:
        copy.wait_recv()
    for copy in shares[-per:]:
        copy.wait_send()
    for copy in gather.copies:
        copy.wait_send()


def forward(x, shards, small_tile, tables, sel_shard, sel_lane):
    n_layers = shards[0].shape[0]
    bf16, f32 = jnp.bfloat16, jnp.float32
    chips = (4, 4, 4, 2)
    full = [(chips + tensor.shape[1:], bf16) for tensor in shards]
    shapes = full * n_layers + [(chips + small_tile.shape, bf16), ((n_layers, N_VEC), f32)]
    kept = [((SEQ, WIDTH), bf16)] + [((2, SEQ, width), bf16) for width in (WIDTH, WIDTH, WIDTH, HIDDEN)]
    kept += [((SEQ, 3 * WIDTH), bf16), ((N_TILES, SEQ, TILE), f32)]
    shapes += kept * n_layers
    n_parts = len(GATHER_PARTS) * n_layers + 1
    dma = pltpu.SemaphoreType.DMA
    scratch = [pltpu.VMEM(*s) for s in full]
    scratch += [pltpu.VMEM(chips + small_tile.shape, bf16), pltpu.VMEM((SEQ, WIDTH), f32), pltpu.VMEM((N_TILES, SEQ, TILE), f32)]
    scratch += [pltpu.VMEM((SEQ, width), bf16) for width in (WIDTH, WIDTH, 3 * WIDTH, WIDTH, HIDDEN, WIDTH)]
    scratch += [dma((n_parts, 9)), dma((n_parts, 9)), dma((n_parts, 10)), dma((n_parts, 10)), dma((4 * n_layers + 1,)),
                dma((4, N_TILES)), dma((7,)), dma((4 * n_layers,)), dma((4 * n_layers,))]
    out_specs = [ANY] * len(shapes)
    out_specs[4 * n_layers + 1] = IN_VMEM
    outs = pl.pallas_call(
        functools.partial(forward_kernel, n_layers),
        out_shape=[jax.ShapeDtypeStruct(s, d) for s, d in shapes],
        in_specs=[IN_VMEM] * 11,
        out_specs=out_specs,
        scratch_shapes=scratch,
        compiler_params=pltpu.CompilerParams(collective_id=0, has_side_effects=True, vmem_limit_bytes=VMEM_LIMIT),
        cost_estimate=pl.CostEstimate(flops=20 * 10**9, bytes_accessed=10**8, transcendentals=10**7),
        name='forward_layers',
    )(x, *tables, sel_shard, sel_lane, *shards, small_tile)
    weights = [[t.reshape((-1, t.shape[-1])) for t in outs[4 * k:4 * k + 4]] for k in range(n_layers)]
    outs = outs[4 * n_layers + 1:]
    return weights, outs[0], [outs[1 + 7 * k:8 + 7 * k] for k in range(n_layers)]


REDUCE_PARTS = ((0, 0, 1024, 0), (0, 1024, 1024, 1), (1, 0, 256, 2), (1, 256, 256, 3),
                (2, 0, 1024, 4), (2, 1024, 512, 5), (3, 0, 512, 5), (4, 0, 128, 4))


def reduce_kernel(*refs):
    grads, sums, refs = refs[:5], refs[5:10], refs[10:]
    n_parts = len(REDUCE_PARTS)
    kept, refs = refs[:n_parts], refs[n_parts:]
    came, refs = [refs[6 * n:6 * n + 6] for n in range(n_parts)], refs[6 * n_parts:]
    send_sem, recv_sem, load_sem, tile = refs
    chip, core = place()
    entry_barrier(chip, core)
    copies = []
    started = {}

    def reach(n, slot, src, dst, target, to_core=core):
        copy = pltpu.make_async_remote_copy(
            src_ref=src, dst_ref=dst, send_sem=send_sem.at[n, slot], recv_sem=recv_sem.at[n, slot],
            device_id=device_at(target, to_core), device_id_type=MESH)
        copy.start()
        copies.append(copy)
        started[n, slot] = copy

    def at_axis(ref, axis, value, n_axes, lead=()):
        every = [pl.ds(0, 4)] * n_axes
        every[axis] = value
        return ref.at[tuple(lead) + tuple(every)]

    def add_into(dst, src, n_axes):
        if n_axes == 0:
            dst[...] += src[...]
            return
        rows, cols = dst.shape[-2:]

        @pl.loop(0, 4 ** n_axes)
        def _(k):
            index = (k,) if n_axes == 1 else (k // 4, lax.rem(k, 4))
            dst[index] += src[index]

    plans = [colour_plan(part[3]) for part in REDUCE_PARTS]

    loads = {}
    for slot in (1, 0):
        for n, (arr, col, width, colour) in enumerate(REDUCE_PARTS):
            order, (one, two) = plans[n]
            axis = order[0]
            mine = chip[axis]
            target = moved(chip, axis, one)
            theirs = flip(mine, one) if slot == 0 else flip(mine, 2)
            cols = grads[arr].at[:, :, :, :, pl.ds(col, width)]
            reach(n, slot, at_axis(cols, axis, theirs, 3), came[n][0].at[slot], target)
    for slot in (1, 0):
        for n, (arr, col, width, colour) in enumerate(REDUCE_PARTS):
            order, (one, two) = plans[n]
            axis = order[0]
            keep = chip[axis] if slot == 0 else flip(chip[axis], two)
            cols = grads[arr].at[:, :, :, :, pl.ds(col, width)]
            loads[n, slot] = pltpu.make_async_copy(at_axis(cols, axis, keep, 3), kept[n].at[slot], load_sem.at[n, slot])
            loads[n, slot].start()

    def remaining(order, stage):
        return [axis for axis in range(3) if axis not in order[:stage]]

    for n in range(n_parts):
        order, (one, two) = plans[n]
        loads[n, 1].wait()
        started[n, 1].wait_recv()
        add_into(kept[n].at[1], came[n][0].at[1], 2)
        reach(n, 2, kept[n].at[1], came[n][1], moved(chip, order[0], two))
    for n in range(n_parts):
        loads[n, 0].wait()
        started[n, 0].wait_recv()
        add_into(kept[n].at[0], came[n][0].at[0], 2)

    def held(n, stage):
        order, _ = plans[n]
        axes = remaining(order, 1)
        ref = kept[n].at[0]
        if stage == 1:
            return ref, axes.index(order[1]), 2
        fixed = axes.index(order[1])
        return at_axis(ref, fixed, chip[order[1]], 2), 0, 1

    for stage in (1, 2):
        base = 3 * stage
        for n in range(n_parts):
            order, (one, two) = plans[n]
            ref, spot, n_axes = held(n, stage)
            mine = chip[order[stage]]
            started[n, base - 1].wait_recv()
            arrived = came[n][2 * stage - 1]
            for slot in (1, 0):
                theirs = flip(mine, one) if slot == 0 else flip(mine, 2)
                view = at_axis(ref, spot, theirs, n_axes)
                add_into(view, at_axis(arrived, spot, theirs, n_axes), n_axes - 1)
                reach(n, base + slot, view, came[n][2 * stage].at[slot], moved(chip, order[stage], one))
            for keep in (flip(mine, two), mine):
                add_into(at_axis(ref, spot, keep, n_axes), at_axis(arrived, spot, keep, n_axes), n_axes - 1)
        for n in range(n_parts):
            order, (one, two) = plans[n]
            ref, spot, n_axes = held(n, stage)
            mine = chip[order[stage]]
            started[n, base + 1].wait_recv()
            view = at_axis(ref, spot, flip(mine, two), n_axes)
            add_into(view, came[n][2 * stage].at[1], n_axes - 1)
            reach(n, base + 2, view, came[n][2 * stage + 1], moved(chip, order[stage], two))
        for n in range(n_parts):
            order, _ = plans[n]
            ref, spot, n_axes = held(n, stage)
            started[n, base].wait_recv()
            add_into(at_axis(ref, spot, chip[order[stage]], n_axes), came[n][2 * stage].at[0], n_axes - 1)

    for n, (arr, col, width, colour) in enumerate(REDUCE_PARTS):
        order, _ = plans[n]
        ref, _, _ = held(n, 2)
        box = ref.at[chip[order[2]]]
        started[n, 8].wait_recv()
        add_into(box, came[n][5], 0)
        if arr == 4:
            reach(n, 9, box, tile, chip, 1 - core)
            continue
        rows = box.shape[0] // 2
        theirs = box.at[pl.ds(pl.multiple_of((1 - core) * rows, rows), rows)]
        reach(n, 9, theirs, sums[arr].at[core, :, pl.ds(col, width)], chip, 1 - core)
    for n, (arr, col, width, colour) in enumerate(REDUCE_PARTS):
        order, _ = plans[n]
        ref, _, _ = held(n, 2)
        box = ref.at[chip[order[2]]]
        started[n, 9].wait_recv()
        if arr == 4:
            sums[4][...] = box[...] + tile[...]
            continue
        rows = box.shape[0] // 2
        sums[arr][core, :, pl.ds(col, width)] = box[pl.ds(pl.multiple_of(core * rows, rows), rows), :]
    for copy in copies:
        copy.wait_send()


def reduce_all(up, down, qkv, out, small):
    grads = [tensor.reshape((4, 4, 4, -1, tensor.shape[-1])) for tensor in (up, down, qkv, out, small)]
    shapes = [jax.ShapeDtypeStruct((2, g.shape[3] // 2, g.shape[4]), jnp.float32) for g in grads[:4]]
    shapes.append(jax.ShapeDtypeStruct((8, 128), jnp.float32))
    kept, came = [], []
    for arr, col, width, colour in REDUCE_PARTS:
        block = (grads[arr].shape[3], width)
        kept.append(pltpu.VMEM((2, 4, 4) + block, jnp.float32))
        for lead in ((2, 4, 4), (4, 4), (2, 4), (4,), (2,), ()):
            came.append(pltpu.VMEM(lead + block, jnp.float32))
    n_parts = len(REDUCE_PARTS)
    return pl.pallas_call(
        reduce_kernel,
        out_shape=shapes,
        in_specs=[ANY] * 5,
        out_specs=[IN_VMEM] * 5,
        scratch_shapes=kept + came + [pltpu.SemaphoreType.DMA((n_parts, 10)), pltpu.SemaphoreType.DMA((n_parts, 10)),
                                      pltpu.SemaphoreType.DMA((n_parts, 2)), pltpu.VMEM((8, 128), jnp.float32)],
        compiler_params=pltpu.CompilerParams(collective_id=1, has_side_effects=True, vmem_limit_bytes=VMEM_LIMIT),
        name='reduce_gradients',
    )(*grads)


def backward_kernel(dout_ref, h_ref, g1_ref, g2_ref, cos_ref, sina_ref, sinb_ref, qkv_ref, pre_hbm, wqkv, wout, wup, wdown,
                    dh_ref, dpre_ref, dqkv_ref, dg1_ref, db1_ref, dg2_ref, db2_ref, dqkvb_ref, dupb_ref, dsum_ref,
                    wqkv_v, wout_v, wup_v, wdown_v, pre_v, dn2, dn1, dctx, dk_acc, dv_acc, tile_sems, wout_sem, qkv_sems):
    def tile_loads(t, slot):
        start = pl.multiple_of(t * TILE, TILE)
        return (pltpu.make_async_copy(wdown.at[pl.ds(start, TILE)], wdown_v.at[slot], tile_sems.at[slot, 0]),
                pltpu.make_async_copy(pre_hbm.at[t], pre_v.at[slot], tile_sems.at[slot, 1]),
                pltpu.make_async_copy(wup.at[:, pl.ds(start, TILE)], wup_v.at[slot], tile_sems.at[slot, 2]))

    def qkv_load(k):
        return pltpu.make_async_copy(wqkv.at[:, pl.ds(k * WIDTH, WIDTH)], wqkv_v.at[k % 2], qkv_sems.at[k % 2])

    for t in range(2):
        for load in tile_loads(t, t):
            load.start()
    load_out = pltpu.make_async_copy(wout, wout_v, wout_sem)
    load_out.start()
    for k in range(2):
        qkv_load(k).start()
    dsum_ref[...] = jnp.sum(dout_ref[...].astype(jnp.float32), axis=0, keepdims=True)
    dn2[...] = jnp.zeros_like(dn2)

    @pl.loop(0, N_TILES)
    def _(t):
        slot = lax.rem(t, 2)
        cols = pl.ds(pl.multiple_of(t * TILE, TILE), TILE)
        for load in tile_loads(t, slot):
            load.wait()
        d_act = dot_t(dout_ref[...], wdown_v[slot]).astype(jnp.bfloat16).astype(jnp.float32)
        pre = pre_v[slot]
        slope = 0.5 * (1.0 + lax.erf(pre * INV_SQRT2)) + pre * (INV_SQRT2PI * jnp.exp(-0.5 * pre * pre))
        d_pre = d_act * slope
        dupb_ref[:, cols] = jnp.sum(d_pre, axis=0, keepdims=True)
        d_pre = d_pre.astype(jnp.bfloat16)
        dpre_ref[:, cols] = d_pre
        dn2[...] += dot_t(d_pre, wup_v[slot])

        @pl.when(t + 2 < N_TILES)
        def _():
            for load in tile_loads(t + 2, slot):
                load.start()

    load_out.wait()
    for k in range(2):
        rows = slice(k * 512, (k + 1) * 512)
        dctx[:, rows] = dot_t(dout_ref[...], wout_v[rows, :]).astype(jnp.bfloat16)

    @pl.loop(0, WIDTH // PAIR)
    def _(pair):
        at = lanes(pair * PAIR)
        keys = split_heads(qkv_ref[:, lanes(WIDTH + pair * PAIR)])
        values = split_heads(qkv_ref[:, lanes(2 * WIDTH + pair * PAIR)])
        q_t = qkv_ref[:, at].T
        dc_t = dctx[:, at].T
        dbq = jnp.zeros((1, PAIR), jnp.float32)
        for i in range(SEQ // PAIR):
            n = (i + 1) * 2 * PAIR
            rows = slice(i * PAIR, (i + 1) * PAIR)
            probs = probabilities(qkv_ref[rows, at], keys[:n], i)
            d_all = dot_t(dctx[rows, at], values[:n]).astype(jnp.bfloat16).astype(jnp.float32)
            d_probs = [d_all[:, j * PAIR:(j + 1) * PAIR] for j in range(2 * i + 2)]
            d_scores = [None] * (2 * i + 2)
            for head in range(2):
                mean = probs[head] * d_probs[head]
                for j in range(1, i + 1):
                    mean = mean + probs[2 * j + head] * d_probs[2 * j + head]
                mean = jnp.sum(mean, axis=1, keepdims=True)
                for j in range(head, 2 * i + 2, 2):
                    d_scores[j] = (probs[j] * (d_probs[j] - mean) * SCALE).astype(jnp.bfloat16)
            d_scores = jnp.concatenate(d_scores, axis=1)
            probs = jnp.concatenate([p.astype(jnp.bfloat16) for p in probs], axis=1)
            d_query = dot(d_scores, keys[:n]).astype(jnp.bfloat16).astype(jnp.float32)
            d_query = turn_back(d_query, cos_ref[rows, :], sina_ref[rows, :], sinb_ref[rows, :])
            dbq = dbq + jnp.sum(d_query, axis=0, keepdims=True)
            dqkv_ref[rows, at] = d_query.astype(jnp.bfloat16)
            d_keys = dot(q_t[:, rows], d_scores)
            d_values = dot(dc_t[:, rows], probs)
            old = 2 * i * PAIR
            if i:
                dk_acc[:, :old] += d_keys[:, :old]
                dv_acc[:, :old] += d_values[:, :old]
            dk_acc[:, old:n] = d_keys[:, old:]
            dv_acc[:, old:n] = d_values[:, old:]
        dqkvb_ref[:, at] = dbq
        first = lax.broadcasted_iota(jnp.int32, (PAIR, PAIR), 0) < PAIR // 2
        dbk = jnp.zeros((1, PAIR), jnp.float32)
        dbv = jnp.zeros((1, PAIR), jnp.float32)
        for j in range(SEQ // PAIR):
            rows = slice(j * PAIR, (j + 1) * PAIR)
            left, right = slice(2 * j * PAIR, (2 * j + 1) * PAIR), slice((2 * j + 1) * PAIR, (2 * j + 2) * PAIR)
            d_key = jnp.where(first, dk_acc[:, left], dk_acc[:, right]).T.astype(jnp.bfloat16).astype(jnp.float32)
            d_key = turn_back(d_key, cos_ref[rows, :], sina_ref[rows, :], sinb_ref[rows, :])
            dbk = dbk + jnp.sum(d_key, axis=0, keepdims=True)
            dqkv_ref[rows, lanes(WIDTH + pair * PAIR)] = d_key.astype(jnp.bfloat16)
            d_value = jnp.where(first, dv_acc[:, left], dv_acc[:, right]).T.astype(jnp.bfloat16)
            dbv = dbv + jnp.sum(d_value.astype(jnp.float32), axis=0, keepdims=True)
            dqkv_ref[rows, lanes(2 * WIDTH + pair * PAIR)] = d_value
        dqkvb_ref[:, lanes(WIDTH + pair * PAIR)] = dbk
        dqkvb_ref[:, lanes(2 * WIDTH + pair * PAIR)] = dbv

    for k in range(3):
        qkv_load(k).wait()
        part = dot_t(dqkv_ref[:, k * WIDTH:(k + 1) * WIDTH], wqkv_v[k % 2])
        if k == 0:
            dn1[...] = part
            qkv_load(2).start()
        else:
            dn1[...] += part

    for ref in (dg1_ref, db1_ref, dg2_ref, db2_ref):
        ref[...] = jnp.zeros_like(ref)

    @pl.loop(0, SEQ // LN_ROWS)
    def _(r):
        rows = pl.ds(pl.multiple_of(r * LN_ROWS, LN_ROWS), LN_ROWS)
        scaled, inverse = normalised(h_ref[rows, :].astype(jnp.float32))
        d1 = dn1[rows, :].astype(jnp.bfloat16).astype(jnp.float32)
        d2 = dn2[rows, :].astype(jnp.bfloat16).astype(jnp.float32)
        dg1_ref[...] += jnp.sum(d1 * scaled, axis=0, keepdims=True)
        db1_ref[...] += jnp.sum(d1, axis=0, keepdims=True)
        dg2_ref[...] += jnp.sum(d2 * scaled, axis=0, keepdims=True)
        db2_ref[...] += jnp.sum(d2, axis=0, keepdims=True)
        d_scaled = d1 * g1_ref[...] + d2 * g2_ref[...]
        d_h = inverse * (d_scaled - jnp.mean(d_scaled, axis=1, keepdims=True)
                         - scaled * jnp.mean(d_scaled * scaled, axis=1, keepdims=True))
        dh_ref[rows, :] = (dout_ref[rows, :].astype(jnp.float32) + d_h).astype(jnp.bfloat16)


def backward_layer(d_out, hidden, weights, vectors, tables, qkv, pre):
    up_weight, down_weight, qkv_weight, out_weight = weights
    g1, g2 = vectors[0].reshape(1, -1), vectors[2].reshape(1, -1)
    bf16, f32 = jnp.bfloat16, jnp.float32
    shapes = [((SEQ, WIDTH), bf16), ((SEQ, HIDDEN), bf16), ((SEQ, 3 * WIDTH), bf16)] + [((1, WIDTH), f32)] * 4
    shapes += [((1, 3 * WIDTH), f32), ((1, HIDDEN), f32), ((1, WIDTH), f32)]
    return pl.pallas_call(
        backward_kernel,
        out_shape=[jax.ShapeDtypeStruct(s, d) for s, d in shapes],
        in_specs=[IN_VMEM] * 8 + [ANY] * 5,
        out_specs=[IN_VMEM] * 10,
        scratch_shapes=[pltpu.VMEM((2, WIDTH, WIDTH), bf16), pltpu.VMEM((WIDTH, WIDTH), bf16), pltpu.VMEM((2, WIDTH, TILE), bf16),
                        pltpu.VMEM((2, TILE, WIDTH), bf16), pltpu.VMEM((2, SEQ, TILE), f32), pltpu.VMEM((SEQ, WIDTH), f32),
                        pltpu.VMEM((SEQ, WIDTH), f32), pltpu.VMEM((SEQ, WIDTH), bf16), pltpu.VMEM((PAIR, 2 * SEQ), f32),
                        pltpu.VMEM((PAIR, 2 * SEQ), f32), pltpu.SemaphoreType.DMA((2, 3)), pltpu.SemaphoreType.DMA,
                        pltpu.SemaphoreType.DMA((2,))],
        compiler_params=pltpu.CompilerParams(vmem_limit_bytes=VMEM_LIMIT),
        cost_estimate=pl.CostEstimate(flops=13 * 10**9, bytes_accessed=45 * 10**6, transcendentals=6 * 10**6),
        name='backward_layer',
    )(d_out, hidden, g1, g2, *tables, qkv, pre, qkv_weight, out_weight, up_weight, down_weight)


def product(einsum_form, first_op, second_op):
    return jnp.einsum(einsum_form, first_op, second_op, preferred_element_type=jnp.float32)


def rope_tables(seq_len, head_dim):
    rot_dim = head_dim // 4
    inv_freq = 1.0 / (10000.0 ** (jnp.arange(0, rot_dim, 2, dtype=jnp.float32) / rot_dim))
    angles = jnp.arange(seq_len, dtype=jnp.float32)[:, None] * inv_freq[None, :]
    cos, sin = jnp.cos(angles), jnp.sin(angles)
    zero = jnp.zeros_like(sin)
    rest = jnp.zeros((seq_len, head_dim - rot_dim), jnp.float32)
    tables = ([cos, cos, rest + 1.0], [-sin, zero, rest], [zero, sin, rest])
    return [jnp.tile(jnp.concatenate(table, axis=1), (1, 2)) for table in tables]


def heads_last(tensor):
    lead = tensor.shape[:-2]
    return tensor.reshape(lead + (16, 3, 64)).swapaxes(-3, -2).reshape(lead + (3072,))


def heads_first(tensor):
    lead = tensor.shape[:-1]
    return tensor.reshape(lead + (3, 16, 64)).swapaxes(-3, -2).reshape(lead + (16, 192))


def vector_places():
    shard, lane, start = [], [], 0
    for k, (share, size) in enumerate(zip(SHARES, SIZES)):
        place_of = np.arange(size)
        if k == 4:
            place_of = heads_last(place_of.reshape(16, 192))
        shard.append(place_of // share)
        lane.append(start + place_of % share)
        start += share
    return [jnp.asarray(np.concatenate(part)[None].astype(np.int32)) for part in (shard, lane)]


def pack_vectors(vectors):
    packed = jnp.concatenate(vectors, axis=-1)
    return jnp.pad(packed, ((0, 0), (0, 128 - packed.shape[-1])))


def solution(mesh):
    shard_axes = ('node', 'local')
    act_spec = P(shard_axes)
    param_spec = P(None, shard_axes)
    pairs = [(i, i + 1 - 2 * (i % 2)) for i in range(mesh.shape['local'])]

    def with_partner(tensor):
        return lax.ppermute(tensor, 'local', pairs)

    def device_step(x, y_cot, ln1_gain, ln1_bias, qkv_weight, qkv_bias, out_weight, out_bias,
                    ln2_gain, ln2_bias, up_weight, up_bias, down_weight, down_bias):
        num_layers = ln1_gain.shape[0]
        core = lax.rem(lax.axis_index('local'), 2)
        tables = rope_tables(x.shape[1], qkv_weight.shape[3] // 3)

        def columns(tensor):
            width = tensor.shape[1] // 2
            mine = lax.dynamic_slice_in_dim(tensor, core * width, width, 1)
            other = with_partner(lax.dynamic_slice_in_dim(tensor, (1 - core) * width, width, 1))
            return jnp.concatenate([jnp.where(core == 0, mine, other), jnp.where(core == 0, other, mine)], axis=0)

        small = (ln1_gain, ln1_bias, ln2_gain, ln2_bias, qkv_bias, out_bias, up_bias, down_bias)
        small_tile = jnp.pad(pack_vectors(small), ((0, 8 - num_layers), (0, 0)))
        weights, vectors, states = forward(x[0], (up_weight, down_weight, heads_last(qkv_weight), out_weight), small_tile,
                                           tables, *vector_places())
        inputs = [x[0]] + [state[0] for state in states]
        d_hidden = y_cot[0]
        sums = [None] * num_layers
        for layer in reversed(range(num_layers)):
            _, normed_attn, normed_mlp, context, act, qkv, pre = states[layer]
            d_out = d_hidden
            gains = [vectors[layer, OFFSETS[k]:OFFSETS[k] + SIZES[k]] for k in range(4)]
            d_hidden, d_pre, d_qkv, dg1, db1, dg2, db2, dqkvb, dupb, dsum = backward_layer(
                d_out, inputs[layer], weights[layer], gains, tables, qkv, pre)
            d_out_cols = columns(d_out)

            def rows(tensor):
                return tensor.reshape((-1, tensor.shape[-1]))

            down_grad = product('sd,se->de', rows(act), d_out_cols)
            out_grad = product('sd,se->de', rows(context), d_out_cols)
            up_grad = product('sd,se->de', rows(normed_mlp), columns(d_pre))
            qkv_grad = product('sd,se->de', rows(normed_attn), columns(d_qkv))
            vector_grads = (dg1, db1, dg2, db2, heads_first(dqkvb), dsum, dupb, dsum)
            packed = pack_vectors([grad.reshape(128, -1) for grad in vector_grads])
            tiles = jnp.pad(packed.reshape(64, 2, 128), ((0, 0), (0, 6), (0, 0)))
            sums[layer] = reduce_all(up_grad, down_grad, qkv_grad, out_grad, tiles)

        def joined(arr):
            return jnp.stack([jnp.concatenate([s[arr][0], s[arr][1]], axis=1) for s in sums]).astype(jnp.bfloat16)

        small_sums = jnp.stack([lax.dynamic_index_in_dim(s[4], core, 0, False) for s in sums]).astype(jnp.bfloat16)
        small_grads, start = [], 0
        for width in SHARES:
            small_grads.append(small_sums[:, start:start + width])
            start += width
        g1, b1, g2, b2, qb, ob, ub, db = small_grads
        return (inputs[-1][None], d_hidden[None], g1, b1, heads_first(joined(2)), qb, joined(3), ob,
                g2, b2, joined(0), ub, joined(1), db)

    return jax.shard_map(device_step, mesh=mesh,
                         in_specs=(act_spec, act_spec) + (param_spec,) * 12,
                         out_specs=(act_spec, act_spec) + (param_spec,) * 12,
                         check_vma=False)
```

```python
import functools
import jax
import jax.numpy as jnp
import numpy as np
from jax import lax
from jax.experimental import pallas as pl
from jax.experimental.pallas import tpu as pltpu
from jax.sharding import PartitionSpec as P

EPSILON = 1e-5
MESH = pl.DeviceIdType.MESH
ANY = pl.BlockSpec(memory_space=pl.ANY)
IN_VMEM = pl.BlockSpec(memory_space=pltpu.VMEM)
ORDERS = ((2, 1, 0), (1, 0, 2), (0, 2, 1))
VMEM_LIMIT = 67 * 10**6


class Chip:
    def __init__(self, where):
        self.where = where
        self.near = [(v, v + 1 - 2 * lax.rem(v, 2), lax.rem(v + 2, 4), 3 - v) for v in where]
        base = (where[0] * 4 + where[1], where[2] * 2)
        steps = ((4, 0), (1, 0), (0, 2))
        self.beside = [[tuple(b + (near[mask] - near[0]) * s if s and mask else b for b, s in zip(base, step))
                        for mask in range(4)] for near, step in zip(self.near, steps)]

    def device(self, axis, mask, core):
        node, local = self.beside[axis][mask]
        return (node, local + core)


def place():
    node = lax.axis_index('node')
    local = lax.axis_index('local')
    return Chip((lax.div(node, 4), lax.rem(node, 4), lax.div(local, 2))), lax.rem(local, 2)


def colour_plan(colour):
    return ORDERS[colour // 2], ((1, 3) if colour % 2 == 0 else (3, 1))


def signal_partners(semaphore, chip, core):
    for axis in range(3):
        for mask in (1, 3):
            pl.semaphore_signal(semaphore, inc=1, device_id=chip.device(axis, mask, core), device_id_type=MESH)
    pl.semaphore_signal(semaphore, inc=1, device_id=chip.device(0, 0, 1 - core), device_id_type=MESH)


def entry_barrier(chip, core):
    barrier = pltpu.get_barrier_semaphore()
    signal_partners(barrier, chip, core)
    pl.semaphore_wait(barrier, 7)


SHARES = (8, 8, 8, 8, 24, 8, 32, 8)
SIZES = tuple(128 * share for share in SHARES)
OFFSETS = tuple(sum(SIZES[:k]) for k in range(len(SIZES)))
N_VEC = sum(SIZES)


SEQ, WIDTH, HIDDEN, TILE = 384, 1024, 4096, 512
N_TILES = HIDDEN // TILE
PAIR = 128
INV_SQRT2 = 0.7071067811865476
INV_SQRT2PI = 0.3989422804014327
SCALE = 0.125


def dot(a, b):
    return lax.dot_general(a, b, (((1,), (0,)), ((), ())), preferred_element_type=jnp.float32)


def dot_t(a, b):
    return lax.dot_general(a, b, (((1,), (1,)), ((), ())), preferred_element_type=jnp.float32)


def lanes(start, width=PAIR):
    return pl.ds(pl.multiple_of(start, PAIR), width)


def turn(x, cos, sin_a, sin_b):
    return x * cos + pltpu.roll(x, PAIR - 8, 1) * sin_a + pltpu.roll(x, 8, 1) * sin_b


def turn_back(d, cos, sin_a, sin_b):
    return d * cos + pltpu.roll(d * sin_a, 8, 1) + pltpu.roll(d * sin_b, PAIR - 8, 1)


def split_heads(x):
    first = lax.broadcasted_iota(jnp.int32, (PAIR, PAIR), 1) < PAIR // 2
    rows = []
    for j in range(SEQ // PAIR):
        block = x[j * PAIR:(j + 1) * PAIR]
        rows += [jnp.where(first, block, jnp.zeros_like(block)), jnp.where(first, jnp.zeros_like(block), block)]
    return jnp.concatenate(rows, axis=0)


def probabilities(q_block, keys, i):
    scores = dot_t(q_block, keys)
    causal = (lax.broadcasted_iota(jnp.int32, (PAIR, PAIR), 0) >= lax.broadcasted_iota(jnp.int32, (PAIR, PAIR), 1))
    probs = [None] * (2 * i + 2)
    for head in range(2):
        chunks = [scores[:, (2 * j + head) * PAIR:(2 * j + head + 1) * PAIR] * SCALE for j in range(i + 1)]
        chunks[i] = jnp.where(causal, chunks[i], -1e30)
        top = chunks[0]
        for chunk in chunks[1:]:
            top = jnp.maximum(top, chunk)
        top = jnp.max(top, axis=1, keepdims=True)
        chunks = [jnp.exp(chunk - top) for chunk in chunks]
        total = chunks[0]
        for chunk in chunks[1:]:
            total = total + chunk
        inverse = 1.0 / jnp.sum(total, axis=1, keepdims=True)
        for j in range(i + 1):
            probs[2 * j + head] = chunks[j] * inverse
    return probs


def normalised(h):
    center = h - jnp.mean(h, axis=1, keepdims=True)
    inverse = lax.rsqrt(jnp.mean(center * center, axis=1, keepdims=True) + EPSILON)
    return center * inverse, inverse


LN_ROWS = 64


GATHER_PARTS = ((0, 0, 2048, 0), (0, 2048, 2048, 1), (1, 0, 512, 2), (1, 512, 512, 3),
                (2, 0, 2048, 4), (2, 2048, 1024, 5), (3, 0, 1024, 5))


class Gather:
    def __init__(self, chip, core, parts, sems):
        self.chip, self.core, self.parts = chip, core, parts
        self.send_sem, self.recv_sem, self.pass_send, self.pass_recv = sems
        self.copies, self.passed, self.first, self.second = [], {}, {}, {}

    def copy(self, sems, n, slot, where, own, device):
        full, shard, cols, _ = self.parts[n]
        box = full.at[where[0], where[1], where[2], self.core, :, cols]
        copy = pltpu.make_async_remote_copy(
            src_ref=shard if own else box, dst_ref=box, send_sem=sems[0].at[n, slot], recv_sem=sems[1].at[n, slot],
            device_id=device, device_id_type=MESH)
        copy.start()
        self.copies.append(copy)
        return copy

    def reach(self, n, slot, where, own, axis, mask):
        return self.copy((self.send_sem, self.recv_sem), n, slot, where, own, self.chip.device(axis, mask, self.core))

    def pass_on(self, n, slot, where, own=False):
        copy = self.copy((self.pass_send, self.pass_recv), n, slot, where, own, self.chip.device(0, 0, 1 - self.core))
        self.passed.setdefault(n, []).append(copy)

    def span(self, n, stage, mask):
        order, masks = colour_plan(self.parts[n][3])
        where = list(self.chip.where)
        for axis in order[:stage]:
            where[axis] = pl.ds(0, 4)
        where[order[stage]] = self.chip.near[order[stage]][mask]
        return where, order[stage], masks

    def start(self, ns, stage):
        for turn in range(2):
            for n in ns:
                where, axis, masks = self.span(n, stage, 0)
                self.first[n, turn] = self.reach(n, 3 * stage + turn, where, stage == 0, axis, masks[turn])

    def pass_own(self, ns):
        for n in ns:
            self.pass_on(n, 9, self.chip.where, True)

    def middle(self, ns, stage):
        for n in ns:
            order, masks = colour_plan(self.parts[n][3])
            self.first[n, 0].wait_recv()
            where, axis, masks = self.span(n, stage, masks[0])
            self.second[n] = self.reach(n, 3 * stage + 2, where, False, axis, masks[1])
            self.pass_on(n, 3 * stage, where)

    def late(self, ns, stage):
        for n in ns:
            _, masks = colour_plan(self.parts[n][3])
            self.first[n, 1].wait_recv()
            self.pass_on(n, 3 * stage + 1, self.span(n, stage, masks[1])[0])

    def end(self, ns, stage):
        for n in ns:
            self.second[n].wait_recv()
            self.pass_on(n, 3 * stage + 2, self.span(n, stage, 2)[0])

    def arrived(self, ns):
        for n in ns:
            for copy in self.passed.pop(n):
                copy.wait_recv()


def unpack_vectors(small_v, layer, sel_shard, sel_lane, vec_ref):
    tiles = small_v[...].astype(jnp.float32).reshape((PAIR,) + small_v.shape[-2:])
    held = jnp.where(lax.broadcasted_iota(jnp.int32, tiles.shape, 1) == layer, tiles, 0.0)
    held = jnp.sum(held, axis=1).astype(jnp.bfloat16)
    for k in range(N_VEC // WIDTH):
        cols = slice(k * WIDTH, (k + 1) * WIDTH)
        number = lax.broadcasted_iota(jnp.int32, (PAIR, WIDTH), 0)
        pick = (number == sel_lane[:, cols]).astype(jnp.float32).astype(jnp.bfloat16)
        spread = jnp.where(number == sel_shard[:, cols], dot(held, pick), 0.0)
        vec_ref[layer:layer + 1, cols] = jnp.sum(spread, axis=0, keepdims=True)


def forward_kernel(n_layers, *refs):
    x_ref, cos_ref, sina_ref, sinb_ref, sel_shard, sel_lane = refs[:6]
    shards, refs = refs[6:11], refs[11:]
    fulls, refs = refs[:4 * n_layers + 1], refs[4 * n_layers + 1:]
    vec_ref, refs = refs[0], refs[1:]
    saved, refs = refs[:7 * n_layers], refs[7 * n_layers:]
    (wup_v, wdown_v, wqkv_v, wout_v, small_v, acc, pre_v, n1_v, n2_v, qkv_v, ctx_v, act_v, y_v,
     send_sem, recv_sem, pass_send, pass_recv, own_sem, load_sem, save_sem, share_send, share_recv) = refs
    chip, core = place()
    entry_barrier(chip, core)

    parts = []
    for layer in range(n_layers):
        for arr, col, width, colour in GATHER_PARTS:
            cols = pl.ds(col, width)
            parts.append((fulls[4 * layer + arr], shards[arr].at[layer, :, cols], cols, colour))
    parts.append((fulls[-1], shards[4], pl.ds(0, PAIR), 4))
    gather = Gather(chip, core, parts, (send_sem, recv_sem, pass_send, pass_recv))
    per = len(GATHER_PARTS)
    now = list(range(per)) + [len(parts) - 1]
    nxt = list(range(per, 2 * per))

    own = []
    for layer in range(n_layers):
        for arr in range(4):
            own.append((shards[arr].at[layer], fulls[4 * layer + arr]))
    own.append((shards[4], fulls[-1]))
    own = [pltpu.make_async_copy(src, dst.at[*chip.where, core], own_sem.at[k]) for k, (src, dst) in enumerate(own)]
    gather.start(now, 0)
    for copy in own:
        copy.start()
    gather.start(nxt, 0)
    gather.pass_own(now + nxt)
    for copy in own:
        copy.wait()
    for stage in range(3):
        gather.middle(now, stage)
        if stage:
            gather.start(nxt, stage)
        gather.late(now, stage)
        gather.end(now, stage)
        if stage < 2:
            gather.start(now, stage + 1)
            gather.middle(nxt, stage)
            gather.late(nxt, stage)
            gather.end(nxt, stage)

    saves, shares = [], []

    def save(src, dst):
        copy = pltpu.make_async_copy(src, dst, save_sem.at[len(saves)])
        copy.start()
        saves.append(copy)

    def share(src, dst):
        save(src, dst.at[core])
        copy = pltpu.make_async_remote_copy(
            src_ref=src, dst_ref=dst.at[core], send_sem=share_send.at[len(shares)], recv_sem=share_recv.at[len(shares)],
            device_id=chip.device(0, 0, 1 - core), device_id_type=MESH)
        copy.start()
        shares.append(copy)

    def load(layer, arr, k, width=None):
        full, held = fulls[4 * layer + arr].at[:, :, :, :, :, :], (wup_v, wdown_v, wqkv_v, wout_v)[arr]
        if width:
            cols = pl.ds(k * width, width)
            full, held = full.at[:, :, :, :, :, cols], held.at[:, :, :, :, :, cols]
        copy = pltpu.make_async_copy(full, held, load_sem.at[arr, k])
        copy.start()
        return copy

    def matrix(held, cols=slice(None)):
        return held[:, :, :, :, :, cols].reshape((-1, held.shape[-1] if cols == slice(None) else cols.stop - cols.start))

    def have(layer, arrs):
        gather.arrived([n for n in (now if layer == 0 else nxt) if n in gather.passed
                        and (parts[n][0] is fulls[-1] or any(parts[n][0] is fulls[4 * layer + arr] for arr in arrs))])

    for layer in range(n_layers):
        h_ref = y_v if layer else x_ref
        y_hbm, n1_hbm, n2_hbm, ctx_hbm, act_hbm, qkv_hbm, pre_hbm = saved[7 * layer:7 * layer + 7]
        have(layer, [2])
        loads = [load(layer, 2, k, TILE) for k in range(6)]
        if layer == 0:
            fetch = pltpu.make_async_copy(fulls[-1], small_v, load_sem.at[3, 1])
            fetch.start()
            fetch.wait()
            for k in range(n_layers):
                unpack_vectors(small_v, k, sel_shard, sel_lane, vec_ref)
        else:
            for copy in saves:
                copy.wait()
            for copy in shares:
                copy.wait_send()
            saves.clear()

        def vector(k, cols=slice(None)):
            at = OFFSETS[k]
            return vec_ref[layer:layer + 1, at:at + SIZES[k]] if cols == slice(None) else vec_ref[layer:layer + 1, at + cols.start:at + cols.stop]

        for r in range(SEQ // LN_ROWS):
            rows = slice(r * LN_ROWS, (r + 1) * LN_ROWS)
            scaled, _ = normalised(h_ref[rows, :].astype(jnp.float32))
            n1_v[rows, :] = (scaled * vector(0) + vector(1)).astype(jnp.bfloat16)
            n2_v[rows, :] = (scaled * vector(2) + vector(3)).astype(jnp.bfloat16)
        share(n1_v, n1_hbm)
        share(n2_v, n2_hbm)
        for k in range(6):
            cols = slice(k * TILE, (k + 1) * TILE)
            loads[k].wait()
            x = dot(n1_v[...], matrix(wqkv_v, cols)) + vector(4, cols)
            for c in range(TILE // PAIR):
                block = x[:, c * PAIR:(c + 1) * PAIR]
                if k < 4:
                    block = turn(block, cos_ref[...], sina_ref[...], sinb_ref[...])
                at = k * TILE + c * PAIR
                qkv_v[:, at:at + PAIR] = block.astype(jnp.bfloat16)
        save(qkv_v, qkv_hbm)
        have(layer, [0, 1, 3])
        out_load = load(layer, 3, 0)
        up_loads = [load(layer, 0, t, TILE) for t in range(N_TILES)]
        down_load = load(layer, 1, 0)

        @pl.loop(0, WIDTH // PAIR)
        def _(pair):
            keys = split_heads(qkv_v[:, lanes(WIDTH + pair * PAIR)])
            values = split_heads(qkv_v[:, lanes(2 * WIDTH + pair * PAIR)])
            for i in range(SEQ // PAIR):
                n = (i + 1) * 2 * PAIR
                rows = slice(i * PAIR, (i + 1) * PAIR)
                probs = probabilities(qkv_v[rows, lanes(pair * PAIR)], keys[:n], i)
                probs = jnp.concatenate([p.astype(jnp.bfloat16) for p in probs], axis=1)
                ctx_v[rows, lanes(pair * PAIR)] = dot(probs, values[:n]).astype(jnp.bfloat16)

        share(ctx_v, ctx_hbm)
        if layer == 0:
            gather.middle(nxt, 2)
        out_load.wait()
        for cols in (slice(0, TILE), slice(TILE, WIDTH)):
            acc[:, cols] = (h_ref[:, cols].astype(jnp.float32) + dot(ctx_v[...], matrix(wout_v, cols))
                            + (vector(5, cols) + vector(7, cols)))
        down_load.wait()
        for t in range(N_TILES):
            cols = slice(t * TILE, (t + 1) * TILE)
            up_loads[t].wait()
            pre = dot(n2_v[...], matrix(wup_v, cols)) + vector(6, cols)
            pre_v[t] = pre
            act_v[:, cols] = (0.5 * pre * (1.0 + lax.erf(pre * INV_SQRT2))).astype(jnp.bfloat16)
            acc[...] += dot(act_v[:, cols], wdown_v[t // 2, t % 2 * 2:t % 2 * 2 + 2].reshape((TILE, WIDTH)))
            if layer == 0 and t == N_TILES // 2:
                gather.late(nxt, 2)
        save(pre_v, pre_hbm)
        share(act_v, act_hbm)
        y_v[...] = acc[...].astype(jnp.bfloat16)
        save(y_v, y_hbm)
        if layer == 0:
            gather.end(nxt, 2)
    for copy in saves:
        copy.wait()
    per = len(shares) // n_layers
    for copy in shares:
        copy.wait_recv()
    for copy in shares[-per:]:
        copy.wait_send()
    for copy in gather.copies:
        copy.wait_send()


def forward(x, shards, small_tile, tables, sel_shard, sel_lane):
    n_layers = shards[0].shape[0]
    bf16, f32 = jnp.bfloat16, jnp.float32
    chips = (4, 4, 4, 2)
    full = [(chips + tensor.shape[1:], bf16) for tensor in shards]
    shapes = full * n_layers + [(chips + small_tile.shape, bf16), ((n_layers, N_VEC), f32)]
    kept = [((SEQ, WIDTH), bf16)] + [((2, SEQ, width), bf16) for width in (WIDTH, WIDTH, WIDTH, HIDDEN)]
    kept += [((SEQ, 3 * WIDTH), bf16), ((N_TILES, SEQ, TILE), f32)]
    shapes += kept * n_layers
    n_parts = len(GATHER_PARTS) * n_layers + 1
    dma = pltpu.SemaphoreType.DMA
    scratch = [pltpu.VMEM(*s) for s in full]
    scratch += [pltpu.VMEM(chips + small_tile.shape, bf16), pltpu.VMEM((SEQ, WIDTH), f32), pltpu.VMEM((N_TILES, SEQ, TILE), f32)]
    scratch += [pltpu.VMEM((SEQ, width), bf16) for width in (WIDTH, WIDTH, 3 * WIDTH, WIDTH, HIDDEN, WIDTH)]
    scratch += [dma((n_parts, 9)), dma((n_parts, 9)), dma((n_parts, 10)), dma((n_parts, 10)), dma((4 * n_layers + 1,)),
                dma((4, N_TILES)), dma((7,)), dma((4 * n_layers,)), dma((4 * n_layers,))]
    out_specs = [ANY] * len(shapes)
    out_specs[4 * n_layers + 1] = IN_VMEM
    outs = pl.pallas_call(
        functools.partial(forward_kernel, n_layers),
        out_shape=[jax.ShapeDtypeStruct(s, d) for s, d in shapes],
        in_specs=[IN_VMEM] * 11,
        out_specs=out_specs,
        scratch_shapes=scratch,
        compiler_params=pltpu.CompilerParams(collective_id=0, has_side_effects=True, vmem_limit_bytes=VMEM_LIMIT),
        cost_estimate=pl.CostEstimate(flops=20 * 10**9, bytes_accessed=10**8, transcendentals=10**7),
        name='forward_layers',
    )(x, *tables, sel_shard, sel_lane, *shards, small_tile)
    weights = [[t.reshape((-1, t.shape[-1])) for t in outs[4 * k:4 * k + 4]] for k in range(n_layers)]
    outs = outs[4 * n_layers + 1:]
    return weights, outs[0], [outs[1 + 7 * k:8 + 7 * k] for k in range(n_layers)]


WAVES = ((384, 384, 384, 384, 512, 512), (384, 384, 384, 384, 256, 256), (256,) * 6)
COLOURS = range(6)
US_PER_COLUMN, US_PER_STEP = 0.0165, 2.5
WIRE_PARTS = (0.25, 0.5, 0.75, 0.81, 0.88, 0.94, 0.95, 0.97, 0.98, 1)
UP, DOWN, QKV, OUT = range(4)


def pieces(wave, colour):
    if wave == 2:
        return [(QKV, 0, 256 * colour, 0, 256)]
    if colour < 4:
        return [(UP if wave else DOWN, 0 if wave else colour, 384 * colour if wave else 0, 0, 384)]
    if wave:
        return [(UP, 0, 256 * colour + 512, 0, 256)]
    group = 2 * colour - 8
    return [(DOWN, group, 384, 0, 128), (DOWN, group + 1, 384, 128, 128), (OUT, 0, 128 * group, 256, 256)]


def add_into(dst, src, n_axes):
    if n_axes < 2:
        dst[...] += src[...]
        return

    @pl.loop(0, 4)
    def _(k):
        dst[k] += src[k]


def at_axis(ref, axis, value, n_axes):
    every = [pl.ds(0, 4)] * n_axes
    every[axis] = value
    return ref.at[tuple(every)]


class Reduce:
    def __init__(self, chip, core, grads, came, fin, sems, spare, write):
        self.chip, self.core, self.grads, self.came, self.fin = chip, core, grads, came, fin
        self.send_sem, self.recv_sem, (self.spare, self.spare_sem) = sems[0], sems[1], spare
        self.write = write

    def plan(self, k):
        order, (one, two) = colour_plan(k)
        return order, one, two

    def box(self, k, stage):
        order, *_ = colour_plan(k)
        ref = self.came[k][0].at[0]
        axes = [axis for axis in range(3) if axis != order[0]]
        spot = axes.index(order[1])
        if stage == 1:
            return ref, spot, 2
        return at_axis(ref, spot, self.chip.where[order[1]], 2), 0, 1

    def copy(self, k, slot):
        order, one, two = self.plan(k)
        stage, turn = slot // 3, slot % 3
        if slot == 9:
            src, dst = self.final(k).at[1 - self.core], self.fin[k]
            device = self.chip.device(0, 0, 1 - self.core)
        else:
            axis = order[stage]
            device = self.chip.device(axis, two if turn == 2 else one, self.core)
            dst = self.came[k][2 * stage + turn // 2]
            dst = dst if turn == 2 else dst.at[turn]
            value = self.chip.near[axis][(one, 2, two)[turn]]
            if stage:
                ref, spot, n_axes = self.box(k, stage)
                src = at_axis(ref, spot, value, n_axes)
            else:
                src = self.came[k][0].at[1] if turn == 2 else at_axis(self.grads[k], axis, value, 3)
        return pltpu.make_async_remote_copy(src_ref=src, dst_ref=dst, send_sem=self.send_sem.at[k, slot],
                                            recv_sem=self.recv_sem.at[k, slot], device_id=device, device_id_type=MESH)

    def send(self, k, slot):
        self.copy(k, slot).start()

    def start(self):
        for slot in (1, 0):
            for k in COLOURS:
                self.send(k, slot)

    def local(self, k, slot):
        order, _, two = self.plan(k)
        width = self.grads[k].shape[-1]
        return pltpu.make_async_copy(at_axis(self.grads[k], order[0], self.chip.near[order[0]][two if slot else 0], 3),
                                     self.spare.at[k % 2, :, :, :, :, pl.ds(0, width)], self.spare_sem.at[k % 2])

    def first(self, slot):
        self.local(0, slot).start()
        for k in COLOURS:
            if k < 5:
                self.local(k + 1, slot).start()
            self.local(k, slot).wait()
            self.copy(k, slot).wait_recv()
            width = self.grads[k].shape[-1]
            add_into(self.came[k][0].at[slot], self.spare.at[k % 2, :, :, :, :, pl.ds(0, width)], 2)
            if slot:
                self.send(k, 2)

    def halve(self, stage):
        for k in COLOURS:
            order, one, two = self.plan(k)
            ref, spot, n_axes = self.box(k, stage)
            near = self.chip.near[order[stage]]
            self.copy(k, 3 * stage - 1).wait_recv()
            arrived = self.came[k][2 * stage - 1]
            for slot, value in ((1, near[2]), (0, near[one]), (2, near[two]), (2, near[0])):
                add_into(at_axis(ref, spot, value, n_axes), at_axis(arrived, spot, value, n_axes), n_axes - 1)
                if slot < 2:
                    self.send(k, 3 * stage + slot)

    def settle(self, stage, slot):
        for k in COLOURS:
            order, one, two = self.plan(k)
            ref, spot, n_axes = self.box(k, stage)
            value = self.chip.near[order[stage]][two if slot else 0]
            self.copy(k, 3 * stage + slot).wait_recv()
            add_into(at_axis(ref, spot, value, n_axes), self.came[k][2 * stage].at[slot], n_axes - 1)
            if slot:
                self.send(k, 3 * stage + 2)

    def final(self, k):
        order, *_ = colour_plan(k)
        return self.box(k, 2)[0].at[self.chip.where[order[2]]]

    def cross(self):
        for k in COLOURS:
            self.copy(k, 8).wait_recv()
            add_into(self.final(k), self.came[k][5], 0)
            self.send(k, 9)

    def finish(self):
        for k in COLOURS:
            self.write(k, self.core, self.final(k)[self.core])
        for k in COLOURS:
            self.copy(k, 9).wait_recv()
            self.write(k, 1 - self.core, self.fin[k][...])
        for k in COLOURS:
            for slot in range(10):
                self.copy(k, slot).wait_send()

    def steps(self, now):
        todo = [lambda: self.first(1), lambda: self.first(0), lambda: self.halve(1), lambda: self.settle(1, 1),
                lambda: self.settle(1, 0), lambda: self.halve(2), lambda: self.settle(2, 1), lambda: self.settle(2, 0),
                self.cross, self.finish]
        wire = sum(grad.shape[-1] for grad in self.grads) * US_PER_COLUMN
        return [(now + wire * part + US_PER_STEP * (k + 1), k, step) for k, (part, step) in enumerate(zip(WIRE_PARTS, todo))]


class VectorSum:
    def __init__(self, chip, core, total, came, send_sem, recv_sem):
        self.total, self.came, self.send_sem, self.recv_sem = total, came, send_sem, recv_sem
        self.devices = [chip.device(axis, mask, core) for axis in range(3) for mask in (1, 3)]
        self.devices.append(chip.device(0, 0, 1 - core))

    def copy(self, k):
        return pltpu.make_async_remote_copy(src_ref=self.total, dst_ref=self.came.at[k], send_sem=self.send_sem.at[k],
                                            recv_sem=self.recv_sem.at[k], device_id=self.devices[k], device_id_type=MESH)

    def step(self, k):
        if k:
            self.copy(k - 1).wait()
            self.total[...] += self.came[k - 1]
        if k < 7:
            self.copy(k).start()


def backward_kernel(*refs):
    dout_ref, cos_ref, sina_ref, sinb_ref, vec_ref, sel_shard, sel_lane = refs[:7]
    refs = refs[7:]
    (wup, wdown, wqkv, wout), refs = refs[:4], refs[4:]
    (h_hbm, n1_hbm, n2_hbm, ctx_hbm, act_hbm, qkv_hbm, pre_hbm), refs = refs[:7], refs[7:]
    dx_hbm, small_ref, sums, refs = refs[0], refs[1], refs[2:6], refs[6:]
    grads, (dout_cols, dpre_cols, dqkv_cols), refs = refs[:18], refs[18:21], refs[21:]
    came, fins, refs = refs[:108], refs[108:126], refs[126:]
    (spare, tile_v, big_v, rhs_v, wup_v, wdown_v, pre_v, dn1, dn2, dctx, dk_acc, dv_acc, qkv_v, dpre_v, dqkv_v, dh_v, h_v, total,
     came_vec, send_sem, recv_sem, spare_sem, tile_sem, big_sem, rhs_sem, mlp_sem, io_sem, share_sem, share_send, share_recv,
     vec_send, vec_recv) = refs
    chip, core = place()
    entry_barrier(chip, core)
    partner = chip.device(0, 0, 1 - core)
    clock, queue = 0.0, []

    def due(now):
        ready = sorted(item[:2] + (n,) for n, item in enumerate(queue) if item[0] <= now)
        found = [queue[n][2] for *_, n in ready]
        queue[:] = [item for item in queue if item[0] > now]
        return found

    def run(steps):
        for step in steps:
            step()

    def start(copies):
        for copy in copies:
            copy.start()
        return copies

    def wait(copies):
        for copy in copies:
            copy.wait()

    def hooks(count, each):
        return [(n, due(clock + each * (n + 1))) for n in range(count)]

    def at_hooks(n, planned):
        for when, steps in planned:
            if steps:
                @pl.when(n == when)
                def _():
                    run(steps)

    def share(k, src, width, dst):
        def half(which):
            return src.at[:, pl.ds(pl.multiple_of(which * width, PAIR), width)]
        mine = pltpu.make_async_copy(half(core), dst.at[core], share_sem.at[k])
        other = pltpu.make_async_remote_copy(
            src_ref=half(1 - core), dst_ref=dst.at[core], send_sem=share_send.at[k],
            recv_sem=share_recv.at[k], device_id=partner, device_id_type=MESH)
        return start([mine, other])

    def tokens_load(src, first, slot):
        return start([pltpu.make_async_copy(src.at[k, :, pl.ds(first, WIDTH)], big_v.at[slot, pl.ds(k * SEQ, SEQ)],
                                            big_sem.at[slot, k]) for k in range(2)])

    def whole_load(src, slot):
        return pltpu.make_async_copy(src, big_v.at[slot], big_sem.at[slot, 2])

    def rhs_load(src, first, width, slot):
        return start([pltpu.make_async_copy(src.at[k, :, pl.ds(first, width)],
                                            rhs_v.at[slot, pl.ds(k * SEQ, SEQ), pl.ds(0, width)], rhs_sem.at[slot, k])
                      for k in range(2)])

    def product(lhs_slot, rhs_slot, width, out_slot):
        value = lax.dot_general(big_v[lhs_slot, 0:2 * SEQ, :], rhs_v[rhs_slot, :, 0:width], (((0,), (0,)), ((), ())),
                                preferred_element_type=jnp.float32)
        tile_v[out_slot, :, :, :, :, :, 0:width] = value.reshape(tile_v.shape[1:-1] + (width,))

    def columns_of(wave, colour, first, width):
        return grads[6 * wave + colour].at[:, :, :, :, :, pl.ds(first, width)]

    def launch(wave):
        def write(k, half, block):
            for arr, group, col, first, width in pieces(wave, k):
                size = sums[arr].shape[-1] // 2
                at = pl.ds(pl.multiple_of(half * size + col, PAIR), width)
                sums[arr][group, :, at] = block[:, first:first + width].astype(jnp.bfloat16)
        current = Reduce(chip, core, grads[6 * wave:6 * wave + 6], [came[36 * wave + 6 * k:36 * wave + 6 * k + 6] for k in COLOURS],
                         fins[6 * wave:6 * wave + 6], (send_sem.at[wave], recv_sem.at[wave]), (spare, spare_sem), write)
        current.start()
        queue.extend(current.steps(clock))

    def tile_loads(t, slot):
        at = pl.multiple_of(t * TILE, TILE)
        return [pltpu.make_async_copy(wdown.at[pl.ds(at, TILE)], wdown_v.at[slot], mlp_sem.at[slot, 0]),
                pltpu.make_async_copy(pre_hbm.at[t], pre_v.at[slot], mlp_sem.at[slot, 1]),
                pltpu.make_async_copy(wup.at[:, pl.ds(at, TILE)], wup_v.at[slot], mlp_sem.at[slot, 2])]

    def vector_at(k, first=0, width=None):
        return pl.ds(pl.multiple_of(OFFSETS[k] + first, PAIR), width or SIZES[k])

    out_share = share(0, dout_ref, TILE, dout_cols)
    loads = tokens_load(act_hbm, 0, 0)
    input_loads = start([pltpu.make_async_copy(qkv_hbm, qkv_v, io_sem.at[0]), pltpu.make_async_copy(h_hbm, h_v, io_sem.at[1])])
    for t in range(2):
        start(tile_loads(t, t))
    d_sum = jnp.sum(dout_ref[...].astype(jnp.float32), axis=0, keepdims=True)
    total[:, vector_at(5)] = d_sum
    total[:, vector_at(7)] = d_sum
    wait(out_share)
    wait(rhs_load(dout_cols, 0, TILE, 0))
    outs = [[], []]
    for z in range(5):
        slot = z % 2
        wait(loads)
        if z < 4:
            loads = tokens_load(act_hbm if z < 3 else ctx_hbm, (z + 1) % 4 * WIDTH, 1 - slot)
        wait(outs[slot])
        product(slot, 0, TILE, slot)
        found = []
        if z < 4:
            for k in range(4):
                for colour, col, first, width in ((k, 0, 0, 384), (4 + k // 2, 384, k % 2 * PAIR, PAIR)):
                    for c in range(2):
                        found.append((tile_v.at[slot, :, :, 2 * c + k // 2, k % 2, :, pl.ds(col, width)],
                                      columns_of(0, colour, first, width).at[z, :, :, c]))
        else:
            for k in range(2):
                found.append((tile_v.at[slot, :, :, :, :, :, pl.ds(256 * k, 256)], columns_of(0, 4 + k, 256, 256)))
        outs[slot] = start([pltpu.make_async_copy(*one, tile_sem.at[slot, n]) for n, one in enumerate(found)])
    wait(outs[0] + outs[1])
    clock += 8
    launch(0)

    n2_loads = tokens_load(n2_hbm, 0, 0)
    out_load = whole_load(wout, 1)
    out_load.start()
    dn2[...] = jnp.zeros_like(dn2)

    def pre_copy(t, slot, to_partner):
        dst = dpre_cols.at[core, :, pl.ds(pl.multiple_of(lax.rem(t, 4) * TILE, TILE), TILE)]
        if to_partner:
            return pltpu.make_async_remote_copy(
                src_ref=dpre_v.at[slot], dst_ref=dst, send_sem=share_send.at[2 + t],
                recv_sem=share_recv.at[2 + t], device_id=partner, device_id_type=MESH)
        return pltpu.make_async_copy(dpre_v.at[slot], dst, share_sem.at[2 + slot])

    def pre_act(t, begin):
        for to_partner in (False, True):
            @pl.when(lax.div(t, 4) == (1 - core if to_partner else core))
            def _():
                copy = pre_copy(t, lax.rem(t, 2), to_partner)
                if begin:
                    copy.start()
                elif to_partner:
                    copy.wait_send()
                else:
                    copy.wait()

    planned = hooks(N_TILES, 2.1)

    @pl.loop(0, N_TILES)
    def _(t):
        slot = lax.rem(t, 2)
        wait(tile_loads(t, slot))
        d_act = dot_t(dout_ref[...], wdown_v[slot]).astype(jnp.bfloat16).astype(jnp.float32)
        pre = pre_v[slot]
        slope = 0.5 * (1.0 + lax.erf(pre * INV_SQRT2)) + pre * (INV_SQRT2PI * jnp.exp(-0.5 * pre * pre))
        d_pre = d_act * slope
        total[:, vector_at(6, t * TILE, TILE)] = jnp.sum(d_pre, axis=0, keepdims=True)

        @pl.when(t > 1)
        def _():
            pre_act(t - 2, False)

        dpre_v[slot] = d_pre.astype(jnp.bfloat16)
        pre_act(t, True)
        dn2[...] += dot_t(dpre_v[slot], wup_v[slot])

        @pl.when(t + 2 < N_TILES)
        def _():
            start(tile_loads(t + 2, slot))

        at_hooks(t, planned)

    clock += 2.1 * N_TILES
    for t in range(N_TILES - 2, N_TILES):
        pre_act(t, False)
    for t in range(4):
        pre_copy(4 * core + t, 0, True).wait_recv()

    def gradient_wave(wave, source, lhs_slot):
        widths = WAVES[wave]
        loads = rhs_load(source, 0, widths[0], 0)
        outs = [[], []]
        for k in COLOURS:
            slot, width = k % 2, widths[k]
            wait(loads)
            if k < 5:
                loads = rhs_load(source, sum(widths[:k + 1]), widths[k + 1], 1 - slot)
            wait(outs[slot])
            product(lhs_slot, slot, width, slot)
            outs[slot] = start([pltpu.make_async_copy(tile_v.at[slot, :, :, :, :, :, pl.ds(0, width)],
                                                      columns_of(wave, k, 0, width), tile_sem.at[slot, 0])])
        wait(outs[0] + outs[1])
        launch(wave)

    wait(n2_loads)
    clock += 5
    gradient_wave(1, dpre_cols, 0)

    out_load.wait()
    for k in range(2):
        rows = slice(k * TILE, (k + 1) * TILE)
        dctx[:, rows] = dot_t(dout_ref[...], big_v[1, rows, :]).astype(jnp.bfloat16)
    qkv_loads = [whole_load(wqkv.at[:, pl.ds(k * WIDTH, WIDTH)], k % 2) for k in range(3)]
    start(qkv_loads[:2])
    wait(input_loads)
    clock += 2
    run(due(clock))
    planned = hooks(N_TILES, 2.0)

    @pl.loop(0, WIDTH // PAIR)
    def _(pair):
        at = lanes(pair * PAIR)
        keys = split_heads(qkv_v[:, lanes(WIDTH + pair * PAIR)])
        values = split_heads(qkv_v[:, lanes(2 * WIDTH + pair * PAIR)])
        q_t = qkv_v[:, at].T
        dc_t = dctx[:, at].T
        bias_sums = [jnp.zeros((1, PAIR), jnp.float32)] * 3
        for i in range(SEQ // PAIR):
            n = (i + 1) * 2 * PAIR
            rows = slice(i * PAIR, (i + 1) * PAIR)
            probs = probabilities(qkv_v[rows, at], keys[:n], i)
            d_all = dot_t(dctx[rows, at], values[:n]).astype(jnp.bfloat16).astype(jnp.float32)
            d_probs = [d_all[:, j * PAIR:(j + 1) * PAIR] for j in range(2 * i + 2)]
            d_scores = [None] * (2 * i + 2)
            for head in range(2):
                mean = probs[head] * d_probs[head]
                for j in range(1, i + 1):
                    mean = mean + probs[2 * j + head] * d_probs[2 * j + head]
                mean = jnp.sum(mean, axis=1, keepdims=True)
                for j in range(head, 2 * i + 2, 2):
                    d_scores[j] = (probs[j] * (d_probs[j] - mean) * SCALE).astype(jnp.bfloat16)
            d_scores = jnp.concatenate(d_scores, axis=1)
            probs = jnp.concatenate([p.astype(jnp.bfloat16) for p in probs], axis=1)
            d_query = dot(d_scores, keys[:n]).astype(jnp.bfloat16).astype(jnp.float32)
            d_query = turn_back(d_query, cos_ref[rows, :], sina_ref[rows, :], sinb_ref[rows, :])
            bias_sums[0] = bias_sums[0] + jnp.sum(d_query, axis=0, keepdims=True)
            dqkv_v[rows, at] = d_query.astype(jnp.bfloat16)
            d_keys = dot(q_t[:, rows], d_scores)
            d_values = dot(dc_t[:, rows], probs)
            old = 2 * i * PAIR
            if i:
                dk_acc[:, :old] += d_keys[:, :old]
                dv_acc[:, :old] += d_values[:, :old]
            dk_acc[:, old:n] = d_keys[:, old:]
            dv_acc[:, old:n] = d_values[:, old:]
        first = lax.broadcasted_iota(jnp.int32, (PAIR, PAIR), 0) < PAIR // 2
        for j in range(SEQ // PAIR):
            rows = slice(j * PAIR, (j + 1) * PAIR)
            left, right = slice(2 * j * PAIR, (2 * j + 1) * PAIR), slice((2 * j + 1) * PAIR, (2 * j + 2) * PAIR)
            d_key = jnp.where(first, dk_acc[:, left], dk_acc[:, right]).T.astype(jnp.bfloat16).astype(jnp.float32)
            d_key = turn_back(d_key, cos_ref[rows, :], sina_ref[rows, :], sinb_ref[rows, :])
            bias_sums[1] = bias_sums[1] + jnp.sum(d_key, axis=0, keepdims=True)
            dqkv_v[rows, lanes(WIDTH + pair * PAIR)] = d_key.astype(jnp.bfloat16)
            d_value = jnp.where(first, dv_acc[:, left], dv_acc[:, right]).T.astype(jnp.bfloat16)
            bias_sums[2] = bias_sums[2] + jnp.sum(d_value.astype(jnp.float32), axis=0, keepdims=True)
            dqkv_v[rows, lanes(2 * WIDTH + pair * PAIR)] = d_value
        for k, bias_sum in enumerate(bias_sums):
            total[:, vector_at(4, k * WIDTH + pair * PAIR, PAIR)] = bias_sum
        at_hooks(pair, planned)

    clock += 2.0 * N_TILES
    qkv_share = share(1, dqkv_v, 3 * TILE, dqkv_cols)
    for k in range(3):
        qkv_loads[k].wait()
        part = dot_t(dqkv_v[:, k * WIDTH:(k + 1) * WIDTH], big_v[k % 2])
        if k == 0:
            dn1[...] = part
            qkv_loads[2].start()
        else:
            dn1[...] += part
    n1_loads = tokens_load(n1_hbm, 0, 1)
    for k in range(4):
        total[:, vector_at(k)] = jnp.zeros((1, WIDTH), jnp.float32)

    @pl.loop(0, SEQ // LN_ROWS)
    def _(r):
        rows = pl.ds(pl.multiple_of(r * LN_ROWS, LN_ROWS), LN_ROWS)
        scaled, inverse = normalised(h_v[rows, :].astype(jnp.float32))
        d1 = dn1[rows, :].astype(jnp.bfloat16).astype(jnp.float32)
        d2 = dn2[rows, :].astype(jnp.bfloat16).astype(jnp.float32)
        for k, value in enumerate((d1 * scaled, d1, d2 * scaled, d2)):
            total[:, vector_at(k)] += jnp.sum(value, axis=0, keepdims=True)
        g1, g2 = [vec_ref[:, OFFSETS[k]:OFFSETS[k] + WIDTH] for k in (0, 2)]
        d_scaled = d1 * g1 + d2 * g2
        d_h = inverse * (d_scaled - jnp.mean(d_scaled, axis=1, keepdims=True)
                         - scaled * jnp.mean(d_scaled * scaled, axis=1, keepdims=True))
        dh_v[rows, :] = (dout_ref[rows, :].astype(jnp.float32) + d_h).astype(jnp.bfloat16)

    clock += 6
    run(due(clock))
    wait(n1_loads + qkv_share)
    clock += 4
    gradient_wave(2, dqkv_cols, 1)
    run(due(clock))

    dx_copy = pltpu.make_async_copy(dh_v, dx_hbm, io_sem.at[2])
    dx_copy.start()
    rest = due(10 ** 9)
    vectors = VectorSum(chip, core, total, came_vec, vec_send, vec_recv)
    for k in range(8):
        vectors.step(k)
        run(rest[:2])
        rest = rest[2:]
    run(rest)
    node, local = chip.device(0, 0, core)
    me = node * 8 + local
    row = jnp.zeros((8, PAIR), jnp.float32)
    for k in range(N_VEC // WIDTH):
        cols = slice(k * WIDTH, (k + 1) * WIDTH)
        mine = (sel_shard[:, cols] == me).astype(jnp.float32)
        left = jnp.zeros((8, WIDTH), jnp.float32) + total[:, cols] * mine
        pick = (lax.broadcasted_iota(jnp.int32, (PAIR, WIDTH), 0) == sel_lane[:, cols]).astype(jnp.float32).astype(jnp.bfloat16)
        for _ in range(3):
            high = left.astype(jnp.bfloat16)
            row = row + dot_t(high, pick)
            left = left - high.astype(jnp.float32)
    small_ref[...] = row.astype(jnp.bfloat16)
    dx_copy.wait()


def backward(number, d_out, tables, vectors, sel_shard, sel_lane, weights, saved):
    bf16, f32 = jnp.bfloat16, jnp.float32
    dma = pltpu.SemaphoreType.DMA
    shapes = [((SEQ, WIDTH), bf16), ((8, PAIR), bf16)]
    shapes += [((groups, 8, width), bf16) for groups, width in ((1, HIDDEN), (4, WIDTH), (1, 3 * WIDTH), (1, WIDTH))]
    blocks = [(2, 8, width) for wave in WAVES for width in wave]
    shapes += [((4, 4, 4) + block, f32) for block in blocks]
    shapes += [((2, SEQ, width), bf16) for width in (TILE, 4 * TILE, 3 * TILE)]
    leads = ((2, 4, 4), (4, 4), (2, 4), (4,), (2,), ())
    scratch = [pltpu.VMEM(lead + block, f32) for block in blocks for lead in leads]
    scratch += [pltpu.VMEM(block[1:], f32) for block in blocks]
    wide, row = (SEQ, WIDTH), (1, N_VEC)
    scratch += [pltpu.VMEM(*s) for s in (
        ((2, 4, 4, 2, 8, TILE), f32), ((2, 4, 4, 4, 2, 8, TILE), f32), ((2, WIDTH, WIDTH), bf16), ((2, 2 * SEQ, TILE), bf16),
        ((2, WIDTH, TILE), bf16), ((2, TILE, WIDTH), bf16), ((2, SEQ, TILE), f32), (wide, f32), (wide, f32), (wide, bf16),
        ((PAIR, 2 * SEQ), f32), ((PAIR, 2 * SEQ), f32), ((SEQ, 3 * WIDTH), bf16), ((2, SEQ, TILE), bf16), ((SEQ, 3 * WIDTH), bf16),
        (wide, bf16), (wide, bf16), (row, f32), ((7,) + row, f32))]
    scratch += [dma(s) for s in ((3, 6, 10), (3, 6, 10), (2,), (2, 16), (2, 3), (2, 2), (2, 3), (3,), (4,),
                                 (10,), (10,), (7,), (7,))]
    out_specs = [ANY] + [IN_VMEM] * 5 + [ANY] * (len(shapes) - 6)
    outs = pl.pallas_call(
        backward_kernel,
        out_shape=[jax.ShapeDtypeStruct(s, d) for s, d in shapes],
        in_specs=[IN_VMEM] * 7 + [ANY] * 11,
        out_specs=out_specs,
        scratch_shapes=scratch,
        compiler_params=pltpu.CompilerParams(collective_id=number, has_side_effects=True, vmem_limit_bytes=VMEM_LIMIT),
        cost_estimate=pl.CostEstimate(flops=20 * 10**9, bytes_accessed=10**8, transcendentals=10**7),
        name='backward_layer',
    )(d_out, *tables, vectors, sel_shard, sel_lane, *weights, *saved)
    return outs[0], outs[1][0], [s.reshape((-1, s.shape[-1])) for s in outs[2:6]]


def rope_tables(seq_len, head_dim):
    rot_dim = head_dim // 4
    inv_freq = 1.0 / (10000.0 ** (jnp.arange(0, rot_dim, 2, dtype=jnp.float32) / rot_dim))
    angles = jnp.arange(seq_len, dtype=jnp.float32)[:, None] * inv_freq[None, :]
    cos, sin = jnp.cos(angles), jnp.sin(angles)
    zero = jnp.zeros_like(sin)
    rest = jnp.zeros((seq_len, head_dim - rot_dim), jnp.float32)
    tables = ([cos, cos, rest + 1.0], [-sin, zero, rest], [zero, sin, rest])
    return [jnp.tile(jnp.concatenate(table, axis=1), (1, 2)) for table in tables]


def heads_last(tensor):
    lead = tensor.shape[:-2]
    return tensor.reshape(lead + (16, 3, 64)).swapaxes(-3, -2).reshape(lead + (3072,))


def heads_first(tensor):
    lead = tensor.shape[:-1]
    return tensor.reshape(lead + (3, 16, 64)).swapaxes(-3, -2).reshape(lead + (16, 192))


def vector_places():
    shard, lane, start = [], [], 0
    for k, (share, size) in enumerate(zip(SHARES, SIZES)):
        place_of = np.arange(size)
        if k == 4:
            place_of = heads_last(place_of.reshape(16, 192))
        shard.append(place_of // share)
        lane.append(start + place_of % share)
        start += share
    return [jnp.asarray(np.concatenate(part)[None].astype(np.int32)) for part in (shard, lane)]


def pack_vectors(vectors):
    packed = jnp.concatenate(vectors, axis=-1)
    return jnp.pad(packed, ((0, 0), (0, 128 - packed.shape[-1])))


def solution(mesh):
    shard_axes = ('node', 'local')
    act_spec = P(shard_axes)
    param_spec = P(None, shard_axes)
    def device_step(x, y_cot, ln1_gain, ln1_bias, qkv_weight, qkv_bias, out_weight, out_bias,
                    ln2_gain, ln2_bias, up_weight, up_bias, down_weight, down_bias):
        num_layers = ln1_gain.shape[0]
        tables = rope_tables(x.shape[1], qkv_weight.shape[3] // 3)

        small = (ln1_gain, ln1_bias, ln2_gain, ln2_bias, qkv_bias, out_bias, up_bias, down_bias)
        small_tile = jnp.pad(pack_vectors(small), ((0, 8 - num_layers), (0, 0)))
        places = vector_places()
        weights, vectors, saved = forward(x[0], (up_weight, down_weight, heads_last(qkv_weight), out_weight), small_tile,
                                          tables, *places)
        hidden = [x[0]] + [layer[0] for layer in saved]
        saved = [[hidden[k]] + list(saved[k][1:]) for k in range(num_layers)]
        d_hidden, results = y_cot[0], []
        for k in reversed(range(num_layers)):
            d_hidden, *result = backward(k + 1, d_hidden, tables, vectors[k:k + 1], *places, weights[k], saved[k])
            results.insert(0, result)
        small_sums = jnp.stack([result[0] for result in results])
        up, down, qkv, out = [jnp.stack([result[1][arr] for result in results]) for arr in range(4)]
        small_grads, start = [], 0
        for width in SHARES:
            small_grads.append(small_sums[:, start:start + width])
            start += width
        g1, b1, g2, b2, qb, ob, ub, db = small_grads
        return (hidden[-1][None], d_hidden[None], g1, b1, heads_first(qkv), qb, out, ob, g2, b2, up, ub, down, db)

    return jax.shard_map(device_step, mesh=mesh,
                         in_specs=(act_spec, act_spec) + (param_spec,) * 12,
                         out_specs=(act_spec, act_spec) + (param_spec,) * 12,
                         check_vma=False)
```

```python
import functools
import jax
import jax.numpy as jnp
import numpy as np
from jax import lax
from jax.experimental import pallas as pl
from jax.experimental.pallas import tpu as pltpu
from jax.sharding import PartitionSpec as P

BF16, F32 = jnp.bfloat16, jnp.float32
EPSILON = 1e-5
MESH = pl.DeviceIdType.MESH
ANY = pl.BlockSpec(memory_space=pl.ANY)
IN_VMEM = pl.BlockSpec(memory_space=pltpu.VMEM)
VMEM_LIMIT = 67 * 10**6
LAYERS, AXES, SIDE, CORES, ROWS, PARTNERS = 2, 3, 4, 2, 8, 7
CHIPS = (SIDE, SIDE, SIDE)
SHARDS = SIDE * SIDE * SIDE * CORES
SEQ, WIDTH, HIDDEN, TILE, PAIR, LN_ROWS = 384, 1024, 4096, 512, 128, 64
HEADS, HEAD, PARTS = 16, 64, 3
QKV = PARTS * WIDTH
N_TILES, N_PAIRS, N_BLOCKS = HIDDEN // TILE, WIDTH // PAIR, SEQ // PAIR
TWICE = 2 * PAIR
INV_SQRT2, INV_SQRT2PI, SCALE = 0.7071067811865476, 0.3989422804014327, 0.125
SHARES = (8, 8, 8, 8, 24, 8, 32, 8)
SIZES = tuple(SHARDS * share for share in SHARES)
OFFSETS = tuple(sum(SIZES[:k]) for k in range(len(SIZES)))
N_VEC = sum(SIZES)
GAIN1, BIAS1, GAIN2, BIAS2, QKV_BIAS, OUT_BIAS, UP_BIAS, DOWN_BIAS = range(len(SHARES))
ORDERS = ((2, 1, 0), (1, 0, 2), (0, 2, 1))
HALVES = range(2)
OWN, ONE, CROSS, TWO = range(SIDE)
A, B, C = range(AXES)
UP, DOWN, MIX = range(3)
SELF = 3
PASSES = [(stage, step) for stage in range(AXES) for step in range(AXES)] + [(A, SELF)]


class Chip:
    def __init__(self):
        node, local = lax.axis_index('node'), lax.axis_index('local')
        self.core, self.other = lax.rem(local, CORES), 1 - lax.rem(local, CORES)
        self.where = (lax.div(node, SIDE), lax.rem(node, SIDE), lax.div(local, CORES))
        self.base = (node, local - self.core)
        self.strides = ((SIDE, 0), (1, 0), (0, CORES))
        self.near = [(v, v + 1 - 2 * parity(v), lax.rem(v + 2, SIDE), SIDE - 1 - v) for v in self.where]

        self.gaps = [near[3] - near[1] for near in self.near]

    def at(self, axis, role, half):
        near = self.near[axis]
        if role in (OWN, CROSS):
            return near[role]
        return near[role] + half * self.gaps[axis] if role == ONE else near[role] - half * self.gaps[axis]

    def device(self, axis, role, half):
        shift = self.at(axis, role, half) - self.where[axis]
        node, local = [b + shift * s if s else b for b, s in zip(self.base, self.strides[axis])]
        return (node, local + self.core)

    def partner(self):
        node, local = self.base
        return (node, local + self.other)

    def signal_partners(self, semaphore):
        for axis in range(AXES):
            for role in (ONE, TWO):
                pl.semaphore_signal(semaphore, inc=1, device_id=self.device(axis, role, A), device_id_type=MESH)
        pl.semaphore_signal(semaphore, inc=1, device_id=self.partner(), device_id_type=MESH)


def enter():
    chip = Chip()
    barrier = pltpu.get_barrier_semaphore()
    chip.signal_partners(barrier)
    pl.semaphore_wait(barrier, PARTNERS)
    return chip


def remote(src, dst, send_sem, recv_sem, device):
    return pltpu.make_async_remote_copy(src_ref=src, dst_ref=dst, send_sem=send_sem, recv_sem=recv_sem, device_id=device,
                                        device_id_type=MESH)


def start(copies):
    for copy in copies:
        copy.start()
    return copies


def wait(copies):
    for copy in copies:
        copy.wait()


def loop(count):
    return pl.loop(0, count)


def halves(body):
    loop(len(HALVES))(body)


def parity(n):
    return lax.rem(n, 2)


def pool(sems):
    return (sems.at[n] for n in range(sems.shape[0]))


def contract(a, b, a_axis, b_axis):
    return lax.dot_general(a, b, (((a_axis,), (b_axis,)), ((), ())), preferred_element_type=F32)


def dot(a, b):
    return contract(a, b, 1, 0)


def dot_t(a, b):
    return contract(a, b, 1, 1)


def row_sum(x):
    return jnp.sum(x, axis=1, keepdims=True)


def column_sum(x):
    return jnp.sum(x, axis=0, keepdims=True)


def rounded(x):
    return x.astype(BF16).astype(F32)


def lanes(first, width=PAIR):
    return pl.ds(pl.multiple_of(first, PAIR), width)


def turn(x, cos, sin_a, sin_b):
    return x * cos + pltpu.roll(x, PAIR - ROWS, 1) * sin_a + pltpu.roll(x, ROWS, 1) * sin_b


def turn_back(d, cos, sin_a, sin_b):
    return d * cos + pltpu.roll(d * sin_a, ROWS, 1) + pltpu.roll(d * sin_b, PAIR - ROWS, 1)


def iota(shape, axis):
    return lax.broadcasted_iota(jnp.int32, shape, axis)


def block_rows(j):
    return slice(j * PAIR, (j + 1) * PAIR)


def split_heads(x):
    first = iota((PAIR, PAIR), 1) < HEAD
    rows = []
    for j in range(N_BLOCKS):
        block = x[block_rows(j)]
        rows += [jnp.where(first, block, jnp.zeros_like(block)), jnp.where(first, jnp.zeros_like(block), block)]
    return jnp.concatenate(rows, axis=0)


def total_of(chunks, join=jnp.add):
    return functools.reduce(join, chunks)


def probabilities(q_block, keys, i):
    scores = dot_t(q_block, keys)
    causal = iota((PAIR, PAIR), 0) >= iota((PAIR, PAIR), 1)
    chunks = [scores[:, block_rows(j)] * SCALE for j in range(CORES * (i + 1))]
    for head in HALVES:
        mine = slice(head, None, CORES)
        *ahead, last = chunks[mine]
        held = ahead + [jnp.where(causal, last, -1e30)]
        top = jnp.max(total_of(held, jnp.maximum), axis=1, keepdims=True)
        held = [jnp.exp(chunk - top) for chunk in held]
        inverse = 1.0 / row_sum(total_of(held))
        chunks[mine] = [chunk * inverse for chunk in held]
    return chunks


def side_by_side(chunks):
    return jnp.concatenate([chunk.astype(BF16) for chunk in chunks], axis=1)


def row_mean(x):
    return jnp.mean(x, axis=1, keepdims=True)


def normalised(h):
    center = h - row_mean(h)
    inverse = lax.rsqrt(row_mean(center * center) + EPSILON)
    return center * inverse, inverse


class Gather:
    def __init__(self, chip, shards, fulls, sems):
        self.chip, self.shards, self.fulls = chip, shards, fulls
        self.send_sem, self.recv_sem, self.pass_send, self.pass_recv = sems

    def box(self, layer, k, half, stage, role, own=False):
        width = self.fulls[k].shape[-1] // len(HALVES)
        cols = lanes(half * width, width)
        if own:
            return self.shards[k].at[layer, :, cols]
        where = list(self.chip.where)
        for axis in ORDERS[k][:stage]:
            where[axis] = pl.ds(0, SIDE)
        axis = ORDERS[k][stage]
        where[axis] = self.chip.at(axis, role, half)
        return self.fulls[k].at[layer, where[0], where[1], where[2], self.chip.core, :, cols]

    def reach(self, layer, k, half, stage, step):
        slot, role = AXES * stage + step, ONE if step == C else OWN
        src = self.box(layer, k, half, stage, role, stage == A and step < C)
        return remote(src, self.box(layer, k, half, stage, role), self.send_sem.at[layer, k, half, slot],
                      self.recv_sem.at[layer, k, half, slot], self.chip.device(ORDERS[k][stage], TWO if step else ONE, half))

    def passing(self, layer, k, half, stage, step):
        role = (ONE, TWO, CROSS, OWN)[step]
        slot = AXES * AXES if step == SELF else AXES * stage + step
        return remote(self.box(layer, k, half, stage, role, step == SELF), self.box(layer, k, half, stage, role),
                      self.pass_send.at[layer, k, half, slot], self.pass_recv.at[layer, k, half, slot], self.chip.partner())

    def each(self, action):
        for k in (UP, DOWN, MIX):
            @halves
            def _(half):
                action(k, half)

    def begin(self, layer, stage):
        for step in HALVES:
            self.each(lambda k, half: self.reach(layer, k, half, stage, step).start())

    def own(self, layer):
        self.each(lambda k, half: self.passing(layer, k, half, A, SELF).start())

    def middle(self, layer, stage):
        def action(k, half):
            self.reach(layer, k, half, stage, A).wait_recv()
            self.reach(layer, k, half, stage, C).start()
            self.passing(layer, k, half, stage, A).start()
        self.each(action)

    def end(self, layer, stage, steps=(B, C)):
        def action(k, half):
            for step in steps:
                self.reach(layer, k, half, stage, step).wait_recv()
                self.passing(layer, k, half, stage, step).start()
        self.each(action)

    def arrived(self, layer, k):
        @halves
        def _(half):
            for stage, step in PASSES:
                self.passing(layer, k, half, stage, step).wait_recv()

    def left(self):
        def action(layer, k, half):
            for slot, (stage, step) in enumerate(PASSES):
                box = self.box(A, UP, A, stage, OWN, step == SELF)
                for sem in (self.pass_send,) if step == SELF else (self.send_sem, self.pass_send):
                    sem = sem.at[layer, k, half, slot]
                    remote(box, box, sem, sem, self.chip.partner()).wait_send()

        @loop(LAYERS)
        def _(layer):
            @loop(AXES)
            def _(k):
                halves(lambda half: action(layer, k, half))


def pick_lanes(sel_lane, cols):
    return (iota((PAIR, WIDTH), 0) == sel_lane[:, cols]).astype(F32).astype(BF16)


def vector_blocks():
    return [slice(k * WIDTH, (k + 1) * WIDTH) for k in range(N_VEC // WIDTH)]


def unpack_vectors(small_v, layer, sel_shard, sel_lane, vec_ref):
    tiles = small_v[...].astype(F32).reshape((SHARDS, ROWS, PAIR))
    held = jnp.sum(jnp.where(iota(tiles.shape, 1) == layer, tiles, 0.0), axis=1).astype(BF16)
    for cols in vector_blocks():
        spread = dot(held, pick_lanes(sel_lane, cols))
        spread = jnp.where(iota((SHARDS, WIDTH), 0) == sel_shard[:, cols], spread, 0.0)
        vec_ref[layer:layer + 1, cols] = column_sum(spread)


def forward_kernel(x_ref, tables, sel_shard, sel_lane, up_s, down_s, mix_s, small_ref, up_f, down_f, mix_f, small_full, vec_ref,
                   y_hbm, h_hbm, n1_hbm, n2_hbm, ctx_hbm, act_hbm, qkv_hbm, pre_hbm, up_v, down_v, mix_v, small_v, acc, pre_v,
                   n1_v, n2_v, qkv_v, ctx_v, y_v, n1_t, n2_t, ctx_t, act_t, send_sem, recv_sem, pass_send, pass_recv,
                   small_send, small_recv, own_sems, load_sem, save_sem, share_send, share_recv):
    shards, fulls, own_sem = (up_s, down_s, mix_s), (up_f, down_f, mix_f), pool(own_sems)
    chip = enter()
    gather = Gather(chip, shards, fulls, (send_sem, recv_sem, pass_send, pass_recv))

    def small_copy(slot, where, device):
        place = small_full.at[(*where, chip.core)]
        return remote(place, place, small_send.at[slot], small_recv.at[slot], device)

    def small_reach(stage, step):
        where = list(chip.where)
        for axis in range(stage):
            where[axis] = pl.ds(0, SIDE)
        where[stage] = chip.at(stage, ONE if step == C else OWN, A)
        return small_copy(AXES * stage + step, where, chip.device(stage, TWO if step else ONE, A))

    def small_begin(stage):
        small_reach(stage, A).start()
        small_reach(stage, B).start()

    def small_middle(stage):
        small_reach(stage, A).wait_recv()
        small_reach(stage, C).start()

    def small_end(stage):
        small_reach(stage, B).wait_recv()
        small_reach(stage, C).wait_recv()

    small_pass = small_copy(AXES * AXES, [pl.ds(0, SIDE)] * AXES, chip.partner())
    here = (*chip.where, chip.core)
    own = [pltpu.make_async_copy(small_ref, small_full.at[here], next(own_sem))]
    for shard, full in zip(shards, fulls):
        for layer in range(LAYERS):
            own.append(pltpu.make_async_copy(shard.at[layer], full.at[(layer, *here)], next(own_sem)))
    with jax.named_scope('ag0'):
        gather.begin(A, A)
        start(own)
        gather.begin(B, A)
        gather.own(A)
        gather.own(B)
        wait(own)
        small_begin(A)
        gather.middle(A, A)
        small_middle(A)
        gather.middle(B, A)
        gather.end(A, A)
    with jax.named_scope('ag1'):
        gather.begin(A, B)
        small_end(A)
        small_begin(B)
        gather.end(B, A)
        gather.begin(B, B)
        gather.middle(A, B)
        small_middle(B)
        gather.middle(B, B)
        gather.end(A, B)
    with jax.named_scope('ag2_start'):
        gather.begin(A, C)
        small_end(B)
        small_begin(C)
        gather.end(B, B)
    with jax.named_scope('ag2_middle'):
        gather.middle(A, C)
        gather.begin(B, C)
        small_middle(C)
    y_v[...] = x_ref[...]
    with jax.named_scope('ag2_late'):
        gather.end(A, C, (B,))
    with jax.named_scope('small_end'):
        small_end(C)
        small_pass.start()
        small_pass.wait_recv()
        fetch = pltpu.make_async_copy(small_full, small_v, next(own_sem))
        fetch.start()
        fetch.wait()
    with jax.named_scope('unpack'):
        for layer in range(LAYERS):
            unpack_vectors(small_v, layer, sel_shard, sel_lane, vec_ref)
    with jax.named_scope('ag2_end'):
        gather.end(A, C, (C,))

    def saves(layer):
        pairs = [(y_v, h_hbm.at[layer]), (qkv_v, qkv_hbm.at[layer]), (pre_v, pre_hbm.at[layer])]
        kept = [pltpu.make_async_copy(src, dst, save_sem.at[n]) for n, (src, dst) in enumerate(pairs)]
        for n, (src, dst) in enumerate(((n1_t, n1_hbm), (n2_t, n2_hbm), (ctx_t, ctx_hbm), (act_t, act_hbm))):
            dst = dst.at[layer, chip.core]
            kept.append((pltpu.make_async_copy(src, dst, save_sem.at[PARTS + n]),
                         remote(src, dst, share_send.at[layer, n], share_recv.at[layer, n], chip.partner())))
        return kept

    def settle(layer):
        _, qkv_save, pre_save, *shares = saves(layer)
        wait([qkv_save, pre_save])
        for share in shares:
            wait(share)

    @loop(LAYERS)
    def _(layer):
        def vector(k, first=0, width=None):
            return vec_ref[pl.ds(layer, 1), lanes(OFFSETS[k] + first, width or SIZES[k])]

        def load(k, piece):
            if k == DOWN:
                return pltpu.make_async_copy(fulls[k].at[layer, piece], down_v.at[piece], load_sem.at[k, piece])
            cols = lanes(piece * WIDTH, WIDTH)
            return pltpu.make_async_copy(fulls[k].at[layer, :, :, :, :, :, cols], (up_v, None, mix_v)[k].at[:, :, :, :, :, cols],
                                         load_sem.at[k, piece])

        def matrix(held, piece):
            return held[:, :, :, :, :, lanes(piece * WIDTH, WIDTH)].reshape((WIDTH, WIDTH))

        def have(k):
            for which in range(LAYERS):
                @pl.when(layer == which)
                def _():
                    gather.arrived(which, k)

        def meanwhile(action):
            @pl.when(layer == A)
            def _():
                action()

        h_save, qkv_save, pre_save, n1_share, n2_share, ctx_share, act_share = saves(layer)
        with jax.named_scope('have_mix'):
            have(MIX)
            start([load(MIX, k) for k in range(SIDE)])

        h_save.start()

        @pl.when(layer == B)
        def _():
            settle(A)

        with jax.named_scope('ln'):
            @loop(SEQ // LN_ROWS)
            def _(r):
                rows = pl.ds(pl.multiple_of(r * LN_ROWS, LN_ROWS), LN_ROWS)
                scaled, _ = normalised(y_v[rows, :].astype(F32))
                n1_v[rows, :] = (scaled * vector(GAIN1) + vector(BIAS1)).astype(BF16)
                n2_v[rows, :] = (scaled * vector(GAIN2) + vector(BIAS2)).astype(BF16)

        for src, dst, share in ((n1_v, n1_t, n1_share), (n2_v, n2_t, n2_share)):
            dst[...] = src[...].T
            start(share)

        with jax.named_scope('qkv'):
            @loop(PARTS)
            def _(k):
                load(MIX, k).wait()
                x = dot(n1_v[...], matrix(mix_v, k)) + vector(QKV_BIAS, k * WIDTH, WIDTH)

                @pl.when(k < C)
                def _():
                    for c in range(N_PAIRS):
                        block = turn(x[:, block_rows(c)], *[tables[n] for n in range(PARTS)])
                        qkv_v[:, lanes(k * WIDTH + c * PAIR)] = block.astype(BF16)

                @pl.when(k == C)
                def _():
                    qkv_v[:, lanes(k * WIDTH, WIDTH)] = x.astype(BF16)

        qkv_save.start()
        with jax.named_scope('have_up'):
            have(UP)
            have(DOWN)

        start([load(UP, k) for k in range(SIDE)] + [load(DOWN, k) for k in range(SIDE)])
        with jax.named_scope('mid'):
            meanwhile(lambda: gather.middle(B, C))

        with jax.named_scope('fattn'):
            @loop(N_PAIRS)
            def _(pair):
                keys = split_heads(qkv_v[:, lanes(WIDTH + pair * PAIR)])
                values = split_heads(qkv_v[:, lanes(C * WIDTH + pair * PAIR)])
                for i in range(N_BLOCKS):
                    n = (i + 1) * CORES * PAIR
                    probs = probabilities(qkv_v[block_rows(i), lanes(pair * PAIR)], keys[:n], i)
                    ctx_v[block_rows(i), lanes(pair * PAIR)] = dot(side_by_side(probs), values[:n]).astype(BF16)

        ctx_t[...] = ctx_v[...].T
        start(ctx_share)
        meanwhile(lambda: gather.end(B, C, (B,)))
        with jax.named_scope('fout'):
            load(MIX, PARTS).wait()
            acc[...] = y_v[...].astype(F32) + dot(ctx_v[...], matrix(mix_v, PARTS)) + (vector(OUT_BIAS) + vector(DOWN_BIAS))

        with jax.named_scope('fmlp'):
            @loop(SIDE)
            def _(t):
                cols = lanes(t * WIDTH, WIDTH)
                load(UP, t).wait()
                pre = dot(n2_v[...], matrix(up_v, t)) + vector(UP_BIAS, t * WIDTH, WIDTH)
                for k in HALVES:
                    pre_v[CORES * t + k] = pre[:, k * TILE:(k + 1) * TILE]
                act = (0.5 * pre * (1.0 + lax.erf(pre * INV_SQRT2))).astype(BF16)
                act_t[cols, :] = act.T
                load(DOWN, t).wait()
                acc[...] += dot(act, down_v[t].reshape((WIDTH, WIDTH)))

        pre_save.start()
        start(act_share)
        h_save.wait()
        y_v[...] = acc[...].astype(BF16)
        with jax.named_scope('fend'):
            meanwhile(lambda: gather.end(B, C, (C,)))

    with jax.named_scope('ftail'):
        last = pltpu.make_async_copy(y_v, y_hbm, next(own_sem))
        last.start()
        for stage in range(AXES):
            for step in range(AXES):
                small_reach(stage, step).wait_send()
        small_pass.wait_send()
        gather.left()
        settle(LAYERS - 1)
        last.wait()


def forward(x, shards, small_tile, tables, places):
    grid = CHIPS + (CORES,)
    full = [(LAYERS,) + grid + tensor.shape[1:] for tensor in shards]
    shapes = [(shape, BF16) for shape in full] + [(grid + small_tile.shape, BF16), ((LAYERS, N_VEC), F32), ((SEQ, WIDTH), BF16),
                                                  ((LAYERS, SEQ, WIDTH), BF16)]
    shapes += [((LAYERS, CORES, width, SEQ), BF16) for width in (WIDTH, WIDTH, WIDTH, HIDDEN)]
    shapes += [((LAYERS, SEQ, QKV), BF16), ((LAYERS, N_TILES, SEQ, TILE), F32)]
    dma = pltpu.SemaphoreType.DMA
    slots = AXES * AXES
    scratch = [pltpu.VMEM(shape[1:], BF16) for shape in full] + [pltpu.VMEM(grid + small_tile.shape, BF16)]
    scratch += [pltpu.VMEM((SEQ, WIDTH), F32), pltpu.VMEM((N_TILES, SEQ, TILE), F32)]
    scratch += [pltpu.VMEM((SEQ, width), BF16) for width in (WIDTH, WIDTH, QKV, WIDTH, WIDTH)]
    scratch += [pltpu.VMEM((width, SEQ), BF16) for width in (WIDTH, WIDTH, WIDTH, HIDDEN)]
    scratch += [dma((LAYERS, AXES, len(HALVES), n)) for n in (slots, slots, slots + 1, slots + 1)]
    scratch += [dma(shape) for shape in ((slots + 1,), (slots + 1,), (slots + 1,), (AXES, SIDE), (PARTNERS,), (LAYERS, SIDE), (LAYERS, SIDE))]
    out_specs = [IN_VMEM if dtype == F32 and len(shape) == LAYERS else ANY for shape, dtype in shapes]
    return pl.pallas_call(
        forward_kernel,
        out_shape=[jax.ShapeDtypeStruct(*s) for s in shapes],
        in_specs=[IN_VMEM] * 8,
        out_specs=out_specs,
        scratch_shapes=scratch,
        compiler_params=pltpu.CompilerParams(collective_id=0, has_side_effects=True, vmem_limit_bytes=VMEM_LIMIT),
        name='forward_layers',
    )(x, tables, *places, *shards, small_tile)


WAVES = ((384, 384, 512), (384, 384, 256), (256, 256, 256))
LEADS = ((2,) + CHIPS[1:], CHIPS[1:], (2, SIDE), (SIDE,), (2,), ())
W_UP, W_DOWN, W_QKV, W_OUT = range(4)
STEPS = ((1, (2,)), (0, ()), (2, (4, 3)), (4, (5,)), (3, ()), (5, (7, 6)), (7, (8,)), (6, ()), (8, (9,)), (9, ()))
LAST = AXES * AXES
US_COLUMN, US_HOP, US_ADD, US_STEP = 0.022, 2.5, 0.0013, 0.2
US_FIRST, US_TILE, US_UP, US_PAIR, US_NORM, US_QKV = 10, 1.5, 6, 2.15, 6, 5


class Schedule:
    def __init__(self):
        self.now, self.free, self.lines = 0.0, {}, []

    def send(self, link, columns):
        self.free[link] = max(self.free.get(link, 0.0), self.now) + columns * US_COLUMN
        return self.free[link] + US_HOP

    def due(self, limit):
        found = []
        while self.lines:
            line = min(self.lines, key=lambda one: one[A][A]())
            ready = line[A][A]()
            if limit is not None and ready > limit:
                break
            _, run, sends, cost = line.pop(A)
            self.lines = [one for one in self.lines if one]
            self.now = max(self.now, ready) + cost
            sends()
            found.append(run)
        return found

    def run(self, limit):
        for step in self.due(limit):
            step()

    def passed(self, cost):
        self.now += cost
        self.run(self.now)

    def hooks(self, count, cost):
        planned = []
        for _ in range(count):
            self.now += cost
            planned.append(self.due(self.now))
        return planned


def at_hooks(n, planned):
    for when, steps in enumerate(planned):
        if steps:
            @pl.when(n == when)
            def _():
                for step in steps:
                    step()


def add_into(dst, src, n_axes):
    if n_axes < 2:
        dst[...] += src[...]
        return

    @loop(SIDE)
    def _(k):
        dst[k] += src[k]


def at_axis(ref, axis, value, n_axes):
    every = [pl.ds(0, SIDE)] * n_axes
    every[axis] = value
    return ref.at[tuple(every)]


class Reduce:
    def __init__(self, chip, schedule, wave, grads, came, fin, sems, spare, write):
        self.wave, self.chip, self.schedule, self.widths, self.grads, self.came, self.fin = wave, chip, schedule, WAVES[wave], grads, came, fin
        (self.send_sem, self.recv_sem), (self.spare, self.spare_sem), self.write, self.times = sems, spare, write, {}

    def box(self, a, half, stage):
        order = ORDERS[a]
        ref = self.came[a][A].at[half, A]
        spot = [axis for axis in range(AXES) if axis != order[A]].index(order[B])
        if stage == B:
            return ref, spot, C
        return at_axis(ref, spot, self.chip.where[order[B]], C), A, B

    def copy(self, a, half, slot):
        stage, turn = divmod(slot, AXES)
        sems = self.send_sem.at[a, half, slot], self.recv_sem.at[a, half, slot]
        if slot == LAST:
            return remote(self.total(a, half).at[self.chip.other], self.fin[a].at[half], *sems, self.chip.partner())
        axis = ORDERS[a][stage]
        dst = self.came[a][CORES * stage + turn // C].at[half]
        value = self.chip.at(axis, (ONE, CROSS, TWO)[turn], half)
        if stage:
            ref, spot, n_axes = self.box(a, half, stage)
            src = at_axis(ref, spot, value, n_axes)
        else:
            src = self.came[a][A].at[half, B] if turn == C else at_axis(self.grads[a].at[half], axis, value, AXES)
        return remote(src, dst if turn == C else dst.at[turn], *sems, self.chip.device(axis, TWO if turn == C else ONE, half))

    def each(self, action):
        for a in range(AXES):
            halves(lambda half: action(a, half))

    def sending(self, slot):
        stage = slot // AXES
        share = SIDE ** (CORES * stage)
        self.times[slot] = self.schedule.now + US_HOP if slot == LAST else max(
            self.schedule.send(ORDERS[a][stage], self.widths[a] / share) for a in range(AXES))

    def begin(self):
        for slot in (B, A):
            self.each(lambda a, half: self.copy(a, half, slot).start())
            self.sending(slot)
        self.schedule.lines.append([
            (lambda slot=slot: self.times[slot], lambda k=k: self.step(k), lambda sent=sent: [self.sending(n) for n in sent],
             CORES * US_ADD * sum(self.widths) if k < C else US_STEP) for k, (slot, sent) in enumerate(STEPS)])

    def step(self, k):
        with jax.named_scope(f'w{self.wave}s{k}'):
            self.work(k)

    def work(self, k):
        (self.first, self.first, self.halve, self.settle, self.settle, self.halve, self.settle, self.settle, self.cross,
         self.finish)[k](*divmod(STEPS[k][A], AXES))

    def first(self, _, slot):
        def local(a, half):
            axis = ORDERS[a][A]
            return pltpu.make_async_copy(at_axis(self.grads[a].at[half], axis, self.chip.at(axis, TWO if slot else OWN, half), AXES),
                                         self.spare.at[half, :, :, :, :, pl.ds(0, self.widths[a])], self.spare_sem.at[half])
        for half in HALVES:
            local(A, half).start()
        for a in range(AXES):
            @halves
            def _(half):
                local(a, half).wait()
                self.copy(a, half, slot).wait_recv()
                add_into(self.came[a][A].at[half, slot], self.spare.at[half, :, :, :, :, pl.ds(0, self.widths[a])], C)
                if slot:
                    self.copy(a, half, C).start()
                if a < C:
                    local(a + 1, half).start()

    def halve(self, before, _):
        stage = before + 1

        def action(a, half):
            ref, spot, n_axes = self.box(a, half, stage)
            self.copy(a, half, AXES * before + C).wait_recv()
            for turn, role in ((B, CROSS), (A, ONE), (C, TWO), (C, OWN)):
                value = self.chip.at(ORDERS[a][stage], role, half)
                add_into(at_axis(ref, spot, value, n_axes), at_axis(self.came[a][stage + before].at[half], spot, value, n_axes),
                         n_axes - 1)
                if turn < C:
                    self.copy(a, half, AXES * stage + turn).start()
        self.each(action)

    def settle(self, stage, turn):
        def action(a, half):
            ref, spot, n_axes = self.box(a, half, stage)
            self.copy(a, half, AXES * stage + turn).wait_recv()
            value = self.chip.at(ORDERS[a][stage], TWO if turn else OWN, half)
            add_into(at_axis(ref, spot, value, n_axes), self.came[a][CORES * stage].at[half, turn], n_axes - 1)
            if turn:
                self.copy(a, half, AXES * stage + C).start()
        self.each(action)

    def total(self, a, half):
        ref, *_ = self.box(a, half, C)
        return ref.at[self.chip.where[ORDERS[a][C]]]

    def cross(self, *_):
        def action(a, half):
            self.copy(a, half, LAST - 1).wait_recv()
            add_into(self.total(a, half), self.came[a][-1].at[half], A)
            self.copy(a, half, LAST).start()
        self.each(action)

    def finish(self, *_):
        def action(a, half):
            self.write(a, half, self.chip.core, self.total(a, half)[self.chip.core])
            self.copy(a, half, LAST).wait_recv()
            self.write(a, half, self.chip.other, self.fin[a][half])
            self.copy(a, half, LAST).wait_send()
            for stage in range(AXES):
                block = self.came[a][CORES * stage].at[half, A]

                @loop(AXES)
                def _(turn):
                    sem = self.send_sem.at[a, half, AXES * stage + turn]
                    remote(block, block, sem, sem, self.chip.partner()).wait_send()
        self.each(action)


class VectorSum:
    def __init__(self, chip, schedule, total, came, sems, finish):
        self.schedule, self.total, self.came, self.sems, self.finish, self.ready = schedule, total, came, sems, finish, 0.0
        self.links = [axis for axis in range(AXES) for _ in HALVES] + [AXES]
        self.devices = [chip.device(axis, role, A) for axis in range(AXES) for role in (ONE, TWO)] + [chip.partner()]

    def copy(self, k):
        return remote(self.total, self.came.at[k], self.sems.at[A, k], self.sems.at[B, k], self.devices[k])

    def sending(self, k):
        if k < PARTNERS:
            self.ready = self.schedule.send(self.links[k], N_VEC / (SIDE * SIDE * ROWS * CORES))

    def step(self, k):
        with jax.named_scope(f'vec{k}'):
            self.copy(k - 1).wait()
            self.total[...] += self.came[k - 1]
        if k < PARTNERS:
            self.copy(k).start()
        else:
            self.finish()

    def begin(self):
        self.copy(A).start()
        self.sending(A)
        self.schedule.lines.append([
            (lambda: self.ready, lambda k=k: self.step(k), lambda k=k: self.sending(k), US_STEP) for k in range(1, PARTNERS + 1)])


def backward_kernel(ycot_ref, tables, vec_ref, sel_shard, sel_lane, up_hbm, down_hbm, mix_hbm, h_hbm, n1_hbm, n2_hbm, ctx_hbm,
                    act_hbm, qkv_hbm, pre_hbm, dx_hbm, small_ref, up_sum, down_sum, qkv_sum, out_sum, dout_cols, dpre_cols,
                    dqkv_cols, *refs):
    n_arrays, sums = AXES * len(WAVES), (up_sum, down_sum, qkv_sum, out_sum)
    grads, refs = refs[:n_arrays], refs[n_arrays:]
    (spare, tile_v, big_v, weight_v, rhs_v, wup_v, wdown_v, pre_v, dn1, dn2, dctx, dk_acc, dv_acc, qkv_v, dpre_v, dqkv_v, dh_v, h_v,
     total, came_vec, send_sem, recv_sem, spare_sem, tile_sem, big_sem, weight_sem, rhs_sem, mlp_sem, io_sem, own_sem, share_send,
     share_recv, pre_sem, vec_sem, credit, *refs) = refs
    fins, came = refs[:n_arrays], refs[n_arrays:]
    chip = enter()
    core, other = chip.core, chip.other
    dh_v[...] = ycot_ref[...]

    @loop(LAYERS)
    def _(turn_no):
        layer = LAYERS - 1 - turn_no
        schedule = Schedule()

        def half_copies(k, src, dst):
            width = dst.shape[-1]
            mine, away = [src.at[:, lanes(which * width, width)] for which in (core, other)]
            place = dst.at[layer, core]
            return start([pltpu.make_async_copy(mine, place, own_sem.at[k]), remote(away, place, share_send.at[k], share_recv.at[k], chip.partner())])

        def tokens_load(src, part, slot):
            return [pltpu.make_async_copy(src.at[layer, k, pl.ds(part * WIDTH, WIDTH)], big_v.at[slot, :, pl.ds(k * SEQ, SEQ)],
                                          big_sem.at[slot, k]) for k in range(CORES)]

        def weight_load(k, slot):
            return pltpu.make_async_copy(mix_hbm.at[layer, :, lanes(k * WIDTH, WIDTH)], weight_v.at[slot], weight_sem.at[slot])

        def rhs_load(src, first, width, slot):
            return [pltpu.make_async_copy(src.at[layer, k, :, lanes(first, width)],
                                          rhs_v.at[slot, pl.ds(k * SEQ, SEQ), pl.ds(0, width)], rhs_sem.at[slot, k])
                    for k in range(CORES)]

        def tile_loads(t, slot):
            rows = lanes(t * TILE, TILE)
            pairs = ((down_hbm.at[layer, rows], wdown_v), (pre_hbm.at[layer, t], pre_v), (up_hbm.at[layer, :, rows], wup_v))
            return [pltpu.make_async_copy(src, dst.at[slot], mlp_sem.at[slot, n]) for n, (src, dst) in enumerate(pairs)]

        def product(lhs_slot, rhs_slot, width, out_slot):
            value = dot(big_v[lhs_slot], rhs_v[rhs_slot, :, 0:width])
            tile_v[out_slot, :, :, :, :, :, 0:width] = value.reshape(CHIPS + (CORES, ROWS, width))

        def tile_out(slot, src, dst):
            return pltpu.make_async_copy(src, dst, tile_sem.at[slot])

        def tile_done(slot, width):
            block = tile_v.at[slot, :, :, :, :, :, pl.ds(0, width)]
            tile_out(slot, block, grads[C].at[layer, A, :, :, :, :, :, pl.ds(0, width)]).wait()

        def columns(wave, a, half, first, width):
            return grads[AXES * wave + a].at[layer, half, :, :, :, :, :, pl.ds(first, width)]

        def vector_at(k, first=0, width=None):
            return lanes(OFFSETS[k] + first, width or SIZES[k])

        def launch(wave):
            def write(a, half, side, block):
                def put(arr, group, col, first, width):
                    size = sums[arr].shape[-1] // CORES
                    sums[arr][layer, group, :, lanes(side * size + col, width)] = block[:, first:first + width].astype(BF16)
                width, colour = WAVES[wave][a], CORES * a + half
                if wave:
                    first = colour * width if wave == C or a < C else SIDE * WAVES[wave][A] + half * width
                    put(W_QKV if wave == C else W_UP, A, first, A, width)
                elif a < C:
                    put(W_DOWN, colour, A, A, width)
                else:
                    for k in HALVES:
                        put(W_DOWN, CORES * half + k, WAVES[A][A], k * PAIR, PAIR)
                    put(W_OUT, A, half * TWICE, TWICE, TWICE)

            @pl.when(turn_no > A)
            def _():
                pl.semaphore_wait(credit.at[wave], PARTNERS)

            where = slice(AXES * wave, AXES * (wave + 1))
            count = len(LEADS)
            Reduce(chip, schedule, wave, [grad.at[layer] for grad in grads[where]],
                   [came[count * (AXES * wave + a):count * (AXES * wave + a + 1)] for a in range(AXES)],
                   fins[where], (send_sem.at[wave], recv_sem.at[wave]), (spare, spare_sem), write).begin()

        out_share = half_copies(A, dh_v, dout_cols)
        start(tokens_load(act_hbm, A, A) + tokens_load(ctx_hbm, A, B) + [weight_load(PARTS, B), weight_load(A, A)])
        input_loads = start([pltpu.make_async_copy(qkv_hbm.at[layer], qkv_v, io_sem.at[A]),
                             pltpu.make_async_copy(h_hbm.at[layer], h_v, io_sem.at[B])])
        for t in HALVES:
            start(tile_loads(t, t))
        d_sum = column_sum(dh_v[...].astype(F32))
        total[:, vector_at(OUT_BIAS)] = d_sum
        total[:, vector_at(DOWN_BIAS)] = d_sum
        weight_load(PARTS, B).wait()
        dctx[...] = dot_t(dh_v[...], weight_v[B]).astype(BF16)
        weight_load(B, B).start()

        with jax.named_scope('dw0'):
            wait(out_share)
            wait(start(rhs_load(dout_cols, A, TILE, A)))
            wait(tokens_load(ctx_hbm, A, B))
            product(B, A, TILE, B)
            start(tokens_load(act_hbm, B, B))
            for k in HALVES:
                tile_out(B, tile_v.at[B, :, :, :, :, :, pl.ds(k * TWICE, TWICE)], columns(A, C, k, TWICE, TWICE)).start()

            @loop(SIDE)
            def _(z):
                slot = parity(z)
                wait(tokens_load(act_hbm, z, slot))

                @pl.when(z > A)
                def _():
                    tile_done(slot, TILE)

                product(slot, A, TILE, slot)

                @pl.when(z + CORES < SIDE)
                def _():
                    start(tokens_load(act_hbm, z + CORES, slot))

                split = WAVES[A][A]
                for k in range(SIDE):
                    a, half = divmod(k, CORES)
                    for c in range(CORES):
                        block = tile_v.at[slot, :, :, CORES * c + a, half]
                        tile_out(slot, block.at[:, :, :, pl.ds(0, split)], grads[a].at[layer, half, z, :, :, c]).start()
                        tile_out(slot, block.at[:, :, :, pl.ds(split, PAIR)],
                                 grads[C].at[layer, a, z, :, :, c, :, pl.ds(half * PAIR, PAIR)]).start()

            start(tokens_load(n2_hbm, A, A))
            for slot in HALVES:
                tile_done(slot, TILE)

        schedule.passed(US_FIRST)
        launch(A)

        dn2[...] = jnp.zeros_like(dn2)

        def pre_copy(t, slot, away):
            place = dpre_cols.at[layer, core, :, lanes(lax.rem(t, SIDE) * TILE, TILE)]
            if away:
                return remote(dpre_v.at[slot], place, pre_sem.at[A, t], pre_sem.at[B, t], chip.partner())
            return pltpu.make_async_copy(dpre_v.at[slot], place, own_sem.at[CORES + slot])

        def pre_act(t, leave):
            for away, whose in ((False, core), (True, other)):
                @pl.when(lax.div(t, SIDE) == whose)
                def _():
                    copy = pre_copy(t, parity(t), away)
                    if leave:
                        copy.start()
                    elif away:
                        copy.wait_send()
                    else:
                        copy.wait()

        tile_hooks = schedule.hooks(N_TILES, US_TILE)

        with jax.named_scope('mlp'):
            @loop(N_TILES)
            def _(t):
                slot = parity(t)
                wait(tile_loads(t, slot))
                d_act = rounded(dot_t(dh_v[...], wdown_v[slot]))
                pre = pre_v[slot]
                slope = 0.5 * (1.0 + lax.erf(pre * INV_SQRT2)) + pre * (INV_SQRT2PI * jnp.exp(-0.5 * pre * pre))
                d_pre = d_act * slope
                total[:, vector_at(UP_BIAS, t * TILE, TILE)] = column_sum(d_pre)

                @pl.when(t > B)
                def _():
                    pre_act(t - CORES, False)

                dpre_v[slot] = d_pre.astype(BF16)
                pre_act(t, True)
                dn2[...] += dot_t(dpre_v[slot], wup_v[slot])

                @pl.when(t + CORES < N_TILES)
                def _():
                    start(tile_loads(t + CORES, slot))

                at_hooks(t, tile_hooks)

        for t in HALVES:
            pre_act(N_TILES - CORES + t, False)
        for t in range(SIDE):
            pre_copy(SIDE * core + t, A, True).wait_recv()

        def gradient_wave(wave, source, first, orders):
            width = WAVES[wave][orders[0]]

            def load(k, slot):
                return rhs_load(source, first + k * width, width, slot)

            def out(k, slot):
                block = tile_v.at[slot, :, :, :, :, :, pl.ds(0, width)]
                for n, a in enumerate(orders):
                    @pl.when(lax.div(k, CORES) == n)
                    def _():
                        tile_out(slot, block, columns(wave, a, parity(k), 0, width)).start()

            count = CORES * len(orders)
            start(load(A, A))

            @loop(count)
            def _(k):
                slot = parity(k)
                wait(load(k, slot))

                @pl.when(k + 1 < count)
                def _():
                    start(load(k + 1, 1 - slot))

                @pl.when(k > B)
                def _():
                    tile_done(slot, width)

                product(A, slot, width, slot)
                out(k, slot)

            for slot in HALVES:
                tile_done(slot, width)

        wait(tokens_load(n2_hbm, A, A))
        with jax.named_scope('dw1'):
            gradient_wave(B, dpre_cols, A, (A, B))
            gradient_wave(B, dpre_cols, SIDE * WAVES[B][A], (C,))
        schedule.passed(US_UP)
        launch(B)
        start(tokens_load(n1_hbm, A, A))

        wait(input_loads)
        pair_hooks = schedule.hooks(N_PAIRS, US_PAIR)

        with jax.named_scope('attn'):
            @loop(N_PAIRS)
            def _(pair):
                at = lanes(pair * PAIR)
                keys = split_heads(qkv_v[:, lanes(WIDTH + pair * PAIR)])
                values = split_heads(qkv_v[:, lanes(C * WIDTH + pair * PAIR)])
                q_t = qkv_v[:, at].T
                dc_t = dctx[:, at].T
                bias_sums = [jnp.zeros((1, PAIR), F32)] * PARTS

                def turned_back(n, d, rows, to):
                    d = turn_back(rounded(d), *[tables[k, rows, :] for k in range(PARTS)])
                    bias_sums[n] = bias_sums[n] + column_sum(d)
                    dqkv_v[rows, to] = d.astype(BF16)

                for i in range(N_BLOCKS):
                    old, n = i * TWICE, (i + 1) * TWICE
                    rows = block_rows(i)
                    probs = probabilities(qkv_v[rows, at], keys[:n], i)
                    d_all = rounded(dot_t(dctx[rows, at], values[:n]))
                    d_scores = [d_all[:, block_rows(j)] for j in range(CORES * (i + 1))]
                    for head in HALVES:
                        mine = slice(head, None, CORES)
                        mean = row_sum(total_of([p * d for p, d in zip(probs[mine], d_scores[mine])]))
                        d_scores[mine] = [p * (d - mean) * SCALE for p, d in zip(probs[mine], d_scores[mine])]
                    d_scores, probs = side_by_side(d_scores), side_by_side(probs)
                    turned_back(A, dot(d_scores, keys[:n]), rows, at)
                    for acc, left, right in ((dk_acc, q_t, d_scores), (dv_acc, dc_t, probs)):
                        part = dot(left[:, rows], right)
                        if i:
                            acc[:, :old] += part[:, :old]
                        acc[:, old:n] = part[:, old:]
                first = iota((PAIR, PAIR), 0) < HEAD
                for j in range(N_BLOCKS):
                    rows = block_rows(j)
                    d_key, d_value = [jnp.where(first, acc[:, block_rows(CORES * j)], acc[:, block_rows(CORES * j + 1)]).T
                                      for acc in (dk_acc, dv_acc)]
                    turned_back(B, d_key, rows, lanes(WIDTH + pair * PAIR))
                    d_value = d_value.astype(BF16)
                    bias_sums[C] = bias_sums[C] + column_sum(d_value.astype(F32))
                    dqkv_v[rows, lanes(C * WIDTH + pair * PAIR)] = d_value
                for k, bias_sum in enumerate(bias_sums):
                    total[:, vector_at(QKV_BIAS, k * WIDTH + pair * PAIR, PAIR)] = bias_sum
                at_hooks(pair, pair_hooks)

        qkv_share = half_copies(B, dqkv_v, dqkv_cols)
        dn1[...] = jnp.zeros_like(dn1)

        with jax.named_scope('dn1'):
            @loop(PARTS)
            def _(k):
                slot = parity(k)
                weight_load(k, slot).wait()
                dn1[...] += dot_t(dqkv_v[:, lanes(k * WIDTH, WIDTH)], weight_v[slot])

                @pl.when(k == A)
                def _():
                    weight_load(C, A).start()

        for k in (GAIN1, BIAS1, GAIN2, BIAS2):
            total[:, vector_at(k)] = jnp.zeros((1, WIDTH), F32)

        with jax.named_scope('lnb'):
            @loop(SEQ // LN_ROWS)
            def _(r):
                rows = pl.ds(pl.multiple_of(r * LN_ROWS, LN_ROWS), LN_ROWS)
                scaled, inverse = normalised(h_v[rows, :].astype(F32))
                d1, d2 = rounded(dn1[rows, :]), rounded(dn2[rows, :])
                for k, value in ((GAIN1, d1 * scaled), (BIAS1, d1), (GAIN2, d2 * scaled), (BIAS2, d2)):
                    total[:, vector_at(k)] += column_sum(value)
                g1, g2 = [vec_ref[pl.ds(layer, 1), lanes(OFFSETS[k], WIDTH)] for k in (GAIN1, GAIN2)]
                d_scaled = d1 * g1 + d2 * g2
                d_h = inverse * (d_scaled - row_mean(d_scaled) - scaled * row_mean(d_scaled * scaled))
                dh_v[rows, :] = (dh_v[rows, :].astype(F32) + d_h).astype(BF16)

        schedule.passed(US_NORM)
        wait(qkv_share + tokens_load(n1_hbm, A, A))
        with jax.named_scope('dw2'):
            gradient_wave(C, dqkv_cols, A, (A, B, C))
        schedule.passed(US_QKV)

        def own_part():
            with jax.named_scope('own'):
                node, local = chip.base
                me = node * (SIDE * CORES) + local + core
                row = jnp.zeros((ROWS, PAIR), F32)
                for cols in vector_blocks():
                    left = jnp.zeros((ROWS, WIDTH), F32) + total[:, cols] * (sel_shard[:, cols] == me).astype(F32)
                    for _ in range(PARTS):
                        row = row + dot_t(left.astype(BF16), pick_lanes(sel_lane, cols))
                        left = left - rounded(left)
                small_ref[layer] = row.astype(BF16)

        launch(C)
        VectorSum(chip, schedule, total, came_vec, vec_sem, own_part).begin()
        schedule.run(None)

        @pl.when(turn_no == A)
        def _():
            for wave in range(len(WAVES)):
                chip.signal_partners(credit.at[wave])

    dx_copy = pltpu.make_async_copy(dh_v, dx_hbm, io_sem.at[A])
    dx_copy.start()
    dx_copy.wait()


def backward(y_cot, tables, vectors, places, weights, saved):
    dma, one = pltpu.SemaphoreType.DMA, (1,)
    pair, wide, row = (len(HALVES),), (SEQ, WIDTH), one + (N_VEC,)
    shapes = [(wide, BF16), ((LAYERS, ROWS, PAIR), BF16)]
    shapes += [((LAYERS, groups, ROWS, width), BF16) for groups, width in ((*one, HIDDEN), (SIDE, WIDTH), (*one, QKV), (*one, WIDTH))]
    in_vmem = len(shapes)
    shapes += [((LAYERS, CORES, SEQ, width), BF16) for width in (TILE, SIDE * TILE, PARTS * TILE)]
    blocks = [(CORES, ROWS, width) for wave in WAVES for width in wave]
    shapes += [((LAYERS,) + pair + CHIPS + block, F32) for block in blocks]
    tile = (CORES, ROWS, TILE)
    scratch = [(pair + CHIPS[1:] + tile, F32), (pair + CHIPS + tile, F32)]
    scratch += [(pair + shape, BF16) for shape in ((WIDTH, CORES * SEQ), (WIDTH, WIDTH), (CORES * SEQ, TILE), (WIDTH, TILE), (TILE, WIDTH))]
    scratch += [(pair + (SEQ, TILE), F32), (wide, F32), (wide, F32), (wide, BF16)] + [((PAIR, CORES * SEQ), F32)] * CORES
    scratch += [((SEQ, QKV), BF16), (pair + (SEQ, TILE), BF16), ((SEQ, QKV), BF16), (wide, BF16), (wide, BF16), (row, F32),
                ((PARTNERS,) + row, F32)]
    slots = (len(WAVES), AXES) + pair + (len(STEPS),)
    sems = [dma(shape) for shape in (slots, slots, pair, pair, pair + pair, pair, pair + pair, pair + (PARTS,), pair,
                                     (SIDE,), pair, pair, pair + (N_TILES,), pair + (PARTNERS,))]
    late = [(pair + block[1:], F32) for block in blocks] + [(pair + lead + block, F32) for block in blocks for lead in LEADS]
    outs = pl.pallas_call(
        backward_kernel,
        out_shape=[jax.ShapeDtypeStruct(*s) for s in shapes],
        in_specs=[IN_VMEM] * (SIDE + 1) + [ANY] * (AXES + PARTNERS),
        out_specs=[ANY] + [IN_VMEM] * (in_vmem - 1) + [ANY] * (len(shapes) - in_vmem),
        scratch_shapes=[pltpu.VMEM(*s) for s in scratch] + sems + [pltpu.SemaphoreType.REGULAR((len(WAVES),))]
        + [pltpu.VMEM(*s) for s in late],
        compiler_params=pltpu.CompilerParams(collective_id=1, has_side_effects=True, vmem_limit_bytes=VMEM_LIMIT),
        name='backward_layers',
    )(y_cot, tables, vectors, *places, *weights, *saved)
    d_x, small, *sums = outs[:in_vmem]
    return d_x, small[:, 0], [s.reshape((LAYERS, -1, s.shape[-1])) for s in sums]


def rope_tables():
    rot_dim = HEAD // SIDE
    inv_freq = 1.0 / (10000.0 ** (jnp.arange(0, rot_dim, 2, dtype=F32) / rot_dim))
    angles = jnp.arange(SEQ, dtype=F32)[:, None] * inv_freq[None, :]
    cos, sin = jnp.cos(angles), jnp.sin(angles)
    zero = jnp.zeros_like(sin)
    rest = jnp.zeros((SEQ, HEAD - rot_dim), F32)
    tables = ([cos, cos, rest + 1.0], [-sin, zero, rest], [zero, sin, rest])
    return jnp.stack([jnp.tile(jnp.concatenate(table, axis=1), (1, 2)) for table in tables])


def heads_last(tensor):
    lead = tensor.shape[:-2]
    return tensor.reshape(lead + (HEADS, PARTS, HEAD)).swapaxes(-3, -2).reshape(lead + (QKV,))


def heads_first(tensor):
    lead = tensor.shape[:-1]
    return tensor.reshape(lead + (PARTS, HEADS, HEAD)).swapaxes(-3, -2).reshape(lead + (HEADS, PARTS * HEAD))


def vector_places():
    shard, lane, first = [], [], 0
    for k, (share, size) in enumerate(zip(SHARES, SIZES)):
        place = np.arange(size)
        if k == QKV_BIAS:
            place = heads_last(place.reshape(HEADS, -1))
        shard.append(place // share)
        lane.append(first + place % share)
        first += share
    return [jnp.asarray(np.concatenate(part)[None].astype(np.int32)) for part in (shard, lane)]


def solution(mesh):
    shard_axes = ('node', 'local')
    act_spec = P(shard_axes)
    param_spec = P(None, shard_axes)

    def device_step(x, y_cot, ln1_gain, ln1_bias, qkv_weight, qkv_bias, out_weight, out_bias,
                    ln2_gain, ln2_bias, up_weight, up_bias, down_weight, down_bias):
        tables, places = rope_tables(), vector_places()
        small = (ln1_gain, ln1_bias, ln2_gain, ln2_bias, qkv_bias, out_bias, up_bias, down_bias)
        small_tile = jnp.pad(jnp.concatenate(small, axis=1), ((0, ROWS - LAYERS), (0, PAIR - sum(SHARES))))
        mix = jnp.concatenate([heads_last(qkv_weight), out_weight], axis=-1)
        *weights, _, vectors, y_out, hidden, n1, n2, ctx, act, qkv, pre = forward(
            x[0], (up_weight, down_weight, mix), small_tile, tables, places)
        weights = [tensor.reshape((LAYERS, -1, tensor.shape[-1])) for tensor in weights]
        d_x, small_sums, (up, down, qkv, out) = backward(
            y_cot[0], tables, vectors, places, weights, (hidden, n1, n2, ctx, act, qkv, pre))
        small_grads, first = [], 0
        for share in SHARES:
            small_grads.append(small_sums[:, first:first + share])
            first += share
        g1, b1, g2, b2, qb, ob, ub, db = small_grads
        return (y_out[None], d_x[None], g1, b1, heads_first(qkv), qb, out, ob, g2, b2, up, ub, down, db)

    return jax.shard_map(device_step, mesh=mesh,
                         in_specs=(act_spec, act_spec) + (param_spec,) * 12,
                         out_specs=(act_spec, act_spec) + (param_spec,) * 12,
                         check_vma=False)
```

```python
import functools
import jax
import jax.numpy as jnp
import numpy as np
from jax import lax
from jax.experimental import pallas as pl
from jax.experimental.pallas import tpu as pltpu
from jax.sharding import PartitionSpec as P

BF16, F32 = jnp.bfloat16, jnp.float32
EPSILON = 1e-5
MESH = pl.DeviceIdType.MESH
ANY = pl.BlockSpec(memory_space=pl.ANY)
IN_VMEM = pl.BlockSpec(memory_space=pltpu.VMEM)
VMEM_LIMIT = 67 * 10**6
LAYERS, AXES, SIDE, CORES, ROWS, PARTNERS = 2, 3, 4, 2, 8, 7
CHIPS = (SIDE, SIDE, SIDE)
SHARDS = SIDE * SIDE * SIDE * CORES
SEQ, WIDTH, HIDDEN, TILE, PAIR, LN_ROWS = 384, 1024, 4096, 512, 128, 64
HEADS, HEAD, PARTS = 16, 64, 3
QKV = PARTS * WIDTH
N_TILES, N_PAIRS, N_BLOCKS = HIDDEN // TILE, WIDTH // PAIR, SEQ // PAIR
TWICE = 2 * PAIR
INV_SQRT2, INV_SQRT2PI, SCALE = 0.7071067811865476, 0.3989422804014327, 0.125
SHARES = (8, 8, 8, 8, 24, 8, 32, 8)
SIZES = tuple(SHARDS * share for share in SHARES)
OFFSETS = tuple(sum(SIZES[:k]) for k in range(len(SIZES)))
N_VEC = sum(SIZES)
GAIN1, BIAS1, GAIN2, BIAS2, QKV_BIAS, OUT_BIAS, UP_BIAS, DOWN_BIAS = range(len(SHARES))
ORDERS = ((2, 1, 0), (1, 0, 2), (0, 2, 1))
HALVES = range(2)
OWN, ONE, CROSS, TWO = range(SIDE)
A, B, C = range(AXES)
UP, DOWN, MIX = range(3)
SELF = 3
PASSES = [(stage, step) for stage in range(AXES) for step in range(AXES)] + [(A, SELF)]


class Chip:
    def __init__(self):
        node, local = lax.axis_index('node'), lax.axis_index('local')
        self.core, self.other = lax.rem(local, CORES), 1 - lax.rem(local, CORES)
        self.where = (lax.div(node, SIDE), lax.rem(node, SIDE), lax.div(local, CORES))
        self.base = (node, local - self.core)
        self.strides = ((SIDE, 0), (1, 0), (0, CORES))
        self.near = [(v, v + 1 - 2 * parity(v), lax.rem(v + 2, SIDE), SIDE - 1 - v) for v in self.where]

        self.gaps = [near[3] - near[1] for near in self.near]

    def at(self, axis, role, half):
        near = self.near[axis]
        if role in (OWN, CROSS):
            return near[role]
        return near[role] + half * self.gaps[axis] if role == ONE else near[role] - half * self.gaps[axis]

    def device(self, axis, role, half):
        shift = self.at(axis, role, half) - self.where[axis]
        node, local = [b + shift * s if s else b for b, s in zip(self.base, self.strides[axis])]
        return (node, local + self.core)

    def partner(self):
        node, local = self.base
        return (node, local + self.other)

    def signal_partners(self, semaphore):
        for axis in range(AXES):
            for role in (ONE, TWO):
                pl.semaphore_signal(semaphore, inc=1, device_id=self.device(axis, role, A), device_id_type=MESH)
        pl.semaphore_signal(semaphore, inc=1, device_id=self.partner(), device_id_type=MESH)


def enter():
    chip = Chip()
    barrier = pltpu.get_barrier_semaphore()
    chip.signal_partners(barrier)
    pl.semaphore_wait(barrier, PARTNERS)
    return chip


def remote(src, dst, send_sem, recv_sem, device):
    return pltpu.make_async_remote_copy(src_ref=src, dst_ref=dst, send_sem=send_sem, recv_sem=recv_sem, device_id=device,
                                        device_id_type=MESH)


def start(copies):
    for copy in copies:
        copy.start()
    return copies


def wait(copies):
    for copy in copies:
        copy.wait()


def loop(count):
    return pl.loop(0, count)


def halves(body):
    loop(len(HALVES))(body)


def parity(n):
    return lax.rem(n, 2)


def pool(sems):
    return (sems.at[n] for n in range(sems.shape[0]))


def contract(a, b, a_axis, b_axis):
    return lax.dot_general(a, b, (((a_axis,), (b_axis,)), ((), ())), preferred_element_type=F32)


def dot(a, b):
    return contract(a, b, 1, 0)


def dot_t(a, b):
    return contract(a, b, 1, 1)


def row_sum(x):
    return jnp.sum(x, axis=1, keepdims=True)


def column_sum(x):
    return jnp.sum(x, axis=0, keepdims=True)


def rounded(x):
    return x.astype(BF16).astype(F32)


def lanes(first, width=PAIR):
    return pl.ds(pl.multiple_of(first, PAIR), width)


def turn(x, cos, sin_a, sin_b):
    return x * cos + pltpu.roll(x, PAIR - ROWS, 1) * sin_a + pltpu.roll(x, ROWS, 1) * sin_b


def turn_back(d, cos, sin_a, sin_b):
    return d * cos + pltpu.roll(d * sin_a, ROWS, 1) + pltpu.roll(d * sin_b, PAIR - ROWS, 1)


def iota(shape, axis):
    return lax.broadcasted_iota(jnp.int32, shape, axis)


def block_rows(j):
    return slice(j * PAIR, (j + 1) * PAIR)


def split_heads(x):
    first = iota((PAIR, PAIR), 1) < HEAD
    rows = []
    for j in range(N_BLOCKS):
        block = x[block_rows(j)]
        rows += [jnp.where(first, block, jnp.zeros_like(block)), jnp.where(first, jnp.zeros_like(block), block)]
    return jnp.concatenate(rows, axis=0)


def total_of(chunks, join=jnp.add):
    return functools.reduce(join, chunks)


def probabilities(q_block, keys, i):
    scores = dot_t(q_block, keys)
    causal = iota((PAIR, PAIR), 0) >= iota((PAIR, PAIR), 1)
    chunks = [scores[:, block_rows(j)] * SCALE for j in range(CORES * (i + 1))]
    for head in HALVES:
        mine = slice(head, None, CORES)
        *ahead, last = chunks[mine]
        held = ahead + [jnp.where(causal, last, -1e30)]
        top = jnp.max(total_of(held, jnp.maximum), axis=1, keepdims=True)
        held = [jnp.exp(chunk - top) for chunk in held]
        inverse = 1.0 / row_sum(total_of(held))
        chunks[mine] = [chunk * inverse for chunk in held]
    return chunks


def side_by_side(chunks):
    return jnp.concatenate([chunk.astype(BF16) for chunk in chunks], axis=1)


def row_mean(x):
    return jnp.mean(x, axis=1, keepdims=True)


def normalised(h):
    center = h - row_mean(h)
    inverse = lax.rsqrt(row_mean(center * center) + EPSILON)
    return center * inverse, inverse


class Gather:
    def __init__(self, chip, shards, fulls, sems):
        self.chip, self.shards, self.fulls = chip, shards, fulls
        self.send_sem, self.recv_sem, self.pass_send, self.pass_recv = sems

    def box(self, layer, k, half, stage, role, own=False):
        width = self.fulls[k].shape[-1] // len(HALVES)
        cols = lanes(half * width, width)
        if own:
            return self.shards[k].at[layer, :, cols]
        where = list(self.chip.where)
        for axis in ORDERS[k][:stage]:
            where[axis] = pl.ds(0, SIDE)
        axis = ORDERS[k][stage]
        where[axis] = self.chip.at(axis, role, half)
        return self.fulls[k].at[layer, where[0], where[1], where[2], self.chip.core, :, cols]

    def reach(self, layer, k, half, stage, step):
        slot, role = AXES * stage + step, ONE if step == C else OWN
        src = self.box(layer, k, half, stage, role, stage == A and step < C)
        return remote(src, self.box(layer, k, half, stage, role), self.send_sem.at[layer, k, half, slot],
                      self.recv_sem.at[layer, k, half, slot], self.chip.device(ORDERS[k][stage], TWO if step else ONE, half))

    def passing(self, layer, k, half, stage, step):
        role = (ONE, TWO, CROSS, OWN)[step]
        slot = AXES * AXES if step == SELF else AXES * stage + step
        return remote(self.box(layer, k, half, stage, role, step == SELF), self.box(layer, k, half, stage, role),
                      self.pass_send.at[layer, k, half, slot], self.pass_recv.at[layer, k, half, slot], self.chip.partner())

    def each(self, action):
        for k in (MIX, UP, DOWN):
            @halves
            def _(half):
                action(k, half)

    def begin(self, layer, stage):
        for step in HALVES:
            self.each(lambda k, half: self.reach(layer, k, half, stage, step).start())

    def own(self, layer):
        self.each(lambda k, half: self.passing(layer, k, half, A, SELF).start())

    def middle(self, layer, stage):
        def action(k, half):
            self.reach(layer, k, half, stage, A).wait_recv()
            self.reach(layer, k, half, stage, C).start()
            self.passing(layer, k, half, stage, A).start()
        self.each(action)

    def end(self, layer, stage, steps=(B, C)):
        def action(k, half):
            for step in steps:
                self.reach(layer, k, half, stage, step).wait_recv()
                self.passing(layer, k, half, stage, step).start()
        self.each(action)

    def arrived(self, layer, k):
        @halves
        def _(half):
            for stage, step in PASSES:
                self.passing(layer, k, half, stage, step).wait_recv()

    def left(self):
        def action(layer, k, half):
            for slot, (stage, step) in enumerate(PASSES):
                box = self.box(A, UP, A, stage, OWN, step == SELF)
                for sem in (self.pass_send,) if step == SELF else (self.send_sem, self.pass_send):
                    sem = sem.at[layer, k, half, slot]
                    remote(box, box, sem, sem, self.chip.partner()).wait_send()

        @loop(LAYERS)
        def _(layer):
            @loop(AXES)
            def _(k):
                halves(lambda half: action(layer, k, half))


def pick_lanes(sel_lane, cols):
    return (iota((PAIR, WIDTH), 0) == sel_lane[:, cols]).astype(F32).astype(BF16)


def vector_blocks():
    return [slice(k * WIDTH, (k + 1) * WIDTH) for k in range(N_VEC // WIDTH)]


def unpack_vectors(small_v, layer, sel_shard, sel_lane, vec_ref):
    tiles = small_v[...].astype(F32).reshape((SHARDS, ROWS, PAIR))
    held = jnp.sum(jnp.where(iota(tiles.shape, 1) == layer, tiles, 0.0), axis=1).astype(BF16)
    for cols in vector_blocks():
        spread = dot(held, pick_lanes(sel_lane, cols))
        spread = jnp.where(iota((SHARDS, WIDTH), 0) == sel_shard[:, cols], spread, 0.0)
        vec_ref[layer:layer + 1, cols] = column_sum(spread)


def forward_kernel(x_hbm, tables_hbm, places_hbm, up_s, down_s, mix_s, small_ref, up_f, down_f, mix_f, small_full, vec_ref,
                   y_hbm, h_hbm, n1_hbm, n2_hbm, ctx_hbm, act_hbm, qkv_hbm, pre_hbm, up_v, down_v, mix_v, small_v, acc, pre_v,
                   n1_v, n2_v, qkv_v, ctx_v, y_v, n1_t, n2_t, ctx_t, act_t, send_sem, recv_sem, pass_send, pass_recv,
                   small_send, small_recv, own_sems, load_sem, save_sem, share_send, share_recv, act_save, act_send, act_recv, tables,
                   places):
    shards, fulls, own_sem = (up_s, down_s, mix_s), (up_f, down_f, mix_f), pool(own_sems)
    chip = enter()
    gather = Gather(chip, shards, fulls, (send_sem, recv_sem, pass_send, pass_recv))

    def small_copy(slot, where, device):
        place = small_full.at[(*where, chip.core)]
        return remote(place, place, small_send.at[slot], small_recv.at[slot], device)

    def small_reach(stage, step):
        where = list(chip.where)
        for axis in range(stage):
            where[axis] = pl.ds(0, SIDE)
        where[stage] = chip.at(stage, ONE if step == C else OWN, A)
        return small_copy(AXES * stage + step, where, chip.device(stage, TWO if step else ONE, A))

    def small_begin(stage):
        small_reach(stage, A).start()
        small_reach(stage, B).start()

    def small_middle(stage):
        small_reach(stage, A).wait_recv()
        small_reach(stage, C).start()

    def small_end(stage):
        small_reach(stage, B).wait_recv()
        small_reach(stage, C).wait_recv()

    small_pass = small_copy(AXES * AXES, [pl.ds(0, SIDE)] * AXES, chip.partner())
    here = (*chip.where, chip.core)
    own = [pltpu.make_async_copy(small_ref, small_full.at[here], next(own_sem))]
    for shard, full in zip(shards, fulls):
        for layer in range(LAYERS):
            own.append(pltpu.make_async_copy(shard.at[layer], full.at[(layer, *here)], next(own_sem)))
    loads = [
        pltpu.make_async_copy(src, dst, next(own_sem)) for src, dst in ((x_hbm, y_v), (tables_hbm, tables), (places_hbm, places))]
    with jax.named_scope('ag0'):
        gather.begin(A, A)
        start(own)
        gather.begin(B, A)
        wait(own)
        small_begin(A)
        gather.own(A)
        gather.own(B)
        start(loads)
        gather.middle(A, A)
        small_middle(A)
        gather.middle(B, A)
        small_end(A)
        small_begin(B)
        gather.end(A, A)
    with jax.named_scope('ag1'):
        gather.begin(A, B)
        gather.end(B, A)
        small_middle(B)
        gather.begin(B, B)
        small_end(B)
        small_begin(C)
        gather.middle(A, B)
        small_middle(C)
        gather.middle(B, B)
        gather.end(A, B)
    with jax.named_scope('ag2_start'):
        gather.begin(A, C)
        small_end(C)
        small_pass.start()
        gather.end(B, B)
    with jax.named_scope('ag2_middle'):
        gather.middle(A, C)
        gather.begin(B, C)
    with jax.named_scope('unpack'):
        small_pass.wait_recv()
        fetch = pltpu.make_async_copy(small_full, small_v, next(own_sem))
        fetch.start()
        fetch.wait()
        wait(loads)
        for layer in range(LAYERS):
            unpack_vectors(small_v, layer, places[A:B], places[B:C], vec_ref)
    with jax.named_scope('ag2_late'):
        gather.end(A, C, (B,))
    with jax.named_scope('ag2_end'):
        gather.end(A, C, (C,))

    def saves(layer):
        pairs = [(y_v, h_hbm.at[layer]), (qkv_v, qkv_hbm.at[layer])]
        kept = [pltpu.make_async_copy(src, dst, save_sem.at[n]) for n, (src, dst) in enumerate(pairs)]
        for n, (src, dst) in enumerate(((n1_t, n1_hbm), (n2_t, n2_hbm), (ctx_t, ctx_hbm))):
            dst = dst.at[layer, chip.core]
            kept.append((pltpu.make_async_copy(src, dst, save_sem.at[CORES + n]),
                         remote(src, dst, share_send.at[layer, n], share_recv.at[layer, n], chip.partner())))
        return kept

    def quarter(layer, t):
        rows, tiles = pl.ds(t * WIDTH, WIDTH), pl.ds(CORES * t, CORES)
        src, dst = act_t.at[rows], act_hbm.at[layer, chip.core, rows]
        return [pltpu.make_async_copy(pre_v.at[tiles], pre_hbm.at[layer, tiles], act_save.at[A, t]),
                pltpu.make_async_copy(src, dst, act_save.at[B, t]),
                remote(src, dst, act_send.at[layer, t], act_recv.at[layer, t], chip.partner())]

    def settle(layer):
        _, qkv_save, *shares = saves(layer)
        qkv_save.wait()
        for share in shares:
            wait(share)

        @loop(SIDE)
        def _(t):
            wait(quarter(layer, t))

    @loop(LAYERS)
    def _(layer):
        def vector(k, first=0, width=None):
            return vec_ref[pl.ds(layer, 1), lanes(OFFSETS[k] + first, width or SIZES[k])]

        def load(k, piece):
            if k == DOWN:
                return pltpu.make_async_copy(fulls[k].at[layer, piece], down_v.at[piece], load_sem.at[k, piece])
            cols = lanes(piece * WIDTH, WIDTH)
            return pltpu.make_async_copy(fulls[k].at[layer, :, :, :, :, :, cols], (up_v, None, mix_v)[k].at[:, :, :, :, :, cols],
                                         load_sem.at[k, piece])

        def matrix(held, piece):
            return held[:, :, :, :, :, lanes(piece * WIDTH, WIDTH)].reshape((WIDTH, WIDTH))

        def have(k):
            for which in range(LAYERS):
                @pl.when(layer == which)
                def _():
                    gather.arrived(which, k)

        def meanwhile(action):
            @pl.when(layer == A)
            def _():
                action()

        h_save, qkv_save, n1_share, n2_share, ctx_share = saves(layer)
        with jax.named_scope('have_mix'):
            have(MIX)
            start([load(MIX, k) for k in range(SIDE)])

        h_save.start()

        @pl.when(layer == B)
        def _():
            settle(A)

        with jax.named_scope('ln'):
            @loop(SEQ // LN_ROWS)
            def _(r):
                rows = pl.ds(pl.multiple_of(r * LN_ROWS, LN_ROWS), LN_ROWS)
                scaled, _ = normalised(y_v[rows, :].astype(F32))
                n1_v[rows, :] = (scaled * vector(GAIN1) + vector(BIAS1)).astype(BF16)
                n2_v[rows, :] = (scaled * vector(GAIN2) + vector(BIAS2)).astype(BF16)

        for src, dst, share in ((n1_v, n1_t, n1_share), (n2_v, n2_t, n2_share)):
            dst[...] = src[...].T
            start(share)

        with jax.named_scope('qkv'):
            @loop(PARTS)
            def _(k):
                load(MIX, k).wait()
                x = dot(n1_v[...], matrix(mix_v, k)) + vector(QKV_BIAS, k * WIDTH, WIDTH)

                @pl.when(k < C)
                def _():
                    for c in range(N_PAIRS):
                        block = turn(x[:, block_rows(c)], *[tables[n] for n in range(PARTS)])
                        qkv_v[:, lanes(k * WIDTH + c * PAIR)] = block.astype(BF16)

                @pl.when(k == C)
                def _():
                    qkv_v[:, lanes(k * WIDTH, WIDTH)] = x.astype(BF16)

        qkv_save.start()
        with jax.named_scope('have_up'):
            have(UP)
            have(DOWN)

        start([load(UP, k) for k in range(SIDE)] + [load(DOWN, k) for k in range(SIDE)])
        with jax.named_scope('mid'):
            meanwhile(lambda: gather.middle(B, C))

        with jax.named_scope('fattn'):
            @loop(N_PAIRS)
            def _(pair):
                keys = split_heads(qkv_v[:, lanes(WIDTH + pair * PAIR)])
                values = split_heads(qkv_v[:, lanes(C * WIDTH + pair * PAIR)])
                for i in range(N_BLOCKS):
                    n = (i + 1) * CORES * PAIR
                    probs = probabilities(qkv_v[block_rows(i), lanes(pair * PAIR)], keys[:n], i)
                    ctx_v[block_rows(i), lanes(pair * PAIR)] = dot(side_by_side(probs), values[:n]).astype(BF16)

        ctx_t[...] = ctx_v[...].T
        start(ctx_share)
        meanwhile(lambda: gather.end(B, C, (B,)))
        with jax.named_scope('fout'):
            load(MIX, PARTS).wait()
            acc[...] = y_v[...].astype(F32) + dot(ctx_v[...], matrix(mix_v, PARTS)) + (vector(OUT_BIAS) + vector(DOWN_BIAS))

        with jax.named_scope('fmlp'):
            @loop(SIDE)
            def _(t):
                cols = lanes(t * WIDTH, WIDTH)
                load(UP, t).wait()
                pre = dot(n2_v[...], matrix(up_v, t)) + vector(UP_BIAS, t * WIDTH, WIDTH)
                for k in HALVES:
                    pre_v[CORES * t + k] = pre[:, k * TILE:(k + 1) * TILE]
                act = (0.5 * pre * (1.0 + lax.erf(pre * INV_SQRT2))).astype(BF16)
                act_t[cols, :] = act.T
                start(quarter(layer, t))
                load(DOWN, t).wait()
                acc[...] += dot(act, down_v[t].reshape((WIDTH, WIDTH)))

        h_save.wait()
        y_v[...] = acc[...].astype(BF16)
        with jax.named_scope('fend'):
            meanwhile(lambda: gather.end(B, C, (C,)))

    with jax.named_scope('ftail'):
        last = pltpu.make_async_copy(y_v, y_hbm, next(own_sem))
        last.start()
        for stage in range(AXES):
            for step in range(AXES):
                small_reach(stage, step).wait_send()
        small_pass.wait_send()
        gather.left()
        settle(LAYERS - 1)
        last.wait()


def forward(x, shards, small_tile, tables, places):
    grid = CHIPS + (CORES,)
    full = [(LAYERS,) + grid + tensor.shape[1:] for tensor in shards]
    shapes = [(shape, BF16) for shape in full] + [(grid + small_tile.shape, BF16), ((LAYERS, N_VEC), F32), ((SEQ, WIDTH), BF16),
                                                  ((LAYERS, SEQ, WIDTH), BF16)]
    shapes += [((LAYERS, CORES, width, SEQ), BF16) for width in (WIDTH, WIDTH, WIDTH, HIDDEN)]
    shapes += [((LAYERS, SEQ, QKV), BF16), ((LAYERS, N_TILES, SEQ, TILE), F32)]
    dma = pltpu.SemaphoreType.DMA
    slots = AXES * AXES
    scratch = [pltpu.VMEM(shape[1:], BF16) for shape in full] + [pltpu.VMEM(grid + small_tile.shape, BF16)]
    scratch += [pltpu.VMEM((SEQ, WIDTH), F32), pltpu.VMEM((N_TILES, SEQ, TILE), F32)]
    scratch += [pltpu.VMEM((SEQ, width), BF16) for width in (WIDTH, WIDTH, QKV, WIDTH, WIDTH)]
    scratch += [pltpu.VMEM((width, SEQ), BF16) for width in (WIDTH, WIDTH, WIDTH, HIDDEN)]
    scratch += [dma((LAYERS, AXES, len(HALVES), n)) for n in (slots, slots, slots + 1, slots + 1)]
    scratch += [dma(shape) for shape in ((slots + 1,), (slots + 1,), (slots + PARTNERS,), (AXES, SIDE), (SIDE + 1,), (LAYERS, AXES), (LAYERS, AXES), (CORES, SIDE), (LAYERS, SIDE), (LAYERS, SIDE))]
    scratch += [pltpu.VMEM(tables.shape, F32), pltpu.VMEM(places.shape, jnp.int32)]
    out_specs = [IN_VMEM if dtype == F32 and len(shape) == LAYERS else ANY for shape, dtype in shapes]
    return pl.pallas_call(
        forward_kernel,
        out_shape=[jax.ShapeDtypeStruct(*s) for s in shapes],
        in_specs=[ANY] * AXES + [IN_VMEM] * SIDE,
        out_specs=out_specs,
        scratch_shapes=scratch,
        compiler_params=pltpu.CompilerParams(collective_id=0, has_side_effects=True, vmem_limit_bytes=VMEM_LIMIT),
        name='forward_layers',
    )(x, tables, places, *shards, small_tile)


WAVES = ((384, 384, 512), (384, 384, 256), (256, 256, 256))
LEADS = ((2,) + CHIPS[1:], CHIPS[1:], (2, SIDE), (SIDE,), (2,), ())
W_UP, W_DOWN, W_QKV, W_OUT = range(4)
STEPS = ((1, (2,)), (0, ()), (2, (4, 3)), (4, (5,)), (3, ()), (5, (7, 6)), (7, (8,)), (6, ()), (8, (9,)), (9, ()))
LAST = AXES * AXES
US_COLUMN, US_HOP, US_ADD, US_STEP = 0.022, 2.5, 0.0013, 0.2
US_FIRST, US_TILE, US_GRADIENT, US_PAIR, US_NORM = 10, 1.5, 0.004, 2.15, 6


class Schedule:
    def __init__(self):
        self.now, self.free, self.lines = 0.0, {}, []

    def send(self, link, columns):
        self.free[link] = max(self.free.get(link, 0.0), self.now) + columns * US_COLUMN
        return self.free[link] + US_HOP

    def due(self, limit):
        found = []
        while self.lines:
            line = min(self.lines, key=lambda one: one[A][A]())
            ready = line[A][A]()
            if limit is not None and ready > limit:
                break
            _, run, sends, cost = line.pop(A)
            self.lines = [one for one in self.lines if one]
            self.now = max(self.now, ready) + cost
            sends()
            found.append(run)
        return found

    def run(self, limit):
        for step in self.due(limit):
            step()

    def passed(self, cost):
        self.now += cost
        self.run(self.now)

    def hooks(self, count, cost):
        planned = []
        for _ in range(count):
            self.now += cost
            planned.append(self.due(self.now))
        return planned


def at_hooks(n, planned):
    for when, steps in enumerate(planned):
        if steps:
            @pl.when(n == when)
            def _():
                for step in steps:
                    step()


def add_into(dst, src, n_axes):
    if n_axes < 2:
        dst[...] += src[...]
        return

    @loop(SIDE)
    def _(k):
        dst[k] += src[k]


def at_axis(ref, axis, value, n_axes):
    every = [pl.ds(0, SIDE)] * n_axes
    every[axis] = value
    return ref.at[tuple(every)]


class Reduce:
    def __init__(self, chip, schedule, wave, grads, came, fin, sems, spare, write):
        self.wave, self.chip, self.schedule, self.widths, self.grads, self.came, self.fin = wave, chip, schedule, WAVES[wave], grads, came, fin
        (self.send_sem, self.recv_sem), (self.spare, self.spare_sem), self.write, self.times = sems, spare, write, {}

    def box(self, a, half, stage):
        order = ORDERS[a]
        ref = self.came[a][A].at[half, A]
        spot = [axis for axis in range(AXES) if axis != order[A]].index(order[B])
        if stage == B:
            return ref, spot, C
        return at_axis(ref, spot, self.chip.where[order[B]], C), A, B

    def copy(self, a, half, slot):
        stage, turn = divmod(slot, AXES)
        sems = self.send_sem.at[a, half, slot], self.recv_sem.at[a, half, slot]
        if slot == LAST:
            return remote(self.total(a, half).at[self.chip.other], self.fin[a].at[half], *sems, self.chip.partner())
        axis = ORDERS[a][stage]
        dst = self.came[a][CORES * stage + turn // C].at[half]
        value = self.chip.at(axis, (ONE, CROSS, TWO)[turn], half)
        if stage:
            ref, spot, n_axes = self.box(a, half, stage)
            src = at_axis(ref, spot, value, n_axes)
        else:
            src = self.came[a][A].at[half, B] if turn == C else at_axis(self.grads[a].at[half], axis, value, AXES)
        return remote(src, dst if turn == C else dst.at[turn], *sems, self.chip.device(axis, TWO if turn == C else ONE, half))

    def each(self, action):
        for a in range(AXES):
            halves(lambda half: action(a, half))

    def sending(self, slot):
        stage = slot // AXES
        share = SIDE ** (CORES * stage)
        self.times[slot] = self.schedule.now + US_HOP if slot == LAST else max(
            self.schedule.send(ORDERS[a][stage], self.widths[a] / share) for a in range(AXES))

    def begin(self):
        for slot in (B, A):
            self.each(lambda a, half: self.copy(a, half, slot).start())
            self.sending(slot)
        self.schedule.lines.append([
            (lambda slot=slot: self.times[slot], lambda k=k: self.step(k), lambda sent=sent: [self.sending(n) for n in sent],
             CORES * US_ADD * sum(self.widths) if k < C else US_STEP) for k, (slot, sent) in enumerate(STEPS)])

    def step(self, k):
        with jax.named_scope(f'w{self.wave}s{k}'):
            self.work(k)

    def work(self, k):
        (self.first, self.first, self.halve, self.settle, self.settle, self.halve, self.settle, self.settle, self.cross,
         self.finish)[k](*divmod(STEPS[k][A], AXES))

    def first(self, _, slot):
        def local(a, half, piece=None):
            axis = ORDERS[a][A]
            src = at_axis(self.grads[a].at[half], axis, self.chip.at(axis, TWO if slot else OWN, half), AXES)
            dst = self.spare.at[half, :, :, :, :, pl.ds(0, self.widths[a])]
            if piece is not None:
                src, dst = src.at[piece], dst.at[piece]
            return pltpu.make_async_copy(src, dst, self.spare_sem.at[half])

        def begin(a, half):
            loop(SIDE)(lambda piece: local(a, half, piece).start())

        halves(lambda half: begin(A, half))
        for a in range(AXES):
            @halves
            def _(half):
                local(a, half).wait()
                self.copy(a, half, slot).wait_recv()
                add_into(self.came[a][A].at[half, slot], self.spare.at[half, :, :, :, :, pl.ds(0, self.widths[a])], C)
                if slot:
                    self.copy(a, half, C).start()
                if a < C:
                    begin(a + 1, half)

    def halve(self, before, _):
        stage = before + 1

        def action(a, half):
            ref, spot, n_axes = self.box(a, half, stage)
            self.copy(a, half, AXES * before + C).wait_recv()
            for turn, role in ((B, CROSS), (A, ONE), (C, TWO), (C, OWN)):
                value = self.chip.at(ORDERS[a][stage], role, half)
                add_into(at_axis(ref, spot, value, n_axes), at_axis(self.came[a][stage + before].at[half], spot, value, n_axes),
                         n_axes - 1)
                if turn < C:
                    self.copy(a, half, AXES * stage + turn).start()
        self.each(action)

    def settle(self, stage, turn):
        def action(a, half):
            ref, spot, n_axes = self.box(a, half, stage)
            self.copy(a, half, AXES * stage + turn).wait_recv()
            value = self.chip.at(ORDERS[a][stage], TWO if turn else OWN, half)
            add_into(at_axis(ref, spot, value, n_axes), self.came[a][CORES * stage].at[half, turn], n_axes - 1)
            if turn:
                self.copy(a, half, AXES * stage + C).start()
        self.each(action)

    def total(self, a, half):
        ref, *_ = self.box(a, half, C)
        return ref.at[self.chip.where[ORDERS[a][C]]]

    def cross(self, *_):
        def action(a, half):
            self.copy(a, half, LAST - 1).wait_recv()
            add_into(self.total(a, half), self.came[a][-1].at[half], A)
            self.copy(a, half, LAST).start()
        self.each(action)

    def finish(self, *_):
        def action(a, half):
            self.write(a, half, self.chip.core, self.total(a, half)[self.chip.core])
            self.copy(a, half, LAST).wait_recv()
            self.write(a, half, self.chip.other, self.fin[a][half])
            self.copy(a, half, LAST).wait_send()
            for stage in range(AXES):
                block = self.came[a][CORES * stage].at[half, A]

                @loop(AXES)
                def _(turn):
                    sem = self.send_sem.at[a, half, AXES * stage + turn]
                    remote(block, block, sem, sem, self.chip.partner()).wait_send()
        self.each(action)


class VectorSum:
    def __init__(self, chip, schedule, total, came, sems, finish):
        self.schedule, self.total, self.came, self.sems, self.finish, self.ready = schedule, total, came, sems, finish, 0.0
        self.links = [axis for axis in range(AXES) for _ in HALVES] + [AXES]
        self.devices = [chip.device(axis, role, A) for axis in range(AXES) for role in (ONE, TWO)] + [chip.partner()]

    def copy(self, k):
        return remote(self.total, self.came.at[k], self.sems.at[A, k], self.sems.at[B, k], self.devices[k])

    def sending(self, k):
        if k < PARTNERS:
            self.ready = self.schedule.send(self.links[k], N_VEC / (SIDE * SIDE * ROWS * CORES))

    def step(self, k):
        with jax.named_scope(f'vec{k}'):
            self.copy(k - 1).wait()
            self.total[...] += self.came[k - 1]
        if k < PARTNERS:
            self.copy(k).start()
        else:
            self.finish()

    def begin(self):
        self.copy(A).start()
        self.sending(A)
        self.schedule.lines.append([
            (lambda: self.ready, lambda k=k: self.step(k), lambda k=k: self.sending(k), US_STEP) for k in range(1, PARTNERS + 1)])


def backward_kernel(ycot_ref, tables, vec_ref, places, up_hbm, down_hbm, mix_hbm, h_hbm, n1_hbm, n2_hbm, ctx_hbm,
                    act_hbm, qkv_hbm, pre_hbm, dx_hbm, small_ref, up_sum, down_sum, qkv_sum, out_sum, dout_cols, dpre_cols,
                    dqkv_cols, *refs):
    n_arrays, sums = AXES * len(WAVES), (up_sum, down_sum, qkv_sum, out_sum)
    grads, refs = refs[:n_arrays], refs[n_arrays:]
    (spare, tile_v, big_v, weight_v, rhs_v, wup_v, wdown_v, pre_v, dn1, dn2, dctx, dk_acc, dv_acc, qkv_v, dpre_v, dqkv_v, dh_v, h_v,
     total, came_vec, send_sem, recv_sem, spare_sem, tile_sem, big_sem, weight_sem, rhs_sem, mlp_sem, io_sem, own_sem, share_send,
     share_recv, pre_sem, vec_sem, credit, *refs) = refs
    fins, came = refs[:n_arrays], refs[n_arrays:]
    chip = enter()
    core, other = chip.core, chip.other
    dh_v[...] = ycot_ref[...]

    @loop(LAYERS)
    def _(turn_no):
        layer = LAYERS - 1 - turn_no
        schedule = Schedule()

        def half_copies(k, src, dst):
            width = dst.shape[-1]
            mine, away = [src.at[:, lanes(which * width, width)] for which in (core, other)]
            place = dst.at[layer, core]
            return start([pltpu.make_async_copy(mine, place, own_sem.at[k]), remote(away, place, share_send.at[k], share_recv.at[k], chip.partner())])

        def tokens_load(src, part, slot):
            return [pltpu.make_async_copy(src.at[layer, k, pl.ds(part * WIDTH, WIDTH)], big_v.at[slot, :, pl.ds(k * SEQ, SEQ)],
                                          big_sem.at[slot, k]) for k in range(CORES)]

        def weight_load(k, slot):
            return pltpu.make_async_copy(mix_hbm.at[layer, :, lanes(k * WIDTH, WIDTH)], weight_v.at[slot], weight_sem.at[slot])

        def rhs_load(src, first, width, slot):
            return [pltpu.make_async_copy(src.at[layer, k, :, lanes(first, width)],
                                          rhs_v.at[slot, pl.ds(k * SEQ, SEQ), pl.ds(0, width)], rhs_sem.at[slot, k])
                    for k in range(CORES)]

        def tile_loads(t, slot):
            rows = lanes(t * TILE, TILE)
            pairs = ((down_hbm.at[layer, rows], wdown_v), (pre_hbm.at[layer, t], pre_v), (up_hbm.at[layer, :, rows], wup_v))
            return [pltpu.make_async_copy(src, dst.at[slot], mlp_sem.at[slot, n]) for n, (src, dst) in enumerate(pairs)]

        def product(lhs_slot, rhs_slot, width, out_slot):
            value = dot(big_v[lhs_slot], rhs_v[rhs_slot, :, 0:width])
            tile_v[out_slot, :, :, :, :, :, 0:width] = value.reshape(CHIPS + (CORES, ROWS, width))

        def tile_out(slot, src, dst):
            return pltpu.make_async_copy(src, dst, tile_sem.at[slot])

        def tile_done(slot, width):
            block = tile_v.at[slot, :, :, :, :, :, pl.ds(0, width)]
            tile_out(slot, block, grads[C].at[layer, A, :, :, :, :, :, pl.ds(0, width)]).wait()

        def columns(wave, a, half, first, width):
            return grads[AXES * wave + a].at[layer, half, :, :, :, :, :, pl.ds(first, width)]

        def vector_at(k, first=0, width=None):
            return lanes(OFFSETS[k] + first, width or SIZES[k])

        def launch(wave):
            def write(a, half, side, block):
                def put(arr, group, col, first, width):
                    size = sums[arr].shape[-1] // CORES
                    sums[arr][layer, group, :, lanes(side * size + col, width)] = block[:, first:first + width].astype(BF16)
                width, colour = WAVES[wave][a], CORES * a + half
                if wave:
                    first = colour * width if wave == C or a < C else SIDE * WAVES[wave][A] + half * width
                    put(W_QKV if wave == C else W_UP, A, first, A, width)
                elif a < C:
                    put(W_DOWN, colour, A, A, width)
                else:
                    for k in HALVES:
                        put(W_DOWN, CORES * half + k, WAVES[A][A], k * PAIR, PAIR)
                    put(W_OUT, A, half * TWICE, TWICE, TWICE)

            @pl.when(turn_no > A)
            def _():
                pl.semaphore_wait(credit.at[wave], PARTNERS)

            where = slice(AXES * wave, AXES * (wave + 1))
            count = len(LEADS)
            Reduce(chip, schedule, wave, [grad.at[layer] for grad in grads[where]],
                   [came[count * (AXES * wave + a):count * (AXES * wave + a + 1)] for a in range(AXES)],
                   fins[where], (send_sem.at[wave], recv_sem.at[wave]), (spare, spare_sem), write).begin()

        out_share = half_copies(A, dh_v, dout_cols)
        start(tokens_load(act_hbm, A, A) + tokens_load(ctx_hbm, A, B) + [weight_load(PARTS, B), weight_load(A, A)])
        input_loads = start([pltpu.make_async_copy(qkv_hbm.at[layer], qkv_v, io_sem.at[A]),
                             pltpu.make_async_copy(h_hbm.at[layer], h_v, io_sem.at[B])])
        for t in HALVES:
            start(tile_loads(t, t))
        d_sum = column_sum(dh_v[...].astype(F32))
        total[:, vector_at(OUT_BIAS)] = d_sum
        total[:, vector_at(DOWN_BIAS)] = d_sum
        weight_load(PARTS, B).wait()
        dctx[...] = dot_t(dh_v[...], weight_v[B]).astype(BF16)
        weight_load(B, B).start()

        with jax.named_scope('dw0'):
            wait(out_share)
            wait(start(rhs_load(dout_cols, A, TILE, A)))
            wait(tokens_load(ctx_hbm, A, B))
            product(B, A, TILE, B)
            start(tokens_load(act_hbm, B, B))
            for k in HALVES:
                tile_out(B, tile_v.at[B, :, :, :, :, :, pl.ds(k * TWICE, TWICE)], columns(A, C, k, TWICE, TWICE)).start()

            @loop(SIDE)
            def _(z):
                slot = parity(z)
                wait(tokens_load(act_hbm, z, slot))

                @pl.when(z > A)
                def _():
                    tile_done(slot, TILE)

                product(slot, A, TILE, slot)

                @pl.when(z + CORES < SIDE)
                def _():
                    start(tokens_load(act_hbm, z + CORES, slot))

                split = WAVES[A][A]
                for k in range(SIDE):
                    a, half = divmod(k, CORES)
                    for c in range(CORES):
                        block = tile_v.at[slot, :, :, CORES * c + a, half]
                        tile_out(slot, block.at[:, :, :, pl.ds(0, split)], grads[a].at[layer, half, z, :, :, c]).start()
                        tile_out(slot, block.at[:, :, :, pl.ds(split, PAIR)],
                                 grads[C].at[layer, a, z, :, :, c, :, pl.ds(half * PAIR, PAIR)]).start()

            start(tokens_load(n2_hbm, A, A))
            for slot in HALVES:
                tile_done(slot, TILE)

        schedule.passed(US_FIRST)
        launch(A)

        dn2[...] = jnp.zeros_like(dn2)

        def pre_copy(t, slot, away):
            place = dpre_cols.at[layer, core, :, lanes(lax.rem(t, SIDE) * TILE, TILE)]
            if away:
                return remote(dpre_v.at[slot], place, pre_sem.at[A, t], pre_sem.at[B, t], chip.partner())
            return pltpu.make_async_copy(dpre_v.at[slot], place, own_sem.at[CORES + slot])

        def pre_act(t, leave):
            for away, whose in ((False, core), (True, other)):
                @pl.when(lax.div(t, SIDE) == whose)
                def _():
                    copy = pre_copy(t, parity(t), away)
                    if leave:
                        copy.start()
                    elif away:
                        copy.wait_send()
                    else:
                        copy.wait()

        tile_hooks = schedule.hooks(N_TILES, US_TILE)

        with jax.named_scope('mlp'):
            @loop(N_TILES)
            def _(t):
                slot = parity(t)
                wait(tile_loads(t, slot))
                d_act = rounded(dot_t(dh_v[...], wdown_v[slot]))
                pre = pre_v[slot]
                slope = 0.5 * (1.0 + lax.erf(pre * INV_SQRT2)) + pre * (INV_SQRT2PI * jnp.exp(-0.5 * pre * pre))
                d_pre = d_act * slope
                total[:, vector_at(UP_BIAS, t * TILE, TILE)] = column_sum(d_pre)

                @pl.when(t > B)
                def _():
                    pre_act(t - CORES, False)

                dpre_v[slot] = d_pre.astype(BF16)
                pre_act(t, True)
                dn2[...] += dot_t(dpre_v[slot], wup_v[slot])

                @pl.when(t + CORES < N_TILES)
                def _():
                    start(tile_loads(t + CORES, slot))

                at_hooks(t, tile_hooks)

        for t in HALVES:
            pre_act(N_TILES - CORES + t, False)
        for t in range(SIDE):
            pre_copy(SIDE * core + t, A, True).wait_recv()

        def gradient_wave(wave, source, first, orders):
            width = WAVES[wave][orders[0]]

            def load(k, slot):
                return rhs_load(source, first + k * width, width, slot)

            def out(k, slot):
                block = tile_v.at[slot, :, :, :, :, :, pl.ds(0, width)]
                for n, a in enumerate(orders):
                    @pl.when(lax.div(k, CORES) == n)
                    def _():
                        place = columns(wave, a, parity(k), 0, width)
                        start([tile_out(slot, block.at[z], place.at[z]) for z in range(SIDE)])

            count = CORES * len(orders)
            planned = schedule.hooks(count, width * US_GRADIENT)
            start(load(A, A))

            @loop(count)
            def _(k):
                slot = parity(k)
                wait(load(k, slot))

                @pl.when(k + 1 < count)
                def _():
                    start(load(k + 1, 1 - slot))

                @pl.when(k > B)
                def _():
                    tile_done(slot, width)

                product(A, slot, width, slot)
                out(k, slot)
                at_hooks(k, planned)

            for slot in HALVES:
                tile_done(slot, width)

        wait(tokens_load(n2_hbm, A, A))
        with jax.named_scope('dw1'):
            gradient_wave(B, dpre_cols, A, (A, B))
            gradient_wave(B, dpre_cols, SIDE * WAVES[B][A], (C,))
        launch(B)
        start(tokens_load(n1_hbm, A, A))

        wait(input_loads)
        pair_hooks = schedule.hooks(N_PAIRS, US_PAIR)

        with jax.named_scope('attn'):
            @loop(N_PAIRS)
            def _(pair):
                at = lanes(pair * PAIR)
                keys = split_heads(qkv_v[:, lanes(WIDTH + pair * PAIR)])
                values = split_heads(qkv_v[:, lanes(C * WIDTH + pair * PAIR)])
                q_t = qkv_v[:, at].T
                dc_t = dctx[:, at].T
                bias_sums = [jnp.zeros((1, PAIR), F32)] * PARTS

                def turned_back(n, d, rows, to):
                    d = turn_back(rounded(d), *[tables[k, rows, :] for k in range(PARTS)])
                    bias_sums[n] = bias_sums[n] + column_sum(d)
                    dqkv_v[rows, to] = d.astype(BF16)

                for i in range(N_BLOCKS):
                    old, n = i * TWICE, (i + 1) * TWICE
                    rows = block_rows(i)
                    probs = probabilities(qkv_v[rows, at], keys[:n], i)
                    d_all = rounded(dot_t(dctx[rows, at], values[:n]))
                    d_scores = [d_all[:, block_rows(j)] for j in range(CORES * (i + 1))]
                    for head in HALVES:
                        mine = slice(head, None, CORES)
                        mean = row_sum(total_of([p * d for p, d in zip(probs[mine], d_scores[mine])]))
                        d_scores[mine] = [p * (d - mean) * SCALE for p, d in zip(probs[mine], d_scores[mine])]
                    d_scores, probs = side_by_side(d_scores), side_by_side(probs)
                    turned_back(A, dot(d_scores, keys[:n]), rows, at)
                    for acc, left, right in ((dk_acc, q_t, d_scores), (dv_acc, dc_t, probs)):
                        part = dot(left[:, rows], right)
                        if i:
                            acc[:, :old] += part[:, :old]
                        acc[:, old:n] = part[:, old:]
                first = iota((PAIR, PAIR), 0) < HEAD
                for j in range(N_BLOCKS):
                    rows = block_rows(j)
                    d_key, d_value = [jnp.where(first, acc[:, block_rows(CORES * j)], acc[:, block_rows(CORES * j + 1)]).T
                                      for acc in (dk_acc, dv_acc)]
                    turned_back(B, d_key, rows, lanes(WIDTH + pair * PAIR))
                    d_value = d_value.astype(BF16)
                    bias_sums[C] = bias_sums[C] + column_sum(d_value.astype(F32))
                    dqkv_v[rows, lanes(C * WIDTH + pair * PAIR)] = d_value
                for k, bias_sum in enumerate(bias_sums):
                    total[:, vector_at(QKV_BIAS, k * WIDTH + pair * PAIR, PAIR)] = bias_sum
                at_hooks(pair, pair_hooks)

        qkv_share = half_copies(B, dqkv_v, dqkv_cols)
        dn1[...] = jnp.zeros_like(dn1)

        with jax.named_scope('dn1'):
            @loop(PARTS)
            def _(k):
                slot = parity(k)
                weight_load(k, slot).wait()
                dn1[...] += dot_t(dqkv_v[:, lanes(k * WIDTH, WIDTH)], weight_v[slot])

                @pl.when(k == A)
                def _():
                    weight_load(C, A).start()

        for k in (GAIN1, BIAS1, GAIN2, BIAS2):
            total[:, vector_at(k)] = jnp.zeros((1, WIDTH), F32)

        with jax.named_scope('lnb'):
            @loop(SEQ // LN_ROWS)
            def _(r):
                rows = pl.ds(pl.multiple_of(r * LN_ROWS, LN_ROWS), LN_ROWS)
                scaled, inverse = normalised(h_v[rows, :].astype(F32))
                d1, d2 = rounded(dn1[rows, :]), rounded(dn2[rows, :])
                for k, value in ((GAIN1, d1 * scaled), (BIAS1, d1), (GAIN2, d2 * scaled), (BIAS2, d2)):
                    total[:, vector_at(k)] += column_sum(value)
                g1, g2 = [vec_ref[pl.ds(layer, 1), lanes(OFFSETS[k], WIDTH)] for k in (GAIN1, GAIN2)]
                d_scaled = d1 * g1 + d2 * g2
                d_h = inverse * (d_scaled - row_mean(d_scaled) - scaled * row_mean(d_scaled * scaled))
                dh_v[rows, :] = (dh_v[rows, :].astype(F32) + d_h).astype(BF16)

        schedule.passed(US_NORM)
        wait(qkv_share + tokens_load(n1_hbm, A, A))
        with jax.named_scope('dw2'):
            gradient_wave(C, dqkv_cols, A, (A, B, C))
        schedule.passed(US_STEP)

        def own_part():
            with jax.named_scope('own'):
                node, local = chip.base
                me = node * (SIDE * CORES) + local + core
                row = jnp.zeros((ROWS, PAIR), F32)
                for cols in vector_blocks():
                    left = jnp.zeros((ROWS, WIDTH), F32) + total[:, cols] * (places[A:B, cols] == me).astype(F32)
                    for _ in range(PARTS):
                        row = row + dot_t(left.astype(BF16), pick_lanes(places[B:C], cols))
                        left = left - rounded(left)
                small_ref[layer] = row.astype(BF16)

        launch(C)
        VectorSum(chip, schedule, total, came_vec, vec_sem, own_part).begin()
        schedule.run(None)

        @pl.when(turn_no == A)
        def _():
            for wave in range(len(WAVES)):
                chip.signal_partners(credit.at[wave])

    dx_copy = pltpu.make_async_copy(dh_v, dx_hbm, io_sem.at[A])
    dx_copy.start()
    dx_copy.wait()


def backward(y_cot, tables, vectors, places, weights, saved):
    dma, one = pltpu.SemaphoreType.DMA, (1,)
    pair, wide, row = (len(HALVES),), (SEQ, WIDTH), one + (N_VEC,)
    shapes = [(wide, BF16), ((LAYERS, ROWS, PAIR), BF16)]
    shapes += [((LAYERS, groups, ROWS, width), BF16) for groups, width in ((*one, HIDDEN), (SIDE, WIDTH), (*one, QKV), (*one, WIDTH))]
    in_vmem = len(shapes)
    shapes += [((LAYERS, CORES, SEQ, width), BF16) for width in (TILE, SIDE * TILE, PARTS * TILE)]
    blocks = [(CORES, ROWS, width) for wave in WAVES for width in wave]
    shapes += [((LAYERS,) + pair + CHIPS + block, F32) for block in blocks]
    tile = (CORES, ROWS, TILE)
    scratch = [(pair + CHIPS[1:] + tile, F32), (pair + CHIPS + tile, F32)]
    scratch += [(pair + shape, BF16) for shape in ((WIDTH, CORES * SEQ), (WIDTH, WIDTH), (CORES * SEQ, TILE), (WIDTH, TILE), (TILE, WIDTH))]
    scratch += [(pair + (SEQ, TILE), F32), (wide, F32), (wide, F32), (wide, BF16)] + [((PAIR, CORES * SEQ), F32)] * CORES
    scratch += [((SEQ, QKV), BF16), (pair + (SEQ, TILE), BF16), ((SEQ, QKV), BF16), (wide, BF16), (wide, BF16), (row, F32),
                ((PARTNERS,) + row, F32)]
    slots = (len(WAVES), AXES) + pair + (len(STEPS),)
    sems = [dma(shape) for shape in (slots, slots, pair, pair, pair + pair, pair, pair + pair, pair + (PARTS,), pair,
                                     (SIDE,), pair, pair, pair + (N_TILES,), pair + (PARTNERS,))]
    late = [(pair + block[1:], F32) for block in blocks] + [(pair + lead + block, F32) for block in blocks for lead in LEADS]
    outs = pl.pallas_call(
        backward_kernel,
        out_shape=[jax.ShapeDtypeStruct(*s) for s in shapes],
        in_specs=[IN_VMEM] * SIDE + [ANY] * (AXES + PARTNERS),
        out_specs=[ANY] + [IN_VMEM] * (in_vmem - 1) + [ANY] * (len(shapes) - in_vmem),
        scratch_shapes=[pltpu.VMEM(*s) for s in scratch] + sems + [pltpu.SemaphoreType.REGULAR((len(WAVES),))]
        + [pltpu.VMEM(*s) for s in late],
        compiler_params=pltpu.CompilerParams(collective_id=1, has_side_effects=True, vmem_limit_bytes=VMEM_LIMIT),
        name='backward_layers',
    )(y_cot, tables, vectors, places, *weights, *saved)
    d_x, small, *sums = outs[:in_vmem]
    return d_x, small[:, 0], [s.reshape((LAYERS, -1, s.shape[-1])) for s in sums]


def finish_kernel(*refs):
    n_large = PARTNERS - CORES
    large, small_ref, refs = refs[:n_large], refs[n_large], refs[n_large + 1:]
    outs, small_outs, refs = refs[:n_large], refs[n_large:n_large + len(SHARES)], refs[n_large + len(SHARES):]
    held, sems = refs[:n_large], refs[n_large]
    loads = start([pltpu.make_async_copy(src, dst, sems.at[n]) for n, (src, dst) in enumerate(zip(large, held))])
    first = 0
    for share, out in zip(SHARES, small_outs):
        out[...] = small_ref[:, first:first + share]
        first += share
    stores = []
    for load, src, dst in zip(loads, held, outs):
        load.wait()
        stores += start([pltpu.make_async_copy(src, dst, sems.at[n_large + len(stores)])])
    wait(stores)


def finish(large, small):
    shapes = [jax.ShapeDtypeStruct(t.shape, BF16) for t in large] + [jax.ShapeDtypeStruct((LAYERS, share), BF16) for share in SHARES]
    outs = pl.pallas_call(
        finish_kernel,
        out_shape=shapes,
        in_specs=[ANY] * len(large) + [IN_VMEM],
        out_specs=[ANY] * len(large) + [IN_VMEM] * len(SHARES),
        scratch_shapes=[pltpu.VMEM(t.shape, BF16) for t in large] + [pltpu.SemaphoreType.DMA((CORES * len(large),))],
        name='finish',
    )(*large, small)
    return outs[:len(large)], outs[len(large):]


def rope_tables():
    rot_dim = HEAD // SIDE
    inv_freq = 1.0 / (10000.0 ** (jnp.arange(0, rot_dim, 2, dtype=F32) / rot_dim))
    angles = jnp.arange(SEQ, dtype=F32)[:, None] * inv_freq[None, :]
    cos, sin = jnp.cos(angles), jnp.sin(angles)
    zero = jnp.zeros_like(sin)
    rest = jnp.zeros((SEQ, HEAD - rot_dim), F32)
    tables = ([cos, cos, rest + 1.0], [-sin, zero, rest], [zero, sin, rest])
    return jnp.stack([jnp.tile(jnp.concatenate(table, axis=1), (1, 2)) for table in tables])


def heads_last(tensor):
    lead = tensor.shape[:-2]
    return tensor.reshape(lead + (HEADS, PARTS, HEAD)).swapaxes(-3, -2).reshape(lead + (QKV,))


def heads_first(tensor):
    lead = tensor.shape[:-1]
    return tensor.reshape(lead + (PARTS, HEADS, HEAD)).swapaxes(-3, -2).reshape(lead + (HEADS, PARTS * HEAD))


def vector_places():
    shard, lane, first = [], [], 0
    for k, (share, size) in enumerate(zip(SHARES, SIZES)):
        place = np.arange(size)
        if k == QKV_BIAS:
            place = heads_last(place.reshape(HEADS, -1))
        shard.append(place // share)
        lane.append(first + place % share)
        first += share
    return jnp.asarray(np.stack([np.concatenate(shard), np.concatenate(lane)]).astype(np.int32))


def solution(mesh):
    shard_axes = ('node', 'local')
    act_spec = P(shard_axes)
    param_spec = P(None, shard_axes)

    def device_step(x, y_cot, ln1_gain, ln1_bias, qkv_weight, qkv_bias, out_weight, out_bias,
                    ln2_gain, ln2_bias, up_weight, up_bias, down_weight, down_bias):
        tables, places = rope_tables(), vector_places()
        small = (ln1_gain, ln1_bias, ln2_gain, ln2_bias, qkv_bias, out_bias, up_bias, down_bias)
        small_tile = jnp.pad(jnp.concatenate(small, axis=1), ((0, ROWS - LAYERS), (0, PAIR - sum(SHARES))))
        mix = jnp.concatenate([heads_last(qkv_weight), out_weight], axis=-1)
        *weights, _, vectors, y_out, hidden, n1, n2, ctx, act, qkv, pre = forward(
            x[0], (up_weight, down_weight, mix), small_tile, tables, places)
        weights = [tensor.reshape((LAYERS, -1, tensor.shape[-1])) for tensor in weights]
        d_x, small_sums, (up, down, qkv, out) = backward(
            y_cot[0], tables, vectors, places, weights, (hidden, n1, n2, ctx, act, qkv, pre))
        (y_out, d_x, up, down, out), (g1, b1, g2, b2, qb, ob, ub, db) = finish((y_out, d_x, up, down, out), small_sums)
        return (y_out[None], d_x[None], g1, b1, heads_first(qkv), qb, out, ob, g2, b2, up, ub, down, db)

    return jax.shard_map(device_step, mesh=mesh,
                         in_specs=(act_spec, act_spec) + (param_spec,) * 12,
                         out_specs=(act_spec, act_spec) + (param_spec,) * 12,
                         check_vma=False)
```

```python
import functools
import jax
import jax.numpy as jnp
import numpy as np
from jax import lax
from jax.experimental import pallas as pl
from jax.experimental.pallas import tpu as pltpu
from jax.sharding import PartitionSpec as P

BF16, F32 = jnp.bfloat16, jnp.float32
EPSILON = 1e-5
MESH = pl.DeviceIdType.MESH
ANY = pl.BlockSpec(memory_space=pl.ANY)
IN_VMEM = pl.BlockSpec(memory_space=pltpu.VMEM)
VMEM_LIMIT = 67 * 10**6
LAYERS, AXES, SIDE, CORES, ROWS, PARTNERS = 2, 3, 4, 2, 8, 10
CHIPS = (SIDE, SIDE, SIDE)
SHARDS = SIDE * SIDE * SIDE * CORES
SEQ, WIDTH, HIDDEN, TILE, PAIR, LN_ROWS = 384, 1024, 4096, 512, 128, 64
HEADS, HEAD, PARTS = 16, 64, 3
QKV = PARTS * WIDTH
N_TILES, N_PAIRS, N_BLOCKS = HIDDEN // TILE, WIDTH // PAIR, SEQ // PAIR
TWICE = 2 * PAIR
INV_SQRT2, INV_SQRT2PI, SCALE = 0.7071067811865476, 0.3989422804014327, 0.125
SHARES = (8, 8, 8, 8, 24, 8, 32, 8)
SIZES = tuple(SHARDS * share for share in SHARES)
OFFSETS = tuple(sum(SIZES[:k]) for k in range(len(SIZES)))
N_VEC = sum(SIZES)
GAIN1, BIAS1, GAIN2, BIAS2, QKV_BIAS, OUT_BIAS, UP_BIAS, DOWN_BIAS = range(len(SHARES))
ORDERS = ((2, 1, 0), (1, 0, 2), (0, 2, 1))
HALVES = range(2)
OWN, ONE, CROSS, TWO = range(SIDE)
ROLES = (ONE, TWO, CROSS)
A, B, C = range(AXES)
UP, DOWN, MIX = range(3)
SELF = 3
PASSES = [(stage, step) for stage in range(AXES) for step in range(AXES)] + [(A, SELF)]


class Chip:
    def __init__(self):
        node, local = lax.axis_index('node'), lax.axis_index('local')
        self.core, self.other = lax.rem(local, CORES), 1 - lax.rem(local, CORES)
        self.where = (lax.div(node, SIDE), lax.rem(node, SIDE), lax.div(local, CORES))
        self.base = (node, local - self.core)
        self.strides = ((SIDE, 0), (1, 0), (0, CORES))
        self.near = [(v, v + 1 - 2 * parity(v), lax.rem(v + 2, SIDE), SIDE - 1 - v) for v in self.where]

        self.gaps = [near[3] - near[1] for near in self.near]

    def at(self, axis, role, half):
        near = self.near[axis]
        if role in (OWN, CROSS):
            return near[role]
        return near[role] + half * self.gaps[axis] if role == ONE else near[role] - half * self.gaps[axis]

    def device(self, axis, role, half):
        shift = self.at(axis, role, half) - self.where[axis]
        node, local = [b + shift * s if s else b for b, s in zip(self.base, self.strides[axis])]
        return (node, local + self.core)

    def partner(self):
        node, local = self.base
        return (node, local + self.other)

    def signal_partners(self, semaphore):
        for axis in range(AXES):
            for role in ROLES:
                pl.semaphore_signal(semaphore, inc=1, device_id=self.device(axis, role, A), device_id_type=MESH)
        pl.semaphore_signal(semaphore, inc=1, device_id=self.partner(), device_id_type=MESH)


def enter():
    chip = Chip()
    barrier = pltpu.get_barrier_semaphore()
    chip.signal_partners(barrier)
    pl.semaphore_wait(barrier, PARTNERS)
    return chip


def remote(src, dst, send_sem, recv_sem, device):
    return pltpu.make_async_remote_copy(src_ref=src, dst_ref=dst, send_sem=send_sem, recv_sem=recv_sem, device_id=device,
                                        device_id_type=MESH)


def start(copies):
    for copy in copies:
        copy.start()
    return copies


def wait(copies):
    for copy in copies:
        copy.wait()


def loop(count):
    return pl.loop(0, count)


def halves(body):
    loop(len(HALVES))(body)


def parity(n):
    return lax.rem(n, 2)


def pool(sems):
    return (sems.at[n] for n in range(sems.shape[0]))


def contract(a, b, a_axis, b_axis):
    return lax.dot_general(a, b, (((a_axis,), (b_axis,)), ((), ())), preferred_element_type=F32)


def dot(a, b):
    return contract(a, b, 1, 0)


def dot_t(a, b):
    return contract(a, b, 1, 1)


def row_sum(x):
    return jnp.sum(x, axis=1, keepdims=True)


def column_sum(x):
    return jnp.sum(x, axis=0, keepdims=True)


def rounded(x):
    return x.astype(BF16).astype(F32)


def lanes(first, width=PAIR):
    return pl.ds(pl.multiple_of(first, PAIR), width)


def turn(x, cos, sin_a, sin_b):
    return x * cos + pltpu.roll(x, PAIR - ROWS, 1) * sin_a + pltpu.roll(x, ROWS, 1) * sin_b


def turn_back(d, cos, sin_a, sin_b):
    return d * cos + pltpu.roll(d * sin_a, ROWS, 1) + pltpu.roll(d * sin_b, PAIR - ROWS, 1)


def iota(shape, axis):
    return lax.broadcasted_iota(jnp.int32, shape, axis)


def block_rows(j):
    return slice(j * PAIR, (j + 1) * PAIR)


def split_heads(x):
    first = iota((PAIR, PAIR), 1) < HEAD
    rows = []
    for j in range(N_BLOCKS):
        block = x[block_rows(j)]
        rows += [jnp.where(first, block, jnp.zeros_like(block)), jnp.where(first, jnp.zeros_like(block), block)]
    return jnp.concatenate(rows, axis=0)


def total_of(chunks, join=jnp.add):
    return functools.reduce(join, chunks)


def probabilities(q_block, keys, i):
    scores = dot_t(q_block, keys)
    causal = iota((PAIR, PAIR), 0) >= iota((PAIR, PAIR), 1)
    chunks = [scores[:, block_rows(j)] * SCALE for j in range(CORES * (i + 1))]
    for head in HALVES:
        mine = slice(head, None, CORES)
        *ahead, last = chunks[mine]
        held = ahead + [jnp.where(causal, last, -1e30)]
        top = jnp.max(total_of(held, jnp.maximum), axis=1, keepdims=True)
        held = [jnp.exp(chunk - top) for chunk in held]
        inverse = 1.0 / row_sum(total_of(held))
        chunks[mine] = [chunk * inverse for chunk in held]
    return chunks


def side_by_side(chunks):
    return jnp.concatenate([chunk.astype(BF16) for chunk in chunks], axis=1)


def row_mean(x):
    return jnp.mean(x, axis=1, keepdims=True)


def normalised(h):
    center = h - row_mean(h)
    inverse = lax.rsqrt(row_mean(center * center) + EPSILON)
    return center * inverse, inverse


class Gather:
    def __init__(self, chip, shards, fulls, sems):
        self.chip, self.shards, self.fulls = chip, shards, fulls
        self.send_sem, self.recv_sem, self.pass_send, self.pass_recv = sems

    def box(self, layer, k, half, stage, role, own=False):
        width = self.fulls[k].shape[-1] // len(HALVES)
        cols = lanes(half * width, width)
        if own:
            return self.shards[k].at[layer, :, cols]
        where = list(self.chip.where)
        for axis in ORDERS[k][:stage]:
            where[axis] = pl.ds(0, SIDE)
        axis = ORDERS[k][stage]
        where[axis] = self.chip.at(axis, role, half)
        return self.fulls[k].at[layer, where[0], where[1], where[2], self.chip.core, :, cols]

    def reach(self, layer, k, half, stage, step):
        slot, on = AXES * stage + step, stage == C and step == C
        src = self.box(layer, k, half, stage, ONE if on else OWN, stage == A)
        return remote(src, self.box(layer, k, half, stage, ONE if on else OWN), self.send_sem.at[layer, k, half, slot],
                      self.recv_sem.at[layer, k, half, slot], self.chip.device(ORDERS[k][stage], TWO if on else ROLES[step], half))

    def passing(self, layer, k, half, stage, step):
        role = (*ROLES, OWN)[step]
        slot = AXES * AXES if step == SELF else AXES * stage + step
        return remote(self.box(layer, k, half, stage, role, step == SELF), self.box(layer, k, half, stage, role),
                      self.pass_send.at[layer, k, half, slot], self.pass_recv.at[layer, k, half, slot], self.chip.partner())

    def each(self, action):
        for k in (MIX, UP, DOWN):
            @halves
            def _(half):
                action(k, half)

    def begin(self, layer, stage):
        for step in range(AXES if stage < C else C):
            self.each(lambda k, half: self.reach(layer, k, half, stage, step).start())

    def own(self, layer):
        self.each(lambda k, half: self.passing(layer, k, half, A, SELF).start())

    def middle(self, layer):
        stage = C

        def action(k, half):
            self.reach(layer, k, half, stage, A).wait_recv()
            self.reach(layer, k, half, stage, C).start()
            self.passing(layer, k, half, stage, A).start()
        self.each(action)

    def end(self, layer, stage, steps=range(AXES)):
        def action(k, half):
            for step in steps:
                self.reach(layer, k, half, stage, step).wait_recv()
                self.passing(layer, k, half, stage, step).start()
        self.each(action)

    def arrived(self, layer, k):
        @halves
        def _(half):
            for stage, step in PASSES:
                self.passing(layer, k, half, stage, step).wait_recv()

    def left(self):
        def action(layer, k, half):
            for slot, (stage, step) in enumerate(PASSES):
                box = self.box(A, UP, A, stage, OWN, step == SELF)
                for sem in (self.pass_send,) if step == SELF else (self.send_sem, self.pass_send):
                    sem = sem.at[layer, k, half, slot]
                    remote(box, box, sem, sem, self.chip.partner()).wait_send()

        @loop(LAYERS)
        def _(layer):
            @loop(AXES)
            def _(k):
                halves(lambda half: action(layer, k, half))


def pick_lanes(sel_lane, cols):
    return (iota((PAIR, WIDTH), 0) == sel_lane[:, cols]).astype(F32).astype(BF16)


def vector_blocks():
    return [slice(k * WIDTH, (k + 1) * WIDTH) for k in range(N_VEC // WIDTH)]


def unpack_vectors(small_v, layer, sel_shard, sel_lane, vec_ref):
    tiles = small_v[...].astype(F32).reshape((SHARDS, ROWS, PAIR))
    held = jnp.sum(jnp.where(iota(tiles.shape, 1) == layer, tiles, 0.0), axis=1).astype(BF16)
    for cols in vector_blocks():
        spread = dot(held, pick_lanes(sel_lane, cols))
        spread = jnp.where(iota((SHARDS, WIDTH), 0) == sel_shard[:, cols], spread, 0.0)
        vec_ref[layer:layer + 1, cols] = column_sum(spread)


def forward_kernel(x_hbm, tables_hbm, places_hbm, up_s, down_s, mix_s, small_ref, up_f, down_f, mix_f, small_full, vec_ref,
                   y_hbm, h_hbm, n1_hbm, n2_hbm, ctx_hbm, act_hbm, qkv_hbm, pre_hbm, up_v, down_v, mix_v, small_v, acc, pre_v,
                   n1_v, n2_v, qkv_v, ctx_v, y_v, n1_t, n2_t, ctx_t, act_t, send_sem, recv_sem, pass_send, pass_recv,
                   small_send, small_recv, own_sems, load_sem, save_sem, share_send, share_recv, act_save, act_send, act_recv, tables,
                   places):
    shards, fulls, own_sem = (up_s, down_s, mix_s), (up_f, down_f, mix_f), pool(own_sems)
    chip = enter()
    gather = Gather(chip, shards, fulls, (send_sem, recv_sem, pass_send, pass_recv))

    def small_copy(slot, where, device):
        place = small_full.at[(*where, chip.core)]
        return remote(place, place, small_send.at[slot], small_recv.at[slot], device)

    def small_reach(stage, step):
        where = list(chip.where)
        for axis in range(stage):
            where[axis] = pl.ds(0, SIDE)
        return small_copy(AXES * stage + step, where, chip.device(stage, ROLES[step], A))

    def small_begin(stage):
        start([small_reach(stage, step) for step in range(AXES)])

    def small_end(stage):
        for step in range(AXES):
            small_reach(stage, step).wait_recv()

    small_pass = small_copy(AXES * AXES, [pl.ds(0, SIDE)] * AXES, chip.partner())
    here = (*chip.where, chip.core)
    own = [pltpu.make_async_copy(small_ref, small_full.at[here], next(own_sem))]
    for shard, full in zip(shards, fulls):
        for layer in range(LAYERS):
            own.append(pltpu.make_async_copy(shard.at[layer], full.at[(layer, *here)], next(own_sem)))
    loads = [
        pltpu.make_async_copy(src, dst, next(own_sem)) for src, dst in ((x_hbm, y_v), (tables_hbm, tables), (places_hbm, places))]
    with jax.named_scope('ag0'):
        gather.begin(A, A)
        start(own)
        gather.begin(B, A)
        wait(own)
        small_begin(A)
        gather.own(A)
        gather.own(B)
        start(loads)
        gather.end(A, A)
    with jax.named_scope('ag1'):
        gather.begin(A, B)
        small_end(A)
        small_begin(B)
        gather.end(B, A)
        gather.begin(B, B)
        small_end(B)
        small_begin(C)
        gather.end(A, B)
    with jax.named_scope('ag2_start'):
        gather.begin(A, C)
        small_end(C)
        small_pass.start()
        gather.end(B, B)
    with jax.named_scope('ag2_middle'):
        gather.middle(A)
        gather.begin(B, C)
    with jax.named_scope('unpack'):
        small_pass.wait_recv()
        fetch = pltpu.make_async_copy(small_full, small_v, next(own_sem))
        fetch.start()
        fetch.wait()
        wait(loads)
        for layer in range(LAYERS):
            unpack_vectors(small_v, layer, places[A:B], places[B:C], vec_ref)
    with jax.named_scope('ag2_late'):
        gather.end(A, C, (B,))
    with jax.named_scope('ag2_end'):
        gather.end(A, C, (C,))

    def saves(layer):
        pairs = [(y_v, h_hbm.at[layer]), (qkv_v, qkv_hbm.at[layer])]
        kept = [pltpu.make_async_copy(src, dst, save_sem.at[n]) for n, (src, dst) in enumerate(pairs)]
        for n, (src, dst) in enumerate(((n1_t, n1_hbm), (n2_t, n2_hbm), (ctx_t, ctx_hbm))):
            dst = dst.at[layer, chip.core]
            kept.append((pltpu.make_async_copy(src, dst, save_sem.at[CORES + n]),
                         remote(src, dst, share_send.at[layer, n], share_recv.at[layer, n], chip.partner())))
        return kept

    def quarter(layer, t):
        rows, tiles = pl.ds(t * WIDTH, WIDTH), pl.ds(CORES * t, CORES)
        src, dst = act_t.at[rows], act_hbm.at[layer, chip.core, rows]
        return [pltpu.make_async_copy(pre_v.at[tiles], pre_hbm.at[layer, tiles], act_save.at[A, t]),
                pltpu.make_async_copy(src, dst, act_save.at[B, t]),
                remote(src, dst, act_send.at[layer, t], act_recv.at[layer, t], chip.partner())]

    def settle(layer):
        _, qkv_save, *shares = saves(layer)
        qkv_save.wait()
        for share in shares:
            wait(share)

        @loop(SIDE)
        def _(t):
            wait(quarter(layer, t))

    @loop(LAYERS)
    def _(layer):
        def vector(k, first=0, width=None):
            return vec_ref[pl.ds(layer, 1), lanes(OFFSETS[k] + first, width or SIZES[k])]

        def load(k, piece):
            if k == DOWN:
                return pltpu.make_async_copy(fulls[k].at[layer, piece], down_v.at[piece], load_sem.at[k, piece])
            cols = lanes(piece * WIDTH, WIDTH)
            return pltpu.make_async_copy(fulls[k].at[layer, :, :, :, :, :, cols], (up_v, None, mix_v)[k].at[:, :, :, :, :, cols],
                                         load_sem.at[k, piece])

        def matrix(held, piece):
            return held[:, :, :, :, :, lanes(piece * WIDTH, WIDTH)].reshape((WIDTH, WIDTH))

        def have(k):
            for which in range(LAYERS):
                @pl.when(layer == which)
                def _():
                    gather.arrived(which, k)

        def meanwhile(action):
            @pl.when(layer == A)
            def _():
                action()

        h_save, qkv_save, n1_share, n2_share, ctx_share = saves(layer)
        with jax.named_scope('have_mix'):
            have(MIX)
            start([load(MIX, k) for k in range(SIDE)])

        h_save.start()

        @pl.when(layer == B)
        def _():
            settle(A)

        with jax.named_scope('ln'):
            @loop(SEQ // LN_ROWS)
            def _(r):
                rows = pl.ds(pl.multiple_of(r * LN_ROWS, LN_ROWS), LN_ROWS)
                scaled, _ = normalised(y_v[rows, :].astype(F32))
                n1_v[rows, :] = (scaled * vector(GAIN1) + vector(BIAS1)).astype(BF16)
                n2_v[rows, :] = (scaled * vector(GAIN2) + vector(BIAS2)).astype(BF16)

        for src, dst, share in ((n1_v, n1_t, n1_share), (n2_v, n2_t, n2_share)):
            dst[...] = src[...].T
            start(share)

        with jax.named_scope('qkv'):
            @loop(PARTS)
            def _(k):
                load(MIX, k).wait()
                x = dot(n1_v[...], matrix(mix_v, k)) + vector(QKV_BIAS, k * WIDTH, WIDTH)

                @pl.when(k < C)
                def _():
                    for c in range(N_PAIRS):
                        block = turn(x[:, block_rows(c)], *[tables[n] for n in range(PARTS)])
                        qkv_v[:, lanes(k * WIDTH + c * PAIR)] = block.astype(BF16)

                @pl.when(k == C)
                def _():
                    qkv_v[:, lanes(k * WIDTH, WIDTH)] = x.astype(BF16)

        qkv_save.start()
        with jax.named_scope('have_up'):
            have(UP)
            have(DOWN)

        start([load(UP, k) for k in range(SIDE)] + [load(DOWN, k) for k in range(SIDE)])
        with jax.named_scope('mid'):
            meanwhile(lambda: gather.middle(B))

        with jax.named_scope('fattn'):
            @loop(N_PAIRS)
            def _(pair):
                keys = split_heads(qkv_v[:, lanes(WIDTH + pair * PAIR)])
                values = split_heads(qkv_v[:, lanes(C * WIDTH + pair * PAIR)])
                for i in range(N_BLOCKS):
                    n = (i + 1) * CORES * PAIR
                    probs = probabilities(qkv_v[block_rows(i), lanes(pair * PAIR)], keys[:n], i)
                    ctx_v[block_rows(i), lanes(pair * PAIR)] = dot(side_by_side(probs), values[:n]).astype(BF16)

        ctx_t[...] = ctx_v[...].T
        start(ctx_share)
        meanwhile(lambda: gather.end(B, C, (B,)))
        with jax.named_scope('fout'):
            load(MIX, PARTS).wait()
            acc[...] = y_v[...].astype(F32) + dot(ctx_v[...], matrix(mix_v, PARTS)) + (vector(OUT_BIAS) + vector(DOWN_BIAS))

        with jax.named_scope('fmlp'):
            @loop(SIDE)
            def _(t):
                cols = lanes(t * WIDTH, WIDTH)
                load(UP, t).wait()
                pre = dot(n2_v[...], matrix(up_v, t)) + vector(UP_BIAS, t * WIDTH, WIDTH)
                for k in HALVES:
                    pre_v[CORES * t + k] = pre[:, k * TILE:(k + 1) * TILE]
                act = (0.5 * pre * (1.0 + lax.erf(pre * INV_SQRT2))).astype(BF16)
                act_t[cols, :] = act.T
                start(quarter(layer, t))
                load(DOWN, t).wait()
                acc[...] += dot(act, down_v[t].reshape((WIDTH, WIDTH)))

        h_save.wait()
        y_v[...] = acc[...].astype(BF16)
        with jax.named_scope('fend'):
            meanwhile(lambda: gather.end(B, C, (C,)))

    with jax.named_scope('ftail'):
        last = pltpu.make_async_copy(y_v, y_hbm, next(own_sem))
        last.start()
        for stage in range(AXES):
            for step in range(AXES):
                small_reach(stage, step).wait_send()
        small_pass.wait_send()
        gather.left()
        settle(LAYERS - 1)
        last.wait()


def forward(x, shards, small_tile, tables, places):
    grid = CHIPS + (CORES,)
    full = [(LAYERS,) + grid + tensor.shape[1:] for tensor in shards]
    shapes = [(shape, BF16) for shape in full] + [(grid + small_tile.shape, BF16), ((LAYERS, N_VEC), F32), ((SEQ, WIDTH), BF16),
                                                  ((LAYERS, SEQ, WIDTH), BF16)]
    shapes += [((LAYERS, CORES, width, SEQ), BF16) for width in (WIDTH, WIDTH, WIDTH, HIDDEN)]
    shapes += [((LAYERS, SEQ, QKV), BF16), ((LAYERS, N_TILES, SEQ, TILE), F32)]
    dma = pltpu.SemaphoreType.DMA
    slots = AXES * AXES
    scratch = [pltpu.VMEM(shape[1:], BF16) for shape in full] + [pltpu.VMEM(grid + small_tile.shape, BF16)]
    scratch += [pltpu.VMEM((SEQ, WIDTH), F32), pltpu.VMEM((N_TILES, SEQ, TILE), F32)]
    scratch += [pltpu.VMEM((SEQ, width), BF16) for width in (WIDTH, WIDTH, QKV, WIDTH, WIDTH)]
    scratch += [pltpu.VMEM((width, SEQ), BF16) for width in (WIDTH, WIDTH, WIDTH, HIDDEN)]
    scratch += [dma((LAYERS, AXES, len(HALVES), n)) for n in (slots, slots, slots + 1, slots + 1)]
    scratch += [dma(shape) for shape in ((slots + 1,), (slots + 1,), (slots + SIDE + AXES,), (AXES, SIDE), (SIDE + 1,), (LAYERS, AXES), (LAYERS, AXES), (CORES, SIDE), (LAYERS, SIDE), (LAYERS, SIDE))]
    scratch += [pltpu.VMEM(tables.shape, F32), pltpu.VMEM(places.shape, jnp.int32)]
    out_specs = [IN_VMEM if dtype == F32 and len(shape) == LAYERS else ANY for shape, dtype in shapes]
    return pl.pallas_call(
        forward_kernel,
        out_shape=[jax.ShapeDtypeStruct(*s) for s in shapes],
        in_specs=[ANY] * AXES + [IN_VMEM] * SIDE,
        out_specs=out_specs,
        scratch_shapes=scratch,
        compiler_params=pltpu.CompilerParams(collective_id=0, has_side_effects=True, vmem_limit_bytes=VMEM_LIMIT),
        name='forward_layers',
    )(x, tables, places, *shards, small_tile)


WAVES = ((384, 384, 512), (384, 384, 256), (256, 256, 256))
LEADS = ((2,) + CHIPS[1:], CHIPS[1:], (AXES, SIDE), (AXES,))
W_UP, W_DOWN, W_QKV, W_OUT = range(4)
STEPS = ((1, (2,)), (0, ()), (2, (3, 4, 5)), (5, (6, 7, 8)), (8, (9,)), (9, ()))
LAST = AXES * AXES
CARRIED = ((1, 3), (2, 0))
US_COLUMN, US_HOP, US_ADD, US_STEP = 0.022, 2.5, 0.0013, 0.2
US_FIRST, US_OUT, US_TILE, US_GRADIENT, US_PAIR, US_NORM = 4, 1.2, 1.5, 0.002, 2.15, 6


class Schedule:
    def __init__(self):
        self.now, self.free, self.lines = 0.0, {}, []

    def send(self, link, columns):
        self.free[link] = max(self.free.get(link, 0.0), self.now) + columns * US_COLUMN
        return self.free[link] + US_HOP

    def due(self, limit):
        found = []
        while self.lines:
            line = min(self.lines, key=lambda one: one[A][A]())
            ready = line[A][A]()
            if limit is not None and ready > limit:
                break
            _, run, sends, cost = line.pop(A)
            self.lines = [one for one in self.lines if one]
            self.now = max(self.now, ready) + cost
            sends()
            found.append(run)
        return found

    def run(self, limit):
        for step in self.due(limit):
            step()

    def passed(self, cost):
        self.now += cost
        self.run(self.now)

    def hooks(self, count, cost):
        planned = []
        for _ in range(count):
            self.now += cost
            planned.append(self.due(self.now))
        return planned


def at_hooks(n, planned):
    for when, steps in enumerate(planned):
        if steps:
            @pl.when(n == when)
            def _():
                for step in steps:
                    step()


def add_into(dst, src, n_axes):
    if n_axes < 2:
        dst[...] += src[...]
        return

    @loop(SIDE)
    def _(k):
        dst[k] += src[k]


def at_axis(ref, axis, value, n_axes):
    every = [pl.ds(0, SIDE)] * n_axes
    every[axis] = value
    return ref.at[tuple(every)]


class Reduce:
    def __init__(self, chip, schedule, wave, grads, came, fin, sems, spare, write, done, when=None):
        self.wave, self.chip, self.schedule, self.widths, self.grads = wave, chip, schedule, WAVES[wave], grads
        self.came, self.fin, (self.send_sem, self.recv_sem), (self.spare, self.spare_sem) = came, fin, sems, spare
        self.write, self.done, self.when, self.times = write, done, when, {}

    def box(self, a, half, stage):
        order = ORDERS[a]
        ref = self.came[a][A].at[half, A]
        spot = [axis for axis in range(AXES) if axis != order[A]].index(order[B])
        if stage == B:
            return ref, spot, C
        return at_axis(ref, spot, self.chip.where[order[B]], C), A, B

    def copy(self, a, half, slot):
        stage, turn = divmod(slot, AXES)
        sems = self.send_sem.at[a, half, slot], self.recv_sem.at[a, half, slot]
        if slot == LAST:
            return remote(self.total(a, half).at[self.chip.other], self.fin[a].at[half], *sems, self.chip.partner())
        axis = ORDERS[a][stage]
        if stage:
            role = ROLES[turn]
            ref, spot, n_axes = self.box(a, half, stage)
            src, dst = at_axis(ref, spot, self.chip.at(axis, role, half), n_axes), self.came[a][stage + 1].at[half, turn]
        elif turn == C:
            role, src, dst = TWO, self.came[a][A].at[half, B], self.came[a][B].at[half]
        else:
            role, value = ONE, self.chip.at(axis, (ONE, CROSS)[turn], half)
            src, dst = at_axis(self.grads[a].at[half], axis, value, AXES), self.came[a][A].at[half, turn]
        return remote(src, dst, *sems, self.chip.device(axis, role, half))

    def each(self, action):
        for a in range(AXES):
            halves(lambda half: action(a, half))

    def sending(self, slot):
        stage = slot // AXES
        share = SIDE ** (CORES * stage)
        self.times[slot] = self.schedule.now + US_HOP if slot == LAST else max(
            self.schedule.send(ORDERS[a][stage], self.widths[a] / share) for a in range(AXES))

    def begin(self):
        for slot in (B, A):
            self.each(lambda a, half: self.copy(a, half, slot).start())

    def plan(self, first=0, last=None):
        for slot in (B, A):
            self.times[slot] = self.schedule.now
            if not first:
                self.sending(slot)
        for _, sent in STEPS[:first]:
            self.times.update((slot, self.schedule.now + US_HOP) for slot in sent)
        self.schedule.lines.append([
            (lambda slot=slot: self.times[slot], lambda k=k: self.step(k), lambda sent=sent: [self.sending(n) for n in sent],
             CORES * US_ADD * sum(self.widths) if k < C else US_STEP) for k, (slot, sent) in enumerate(STEPS)][first:last])

    def step(self, k):
        def work():
            with jax.named_scope(f'w{self.wave}s{k}'):
                (self.first, self.first, self.spread, self.spread, self.cross, self.finish)[k](STEPS[k][A])
        if self.when is None:
            work()
        else:
            pl.when(self.when)(work)

    def first(self, slot):
        def local(a, half, piece=None):
            axis = ORDERS[a][A]
            src = at_axis(self.grads[a].at[half], axis, self.chip.at(axis, TWO if slot else OWN, half), AXES)
            dst = self.spare.at[half, :, :, :, :, pl.ds(0, self.widths[a])]
            if piece is not None:
                src, dst = src.at[piece], dst.at[piece]
            return pltpu.make_async_copy(src, dst, self.spare_sem.at[half])

        def begin(a, half):
            loop(SIDE)(lambda piece: local(a, half, piece).start())

        halves(lambda half: begin(A, half))
        for a in range(AXES):
            @halves
            def _(half):
                local(a, half).wait()
                self.copy(a, half, slot).wait_recv()
                add_into(self.came[a][A].at[half, slot], self.spare.at[half, :, :, :, :, pl.ds(0, self.widths[a])], C)
                if slot:
                    self.copy(a, half, C).start()
                if a < C:
                    begin(a + 1, half)

    def gathered(self, a, half, stage, view):
        for turn in range(AXES):
            self.copy(a, half, AXES * stage + turn).wait_recv()
        view[...] += total_of([self.came[a][stage + 1][half, turn] for turn in range(AXES)])

    def spread(self, slot):
        before = slot // AXES

        def action(a, half):
            ref, spot, n_axes = self.box(a, half, before + 1)
            if before:
                self.gathered(a, half, before, ref)
            else:
                self.copy(a, half, slot).wait_recv()
                add_into(ref, self.came[a][B].at[half], C)
            for turn in range(AXES):
                self.copy(a, half, AXES * (before + 1) + turn).start()
        self.each(action)

    def total(self, a, half):
        ref, *_ = self.box(a, half, C)
        return ref.at[self.chip.where[ORDERS[a][C]]]

    def cross(self, _):
        def action(a, half):
            self.gathered(a, half, C, self.total(a, half))
            self.copy(a, half, LAST).start()
        self.each(action)

    def finish(self, _):
        def action(a, half):
            self.write(a, half, self.chip.core, self.total(a, half)[self.chip.core])
            self.copy(a, half, LAST).wait_recv()
            self.write(a, half, self.chip.other, self.fin[a][half])
            self.copy(a, half, LAST).wait_send()
            for block, slot in ((self.came[a][A].at[half, A], A), (self.came[a][C].at[half, A], AXES),
                                (self.came[a][AXES].at[half, A], CORES * AXES)):
                @loop(AXES)
                def _(turn):
                    sem = self.send_sem.at[a, half, slot + turn]
                    remote(block, block, sem, sem, self.chip.partner()).wait_send()
        self.each(action)
        self.done()


class VectorSum:
    def __init__(self, chip, schedule, total, came, sems, finish, when=None):
        self.schedule, self.total, self.came, self.sems, self.finish, self.when, self.ready = schedule, total, came, sems, finish, when, 0.0
        self.devices = [[chip.device(axis, role, A) for role in ROLES] for axis in range(AXES)] + [[chip.partner()]]

    def copies(self, k):
        return [remote(self.total, self.came.at[AXES * k + n], self.sems.at[A, AXES * k + n], self.sems.at[B, AXES * k + n], device)
                for n, device in enumerate(self.devices[k])]

    def sending(self, k):
        if k < SIDE:
            self.ready = self.schedule.send(k, N_VEC / (SIDE * SIDE * ROWS))

    def step(self, k):
        def work():
            with jax.named_scope(f'vec{k}'):
                wait(self.copies(k - 1))
                for n in range(len(self.devices[k - 1])):
                    self.total[...] += self.came[AXES * (k - 1) + n]
            if k < SIDE:
                start(self.copies(k))
            else:
                self.finish()
        if self.when is None:
            work()
        else:
            pl.when(self.when)(work)

    def begin(self):
        start(self.copies(A))

    def plan(self):
        self.sending(A)
        self.schedule.lines.append([
            (lambda: self.ready, lambda k=k: self.step(k), lambda k=k: self.sending(k), US_STEP) for k in range(1, SIDE + 1)])


def backward_kernel(ycot_hbm, tables, vec_ref, places, up_hbm, down_hbm, mix_hbm, h_hbm, n1_hbm, n2_hbm, ctx_hbm,
                    act_hbm, qkv_hbm, pre_hbm, dx_hbm, small_ref, up_sum, down_sum, qkv_sum, out_sum, dout_cols, dpre_cols,
                    dqkv_cols, *refs):
    n_arrays, sums = AXES * len(WAVES), (up_sum, down_sum, qkv_sum, out_sum)
    grads, refs = refs[:n_arrays], refs[n_arrays:]
    (spare, tile_v, big_v, rhs_v, wup_v, wdown_v, pre_v, dn1, dn2, dctx, dk_acc, dv_acc, qkv_v, dpre_v, dqkv_v, dh_v, h_v,
     totals, came_vec, send_sem, recv_sem, spare_sem, tile_sem, big_sem, rhs_sem, mlp_sem, io_sem, own_sem, share_send,
     share_recv, pre_sem, vec_sem, credit, *refs) = refs
    fins, came = refs[:n_arrays], refs[n_arrays:]
    chip = enter()
    core, other = chip.core, chip.other
    first_in = pltpu.make_async_copy(ycot_hbm, dh_v, io_sem.at[A])
    first_in.start()

    def half_copies(layer, k, src, dst):
        width = dst.shape[-1]
        mine, away = [src.at[:, lanes(which * width, width)] for which in (core, other)]
        place = dst.at[layer, core]
        return [pltpu.make_async_copy(mine, place, own_sem.at[k]), remote(away, place, share_send.at[k], share_recv.at[k], chip.partner())]

    def tokens_load(layer, src, part, slot):
        return [pltpu.make_async_copy(src.at[layer, k, pl.ds(part * WIDTH, WIDTH)], big_v.at[slot, :, pl.ds(k * SEQ, SEQ)],
                                      big_sem.at[slot, k]) for k in range(CORES)]

    def weight_load(layer, k, slot):
        return pltpu.make_async_copy(mix_hbm.at[layer, :, lanes(k * WIDTH, WIDTH)], big_v.at[slot], big_sem.at[slot, CORES])

    def tile_loads(layer, t, slot):
        rows = lanes(t * TILE, TILE)
        pairs = ((down_hbm.at[layer, rows], wdown_v), (pre_hbm.at[layer, t], pre_v), (up_hbm.at[layer, :, rows], wup_v))
        return [pltpu.make_async_copy(src, dst.at[slot], mlp_sem.at[slot, n]) for n, (src, dst) in enumerate(pairs)]

    def input_loads(layer):
        return [pltpu.make_async_copy(qkv_hbm.at[layer], qkv_v, io_sem.at[B]), pltpu.make_async_copy(h_hbm.at[layer], h_v, io_sem.at[C])]

    def prefetch(layer):
        start(tokens_load(layer, act_hbm, A, A) + tokens_load(layer, act_hbm, B, B) + [weight_load(layer, AXES, C)])
        start(tokens_load(layer, ctx_hbm, A, AXES) + input_loads(layer))
        for t in HALVES:
            start(tile_loads(layer, t, t))

    prefetch(LAYERS - 1)
    first_in.wait()
    start(half_copies(LAYERS - 1, A, dh_v, dout_cols))

    def vector_at(k, first=0, width=None):
        return lanes(OFFSETS[k] + first, width or SIZES[k])

    def reduction(schedule, layer, wave, when):
        def write(a, half, side, block):
            def put(arr, group, col, first, width):
                size = sums[arr].shape[-1] // CORES
                sums[arr][layer, group, :, lanes(side * size + col, width)] = block[:, first:first + width].astype(BF16)
            width, colour = WAVES[wave][a], CORES * a + half
            if wave:
                first = colour * width if wave == C or a < C else SIDE * WAVES[wave][A] + half * width
                put(W_QKV if wave == C else W_UP, A, first, A, width)
            elif a < C:
                put(W_DOWN, colour, A, A, width)
            else:
                for k in HALVES:
                    put(W_DOWN, CORES * half + k, WAVES[A][A], k * PAIR, PAIR)
                put(W_OUT, A, half * TWICE, TWICE, TWICE)

        def done():
            @pl.when(layer == LAYERS - 1)
            def _():
                chip.signal_partners(credit.at[wave])

        where = slice(AXES * wave, AXES * (wave + 1))
        count = len(LEADS)
        return Reduce(chip, schedule, wave, [grad.at[layer] for grad in grads[where]],
                      [came[count * (AXES * wave + a):count * (AXES * wave + a + 1)] for a in range(AXES)],
                      fins[where], (send_sem.at[wave], recv_sem.at[wave]), (spare, spare_sem), write, done, when)

    def vector_sum(schedule, layer, when):
        def own_part():
            with jax.named_scope('own'):
                node, local = chip.base
                me = node * (SIDE * CORES) + local + core
                row = jnp.zeros((ROWS, PAIR), F32)
                for cols in vector_blocks():
                    left = jnp.zeros((ROWS, WIDTH), F32) + totals[layer, :, cols] * (places[A:B, cols] == me).astype(F32)
                    for _ in range(PARTS):
                        row = row + dot_t(left.astype(BF16), pick_lanes(places[B:C], cols))
                        left = left - rounded(left)
                small_ref[layer] = row.astype(BF16)

            @pl.when(layer == LAYERS - 1)
            def _():
                chip.signal_partners(credit.at[AXES])

        return VectorSum(chip, schedule, totals.at[layer], came_vec, vec_sem, own_part, when)

    def run_on(schedule, layer, when):
        for wave, step in CARRIED:
            reduction(schedule, layer, wave, when).plan(step)
        vector_sum(schedule, layer, when).plan()

    @loop(LAYERS)
    def _(turn_no):
        layer = LAYERS - 1 - turn_no
        total = totals.at[layer]
        schedule = Schedule()

        run_on(schedule, layer + 1, turn_no > A)

        def rhs_load(src, first, width, k):
            cols = lanes(first, width)
            return [pltpu.make_async_copy(src.at[layer, n, :, cols], rhs_v.at[pl.ds(n * SEQ, SEQ), cols], rhs_sem.at[k, n])
                    for n in range(CORES)]

        def product(lhs_slot, first, width, out_slot):
            value = dot(big_v[lhs_slot, :, 0:CORES * SEQ], rhs_v[:, lanes(first, width)])
            tile_v[out_slot, :, :, :, :, :, 0:width] = value.reshape(CHIPS + (CORES, ROWS, width))

        def tile_out(slot, src, dst):
            return pltpu.make_async_copy(src, dst, tile_sem.at[slot])

        def tile_done(slot, width):
            block = tile_v.at[slot, :, :, :, :, :, pl.ds(0, width)]
            tile_out(slot, block, grads[C].at[layer, A, :, :, :, :, :, pl.ds(0, width)]).wait()

        def columns(wave, a, half, first, width):
            return grads[AXES * wave + a].at[layer, half, :, :, :, :, :, pl.ds(first, width)]

        def launch(wave):
            @pl.when(turn_no > A)
            def _():
                pl.semaphore_wait(credit.at[wave], PARTNERS)

            current = reduction(schedule, layer, wave, None)
            if wave == C:
                @pl.when(turn_no > A)
                def _():
                    pl.semaphore_wait(credit.at[AXES], PARTNERS)

                vector_sum(schedule, layer, None).begin()
                current.begin()
            else:
                current.begin()
                current.plan(last=dict(CARRIED).get(wave))

        d_sum = column_sum(dh_v[...].astype(F32))
        total[:, vector_at(OUT_BIAS)] = d_sum
        total[:, vector_at(DOWN_BIAS)] = d_sum
        weight_load(layer, AXES, C).wait()
        dctx[...] = dot_t(dh_v[...], big_v[C]).astype(BF16)
        start(tokens_load(layer, act_hbm, C, C))

        wait(half_copies(layer, A, dh_v, dout_cols))
        wait(start(rhs_load(dout_cols, A, TILE, A)))
        wait(tokens_load(layer, ctx_hbm, A, AXES))
        product(AXES, A, TILE, B)
        start(tokens_load(layer, act_hbm, AXES, AXES))
        for k in HALVES:
            tile_out(B, tile_v.at[B, :, :, :, :, :, pl.ds(k * TWICE, TWICE)], columns(A, C, k, TWICE, TWICE)).start()
        schedule.passed(US_FIRST)
        out_hooks = schedule.hooks(SIDE, US_OUT)

        @loop(SIDE)
        def _(z):
            slot = parity(z)
            wait(tokens_load(layer, act_hbm, z, z))

            @pl.when(z > A)
            def _():
                tile_done(slot, TILE)

            product(z, A, TILE, slot)
            split = WAVES[A][A]
            for k in range(SIDE):
                a, half = divmod(k, CORES)
                for c in range(CORES):
                    block = tile_v.at[slot, :, :, CORES * c + a, half]
                    tile_out(slot, block.at[:, :, :, pl.ds(0, split)], grads[a].at[layer, half, z, :, :, c]).start()
                    tile_out(slot, block.at[:, :, :, pl.ds(split, PAIR)],
                             grads[C].at[layer, a, z, :, :, c, :, pl.ds(half * PAIR, PAIR)]).start()
            at_hooks(z, out_hooks)

        start(tokens_load(layer, n2_hbm, A, A))
        for slot in HALVES:
            tile_done(slot, TILE)
        schedule.passed(US_STEP)
        launch(A)
        start([weight_load(layer, k, k + 1) for k in range(PARTS)])

        dn2[...] = jnp.zeros_like(dn2)

        def pre_copy(t, slot, away):
            place = dpre_cols.at[layer, core, :, lanes(lax.rem(t, SIDE) * TILE, TILE)]
            if away:
                return remote(dpre_v.at[slot], place, pre_sem.at[A, t], pre_sem.at[B, t], chip.partner())
            return pltpu.make_async_copy(dpre_v.at[slot], place, own_sem.at[CORES + slot])

        def pre_act(t, leave):
            for away, whose in ((False, core), (True, other)):
                @pl.when(lax.div(t, SIDE) == whose)
                def _():
                    copy = pre_copy(t, parity(t), away)
                    if leave:
                        copy.start()
                    elif away:
                        copy.wait_send()
                    else:
                        copy.wait()

        tile_hooks = schedule.hooks(N_TILES, US_TILE)

        with jax.named_scope('mlp'):
            @loop(N_TILES)
            def _(t):
                slot = parity(t)
                wait(tile_loads(layer, t, slot))
                d_act = rounded(dot_t(dh_v[...], wdown_v[slot]))
                pre = pre_v[slot]
                slope = 0.5 * (1.0 + lax.erf(pre * INV_SQRT2)) + pre * (INV_SQRT2PI * jnp.exp(-0.5 * pre * pre))
                d_pre = d_act * slope
                total[:, vector_at(UP_BIAS, t * TILE, TILE)] = column_sum(d_pre)

                @pl.when(t > B)
                def _():
                    pre_act(t - CORES, False)

                dpre_v[slot] = d_pre.astype(BF16)
                pre_act(t, True)
                dn2[...] += dot_t(dpre_v[slot], wup_v[slot])

                @pl.when(t + CORES < N_TILES)
                def _():
                    start(tile_loads(layer, t + CORES, slot))

                at_hooks(t, tile_hooks)

        for t in HALVES:
            pre_act(N_TILES - CORES + t, False)
        for t in range(SIDE):
            pre_copy(SIDE * core + t, A, True).wait_recv()

        def gradient_loads(wave, source):
            first = 0
            for k in range(CORES * AXES):
                width = WAVES[wave][k // CORES]
                start(rhs_load(source, first, width, k))
                first += width

        def gradient_wave(wave, source, first, base, orders):
            width, count = WAVES[wave][orders[A]], CORES * len(orders)
            planned = schedule.hooks(count, width * US_GRADIENT)

            @loop(count)
            def _(k):
                slot = parity(k)
                wait(rhs_load(source, first + k * width, width, base + k))

                @pl.when(k > B)
                def _():
                    tile_done(slot, width)

                product(A, first + k * width, width, slot)
                block = tile_v.at[slot, :, :, :, :, :, pl.ds(0, width)]
                for n, a in enumerate(orders):
                    @pl.when(lax.div(k, CORES) == n)
                    def _():
                        tile_out(slot, block, columns(wave, a, parity(k), 0, width)).start()
                at_hooks(k, planned)

            for slot in HALVES:
                tile_done(slot, width)

        gradient_loads(B, dpre_cols)
        wait(tokens_load(layer, n2_hbm, A, A))
        with jax.named_scope('dw1'):
            gradient_wave(B, dpre_cols, A, A, (A, B))
            gradient_wave(B, dpre_cols, SIDE * WAVES[B][A], SIDE, (C,))
        launch(B)
        start(tokens_load(layer, n1_hbm, A, A))

        wait(input_loads(layer))
        pair_hooks = schedule.hooks(N_PAIRS, US_PAIR)

        with jax.named_scope('attn'):
            @loop(N_PAIRS)
            def _(pair):
                at = lanes(pair * PAIR)
                keys = split_heads(qkv_v[:, lanes(WIDTH + pair * PAIR)])
                values = split_heads(qkv_v[:, lanes(C * WIDTH + pair * PAIR)])
                q_t = qkv_v[:, at].T
                dc_t = dctx[:, at].T
                bias_sums = [jnp.zeros((1, PAIR), F32)] * PARTS

                def turned_back(n, d, rows, to):
                    d = turn_back(rounded(d), *[tables[k, rows, :] for k in range(PARTS)])
                    bias_sums[n] = bias_sums[n] + column_sum(d)
                    dqkv_v[rows, to] = d.astype(BF16)

                for i in range(N_BLOCKS):
                    old, n = i * TWICE, (i + 1) * TWICE
                    rows = block_rows(i)
                    probs = probabilities(qkv_v[rows, at], keys[:n], i)
                    d_all = rounded(dot_t(dctx[rows, at], values[:n]))
                    d_scores = [d_all[:, block_rows(j)] for j in range(CORES * (i + 1))]
                    for head in HALVES:
                        mine = slice(head, None, CORES)
                        mean = row_sum(total_of([p * d for p, d in zip(probs[mine], d_scores[mine])]))
                        d_scores[mine] = [p * (d - mean) * SCALE for p, d in zip(probs[mine], d_scores[mine])]
                    d_scores, probs = side_by_side(d_scores), side_by_side(probs)
                    turned_back(A, dot(d_scores, keys[:n]), rows, at)
                    for acc, left, right in ((dk_acc, q_t, d_scores), (dv_acc, dc_t, probs)):
                        part = dot(left[:, rows], right)
                        if i:
                            acc[:, :old] += part[:, :old]
                        acc[:, old:n] = part[:, old:]
                first = iota((PAIR, PAIR), 0) < HEAD
                for j in range(N_BLOCKS):
                    rows = block_rows(j)
                    d_key, d_value = [jnp.where(first, acc[:, block_rows(CORES * j)], acc[:, block_rows(CORES * j + 1)]).T
                                      for acc in (dk_acc, dv_acc)]
                    turned_back(B, d_key, rows, lanes(WIDTH + pair * PAIR))
                    d_value = d_value.astype(BF16)
                    bias_sums[C] = bias_sums[C] + column_sum(d_value.astype(F32))
                    dqkv_v[rows, lanes(C * WIDTH + pair * PAIR)] = d_value
                for k, bias_sum in enumerate(bias_sums):
                    total[:, vector_at(QKV_BIAS, k * WIDTH + pair * PAIR, PAIR)] = bias_sum
                at_hooks(pair, pair_hooks)

        qkv_share = start(half_copies(layer, B, dqkv_v, dqkv_cols))
        dn1[...] = jnp.zeros_like(dn1)

        with jax.named_scope('dn1'):
            @loop(PARTS)
            def _(k):
                weight_load(layer, k, k + 1).wait()
                dn1[...] += dot_t(dqkv_v[:, lanes(k * WIDTH, WIDTH)], big_v[k + 1])

        for k in (GAIN1, BIAS1, GAIN2, BIAS2):
            total[:, vector_at(k)] = jnp.zeros((1, WIDTH), F32)

        with jax.named_scope('lnb'):
            @loop(SEQ // LN_ROWS)
            def _(r):
                rows = pl.ds(pl.multiple_of(r * LN_ROWS, LN_ROWS), LN_ROWS)
                scaled, inverse = normalised(h_v[rows, :].astype(F32))
                d1, d2 = rounded(dn1[rows, :]), rounded(dn2[rows, :])
                for k, value in ((GAIN1, d1 * scaled), (BIAS1, d1), (GAIN2, d2 * scaled), (BIAS2, d2)):
                    total[:, vector_at(k)] += column_sum(value)
                g1, g2 = [vec_ref[pl.ds(layer, 1), lanes(OFFSETS[k], WIDTH)] for k in (GAIN1, GAIN2)]
                d_scaled = d1 * g1 + d2 * g2
                d_h = inverse * (d_scaled - row_mean(d_scaled) - scaled * row_mean(d_scaled * scaled))
                dh_v[rows, :] = (dh_v[rows, :].astype(F32) + d_h).astype(BF16)

        schedule.passed(US_NORM)
        wait(qkv_share)
        gradient_loads(C, dqkv_cols)

        @pl.when(turn_no == A)
        def _():
            start(half_copies(layer - 1, A, dh_v, dout_cols))

        wait(tokens_load(layer, n1_hbm, A, A))
        with jax.named_scope('dw2'):
            gradient_wave(C, dqkv_cols, A, A, (A, B, C))

        @pl.when(turn_no == A)
        def _():
            prefetch(layer - 1)

        schedule.run(None)
        launch(C)

    dx_copy = pltpu.make_async_copy(dh_v, dx_hbm, io_sem.at[A])
    dx_copy.start()
    schedule = Schedule()
    run_on(schedule, A, None)
    schedule.run(None)
    dx_copy.wait()


def backward(y_cot, tables, vectors, places, weights, saved):
    dma, one = pltpu.SemaphoreType.DMA, (1,)
    pair, wide, row = (len(HALVES),), (SEQ, WIDTH), one + (N_VEC,)
    shapes = [(wide, BF16), ((LAYERS, ROWS, PAIR), BF16)]
    shapes += [((LAYERS, groups, ROWS, width), BF16) for groups, width in ((*one, HIDDEN), (SIDE, WIDTH), (*one, QKV), (*one, WIDTH))]
    in_vmem = len(shapes)
    shapes += [((LAYERS, CORES, SEQ, width), BF16) for width in (TILE, SIDE * TILE, PARTS * TILE)]
    blocks = [(CORES, ROWS, width) for wave in WAVES for width in wave]
    shapes += [((LAYERS,) + pair + CHIPS + block, F32) for block in blocks]
    tile = (CORES, ROWS, TILE)
    scratch = [(pair + CHIPS[1:] + tile, F32), (pair + CHIPS + tile, F32), ((SIDE, WIDTH, WIDTH), BF16), ((CORES * SEQ, SIDE * TILE), BF16)]
    scratch += [(pair + shape, BF16) for shape in ((WIDTH, TILE), (TILE, WIDTH))]
    scratch += [(pair + (SEQ, TILE), F32), (wide, F32), (wide, F32), (wide, BF16)] + [((PAIR, CORES * SEQ), F32)] * CORES
    scratch += [((SEQ, QKV), BF16), (pair + (SEQ, TILE), BF16), ((SEQ, QKV), BF16), (wide, BF16), (wide, BF16), ((LAYERS,) + row, F32),
                ((PARTNERS,) + row, F32)]
    slots = (len(WAVES), AXES) + pair + (LAST + 1,)
    sems = [dma(shape) for shape in (slots, slots, pair, pair, (SIDE, AXES), (CORES * AXES, CORES), pair + (PARTS,), (AXES,),
                                     (SIDE,), pair, pair, pair + (N_TILES,), pair + (PARTNERS,))]
    late = [(pair + block[1:], F32) for block in blocks] + [(pair + lead + block, F32) for block in blocks for lead in LEADS]
    outs = pl.pallas_call(
        backward_kernel,
        out_shape=[jax.ShapeDtypeStruct(*s) for s in shapes],
        in_specs=[ANY] + [IN_VMEM] * AXES + [ANY] * PARTNERS,
        out_specs=[ANY] + [IN_VMEM] * (in_vmem - 1) + [ANY] * (len(shapes) - in_vmem),
        scratch_shapes=[pltpu.VMEM(*s) for s in scratch] + sems + [pltpu.SemaphoreType.REGULAR((SIDE,))]
        + [pltpu.VMEM(*s) for s in late],
        compiler_params=pltpu.CompilerParams(collective_id=1, has_side_effects=True, vmem_limit_bytes=VMEM_LIMIT),
        name='backward_layers',
    )(y_cot, tables, vectors, places, *weights, *saved)
    d_x, small, *sums = outs[:in_vmem]
    return d_x, small[:, 0], [s.reshape((LAYERS, -1, s.shape[-1])) for s in sums]


def finish_kernel(*refs):
    n_large = CORES + AXES
    large, small_ref, refs = refs[:n_large], refs[n_large], refs[n_large + 1:]
    outs, small_outs, refs = refs[:n_large], refs[n_large:n_large + len(SHARES)], refs[n_large + len(SHARES):]
    held, sems = refs[:n_large], refs[n_large]
    loads = start([pltpu.make_async_copy(src, dst, sems.at[n]) for n, (src, dst) in enumerate(zip(large, held))])
    first = 0
    for share, out in zip(SHARES, small_outs):
        out[...] = small_ref[:, first:first + share]
        first += share
    stores = []
    for load, src, dst in zip(loads, held, outs):
        load.wait()
        stores += start([pltpu.make_async_copy(src, dst, sems.at[n_large + len(stores)])])
    wait(stores)


def finish(large, small):
    shapes = [jax.ShapeDtypeStruct(t.shape, BF16) for t in large] + [jax.ShapeDtypeStruct((LAYERS, share), BF16) for share in SHARES]
    outs = pl.pallas_call(
        finish_kernel,
        out_shape=shapes,
        in_specs=[ANY] * len(large) + [IN_VMEM],
        out_specs=[ANY] * len(large) + [IN_VMEM] * len(SHARES),
        scratch_shapes=[pltpu.VMEM(t.shape, BF16) for t in large] + [pltpu.SemaphoreType.DMA((CORES * len(large),))],
        name='finish',
    )(*large, small)
    return outs[:len(large)], outs[len(large):]


def rope_tables():
    rot_dim = HEAD // SIDE
    inv_freq = 1.0 / (10000.0 ** (jnp.arange(0, rot_dim, 2, dtype=F32) / rot_dim))
    angles = jnp.arange(SEQ, dtype=F32)[:, None] * inv_freq[None, :]
    cos, sin = jnp.cos(angles), jnp.sin(angles)
    zero = jnp.zeros_like(sin)
    rest = jnp.zeros((SEQ, HEAD - rot_dim), F32)
    tables = ([cos, cos, rest + 1.0], [-sin, zero, rest], [zero, sin, rest])
    return jnp.stack([jnp.tile(jnp.concatenate(table, axis=1), (1, 2)) for table in tables])


def heads_last(tensor):
    lead = tensor.shape[:-2]
    return tensor.reshape(lead + (HEADS, PARTS, HEAD)).swapaxes(-3, -2).reshape(lead + (QKV,))


def heads_first(tensor):
    lead = tensor.shape[:-1]
    return tensor.reshape(lead + (PARTS, HEADS, HEAD)).swapaxes(-3, -2).reshape(lead + (HEADS, PARTS * HEAD))


def vector_places():
    shard, lane, first = [], [], 0
    for k, (share, size) in enumerate(zip(SHARES, SIZES)):
        place = np.arange(size)
        if k == QKV_BIAS:
            place = heads_last(place.reshape(HEADS, -1))
        shard.append(place // share)
        lane.append(first + place % share)
        first += share
    return jnp.asarray(np.stack([np.concatenate(shard), np.concatenate(lane)]).astype(np.int32))


def solution(mesh):
    shard_axes = ('node', 'local')
    act_spec = P(shard_axes)
    param_spec = P(None, shard_axes)

    def device_step(x, y_cot, ln1_gain, ln1_bias, qkv_weight, qkv_bias, out_weight, out_bias,
                    ln2_gain, ln2_bias, up_weight, up_bias, down_weight, down_bias):
        tables, places = rope_tables(), vector_places()
        small = (ln1_gain, ln1_bias, ln2_gain, ln2_bias, qkv_bias, out_bias, up_bias, down_bias)
        small_tile = jnp.pad(jnp.concatenate(small, axis=1), ((0, ROWS - LAYERS), (0, PAIR - sum(SHARES))))
        mix = jnp.concatenate([heads_last(qkv_weight), out_weight], axis=-1)
        *weights, _, vectors, y_out, hidden, n1, n2, ctx, act, qkv, pre = forward(
            x[0], (up_weight, down_weight, mix), small_tile, tables, places)
        weights = [tensor.reshape((LAYERS, -1, tensor.shape[-1])) for tensor in weights]
        d_x, small_sums, (up, down, qkv, out) = backward(
            y_cot[0], tables, vectors, places, weights, (hidden, n1, n2, ctx, act, qkv, pre))
        (y_out, d_x, up, down, out), (g1, b1, g2, b2, qb, ob, ub, db) = finish((y_out, d_x, up, down, out), small_sums)
        return (y_out[None], d_x[None], g1, b1, heads_first(qkv), qb, out, ob, g2, b2, up, ub, down, db)

    return jax.shard_map(device_step, mesh=mesh,
                         in_specs=(act_spec, act_spec) + (param_spec,) * 12,
                         out_specs=(act_spec, act_spec) + (param_spec,) * 12,
                         check_vma=False)
```

```python
import functools
import jax
import jax.numpy as jnp
import numpy as np
from jax import lax
from jax.experimental import pallas as pl
from jax.experimental.pallas import tpu as pltpu
from jax.sharding import PartitionSpec as P

BF16, F32 = jnp.bfloat16, jnp.float32
EPSILON = 1e-5
MESH = pl.DeviceIdType.MESH
ANY = pl.BlockSpec(memory_space=pl.ANY)
IN_VMEM = pl.BlockSpec(memory_space=pltpu.VMEM)
VMEM_LIMIT = 67 * 10**6
LAYERS, AXES, SIDE, CORES, ROWS, PARTNERS = 2, 3, 4, 2, 8, 10
CHIPS = (SIDE, SIDE, SIDE)
SHARDS = SIDE * SIDE * SIDE * CORES
SEQ, WIDTH, HIDDEN, TILE, PAIR, LN_ROWS = 384, 1024, 4096, 512, 128, 64
HEADS, HEAD, PARTS = 16, 64, 3
QKV = PARTS * WIDTH
N_TILES, N_PAIRS, N_BLOCKS = HIDDEN // TILE, WIDTH // PAIR, SEQ // PAIR
TWICE = 2 * PAIR
INV_SQRT2, INV_SQRT2PI, SCALE = 0.7071067811865476, 0.3989422804014327, 0.125
SHARES = (8, 8, 8, 8, 24, 8, 32, 8)
SIZES = tuple(SHARDS * share for share in SHARES)
OFFSETS = tuple(sum(SIZES[:k]) for k in range(len(SIZES)))
N_VEC = sum(SIZES)
GAIN1, BIAS1, GAIN2, BIAS2, QKV_BIAS, OUT_BIAS, UP_BIAS, DOWN_BIAS = range(len(SHARES))
ORDERS = ((2, 1, 0), (1, 0, 2), (0, 2, 1))
HALVES = range(2)
OWN, ONE, CROSS, TWO = range(SIDE)
ROLES = (ONE, TWO, CROSS)
A, B, C = range(AXES)
UP, DOWN, MIX = range(3)
SELF = 3
PASSES = [(stage, step) for stage in range(AXES) for step in range(AXES)] + [(A, SELF)]


class Chip:
    def __init__(self):
        node, local = lax.axis_index('node'), lax.axis_index('local')
        self.core, self.other = lax.rem(local, CORES), 1 - lax.rem(local, CORES)
        self.where = (lax.div(node, SIDE), lax.rem(node, SIDE), lax.div(local, CORES))
        self.base = (node, local - self.core)
        self.strides = ((SIDE, 0), (1, 0), (0, CORES))
        self.near = [(v, v + 1 - 2 * parity(v), lax.rem(v + 2, SIDE), SIDE - 1 - v) for v in self.where]

        self.gaps = [near[3] - near[1] for near in self.near]

    def at(self, axis, role, half):
        near = self.near[axis]
        if role in (OWN, CROSS):
            return near[role]
        return near[role] + half * self.gaps[axis] if role == ONE else near[role] - half * self.gaps[axis]

    def device(self, axis, role, half):
        shift = self.at(axis, role, half) - self.where[axis]
        node, local = [b + shift * s if s else b for b, s in zip(self.base, self.strides[axis])]
        return (node, local + self.core)

    def partner(self):
        node, local = self.base
        return (node, local + self.other)

    def signal_partners(self, semaphore):
        for axis in range(AXES):
            for role in ROLES:
                pl.semaphore_signal(semaphore, inc=1, device_id=self.device(axis, role, A), device_id_type=MESH)
        pl.semaphore_signal(semaphore, inc=1, device_id=self.partner(), device_id_type=MESH)


def enter():
    chip = Chip()
    barrier = pltpu.get_barrier_semaphore()
    chip.signal_partners(barrier)
    pl.semaphore_wait(barrier, PARTNERS)
    return chip


def remote(src, dst, send_sem, recv_sem, device):
    return pltpu.make_async_remote_copy(src_ref=src, dst_ref=dst, send_sem=send_sem, recv_sem=recv_sem, device_id=device,
                                        device_id_type=MESH)


def start(copies):
    for copy in copies:
        copy.start()
    return copies


def wait(copies):
    for copy in copies:
        copy.wait()


def loop(count):
    return pl.loop(0, count)


def halves(body):
    loop(len(HALVES))(body)


def parity(n):
    return lax.rem(n, 2)


def pool(sems):
    return (sems.at[n] for n in range(sems.shape[0]))


def contract(a, b, a_axis, b_axis):
    return lax.dot_general(a, b, (((a_axis,), (b_axis,)), ((), ())), preferred_element_type=F32)


def dot(a, b):
    return contract(a, b, 1, 0)


def dot_t(a, b):
    return contract(a, b, 1, 1)


def row_sum(x):
    return jnp.sum(x, axis=1, keepdims=True)


def column_sum(x):
    return jnp.sum(x, axis=0, keepdims=True)


def rounded(x):
    return x.astype(BF16).astype(F32)


def lanes(first, width=PAIR):
    return pl.ds(pl.multiple_of(first, PAIR), width)


def turn(x, cos, sin_a, sin_b):
    return x * cos + pltpu.roll(x, PAIR - ROWS, 1) * sin_a + pltpu.roll(x, ROWS, 1) * sin_b


def turn_back(d, cos, sin_a, sin_b):
    return d * cos + pltpu.roll(d * sin_a, ROWS, 1) + pltpu.roll(d * sin_b, PAIR - ROWS, 1)


def iota(shape, axis):
    return lax.broadcasted_iota(jnp.int32, shape, axis)


def block_rows(j):
    return slice(j * PAIR, (j + 1) * PAIR)


def split_heads(x):
    first = iota((PAIR, PAIR), 1) < HEAD
    rows = []
    for j in range(N_BLOCKS):
        block = x[block_rows(j)]
        rows += [jnp.where(first, block, jnp.zeros_like(block)), jnp.where(first, jnp.zeros_like(block), block)]
    return jnp.concatenate(rows, axis=0)


def total_of(chunks, join=jnp.add):
    return functools.reduce(join, chunks)


def probabilities(q_block, keys, i):
    scores = dot_t(q_block, keys)
    causal = iota((PAIR, PAIR), 0) >= iota((PAIR, PAIR), 1)
    chunks = [scores[:, block_rows(j)] * SCALE for j in range(CORES * (i + 1))]
    for head in HALVES:
        mine = slice(head, None, CORES)
        *ahead, last = chunks[mine]
        held = ahead + [jnp.where(causal, last, -1e30)]
        top = jnp.max(total_of(held, jnp.maximum), axis=1, keepdims=True)
        held = [jnp.exp(chunk - top) for chunk in held]
        inverse = 1.0 / row_sum(total_of(held))
        chunks[mine] = [chunk * inverse for chunk in held]
    return chunks


def side_by_side(chunks):
    return jnp.concatenate([chunk.astype(BF16) for chunk in chunks], axis=1)


def row_mean(x):
    return jnp.mean(x, axis=1, keepdims=True)


def normalised(h):
    center = h - row_mean(h)
    inverse = lax.rsqrt(row_mean(center * center) + EPSILON)
    return center * inverse, inverse


class Gather:
    def __init__(self, chip, shards, fulls, sems):
        self.chip, self.shards, self.fulls = chip, shards, fulls
        self.send_sem, self.recv_sem, self.pass_send, self.pass_recv = sems

    def box(self, layer, k, half, stage, role, own=False):
        width = self.fulls[k].shape[-1] // len(HALVES)
        cols = lanes(half * width, width)
        if own:
            return self.shards[k].at[layer, :, cols]
        where = list(self.chip.where)
        for axis in ORDERS[k][:stage]:
            where[axis] = pl.ds(0, SIDE)
        axis = ORDERS[k][stage]
        where[axis] = self.chip.at(axis, role, half)
        return self.fulls[k].at[layer, where[0], where[1], where[2], self.chip.core, :, cols]

    def reach(self, layer, k, half, stage, step):
        slot, on = AXES * stage + step, stage > A and step == C
        src = self.box(layer, k, half, stage, ONE if on else OWN, stage == A)
        return remote(src, self.box(layer, k, half, stage, ONE if on else OWN), self.send_sem.at[layer, k, half, slot],
                      self.recv_sem.at[layer, k, half, slot], self.chip.device(ORDERS[k][stage], TWO if on else ROLES[step], half))

    def passing(self, layer, k, half, stage, step):
        role = (*ROLES, OWN)[step]
        slot = AXES * AXES if step == SELF else AXES * stage + step
        return remote(self.box(layer, k, half, stage, role, step == SELF), self.box(layer, k, half, stage, role),
                      self.pass_send.at[layer, k, half, slot], self.pass_recv.at[layer, k, half, slot], self.chip.partner())

    def each(self, action):
        for k in (MIX, UP, DOWN):
            @halves
            def _(half):
                action(k, half)

    def begin(self, layer, stage):
        for step in range(C if stage else AXES):
            self.each(lambda k, half: self.reach(layer, k, half, stage, step).start())

    def own(self, layer):
        self.each(lambda k, half: self.passing(layer, k, half, A, SELF).start())

    def middle(self, layer, stage):
        def action(k, half):
            self.reach(layer, k, half, stage, A).wait_recv()
            self.reach(layer, k, half, stage, C).start()
            self.passing(layer, k, half, stage, A).start()
        self.each(action)

    def end(self, layer, stage, steps=range(AXES)):
        def action(k, half):
            for step in steps:
                self.reach(layer, k, half, stage, step).wait_recv()
                self.passing(layer, k, half, stage, step).start()
        self.each(action)

    def arrived(self, layer, k):
        @halves
        def _(half):
            for stage, step in PASSES:
                self.passing(layer, k, half, stage, step).wait_recv()

    def left(self):
        def action(layer, k, half):
            for slot, (stage, step) in enumerate(PASSES):
                box = self.box(A, UP, A, stage, OWN, step == SELF)
                for sem in (self.pass_send,) if step == SELF else (self.send_sem, self.pass_send):
                    sem = sem.at[layer, k, half, slot]
                    remote(box, box, sem, sem, self.chip.partner()).wait_send()

        @loop(LAYERS)
        def _(layer):
            @loop(AXES)
            def _(k):
                halves(lambda half: action(layer, k, half))


def pick_lanes(sel_lane, cols):
    return (iota((PAIR, WIDTH), 0) == sel_lane[:, cols]).astype(F32).astype(BF16)


def vector_blocks():
    return [slice(k * WIDTH, (k + 1) * WIDTH) for k in range(N_VEC // WIDTH)]


def unpack_vectors(small_v, layer, sel_shard, sel_lane, vec_ref):
    tiles = small_v[...].astype(F32).reshape((SHARDS, ROWS, PAIR))
    held = jnp.sum(jnp.where(iota(tiles.shape, 1) == layer, tiles, 0.0), axis=1).astype(BF16)
    for cols in vector_blocks():
        spread = dot(held, pick_lanes(sel_lane, cols))
        spread = jnp.where(iota((SHARDS, WIDTH), 0) == sel_shard[:, cols], spread, 0.0)
        vec_ref[layer:layer + 1, cols] = column_sum(spread)


def forward_kernel(x_hbm, tables_hbm, places_hbm, up_s, down_s, mix_s, small_ref, up_f, down_f, mix_f, small_full, vec_ref,
                   y_hbm, h_hbm, n1_hbm, n2_hbm, ctx_hbm, act_hbm, qkv_hbm, pre_hbm, up_v, down_v, mix_v, small_v, acc, pre_v,
                   n1_v, n2_v, qkv_v, ctx_v, y_v, n1_t, n2_t, ctx_t, act_t, send_sem, recv_sem, pass_send, pass_recv,
                   small_send, small_recv, own_sems, load_sem, save_sem, share_send, share_recv, act_save, act_send, act_recv, tables,
                   places):
    shards, fulls, own_sem = (up_s, down_s, mix_s), (up_f, down_f, mix_f), pool(own_sems)
    chip = enter()
    gather = Gather(chip, shards, fulls, (send_sem, recv_sem, pass_send, pass_recv))

    def small_copy(slot, where, device):
        place = small_full.at[(*where, chip.core)]
        return remote(place, place, small_send.at[slot], small_recv.at[slot], device)

    def small_reach(stage, step):
        where = list(chip.where)
        for axis in range(stage):
            where[axis] = pl.ds(0, SIDE)
        return small_copy(AXES * stage + step, where, chip.device(stage, ROLES[step], A))

    def small_begin(stage):
        start([small_reach(stage, step) for step in range(AXES)])

    def small_end(stage):
        for step in range(AXES):
            small_reach(stage, step).wait_recv()

    small_pass = small_copy(AXES * AXES, [pl.ds(0, SIDE)] * AXES, chip.partner())
    here = (*chip.where, chip.core)
    own = [pltpu.make_async_copy(small_ref, small_full.at[here], next(own_sem))]
    for shard, full in zip(shards, fulls):
        for layer in range(LAYERS):
            own.append(pltpu.make_async_copy(shard.at[layer], full.at[(layer, *here)], next(own_sem)))
    loads = [
        pltpu.make_async_copy(src, dst, next(own_sem)) for src, dst in ((x_hbm, y_v), (tables_hbm, tables), (places_hbm, places))]
    with jax.named_scope('ag0'):
        gather.begin(A, A)
        start(own)
        gather.begin(B, A)
        wait(own)
        small_begin(A)
        gather.own(A)
        gather.own(B)
        start(loads)
        gather.end(A, A)
    with jax.named_scope('ag1'):
        gather.begin(A, B)
        small_end(A)
        small_begin(B)
        gather.end(B, A)
        gather.begin(B, B)
        gather.middle(A, B)
        small_end(B)
        small_begin(C)
        gather.middle(B, B)
        gather.end(A, B, (B, C))
    with jax.named_scope('ag2_start'):
        gather.begin(A, C)
        small_end(C)
        small_pass.start()
        gather.end(B, B, (B, C))
    with jax.named_scope('ag2_middle'):
        gather.middle(A, C)
        gather.begin(B, C)
    with jax.named_scope('unpack'):
        small_pass.wait_recv()
        fetch = pltpu.make_async_copy(small_full, small_v, next(own_sem))
        fetch.start()
        fetch.wait()
        wait(loads)
        for layer in range(LAYERS):
            unpack_vectors(small_v, layer, places[A:B], places[B:C], vec_ref)
    with jax.named_scope('ag2_late'):
        gather.end(A, C, (B,))
    with jax.named_scope('ag2_end'):
        gather.end(A, C, (C,))

    def saves(layer):
        pairs = [(y_v, h_hbm.at[layer]), (qkv_v, qkv_hbm.at[layer])]
        kept = [pltpu.make_async_copy(src, dst, save_sem.at[n]) for n, (src, dst) in enumerate(pairs)]
        for n, (src, dst) in enumerate(((n1_t, n1_hbm), (n2_t, n2_hbm), (ctx_t, ctx_hbm))):
            dst = dst.at[layer, chip.core]
            kept.append((pltpu.make_async_copy(src, dst, save_sem.at[CORES + n]),
                         remote(src, dst, share_send.at[layer, n], share_recv.at[layer, n], chip.partner())))
        return kept

    def quarter(layer, t):
        rows, tiles = pl.ds(t * WIDTH, WIDTH), pl.ds(CORES * t, CORES)
        src, dst = act_t.at[rows], act_hbm.at[layer, chip.core, rows]
        return [pltpu.make_async_copy(pre_v.at[tiles], pre_hbm.at[layer, tiles], act_save.at[A, t]),
                pltpu.make_async_copy(src, dst, act_save.at[B, t]),
                remote(src, dst, act_send.at[layer, t], act_recv.at[layer, t], chip.partner())]

    def settle(layer):
        _, qkv_save, *shares = saves(layer)
        qkv_save.wait()
        for share in shares:
            wait(share)

        @loop(SIDE)
        def _(t):
            wait(quarter(layer, t))

    @loop(LAYERS)
    def _(layer):
        def vector(k, first=0, width=None):
            return vec_ref[pl.ds(layer, 1), lanes(OFFSETS[k] + first, width or SIZES[k])]

        def load(k, piece):
            if k == DOWN:
                return pltpu.make_async_copy(fulls[k].at[layer, piece], down_v.at[piece], load_sem.at[k, piece])
            cols = lanes(piece * WIDTH, WIDTH)
            return pltpu.make_async_copy(fulls[k].at[layer, :, :, :, :, :, cols], (up_v, None, mix_v)[k].at[:, :, :, :, :, cols],
                                         load_sem.at[k, piece])

        def matrix(held, piece):
            return held[:, :, :, :, :, lanes(piece * WIDTH, WIDTH)].reshape((WIDTH, WIDTH))

        def have(k):
            for which in range(LAYERS):
                @pl.when(layer == which)
                def _():
                    gather.arrived(which, k)

        def meanwhile(action):
            @pl.when(layer == A)
            def _():
                action()

        h_save, qkv_save, n1_share, n2_share, ctx_share = saves(layer)
        with jax.named_scope('have_mix'):
            have(MIX)
            start([load(MIX, k) for k in range(SIDE)])

        h_save.start()

        @pl.when(layer == B)
        def _():
            settle(A)

        with jax.named_scope('ln'):
            @loop(SEQ // LN_ROWS)
            def _(r):
                rows = pl.ds(pl.multiple_of(r * LN_ROWS, LN_ROWS), LN_ROWS)
                scaled, _ = normalised(y_v[rows, :].astype(F32))
                n1_v[rows, :] = (scaled * vector(GAIN1) + vector(BIAS1)).astype(BF16)
                n2_v[rows, :] = (scaled * vector(GAIN2) + vector(BIAS2)).astype(BF16)

        for src, dst, share in ((n1_v, n1_t, n1_share), (n2_v, n2_t, n2_share)):
            dst[...] = src[...].T
            start(share)

        with jax.named_scope('qkv'):
            @loop(PARTS)
            def _(k):
                load(MIX, k).wait()
                x = dot(n1_v[...], matrix(mix_v, k)) + vector(QKV_BIAS, k * WIDTH, WIDTH)

                @pl.when(k < C)
                def _():
                    for c in range(N_PAIRS):
                        block = turn(x[:, block_rows(c)], *[tables[n] for n in range(PARTS)])
                        qkv_v[:, lanes(k * WIDTH + c * PAIR)] = block.astype(BF16)

                @pl.when(k == C)
                def _():
                    qkv_v[:, lanes(k * WIDTH, WIDTH)] = x.astype(BF16)

        qkv_save.start()
        with jax.named_scope('have_up'):
            have(UP)
            have(DOWN)

        start([load(UP, k) for k in range(SIDE)] + [load(DOWN, k) for k in range(SIDE)])
        with jax.named_scope('fattn'):
            @loop(N_PAIRS)
            def _(pair):
                keys = split_heads(qkv_v[:, lanes(WIDTH + pair * PAIR)])
                values = split_heads(qkv_v[:, lanes(C * WIDTH + pair * PAIR)])
                for i in range(N_BLOCKS):
                    n = (i + 1) * CORES * PAIR
                    probs = probabilities(qkv_v[block_rows(i), lanes(pair * PAIR)], keys[:n], i)
                    ctx_v[block_rows(i), lanes(pair * PAIR)] = dot(side_by_side(probs), values[:n]).astype(BF16)

                @pl.when((layer == A) & (pair == C))
                def _():
                    gather.middle(B, C)

        ctx_t[...] = ctx_v[...].T
        start(ctx_share)
        meanwhile(lambda: gather.end(B, C, (B,)))
        with jax.named_scope('fout'):
            load(MIX, PARTS).wait()
            acc[...] = y_v[...].astype(F32) + dot(ctx_v[...], matrix(mix_v, PARTS)) + (vector(OUT_BIAS) + vector(DOWN_BIAS))

        with jax.named_scope('fmlp'):
            @loop(SIDE)
            def _(t):
                cols = lanes(t * WIDTH, WIDTH)
                load(UP, t).wait()
                pre = dot(n2_v[...], matrix(up_v, t)) + vector(UP_BIAS, t * WIDTH, WIDTH)
                for k in HALVES:
                    pre_v[CORES * t + k] = pre[:, k * TILE:(k + 1) * TILE]
                act = (0.5 * pre * (1.0 + lax.erf(pre * INV_SQRT2))).astype(BF16)
                act_t[cols, :] = act.T
                start(quarter(layer, t))
                load(DOWN, t).wait()
                acc[...] += dot(act, down_v[t].reshape((WIDTH, WIDTH)))

        h_save.wait()
        y_v[...] = acc[...].astype(BF16)
        with jax.named_scope('fend'):
            meanwhile(lambda: gather.end(B, C, (C,)))

    with jax.named_scope('ftail'):
        last = pltpu.make_async_copy(y_v, y_hbm, next(own_sem))
        last.start()
        for stage in range(AXES):
            for step in range(AXES):
                small_reach(stage, step).wait_send()
        small_pass.wait_send()
        gather.left()
        settle(LAYERS - 1)
        last.wait()


def forward(x, shards, small_tile, tables, places):
    grid = CHIPS + (CORES,)
    full = [(LAYERS,) + grid + tensor.shape[1:] for tensor in shards]
    shapes = [(shape, BF16) for shape in full] + [(grid + small_tile.shape, BF16), ((LAYERS, N_VEC), F32), ((SEQ, WIDTH), BF16),
                                                  ((LAYERS, SEQ, WIDTH), BF16)]
    shapes += [((LAYERS, CORES, width, SEQ), BF16) for width in (WIDTH, WIDTH, WIDTH, HIDDEN)]
    shapes += [((LAYERS, SEQ, QKV), BF16), ((LAYERS, N_TILES, SEQ, TILE), F32)]
    dma = pltpu.SemaphoreType.DMA
    slots = AXES * AXES
    scratch = [pltpu.VMEM(shape[1:], BF16) for shape in full] + [pltpu.VMEM(grid + small_tile.shape, BF16)]
    scratch += [pltpu.VMEM((SEQ, WIDTH), F32), pltpu.VMEM((N_TILES, SEQ, TILE), F32)]
    scratch += [pltpu.VMEM((SEQ, width), BF16) for width in (WIDTH, WIDTH, QKV, WIDTH, WIDTH)]
    scratch += [pltpu.VMEM((width, SEQ), BF16) for width in (WIDTH, WIDTH, WIDTH, HIDDEN)]
    scratch += [dma((LAYERS, AXES, len(HALVES), n)) for n in (slots, slots, slots + 1, slots + 1)]
    scratch += [dma(shape) for shape in ((slots + 1,), (slots + 1,), (slots + SIDE + AXES,), (AXES, SIDE), (SIDE + 1,), (LAYERS, AXES), (LAYERS, AXES), (CORES, SIDE), (LAYERS, SIDE), (LAYERS, SIDE))]
    scratch += [pltpu.VMEM(tables.shape, F32), pltpu.VMEM(places.shape, jnp.int32)]
    out_specs = [IN_VMEM if dtype == F32 and len(shape) == LAYERS else ANY for shape, dtype in shapes]
    return pl.pallas_call(
        forward_kernel,
        out_shape=[jax.ShapeDtypeStruct(*s) for s in shapes],
        in_specs=[ANY] * AXES + [IN_VMEM] * SIDE,
        out_specs=out_specs,
        scratch_shapes=scratch,
        compiler_params=pltpu.CompilerParams(collective_id=0, has_side_effects=True, vmem_limit_bytes=VMEM_LIMIT),
        name='forward_layers',
    )(x, tables, places, *shards, small_tile)


WAVES = ((384, 384, 512), (384, 384, 256), (256, 256, 256))
LEADS = ((2,) + CHIPS[1:], CHIPS[1:], (2, SIDE), (SIDE,), (AXES,))
W_UP, W_DOWN, W_QKV, W_OUT = range(4)
STEPS = ((1, (2,)), (0, ()), (2, (4, 3)), (4, (5,)), (3, ()), (5, (6, 7, 8)), (8, (9,)), (9, ()))
LAST = AXES * AXES
CARRIED = ((0, 6), (1, 4), (2, 0))
US_COLUMN, US_HOP, US_ADD, US_STEP = 0.022, 2.5, 0.0013, 0.2
US_FIRST, US_OUT, US_TILE, US_GRADIENT, US_PAIR, US_NORM = 4, 1.2, 1.5, 0.002, 2.15, 6


class Schedule:
    def __init__(self):
        self.now, self.free, self.lines = 0.0, {}, []

    def send(self, link, columns):
        self.free[link] = max(self.free.get(link, 0.0), self.now) + columns * US_COLUMN
        return self.free[link] + US_HOP

    def due(self, limit):
        found = []
        while self.lines:
            line = min(self.lines, key=lambda one: one[A][A]())
            ready = line[A][A]()
            if limit is not None and ready > limit:
                break
            _, run, sends, cost = line.pop(A)
            self.lines = [one for one in self.lines if one]
            self.now = max(self.now, ready) + cost
            sends()
            found.append(run)
        return found

    def run(self, limit):
        for step in self.due(limit):
            step()

    def passed(self, cost):
        self.now += cost
        self.run(self.now)

    def hooks(self, count, cost):
        planned = []
        for _ in range(count):
            self.now += cost
            planned.append(self.due(self.now))
        return planned


def at_hooks(n, planned):
    for when, steps in enumerate(planned):
        if steps:
            @pl.when(n == when)
            def _():
                for step in steps:
                    step()


def add_into(dst, src, n_axes):
    if n_axes < 2:
        dst[...] += src[...]
        return

    @loop(SIDE)
    def _(k):
        dst[k] += src[k]


def at_axis(ref, axis, value, n_axes):
    every = [pl.ds(0, SIDE)] * n_axes
    every[axis] = value
    return ref.at[tuple(every)]


class Reduce:
    def __init__(self, chip, schedule, wave, grads, came, fin, sems, spare, write, done, when=None):
        self.wave, self.chip, self.schedule, self.widths, self.grads = wave, chip, schedule, WAVES[wave], grads
        self.came, self.fin, (self.send_sem, self.recv_sem), (self.spare, self.spare_sem) = came, fin, sems, spare
        self.write, self.done, self.when, self.times = write, done, when, {}

    def box(self, a, half, stage):
        order = ORDERS[a]
        ref = self.came[a][A].at[half, A]
        spot = [axis for axis in range(AXES) if axis != order[A]].index(order[B])
        if stage == B:
            return ref, spot, C
        return at_axis(ref, spot, self.chip.where[order[B]], C), A, B

    def copy(self, a, half, slot):
        stage, turn = divmod(slot, AXES)
        sems = self.send_sem.at[a, half, slot], self.recv_sem.at[a, half, slot]
        if slot == LAST:
            return remote(self.total(a, half).at[self.chip.other], self.fin[a].at[half], *sems, self.chip.partner())
        axis = ORDERS[a][stage]
        if stage == C:
            role = value = ROLES[turn]
            dst = self.came[a][SIDE].at[half, turn]
        else:
            role, value = TWO if turn == C else ONE, (ONE, CROSS, TWO)[turn]
            dst = self.came[a][CORES * stage + turn // C].at[half]
            dst = dst if turn == C else dst.at[turn]
        value = self.chip.at(axis, value, half)
        if stage:
            ref, spot, n_axes = self.box(a, half, stage)
            src = at_axis(ref, spot, value, n_axes)
        else:
            src = self.came[a][A].at[half, B] if turn == C else at_axis(self.grads[a].at[half], axis, value, AXES)
        return remote(src, dst, *sems, self.chip.device(axis, role, half))

    def each(self, action):
        for a in range(AXES):
            halves(lambda half: action(a, half))

    def sending(self, slot):
        stage = slot // AXES
        share = SIDE ** (CORES * stage)
        self.times[slot] = self.schedule.now + US_HOP if slot == LAST else max(
            self.schedule.send(ORDERS[a][stage], self.widths[a] / share) for a in range(AXES))

    def begin(self):
        for slot in (B, A):
            self.each(lambda a, half: self.copy(a, half, slot).start())

    def plan(self, first=0, last=None):
        for slot in (B, A):
            self.times[slot] = self.schedule.now
            if not first:
                self.sending(slot)
        for _, sent in STEPS[:first]:
            self.times.update((slot, self.schedule.now + US_HOP) for slot in sent)
        self.schedule.lines.append([
            (lambda slot=slot: self.times[slot], lambda k=k: self.step(k), lambda sent=sent: [self.sending(n) for n in sent],
             CORES * US_ADD * sum(self.widths) if k < C else US_STEP) for k, (slot, sent) in enumerate(STEPS)][first:last])

    def step(self, k):
        def work():
            with jax.named_scope(f'w{self.wave}s{k}'):
                (self.first, self.first, self.halve, self.settle, self.settle, self.spread, self.cross, self.finish)[k](STEPS[k][A])
        if self.when is None:
            work()
        else:
            pl.when(self.when)(work)

    def first(self, slot):
        def local(a, half):
            axis = ORDERS[a][A]
            return pltpu.make_async_copy(at_axis(self.grads[a].at[half], axis, self.chip.at(axis, TWO if slot else OWN, half), AXES),
                                         self.spare.at[a, half, :, :, :, :, pl.ds(0, self.widths[a])], self.spare_sem.at[a, half])

        def action(a, half):
            local(a, half).wait()
            self.copy(a, half, slot).wait_recv()
            add_into(self.came[a][A].at[half, slot], self.spare.at[a, half, :, :, :, :, pl.ds(0, self.widths[a])], C)
            if slot:
                self.copy(a, half, C).start()

        self.each(lambda a, half: local(a, half).start())
        self.each(action)

    def halve(self, slot):
        def action(a, half):
            ref, spot, n_axes = self.box(a, half, B)
            self.copy(a, half, slot).wait_recv()
            for turn, role in ((B, CROSS), (A, ONE), (C, TWO), (C, OWN)):
                value = self.chip.at(ORDERS[a][B], role, half)
                add_into(at_axis(ref, spot, value, n_axes), at_axis(self.came[a][B].at[half], spot, value, n_axes), B)
                if turn < C:
                    self.copy(a, half, AXES + turn).start()
        self.each(action)

    def settle(self, slot):
        def action(a, half):
            ref, spot, n_axes = self.box(a, half, B)
            self.copy(a, half, slot).wait_recv()
            value = self.chip.at(ORDERS[a][B], TWO if slot > AXES else OWN, half)
            add_into(at_axis(ref, spot, value, n_axes), self.came[a][C].at[half, slot - AXES], B)
            if slot > AXES:
                self.copy(a, half, AXES + C).start()
        self.each(action)

    def spread(self, slot):
        def action(a, half):
            ref, *_ = self.box(a, half, C)
            self.copy(a, half, slot).wait_recv()
            add_into(ref, self.came[a][AXES].at[half], B)
            for turn in range(AXES):
                self.copy(a, half, CORES * AXES + turn).start()
        self.each(action)

    def total(self, a, half):
        ref, *_ = self.box(a, half, C)
        return ref.at[self.chip.where[ORDERS[a][C]]]

    def cross(self, _):
        def action(a, half):
            for turn in range(AXES):
                self.copy(a, half, CORES * AXES + turn).wait_recv()
            self.total(a, half)[...] += total_of([self.came[a][SIDE][half, turn] for turn in range(AXES)])
            self.copy(a, half, LAST).start()
        self.each(action)

    def finish(self, _):
        def action(a, half):
            self.write(a, half, self.chip.core, self.total(a, half)[self.chip.core])
            self.copy(a, half, LAST).wait_recv()
            self.write(a, half, self.chip.other, self.fin[a][half])
            self.copy(a, half, LAST).wait_send()
            for block, slot in ((self.came[a][A].at[half, A], A), (self.came[a][C].at[half, A], AXES),
                                (self.came[a][SIDE].at[half, A], CORES * AXES)):
                @loop(AXES)
                def _(turn):
                    sem = self.send_sem.at[a, half, slot + turn]
                    remote(block, block, sem, sem, self.chip.partner()).wait_send()
        self.each(action)
        self.done()


class VectorSum:
    def __init__(self, chip, schedule, total, came, sems, finish, when=None):
        self.schedule, self.total, self.came, self.sems, self.finish, self.when, self.ready = schedule, total, came, sems, finish, when, 0.0
        self.devices = [[chip.device(axis, role, A) for role in ROLES] for axis in range(AXES)] + [[chip.partner()]]

    def copies(self, k):
        return [remote(self.total, self.came.at[AXES * k + n], self.sems.at[A, AXES * k + n], self.sems.at[B, AXES * k + n], device)
                for n, device in enumerate(self.devices[k])]

    def sending(self, k):
        if k < SIDE:
            self.ready = self.schedule.send(k, N_VEC / (SIDE * SIDE * ROWS))

    def step(self, k):
        def work():
            with jax.named_scope(f'vec{k}'):
                wait(self.copies(k - 1))
                for n in range(len(self.devices[k - 1])):
                    self.total[...] += self.came[AXES * (k - 1) + n]
            if k < SIDE:
                start(self.copies(k))
            else:
                self.finish()
        if self.when is None:
            work()
        else:
            pl.when(self.when)(work)

    def begin(self):
        start(self.copies(A))

    def plan(self):
        self.sending(A)
        self.schedule.lines.append([
            (lambda: self.ready, lambda k=k: self.step(k), lambda k=k: self.sending(k), US_STEP) for k in range(1, SIDE + 1)])


def backward_kernel(ycot_hbm, tables, vec_ref, places, up_hbm, down_hbm, mix_hbm, h_hbm, n1_hbm, n2_hbm, ctx_hbm,
                    act_hbm, qkv_hbm, pre_hbm, dx_hbm, small_ref, up_sum, down_sum, qkv_sum, out_sum, dout_cols, dpre_cols,
                    dqkv_cols, *refs):
    n_arrays, sums = AXES * len(WAVES), (up_sum, down_sum, qkv_sum, out_sum)
    grads, refs = refs[:n_arrays], refs[n_arrays:]
    (spare, tile_v, big_v, rhs_v, wup_v, wdown_v, pre_v, dn1, dn2, dctx, dk_acc, dv_acc, qkv_v, dpre_v, dqkv_v, dh_v, h_v,
     totals, came_vec, send_sem, recv_sem, spare_sem, tile_sem, big_sem, rhs_sem, mlp_sem, io_sem, own_sem, share_send,
     share_recv, pre_sem, vec_sem, credit, *refs) = refs
    fins, came = refs[:n_arrays], refs[n_arrays:]
    with jax.named_scope('enter'):
        chip = enter()
    core, other = chip.core, chip.other
    first_in = pltpu.make_async_copy(ycot_hbm, dh_v, io_sem.at[A])
    first_in.start()

    def half_copies(layer, k, src, dst):
        width = dst.shape[-1]
        mine, away = [src.at[:, lanes(which * width, width)] for which in (core, other)]
        place = dst.at[layer, core]
        return [pltpu.make_async_copy(mine, place, own_sem.at[k]), remote(away, place, share_send.at[k], share_recv.at[k], chip.partner())]

    def tokens_load(layer, src, part, slot):
        return [pltpu.make_async_copy(src.at[layer, k, pl.ds(part * WIDTH, WIDTH)], big_v.at[slot, :, pl.ds(k * SEQ, SEQ)],
                                      big_sem.at[slot, k]) for k in range(CORES)]

    def weight_load(layer, k, slot):
        return pltpu.make_async_copy(mix_hbm.at[layer, :, lanes(k * WIDTH, WIDTH)], big_v.at[slot], big_sem.at[slot, CORES])

    def tile_loads(layer, t, slot):
        rows = lanes(t * TILE, TILE)
        pairs = ((down_hbm.at[layer, rows], wdown_v), (pre_hbm.at[layer, t], pre_v), (up_hbm.at[layer, :, rows], wup_v))
        return [pltpu.make_async_copy(src, dst.at[slot], mlp_sem.at[slot, n]) for n, (src, dst) in enumerate(pairs)]

    def input_loads(layer):
        return [pltpu.make_async_copy(qkv_hbm.at[layer], qkv_v, io_sem.at[B]), pltpu.make_async_copy(h_hbm.at[layer], h_v, io_sem.at[C])]

    def prefetch(layer):
        start(tokens_load(layer, act_hbm, A, A) + tokens_load(layer, act_hbm, B, B) + [weight_load(layer, AXES, C)])
        start(tokens_load(layer, ctx_hbm, A, AXES) + input_loads(layer))
        for t in HALVES:
            start(tile_loads(layer, t, t))

    prefetch(LAYERS - 1)
    with jax.named_scope('first_in'):
        first_in.wait()
    dx_copy = pltpu.make_async_copy(dh_v, dx_hbm, io_sem.at[A])
    start(half_copies(LAYERS - 1, A, dh_v, dout_cols))

    def vector_at(k, first=0, width=None):
        return lanes(OFFSETS[k] + first, width or SIZES[k])

    def reduction(schedule, layer, wave, when):
        def write(a, half, side, block):
            def put(arr, group, col, first, width):
                size = sums[arr].shape[-1] // CORES
                sums[arr][layer, group, :, lanes(side * size + col, width)] = block[:, first:first + width].astype(BF16)
            width, colour = WAVES[wave][a], CORES * a + half
            if wave:
                first = colour * width if wave == C or a < C else SIDE * WAVES[wave][A] + half * width
                put(W_QKV if wave == C else W_UP, A, first, A, width)
            elif a < C:
                put(W_DOWN, colour, A, A, width)
            else:
                for k in HALVES:
                    put(W_DOWN, CORES * half + k, WAVES[A][A], k * PAIR, PAIR)
                put(W_OUT, A, half * TWICE, TWICE, TWICE)

        def done():
            @pl.when(layer == LAYERS - 1)
            def _():
                chip.signal_partners(credit.at[wave])

        where = slice(AXES * wave, AXES * (wave + 1))
        count = len(LEADS)
        return Reduce(chip, schedule, wave, [grad.at[layer] for grad in grads[where]],
                      [came[count * (AXES * wave + a):count * (AXES * wave + a + 1)] for a in range(AXES)],
                      fins[where], (send_sem.at[wave], recv_sem.at[wave]), (spare, spare_sem), write, done, when)

    def vector_sum(schedule, layer, when):
        def own_part():
            with jax.named_scope('own'):
                node, local = chip.base
                me = node * (SIDE * CORES) + local + core
                row = jnp.zeros((ROWS, PAIR), F32)
                for cols in vector_blocks():
                    left = jnp.zeros((ROWS, WIDTH), F32) + totals[layer, :, cols] * (places[A:B, cols] == me).astype(F32)
                    for _ in range(PARTS):
                        row = row + dot_t(left.astype(BF16), pick_lanes(places[B:C], cols))
                        left = left - rounded(left)
                small_ref[layer] = row.astype(BF16)

            @pl.when(layer == LAYERS - 1)
            def _():
                chip.signal_partners(credit.at[AXES])

        return VectorSum(chip, schedule, totals.at[layer], came_vec, vec_sem, own_part, when)

    def run_on(schedule, layer, when):
        for wave, step in CARRIED:
            reduction(schedule, layer, wave, when).plan(step)
        vector_sum(schedule, layer, when).plan()

    @loop(LAYERS + 1)
    def _(turn_no):
        layer = LAYERS - 1 - turn_no
        working = pl.when(turn_no < LAYERS)
        total = totals.at[layer]
        schedule = Schedule()

        run_on(schedule, layer + 1, turn_no > A)

        def rhs_load(src, first, width, k):
            cols = lanes(first, width)
            return [pltpu.make_async_copy(src.at[layer, n, :, cols], rhs_v.at[pl.ds(n * SEQ, SEQ), cols], rhs_sem.at[k, n])
                    for n in range(CORES)]

        def product(lhs_slot, first, width, out_slot):
            value = dot(big_v[lhs_slot, :, 0:CORES * SEQ], rhs_v[:, lanes(first, width)])
            tile_v[out_slot, :, :, :, :, :, 0:width] = value.reshape(CHIPS + (CORES, ROWS, width))

        def tile_out(slot, src, dst):
            return pltpu.make_async_copy(src, dst, tile_sem.at[slot])

        def tile_done(slot, width):
            block = tile_v.at[slot, :, :, :, :, :, pl.ds(0, width)]
            tile_out(slot, block, grads[C].at[layer, A, :, :, :, :, :, pl.ds(0, width)]).wait()

        def columns(wave, a, half, first, width):
            return grads[AXES * wave + a].at[layer, half, :, :, :, :, :, pl.ds(first, width)]

        def launch(wave):
            @pl.when(turn_no == B)
            def _():
                pl.semaphore_wait(credit.at[wave], PARTNERS)

            current = reduction(schedule, layer, wave, turn_no < LAYERS)
            if wave == C:
                @pl.when(turn_no == B)
                def _():
                    pl.semaphore_wait(credit.at[AXES], PARTNERS)

                @working
                def _():
                    vector_sum(schedule, layer, None).begin()

            working(current.begin)
            if wave < C:
                current.plan(last=dict(CARRIED)[wave])

        @working
        def _():
            with jax.named_scope('dw_out'):
                d_sum = column_sum(dh_v[...].astype(F32))
                total[:, vector_at(OUT_BIAS)] = d_sum
                total[:, vector_at(DOWN_BIAS)] = d_sum
                weight_load(layer, AXES, C).wait()
                dctx[...] = dot_t(dh_v[...], big_v[C]).astype(BF16)
                start(tokens_load(layer, act_hbm, C, C))

                wait(half_copies(layer, A, dh_v, dout_cols))
                wait(start(rhs_load(dout_cols, A, TILE, A)))
                wait(tokens_load(layer, ctx_hbm, A, AXES))
                product(AXES, A, TILE, B)
                start(tokens_load(layer, act_hbm, AXES, AXES))
                for k in HALVES:
                    tile_out(B, tile_v.at[B, :, :, :, :, :, pl.ds(k * TWICE, TWICE)], columns(A, C, k, TWICE, TWICE)).start()

        schedule.passed(US_FIRST)
        out_hooks = schedule.hooks(SIDE, US_OUT)

        @loop(SIDE)
        def _(z):
            @working
            def _():
                slot = parity(z)
                wait(tokens_load(layer, act_hbm, z, z))

                @pl.when(z > A)
                def _():
                    tile_done(slot, TILE)

                product(z, A, TILE, slot)
                split = WAVES[A][A]
                for k in range(SIDE):
                    a, half = divmod(k, CORES)
                    for c in range(CORES):
                        block = tile_v.at[slot, :, :, CORES * c + a, half]
                        tile_out(slot, block.at[:, :, :, pl.ds(0, split)], grads[a].at[layer, half, z, :, :, c]).start()
                        tile_out(slot, block.at[:, :, :, pl.ds(split, PAIR)],
                                 grads[C].at[layer, a, z, :, :, c, :, pl.ds(half * PAIR, PAIR)]).start()

            at_hooks(z, out_hooks)

        @working
        def _():
            start(tokens_load(layer, n2_hbm, A, A) + [weight_load(layer, k, k + 1) for k in range(PARTS)])
            for slot in HALVES:
                tile_done(slot, TILE)

        schedule.passed(US_STEP)
        launch(A)

        @working
        def _():
            dn2[...] = jnp.zeros_like(dn2)

        def pre_copy(t, slot, away):
            place = dpre_cols.at[layer, core, :, lanes(lax.rem(t, SIDE) * TILE, TILE)]
            if away:
                return remote(dpre_v.at[slot], place, pre_sem.at[A, t], pre_sem.at[B, t], chip.partner())
            return pltpu.make_async_copy(dpre_v.at[slot], place, own_sem.at[CORES + slot])

        def pre_act(t, leave):
            for away, whose in ((False, core), (True, other)):
                @pl.when(lax.div(t, SIDE) == whose)
                def _():
                    copy = pre_copy(t, parity(t), away)
                    if leave:
                        copy.start()
                    elif away:
                        copy.wait_send()
                    else:
                        copy.wait()

        tile_hooks = schedule.hooks(N_TILES, US_TILE)

        with jax.named_scope('mlp'):
            @loop(N_TILES)
            def _(t):
                @working
                def _():
                    slot = parity(t)
                    wait(tile_loads(layer, t, slot))
                    d_act = rounded(dot_t(dh_v[...], wdown_v[slot]))
                    pre = pre_v[slot]
                    slope = 0.5 * (1.0 + lax.erf(pre * INV_SQRT2)) + pre * (INV_SQRT2PI * jnp.exp(-0.5 * pre * pre))
                    d_pre = d_act * slope
                    total[:, vector_at(UP_BIAS, t * TILE, TILE)] = column_sum(d_pre)

                    @pl.when(t > B)
                    def _():
                        pre_act(t - CORES, False)

                    dpre_v[slot] = d_pre.astype(BF16)
                    pre_act(t, True)
                    dn2[...] += dot_t(dpre_v[slot], wup_v[slot])

                    @pl.when(t + CORES < N_TILES)
                    def _():
                        start(tile_loads(layer, t + CORES, slot))

                at_hooks(t, tile_hooks)

        @working
        def _():
            for t in HALVES:
                pre_act(N_TILES - CORES + t, False)
            for t in range(SIDE):
                pre_copy(SIDE * core + t, A, True).wait_recv()

        def gradient_loads(wave, source):
            first = 0
            for k in range(CORES * AXES):
                width = WAVES[wave][k // CORES]
                start(rhs_load(source, first, width, k))
                first += width

        def gradient_wave(wave, source, first, base, orders):
            width, count = WAVES[wave][orders[A]], CORES * len(orders)
            planned = schedule.hooks(count, width * US_GRADIENT)

            @loop(count)
            def _(k):
                @working
                def _():
                    slot = parity(k)
                    wait(rhs_load(source, first + k * width, width, base + k))

                    @pl.when(k > B)
                    def _():
                        tile_done(slot, width)

                    product(A, first + k * width, width, slot)
                    block = tile_v.at[slot, :, :, :, :, :, pl.ds(0, width)]
                    for n, a in enumerate(orders):
                        @pl.when(lax.div(k, CORES) == n)
                        def _():
                            tile_out(slot, block, columns(wave, a, parity(k), 0, width)).start()

                at_hooks(k, planned)

            @working
            def _():
                for slot in HALVES:
                    tile_done(slot, width)

        @working
        def _():
            gradient_loads(B, dpre_cols)
            wait(tokens_load(layer, n2_hbm, A, A))

        with jax.named_scope('dw1'):
            gradient_wave(B, dpre_cols, A, A, (A, B))
            gradient_wave(B, dpre_cols, SIDE * WAVES[B][A], SIDE, (C,))
        launch(B)
        @working
        def _():
            start(tokens_load(layer, n1_hbm, A, A))
            wait(input_loads(layer))

        pair_hooks = schedule.hooks(N_PAIRS, US_PAIR)

        with jax.named_scope('attn'):
            @loop(N_PAIRS)
            def _(pair):
                @working
                def _():
                    at = lanes(pair * PAIR)
                    keys = split_heads(qkv_v[:, lanes(WIDTH + pair * PAIR)])
                    values = split_heads(qkv_v[:, lanes(C * WIDTH + pair * PAIR)])
                    q_t = qkv_v[:, at].T
                    dc_t = dctx[:, at].T
                    bias_sums = [jnp.zeros((1, PAIR), F32)] * PARTS

                    def turned_back(n, d, rows, to):
                        d = turn_back(rounded(d), *[tables[k, rows, :] for k in range(PARTS)])
                        bias_sums[n] = bias_sums[n] + column_sum(d)
                        dqkv_v[rows, to] = d.astype(BF16)

                    for i in range(N_BLOCKS):
                        old, n = i * TWICE, (i + 1) * TWICE
                        rows = block_rows(i)
                        probs = probabilities(qkv_v[rows, at], keys[:n], i)
                        d_all = rounded(dot_t(dctx[rows, at], values[:n]))
                        d_scores = [d_all[:, block_rows(j)] for j in range(CORES * (i + 1))]
                        for head in HALVES:
                            mine = slice(head, None, CORES)
                            mean = row_sum(total_of([p * d for p, d in zip(probs[mine], d_scores[mine])]))
                            d_scores[mine] = [p * (d - mean) * SCALE for p, d in zip(probs[mine], d_scores[mine])]
                        d_scores, probs = side_by_side(d_scores), side_by_side(probs)
                        turned_back(A, dot(d_scores, keys[:n]), rows, at)
                        for acc, left, right in ((dk_acc, q_t, d_scores), (dv_acc, dc_t, probs)):
                            part = dot(left[:, rows], right)
                            if i:
                                acc[:, :old] += part[:, :old]
                            acc[:, old:n] = part[:, old:]
                    first = iota((PAIR, PAIR), 0) < HEAD
                    for j in range(N_BLOCKS):
                        rows = block_rows(j)
                        d_key, d_value = [jnp.where(first, acc[:, block_rows(CORES * j)], acc[:, block_rows(CORES * j + 1)]).T
                                          for acc in (dk_acc, dv_acc)]
                        turned_back(B, d_key, rows, lanes(WIDTH + pair * PAIR))
                        d_value = d_value.astype(BF16)
                        bias_sums[C] = bias_sums[C] + column_sum(d_value.astype(F32))
                        dqkv_v[rows, lanes(C * WIDTH + pair * PAIR)] = d_value
                    for k, bias_sum in enumerate(bias_sums):
                        total[:, vector_at(QKV_BIAS, k * WIDTH + pair * PAIR, PAIR)] = bias_sum

                at_hooks(pair, pair_hooks)

        @working
        def _():
            start(half_copies(layer, B, dqkv_v, dqkv_cols))
            dn1[...] = jnp.zeros_like(dn1)

            with jax.named_scope('dn1'):
                @loop(PARTS)
                def _(k):
                    weight_load(layer, k, k + 1).wait()
                    dn1[...] += dot_t(dqkv_v[:, lanes(k * WIDTH, WIDTH)], big_v[k + 1])

            for k in (GAIN1, BIAS1, GAIN2, BIAS2):
                total[:, vector_at(k)] = jnp.zeros((1, WIDTH), F32)

            with jax.named_scope('lnb'):
                @loop(SEQ // LN_ROWS)
                def _(r):
                    rows = pl.ds(pl.multiple_of(r * LN_ROWS, LN_ROWS), LN_ROWS)
                    scaled, inverse = normalised(h_v[rows, :].astype(F32))
                    d1, d2 = rounded(dn1[rows, :]), rounded(dn2[rows, :])
                    for k, value in ((GAIN1, d1 * scaled), (BIAS1, d1), (GAIN2, d2 * scaled), (BIAS2, d2)):
                        total[:, vector_at(k)] += column_sum(value)
                    g1, g2 = [vec_ref[pl.ds(layer, 1), lanes(OFFSETS[k], WIDTH)] for k in (GAIN1, GAIN2)]
                    d_scaled = d1 * g1 + d2 * g2
                    d_h = inverse * (d_scaled - row_mean(d_scaled) - scaled * row_mean(d_scaled * scaled))
                    dh_v[rows, :] = (dh_v[rows, :].astype(F32) + d_h).astype(BF16)

        schedule.passed(US_NORM)
        @working
        def _():
            wait(half_copies(layer, B, dqkv_v, dqkv_cols))
            gradient_loads(C, dqkv_cols)
            wait(tokens_load(layer, n1_hbm, A, A))

        @pl.when(turn_no == A)
        def _():
            start(half_copies(layer - 1, A, dh_v, dout_cols))

        @pl.when(turn_no == B)
        def _():
            dx_copy.start()

        with jax.named_scope('dw2'):
            gradient_wave(C, dqkv_cols, A, A, (A, B, C))

        @pl.when(turn_no == A)
        def _():
            prefetch(layer - 1)

        schedule.run(None)
        launch(C)

    dx_copy.wait()


def backward(y_cot, tables, vectors, places, weights, saved):
    dma, one = pltpu.SemaphoreType.DMA, (1,)
    pair, wide, row = (len(HALVES),), (SEQ, WIDTH), one + (N_VEC,)
    shapes = [(wide, BF16), ((LAYERS, ROWS, PAIR), BF16)]
    shapes += [((LAYERS, groups, ROWS, width), BF16) for groups, width in ((*one, HIDDEN), (SIDE, WIDTH), (*one, QKV), (*one, WIDTH))]
    in_vmem = len(shapes)
    shapes += [((LAYERS, CORES, SEQ, width), BF16) for width in (TILE, SIDE * TILE, PARTS * TILE)]
    blocks = [(CORES, ROWS, width) for wave in WAVES for width in wave]
    shapes += [((LAYERS,) + pair + CHIPS + block, F32) for block in blocks]
    tile = (CORES, ROWS, TILE)
    scratch = [((AXES,) + pair + CHIPS[1:] + tile, F32), (pair + CHIPS + tile, F32), ((SIDE, WIDTH, WIDTH), BF16), ((CORES * SEQ, SIDE * TILE), BF16)]
    scratch += [(pair + shape, BF16) for shape in ((WIDTH, TILE), (TILE, WIDTH))]
    scratch += [(pair + (SEQ, TILE), F32), (wide, F32), (wide, F32), (wide, BF16)] + [((PAIR, CORES * SEQ), F32)] * CORES
    scratch += [((SEQ, QKV), BF16), (pair + (SEQ, TILE), BF16), ((SEQ, QKV), BF16), (wide, BF16), (wide, BF16), ((LAYERS,) + row, F32),
                ((PARTNERS,) + row, F32)]
    slots = (len(WAVES), AXES) + pair + (LAST + 1,)
    sems = [dma(shape) for shape in (slots, slots, (AXES,) + pair, pair, (SIDE, AXES), (CORES * AXES, CORES), pair + (PARTS,), (AXES,),
                                     (SIDE,), pair, pair, pair + (N_TILES,), pair + (PARTNERS,))]
    late = [(pair + block[1:], F32) for block in blocks] + [(pair + lead + block, F32) for block in blocks for lead in LEADS]
    outs = pl.pallas_call(
        backward_kernel,
        out_shape=[jax.ShapeDtypeStruct(*s) for s in shapes],
        in_specs=[ANY] + [IN_VMEM] * AXES + [ANY] * PARTNERS,
        out_specs=[ANY] + [IN_VMEM] * (in_vmem - 1) + [ANY] * (len(shapes) - in_vmem),
        scratch_shapes=[pltpu.VMEM(*s) for s in scratch] + sems + [pltpu.SemaphoreType.REGULAR((SIDE,))]
        + [pltpu.VMEM(*s) for s in late],
        compiler_params=pltpu.CompilerParams(collective_id=1, has_side_effects=True, vmem_limit_bytes=VMEM_LIMIT),
        name='backward_layers',
    )(y_cot, tables, vectors, places, *weights, *saved)
    d_x, small, *sums = outs[:in_vmem]
    return d_x, small[:, 0], [s.reshape((LAYERS, -1, s.shape[-1])) for s in sums]


def finish_kernel(*refs):
    n_large = CORES + AXES
    large, small_ref, refs = refs[:n_large], refs[n_large], refs[n_large + 1:]
    outs, small_outs, refs = refs[:n_large], refs[n_large:n_large + len(SHARES)], refs[n_large + len(SHARES):]
    held, sems = refs[:n_large], refs[n_large]
    loads = start([pltpu.make_async_copy(src, dst, sems.at[n]) for n, (src, dst) in enumerate(zip(large, held))])
    first = 0
    for share, out in zip(SHARES, small_outs):
        out[...] = small_ref[:, first:first + share]
        first += share
    stores = []
    for load, src, dst in zip(loads, held, outs):
        load.wait()
        stores += start([pltpu.make_async_copy(src, dst, sems.at[n_large + len(stores)])])
    wait(stores)


def finish(large, small):
    shapes = [jax.ShapeDtypeStruct(t.shape, BF16) for t in large] + [jax.ShapeDtypeStruct((LAYERS, share), BF16) for share in SHARES]
    outs = pl.pallas_call(
        finish_kernel,
        out_shape=shapes,
        in_specs=[ANY] * len(large) + [IN_VMEM],
        out_specs=[ANY] * len(large) + [IN_VMEM] * len(SHARES),
        scratch_shapes=[pltpu.VMEM(t.shape, BF16) for t in large] + [pltpu.SemaphoreType.DMA((CORES * len(large),))],
        name='finish',
    )(*large, small)
    return outs[:len(large)], outs[len(large):]


def rope_tables():
    rot_dim = HEAD // SIDE
    inv_freq = 1.0 / (10000.0 ** (jnp.arange(0, rot_dim, 2, dtype=F32) / rot_dim))
    angles = jnp.arange(SEQ, dtype=F32)[:, None] * inv_freq[None, :]
    cos, sin = jnp.cos(angles), jnp.sin(angles)
    zero = jnp.zeros_like(sin)
    rest = jnp.zeros((SEQ, HEAD - rot_dim), F32)
    tables = ([cos, cos, rest + 1.0], [-sin, zero, rest], [zero, sin, rest])
    return jnp.stack([jnp.tile(jnp.concatenate(table, axis=1), (1, 2)) for table in tables])


def heads_last(tensor):
    lead = tensor.shape[:-2]
    return tensor.reshape(lead + (HEADS, PARTS, HEAD)).swapaxes(-3, -2).reshape(lead + (QKV,))


def heads_first(tensor):
    lead = tensor.shape[:-1]
    return tensor.reshape(lead + (PARTS, HEADS, HEAD)).swapaxes(-3, -2).reshape(lead + (HEADS, PARTS * HEAD))


def vector_places():
    shard, lane, first = [], [], 0
    for k, (share, size) in enumerate(zip(SHARES, SIZES)):
        place = np.arange(size)
        if k == QKV_BIAS:
            place = heads_last(place.reshape(HEADS, -1))
        shard.append(place // share)
        lane.append(first + place % share)
        first += share
    return jnp.asarray(np.stack([np.concatenate(shard), np.concatenate(lane)]).astype(np.int32))


def solution(mesh):
    shard_axes = ('node', 'local')
    act_spec = P(shard_axes)
    param_spec = P(None, shard_axes)

    def device_step(x, y_cot, ln1_gain, ln1_bias, qkv_weight, qkv_bias, out_weight, out_bias,
                    ln2_gain, ln2_bias, up_weight, up_bias, down_weight, down_bias):
        tables, places = rope_tables(), vector_places()
        small = (ln1_gain, ln1_bias, ln2_gain, ln2_bias, qkv_bias, out_bias, up_bias, down_bias)
        small_tile = jnp.pad(jnp.concatenate(small, axis=1), ((0, ROWS - LAYERS), (0, PAIR - sum(SHARES))))
        mix = jnp.concatenate([heads_last(qkv_weight), out_weight], axis=-1)
        *weights, _, vectors, y_out, hidden, n1, n2, ctx, act, qkv, pre = forward(
            x[0], (up_weight, down_weight, mix), small_tile, tables, places)
        weights = [tensor.reshape((LAYERS, -1, tensor.shape[-1])) for tensor in weights]
        d_x, small_sums, (up, down, qkv, out) = backward(
            y_cot[0], tables, vectors, places, weights, (hidden, n1, n2, ctx, act, qkv, pre))
        (y_out, d_x, up, down, out), (g1, b1, g2, b2, qb, ob, ub, db) = finish((y_out, d_x, up, down, out), small_sums)
        return (y_out[None], d_x[None], g1, b1, heads_first(qkv), qb, out, ob, g2, b2, up, ub, down, db)

    return jax.shard_map(device_step, mesh=mesh,
                         in_specs=(act_spec, act_spec) + (param_spec,) * 12,
                         out_specs=(act_spec, act_spec) + (param_spec,) * 12,
                         check_vma=False)
```

```python
import functools
import jax
import jax.numpy as jnp
import numpy as np
from jax import lax
from jax.experimental import pallas as pl
from jax.experimental.pallas import tpu as pltpu
from jax.sharding import PartitionSpec as P

BF16, F32 = jnp.bfloat16, jnp.float32
EPSILON = 1e-5
MESH = pl.DeviceIdType.MESH
ANY = pl.BlockSpec(memory_space=pl.ANY)
IN_VMEM = pl.BlockSpec(memory_space=pltpu.VMEM)
VMEM_LIMIT = 67 * 10**6
LAYERS, AXES, SIDE, CORES, ROWS, PARTNERS = 2, 3, 4, 2, 8, 10
CHIPS = (SIDE, SIDE, SIDE)
SHARDS = SIDE * SIDE * SIDE * CORES
SEQ, WIDTH, HIDDEN, TILE, PAIR, LN_ROWS = 384, 1024, 4096, 512, 128, 64
HEADS, HEAD, PARTS = 16, 64, 3
QKV = PARTS * WIDTH
N_TILES, N_PAIRS, N_BLOCKS = HIDDEN // TILE, WIDTH // PAIR, SEQ // PAIR
TWICE = 2 * PAIR
INV_SQRT2, INV_SQRT2PI, SCALE = 0.7071067811865476, 0.3989422804014327, 0.125
SHARES = (8, 8, 8, 8, 24, 8, 32, 8)
SIZES = tuple(SHARDS * share for share in SHARES)
OFFSETS = tuple(sum(SIZES[:k]) for k in range(len(SIZES)))
N_VEC = sum(SIZES)
GAIN1, BIAS1, GAIN2, BIAS2, QKV_BIAS, OUT_BIAS, UP_BIAS, DOWN_BIAS = range(len(SHARES))
ORDERS = ((2, 1, 0), (1, 0, 2), (0, 2, 1))
HALVES = range(2)
OWN, ONE, CROSS, TWO = range(SIDE)
ROLES = (ONE, TWO, CROSS)
A, B, C = range(AXES)
UP, DOWN, MIX = range(3)
SELF = 3


class Chip:
    def __init__(self):
        node, local = lax.axis_index('node'), lax.axis_index('local')
        self.core, self.other = lax.rem(local, CORES), 1 - lax.rem(local, CORES)
        self.where = (lax.div(node, SIDE), lax.rem(node, SIDE), lax.div(local, CORES))
        self.base = (node, local - self.core)
        self.strides = ((SIDE, 0), (1, 0), (0, CORES))
        self.near = [(v, v + 1 - 2 * parity(v), lax.rem(v + 2, SIDE), SIDE - 1 - v) for v in self.where]

        self.gaps = [near[3] - near[1] for near in self.near]

    def at(self, axis, role, half):
        near = self.near[axis]
        if role in (OWN, CROSS):
            return near[role]
        return near[role] + half * self.gaps[axis] if role == ONE else near[role] - half * self.gaps[axis]

    def device(self, axis, role, half):
        shift = self.at(axis, role, half) - self.where[axis]
        node, local = [b + shift * s if s else b for b, s in zip(self.base, self.strides[axis])]
        return (node, local + self.core)

    def partner(self):
        node, local = self.base
        return (node, local + self.other)

    def signal_partners(self, semaphore):
        for axis in range(AXES):
            for role in ROLES:
                pl.semaphore_signal(semaphore, inc=1, device_id=self.device(axis, role, A), device_id_type=MESH)
        pl.semaphore_signal(semaphore, inc=1, device_id=self.partner(), device_id_type=MESH)


def enter(chip):
    barrier = pltpu.get_barrier_semaphore()
    chip.signal_partners(barrier)
    pl.semaphore_wait(barrier, PARTNERS)


def remote(src, dst, send_sem, recv_sem, device):
    return pltpu.make_async_remote_copy(src_ref=src, dst_ref=dst, send_sem=send_sem, recv_sem=recv_sem, device_id=device,
                                        device_id_type=MESH)


def start(copies):
    for copy in copies:
        copy.start()
    return copies


def wait(copies):
    for copy in copies:
        copy.wait()


def loop(count):
    return pl.loop(0, count)


def halves(body):
    loop(len(HALVES))(body)


def parity(n):
    return lax.rem(n, 2)


def pool(sems):
    return (sems.at[n] for n in range(sems.shape[0]))


def contract(a, b, a_axis, b_axis):
    return lax.dot_general(a, b, (((a_axis,), (b_axis,)), ((), ())), preferred_element_type=F32)


def dot(a, b):
    return contract(a, b, 1, 0)


def dot_t(a, b):
    return contract(a, b, 1, 1)


def row_sum(x):
    return jnp.sum(x, axis=1, keepdims=True)


def column_sum(x):
    return jnp.sum(x, axis=0, keepdims=True)


def rounded(x):
    return x.astype(BF16).astype(F32)


def lanes(first, width=PAIR):
    return pl.ds(pl.multiple_of(first, PAIR), width)


def turn(x, cos, sin_a, sin_b):
    return x * cos + pltpu.roll(x, PAIR - ROWS, 1) * sin_a + pltpu.roll(x, ROWS, 1) * sin_b


def turn_back(d, cos, sin_a, sin_b):
    return d * cos + pltpu.roll(d * sin_a, ROWS, 1) + pltpu.roll(d * sin_b, PAIR - ROWS, 1)


def iota(shape, axis):
    return lax.broadcasted_iota(jnp.int32, shape, axis)


def block_rows(j):
    return slice(j * PAIR, (j + 1) * PAIR)


def split_heads(x):
    first = iota((PAIR, PAIR), 1) < HEAD
    rows = []
    for j in range(N_BLOCKS):
        block = x[block_rows(j)]
        rows += [jnp.where(first, block, jnp.zeros_like(block)), jnp.where(first, jnp.zeros_like(block), block)]
    return jnp.concatenate(rows, axis=0)


def total_of(chunks, join=jnp.add):
    return functools.reduce(join, chunks)


def probabilities(q_block, keys, i):
    scores = dot_t(q_block, keys)
    causal = iota((PAIR, PAIR), 0) >= iota((PAIR, PAIR), 1)
    chunks = [scores[:, block_rows(j)] * SCALE for j in range(CORES * (i + 1))]
    for head in HALVES:
        mine = slice(head, None, CORES)
        *ahead, last = chunks[mine]
        held = ahead + [jnp.where(causal, last, -1e30)]
        top = jnp.max(total_of(held, jnp.maximum), axis=1, keepdims=True)
        held = [jnp.exp(chunk - top) for chunk in held]
        inverse = 1.0 / row_sum(total_of(held))
        chunks[mine] = [chunk * inverse for chunk in held]
    return chunks


def side_by_side(chunks):
    return jnp.concatenate([chunk.astype(BF16) for chunk in chunks], axis=1)


def row_mean(x):
    return jnp.mean(x, axis=1, keepdims=True)


def normalised(h):
    center = h - row_mean(h)
    inverse = lax.rsqrt(row_mean(center * center) + EPSILON)
    return center * inverse, inverse


class Gather:
    def __init__(self, chip, shards, fulls, sems):
        self.chip, self.shards, self.fulls = chip, shards, fulls
        self.send_sem, self.recv_sem, self.pass_send, self.pass_recv = sems

    def box(self, layer, k, half, stage, role, own=False):
        width = self.fulls[k].shape[-1] // len(HALVES)
        cols = lanes(half * width, width)
        if own:
            return self.shards[k].at[layer, :, cols]
        where = list(self.chip.where)
        for axis in ORDERS[k][:stage]:
            where[axis] = pl.ds(0, SIDE)
        axis = ORDERS[k][stage]
        where[axis] = self.chip.at(axis, role, half)
        return self.fulls[k].at[layer, where[0], where[1], where[2], self.chip.core, :, cols]

    def reach(self, layer, k, half, stage, step):
        slot, on = AXES * stage + step, stage > A and step == C
        src = self.box(layer, k, half, stage, ONE if on else OWN, stage == A)
        return remote(src, self.box(layer, k, half, stage, ONE if on else OWN), self.send_sem.at[layer, k, stage],
                      self.recv_sem.at[layer, k, half, slot], self.chip.device(ORDERS[k][stage], TWO if on else ROLES[step], half))

    def passing(self, layer, k, half, stage, step):
        role = (*ROLES, OWN)[step]
        return remote(self.box(layer, k, half, stage, role, step == SELF), self.box(layer, k, half, stage, role),
                      self.pass_send.at[layer, k], self.pass_recv.at[layer, k], self.chip.partner())

    def each(self, action):
        for k in (MIX, UP, DOWN):
            @halves
            def _(half):
                action(k, half)

    def begin(self, layer, stage):
        for step in range(C if stage else AXES):
            self.each(lambda k, half: self.reach(layer, k, half, stage, step).start())

    def own(self, layer):
        self.each(lambda k, half: self.passing(layer, k, half, A, SELF).start())

    def middle(self, layer, stage):
        def action(k, half):
            self.reach(layer, k, half, stage, A).wait_recv()
            self.reach(layer, k, half, stage, C).start()
            self.passing(layer, k, half, stage, A).start()
        self.each(action)

    def end(self, layer, stage, steps=range(AXES)):
        def action(k, half):
            for step in steps:
                self.reach(layer, k, half, stage, step).wait_recv()
                self.passing(layer, k, half, stage, step).start()
        self.each(action)

    def arrived(self, layer, k):
        box = self.fulls[k].at[layer, :, :, :, self.chip.other]
        remote(box, box, self.pass_send.at[layer, k], self.pass_recv.at[layer, k], self.chip.partner()).wait_recv()

    def left(self):
        three, full = pl.ds(0, AXES), self.fulls[UP].at[A]
        boxes = (full.at[three, A, A, A], full.at[:, three, A, A], full.at[:, :, three, A])

        @loop(LAYERS)
        def _(layer):
            @loop(AXES)
            def _(k):
                for stage, box in enumerate(boxes):
                    sem = self.send_sem.at[layer, k, stage]
                    remote(box, box, sem, sem, self.chip.partner()).wait_send()
                box, sem = full.at[:, :, :, A], self.pass_send.at[layer, k]
                remote(box, box, sem, sem, self.chip.partner()).wait_send()


def pick_lanes(sel_lane, cols):
    return (iota((PAIR, WIDTH), 0) == sel_lane[:, cols]).astype(F32).astype(BF16)


def vector_blocks():
    return [slice(k * WIDTH, (k + 1) * WIDTH) for k in range(N_VEC // WIDTH)]


def unpack_vectors(small_v, layer, sel_shard, sel_lane, vec_ref):
    tiles = small_v[...].astype(F32).reshape((SHARDS, ROWS, PAIR))
    held = jnp.sum(jnp.where(iota(tiles.shape, 1) == layer, tiles, 0.0), axis=1).astype(BF16)
    for cols in vector_blocks():
        spread = dot(held, pick_lanes(sel_lane, cols))
        spread = jnp.where(iota((SHARDS, WIDTH), 0) == sel_shard[:, cols], spread, 0.0)
        vec_ref[layer:layer + 1, cols] = column_sum(spread)


def forward_kernel(x_hbm, tables_hbm, places_hbm, up_s, down_s, mix_s, small_ref, up_f, down_f, mix_f, small_full, vec_ref,
                   y_hbm, h_hbm, n1_hbm, n2_hbm, ctx_hbm, act_hbm, qkv_hbm, pre_hbm, up_v, down_v, mix_v, small_v, acc, pre_v,
                   n1_v, n2_v, qkv_v, ctx_v, y_v, n1_t, n2_t, ctx_t, act_t, send_sem, recv_sem, pass_send, pass_recv,
                   small_send, small_recv, own_sems, load_sem, save_sem, share_send, share_recv, act_save, act_send, act_recv, tables,
                   places):
    shards, fulls, own_sem = (up_s, down_s, mix_s), (up_f, down_f, mix_f), pool(own_sems)
    chip = Chip()
    enter(chip)
    gather = Gather(chip, shards, fulls, (send_sem, recv_sem, pass_send, pass_recv))

    def small_copy(slot, where, device):
        place = small_full.at[(*where, chip.core)]
        return remote(place, place, small_send.at[slot], small_recv.at[slot], device)

    def small_reach(stage, step):
        where = list(chip.where)
        for axis in range(stage):
            where[axis] = pl.ds(0, SIDE)
        return small_copy(AXES * stage + step, where, chip.device(stage, ROLES[step], A))

    def small_begin(stage):
        start([small_reach(stage, step) for step in range(AXES)])

    def small_end(stage):
        for step in range(AXES):
            small_reach(stage, step).wait_recv()

    small_pass = small_copy(AXES * AXES, [pl.ds(0, SIDE)] * AXES, chip.partner())
    here = (*chip.where, chip.core)
    own = [pltpu.make_async_copy(small_ref, small_full.at[here], next(own_sem))]
    for shard, full in zip(shards, fulls):
        for layer in range(LAYERS):
            own.append(pltpu.make_async_copy(shard.at[layer], full.at[(layer, *here)], next(own_sem)))
    loads = [
        pltpu.make_async_copy(src, dst, next(own_sem)) for src, dst in ((x_hbm, y_v), (tables_hbm, tables), (places_hbm, places))]
    with jax.named_scope('ag0'):
        gather.begin(A, A)
        start(own)
        gather.begin(B, A)
        wait(own)
        small_begin(A)
        gather.own(A)
        gather.own(B)
        start(loads)
        gather.end(A, A)
    with jax.named_scope('ag1'):
        gather.begin(A, B)
        small_end(A)
        small_begin(B)
        gather.end(B, A)
        gather.begin(B, B)
        gather.middle(A, B)
        small_end(B)
        small_begin(C)
        gather.middle(B, B)
        gather.end(A, B, (B, C))
    with jax.named_scope('ag2_start'):
        gather.begin(A, C)
        small_end(C)
        small_pass.start()
        gather.end(B, B, (B, C))
    with jax.named_scope('ag2_middle'):
        gather.middle(A, C)
        gather.begin(B, C)
    with jax.named_scope('unpack'):
        small_pass.wait_recv()
        fetch = pltpu.make_async_copy(small_full, small_v, next(own_sem))
        fetch.start()
        fetch.wait()
        wait(loads)
        for layer in range(LAYERS):
            unpack_vectors(small_v, layer, places[A:B], places[B:C], vec_ref)
    with jax.named_scope('ag2_late'):
        gather.end(A, C, (B,))
    with jax.named_scope('ag2_end'):
        gather.end(A, C, (C,))

    def saves(layer):
        pairs = [(y_v, h_hbm.at[layer]), (qkv_v, qkv_hbm.at[layer])]
        kept = [pltpu.make_async_copy(src, dst, save_sem.at[n]) for n, (src, dst) in enumerate(pairs)]
        for n, (src, dst) in enumerate(((n1_t, n1_hbm), (n2_t, n2_hbm), (ctx_t, ctx_hbm))):
            dst = dst.at[layer, chip.core]
            kept.append((pltpu.make_async_copy(src, dst, save_sem.at[CORES + n]),
                         remote(src, dst, share_send.at[layer, n], share_recv.at[layer, n], chip.partner())))
        return kept

    def quarter(layer, t):
        rows, tiles = pl.ds(t * WIDTH, WIDTH), pl.ds(CORES * t, CORES)
        src, dst = act_t.at[rows], act_hbm.at[layer, chip.core, rows]
        return [pltpu.make_async_copy(pre_v.at[tiles], pre_hbm.at[layer, tiles], act_save.at[A, t]),
                pltpu.make_async_copy(src, dst, act_save.at[B, t]),
                remote(src, dst, act_send.at[layer, t], act_recv.at[layer, t], chip.partner())]

    def settle(layer):
        _, qkv_save, *shares = saves(layer)
        qkv_save.wait()
        for share in shares:
            wait(share)

        @loop(SIDE)
        def _(t):
            wait(quarter(layer, t))

    @loop(LAYERS)
    def _(layer):
        def vector(k, first=0, width=None):
            return vec_ref[pl.ds(layer, 1), lanes(OFFSETS[k] + first, width or SIZES[k])]

        def load(k, piece):
            if k == DOWN:
                return pltpu.make_async_copy(fulls[k].at[layer, piece], down_v.at[piece], load_sem.at[k, piece])
            cols = lanes(piece * WIDTH, WIDTH)
            return pltpu.make_async_copy(fulls[k].at[layer, :, :, :, :, :, cols], (up_v, None, mix_v)[k].at[:, :, :, :, :, cols],
                                         load_sem.at[k, piece])

        def matrix(held, piece):
            return held[:, :, :, :, :, lanes(piece * WIDTH, WIDTH)].reshape((WIDTH, WIDTH))

        def have(k):
            gather.arrived(layer, k)

        def meanwhile(action):
            @pl.when(layer == A)
            def _():
                action()

        h_save, qkv_save, n1_share, n2_share, ctx_share = saves(layer)
        with jax.named_scope('have_mix'):
            have(MIX)
            start([load(MIX, k) for k in range(SIDE)])

        h_save.start()

        @pl.when(layer == B)
        def _():
            settle(A)

        with jax.named_scope('ln'):
            @loop(SEQ // LN_ROWS)
            def _(r):
                rows = pl.ds(pl.multiple_of(r * LN_ROWS, LN_ROWS), LN_ROWS)
                scaled, _ = normalised(y_v[rows, :].astype(F32))
                n1_v[rows, :] = (scaled * vector(GAIN1) + vector(BIAS1)).astype(BF16)
                n2_v[rows, :] = (scaled * vector(GAIN2) + vector(BIAS2)).astype(BF16)

        for src, dst, share in ((n1_v, n1_t, n1_share), (n2_v, n2_t, n2_share)):
            dst[...] = src[...].T
            start(share)

        with jax.named_scope('qkv'):
            @loop(PARTS)
            def _(k):
                load(MIX, k).wait()
                x = dot(n1_v[...], matrix(mix_v, k)) + vector(QKV_BIAS, k * WIDTH, WIDTH)

                @pl.when(k < C)
                def _():
                    for c in range(N_PAIRS):
                        block = turn(x[:, block_rows(c)], *[tables[n] for n in range(PARTS)])
                        qkv_v[:, lanes(k * WIDTH + c * PAIR)] = block.astype(BF16)

                @pl.when(k == C)
                def _():
                    qkv_v[:, lanes(k * WIDTH, WIDTH)] = x.astype(BF16)

        qkv_save.start()
        with jax.named_scope('have_up'):
            have(UP)
            have(DOWN)

        start([load(UP, k) for k in range(SIDE)] + [load(DOWN, k) for k in range(SIDE)])
        with jax.named_scope('fattn'):
            def one_pair(pair):
                keys = split_heads(qkv_v[:, lanes(WIDTH + pair * PAIR)])
                values = split_heads(qkv_v[:, lanes(C * WIDTH + pair * PAIR)])
                for i in range(N_BLOCKS):
                    n = (i + 1) * CORES * PAIR
                    probs = probabilities(qkv_v[block_rows(i), lanes(pair * PAIR)], keys[:n], i)
                    ctx_v[block_rows(i), lanes(pair * PAIR)] = dot(side_by_side(probs), values[:n]).astype(BF16)

            @loop(N_PAIRS // CORES)
            def _(two):
                for k in HALVES:
                    one_pair(CORES * two + k)

                @pl.when((layer == A) & (two == A))
                def _():
                    gather.middle(B, C)

        ctx_t[...] = ctx_v[...].T
        start(ctx_share)
        meanwhile(lambda: gather.end(B, C, (B,)))
        with jax.named_scope('fout'):
            load(MIX, PARTS).wait()
            acc[...] = y_v[...].astype(F32) + dot(ctx_v[...], matrix(mix_v, PARTS)) + (vector(OUT_BIAS) + vector(DOWN_BIAS))

        with jax.named_scope('fmlp'):
            @loop(SIDE)
            def _(t):
                cols = lanes(t * WIDTH, WIDTH)
                load(UP, t).wait()
                pre = dot(n2_v[...], matrix(up_v, t)) + vector(UP_BIAS, t * WIDTH, WIDTH)
                for k in HALVES:
                    pre_v[CORES * t + k] = pre[:, k * TILE:(k + 1) * TILE]
                act = (0.5 * pre * (1.0 + lax.erf(pre * INV_SQRT2))).astype(BF16)
                act_t[cols, :] = act.T
                start(quarter(layer, t))
                load(DOWN, t).wait()
                acc[...] += dot(act, down_v[t].reshape((WIDTH, WIDTH)))

        h_save.wait()
        y_v[...] = acc[...].astype(BF16)
        with jax.named_scope('fend'):
            meanwhile(lambda: gather.end(B, C, (C,)))

    with jax.named_scope('ftail'):
        last = pltpu.make_async_copy(y_v, y_hbm, next(own_sem))
        last.start()
        for stage in range(AXES):
            for step in range(AXES):
                small_reach(stage, step).wait_send()
        small_pass.wait_send()
        gather.left()
        settle(LAYERS - 1)
        last.wait()


def forward(x, shards, small_tile, tables, places):
    grid = CHIPS + (CORES,)
    full = [(LAYERS,) + grid + tensor.shape[1:] for tensor in shards]
    shapes = [(shape, BF16) for shape in full] + [(grid + small_tile.shape, BF16), ((LAYERS, N_VEC), F32), ((SEQ, WIDTH), BF16),
                                                  ((LAYERS, SEQ, WIDTH), BF16)]
    shapes += [((LAYERS, CORES, width, SEQ), BF16) for width in (WIDTH, WIDTH, WIDTH, HIDDEN)]
    shapes += [((LAYERS, SEQ, QKV), BF16), ((LAYERS, N_TILES, SEQ, TILE), F32)]
    dma = pltpu.SemaphoreType.DMA
    slots = AXES * AXES
    scratch = [pltpu.VMEM(shape[1:], BF16) for shape in full] + [pltpu.VMEM(grid + small_tile.shape, BF16)]
    scratch += [pltpu.VMEM((SEQ, WIDTH), F32), pltpu.VMEM((N_TILES, SEQ, TILE), F32)]
    scratch += [pltpu.VMEM((SEQ, width), BF16) for width in (WIDTH, WIDTH, QKV, WIDTH, WIDTH)]
    scratch += [pltpu.VMEM((width, SEQ), BF16) for width in (WIDTH, WIDTH, WIDTH, HIDDEN)]
    scratch += [dma(shape) for shape in ((LAYERS, AXES, AXES), (LAYERS, AXES, len(HALVES), slots), (LAYERS, AXES), (LAYERS, AXES))]
    scratch += [dma(shape) for shape in ((slots + 1,), (slots + 1,), (slots + SIDE + AXES,), (AXES, SIDE), (SIDE + 1,), (LAYERS, AXES), (LAYERS, AXES), (CORES, SIDE), (LAYERS, SIDE), (LAYERS, SIDE))]
    scratch += [pltpu.VMEM(tables.shape, F32), pltpu.VMEM(places.shape, jnp.int32)]
    out_specs = [IN_VMEM if dtype == F32 and len(shape) == LAYERS else ANY for shape, dtype in shapes]
    return pl.pallas_call(
        forward_kernel,
        out_shape=[jax.ShapeDtypeStruct(*s) for s in shapes],
        in_specs=[ANY] * AXES + [IN_VMEM] * SIDE,
        out_specs=out_specs,
        scratch_shapes=scratch,
        compiler_params=pltpu.CompilerParams(collective_id=0, has_side_effects=True, vmem_limit_bytes=VMEM_LIMIT),
        name='forward_layers',
    )(x, tables, places, *shards, small_tile)


WAVES = ((384, 384, 512), (384, 384, 256), (256, 256, 256))
LEADS = ((2,) + CHIPS[1:], CHIPS[1:], (2, SIDE), (SIDE,), (AXES,))
W_UP, W_DOWN, W_QKV, W_OUT = range(4)
STEPS = ((1, (2,)), (0, ()), (2, (4, 3)), (4, (5,)), (3, ()), (5, (6, 7, 8)), (8, (9,)), (9, ()))
LAST = AXES * AXES
CARRIED = ((0, 6), (1, 4), (2, 0))
US_COLUMN, US_HOP, US_ADD, US_STEP = 0.022, 2.5, 0.0013, 0.2
US_FIRST, US_OUT, US_TILE, US_GRADIENT, US_PAIR, US_NORM = 4, 1.4, 1.6, 0.0025, 3.6, 2.7


class Schedule:
    def __init__(self):
        self.now, self.free, self.lines = 0.0, {}, []

    def send(self, link, columns):
        self.free[link] = max(self.free.get(link, 0.0), self.now) + columns * US_COLUMN
        return self.free[link] + US_HOP

    def due(self, limit):
        found = []
        while self.lines:
            line = min(self.lines, key=lambda one: one[A][A]())
            ready = line[A][A]()
            if limit is not None and ready > limit:
                break
            _, run, sends, cost = line.pop(A)
            self.lines = [one for one in self.lines if one]
            self.now = max(self.now, ready) + cost
            sends()
            found.append(run)
        return found

    def run(self, limit):
        for step in self.due(limit):
            step()

    def passed(self, cost):
        self.now += cost
        self.run(self.now)

    def hooks(self, count, cost):
        planned = []
        for _ in range(count):
            self.now += cost
            planned.append(self.due(self.now))
        return planned


def at_hooks(n, planned):
    for when, steps in enumerate(planned):
        if steps:
            @pl.when(n == when)
            def _():
                for step in steps:
                    step()


def add_into(dst, src, n_axes):
    if n_axes < 2:
        dst[...] += src[...]
        return

    @loop(SIDE)
    def _(k):
        dst[k] += src[k]


def at_axis(ref, axis, value, n_axes):
    every = [pl.ds(0, SIDE)] * n_axes
    every[axis] = value
    return ref.at[tuple(every)]


class Reduce:
    def __init__(self, chip, schedule, wave, grads, came, fin, sems, spare, write, done, when=None):
        self.wave, self.chip, self.schedule, self.widths, self.grads = wave, chip, schedule, WAVES[wave], grads
        self.came, self.fin, (self.send_sem, self.recv_sem), (self.spare, self.spare_sem) = came, fin, sems, spare
        self.write, self.done, self.when, self.times = write, done, when, {}

    def box(self, a, half, stage):
        order = ORDERS[a]
        ref = self.came[a][A].at[half, A]
        spot = [axis for axis in range(AXES) if axis != order[A]].index(order[B])
        if stage == B:
            return ref, spot, C
        return at_axis(ref, spot, self.chip.where[order[B]], C), A, B

    def copy(self, a, half, slot):
        stage, turn = divmod(slot, AXES)
        sems = self.send_sem.at[a, stage], self.recv_sem.at[a, half, slot]
        if slot == LAST:
            return remote(self.total(a, half).at[self.chip.other], self.fin[a].at[half], *sems, self.chip.partner())
        axis = ORDERS[a][stage]
        if stage == C:
            role = value = ROLES[turn]
            dst = self.came[a][SIDE].at[half, turn]
        else:
            role, value = TWO if turn == C else ONE, (ONE, CROSS, TWO)[turn]
            dst = self.came[a][CORES * stage + turn // C].at[half]
            dst = dst if turn == C else dst.at[turn]
        value = self.chip.at(axis, value, half)
        if stage:
            ref, spot, n_axes = self.box(a, half, stage)
            src = at_axis(ref, spot, value, n_axes)
        else:
            src = self.came[a][A].at[half, B] if turn == C else at_axis(self.grads[a].at[half], axis, value, AXES)
        return remote(src, dst, *sems, self.chip.device(axis, role, half))

    def each(self, action):
        for a in range(AXES):
            halves(lambda half: action(a, half))

    def sending(self, slot):
        stage = slot // AXES
        share = SIDE ** (CORES * stage)
        self.times[slot] = self.schedule.now + US_HOP if slot == LAST else max(
            self.schedule.send(ORDERS[a][stage], self.widths[a] / share) for a in range(AXES))

    def begin(self):
        for slot in (B, A):
            self.each(lambda a, half: self.copy(a, half, slot).start())

    def plan(self, first=0, last=None):
        for slot in (B, A):
            self.times[slot] = self.schedule.now
            if not first:
                self.sending(slot)
        for _, sent in STEPS[:first]:
            self.times.update((slot, self.schedule.now + US_HOP) for slot in sent)
        self.schedule.lines.append([
            (lambda slot=slot: self.times[slot], lambda k=k: self.step(k), lambda sent=sent: [self.sending(n) for n in sent],
             CORES * US_ADD * sum(self.widths) if k < C else US_STEP) for k, (slot, sent) in enumerate(STEPS)][first:last])

    def step(self, k):
        def work():
            with jax.named_scope(f'w{self.wave}s{k}'):
                (self.first, self.first, self.halve, self.settle, self.settle, self.spread, self.cross, self.finish)[k](STEPS[k][A])
        if self.when is None:
            work()
        else:
            pl.when(self.when)(work)

    def held(self, a, half):
        ref = self.spare[A].at[a] if a < C else self.spare[B]
        return ref.at[half, :, :, :, :, pl.ds(0, self.widths[a])]

    def first(self, slot):
        def local(a, half):
            axis = ORDERS[a][A]
            return pltpu.make_async_copy(at_axis(self.grads[a].at[half], axis, self.chip.at(axis, TWO if slot else OWN, half), AXES),
                                         self.held(a, half), self.spare_sem.at[a, half])

        def action(a, half):
            local(a, half).wait()
            self.copy(a, half, slot).wait_recv()
            add_into(self.came[a][A].at[half, slot], self.held(a, half), C)
            if slot:
                self.copy(a, half, C).start()

        self.each(lambda a, half: local(a, half).start())
        self.each(action)

    def halve(self, slot):
        def action(a, half):
            ref, spot, n_axes = self.box(a, half, B)
            self.copy(a, half, slot).wait_recv()
            for turn, role in ((B, CROSS), (A, ONE), (C, TWO), (C, OWN)):
                value = self.chip.at(ORDERS[a][B], role, half)
                add_into(at_axis(ref, spot, value, n_axes), at_axis(self.came[a][B].at[half], spot, value, n_axes), B)
                if turn < C:
                    self.copy(a, half, AXES + turn).start()
        self.each(action)

    def settle(self, slot):
        def action(a, half):
            ref, spot, n_axes = self.box(a, half, B)
            self.copy(a, half, slot).wait_recv()
            value = self.chip.at(ORDERS[a][B], TWO if slot > AXES else OWN, half)
            add_into(at_axis(ref, spot, value, n_axes), self.came[a][C].at[half, slot - AXES], B)
            if slot > AXES:
                self.copy(a, half, AXES + C).start()
        self.each(action)

    def spread(self, slot):
        def action(a, half):
            ref, *_ = self.box(a, half, C)
            self.copy(a, half, slot).wait_recv()
            add_into(ref, self.came[a][AXES].at[half], B)
            for turn in range(AXES):
                self.copy(a, half, CORES * AXES + turn).start()
        self.each(action)

    def total(self, a, half):
        ref, *_ = self.box(a, half, C)
        return ref.at[self.chip.where[ORDERS[a][C]]]

    def cross(self, _):
        def action(a, half):
            for turn in range(AXES):
                self.copy(a, half, CORES * AXES + turn).wait_recv()
            self.total(a, half)[...] += total_of([self.came[a][SIDE][half, turn] for turn in range(AXES)])
            self.copy(a, half, LAST).start()
        self.each(action)

    def finish(self, _):
        def action(a, half):
            self.write(a, half, self.chip.core, self.total(a, half)[self.chip.core])
            self.copy(a, half, LAST).wait_recv()
            self.write(a, half, self.chip.other, self.fin[a][half])
        self.each(action)
        three = pl.ds(0, AXES)
        for a, (grad, fin) in enumerate(zip(self.grads, self.fin)):
            for stage, block in enumerate((grad.at[:, :, :, three], grad.at[:, :, three, A], grad.at[:, three, A, A], fin)):
                sem = self.send_sem.at[a, stage]
                remote(block, block, sem, sem, self.chip.partner()).wait_send()
        self.done()


class VectorSum:
    def __init__(self, chip, schedule, total, came, sems, finish, when=None):
        self.schedule, self.total, self.came, self.sems, self.finish, self.when, self.ready = schedule, total, came, sems, finish, when, 0.0
        self.devices = [[chip.device(axis, role, A) for role in ROLES] for axis in range(AXES)] + [[chip.partner()]]

    def copies(self, k):
        return [remote(self.total, self.came.at[AXES * k + n], self.sems.at[A, AXES * k + n], self.sems.at[B, AXES * k + n], device)
                for n, device in enumerate(self.devices[k])]

    def sending(self, k):
        if k < SIDE:
            self.ready = self.schedule.send(k, N_VEC / (SIDE * SIDE * ROWS))

    def step(self, k):
        def work():
            with jax.named_scope(f'vec{k}'):
                wait(self.copies(k - 1))
                for n in range(len(self.devices[k - 1])):
                    self.total[...] += self.came[AXES * (k - 1) + n]
            if k < SIDE:
                start(self.copies(k))
            else:
                self.finish()
        if self.when is None:
            work()
        else:
            pl.when(self.when)(work)

    def begin(self):
        start(self.copies(A))

    def plan(self):
        self.sending(A)
        self.schedule.lines.append([
            (lambda: self.ready, lambda k=k: self.step(k), lambda k=k: self.sending(k), US_STEP) for k in range(1, SIDE + 1)])


def backward_kernel(ycot_hbm, tables, vec_ref, places, up_hbm, down_hbm, mix_hbm, h_hbm, n1_hbm, n2_hbm, ctx_hbm,
                    act_hbm, qkv_hbm, pre_hbm, dx_hbm, small_ref, up_sum, down_sum, qkv_sum, out_sum, dout_cols, dpre_cols,
                    dqkv_cols, *refs):
    n_arrays, sums = AXES * len(WAVES), (up_sum, down_sum, qkv_sum, out_sum)
    grads, refs = refs[:n_arrays], refs[n_arrays:]
    (spare, spare_wide, tile_v, big_v, rhs_v, wup_v, wdown_v, pre_v, dn1, dn2, dctx, dk_acc, dv_acc, qkv_v, dpre_v, dqkv_v, dh_v, h_v,
     totals, came_vec, send_sem, recv_sem, spare_sem, tile_sem, big_sem, rhs_sem, mlp_sem, io_sem, own_sem, share_send,
     share_recv, pre_sem, vec_sem, credit, *refs) = refs
    fins, came = refs[:n_arrays], refs[n_arrays:]
    first_in = pltpu.make_async_copy(ycot_hbm, dh_v, io_sem.at[A])
    first_in.start()
    chip = Chip()
    core, other = chip.core, chip.other

    def half_copies(layer, k, src, dst):
        width = dst.shape[-1]
        mine, away = [src.at[:, lanes(which * width, width)] for which in (core, other)]
        place = dst.at[layer, core]
        return [pltpu.make_async_copy(mine, place, own_sem.at[k]), remote(away, place, share_send.at[k], share_recv.at[k], chip.partner())]

    def tokens_load(layer, src, part, slot):
        return [pltpu.make_async_copy(src.at[layer, k, pl.ds(part * WIDTH, WIDTH)], big_v.at[slot, :, pl.ds(k * SEQ, SEQ)],
                                      big_sem.at[slot, k]) for k in range(CORES)]

    def weight_load(layer, k, slot):
        return pltpu.make_async_copy(mix_hbm.at[layer, :, lanes(k * WIDTH, WIDTH)], big_v.at[slot], big_sem.at[slot, CORES])

    def tile_loads(layer, t, slot):
        rows = lanes(t * TILE, TILE)
        pairs = ((down_hbm.at[layer, rows], wdown_v), (pre_hbm.at[layer, t], pre_v), (up_hbm.at[layer, :, rows], wup_v))
        return [pltpu.make_async_copy(src, dst.at[slot], mlp_sem.at[slot, n]) for n, (src, dst) in enumerate(pairs)]

    def input_loads(layer):
        return [pltpu.make_async_copy(qkv_hbm.at[layer], qkv_v, io_sem.at[B]), pltpu.make_async_copy(h_hbm.at[layer], h_v, io_sem.at[C])]

    def prefetch(layer):
        start([weight_load(layer, AXES, C)] + tokens_load(layer, ctx_hbm, A, AXES) + tokens_load(layer, act_hbm, A, A))

    def prefetch_more(layer):
        start(tokens_load(layer, act_hbm, B, B) + input_loads(layer))
        for t in HALVES:
            start(tile_loads(layer, t, t))

    prefetch(LAYERS - 1)
    with jax.named_scope('enter'):
        enter(chip)
    with jax.named_scope('first_in'):
        first_in.wait()
    dx_copy = pltpu.make_async_copy(dh_v, dx_hbm, io_sem.at[A])
    start(half_copies(LAYERS - 1, A, dh_v, dout_cols))
    prefetch_more(LAYERS - 1)

    def vector_at(k, first=0, width=None):
        return lanes(OFFSETS[k] + first, width or SIZES[k])

    def reduction(schedule, layer, wave, when):
        def write(a, half, side, block):
            def put(arr, group, col, first, width):
                size = sums[arr].shape[-1] // CORES
                sums[arr][layer, group, :, lanes(side * size + col, width)] = block[:, first:first + width].astype(BF16)
            width, colour = WAVES[wave][a], CORES * a + half
            if wave:
                first = colour * width if wave == C or a < C else SIDE * WAVES[wave][A] + half * width
                put(W_QKV if wave == C else W_UP, A, first, A, width)
            elif a < C:
                put(W_DOWN, colour, A, A, width)
            else:
                for k in HALVES:
                    put(W_DOWN, CORES * half + k, WAVES[A][A], k * PAIR, PAIR)
                put(W_OUT, A, half * TWICE, TWICE, TWICE)

        def done():
            @pl.when(layer == LAYERS - 1)
            def _():
                chip.signal_partners(credit.at[wave])

        where = slice(AXES * wave, AXES * (wave + 1))
        count = len(LEADS)
        return Reduce(chip, schedule, wave, [grad.at[layer] for grad in grads[where]],
                      [came[count * (AXES * wave + a):count * (AXES * wave + a + 1)] for a in range(AXES)],
                      fins[where], (send_sem.at[wave], recv_sem.at[wave]), ((spare, spare_wide), spare_sem), write, done, when)

    def vector_sum(schedule, layer, when):
        def own_part():
            with jax.named_scope('own'):
                node, local = chip.base
                me = node * (SIDE * CORES) + local + core
                row = jnp.zeros((ROWS, PAIR), F32)
                for cols in vector_blocks():
                    left = jnp.zeros((ROWS, WIDTH), F32) + totals[layer, :, cols] * (places[A:B, cols] == me).astype(F32)
                    for _ in range(PARTS):
                        row = row + dot_t(left.astype(BF16), pick_lanes(places[B:C], cols))
                        left = left - rounded(left)
                small_ref[layer] = row.astype(BF16)

            @pl.when(layer == LAYERS - 1)
            def _():
                chip.signal_partners(credit.at[AXES])

        return VectorSum(chip, schedule, totals.at[layer], came_vec, vec_sem, own_part, when)

    def run_on(schedule, layer, when):
        for wave, step in CARRIED:
            reduction(schedule, layer, wave, when).plan(step)
        vector_sum(schedule, layer, when).plan()

    @loop(LAYERS + 1)
    def _(turn_no):
        layer = LAYERS - 1 - turn_no
        working = pl.when(turn_no < LAYERS)
        total = totals.at[layer]
        schedule = Schedule()

        run_on(schedule, layer + 1, turn_no > A)

        def rhs_load(src, first, width, k):
            cols = lanes(first, width)
            return [pltpu.make_async_copy(src.at[layer, n, :, cols], rhs_v.at[pl.ds(n * SEQ, SEQ), cols], rhs_sem.at[k, n])
                    for n in range(CORES)]

        def product(lhs_slot, first, width, out_slot):
            value = dot(big_v[lhs_slot, :, 0:CORES * SEQ], rhs_v[:, lanes(first, width)])
            tile_v[out_slot, :, :, :, :, :, 0:width] = value.reshape(CHIPS + (CORES, ROWS, width))

        def tile_out(slot, src, dst):
            return pltpu.make_async_copy(src, dst, tile_sem.at[slot])

        def tile_done(slot, width):
            block = tile_v.at[slot, :, :, :, :, :, pl.ds(0, width)]
            tile_out(slot, block, block).wait()

        def columns(wave, a, half, first, width):
            return grads[AXES * wave + a].at[layer, half, :, :, :, :, :, pl.ds(first, width)]

        def launch(wave):
            @pl.when(turn_no == B)
            def _():
                pl.semaphore_wait(credit.at[wave], PARTNERS)

            current = reduction(schedule, layer, wave, turn_no < LAYERS)
            if wave == C:
                @pl.when(turn_no == B)
                def _():
                    pl.semaphore_wait(credit.at[AXES], PARTNERS)

                @working
                def _():
                    vector_sum(schedule, layer, None).begin()

            working(current.begin)
            if wave < C:
                current.plan(last=dict(CARRIED)[wave])

        @working
        def _():
            with jax.named_scope('dw_out'):
                d_sum = column_sum(dh_v[...].astype(F32))
                total[:, vector_at(OUT_BIAS)] = d_sum
                total[:, vector_at(DOWN_BIAS)] = d_sum
                weight_load(layer, AXES, C).wait()
                dctx[...] = dot_t(dh_v[...], big_v[C]).astype(BF16)
                start(tokens_load(layer, act_hbm, C, C))

                wait(half_copies(layer, A, dh_v, dout_cols))
                wait(start(rhs_load(dout_cols, A, TILE, A)))
                wait(tokens_load(layer, ctx_hbm, A, AXES))
                product(AXES, A, TILE, B)
                start(tokens_load(layer, act_hbm, AXES, AXES))
                for k in HALVES:
                    tile_out(B, tile_v.at[B, :, :, :, :, :, pl.ds(k * TWICE, TWICE)], columns(A, C, k, TWICE, TWICE)).start()

        schedule.passed(US_FIRST)
        out_hooks = schedule.hooks(SIDE, US_OUT)

        @loop(SIDE)
        def _(z):
            @working
            def _():
                slot = parity(z)
                wait(tokens_load(layer, act_hbm, z, z))

                @pl.when(z > A)
                def _():
                    tile_done(slot, TILE)

                product(z, A, TILE, slot)
                split = WAVES[A][A]
                for k in range(SIDE):
                    a, half = divmod(k, CORES)
                    for c in range(CORES):
                        block = tile_v.at[slot, :, :, CORES * c + a, half]
                        tile_out(slot, block.at[:, :, :, pl.ds(0, split)], grads[a].at[layer, half, z, :, :, c]).start()
                        tile_out(slot, block.at[:, :, :, pl.ds(split, PAIR)],
                                 grads[C].at[layer, a, z, :, :, c, :, pl.ds(half * PAIR, PAIR)]).start()

            at_hooks(z, out_hooks)

        @working
        def _():
            start(tokens_load(layer, n2_hbm, A, A) + [weight_load(layer, k, k + 1) for k in range(PARTS)])
            for slot in HALVES:
                tile_done(slot, TILE)

        schedule.passed(US_STEP)
        launch(A)

        @working
        def _():
            dn2[...] = jnp.zeros_like(dn2)

        def pre_copy(t, slot, away):
            place = dpre_cols.at[layer, core, :, lanes(lax.rem(t, SIDE) * TILE, TILE)]
            if away:
                return remote(dpre_v.at[slot], place, pre_sem.at[A, t], pre_sem.at[B, t], chip.partner())
            return pltpu.make_async_copy(dpre_v.at[slot], place, own_sem.at[CORES + slot])

        def pre_act(t, leave):
            for away, whose in ((False, core), (True, other)):
                @pl.when(lax.div(t, SIDE) == whose)
                def _():
                    copy = pre_copy(t, parity(t), away)
                    if leave:
                        copy.start()
                    elif away:
                        copy.wait_send()
                    else:
                        copy.wait()

        tile_hooks = schedule.hooks(N_TILES, US_TILE)

        with jax.named_scope('mlp'):
            @loop(N_TILES)
            def _(t):
                @working
                def _():
                    slot = parity(t)
                    wait(tile_loads(layer, t, slot))
                    d_act = rounded(dot_t(dh_v[...], wdown_v[slot]))
                    pre = pre_v[slot]
                    slope = 0.5 * (1.0 + lax.erf(pre * INV_SQRT2)) + pre * (INV_SQRT2PI * jnp.exp(-0.5 * pre * pre))
                    d_pre = d_act * slope
                    total[:, vector_at(UP_BIAS, t * TILE, TILE)] = column_sum(d_pre)

                    @pl.when(t > B)
                    def _():
                        pre_act(t - CORES, False)

                    dpre_v[slot] = d_pre.astype(BF16)
                    pre_act(t, True)
                    dn2[...] += dot_t(dpre_v[slot], wup_v[slot])

                    @pl.when(t + CORES < N_TILES)
                    def _():
                        start(tile_loads(layer, t + CORES, slot))

                at_hooks(t, tile_hooks)

        @working
        def _():
            for t in HALVES:
                pre_act(N_TILES - CORES + t, False)
            for t in range(SIDE):
                pre_copy(SIDE * core + t, A, True).wait_recv()

        def gradient_loads(wave, source):
            first = 0
            for a in range(AXES):
                width = CORES * WAVES[wave][a]
                start(rhs_load(source, first, width, a))
                first += width

        def gradient_wave(wave, source, first, orders):
            split, count = WAVES[wave][orders[A]], len(orders)
            width = CORES * split
            planned = schedule.hooks(count, width * US_GRADIENT)

            @loop(count)
            def _(n):
                @working
                def _():
                    slot = parity(n)
                    wait(rhs_load(source, first + n * width, width, orders[A] + n))

                    @pl.when(n > B)
                    def _():
                        tile_done(slot, width)

                    product(A, first + n * width, width, slot)
                    for k, a in enumerate(orders):
                        @pl.when(n == k)
                        def _():
                            for half in HALVES:
                                block = tile_v.at[slot, :, :, :, :, :, pl.ds(half * split, split)]
                                tile_out(slot, block, columns(wave, a, half, 0, split)).start()

                at_hooks(n, planned)

            @working
            def _():
                for slot in range(min(count, CORES)):
                    tile_done(slot, width)

        @working
        def _():
            gradient_loads(B, dpre_cols)
            wait(tokens_load(layer, n2_hbm, A, A))

        with jax.named_scope('dw1'):
            gradient_wave(B, dpre_cols, A, (A, B))
            gradient_wave(B, dpre_cols, SIDE * WAVES[B][A], (C,))
        launch(B)
        @working
        def _():
            start(tokens_load(layer, n1_hbm, A, A))
            wait(input_loads(layer))

        pair_hooks = schedule.hooks(N_PAIRS // CORES, US_PAIR)

        with jax.named_scope('attn'):
            def one_pair(pair, dk_sum, dv_sum):
                at = lanes(pair * PAIR)
                keys = split_heads(qkv_v[:, lanes(WIDTH + pair * PAIR)])
                values = split_heads(qkv_v[:, lanes(C * WIDTH + pair * PAIR)])
                q_t = qkv_v[:, at].T
                dc_t = dctx[:, at].T
                bias_sums = [jnp.zeros((1, PAIR), F32)] * PARTS

                def turned_back(n, d, rows, to):
                    d = turn_back(rounded(d), *[tables[k, rows, :] for k in range(PARTS)])
                    bias_sums[n] = bias_sums[n] + column_sum(d)
                    dqkv_v[rows, to] = d.astype(BF16)

                for i in range(N_BLOCKS):
                    old, n = i * TWICE, (i + 1) * TWICE
                    rows = block_rows(i)
                    probs = probabilities(qkv_v[rows, at], keys[:n], i)
                    d_all = rounded(dot_t(dctx[rows, at], values[:n]))
                    d_scores = [d_all[:, block_rows(j)] for j in range(CORES * (i + 1))]
                    for head in HALVES:
                        mine = slice(head, None, CORES)
                        mean = row_sum(total_of([p * d for p, d in zip(probs[mine], d_scores[mine])]))
                        d_scores[mine] = [p * (d - mean) * SCALE for p, d in zip(probs[mine], d_scores[mine])]
                    d_scores, probs = side_by_side(d_scores), side_by_side(probs)
                    turned_back(A, dot(d_scores, keys[:n]), rows, at)
                    for acc, left, right in ((dk_sum, q_t, d_scores), (dv_sum, dc_t, probs)):
                        part = dot(left[:, rows], right)
                        if i:
                            acc[:, :old] += part[:, :old]
                        acc[:, old:n] = part[:, old:]
                first = iota((PAIR, PAIR), 0) < HEAD
                for j in range(N_BLOCKS):
                    rows = block_rows(j)
                    d_key, d_value = [jnp.where(first, acc[:, block_rows(CORES * j)], acc[:, block_rows(CORES * j + 1)]).T
                                      for acc in (dk_sum, dv_sum)]
                    turned_back(B, d_key, rows, lanes(WIDTH + pair * PAIR))
                    d_value = d_value.astype(BF16)
                    bias_sums[C] = bias_sums[C] + column_sum(d_value.astype(F32))
                    dqkv_v[rows, lanes(C * WIDTH + pair * PAIR)] = d_value
                for k, bias_sum in enumerate(bias_sums):
                    total[:, vector_at(QKV_BIAS, k * WIDTH + pair * PAIR, PAIR)] = bias_sum

            @loop(N_PAIRS // CORES)
            def _(two):
                @working
                def _():
                    for k in HALVES:
                        one_pair(CORES * two + k, dk_acc.at[k], dv_acc.at[k])

                at_hooks(two, pair_hooks)

        @working
        def _():
            start(half_copies(layer, B, dqkv_v, dqkv_cols))
            dn1[...] = jnp.zeros_like(dn1)

            with jax.named_scope('dn1'):
                @loop(PARTS)
                def _(k):
                    weight_load(layer, k, k + 1).wait()
                    dn1[...] += dot_t(dqkv_v[:, lanes(k * WIDTH, WIDTH)], big_v[k + 1])

        schedule.passed(US_NORM)

        @working
        def _():
            for k in (GAIN1, BIAS1, GAIN2, BIAS2):
                total[:, vector_at(k)] = jnp.zeros((1, WIDTH), F32)

            with jax.named_scope('lnb'):
                @loop(SEQ // LN_ROWS)
                def _(r):
                    rows = pl.ds(pl.multiple_of(r * LN_ROWS, LN_ROWS), LN_ROWS)
                    scaled, inverse = normalised(h_v[rows, :].astype(F32))
                    d1, d2 = rounded(dn1[rows, :]), rounded(dn2[rows, :])
                    for k, value in ((GAIN1, d1 * scaled), (BIAS1, d1), (GAIN2, d2 * scaled), (BIAS2, d2)):
                        total[:, vector_at(k)] += column_sum(value)
                    g1, g2 = [vec_ref[pl.ds(layer, 1), lanes(OFFSETS[k], WIDTH)] for k in (GAIN1, GAIN2)]
                    d_scaled = d1 * g1 + d2 * g2
                    d_h = inverse * (d_scaled - row_mean(d_scaled) - scaled * row_mean(d_scaled * scaled))
                    dh_v[rows, :] = (dh_v[rows, :].astype(F32) + d_h).astype(BF16)

        schedule.passed(US_NORM)
        @working
        def _():
            wait(half_copies(layer, B, dqkv_v, dqkv_cols))
            gradient_loads(C, dqkv_cols)
            wait(tokens_load(layer, n1_hbm, A, A))

        @pl.when(turn_no == A)
        def _():
            start(half_copies(layer - 1, A, dh_v, dout_cols))

        @pl.when(turn_no == B)
        def _():
            dx_copy.start()

        with jax.named_scope('dw2'):
            gradient_wave(C, dqkv_cols, A, (A, B, C))

        @pl.when(turn_no == A)
        def _():
            prefetch(layer - 1)
            prefetch_more(layer - 1)

        schedule.run(None)
        launch(C)

    dx_copy.wait()


def backward(y_cot, tables, vectors, places, weights, saved):
    dma, one = pltpu.SemaphoreType.DMA, (1,)
    pair, wide, row = (len(HALVES),), (SEQ, WIDTH), one + (N_VEC,)
    shapes = [(wide, BF16), ((LAYERS, ROWS, PAIR), BF16)]
    shapes += [((LAYERS, groups, ROWS, width), BF16) for groups, width in ((*one, HIDDEN), (SIDE, WIDTH), (*one, QKV), (*one, WIDTH))]
    in_vmem = len(shapes)
    shapes += [((LAYERS, CORES, SEQ, width), BF16) for width in (TILE, SIDE * TILE, PARTS * TILE)]
    blocks = [(CORES, ROWS, width) for wave in WAVES for width in wave]
    shapes += [((LAYERS,) + pair + CHIPS + block, F32) for block in blocks]
    tile = (CORES, ROWS)
    scratch = [(pair + pair + CHIPS[1:] + tile + (WAVES[0][0],), F32), (pair + CHIPS[1:] + tile + (TILE,), F32), (pair + CHIPS + tile + (CORES * WAVES[0][0],), F32), ((SIDE, WIDTH, WIDTH), BF16), ((CORES * SEQ, SIDE * TILE), BF16)]
    scratch += [(pair + shape, BF16) for shape in ((WIDTH, TILE), (TILE, WIDTH))]
    scratch += [(pair + (SEQ, TILE), F32), (wide, F32), (wide, F32), (wide, BF16)] + [(pair + (PAIR, CORES * SEQ), F32)] * CORES
    scratch += [((SEQ, QKV), BF16), (pair + (SEQ, TILE), BF16), ((SEQ, QKV), BF16), (wide, BF16), (wide, BF16), ((LAYERS,) + row, F32),
                ((PARTNERS,) + row, F32)]
    slots = (len(WAVES), AXES) + pair + (LAST + 1,)
    sems = [dma(shape) for shape in ((len(WAVES), AXES, SIDE), slots, (AXES,) + pair, pair, (SIDE, AXES), (AXES, CORES), pair + (PARTS,), (AXES,),
                                     (SIDE,), pair, pair, pair + (N_TILES,), pair + (PARTNERS,))]
    late = [(pair + block[1:], F32) for block in blocks] + [(pair + lead + block, F32) for block in blocks for lead in LEADS]
    outs = pl.pallas_call(
        backward_kernel,
        out_shape=[jax.ShapeDtypeStruct(*s) for s in shapes],
        in_specs=[ANY] + [IN_VMEM] * AXES + [ANY] * PARTNERS,
        out_specs=[ANY] + [IN_VMEM] * (in_vmem - 1) + [ANY] * (len(shapes) - in_vmem),
        scratch_shapes=[pltpu.VMEM(*s) for s in scratch] + sems + [pltpu.SemaphoreType.REGULAR((SIDE,))]
        + [pltpu.VMEM(*s) for s in late],
        compiler_params=pltpu.CompilerParams(collective_id=1, has_side_effects=True, vmem_limit_bytes=VMEM_LIMIT),
        name='backward_layers',
    )(y_cot, tables, vectors, places, *weights, *saved)
    d_x, small, *sums = outs[:in_vmem]
    return d_x, small[:, 0], [s.reshape((LAYERS, -1, s.shape[-1])) for s in sums]


def finish_kernel(*refs):
    n_large = CORES + AXES
    large, small_ref, refs = refs[:n_large], refs[n_large], refs[n_large + 1:]
    outs, small_outs, refs = refs[:n_large], refs[n_large:n_large + len(SHARES)], refs[n_large + len(SHARES):]
    held, sems = refs[:n_large], refs[n_large]
    loads = start([pltpu.make_async_copy(src, dst, sems.at[n]) for n, (src, dst) in enumerate(zip(large, held))])
    first = 0
    for share, out in zip(SHARES, small_outs):
        out[...] = small_ref[:, first:first + share]
        first += share
    stores = []
    for load, src, dst in zip(loads, held, outs):
        load.wait()
        stores += start([pltpu.make_async_copy(src, dst, sems.at[n_large + len(stores)])])
    wait(stores)


def finish(large, small):
    shapes = [jax.ShapeDtypeStruct(t.shape, BF16) for t in large] + [jax.ShapeDtypeStruct((LAYERS, share), BF16) for share in SHARES]
    outs = pl.pallas_call(
        finish_kernel,
        out_shape=shapes,
        in_specs=[ANY] * len(large) + [IN_VMEM],
        out_specs=[ANY] * len(large) + [IN_VMEM] * len(SHARES),
        scratch_shapes=[pltpu.VMEM(t.shape, BF16) for t in large] + [pltpu.SemaphoreType.DMA((CORES * len(large),))],
        name='finish',
    )(*large, small)
    return outs[:len(large)], outs[len(large):]


def rope_tables():
    rot_dim = HEAD // SIDE
    inv_freq = 1.0 / (10000.0 ** (jnp.arange(0, rot_dim, 2, dtype=F32) / rot_dim))
    angles = jnp.arange(SEQ, dtype=F32)[:, None] * inv_freq[None, :]
    cos, sin = jnp.cos(angles), jnp.sin(angles)
    zero = jnp.zeros_like(sin)
    rest = jnp.zeros((SEQ, HEAD - rot_dim), F32)
    tables = ([cos, cos, rest + 1.0], [-sin, zero, rest], [zero, sin, rest])
    return jnp.stack([jnp.tile(jnp.concatenate(table, axis=1), (1, 2)) for table in tables])


def heads_last(tensor):
    lead = tensor.shape[:-2]
    return tensor.reshape(lead + (HEADS, PARTS, HEAD)).swapaxes(-3, -2).reshape(lead + (QKV,))


def heads_first(tensor):
    lead = tensor.shape[:-1]
    return tensor.reshape(lead + (PARTS, HEADS, HEAD)).swapaxes(-3, -2).reshape(lead + (HEADS, PARTS * HEAD))


def vector_places():
    shard, lane, first = [], [], 0
    for k, (share, size) in enumerate(zip(SHARES, SIZES)):
        place = np.arange(size)
        if k == QKV_BIAS:
            place = heads_last(place.reshape(HEADS, -1))
        shard.append(place // share)
        lane.append(first + place % share)
        first += share
    return jnp.asarray(np.stack([np.concatenate(shard), np.concatenate(lane)]).astype(np.int32))


def solution(mesh):
    shard_axes = ('node', 'local')
    act_spec = P(shard_axes)
    param_spec = P(None, shard_axes)

    def device_step(x, y_cot, ln1_gain, ln1_bias, qkv_weight, qkv_bias, out_weight, out_bias,
                    ln2_gain, ln2_bias, up_weight, up_bias, down_weight, down_bias):
        tables, places = rope_tables(), vector_places()
        small = (ln1_gain, ln1_bias, ln2_gain, ln2_bias, qkv_bias, out_bias, up_bias, down_bias)
        small_tile = jnp.pad(jnp.concatenate(small, axis=1), ((0, ROWS - LAYERS), (0, PAIR - sum(SHARES))))
        mix = jnp.concatenate([heads_last(qkv_weight), out_weight], axis=-1)
        *weights, _, vectors, y_out, hidden, n1, n2, ctx, act, qkv, pre = forward(
            x[0], (up_weight, down_weight, mix), small_tile, tables, places)
        weights = [tensor.reshape((LAYERS, -1, tensor.shape[-1])) for tensor in weights]
        d_x, small_sums, (up, down, qkv, out) = backward(
            y_cot[0], tables, vectors, places, weights, (hidden, n1, n2, ctx, act, qkv, pre))
        (y_out, d_x, up, down, out), (g1, b1, g2, b2, qb, ob, ub, db) = finish((y_out, d_x, up, down, out), small_sums)
        return (y_out[None], d_x[None], g1, b1, heads_first(qkv), qb, out, ob, g2, b2, up, ub, down, db)

    return jax.shard_map(device_step, mesh=mesh,
                         in_specs=(act_spec, act_spec) + (param_spec,) * 12,
                         out_specs=(act_spec, act_spec) + (param_spec,) * 12,
                         check_vma=False)
```

```python
import functools
import jax
import jax.numpy as jnp
import numpy as np
from jax import lax
from jax.experimental import pallas as pl
from jax.experimental.pallas import tpu as pltpu
from jax.sharding import PartitionSpec as P

BF16, F32 = jnp.bfloat16, jnp.float32
EPSILON = 1e-5
MESH = pl.DeviceIdType.MESH
ANY = pl.BlockSpec(memory_space=pl.ANY)
IN_VMEM = pl.BlockSpec(memory_space=pltpu.VMEM)
VMEM_LIMIT = 67 * 10**6
LAYERS, AXES, SIDE, CORES, ROWS, PARTNERS = 2, 3, 4, 2, 8, 10
CHIPS = (SIDE, SIDE, SIDE)
SHARDS = SIDE * SIDE * SIDE * CORES
SEQ, WIDTH, HIDDEN, TILE, PAIR, LN_ROWS = 384, 1024, 4096, 512, 128, 64
HEADS, HEAD, PARTS = 16, 64, 3
QKV = PARTS * WIDTH
N_TILES, N_PAIRS, N_BLOCKS = HIDDEN // TILE, WIDTH // PAIR, SEQ // PAIR
TWICE = 2 * PAIR
INV_SQRT2, INV_SQRT2PI, SCALE = 0.7071067811865476, 0.3989422804014327, 0.125
SHARES = (8, 8, 8, 8, 24, 8, 32, 8)
SIZES = tuple(SHARDS * share for share in SHARES)
OFFSETS = tuple(sum(SIZES[:k]) for k in range(len(SIZES)))
N_VEC = sum(SIZES)
GAIN1, BIAS1, GAIN2, BIAS2, QKV_BIAS, OUT_BIAS, UP_BIAS, DOWN_BIAS = range(len(SHARES))
ORDERS = ((2, 1, 0), (1, 0, 2), (0, 2, 1))
HALVES = range(2)
OWN, ONE, CROSS, TWO = range(SIDE)
ROLES = (ONE, TWO, CROSS)
A, B, C = range(AXES)
UP, DOWN, MIX = range(3)
SELF = 3


class Chip:
    def __init__(self):
        node, local = lax.axis_index('node'), lax.axis_index('local')
        self.core, self.other = lax.rem(local, CORES), 1 - lax.rem(local, CORES)
        self.where = (lax.div(node, SIDE), lax.rem(node, SIDE), lax.div(local, CORES))
        self.base = (node, local - self.core)
        self.strides = ((SIDE, 0), (1, 0), (0, CORES))
        self.near = [(v, v + 1 - 2 * parity(v), lax.rem(v + 2, SIDE), SIDE - 1 - v) for v in self.where]

        self.gaps = [near[3] - near[1] for near in self.near]

    def at(self, axis, role, half):
        near = self.near[axis]
        if role in (OWN, CROSS):
            return near[role]
        return near[role] + half * self.gaps[axis] if role == ONE else near[role] - half * self.gaps[axis]

    def device(self, axis, role, half):
        shift = self.at(axis, role, half) - self.where[axis]
        node, local = [b + shift * s if s else b for b, s in zip(self.base, self.strides[axis])]
        return (node, local + self.core)

    def partner(self):
        node, local = self.base
        return (node, local + self.other)

    def signal_partners(self, semaphore):
        for axis in range(AXES):
            for role in ROLES:
                pl.semaphore_signal(semaphore, inc=1, device_id=self.device(axis, role, A), device_id_type=MESH)
        pl.semaphore_signal(semaphore, inc=1, device_id=self.partner(), device_id_type=MESH)


def enter(chip):
    barrier = pltpu.get_barrier_semaphore()
    chip.signal_partners(barrier)
    pl.semaphore_wait(barrier, PARTNERS)


def remote(src, dst, send_sem, recv_sem, device):
    return pltpu.make_async_remote_copy(src_ref=src, dst_ref=dst, send_sem=send_sem, recv_sem=recv_sem, device_id=device,
                                        device_id_type=MESH)


def start(copies):
    for copy in copies:
        copy.start()
    return copies


def wait(copies):
    for copy in copies:
        copy.wait()


def loop(count):
    return pl.loop(0, count)


def halves(body):
    loop(len(HALVES))(body)


def parity(n):
    return lax.rem(n, 2)


def pool(sems):
    return (sems.at[n] for n in range(sems.shape[0]))


def contract(a, b, a_axis, b_axis):
    return lax.dot_general(a, b, (((a_axis,), (b_axis,)), ((), ())), preferred_element_type=F32)


def dot(a, b):
    return contract(a, b, 1, 0)


def dot_t(a, b):
    return contract(a, b, 1, 1)


def row_sum(x):
    return jnp.sum(x, axis=1, keepdims=True)


def column_sum(x):
    return jnp.sum(x, axis=0, keepdims=True)


def rounded(x):
    return x.astype(BF16).astype(F32)


def lanes(first, width=PAIR):
    return pl.ds(pl.multiple_of(first, PAIR), width)


def turn(x, cos, sin_a, sin_b):
    return x * cos + pltpu.roll(x, PAIR - ROWS, 1) * sin_a + pltpu.roll(x, ROWS, 1) * sin_b


def turn_back(d, cos, sin_a, sin_b):
    return d * cos + pltpu.roll(d * sin_a, ROWS, 1) + pltpu.roll(d * sin_b, PAIR - ROWS, 1)


def iota(shape, axis):
    return lax.broadcasted_iota(jnp.int32, shape, axis)


def block_rows(j):
    return slice(j * PAIR, (j + 1) * PAIR)


def split_heads(x):
    first = iota((PAIR, PAIR), 1) < HEAD
    rows = []
    for j in range(N_BLOCKS):
        block = x[block_rows(j)]
        rows += [jnp.where(first, block, jnp.zeros_like(block)), jnp.where(first, jnp.zeros_like(block), block)]
    return jnp.concatenate(rows, axis=0)


def total_of(chunks, join=jnp.add):
    return functools.reduce(join, chunks)


def probabilities(q_block, keys, i):
    scores = dot_t(q_block, keys)
    causal = iota((PAIR, PAIR), 0) >= iota((PAIR, PAIR), 1)
    chunks = [scores[:, block_rows(j)] * SCALE for j in range(CORES * (i + 1))]
    for head in HALVES:
        mine = slice(head, None, CORES)
        *ahead, last = chunks[mine]
        held = ahead + [jnp.where(causal, last, -1e30)]
        top = jnp.max(total_of(held, jnp.maximum), axis=1, keepdims=True)
        held = [jnp.exp(chunk - top) for chunk in held]
        inverse = 1.0 / row_sum(total_of(held))
        chunks[mine] = [chunk * inverse for chunk in held]
    return chunks


def side_by_side(chunks):
    return jnp.concatenate([chunk.astype(BF16) for chunk in chunks], axis=1)


def row_mean(x):
    return jnp.mean(x, axis=1, keepdims=True)


def normalised(h):
    center = h - row_mean(h)
    inverse = lax.rsqrt(row_mean(center * center) + EPSILON)
    return center * inverse, inverse


def half_copies(chip, src, dst, own_sem, send_sem, recv_sem):
    width = dst.shape[-1]
    mine, away = [src.at[:, lanes(which * width, width)] for which in (chip.core, chip.other)]
    place = dst.at[chip.core]
    return [pltpu.make_async_copy(mine, place, own_sem), remote(away, place, send_sem, recv_sem, chip.partner())]


class Gather:
    def __init__(self, chip, shards, fulls, sems):
        self.chip, self.shards, self.fulls = chip, shards, fulls
        self.send_sem, self.recv_sem, self.pass_send, self.pass_recv = sems

    def box(self, layer, k, half, stage, role, own=False):
        width = self.fulls[k].shape[-1] // len(HALVES)
        cols = lanes(half * width, width)
        if own:
            return self.shards[k].at[layer, :, cols]
        where = list(self.chip.where)
        for axis in ORDERS[k][:stage]:
            where[axis] = pl.ds(0, SIDE)
        axis = ORDERS[k][stage]
        where[axis] = self.chip.at(axis, role, half)
        return self.fulls[k].at[layer, where[0], where[1], where[2], self.chip.core, :, cols]

    def reach(self, layer, k, half, stage, step):
        slot, on = AXES * stage + step, stage > A and step == C
        src = self.box(layer, k, half, stage, ONE if on else OWN, stage == A)
        return remote(src, self.box(layer, k, half, stage, ONE if on else OWN), self.send_sem.at[layer, k, stage],
                      self.recv_sem.at[layer, k, half, slot], self.chip.device(ORDERS[k][stage], TWO if on else ROLES[step], half))

    def passing(self, layer, k, half, stage, step):
        role = (*ROLES, OWN)[step]
        return remote(self.box(layer, k, half, stage, role, step == SELF), self.box(layer, k, half, stage, role),
                      self.pass_send.at[layer, k], self.pass_recv.at[layer, k], self.chip.partner())

    def each(self, action):
        for k in (MIX, UP, DOWN):
            @halves
            def _(half):
                action(k, half)

    def begin(self, layer, stage):
        for step in range(C if stage else AXES):
            self.each(lambda k, half: self.reach(layer, k, half, stage, step).start())

    def own(self, layer):
        self.each(lambda k, half: self.passing(layer, k, half, A, SELF).start())

    def middle(self, layer, stage):
        def action(k, half):
            self.reach(layer, k, half, stage, A).wait_recv()
            self.reach(layer, k, half, stage, C).start()
            self.passing(layer, k, half, stage, A).start()
        self.each(action)

    def end(self, layer, stage, steps=range(AXES)):
        def action(k, half):
            for step in steps:
                self.reach(layer, k, half, stage, step).wait_recv()
                self.passing(layer, k, half, stage, step).start()
        self.each(action)

    def arrived(self, layer, k):
        box = self.fulls[k].at[layer, :, :, :, self.chip.other]
        remote(box, box, self.pass_send.at[layer, k], self.pass_recv.at[layer, k], self.chip.partner()).wait_recv()

    def left(self):
        three, full = pl.ds(0, AXES), self.fulls[UP].at[A]
        boxes = (full.at[three, A, A, A], full.at[:, three, A, A], full.at[:, :, three, A])

        @loop(LAYERS)
        def _(layer):
            @loop(AXES)
            def _(k):
                for stage, box in enumerate(boxes):
                    sem = self.send_sem.at[layer, k, stage]
                    remote(box, box, sem, sem, self.chip.partner()).wait_send()
                box, sem = full.at[:, :, :, A], self.pass_send.at[layer, k]
                remote(box, box, sem, sem, self.chip.partner()).wait_send()


def pick_lanes(sel_lane, cols):
    return (iota((PAIR, WIDTH), 0) == sel_lane[:, cols]).astype(F32).astype(BF16)


def vector_blocks():
    return [slice(k * WIDTH, (k + 1) * WIDTH) for k in range(N_VEC // WIDTH)]


def unpack_vectors(small_v, layer, sel_shard, sel_lane, vec_ref):
    tiles = small_v[...].astype(F32).reshape((SHARDS, ROWS, PAIR))
    held = jnp.sum(jnp.where(iota(tiles.shape, 1) == layer, tiles, 0.0), axis=1).astype(BF16)
    for cols in vector_blocks():
        spread = dot(held, pick_lanes(sel_lane, cols))
        spread = jnp.where(iota((SHARDS, WIDTH), 0) == sel_shard[:, cols], spread, 0.0)
        vec_ref[layer:layer + 1, cols] = column_sum(spread)


def forward_kernel(x_hbm, ycot_hbm, tables_hbm, places_hbm, up_s, down_s, mix_s, small_ref, up_f, down_f, mix_f, small_full, vec_ref,
                   dout_cols, y_hbm, h_hbm, n1_hbm, n2_hbm, ctx_hbm, act_hbm, qkv_hbm, pre_hbm, up_v, down_v, mix_v, small_v, acc, pre_v,
                   n1_v, n2_v, qkv_v, ctx_v, y_v, n1_t, n2_t, ctx_t, act_t, send_sem, recv_sem, pass_send, pass_recv,
                   small_send, small_recv, own_sems, load_sem, save_sem, share_send, share_recv, act_save, act_send, act_recv, tables,
                   places):
    shards, fulls, own_sem = (up_s, down_s, mix_s), (up_f, down_f, mix_f), pool(own_sems)
    chip = Chip()
    enter(chip)
    gather = Gather(chip, shards, fulls, (send_sem, recv_sem, pass_send, pass_recv))

    def small_copy(slot, where, device):
        place = small_full.at[(*where, chip.core)]
        return remote(place, place, small_send.at[slot], small_recv.at[slot], device)

    def small_reach(stage, step):
        where = list(chip.where)
        for axis in range(stage):
            where[axis] = pl.ds(0, SIDE)
        return small_copy(AXES * stage + step, where, chip.device(stage, ROLES[step], A))

    def small_begin(stage):
        start([small_reach(stage, step) for step in range(AXES)])

    def small_end(stage):
        for step in range(AXES):
            small_reach(stage, step).wait_recv()

    small_pass = small_copy(AXES * AXES, [pl.ds(0, SIDE)] * AXES, chip.partner())
    here = (*chip.where, chip.core)
    own = [pltpu.make_async_copy(small_ref, small_full.at[here], next(own_sem))]
    for shard, full in zip(shards, fulls):
        for layer in range(LAYERS):
            own.append(pltpu.make_async_copy(shard.at[layer], full.at[(layer, *here)], next(own_sem)))
    loads = [
        pltpu.make_async_copy(src, dst, next(own_sem)) for src, dst in ((x_hbm, y_v), (ycot_hbm, n1_v), (tables_hbm, tables), (places_hbm, places))]
    cot_copies = half_copies(chip, n1_v, dout_cols.at[LAYERS - 1], next(own_sem), next(own_sem), next(own_sem))
    with jax.named_scope('ag0'):
        gather.begin(A, A)
        start(own)
        gather.begin(B, A)
        wait(own)
        small_begin(A)
        gather.own(A)
        gather.own(B)
        start(loads)
        gather.end(A, A)
    with jax.named_scope('ag1'):
        gather.begin(A, B)
        small_end(A)
        small_begin(B)
        gather.end(B, A)
        gather.begin(B, B)
        gather.middle(A, B)
        small_end(B)
        small_begin(C)
        gather.middle(B, B)
        gather.end(A, B, (B, C))
    with jax.named_scope('ag2_start'):
        gather.begin(A, C)
        small_end(C)
        small_pass.start()
        gather.end(B, B, (B, C))
    with jax.named_scope('ag2_middle'):
        gather.middle(A, C)
        gather.begin(B, C)
    with jax.named_scope('unpack'):
        small_pass.wait_recv()
        fetch = pltpu.make_async_copy(small_full, small_v, next(own_sem))
        fetch.start()
        fetch.wait()
        wait(loads)
        start(cot_copies)
        for layer in range(LAYERS):
            unpack_vectors(small_v, layer, places[A:B], places[B:C], vec_ref)
    with jax.named_scope('ag2_late'):
        gather.end(A, C, (B,))
    with jax.named_scope('ag2_end'):
        gather.end(A, C, (C,))
        wait(cot_copies)

    def saves(layer):
        pairs = [(y_v, h_hbm.at[layer]), (qkv_v, qkv_hbm.at[layer])]
        kept = [pltpu.make_async_copy(src, dst, save_sem.at[n]) for n, (src, dst) in enumerate(pairs)]
        for n, (src, dst) in enumerate(((n1_t, n1_hbm), (n2_t, n2_hbm), (ctx_t, ctx_hbm))):
            dst = dst.at[layer, chip.core]
            kept.append((pltpu.make_async_copy(src, dst, save_sem.at[CORES + n]),
                         remote(src, dst, share_send.at[layer, n], share_recv.at[layer, n], chip.partner())))
        return kept

    def quarter(layer, t):
        rows, tiles = pl.ds(t * WIDTH, WIDTH), pl.ds(CORES * t, CORES)
        src, dst = act_t.at[rows], act_hbm.at[layer, chip.core, rows]
        return [pltpu.make_async_copy(pre_v.at[tiles], pre_hbm.at[layer, tiles], act_save.at[A, t]),
                pltpu.make_async_copy(src, dst, act_save.at[B, t]),
                remote(src, dst, act_send.at[layer, t], act_recv.at[layer, t], chip.partner())]

    def settle(layer):
        _, qkv_save, *shares = saves(layer)
        qkv_save.wait()
        for share in shares:
            wait(share)

        @loop(SIDE)
        def _(t):
            wait(quarter(layer, t))

    @loop(LAYERS)
    def _(layer):
        def vector(k, first=0, width=None):
            return vec_ref[pl.ds(layer, 1), lanes(OFFSETS[k] + first, width or SIZES[k])]

        def load(k, piece):
            if k == DOWN:
                return pltpu.make_async_copy(fulls[k].at[layer, piece], down_v.at[piece], load_sem.at[k, piece])
            cols = lanes(piece * WIDTH, WIDTH)
            return pltpu.make_async_copy(fulls[k].at[layer, :, :, :, :, :, cols], (up_v, None, mix_v)[k].at[:, :, :, :, :, cols],
                                         load_sem.at[k, piece])

        def matrix(held, piece):
            return held[:, :, :, :, :, lanes(piece * WIDTH, WIDTH)].reshape((WIDTH, WIDTH))

        def have(k):
            gather.arrived(layer, k)

        def meanwhile(action):
            @pl.when(layer == A)
            def _():
                action()

        h_save, qkv_save, n1_share, n2_share, ctx_share = saves(layer)
        with jax.named_scope('have_mix'):
            have(MIX)
            start([load(MIX, k) for k in range(SIDE)])

        h_save.start()

        @pl.when(layer == B)
        def _():
            settle(A)

        with jax.named_scope('ln'):
            @loop(SEQ // LN_ROWS)
            def _(r):
                rows = pl.ds(pl.multiple_of(r * LN_ROWS, LN_ROWS), LN_ROWS)
                scaled, _ = normalised(y_v[rows, :].astype(F32))
                n1_v[rows, :] = (scaled * vector(GAIN1) + vector(BIAS1)).astype(BF16)
                n2_v[rows, :] = (scaled * vector(GAIN2) + vector(BIAS2)).astype(BF16)

        for src, dst, share in ((n1_v, n1_t, n1_share), (n2_v, n2_t, n2_share)):
            dst[...] = src[...].T
            start(share)

        with jax.named_scope('qkv'):
            @loop(PARTS)
            def _(k):
                load(MIX, k).wait()
                x = dot(n1_v[...], matrix(mix_v, k)) + vector(QKV_BIAS, k * WIDTH, WIDTH)

                @pl.when(k < C)
                def _():
                    for c in range(N_PAIRS):
                        block = turn(x[:, block_rows(c)], *[tables[n] for n in range(PARTS)])
                        qkv_v[:, lanes(k * WIDTH + c * PAIR)] = block.astype(BF16)

                @pl.when(k == C)
                def _():
                    qkv_v[:, lanes(k * WIDTH, WIDTH)] = x.astype(BF16)

        qkv_save.start()
        with jax.named_scope('have_up'):
            have(UP)
            have(DOWN)

        start([load(UP, k) for k in range(SIDE)] + [load(DOWN, k) for k in range(SIDE)])
        with jax.named_scope('fattn'):
            def one_pair(pair):
                keys = split_heads(qkv_v[:, lanes(WIDTH + pair * PAIR)])
                values = split_heads(qkv_v[:, lanes(C * WIDTH + pair * PAIR)])
                for i in range(N_BLOCKS):
                    n = (i + 1) * CORES * PAIR
                    probs = probabilities(qkv_v[block_rows(i), lanes(pair * PAIR)], keys[:n], i)
                    ctx_v[block_rows(i), lanes(pair * PAIR)] = dot(side_by_side(probs), values[:n]).astype(BF16)

            @loop(N_PAIRS // CORES)
            def _(two):
                for k in HALVES:
                    one_pair(CORES * two + k)

                @pl.when((layer == A) & (two == A))
                def _():
                    gather.middle(B, C)

        ctx_t[...] = ctx_v[...].T
        start(ctx_share)
        with jax.named_scope('fout'):
            load(MIX, PARTS).wait()
            acc[...] = y_v[...].astype(F32) + dot(ctx_v[...], matrix(mix_v, PARTS)) + (vector(OUT_BIAS) + vector(DOWN_BIAS))

        with jax.named_scope('fmlp'):
            @loop(SIDE)
            def _(t):
                cols = lanes(t * WIDTH, WIDTH)
                load(UP, t).wait()
                pre = dot(n2_v[...], matrix(up_v, t)) + vector(UP_BIAS, t * WIDTH, WIDTH)
                for k in HALVES:
                    pre_v[CORES * t + k] = pre[:, k * TILE:(k + 1) * TILE]
                act = (0.5 * pre * (1.0 + lax.erf(pre * INV_SQRT2))).astype(BF16)
                act_t[cols, :] = act.T
                start(quarter(layer, t))
                load(DOWN, t).wait()
                acc[...] += dot(act, down_v[t].reshape((WIDTH, WIDTH)))

                @pl.when((layer == A) & (t == B))
                def _():
                    gather.end(B, C, (B,))

        h_save.wait()
        y_v[...] = acc[...].astype(BF16)
        with jax.named_scope('fend'):
            meanwhile(lambda: gather.end(B, C, (C,)))

    with jax.named_scope('ftail'):
        last = pltpu.make_async_copy(y_v, y_hbm, next(own_sem))
        last.start()
        for stage in range(AXES):
            for step in range(AXES):
                small_reach(stage, step).wait_send()
        small_pass.wait_send()
        gather.left()
        settle(LAYERS - 1)
        last.wait()


def forward(x, y_cot, shards, small_tile, tables, places):
    grid = CHIPS + (CORES,)
    full = [(LAYERS,) + grid + tensor.shape[1:] for tensor in shards]
    shapes = [(shape, BF16) for shape in full] + [(grid + small_tile.shape, BF16), ((LAYERS, N_VEC), F32), ((LAYERS, CORES, SEQ, TILE), BF16), ((SEQ, WIDTH), BF16),
                                                  ((LAYERS, SEQ, WIDTH), BF16)]
    shapes += [((LAYERS, CORES, width, SEQ), BF16) for width in (WIDTH, WIDTH, WIDTH, HIDDEN)]
    shapes += [((LAYERS, SEQ, QKV), BF16), ((LAYERS, N_TILES, SEQ, TILE), F32)]
    dma = pltpu.SemaphoreType.DMA
    slots = AXES * AXES
    scratch = [pltpu.VMEM(shape[1:], BF16) for shape in full] + [pltpu.VMEM(grid + small_tile.shape, BF16)]
    scratch += [pltpu.VMEM((SEQ, WIDTH), F32), pltpu.VMEM((N_TILES, SEQ, TILE), F32)]
    scratch += [pltpu.VMEM((SEQ, width), BF16) for width in (WIDTH, WIDTH, QKV, WIDTH, WIDTH)]
    scratch += [pltpu.VMEM((width, SEQ), BF16) for width in (WIDTH, WIDTH, WIDTH, HIDDEN)]
    scratch += [dma(shape) for shape in ((LAYERS, AXES, AXES), (LAYERS, AXES, len(HALVES), slots), (LAYERS, AXES), (LAYERS, AXES))]
    scratch += [dma(shape) for shape in ((slots + 1,), (slots + 1,), (slots + SIDE + SIDE + AXES,), (AXES, SIDE), (SIDE + 1,), (LAYERS, AXES), (LAYERS, AXES), (CORES, SIDE), (LAYERS, SIDE), (LAYERS, SIDE))]
    scratch += [pltpu.VMEM(tables.shape, F32), pltpu.VMEM(places.shape, jnp.int32)]
    out_specs = [IN_VMEM if dtype == F32 and len(shape) == LAYERS else ANY for shape, dtype in shapes]
    return pl.pallas_call(
        forward_kernel,
        out_shape=[jax.ShapeDtypeStruct(*s) for s in shapes],
        in_specs=[ANY] * SIDE + [IN_VMEM] * SIDE,
        out_specs=out_specs,
        scratch_shapes=scratch,
        compiler_params=pltpu.CompilerParams(collective_id=0, has_side_effects=True, vmem_limit_bytes=VMEM_LIMIT),
        name='forward_layers',
    )(x, y_cot, tables, places, *shards, small_tile)


WAVES = ((384, 384, 512), (384, 384, 256), (256, 256, 256))
LEADS = ((2,) + CHIPS[1:], CHIPS[1:], (2, SIDE), (SIDE,), (AXES,))
W_UP, W_DOWN, W_QKV, W_OUT = range(4)
STEPS = ((1, (2,)), (0, ()), (2, (4, 3)), (4, (5,)), (3, ()), (5, (6, 7, 8)), (8, (9,)), (9, ()))
LAST = AXES * AXES
CARRIED = ((0, 6), (1, 4), (2, 0))
US_COLUMN, US_HOP, US_ADD, US_STEP = 0.022, 2.5, 0.0013, 0.2
US_FIRST, US_OUT, US_TILE, US_GRADIENT, US_PAIR, US_NORM = 4, 1.4, 1.6, 0.0025, 3.6, 2.7


class Schedule:
    def __init__(self):
        self.now, self.free, self.lines = 0.0, {}, []

    def send(self, link, columns):
        self.free[link] = max(self.free.get(link, 0.0), self.now) + columns * US_COLUMN
        return self.free[link] + US_HOP

    def due(self, limit):
        found = []
        while self.lines:
            line = min(self.lines, key=lambda one: one[A][A]())
            ready = line[A][A]()
            if limit is not None and ready > limit:
                break
            _, run, sends, cost = line.pop(A)
            self.lines = [one for one in self.lines if one]
            self.now = max(self.now, ready) + cost
            sends()
            found.append(run)
        return found

    def run(self, limit):
        for step in self.due(limit):
            step()

    def passed(self, cost):
        self.now += cost
        self.run(self.now)

    def hooks(self, count, cost):
        planned = []
        for _ in range(count):
            self.now += cost
            planned.append(self.due(self.now))
        return planned


def at_hooks(n, planned):
    for when, steps in enumerate(planned):
        if steps:
            @pl.when(n == when)
            def _():
                for step in steps:
                    step()


def add_into(dst, src, n_axes):
    if n_axes < 2:
        dst[...] += src[...]
        return

    @loop(SIDE)
    def _(k):
        dst[k] += src[k]


def at_axis(ref, axis, value, n_axes):
    every = [pl.ds(0, SIDE)] * n_axes
    every[axis] = value
    return ref.at[tuple(every)]


class Reduce:
    def __init__(self, chip, schedule, wave, grads, came, fin, sems, spare, write, done, when=None):
        self.wave, self.chip, self.schedule, self.widths, self.grads = wave, chip, schedule, WAVES[wave], grads
        self.came, self.fin, (self.send_sem, self.recv_sem), (self.spare, self.spare_sem) = came, fin, sems, spare
        self.write, self.done, self.when, self.times = write, done, when, {}

    def box(self, a, half, stage):
        order = ORDERS[a]
        ref = self.came[a][A].at[half, A]
        spot = [axis for axis in range(AXES) if axis != order[A]].index(order[B])
        if stage == B:
            return ref, spot, C
        return at_axis(ref, spot, self.chip.where[order[B]], C), A, B

    def copy(self, a, half, slot):
        stage, turn = divmod(slot, AXES)
        sems = self.send_sem.at[a, stage], self.recv_sem.at[a, half, slot]
        if slot == LAST:
            return remote(self.total(a, half).at[self.chip.other], self.fin[a].at[half], *sems, self.chip.partner())
        axis = ORDERS[a][stage]
        if stage == C:
            role = value = ROLES[turn]
            dst = self.came[a][SIDE].at[half, turn]
        else:
            role, value = TWO if turn == C else ONE, (ONE, CROSS, TWO)[turn]
            dst = self.came[a][CORES * stage + turn // C].at[half]
            dst = dst if turn == C else dst.at[turn]
        value = self.chip.at(axis, value, half)
        if stage:
            ref, spot, n_axes = self.box(a, half, stage)
            src = at_axis(ref, spot, value, n_axes)
        else:
            src = self.came[a][A].at[half, B] if turn == C else at_axis(self.grads[a].at[half], axis, value, AXES)
        return remote(src, dst, *sems, self.chip.device(axis, role, half))

    def each(self, action):
        for a in range(AXES):
            halves(lambda half: action(a, half))

    def sending(self, slot):
        stage = slot // AXES
        share = SIDE ** (CORES * stage)
        self.times[slot] = self.schedule.now + US_HOP if slot == LAST else max(
            self.schedule.send(ORDERS[a][stage], self.widths[a] / share) for a in range(AXES))

    def begin(self):
        for slot in (B, A):
            self.each(lambda a, half: self.copy(a, half, slot).start())

    def plan(self, first=0, last=None):
        for slot in (B, A):
            self.times[slot] = self.schedule.now
            if not first:
                self.sending(slot)
        for _, sent in STEPS[:first]:
            self.times.update((slot, self.schedule.now + US_HOP) for slot in sent)
        self.schedule.lines.append([
            (lambda slot=slot: self.times[slot], lambda k=k: self.step(k), lambda sent=sent: [self.sending(n) for n in sent],
             CORES * US_ADD * sum(self.widths) if k < C else US_STEP) for k, (slot, sent) in enumerate(STEPS)][first:last])

    def step(self, k):
        def work():
            with jax.named_scope(f'w{self.wave}s{k}'):
                (self.first, self.first, self.halve, self.settle, self.settle, self.spread, self.cross, self.finish)[k](STEPS[k][A])
        if self.when is None:
            work()
        else:
            pl.when(self.when)(work)

    def held(self, a, half):
        ref = self.spare[A].at[a] if a < C else self.spare[B]
        return ref.at[half, :, :, :, :, pl.ds(0, self.widths[a])]

    def first(self, slot):
        def local(a, half):
            axis = ORDERS[a][A]
            return pltpu.make_async_copy(at_axis(self.grads[a].at[half], axis, self.chip.at(axis, TWO if slot else OWN, half), AXES),
                                         self.held(a, half), self.spare_sem.at[a, half])

        def action(a, half):
            local(a, half).wait()
            self.copy(a, half, slot).wait_recv()
            add_into(self.came[a][A].at[half, slot], self.held(a, half), C)
            if slot:
                self.copy(a, half, C).start()

        self.each(lambda a, half: local(a, half).start())
        self.each(action)

    def halve(self, slot):
        def action(a, half):
            ref, spot, n_axes = self.box(a, half, B)
            self.copy(a, half, slot).wait_recv()
            for turn, role in ((B, CROSS), (A, ONE), (C, TWO), (C, OWN)):
                value = self.chip.at(ORDERS[a][B], role, half)
                add_into(at_axis(ref, spot, value, n_axes), at_axis(self.came[a][B].at[half], spot, value, n_axes), B)
                if turn < C:
                    self.copy(a, half, AXES + turn).start()
        self.each(action)

    def settle(self, slot):
        def action(a, half):
            ref, spot, n_axes = self.box(a, half, B)
            self.copy(a, half, slot).wait_recv()
            value = self.chip.at(ORDERS[a][B], TWO if slot > AXES else OWN, half)
            add_into(at_axis(ref, spot, value, n_axes), self.came[a][C].at[half, slot - AXES], B)
            if slot > AXES:
                self.copy(a, half, AXES + C).start()
        self.each(action)

    def spread(self, slot):
        def action(a, half):
            ref, *_ = self.box(a, half, C)
            self.copy(a, half, slot).wait_recv()
            add_into(ref, self.came[a][AXES].at[half], B)
            for turn in range(AXES):
                self.copy(a, half, CORES * AXES + turn).start()
        self.each(action)

    def total(self, a, half):
        ref, *_ = self.box(a, half, C)
        return ref.at[self.chip.where[ORDERS[a][C]]]

    def cross(self, _):
        def action(a, half):
            for turn in range(AXES):
                self.copy(a, half, CORES * AXES + turn).wait_recv()
            self.total(a, half)[...] += total_of([self.came[a][SIDE][half, turn] for turn in range(AXES)])
            self.copy(a, half, LAST).start()
        self.each(action)

    def finish(self, _):
        def action(a, half):
            self.write(a, half, self.chip.core, self.total(a, half)[self.chip.core])
            self.copy(a, half, LAST).wait_recv()
            self.write(a, half, self.chip.other, self.fin[a][half])
        self.each(action)
        three = pl.ds(0, AXES)
        for a, (grad, fin) in enumerate(zip(self.grads, self.fin)):
            for stage, block in enumerate((grad.at[:, :, :, three], grad.at[:, :, three, A], grad.at[:, three, A, A], fin)):
                sem = self.send_sem.at[a, stage]
                remote(block, block, sem, sem, self.chip.partner()).wait_send()
        self.done()


class VectorSum:
    def __init__(self, chip, schedule, total, came, sems, finish, when=None):
        self.schedule, self.total, self.came, self.sems, self.finish, self.when, self.ready = schedule, total, came, sems, finish, when, 0.0
        self.devices = [[chip.device(axis, role, A) for role in ROLES] for axis in range(AXES)] + [[chip.partner()]]

    def copies(self, k):
        return [remote(self.total, self.came.at[AXES * k + n], self.sems.at[A, AXES * k + n], self.sems.at[B, AXES * k + n], device)
                for n, device in enumerate(self.devices[k])]

    def sending(self, k):
        if k < SIDE:
            self.ready = self.schedule.send(k, N_VEC / (SIDE * SIDE * ROWS))

    def step(self, k):
        def work():
            with jax.named_scope(f'vec{k}'):
                wait(self.copies(k - 1))
                for n in range(len(self.devices[k - 1])):
                    self.total[...] += self.came[AXES * (k - 1) + n]
            if k < SIDE:
                start(self.copies(k))
            else:
                self.finish()
        if self.when is None:
            work()
        else:
            pl.when(self.when)(work)

    def begin(self):
        start(self.copies(A))

    def plan(self):
        self.sending(A)
        self.schedule.lines.append([
            (lambda: self.ready, lambda k=k: self.step(k), lambda k=k: self.sending(k), US_STEP) for k in range(1, SIDE + 1)])


def backward_kernel(ycot_hbm, tables, vec_ref, places, up_hbm, down_hbm, mix_hbm, h_hbm, n1_hbm, n2_hbm, ctx_hbm,
                    act_hbm, qkv_hbm, pre_hbm, _, dx_hbm, small_ref, up_sum, down_sum, qkv_sum, out_sum, dout_cols, dpre_cols,
                    dqkv_cols, *refs):
    n_arrays, sums = AXES * len(WAVES), (up_sum, down_sum, qkv_sum, out_sum)
    grads, refs = refs[:n_arrays], refs[n_arrays:]
    (spare, spare_wide, tile_v, big_v, rhs_v, wup_v, wdown_v, pre_v, dn1, dn2, dctx, dk_acc, dv_acc, qkv_v, dpre_v, dqkv_v, dh_v, h_v,
     totals, came_vec, send_sem, recv_sem, spare_sem, tile_sem, big_sem, rhs_sem, mlp_sem, io_sem, own_sem, share_send,
     share_recv, pre_sem, vec_sem, credit, *refs) = refs
    fins, came = refs[:n_arrays], refs[n_arrays:]
    first_in = pltpu.make_async_copy(ycot_hbm, dh_v, io_sem.at[A])
    first_in.start()
    chip = Chip()
    core, other = chip.core, chip.other

    def exchange(layer, k, src, dst):
        return half_copies(chip, src, dst.at[layer], own_sem.at[k], share_send.at[k], share_recv.at[k])

    def tokens_load(layer, src, part, slot):
        return [pltpu.make_async_copy(src.at[layer, k, pl.ds(part * WIDTH, WIDTH)], big_v.at[slot, :, pl.ds(k * SEQ, SEQ)],
                                      big_sem.at[slot, k]) for k in range(CORES)]

    def weight_load(layer, k, slot):
        return pltpu.make_async_copy(mix_hbm.at[layer, :, lanes(k * WIDTH, WIDTH)], big_v.at[slot], big_sem.at[slot, CORES])

    def tile_loads(layer, t, slot):
        rows = lanes(t * TILE, TILE)
        pairs = ((down_hbm.at[layer, rows], wdown_v), (pre_hbm.at[layer, t], pre_v), (up_hbm.at[layer, :, rows], wup_v))
        return [pltpu.make_async_copy(src, dst.at[slot], mlp_sem.at[slot, n]) for n, (src, dst) in enumerate(pairs)]

    def input_loads(layer):
        return [pltpu.make_async_copy(qkv_hbm.at[layer], qkv_v, io_sem.at[B]), pltpu.make_async_copy(h_hbm.at[layer], h_v, io_sem.at[C])]

    def prefetch(layer):
        start([weight_load(layer, AXES, C)] + tokens_load(layer, ctx_hbm, A, AXES) + tokens_load(layer, act_hbm, A, A))

    def prefetch_more(layer):
        start(tokens_load(layer, act_hbm, B, B) + input_loads(layer))
        for t in HALVES:
            start(tile_loads(layer, t, t))

    prefetch(LAYERS - 1)
    with jax.named_scope('enter'):
        enter(chip)
    with jax.named_scope('first_in'):
        first_in.wait()
    dx_copy = pltpu.make_async_copy(dh_v, dx_hbm, io_sem.at[A])
    prefetch_more(LAYERS - 1)

    def vector_at(k, first=0, width=None):
        return lanes(OFFSETS[k] + first, width or SIZES[k])

    def reduction(schedule, layer, wave, when):
        def write(a, half, side, block):
            def put(arr, group, col, first, width):
                size = sums[arr].shape[-1] // CORES
                sums[arr][layer, group, :, lanes(side * size + col, width)] = block[:, first:first + width].astype(BF16)
            width, colour = WAVES[wave][a], CORES * a + half
            if wave:
                first = colour * width if wave == C or a < C else SIDE * WAVES[wave][A] + half * width
                put(W_QKV if wave == C else W_UP, A, first, A, width)
            elif a < C:
                put(W_DOWN, colour, A, A, width)
            else:
                for k in HALVES:
                    put(W_DOWN, CORES * half + k, WAVES[A][A], k * PAIR, PAIR)
                put(W_OUT, A, half * TWICE, TWICE, TWICE)

        def done():
            @pl.when(layer == LAYERS - 1)
            def _():
                chip.signal_partners(credit.at[wave])

        where = slice(AXES * wave, AXES * (wave + 1))
        count = len(LEADS)
        return Reduce(chip, schedule, wave, [grad.at[layer] for grad in grads[where]],
                      [came[count * (AXES * wave + a):count * (AXES * wave + a + 1)] for a in range(AXES)],
                      fins[where], (send_sem.at[wave], recv_sem.at[wave]), ((spare, spare_wide), spare_sem), write, done, when)

    def vector_sum(schedule, layer, when):
        def own_part():
            with jax.named_scope('own'):
                node, local = chip.base
                me = node * (SIDE * CORES) + local + core
                row = jnp.zeros((ROWS, PAIR), F32)
                for k, share in enumerate(SHARES):
                    if k == QKV_BIAS:
                        firsts = [part * WIDTH + lax.div(me, CORES * ROWS) * PAIR for part in range(PARTS)]
                    else:
                        firsts = [lax.div(me * share, PAIR) * PAIR]
                    for first in firsts:
                        cols = lanes(OFFSETS[k] + first)
                        left = jnp.zeros((ROWS, PAIR), F32) + totals[layer, :, cols] * (places[A:B, cols] == me).astype(F32)
                        pick = (iota((PAIR, PAIR), 0) == places[B:C, cols]).astype(F32).astype(BF16)
                        for _ in range(PARTS):
                            row = row + dot_t(left.astype(BF16), pick)
                            left = left - rounded(left)
                small_ref[layer] = row.astype(BF16)

            @pl.when(layer == LAYERS - 1)
            def _():
                chip.signal_partners(credit.at[AXES])

        return VectorSum(chip, schedule, totals.at[layer], came_vec, vec_sem, own_part, when)

    def run_on(schedule, layer, when):
        for wave, step in CARRIED:
            reduction(schedule, layer, wave, when).plan(step)
        vector_sum(schedule, layer, when).plan()

    @loop(LAYERS + 1)
    def _(turn_no):
        layer = LAYERS - 1 - turn_no
        working = pl.when(turn_no < LAYERS)
        total = totals.at[layer]
        schedule = Schedule()

        run_on(schedule, layer + 1, turn_no > A)

        def rhs_load(src, first, width, k):
            cols = lanes(first, width)
            return [pltpu.make_async_copy(src.at[layer, n, :, cols], rhs_v.at[pl.ds(n * SEQ, SEQ), cols], rhs_sem.at[k, n])
                    for n in range(CORES)]

        def product(lhs_slot, first, width, out_slot):
            value = dot(big_v[lhs_slot, :, 0:CORES * SEQ], rhs_v[:, lanes(first, width)])
            tile_v[out_slot, :, :, :, :, :, 0:width] = value.reshape(CHIPS + (CORES, ROWS, width))

        def tile_out(slot, src, dst):
            return pltpu.make_async_copy(src, dst, tile_sem.at[slot])

        def tile_done(slot, width):
            block = tile_v.at[slot, :, :, :, :, :, pl.ds(0, width)]
            tile_out(slot, block, block).wait()

        def columns(wave, a, half, first, width):
            return grads[AXES * wave + a].at[layer, half, :, :, :, :, :, pl.ds(first, width)]

        def launch(wave):
            @pl.when(turn_no == B)
            def _():
                pl.semaphore_wait(credit.at[wave], PARTNERS)

            current = reduction(schedule, layer, wave, turn_no < LAYERS)
            if wave == C:
                @pl.when(turn_no == B)
                def _():
                    pl.semaphore_wait(credit.at[AXES], PARTNERS)

                @working
                def _():
                    vector_sum(schedule, layer, None).begin()

            working(current.begin)
            if wave < C:
                current.plan(last=dict(CARRIED)[wave])

        @working
        def _():
            with jax.named_scope('dw_out'):
                d_sum = column_sum(dh_v[...].astype(F32))
                total[:, vector_at(OUT_BIAS)] = d_sum
                total[:, vector_at(DOWN_BIAS)] = d_sum
                weight_load(layer, AXES, C).wait()
                dctx[...] = dot_t(dh_v[...], big_v[C]).astype(BF16)
                start(tokens_load(layer, act_hbm, C, C))

                @pl.when(turn_no == B)
                def _():
                    wait(exchange(layer, A, dh_v, dout_cols))

                wait(start(rhs_load(dout_cols, A, TILE, A)))
                wait(tokens_load(layer, ctx_hbm, A, AXES))
                product(AXES, A, TILE, B)
                start(tokens_load(layer, act_hbm, AXES, AXES))
                for k in HALVES:
                    tile_out(B, tile_v.at[B, :, :, :, :, :, pl.ds(k * TWICE, TWICE)], columns(A, C, k, TWICE, TWICE)).start()

        schedule.passed(US_FIRST)
        out_hooks = schedule.hooks(SIDE, US_OUT)

        @loop(SIDE)
        def _(z):
            @working
            def _():
                slot = parity(z)
                wait(tokens_load(layer, act_hbm, z, z))

                @pl.when(z > A)
                def _():
                    tile_done(slot, TILE)

                product(z, A, TILE, slot)
                split = WAVES[A][A]
                for k in range(SIDE):
                    a, half = divmod(k, CORES)
                    for c in range(CORES):
                        block = tile_v.at[slot, :, :, CORES * c + a, half]
                        tile_out(slot, block.at[:, :, :, pl.ds(0, split)], grads[a].at[layer, half, z, :, :, c]).start()
                        tile_out(slot, block.at[:, :, :, pl.ds(split, PAIR)],
                                 grads[C].at[layer, a, z, :, :, c, :, pl.ds(half * PAIR, PAIR)]).start()

            at_hooks(z, out_hooks)

        @working
        def _():
            start(tokens_load(layer, n2_hbm, A, A) + [weight_load(layer, k, k + 1) for k in range(PARTS)])
            for slot in HALVES:
                tile_done(slot, TILE)

        schedule.passed(US_STEP)
        launch(A)

        @working
        def _():
            dn2[...] = jnp.zeros_like(dn2)

        def pre_copy(t, slot, away):
            place = dpre_cols.at[layer, core, :, lanes(lax.rem(t, SIDE) * TILE, TILE)]
            if away:
                return remote(dpre_v.at[slot], place, pre_sem.at[A, t], pre_sem.at[B, t], chip.partner())
            return pltpu.make_async_copy(dpre_v.at[slot], place, own_sem.at[CORES + slot])

        def pre_act(t, leave):
            for away, whose in ((False, core), (True, other)):
                @pl.when(lax.div(t, SIDE) == whose)
                def _():
                    copy = pre_copy(t, parity(t), away)
                    if leave:
                        copy.start()
                    elif away:
                        copy.wait_send()
                    else:
                        copy.wait()

        tile_hooks = schedule.hooks(N_TILES, US_TILE)

        with jax.named_scope('mlp'):
            @loop(N_TILES)
            def _(t):
                @working
                def _():
                    slot = parity(t)
                    wait(tile_loads(layer, t, slot))
                    d_act = rounded(dot_t(dh_v[...], wdown_v[slot]))
                    pre = pre_v[slot]
                    slope = 0.5 * (1.0 + lax.erf(pre * INV_SQRT2)) + pre * (INV_SQRT2PI * jnp.exp(-0.5 * pre * pre))
                    d_pre = d_act * slope
                    total[:, vector_at(UP_BIAS, t * TILE, TILE)] = column_sum(d_pre)

                    @pl.when(t > B)
                    def _():
                        pre_act(t - CORES, False)

                    dpre_v[slot] = d_pre.astype(BF16)
                    pre_act(t, True)
                    dn2[...] += dot_t(dpre_v[slot], wup_v[slot])

                    @pl.when(t + CORES < N_TILES)
                    def _():
                        start(tile_loads(layer, t + CORES, slot))

                at_hooks(t, tile_hooks)

        @working
        def _():
            for t in HALVES:
                pre_act(N_TILES - CORES + t, False)
            for t in range(SIDE):
                pre_copy(SIDE * core + t, A, True).wait_recv()

        def gradient_loads(wave, source):
            first = 0
            for a in range(AXES):
                width = CORES * WAVES[wave][a]
                start(rhs_load(source, first, width, a))
                first += width

        def gradient_wave(wave, source, first, orders):
            split, count = WAVES[wave][orders[A]], len(orders)
            width = CORES * split
            planned = schedule.hooks(count, width * US_GRADIENT)

            @loop(count)
            def _(n):
                @working
                def _():
                    slot = parity(n)
                    wait(rhs_load(source, first + n * width, width, orders[A] + n))

                    @pl.when(n > B)
                    def _():
                        tile_done(slot, width)

                    product(A, first + n * width, width, slot)
                    for k, a in enumerate(orders):
                        @pl.when(n == k)
                        def _():
                            for half in HALVES:
                                block = tile_v.at[slot, :, :, :, :, :, pl.ds(half * split, split)]
                                tile_out(slot, block, columns(wave, a, half, 0, split)).start()

                at_hooks(n, planned)

            @working
            def _():
                for slot in range(min(count, CORES)):
                    tile_done(slot, width)

        @working
        def _():
            gradient_loads(B, dpre_cols)
            wait(tokens_load(layer, n2_hbm, A, A))

        with jax.named_scope('dw1'):
            gradient_wave(B, dpre_cols, A, (A, B))
            gradient_wave(B, dpre_cols, SIDE * WAVES[B][A], (C,))
        launch(B)
        @working
        def _():
            start(tokens_load(layer, n1_hbm, A, A))
            wait(input_loads(layer))

        pair_hooks = schedule.hooks(N_PAIRS // CORES, US_PAIR)

        with jax.named_scope('attn'):
            def one_pair(pair, dk_sum, dv_sum):
                at = lanes(pair * PAIR)
                keys = split_heads(qkv_v[:, lanes(WIDTH + pair * PAIR)])
                values = split_heads(qkv_v[:, lanes(C * WIDTH + pair * PAIR)])
                q_t = qkv_v[:, at].T
                dc_t = dctx[:, at].T
                bias_sums = [jnp.zeros((1, PAIR), F32)] * PARTS

                def turned_back(n, d, rows, to):
                    d = turn_back(rounded(d), *[tables[k, rows, :] for k in range(PARTS)])
                    bias_sums[n] = bias_sums[n] + column_sum(d)
                    dqkv_v[rows, to] = d.astype(BF16)

                for i in range(N_BLOCKS):
                    old, n = i * TWICE, (i + 1) * TWICE
                    rows = block_rows(i)
                    probs = probabilities(qkv_v[rows, at], keys[:n], i)
                    d_all = rounded(dot_t(dctx[rows, at], values[:n]))
                    d_scores = [d_all[:, block_rows(j)] for j in range(CORES * (i + 1))]
                    for head in HALVES:
                        mine = slice(head, None, CORES)
                        mean = row_sum(total_of([p * d for p, d in zip(probs[mine], d_scores[mine])]))
                        d_scores[mine] = [p * (d - mean) * SCALE for p, d in zip(probs[mine], d_scores[mine])]
                    d_scores, probs = side_by_side(d_scores), side_by_side(probs)
                    turned_back(A, dot(d_scores, keys[:n]), rows, at)
                    for acc, left, right in ((dk_sum, q_t, d_scores), (dv_sum, dc_t, probs)):
                        part = dot(left[:, rows], right)
                        if i:
                            acc[:, :old] += part[:, :old]
                        acc[:, old:n] = part[:, old:]
                first = iota((PAIR, PAIR), 0) < HEAD
                for j in range(N_BLOCKS):
                    rows = block_rows(j)
                    d_key, d_value = [jnp.where(first, acc[:, block_rows(CORES * j)], acc[:, block_rows(CORES * j + 1)]).T
                                      for acc in (dk_sum, dv_sum)]
                    turned_back(B, d_key, rows, lanes(WIDTH + pair * PAIR))
                    d_value = d_value.astype(BF16)
                    bias_sums[C] = bias_sums[C] + column_sum(d_value.astype(F32))
                    dqkv_v[rows, lanes(C * WIDTH + pair * PAIR)] = d_value
                for k, bias_sum in enumerate(bias_sums):
                    total[:, vector_at(QKV_BIAS, k * WIDTH + pair * PAIR, PAIR)] = bias_sum

            @loop(N_PAIRS // CORES)
            def _(two):
                @working
                def _():
                    for k in HALVES:
                        one_pair(CORES * two + k, dk_acc.at[k], dv_acc.at[k])

                at_hooks(two, pair_hooks)

        @working
        def _():
            start(exchange(layer, B, dqkv_v, dqkv_cols))
            dn1[...] = jnp.zeros_like(dn1)

            with jax.named_scope('dn1'):
                @loop(PARTS)
                def _(k):
                    weight_load(layer, k, k + 1).wait()
                    dn1[...] += dot_t(dqkv_v[:, lanes(k * WIDTH, WIDTH)], big_v[k + 1])

        schedule.passed(US_NORM)

        @working
        def _():
            for k in (GAIN1, BIAS1, GAIN2, BIAS2):
                total[:, vector_at(k)] = jnp.zeros((1, WIDTH), F32)

            with jax.named_scope('lnb'):
                @loop(SEQ // LN_ROWS)
                def _(r):
                    rows = pl.ds(pl.multiple_of(r * LN_ROWS, LN_ROWS), LN_ROWS)
                    scaled, inverse = normalised(h_v[rows, :].astype(F32))
                    d1, d2 = rounded(dn1[rows, :]), rounded(dn2[rows, :])
                    for k, value in ((GAIN1, d1 * scaled), (BIAS1, d1), (GAIN2, d2 * scaled), (BIAS2, d2)):
                        total[:, vector_at(k)] += column_sum(value)
                    g1, g2 = [vec_ref[pl.ds(layer, 1), lanes(OFFSETS[k], WIDTH)] for k in (GAIN1, GAIN2)]
                    d_scaled = d1 * g1 + d2 * g2
                    d_h = inverse * (d_scaled - row_mean(d_scaled) - scaled * row_mean(d_scaled * scaled))
                    dh_v[rows, :] = (dh_v[rows, :].astype(F32) + d_h).astype(BF16)

        schedule.passed(US_NORM)
        @working
        def _():
            wait(exchange(layer, B, dqkv_v, dqkv_cols))
            gradient_loads(C, dqkv_cols)
            wait(tokens_load(layer, n1_hbm, A, A))

        @pl.when(turn_no == A)
        def _():
            start(exchange(layer - 1, A, dh_v, dout_cols))

        @pl.when(turn_no == B)
        def _():
            dx_copy.start()

        with jax.named_scope('dw2'):
            gradient_wave(C, dqkv_cols, A, (A, B, C))

        @pl.when(turn_no == A)
        def _():
            prefetch(layer - 1)
            prefetch_more(layer - 1)

        schedule.run(None)
        launch(C)

    dx_copy.wait()


def backward(y_cot, tables, vectors, places, weights, saved):
    dma, one = pltpu.SemaphoreType.DMA, (1,)
    pair, wide, row = (len(HALVES),), (SEQ, WIDTH), one + (N_VEC,)
    shapes = [(wide, BF16), ((LAYERS, ROWS, PAIR), BF16)]
    shapes += [((LAYERS, groups, ROWS, width), BF16) for groups, width in ((*one, HIDDEN), (SIDE, WIDTH), (*one, QKV), (*one, WIDTH))]
    in_vmem = len(shapes)
    shapes += [((LAYERS, CORES, SEQ, width), BF16) for width in (TILE, SIDE * TILE, PARTS * TILE)]
    blocks = [(CORES, ROWS, width) for wave in WAVES for width in wave]
    shapes += [((LAYERS,) + pair + CHIPS + block, F32) for block in blocks]
    tile = (CORES, ROWS)
    scratch = [(pair + pair + CHIPS[1:] + tile + (WAVES[0][0],), F32), (pair + CHIPS[1:] + tile + (TILE,), F32), (pair + CHIPS + tile + (CORES * WAVES[0][0],), F32), ((SIDE, WIDTH, WIDTH), BF16), ((CORES * SEQ, SIDE * TILE), BF16)]
    scratch += [(pair + shape, BF16) for shape in ((WIDTH, TILE), (TILE, WIDTH))]
    scratch += [(pair + (SEQ, TILE), F32), (wide, F32), (wide, F32), (wide, BF16)] + [(pair + (PAIR, CORES * SEQ), F32)] * CORES
    scratch += [((SEQ, QKV), BF16), (pair + (SEQ, TILE), BF16), ((SEQ, QKV), BF16), (wide, BF16), (wide, BF16), ((LAYERS,) + row, F32),
                ((PARTNERS,) + row, F32)]
    slots = (len(WAVES), AXES) + pair + (LAST + 1,)
    sems = [dma(shape) for shape in ((len(WAVES), AXES, SIDE), slots, (AXES,) + pair, pair, (SIDE, AXES), (AXES, CORES), pair + (PARTS,), (AXES,),
                                     (SIDE,), pair, pair, pair + (N_TILES,), pair + (PARTNERS,))]
    late = [(pair + block[1:], F32) for block in blocks] + [(pair + lead + block, F32) for block in blocks for lead in LEADS]
    outs = pl.pallas_call(
        backward_kernel,
        out_shape=[jax.ShapeDtypeStruct(*s) for s in shapes],
        in_specs=[ANY] + [IN_VMEM] * AXES + [ANY] * (PARTNERS + 1),
        input_output_aliases={SIDE + PARTNERS: in_vmem},
        out_specs=[ANY] + [IN_VMEM] * (in_vmem - 1) + [ANY] * (len(shapes) - in_vmem),
        scratch_shapes=[pltpu.VMEM(*s) for s in scratch] + sems + [pltpu.SemaphoreType.REGULAR((SIDE,))]
        + [pltpu.VMEM(*s) for s in late],
        compiler_params=pltpu.CompilerParams(collective_id=1, has_side_effects=True, vmem_limit_bytes=VMEM_LIMIT),
        name='backward_layers',
    )(y_cot, tables, vectors, places, *weights, *saved)
    d_x, small, *sums = outs[:in_vmem]
    return d_x, small[:, 0], [s.reshape((LAYERS, -1, s.shape[-1])) for s in sums]


def finish_kernel(*refs):
    n_large = CORES + AXES
    large, small_ref, refs = refs[:n_large], refs[n_large], refs[n_large + 1:]
    outs, small_outs, refs = refs[:n_large], refs[n_large:n_large + len(SHARES)], refs[n_large + len(SHARES):]
    held, sems = refs[:n_large], refs[n_large]
    loads = start([pltpu.make_async_copy(src, dst, sems.at[n]) for n, (src, dst) in enumerate(zip(large, held))])
    first = 0
    for share, out in zip(SHARES, small_outs):
        out[...] = small_ref[:, first:first + share]
        first += share
    stores = []
    for load, src, dst in zip(loads, held, outs):
        load.wait()
        stores += start([pltpu.make_async_copy(src, dst, sems.at[n_large + len(stores)])])
    wait(stores)


def finish(large, small):
    shapes = [jax.ShapeDtypeStruct(t.shape, BF16) for t in large] + [jax.ShapeDtypeStruct((LAYERS, share), BF16) for share in SHARES]
    outs = pl.pallas_call(
        finish_kernel,
        out_shape=shapes,
        in_specs=[ANY] * len(large) + [IN_VMEM],
        out_specs=[ANY] * len(large) + [IN_VMEM] * len(SHARES),
        scratch_shapes=[pltpu.VMEM(t.shape, BF16) for t in large] + [pltpu.SemaphoreType.DMA((CORES * len(large),))],
        name='finish',
    )(*large, small)
    return outs[:len(large)], outs[len(large):]


def rope_tables():
    rot_dim, f32 = HEAD // SIDE, np.float32
    inv_freq = f32(1.0) / f32(10000.0) ** (np.arange(0, rot_dim, 2, dtype=f32) / f32(rot_dim))
    angles = np.arange(SEQ, dtype=f32)[:, None] * inv_freq[None, :]
    cos, sin = np.cos(angles), np.sin(angles)
    zero = np.zeros_like(sin)
    rest = np.zeros((SEQ, HEAD - rot_dim), f32)
    tables = ([cos, cos, rest + f32(1.0)], [-sin, zero, rest], [zero, sin, rest])
    return jnp.asarray(np.stack([np.tile(np.concatenate(table, axis=1), (1, 2)) for table in tables]).astype(f32))


def heads_last(tensor):
    lead = tensor.shape[:-2]
    return tensor.reshape(lead + (HEADS, PARTS, HEAD)).swapaxes(-3, -2).reshape(lead + (QKV,))


def heads_first(tensor):
    lead = tensor.shape[:-1]
    return tensor.reshape(lead + (PARTS, HEADS, HEAD)).swapaxes(-3, -2).reshape(lead + (HEADS, PARTS * HEAD))


def vector_places():
    shard, lane, first = [], [], 0
    for k, (share, size) in enumerate(zip(SHARES, SIZES)):
        place = np.arange(size)
        if k == QKV_BIAS:
            place = heads_last(place.reshape(HEADS, -1))
        shard.append(place // share)
        lane.append(first + place % share)
        first += share
    return jnp.asarray(np.stack([np.concatenate(shard), np.concatenate(lane)]).astype(np.int32))


def solution(mesh):
    shard_axes = ('node', 'local')
    act_spec = P(shard_axes)
    param_spec = P(None, shard_axes)

    def device_step(x, y_cot, ln1_gain, ln1_bias, qkv_weight, qkv_bias, out_weight, out_bias,
                    ln2_gain, ln2_bias, up_weight, up_bias, down_weight, down_bias):
        tables, places = rope_tables(), vector_places()
        small = (ln1_gain, ln1_bias, ln2_gain, ln2_bias, qkv_bias, out_bias, up_bias, down_bias)
        small_tile = jnp.pad(jnp.concatenate(small, axis=1), ((0, ROWS - LAYERS), (0, PAIR - sum(SHARES))))
        mix = jnp.concatenate([heads_last(qkv_weight), out_weight], axis=-1)
        *weights, _, vectors, dout_cols, y_out, hidden, n1, n2, ctx, act, qkv, pre = forward(
            x[0], y_cot[0], (up_weight, down_weight, mix), small_tile, tables, places)
        weights = [tensor.reshape((LAYERS, -1, tensor.shape[-1])) for tensor in weights]
        d_x, small_sums, (up, down, qkv, out) = backward(
            y_cot[0], tables, vectors, places, weights, (hidden, n1, n2, ctx, act, qkv, pre, dout_cols))
        (y_out, d_x, up, down, out), (g1, b1, g2, b2, qb, ob, ub, db) = finish((y_out, d_x, up, down, out), small_sums)
        return (y_out[None], d_x[None], g1, b1, heads_first(qkv), qb, out, ob, g2, b2, up, ub, down, db)

    return jax.shard_map(device_step, mesh=mesh,
                         in_specs=(act_spec, act_spec) + (param_spec,) * 12,
                         out_specs=(act_spec, act_spec) + (param_spec,) * 12,
                         check_vma=False)
```

```python
import functools
import jax
import jax.numpy as jnp
import numpy as np
from jax import lax
from jax.experimental import pallas as pl
from jax.experimental.pallas import tpu as pltpu
from jax.sharding import PartitionSpec as P

BF16, F32 = jnp.bfloat16, jnp.float32
EPSILON = 1e-5
MESH = pl.DeviceIdType.MESH
ANY = pl.BlockSpec(memory_space=pl.ANY)
IN_VMEM = pl.BlockSpec(memory_space=pltpu.VMEM)
VMEM_LIMIT = 67 * 10**6
LAYERS, AXES, SIDE, CORES, ROWS, PARTNERS = 2, 3, 4, 2, 8, 10
CHIPS = (SIDE, SIDE, SIDE)
SHARDS = SIDE * SIDE * SIDE * CORES
SEQ, WIDTH, HIDDEN, TILE, PAIR, LN_ROWS = 384, 1024, 4096, 512, 128, 64
HEADS, HEAD, PARTS = 16, 64, 3
QKV = PARTS * WIDTH
N_TILES, N_PAIRS, N_BLOCKS = HIDDEN // TILE, WIDTH // PAIR, SEQ // PAIR
TWICE = 2 * PAIR
INV_SQRT2, INV_SQRT2PI, SCALE = 0.7071067811865476, 0.3989422804014327, 0.125
SHARES = (8, 8, 8, 8, 24, 8, 32, 8)
SIZES = tuple(SHARDS * share for share in SHARES)
OFFSETS = tuple(sum(SIZES[:k]) for k in range(len(SIZES)))
N_VEC = sum(SIZES)
GAIN1, BIAS1, GAIN2, BIAS2, QKV_BIAS, OUT_BIAS, UP_BIAS, DOWN_BIAS = range(len(SHARES))
ORDERS = ((2, 1, 0), (1, 0, 2), (0, 2, 1))
HALVES = range(2)
OWN, ONE, CROSS, TWO = range(SIDE)
ROLES = (ONE, TWO, CROSS)
A, B, C = range(AXES)
UP, DOWN, MIX = range(3)
SELF = 3


class Chip:
    def __init__(self):
        node, local = lax.axis_index('node'), lax.axis_index('local')
        self.core, self.other = lax.rem(local, CORES), 1 - lax.rem(local, CORES)
        self.where = (lax.div(node, SIDE), lax.rem(node, SIDE), lax.div(local, CORES))
        self.base = (node, local - self.core)
        self.strides = ((SIDE, 0), (1, 0), (0, CORES))
        self.near = [(v, v + 1 - 2 * parity(v), lax.rem(v + 2, SIDE), SIDE - 1 - v) for v in self.where]

        self.gaps = [near[3] - near[1] for near in self.near]

    def at(self, axis, role, half):
        near = self.near[axis]
        if role in (OWN, CROSS):
            return near[role]
        return near[role] + half * self.gaps[axis] if role == ONE else near[role] - half * self.gaps[axis]

    def device(self, axis, role, half):
        shift = self.at(axis, role, half) - self.where[axis]
        node, local = [b + shift * s if s else b for b, s in zip(self.base, self.strides[axis])]
        return (node, local + self.core)

    def partner(self):
        node, local = self.base
        return (node, local + self.other)

    def signal_partners(self, semaphore):
        for axis in range(AXES):
            for role in ROLES:
                pl.semaphore_signal(semaphore, inc=1, device_id=self.device(axis, role, A), device_id_type=MESH)
        pl.semaphore_signal(semaphore, inc=1, device_id=self.partner(), device_id_type=MESH)


def enter(chip):
    barrier = pltpu.get_barrier_semaphore()
    chip.signal_partners(barrier)
    pl.semaphore_wait(barrier, PARTNERS)


def remote(src, dst, send_sem, recv_sem, device):
    return pltpu.make_async_remote_copy(src_ref=src, dst_ref=dst, send_sem=send_sem, recv_sem=recv_sem, device_id=device,
                                        device_id_type=MESH)


def start(copies):
    for copy in copies:
        copy.start()
    return copies


def wait(copies):
    for copy in copies:
        copy.wait()


def loop(count):
    return pl.loop(0, count)


def halves(body):
    loop(len(HALVES))(body)


def parity(n):
    return lax.rem(n, 2)


def pool(sems):
    return (sems.at[n] for n in range(sems.shape[0]))


def contract(a, b, a_axis, b_axis):
    return lax.dot_general(a, b, (((a_axis,), (b_axis,)), ((), ())), preferred_element_type=F32)


def dot(a, b):
    return contract(a, b, 1, 0)


def dot_t(a, b):
    return contract(a, b, 1, 1)


def row_sum(x):
    return jnp.sum(x, axis=1, keepdims=True)


def column_sum(x):
    return jnp.sum(x, axis=0, keepdims=True)


def rounded(x):
    return x.astype(BF16).astype(F32)


def lanes(first, width=PAIR):
    return pl.ds(pl.multiple_of(first, PAIR), width)


def turn(x, cos, sin_a, sin_b):
    return x * cos + pltpu.roll(x, PAIR - ROWS, 1) * sin_a + pltpu.roll(x, ROWS, 1) * sin_b


def turn_back(d, cos, sin_a, sin_b):
    return d * cos + pltpu.roll(d * sin_a, ROWS, 1) + pltpu.roll(d * sin_b, PAIR - ROWS, 1)


def iota(shape, axis):
    return lax.broadcasted_iota(jnp.int32, shape, axis)


def block_rows(j):
    return slice(j * PAIR, (j + 1) * PAIR)


def split_heads(x):
    first = iota((PAIR, PAIR), 1) < HEAD
    rows = []
    for j in range(N_BLOCKS):
        block = x[block_rows(j)]
        rows += [jnp.where(first, block, jnp.zeros_like(block)), jnp.where(first, jnp.zeros_like(block), block)]
    return jnp.concatenate(rows, axis=0)


def total_of(chunks, join=jnp.add):
    return functools.reduce(join, chunks)


def probabilities(q_block, keys, i):
    scores = dot_t(q_block, keys)
    causal = iota((PAIR, PAIR), 0) >= iota((PAIR, PAIR), 1)
    chunks = [scores[:, block_rows(j)] * SCALE for j in range(CORES * (i + 1))]
    for head in HALVES:
        mine = slice(head, None, CORES)
        *ahead, last = chunks[mine]
        held = ahead + [jnp.where(causal, last, -1e30)]
        top = jnp.max(total_of(held, jnp.maximum), axis=1, keepdims=True)
        held = [jnp.exp(chunk - top) for chunk in held]
        inverse = 1.0 / row_sum(total_of(held))
        chunks[mine] = [chunk * inverse for chunk in held]
    return chunks


def side_by_side(chunks):
    return jnp.concatenate([chunk.astype(BF16) for chunk in chunks], axis=1)


def row_mean(x):
    return jnp.mean(x, axis=1, keepdims=True)


def normalised(h):
    center = h - row_mean(h)
    inverse = lax.rsqrt(row_mean(center * center) + EPSILON)
    return center * inverse, inverse


def half_copies(chip, src, dst, own_sem, send_sem, recv_sem):
    width = dst.shape[-1]
    mine, away = [src.at[:, lanes(which * width, width)] for which in (chip.core, chip.other)]
    place = dst.at[chip.core]
    return [pltpu.make_async_copy(mine, place, own_sem), remote(away, place, send_sem, recv_sem, chip.partner())]


class Gather:
    def __init__(self, chip, shards, fulls, sems):
        self.chip, self.shards, self.fulls = chip, shards, fulls
        self.send_sem, self.recv_sem, self.pass_send, self.pass_recv = sems

    def box(self, layer, k, half, stage, role, own=False):
        width = self.fulls[k].shape[-1] // len(HALVES)
        cols = lanes(half * width, width)
        if own:
            return self.shards[k].at[layer, :, cols]
        where = list(self.chip.where)
        for axis in ORDERS[k][:stage]:
            where[axis] = pl.ds(0, SIDE)
        axis = ORDERS[k][stage]
        where[axis] = self.chip.at(axis, role, half)
        return self.fulls[k].at[layer, where[0], where[1], where[2], self.chip.core, :, cols]

    def reach(self, layer, k, half, stage, step):
        slot, on = AXES * stage + step, stage > A and step == C
        src = self.box(layer, k, half, stage, ONE if on else OWN, stage == A)
        return remote(src, self.box(layer, k, half, stage, ONE if on else OWN), self.send_sem.at[layer, k, stage],
                      self.recv_sem.at[layer, k, half, slot], self.chip.device(ORDERS[k][stage], TWO if on else ROLES[step], half))

    def passing(self, layer, k, half, stage, step):
        role = (*ROLES, OWN)[step]
        return remote(self.box(layer, k, half, stage, role, step == SELF), self.box(layer, k, half, stage, role),
                      self.pass_send.at[layer, k], self.pass_recv.at[layer, k], self.chip.partner())

    def each(self, action):
        for k in (MIX, UP, DOWN):
            @halves
            def _(half):
                action(k, half)

    def begin(self, layer, stage):
        for step in range(C if stage else AXES):
            self.each(lambda k, half: self.reach(layer, k, half, stage, step).start())

    def own(self, layer):
        self.each(lambda k, half: self.passing(layer, k, half, A, SELF).start())

    def middle(self, layer, stage):
        def action(k, half):
            self.reach(layer, k, half, stage, A).wait_recv()
            self.reach(layer, k, half, stage, C).start()
            self.passing(layer, k, half, stage, A).start()
        self.each(action)

    def end(self, layer, stage, steps=range(AXES)):
        def action(k, half):
            for step in steps:
                self.reach(layer, k, half, stage, step).wait_recv()
                self.passing(layer, k, half, stage, step).start()
        self.each(action)

    def arrived(self, layer, k):
        box = self.fulls[k].at[layer, :, :, :, self.chip.other]
        remote(box, box, self.pass_send.at[layer, k], self.pass_recv.at[layer, k], self.chip.partner()).wait_recv()

    def left(self):
        three, full = pl.ds(0, AXES), self.fulls[UP].at[A]
        boxes = (full.at[three, A, A, A], full.at[:, three, A, A], full.at[:, :, three, A])

        @loop(LAYERS)
        def _(layer):
            @loop(AXES)
            def _(k):
                for stage, box in enumerate(boxes):
                    sem = self.send_sem.at[layer, k, stage]
                    remote(box, box, sem, sem, self.chip.partner()).wait_send()
                box, sem = full.at[:, :, :, A], self.pass_send.at[layer, k]
                remote(box, box, sem, sem, self.chip.partner()).wait_send()


def pick_lanes(sel_lane, cols):
    return (iota((PAIR, WIDTH), 0) == sel_lane[:, cols]).astype(F32).astype(BF16)


def vector_blocks():
    return [slice(k * WIDTH, (k + 1) * WIDTH) for k in range(N_VEC // WIDTH)]


def unpack_vectors(small_v, layer, sel_shard, sel_lane, vec_ref):
    tiles = small_v[...].astype(F32).reshape((SHARDS, ROWS, PAIR))
    held = jnp.sum(jnp.where(iota(tiles.shape, 1) == layer, tiles, 0.0), axis=1).astype(BF16)
    for cols in vector_blocks():
        spread = dot(held, pick_lanes(sel_lane, cols))
        spread = jnp.where(iota((SHARDS, WIDTH), 0) == sel_shard[:, cols], spread, 0.0)
        vec_ref[layer:layer + 1, cols] = column_sum(spread)


def forward_kernel(x_hbm, ycot_hbm, tables_hbm, places_hbm, up_s, down_s, mix_s, small_ref, up_f, down_f, mix_f, small_full, vec_ref,
                   dout_cols, y_hbm, h_hbm, n1_hbm, n2_hbm, ctx_hbm, act_hbm, qkv_hbm, pre_hbm, up_v, down_v, mix_v, small_v, acc, pre_v,
                   n1_v, n2_v, qkv_v, ctx_v, y_v, n1_t, n2_t, ctx_t, act_t, send_sem, recv_sem, pass_send, pass_recv,
                   small_send, small_recv, own_sems, load_sem, save_sem, share_send, share_recv, act_save, act_send, act_recv, tables,
                   places):
    shards, fulls, own_sem = (up_s, down_s, mix_s), (up_f, down_f, mix_f), pool(own_sems)
    chip = Chip()
    with jax.named_scope('enter'):
        enter(chip)
    gather = Gather(chip, shards, fulls, (send_sem, recv_sem, pass_send, pass_recv))

    def small_copy(slot, where, device):
        place = small_full.at[(*where, chip.core)]
        return remote(place, place, small_send.at[slot], small_recv.at[slot], device)

    def small_reach(stage, step):
        where = list(chip.where)
        for axis in range(stage):
            where[axis] = pl.ds(0, SIDE)
        return small_copy(AXES * stage + step, where, chip.device(stage, ROLES[step], A))

    def small_begin(stage):
        start([small_reach(stage, step) for step in range(AXES)])

    def small_end(stage):
        for step in range(AXES):
            small_reach(stage, step).wait_recv()

    small_pass = small_copy(AXES * AXES, [pl.ds(0, SIDE)] * AXES, chip.partner())
    here = (*chip.where, chip.core)
    own = [pltpu.make_async_copy(small_ref, small_full.at[here], next(own_sem))]
    for shard, full in zip(shards, fulls):
        for layer in range(LAYERS):
            own.append(pltpu.make_async_copy(shard.at[layer], full.at[(layer, *here)], next(own_sem)))
    loads = [
        pltpu.make_async_copy(src, dst, next(own_sem)) for src, dst in ((x_hbm, y_v), (ycot_hbm, n1_v), (tables_hbm, tables), (places_hbm, places))]
    cot_copies = half_copies(chip, n1_v, dout_cols.at[LAYERS - 1], next(own_sem), next(own_sem), next(own_sem))
    with jax.named_scope('ag0'):
        gather.begin(A, A)
        start(own)
        gather.begin(B, A)
        wait(own)
        small_begin(A)
        gather.own(A)
        gather.own(B)
        start(loads)
        gather.end(A, A)
    with jax.named_scope('ag1'):
        gather.begin(A, B)
        small_end(A)
        small_begin(B)
        gather.end(B, A)
        gather.begin(B, B)
        gather.middle(A, B)
        small_end(B)
        small_begin(C)
        gather.middle(B, B)
        gather.end(A, B, (B, C))
    with jax.named_scope('ag2_start'):
        gather.begin(A, C)
        small_end(C)
        small_pass.start()
        gather.end(B, B, (B, C))
    with jax.named_scope('ag2_middle'):
        gather.middle(A, C)
        gather.begin(B, C)
    with jax.named_scope('unpack'):
        small_pass.wait_recv()
        fetch = pltpu.make_async_copy(small_full, small_v, next(own_sem))
        fetch.start()
        fetch.wait()
        wait(loads)
        start(cot_copies)
        for layer in range(LAYERS):
            unpack_vectors(small_v, layer, places[A:B], places[B:C], vec_ref)
    with jax.named_scope('ag2_late'):
        gather.end(A, C, (B,))
    with jax.named_scope('ag2_end'):
        gather.end(A, C, (C,))
        wait(cot_copies)

    def saves(layer):
        pairs = [(y_v, h_hbm.at[layer]), (qkv_v, qkv_hbm.at[layer])]
        kept = [pltpu.make_async_copy(src, dst, save_sem.at[n]) for n, (src, dst) in enumerate(pairs)]
        for n, (src, dst) in enumerate(((n1_t, n1_hbm), (n2_t, n2_hbm), (ctx_t, ctx_hbm))):
            dst = dst.at[layer, chip.core]
            kept.append((pltpu.make_async_copy(src, dst, save_sem.at[CORES + n]),
                         remote(src, dst, share_send.at[layer, n], share_recv.at[layer, n], chip.partner())))
        return kept

    def quarter(layer, t):
        rows, tiles = pl.ds(t * WIDTH, WIDTH), pl.ds(CORES * t, CORES)
        src, dst = act_t.at[rows], act_hbm.at[layer, chip.core, rows]
        return [pltpu.make_async_copy(pre_v.at[tiles], pre_hbm.at[layer, tiles], act_save.at[A, t]),
                pltpu.make_async_copy(src, dst, act_save.at[B, t]),
                remote(src, dst, act_send.at[layer, t], act_recv.at[layer, t], chip.partner())]

    def settle(layer):
        _, qkv_save, *shares = saves(layer)
        qkv_save.wait()
        for share in shares:
            wait(share)

        @loop(SIDE)
        def _(t):
            wait(quarter(layer, t))

    @loop(LAYERS)
    def _(layer):
        def vector(k, first=0, width=None):
            return vec_ref[pl.ds(layer, 1), lanes(OFFSETS[k] + first, width or SIZES[k])]

        def load(k, piece):
            if k == DOWN:
                return pltpu.make_async_copy(fulls[k].at[layer, piece], down_v.at[piece], load_sem.at[k, piece])
            cols = lanes(piece * WIDTH, WIDTH)
            return pltpu.make_async_copy(fulls[k].at[layer, :, :, :, :, :, cols], (up_v, None, mix_v)[k].at[:, :, :, :, :, cols],
                                         load_sem.at[k, piece])

        def matrix(held, piece):
            return held[:, :, :, :, :, lanes(piece * WIDTH, WIDTH)].reshape((WIDTH, WIDTH))

        def have(k):
            gather.arrived(layer, k)

        def meanwhile(action):
            @pl.when(layer == A)
            def _():
                action()

        h_save, qkv_save, n1_share, n2_share, ctx_share = saves(layer)
        with jax.named_scope('have_mix'):
            have(MIX)
            start([load(MIX, k) for k in range(SIDE)])

        h_save.start()

        @pl.when(layer == B)
        def _():
            settle(A)

        with jax.named_scope('ln'):
            @loop(SEQ // LN_ROWS)
            def _(r):
                rows = pl.ds(pl.multiple_of(r * LN_ROWS, LN_ROWS), LN_ROWS)
                scaled, _ = normalised(y_v[rows, :].astype(F32))
                n1_v[rows, :] = (scaled * vector(GAIN1) + vector(BIAS1)).astype(BF16)
                n2_v[rows, :] = (scaled * vector(GAIN2) + vector(BIAS2)).astype(BF16)

        for src, dst, share in ((n1_v, n1_t, n1_share), (n2_v, n2_t, n2_share)):
            dst[...] = src[...].T
            start(share)

        with jax.named_scope('qkv'):
            for k in range(PARTS):
                load(MIX, k).wait()
                x = dot(n1_v[...], matrix(mix_v, k)) + vector(QKV_BIAS, k * WIDTH, WIDTH)
                for c in range(N_PAIRS):
                    block = x[:, block_rows(c)]
                    if k < C:
                        block = turn(block, *[tables[n] for n in range(PARTS)])
                    qkv_v[:, lanes(k * WIDTH + c * PAIR)] = block.astype(BF16)

        qkv_save.start()
        with jax.named_scope('have_up'):
            have(UP)
            have(DOWN)

        start([load(UP, k) for k in range(SIDE)] + [load(DOWN, k) for k in range(SIDE)])
        with jax.named_scope('fattn'):
            def one_pair(pair):
                keys = split_heads(qkv_v[:, lanes(WIDTH + pair * PAIR)])
                values = split_heads(qkv_v[:, lanes(C * WIDTH + pair * PAIR)])
                for i in range(N_BLOCKS):
                    n = (i + 1) * CORES * PAIR
                    probs = probabilities(qkv_v[block_rows(i), lanes(pair * PAIR)], keys[:n], i)
                    ctx_v[block_rows(i), lanes(pair * PAIR)] = dot(side_by_side(probs), values[:n]).astype(BF16)

            @loop(N_PAIRS // CORES)
            def _(two):
                for k in HALVES:
                    one_pair(CORES * two + k)

                @pl.when((layer == A) & (two == A))
                def _():
                    gather.middle(B, C)

        ctx_t[...] = ctx_v[...].T
        start(ctx_share)
        with jax.named_scope('fout'):
            load(MIX, PARTS).wait()
            acc[...] = y_v[...].astype(F32) + dot(ctx_v[...], matrix(mix_v, PARTS)) + (vector(OUT_BIAS) + vector(DOWN_BIAS))

        with jax.named_scope('fmlp'):
            @loop(SIDE)
            def _(t):
                cols = lanes(t * WIDTH, WIDTH)
                load(UP, t).wait()
                pre = dot(n2_v[...], matrix(up_v, t)) + vector(UP_BIAS, t * WIDTH, WIDTH)
                for k in HALVES:
                    pre_v[CORES * t + k] = pre[:, k * TILE:(k + 1) * TILE]
                act = (0.5 * pre * (1.0 + lax.erf(pre * INV_SQRT2))).astype(BF16)
                act_t[cols, :] = act.T
                start(quarter(layer, t))
                load(DOWN, t).wait()
                acc[...] += dot(act, down_v[t].reshape((WIDTH, WIDTH)))

                @pl.when((layer == A) & (t == B))
                def _():
                    gather.end(B, C, (B,))

        h_save.wait()
        y_v[...] = acc[...].astype(BF16)
        with jax.named_scope('fend'):
            meanwhile(lambda: gather.end(B, C, (C,)))

    with jax.named_scope('ftail'):
        last = pltpu.make_async_copy(y_v, y_hbm, next(own_sem))
        last.start()
        for stage in range(AXES):
            for step in range(AXES):
                small_reach(stage, step).wait_send()
        small_pass.wait_send()
        gather.left()
        settle(LAYERS - 1)
        last.wait()


def forward(x, y_cot, shards, small_tile, tables, places):
    grid = CHIPS + (CORES,)
    full = [(LAYERS,) + grid + tensor.shape[1:] for tensor in shards]
    shapes = [(shape, BF16) for shape in full] + [(grid + small_tile.shape, BF16), ((LAYERS, N_VEC), F32), ((LAYERS, CORES, SEQ, TILE), BF16), ((SEQ, WIDTH), BF16),
                                                  ((LAYERS, SEQ, WIDTH), BF16)]
    shapes += [((LAYERS, CORES, width, SEQ), BF16) for width in (WIDTH, WIDTH, WIDTH, HIDDEN)]
    shapes += [((LAYERS, SEQ, QKV), BF16), ((LAYERS, N_TILES, SEQ, TILE), F32)]
    dma = pltpu.SemaphoreType.DMA
    slots = AXES * AXES
    scratch = [pltpu.VMEM(shape[1:], BF16) for shape in full] + [pltpu.VMEM(grid + small_tile.shape, BF16)]
    scratch += [pltpu.VMEM((SEQ, WIDTH), F32), pltpu.VMEM((N_TILES, SEQ, TILE), F32)]
    scratch += [pltpu.VMEM((SEQ, width), BF16) for width in (WIDTH, WIDTH, QKV, WIDTH, WIDTH)]
    scratch += [pltpu.VMEM((width, SEQ), BF16) for width in (WIDTH, WIDTH, WIDTH, HIDDEN)]
    scratch += [dma(shape) for shape in ((LAYERS, AXES, AXES), (LAYERS, AXES, len(HALVES), slots), (LAYERS, AXES), (LAYERS, AXES))]
    scratch += [dma(shape) for shape in ((slots + 1,), (slots + 1,), (slots + SIDE + SIDE + AXES,), (AXES, SIDE), (SIDE + 1,), (LAYERS, AXES), (LAYERS, AXES), (CORES, SIDE), (LAYERS, SIDE), (LAYERS, SIDE))]
    scratch += [pltpu.VMEM(tables.shape, F32), pltpu.VMEM(places.shape, jnp.int32)]
    out_specs = [IN_VMEM if dtype == F32 and len(shape) == LAYERS else ANY for shape, dtype in shapes]
    return pl.pallas_call(
        forward_kernel,
        out_shape=[jax.ShapeDtypeStruct(*s) for s in shapes],
        in_specs=[ANY] * SIDE + [IN_VMEM] * SIDE,
        out_specs=out_specs,
        scratch_shapes=scratch,
        compiler_params=pltpu.CompilerParams(collective_id=0, has_side_effects=True, vmem_limit_bytes=VMEM_LIMIT),
        name='forward_layers',
    )(x, y_cot, tables, places, *shards, small_tile)


WAVES = ((384, 384, 512), (384, 384, 256), (256, 256, 256))
LEADS = ((2,) + CHIPS[1:], CHIPS[1:], (2, SIDE), (SIDE,), (AXES,))
W_UP, W_DOWN, W_QKV, W_OUT = range(4)
STEPS = ((1, (2,)), (0, ()), (2, (4, 3)), (4, (5,)), (3, ()), (5, (6, 7, 8)), (8, (9,)), (9, ()))
LAST = AXES * AXES
CARRIED = ((0, 6), (1, 4), (2, 0))
US_COLUMN, US_HOP, US_ADD, US_STEP, US_LATE = 0.022, 2.5, 0.0007, 0.2, 2
US_FIRST, US_OUT, US_TILE, US_GRADIENT, US_PAIR, US_NORM = 2, 1.4, 1.6, 0.0025, 3.6, 2.7


class Schedule:
    def __init__(self):
        self.now, self.free, self.lines = 0.0, {}, []

    def send(self, link, columns):
        self.free[link] = max(self.free.get(link, 0.0), self.now) + columns * US_COLUMN
        return self.free[link] + US_HOP

    def due(self, limit):
        found = []
        while self.lines:
            line = min(self.lines, key=lambda one: one[A][A]())
            ready = line[A][A]()
            if limit is not None and ready > limit:
                break
            _, run, sends, cost = line.pop(A)
            self.lines = [one for one in self.lines if one]
            self.now = max(self.now, ready) + cost
            sends()
            found.append(run)
        return found

    def finish(self, line):
        while line:
            ready, run, sends, cost = line.pop(A)
            self.now = max(self.now, ready()) + cost
            sends()
            run()
        self.lines = [one for one in self.lines if one]

    def run(self, limit):
        for step in self.due(limit):
            step()

    def passed(self, cost):
        self.now += cost
        self.run(self.now)

    def hooks(self, count, cost):
        planned = []
        for _ in range(count):
            self.now += cost
            planned.append(self.due(self.now))
        return planned


def at_hooks(n, planned):
    for when, steps in enumerate(planned):
        if steps:
            @pl.when(n == when)
            def _():
                for step in steps:
                    step()


def add_into(dst, src, n_axes):
    if n_axes < 2:
        dst[...] += src[...]
        return

    @loop(SIDE)
    def _(k):
        dst[k] += src[k]


def at_axis(ref, axis, value, n_axes):
    every = [pl.ds(0, SIDE)] * n_axes
    every[axis] = value
    return ref.at[tuple(every)]


class Reduce:
    def __init__(self, chip, schedule, wave, grads, came, fin, sems, spare, write, done, when=None):
        self.wave, self.chip, self.schedule, self.widths, self.grads = wave, chip, schedule, WAVES[wave], grads
        self.came, self.fin, (self.send_sem, self.recv_sem), (self.spare, self.spare_sem) = came, fin, sems, spare
        self.write, self.done, self.when, self.times = write, done, when, {}

    def box(self, a, half, stage):
        order = ORDERS[a]
        ref = self.came[a][A].at[half, A]
        spot = [axis for axis in range(AXES) if axis != order[A]].index(order[B])
        if stage == B:
            return ref, spot, C
        return at_axis(ref, spot, self.chip.where[order[B]], C), A, B

    def copy(self, a, half, slot):
        stage, turn = divmod(slot, AXES)
        sems = self.send_sem.at[a, stage], self.recv_sem.at[a, half, slot]
        if slot == LAST:
            return remote(self.total(a, half).at[self.chip.other], self.fin[a].at[half], *sems, self.chip.partner())
        axis = ORDERS[a][stage]
        if stage == C:
            role = value = ROLES[turn]
            dst = self.came[a][SIDE].at[half, turn]
        else:
            role, value = TWO if turn == C else ONE, (ONE, CROSS, TWO)[turn]
            dst = self.came[a][CORES * stage + turn // C].at[half]
            dst = dst if turn == C else dst.at[turn]
        value = self.chip.at(axis, value, half)
        if stage:
            ref, spot, n_axes = self.box(a, half, stage)
            src = at_axis(ref, spot, value, n_axes)
        else:
            src = self.came[a][A].at[half, B] if turn == C else at_axis(self.grads[a].at[half], axis, value, AXES)
        return remote(src, dst, *sems, self.chip.device(axis, role, half))

    def each(self, action):
        for a in range(AXES):
            halves(lambda half: action(a, half))

    def sending(self, slot):
        stage = slot // AXES
        share = SIDE ** (CORES * stage)
        self.times[slot] = self.schedule.now + US_HOP if slot == LAST else max(
            self.schedule.send(ORDERS[a][stage], self.widths[a] / share) for a in range(AXES))

    def begin(self):
        for slot in (B, A):
            self.each(lambda a, half: self.copy(a, half, slot).start())

    def plan(self, first=0, last=None):
        for slot in (B, A):
            self.times[slot] = self.schedule.now + US_LATE
            if not first:
                self.sending(slot)
        for _, sent in STEPS[:first]:
            self.times.update((slot, self.schedule.now + US_LATE + US_HOP) for slot in sent)
        line = [
            (lambda slot=slot: self.times[slot], lambda k=k: self.step(k), lambda sent=sent: [self.sending(n) for n in sent],
             CORES * US_ADD * sum(self.widths) if k < C else US_STEP) for k, (slot, sent) in enumerate(STEPS)][first:last]
        self.schedule.lines.append(line)
        return line

    def step(self, k):
        def work():
            with jax.named_scope(f'w{self.wave}s{k}'):
                (self.first, self.first, self.halve, self.settle, self.settle, self.spread, self.cross, self.finish)[k](STEPS[k][A])
        if self.when is None:
            work()
        else:
            pl.when(self.when)(work)

    def held(self, a, half):
        ref = self.spare[A].at[a] if a < C else self.spare[B]
        return ref.at[half, :, :, :, :, pl.ds(0, self.widths[a])]

    def first(self, slot):
        def local(a, half):
            axis = ORDERS[a][A]
            return pltpu.make_async_copy(at_axis(self.grads[a].at[half], axis, self.chip.at(axis, TWO if slot else OWN, half), AXES),
                                         self.held(a, half), self.spare_sem.at[a, half])

        def action(a, half):
            local(a, half).wait()
            self.copy(a, half, slot).wait_recv()
            add_into(self.came[a][A].at[half, slot], self.held(a, half), C)
            if slot:
                self.copy(a, half, C).start()

        self.each(lambda a, half: local(a, half).start())
        self.each(action)

    def halve(self, slot):
        def action(a, half):
            ref, spot, n_axes = self.box(a, half, B)
            self.copy(a, half, slot).wait_recv()
            for turn, role in ((B, CROSS), (A, ONE), (C, TWO), (C, OWN)):
                value = self.chip.at(ORDERS[a][B], role, half)
                add_into(at_axis(ref, spot, value, n_axes), at_axis(self.came[a][B].at[half], spot, value, n_axes), B)
                if turn < C:
                    self.copy(a, half, AXES + turn).start()
        self.each(action)

    def settle(self, slot):
        def action(a, half):
            ref, spot, n_axes = self.box(a, half, B)
            self.copy(a, half, slot).wait_recv()
            value = self.chip.at(ORDERS[a][B], TWO if slot > AXES else OWN, half)
            add_into(at_axis(ref, spot, value, n_axes), self.came[a][C].at[half, slot - AXES], B)
            if slot > AXES:
                self.copy(a, half, AXES + C).start()
        self.each(action)

    def spread(self, slot):
        def action(a, half):
            ref, *_ = self.box(a, half, C)
            self.copy(a, half, slot).wait_recv()
            add_into(ref, self.came[a][AXES].at[half], B)
            for turn in range(AXES):
                self.copy(a, half, CORES * AXES + turn).start()
        self.each(action)

    def total(self, a, half):
        ref, *_ = self.box(a, half, C)
        return ref.at[self.chip.where[ORDERS[a][C]]]

    def cross(self, _):
        def action(a, half):
            for turn in range(AXES):
                self.copy(a, half, CORES * AXES + turn).wait_recv()
            self.total(a, half)[...] += total_of([self.came[a][SIDE][half, turn] for turn in range(AXES)])
            self.copy(a, half, LAST).start()
        self.each(action)

    def finish(self, _):
        def action(a, half):
            self.write(a, half, self.chip.core, self.total(a, half)[self.chip.core])
            self.copy(a, half, LAST).wait_recv()
            self.write(a, half, self.chip.other, self.fin[a][half])
        self.each(action)
        three = pl.ds(0, AXES)
        for a, (grad, fin) in enumerate(zip(self.grads, self.fin)):
            for stage, block in enumerate((grad.at[:, :, :, three], grad.at[:, :, three, A], grad.at[:, three, A, A], fin)):
                sem = self.send_sem.at[a, stage]
                remote(block, block, sem, sem, self.chip.partner()).wait_send()
        self.done()


class VectorSum:
    def __init__(self, chip, schedule, total, came, sems, finish, when=None):
        self.schedule, self.total, self.came, self.sems, self.finish, self.when, self.ready = schedule, total, came, sems, finish, when, 0.0
        self.devices = [[chip.device(axis, role, A) for role in ROLES] for axis in range(AXES)] + [[chip.partner()]]

    def copies(self, k):
        return [remote(self.total, self.came.at[AXES * k + n], self.sems.at[A, AXES * k + n], self.sems.at[B, AXES * k + n], device)
                for n, device in enumerate(self.devices[k])]

    def sending(self, k):
        if k < SIDE:
            self.ready = self.schedule.send(k, N_VEC / (SIDE * SIDE * ROWS))

    def step(self, k):
        def work():
            with jax.named_scope(f'vec{k}'):
                wait(self.copies(k - 1))
                for n in range(len(self.devices[k - 1])):
                    self.total[...] += self.came[AXES * (k - 1) + n]
            if k < SIDE:
                start(self.copies(k))
            else:
                self.finish()
        if self.when is None:
            work()
        else:
            pl.when(self.when)(work)

    def begin(self):
        start(self.copies(A))

    def plan(self):
        self.sending(A)
        self.schedule.lines.append([
            (lambda: self.ready, lambda k=k: self.step(k), lambda k=k: self.sending(k), US_STEP) for k in range(1, SIDE + 1)])


def backward_kernel(ycot_hbm, tables, vec_ref, places, up_hbm, down_hbm, mix_hbm, h_hbm, n1_hbm, n2_hbm, ctx_hbm,
                    act_hbm, qkv_hbm, pre_hbm, _, dx_hbm, small_ref, up_sum, down_sum, qkv_sum, out_sum, dout_cols, dpre_cols,
                    dqkv_cols, *refs):
    n_arrays, sums = AXES * len(WAVES), (up_sum, down_sum, qkv_sum, out_sum)
    grads, refs = refs[:n_arrays], refs[n_arrays:]
    (spare, spare_wide, tile_v, big_v, rhs_v, wup_v, wdown_v, pre_v, dn1, dn2, dctx, dk_acc, dv_acc, qkv_v, dpre_v, dqkv_v, dh_v, h_v,
     totals, came_vec, send_sem, recv_sem, spare_sem, tile_sem, big_sem, rhs_sem, mlp_sem, io_sem, own_sem, share_send,
     share_recv, pre_sem, vec_sem, credit, *refs) = refs
    fins, came = refs[:n_arrays], refs[n_arrays:]
    first_in = pltpu.make_async_copy(ycot_hbm, dh_v, io_sem.at[A])
    first_in.start()
    chip = Chip()
    core, other = chip.core, chip.other

    def exchange(layer, k, src, dst):
        return half_copies(chip, src, dst.at[layer], own_sem.at[k], share_send.at[k], share_recv.at[k])

    def tokens_load(layer, src, part, slot):
        return [pltpu.make_async_copy(src.at[layer, k, pl.ds(part * WIDTH, WIDTH)], big_v.at[slot, :, pl.ds(k * SEQ, SEQ)],
                                      big_sem.at[slot, k]) for k in range(CORES)]

    def weight_load(layer, k, slot):
        return pltpu.make_async_copy(mix_hbm.at[layer, :, lanes(k * WIDTH, WIDTH)], big_v.at[slot], big_sem.at[slot, CORES])

    def tile_loads(layer, t, slot):
        rows = lanes(t * TILE, TILE)
        pairs = ((down_hbm.at[layer, rows], wdown_v), (pre_hbm.at[layer, t], pre_v), (up_hbm.at[layer, :, rows], wup_v))
        return [pltpu.make_async_copy(src, dst.at[slot], mlp_sem.at[slot, n]) for n, (src, dst) in enumerate(pairs)]

    def input_loads(layer):
        return [pltpu.make_async_copy(qkv_hbm.at[layer], qkv_v, io_sem.at[B]), pltpu.make_async_copy(h_hbm.at[layer], h_v, io_sem.at[C])]

    def rhs_load(layer, src, first, width, k):
        cols = lanes(first, width)
        return [pltpu.make_async_copy(src.at[layer, n, :, cols], rhs_v.at[pl.ds(n * SEQ, SEQ), cols], rhs_sem.at[k, n])
                for n in range(CORES)]

    def prefetch(layer):
        start(tokens_load(layer, ctx_hbm, A, AXES) + tokens_load(layer, act_hbm, A, A))

    def prefetch_more(layer):
        start(tokens_load(layer, act_hbm, B, B) + tokens_load(layer, act_hbm, C, C) + input_loads(layer))
        for t in HALVES:
            start(tile_loads(layer, t, t))

    prefetch(LAYERS - 1)
    start(rhs_load(LAYERS - 1, dout_cols, A, TILE, A))
    with jax.named_scope('enter'):
        enter(chip)
    with jax.named_scope('first_in'):
        first_in.wait()
    dx_copy = pltpu.make_async_copy(dh_v, dx_hbm, io_sem.at[A])
    prefetch_more(LAYERS - 1)

    def vector_at(k, first=0, width=None):
        return lanes(OFFSETS[k] + first, width or SIZES[k])

    def reduction(schedule, layer, wave, when):
        def write(a, half, side, block):
            def put(arr, group, col, first, width):
                size = sums[arr].shape[-1] // CORES
                sums[arr][layer, group, :, lanes(side * size + col, width)] = block[:, first:first + width].astype(BF16)
            width, colour = WAVES[wave][a], CORES * a + half
            if wave:
                first = colour * width if wave == C or a < C else SIDE * WAVES[wave][A] + half * width
                put(W_QKV if wave == C else W_UP, A, first, A, width)
            elif a < C:
                put(W_DOWN, colour, A, A, width)
            else:
                for k in HALVES:
                    put(W_DOWN, CORES * half + k, WAVES[A][A], k * PAIR, PAIR)
                put(W_OUT, A, half * TWICE, TWICE, TWICE)

        def done():
            @pl.when(layer == LAYERS - 1)
            def _():
                chip.signal_partners(credit.at[wave])

        where = slice(AXES * wave, AXES * (wave + 1))
        count = len(LEADS)
        return Reduce(chip, schedule, wave, [grad.at[layer] for grad in grads[where]],
                      [came[count * (AXES * wave + a):count * (AXES * wave + a + 1)] for a in range(AXES)],
                      fins[where], (send_sem.at[wave], recv_sem.at[wave]), ((spare, spare_wide), spare_sem), write, done, when)

    def vector_sum(schedule, layer, when):
        def own_part():
            with jax.named_scope('own'):
                node, local = chip.base
                me = node * (SIDE * CORES) + local + core
                row = jnp.zeros((ROWS, PAIR), F32)
                for k, share in enumerate(SHARES):
                    if k == QKV_BIAS:
                        firsts = [part * WIDTH + lax.div(me, CORES * ROWS) * PAIR for part in range(PARTS)]
                    else:
                        firsts = [lax.div(me * share, PAIR) * PAIR]
                    for first in firsts:
                        cols = lanes(OFFSETS[k] + first)
                        left = jnp.zeros((ROWS, PAIR), F32) + totals[layer, :, cols] * (places[A:B, cols] == me).astype(F32)
                        pick = (iota((PAIR, PAIR), 0) == places[B:C, cols]).astype(F32).astype(BF16)
                        for _ in range(PARTS):
                            row = row + dot_t(left.astype(BF16), pick)
                            left = left - rounded(left)
                small_ref[layer] = row.astype(BF16)

            @pl.when(layer == LAYERS - 1)
            def _():
                chip.signal_partners(credit.at[AXES])

        return VectorSum(chip, schedule, totals.at[layer], came_vec, vec_sem, own_part, when)

    def run_on(schedule, layer, when):
        vector_sum(schedule, layer, when).plan()
        return [reduction(schedule, layer, wave, when).plan(step) for wave, step in CARRIED]

    @loop(LAYERS + 1)
    def _(turn_no):
        layer = LAYERS - 1 - turn_no
        working = pl.when(turn_no < LAYERS)
        total = totals.at[layer]
        schedule = Schedule()

        carried = run_on(schedule, layer + 1, turn_no > A)

        def product(lhs_slot, first, width, out_slot):
            value = dot(big_v[lhs_slot, :, 0:CORES * SEQ], rhs_v[:, lanes(first, width)])
            tile_v[out_slot, :, :, :, :, :, 0:width] = value.reshape(CHIPS + (CORES, ROWS, width))

        def tile_out(slot, src, dst):
            return pltpu.make_async_copy(src, dst, tile_sem.at[slot])

        def tile_done(slot, width):
            block = tile_v.at[slot, :, :, :, :, :, pl.ds(0, width)]
            tile_out(slot, block, block).wait()

        def columns(wave, a, half, first, width):
            return grads[AXES * wave + a].at[layer, half, :, :, :, :, :, pl.ds(first, width)]

        def launch(wave):
            schedule.finish(carried[wave])

            @pl.when(turn_no == B)
            def _():
                pl.semaphore_wait(credit.at[wave], PARTNERS)

            current = reduction(schedule, layer, wave, turn_no < LAYERS)
            if wave == C:
                @pl.when(turn_no == B)
                def _():
                    pl.semaphore_wait(credit.at[AXES], PARTNERS)

                @working
                def _():
                    vector_sum(schedule, layer, None).begin()

            working(current.begin)
            if wave < C:
                current.plan(last=dict(CARRIED)[wave])

        @working
        def _():
            with jax.named_scope('dw_out'):
                @pl.when(turn_no == B)
                def _():
                    wait(exchange(layer, A, dh_v, dout_cols))
                    start(rhs_load(layer, dout_cols, A, TILE, A))

                wait(rhs_load(layer, dout_cols, A, TILE, A))
                wait(tokens_load(layer, ctx_hbm, A, AXES))
                product(AXES, A, TILE, B)
                start(tokens_load(layer, act_hbm, AXES, AXES))
                for k in HALVES:
                    tile_out(B, tile_v.at[B, :, :, :, :, :, pl.ds(k * TWICE, TWICE)], columns(A, C, k, TWICE, TWICE)).start()

        schedule.passed(US_FIRST)
        out_hooks = schedule.hooks(SIDE, US_OUT)

        @loop(SIDE)
        def _(z):
            @working
            def _():
                slot = parity(z)
                wait(tokens_load(layer, act_hbm, z, z))

                @pl.when(z > A)
                def _():
                    tile_done(slot, TILE)

                product(z, A, TILE, slot)
                split = WAVES[A][A]
                for k in range(SIDE):
                    a, half = divmod(k, CORES)
                    for c in range(CORES):
                        block = tile_v.at[slot, :, :, CORES * c + a, half]
                        tile_out(slot, block.at[:, :, :, pl.ds(0, split)], grads[a].at[layer, half, z, :, :, c]).start()
                        tile_out(slot, block.at[:, :, :, pl.ds(split, PAIR)],
                                 grads[C].at[layer, a, z, :, :, c, :, pl.ds(half * PAIR, PAIR)]).start()

            at_hooks(z, out_hooks)

        @working
        def _():
            start(tokens_load(layer, n2_hbm, A, A) + [weight_load(layer, k, k + 1) for k in range(PARTS)])
            for slot in HALVES:
                tile_done(slot, TILE)

        schedule.passed(US_STEP)
        launch(A)

        @working
        def _():
            dn2[...] = jnp.zeros_like(dn2)

        def pre_copy(t, slot, away):
            place = dpre_cols.at[layer, core, :, lanes(lax.rem(t, SIDE) * TILE, TILE)]
            if away:
                return remote(dpre_v.at[slot], place, pre_sem.at[A, t], pre_sem.at[B, t], chip.partner())
            return pltpu.make_async_copy(dpre_v.at[slot], place, own_sem.at[CORES + slot])

        def pre_act(t, leave):
            for away, whose in ((False, core), (True, other)):
                @pl.when(lax.div(t, SIDE) == whose)
                def _():
                    copy = pre_copy(t, parity(t), away)
                    if leave:
                        copy.start()
                    elif away:
                        copy.wait_send()
                    else:
                        copy.wait()

        tile_hooks = schedule.hooks(N_TILES, US_TILE)

        with jax.named_scope('mlp'):
            @loop(N_TILES)
            def _(t):
                @working
                def _():
                    slot = parity(t)
                    wait(tile_loads(layer, t, slot))
                    d_act = rounded(dot_t(dh_v[...], wdown_v[slot]))
                    pre = pre_v[slot]
                    slope = 0.5 * (1.0 + lax.erf(pre * INV_SQRT2)) + pre * (INV_SQRT2PI * jnp.exp(-0.5 * pre * pre))
                    d_pre = d_act * slope
                    total[:, vector_at(UP_BIAS, t * TILE, TILE)] = column_sum(d_pre)

                    @pl.when(t > B)
                    def _():
                        pre_act(t - CORES, False)

                    dpre_v[slot] = d_pre.astype(BF16)
                    pre_act(t, True)
                    dn2[...] += dot_t(dpre_v[slot], wup_v[slot])

                    @pl.when(t + CORES < N_TILES)
                    def _():
                        start(tile_loads(layer, t + CORES, slot))

                at_hooks(t, tile_hooks)

        @working
        def _():
            for t in HALVES:
                pre_act(N_TILES - CORES + t, False)
            for t in range(SIDE):
                pre_copy(SIDE * core + t, A, True).wait_recv()

        def gradient_loads(wave, source):
            first = 0
            for a in range(AXES):
                width = CORES * WAVES[wave][a]
                start(rhs_load(layer, source, first, width, a))
                first += width

        def gradient_wave(wave, source, lhs_slot, first, orders):
            split, count = WAVES[wave][orders[A]], len(orders)
            width = CORES * split
            planned = schedule.hooks(count, width * US_GRADIENT)

            @loop(count)
            def _(n):
                @working
                def _():
                    slot = parity(n)
                    wait(rhs_load(layer, source, first + n * width, width, orders[A] + n))

                    @pl.when(n > B)
                    def _():
                        tile_done(slot, width)

                    product(lhs_slot, first + n * width, width, slot)
                    for k, a in enumerate(orders):
                        @pl.when(n == k)
                        def _():
                            for half in HALVES:
                                block = tile_v.at[slot, :, :, :, :, :, pl.ds(half * split, split)]
                                tile_out(slot, block, columns(wave, a, half, 0, split)).start()

                at_hooks(n, planned)

            @working
            def _():
                for slot in range(min(count, CORES)):
                    tile_done(slot, width)

        @working
        def _():
            gradient_loads(B, dpre_cols)
            wait(tokens_load(layer, n2_hbm, A, A))

        with jax.named_scope('dw1'):
            gradient_wave(B, dpre_cols, A, A, (A, B))
            gradient_wave(B, dpre_cols, A, SIDE * WAVES[B][A], (C,))
        launch(B)
        @working
        def _():
            weight_load(layer, AXES, A).start()
            d_sum = column_sum(dh_v[...].astype(F32))
            total[:, vector_at(OUT_BIAS)] = d_sum
            total[:, vector_at(DOWN_BIAS)] = d_sum
            wait(input_loads(layer))
            weight_load(layer, AXES, A).wait()
            dctx[...] = dot_t(dh_v[...], big_v[A]).astype(BF16)

        pair_hooks = schedule.hooks(N_PAIRS // CORES, US_PAIR)

        with jax.named_scope('attn'):
            def one_pair(pair, dk_sum, dv_sum):
                at = lanes(pair * PAIR)
                keys = split_heads(qkv_v[:, lanes(WIDTH + pair * PAIR)])
                values = split_heads(qkv_v[:, lanes(C * WIDTH + pair * PAIR)])
                q_t = qkv_v[:, at].T
                dc_t = dctx[:, at].T
                bias_sums = [jnp.zeros((1, PAIR), F32)] * PARTS

                def turned_back(n, d, rows, to):
                    d = turn_back(rounded(d), *[tables[k, rows, :] for k in range(PARTS)])
                    bias_sums[n] = bias_sums[n] + column_sum(d)
                    dqkv_v[rows, to] = d.astype(BF16)

                for i in range(N_BLOCKS):
                    old, n = i * TWICE, (i + 1) * TWICE
                    rows = block_rows(i)
                    probs = probabilities(qkv_v[rows, at], keys[:n], i)
                    d_all = rounded(dot_t(dctx[rows, at], values[:n]))
                    d_scores = [d_all[:, block_rows(j)] for j in range(CORES * (i + 1))]
                    for head in HALVES:
                        mine = slice(head, None, CORES)
                        mean = row_sum(total_of([p * d for p, d in zip(probs[mine], d_scores[mine])]))
                        d_scores[mine] = [p * (d - mean) * SCALE for p, d in zip(probs[mine], d_scores[mine])]
                    d_scores, probs = side_by_side(d_scores), side_by_side(probs)
                    turned_back(A, dot(d_scores, keys[:n]), rows, at)
                    for acc, left, right in ((dk_sum, q_t, d_scores), (dv_sum, dc_t, probs)):
                        part = dot(left[:, rows], right)
                        if i:
                            acc[:, :old] += part[:, :old]
                        acc[:, old:n] = part[:, old:]
                first = iota((PAIR, PAIR), 0) < HEAD
                for j in range(N_BLOCKS):
                    rows = block_rows(j)
                    d_key, d_value = [jnp.where(first, acc[:, block_rows(CORES * j)], acc[:, block_rows(CORES * j + 1)]).T
                                      for acc in (dk_sum, dv_sum)]
                    turned_back(B, d_key, rows, lanes(WIDTH + pair * PAIR))
                    d_value = d_value.astype(BF16)
                    bias_sums[C] = bias_sums[C] + column_sum(d_value.astype(F32))
                    dqkv_v[rows, lanes(C * WIDTH + pair * PAIR)] = d_value
                for k, bias_sum in enumerate(bias_sums):
                    total[:, vector_at(QKV_BIAS, k * WIDTH + pair * PAIR, PAIR)] = bias_sum

            @loop(N_PAIRS // CORES)
            def _(two):
                @working
                def _():
                    for k in HALVES:
                        one_pair(CORES * two + k, dk_acc.at[k], dv_acc.at[k])

                at_hooks(two, pair_hooks)

        @working
        def _():
            start(exchange(layer, B, dqkv_v, dqkv_cols))
            dn1[...] = jnp.zeros_like(dn1)

            with jax.named_scope('dn1'):
                @loop(PARTS)
                def _(k):
                    weight_load(layer, k, k + 1).wait()
                    dn1[...] += dot_t(dqkv_v[:, lanes(k * WIDTH, WIDTH)], big_v[k + 1])

            start(tokens_load(layer, n1_hbm, A, B))

        schedule.passed(US_NORM)

        @working
        def _():
            for k in (GAIN1, BIAS1, GAIN2, BIAS2):
                total[:, vector_at(k)] = jnp.zeros((1, WIDTH), F32)

            with jax.named_scope('lnb'):
                @loop(SEQ // LN_ROWS)
                def _(r):
                    rows = pl.ds(pl.multiple_of(r * LN_ROWS, LN_ROWS), LN_ROWS)
                    scaled, inverse = normalised(h_v[rows, :].astype(F32))
                    d1, d2 = rounded(dn1[rows, :]), rounded(dn2[rows, :])
                    for k, value in ((GAIN1, d1 * scaled), (BIAS1, d1), (GAIN2, d2 * scaled), (BIAS2, d2)):
                        total[:, vector_at(k)] += column_sum(value)
                    g1, g2 = [vec_ref[pl.ds(layer, 1), lanes(OFFSETS[k], WIDTH)] for k in (GAIN1, GAIN2)]
                    d_scaled = d1 * g1 + d2 * g2
                    d_h = inverse * (d_scaled - row_mean(d_scaled) - scaled * row_mean(d_scaled * scaled))
                    dh_v[rows, :] = (dh_v[rows, :].astype(F32) + d_h).astype(BF16)

        schedule.passed(US_NORM)
        @working
        def _():
            wait(exchange(layer, B, dqkv_v, dqkv_cols))
            gradient_loads(C, dqkv_cols)
            wait(tokens_load(layer, n1_hbm, A, B))

        @pl.when(turn_no == A)
        def _():
            start(exchange(layer - 1, A, dh_v, dout_cols))

        @pl.when(turn_no == B)
        def _():
            dx_copy.start()

        with jax.named_scope('dw2'):
            gradient_wave(C, dqkv_cols, B, A, (A, B, C))

        @pl.when(turn_no == A)
        def _():
            prefetch(layer - 1)
            prefetch_more(layer - 1)

        schedule.run(None)
        launch(C)

    dx_copy.wait()


def backward(y_cot, tables, vectors, places, weights, saved):
    dma, one = pltpu.SemaphoreType.DMA, (1,)
    pair, wide, row = (len(HALVES),), (SEQ, WIDTH), one + (N_VEC,)
    shapes = [(wide, BF16), ((LAYERS, ROWS, PAIR), BF16)]
    shapes += [((LAYERS, groups, ROWS, width), BF16) for groups, width in ((*one, HIDDEN), (SIDE, WIDTH), (*one, QKV), (*one, WIDTH))]
    in_vmem = len(shapes)
    shapes += [((LAYERS, CORES, SEQ, width), BF16) for width in (TILE, SIDE * TILE, PARTS * TILE)]
    blocks = [(CORES, ROWS, width) for wave in WAVES for width in wave]
    shapes += [((LAYERS,) + pair + CHIPS + block, F32) for block in blocks]
    tile = (CORES, ROWS)
    scratch = [(pair + pair + CHIPS[1:] + tile + (WAVES[0][0],), F32), (pair + CHIPS[1:] + tile + (TILE,), F32), (pair + CHIPS + tile + (CORES * WAVES[0][0],), F32), ((SIDE, WIDTH, WIDTH), BF16), ((CORES * SEQ, SIDE * TILE), BF16)]
    scratch += [(pair + shape, BF16) for shape in ((WIDTH, TILE), (TILE, WIDTH))]
    scratch += [(pair + (SEQ, TILE), F32), (wide, F32), (wide, F32), (wide, BF16)] + [(pair + (PAIR, CORES * SEQ), F32)] * CORES
    scratch += [((SEQ, QKV), BF16), (pair + (SEQ, TILE), BF16), ((SEQ, QKV), BF16), (wide, BF16), (wide, BF16), ((LAYERS,) + row, F32),
                ((PARTNERS,) + row, F32)]
    slots = (len(WAVES), AXES) + pair + (LAST + 1,)
    sems = [dma(shape) for shape in ((len(WAVES), AXES, SIDE), slots, (AXES,) + pair, pair, (SIDE, AXES), (AXES, CORES), pair + (PARTS,), (AXES,),
                                     (SIDE,), pair, pair, pair + (N_TILES,), pair + (PARTNERS,))]
    late = [(pair + block[1:], F32) for block in blocks] + [(pair + lead + block, F32) for block in blocks for lead in LEADS]
    outs = pl.pallas_call(
        backward_kernel,
        out_shape=[jax.ShapeDtypeStruct(*s) for s in shapes],
        in_specs=[ANY] + [IN_VMEM] * AXES + [ANY] * (PARTNERS + 1),
        input_output_aliases={SIDE + PARTNERS: in_vmem},
        out_specs=[ANY] + [IN_VMEM] * (in_vmem - 1) + [ANY] * (len(shapes) - in_vmem),
        scratch_shapes=[pltpu.VMEM(*s) for s in scratch] + sems + [pltpu.SemaphoreType.REGULAR((SIDE,))]
        + [pltpu.VMEM(*s) for s in late],
        compiler_params=pltpu.CompilerParams(collective_id=1, has_side_effects=True, vmem_limit_bytes=VMEM_LIMIT),
        name='backward_layers',
    )(y_cot, tables, vectors, places, *weights, *saved)
    d_x, small, *sums = outs[:in_vmem]
    return d_x, small[:, 0], [s.reshape((LAYERS, -1, s.shape[-1])) for s in sums]


def finish_kernel(*refs):
    n_large = CORES + AXES
    large, small_ref, refs = refs[:n_large], refs[n_large], refs[n_large + 1:]
    outs, small_outs, refs = refs[:n_large], refs[n_large:n_large + len(SHARES)], refs[n_large + len(SHARES):]
    held, sems = refs[:n_large], refs[n_large]
    loads = start([pltpu.make_async_copy(src, dst, sems.at[n]) for n, (src, dst) in enumerate(zip(large, held))])
    first = 0
    for share, out in zip(SHARES, small_outs):
        out[...] = small_ref[:, first:first + share]
        first += share
    stores = []
    for load, src, dst in zip(loads, held, outs):
        load.wait()
        stores += start([pltpu.make_async_copy(src, dst, sems.at[n_large + len(stores)])])
    wait(stores)


def finish(large, small):
    shapes = [jax.ShapeDtypeStruct(t.shape, BF16) for t in large] + [jax.ShapeDtypeStruct((LAYERS, share), BF16) for share in SHARES]
    outs = pl.pallas_call(
        finish_kernel,
        out_shape=shapes,
        in_specs=[ANY] * len(large) + [IN_VMEM],
        out_specs=[ANY] * len(large) + [IN_VMEM] * len(SHARES),
        scratch_shapes=[pltpu.VMEM(t.shape, BF16) for t in large] + [pltpu.SemaphoreType.DMA((CORES * len(large),))],
        name='finish',
    )(*large, small)
    return outs[:len(large)], outs[len(large):]


def rope_tables():
    rot_dim, f32 = HEAD // SIDE, np.float32
    inv_freq = f32(1.0) / f32(10000.0) ** (np.arange(0, rot_dim, 2, dtype=f32) / f32(rot_dim))
    angles = np.arange(SEQ, dtype=f32)[:, None] * inv_freq[None, :]
    cos, sin = np.cos(angles), np.sin(angles)
    zero = np.zeros_like(sin)
    rest = np.zeros((SEQ, HEAD - rot_dim), f32)
    tables = ([cos, cos, rest + f32(1.0)], [-sin, zero, rest], [zero, sin, rest])
    return jnp.asarray(np.stack([np.tile(np.concatenate(table, axis=1), (1, 2)) for table in tables]).astype(f32))


def heads_last(tensor):
    lead = tensor.shape[:-2]
    return tensor.reshape(lead + (HEADS, PARTS, HEAD)).swapaxes(-3, -2).reshape(lead + (QKV,))


def heads_first(tensor):
    lead = tensor.shape[:-1]
    return tensor.reshape(lead + (PARTS, HEADS, HEAD)).swapaxes(-3, -2).reshape(lead + (HEADS, PARTS * HEAD))


def vector_places():
    shard, lane, first = [], [], 0
    for k, (share, size) in enumerate(zip(SHARES, SIZES)):
        place = np.arange(size)
        if k == QKV_BIAS:
            place = heads_last(place.reshape(HEADS, -1))
        shard.append(place // share)
        lane.append(first + place % share)
        first += share
    return jnp.asarray(np.stack([np.concatenate(shard), np.concatenate(lane)]).astype(np.int32))


def solution(mesh):
    shard_axes = ('node', 'local')
    act_spec = P(shard_axes)
    param_spec = P(None, shard_axes)

    def device_step(x, y_cot, ln1_gain, ln1_bias, qkv_weight, qkv_bias, out_weight, out_bias,
                    ln2_gain, ln2_bias, up_weight, up_bias, down_weight, down_bias):
        tables, places = rope_tables(), vector_places()
        small = (ln1_gain, ln1_bias, ln2_gain, ln2_bias, qkv_bias, out_bias, up_bias, down_bias)
        small_tile = jnp.pad(jnp.concatenate(small, axis=1), ((0, ROWS - LAYERS), (0, PAIR - sum(SHARES))))
        mix = jnp.concatenate([heads_last(qkv_weight), out_weight], axis=-1)
        *weights, _, vectors, dout_cols, y_out, hidden, n1, n2, ctx, act, qkv, pre = forward(
            x[0], y_cot[0], (up_weight, down_weight, mix), small_tile, tables, places)
        weights = [tensor.reshape((LAYERS, -1, tensor.shape[-1])) for tensor in weights]
        d_x, small_sums, (up, down, qkv, out) = backward(
            y_cot[0], tables, vectors, places, weights, (hidden, n1, n2, ctx, act, qkv, pre, dout_cols))
        (y_out, d_x, up, down, out), (g1, b1, g2, b2, qb, ob, ub, db) = finish((y_out, d_x, up, down, out), small_sums)
        return (y_out[None], d_x[None], g1, b1, heads_first(qkv), qb, out, ob, g2, b2, up, ub, down, db)

    return jax.shard_map(device_step, mesh=mesh,
                         in_specs=(act_spec, act_spec) + (param_spec,) * 12,
                         out_specs=(act_spec, act_spec) + (param_spec,) * 12,
                         check_vma=False)
```

```python
import functools
import jax
import jax.numpy as jnp
import numpy as np
from jax import lax
from jax.experimental import pallas as pl
from jax.experimental.pallas import tpu as pltpu
from jax.sharding import PartitionSpec as P

BF16, F32 = jnp.bfloat16, jnp.float32
EPSILON = 1e-5
MESH = pl.DeviceIdType.MESH
ANY = pl.BlockSpec(memory_space=pl.ANY)
IN_VMEM = pl.BlockSpec(memory_space=pltpu.VMEM)
VMEM_LIMIT = 67 * 10**6
LAYERS, AXES, SIDE, CORES, ROWS, PARTNERS = 2, 3, 4, 2, 8, 10
CHIPS = (SIDE, SIDE, SIDE)
SHARDS = SIDE * SIDE * SIDE * CORES
SEQ, WIDTH, HIDDEN, TILE, PAIR, LN_ROWS = 384, 1024, 4096, 512, 128, 64
HEADS, HEAD, PARTS = 16, 64, 3
QKV = PARTS * WIDTH
N_TILES, N_PAIRS, N_BLOCKS = HIDDEN // TILE, WIDTH // PAIR, SEQ // PAIR
TWICE = 2 * PAIR
INV_SQRT2, INV_SQRT2PI, SCALE = 0.7071067811865476, 0.3989422804014327, 0.125
SHARES = (8, 8, 8, 8, 24, 8, 32, 8)
SIZES = tuple(SHARDS * share for share in SHARES)
OFFSETS = tuple(sum(SIZES[:k]) for k in range(len(SIZES)))
N_VEC = sum(SIZES)
GAIN1, BIAS1, GAIN2, BIAS2, QKV_BIAS, OUT_BIAS, UP_BIAS, DOWN_BIAS = range(len(SHARES))
ORDERS = ((2, 1, 0), (1, 0, 2), (0, 2, 1))
HALVES = range(2)
OWN, ONE, CROSS, TWO = range(SIDE)
ROLES = (ONE, TWO, CROSS)
A, B, C = range(AXES)
UP, DOWN, MIX = range(3)
SELF = 3


class Chip:
    def __init__(self):
        node, local = lax.axis_index('node'), lax.axis_index('local')
        self.core, self.other = lax.rem(local, CORES), 1 - lax.rem(local, CORES)
        self.where = (lax.div(node, SIDE), lax.rem(node, SIDE), lax.div(local, CORES))
        self.base = (node, local - self.core)
        self.strides = ((SIDE, 0), (1, 0), (0, CORES))
        self.near = [(v, v + 1 - 2 * parity(v), lax.rem(v + 2, SIDE), SIDE - 1 - v) for v in self.where]

        self.gaps = [near[3] - near[1] for near in self.near]

    def at(self, axis, role, half):
        near = self.near[axis]
        if role in (OWN, CROSS):
            return near[role]
        return near[role] + half * self.gaps[axis] if role == ONE else near[role] - half * self.gaps[axis]

    def device(self, axis, role, half):
        shift = self.at(axis, role, half) - self.where[axis]
        node, local = [b + shift * s if s else b for b, s in zip(self.base, self.strides[axis])]
        return (node, local + self.core)

    def partner(self):
        node, local = self.base
        return (node, local + self.other)

    def signal_partners(self, semaphore):
        for axis in range(AXES):
            for role in ROLES:
                pl.semaphore_signal(semaphore, inc=1, device_id=self.device(axis, role, A), device_id_type=MESH)
        pl.semaphore_signal(semaphore, inc=1, device_id=self.partner(), device_id_type=MESH)


def enter(chip):
    barrier = pltpu.get_barrier_semaphore()
    chip.signal_partners(barrier)
    pl.semaphore_wait(barrier, PARTNERS)


def remote(src, dst, send_sem, recv_sem, device):
    return pltpu.make_async_remote_copy(src_ref=src, dst_ref=dst, send_sem=send_sem, recv_sem=recv_sem, device_id=device,
                                        device_id_type=MESH)


def start(copies):
    for copy in copies:
        copy.start()
    return copies


def wait(copies):
    for copy in copies:
        copy.wait()


def loop(count):
    return pl.loop(0, count)


def halves(body):
    loop(len(HALVES))(body)


def parity(n):
    return lax.rem(n, 2)


def pool(sems):
    return (sems.at[n] for n in range(sems.shape[0]))


def contract(a, b, a_axis, b_axis):
    return lax.dot_general(a, b, (((a_axis,), (b_axis,)), ((), ())), preferred_element_type=F32)


def dot(a, b):
    return contract(a, b, 1, 0)


def dot_t(a, b):
    return contract(a, b, 1, 1)


def row_sum(x):
    return jnp.sum(x, axis=1, keepdims=True)


def column_sum(x):
    return jnp.sum(x, axis=0, keepdims=True)


def rounded(x):
    return x.astype(BF16).astype(F32)


def lanes(first, width=PAIR):
    return pl.ds(pl.multiple_of(first, PAIR), width)


def turn(x, cos, sin_a, sin_b):
    return x * cos + pltpu.roll(x, PAIR - ROWS, 1) * sin_a + pltpu.roll(x, ROWS, 1) * sin_b


def turn_back(d, cos, sin_a, sin_b):
    return d * cos + pltpu.roll(d * sin_a, ROWS, 1) + pltpu.roll(d * sin_b, PAIR - ROWS, 1)


def iota(shape, axis):
    return lax.broadcasted_iota(jnp.int32, shape, axis)


def block_rows(j):
    return slice(j * PAIR, (j + 1) * PAIR)


def split_heads(x):
    first = iota((PAIR, PAIR), 1) < HEAD
    rows = []
    for j in range(N_BLOCKS):
        block = x[block_rows(j)]
        rows += [jnp.where(first, block, jnp.zeros_like(block)), jnp.where(first, jnp.zeros_like(block), block)]
    return jnp.concatenate(rows, axis=0)


def total_of(chunks, join=jnp.add):
    return functools.reduce(join, chunks)


def probabilities(q_block, keys, i):
    scores = dot_t(q_block, keys)
    causal = iota((PAIR, PAIR), 0) >= iota((PAIR, PAIR), 1)
    chunks = [scores[:, block_rows(j)] * SCALE for j in range(CORES * (i + 1))]
    for head in HALVES:
        mine = slice(head, None, CORES)
        *ahead, last = chunks[mine]
        held = ahead + [jnp.where(causal, last, -1e30)]
        top = jnp.max(total_of(held, jnp.maximum), axis=1, keepdims=True)
        held = [jnp.exp(chunk - top) for chunk in held]
        inverse = 1.0 / row_sum(total_of(held))
        chunks[mine] = [chunk * inverse for chunk in held]
    return chunks


def side_by_side(chunks):
    return jnp.concatenate([chunk.astype(BF16) for chunk in chunks], axis=1)


def row_mean(x):
    return jnp.mean(x, axis=1, keepdims=True)


def normalised(h):
    center = h - row_mean(h)
    inverse = lax.rsqrt(row_mean(center * center) + EPSILON)
    return center * inverse, inverse


def half_copies(chip, src, dst, own_sem, send_sem, recv_sem):
    width = dst.shape[-1]
    mine, away = [src.at[:, lanes(which * width, width)] for which in (chip.core, chip.other)]
    place = dst.at[chip.core]
    return [pltpu.make_async_copy(mine, place, own_sem), remote(away, place, send_sem, recv_sem, chip.partner())]


class Gather:
    def __init__(self, chip, shards, fulls, sems):
        self.chip, self.shards, self.fulls = chip, shards, fulls
        self.send_sem, self.recv_sem, self.pass_send, self.pass_recv = sems

    def box(self, layer, k, half, stage, role, own=False):
        width = self.fulls[k].shape[-1] // len(HALVES)
        cols = lanes(half * width, width)
        if own:
            return self.shards[k].at[layer, :, cols]
        where = list(self.chip.where)
        for axis in ORDERS[k][:stage]:
            where[axis] = pl.ds(0, SIDE)
        axis = ORDERS[k][stage]
        where[axis] = self.chip.at(axis, role, half)
        return self.fulls[k].at[layer, where[0], where[1], where[2], self.chip.core, :, cols]

    def reach(self, layer, k, half, stage, step):
        slot, on = AXES * stage + step, stage > A and step == C
        src = self.box(layer, k, half, stage, ONE if on else OWN, stage == A)
        return remote(src, self.box(layer, k, half, stage, ONE if on else OWN), self.send_sem.at[layer, k, stage],
                      self.recv_sem.at[layer, k, half, slot], self.chip.device(ORDERS[k][stage], TWO if on else ROLES[step], half))

    def passing(self, layer, k, half, stage, step):
        role = (*ROLES, OWN)[step]
        return remote(self.box(layer, k, half, stage, role, step == SELF), self.box(layer, k, half, stage, role),
                      self.pass_send.at[layer, k], self.pass_recv.at[layer, k], self.chip.partner())

    def each(self, action):
        for k in (MIX, UP, DOWN):
            @halves
            def _(half):
                action(k, half)

    def begin(self, layer, stage):
        for step in range(C if stage else AXES):
            self.each(lambda k, half: self.reach(layer, k, half, stage, step).start())

    def own(self, layer):
        self.each(lambda k, half: self.passing(layer, k, half, A, SELF).start())

    def middle(self, layer, stage):
        def action(k, half):
            self.reach(layer, k, half, stage, A).wait_recv()
            self.reach(layer, k, half, stage, C).start()
            self.passing(layer, k, half, stage, A).start()
        self.each(action)

    def end(self, layer, stage, steps=range(AXES)):
        def action(k, half):
            for step in steps:
                self.reach(layer, k, half, stage, step).wait_recv()
                self.passing(layer, k, half, stage, step).start()
        self.each(action)

    def arrived(self, layer, k):
        box = self.fulls[k].at[layer, :, :, :, self.chip.other]
        remote(box, box, self.pass_send.at[layer, k], self.pass_recv.at[layer, k], self.chip.partner()).wait_recv()

    def left(self):
        three, full = pl.ds(0, AXES), self.fulls[UP].at[A]
        boxes = (full.at[three, A, A, A], full.at[:, three, A, A], full.at[:, :, three, A])

        @loop(LAYERS)
        def _(layer):
            @loop(AXES)
            def _(k):
                for stage, box in enumerate(boxes):
                    sem = self.send_sem.at[layer, k, stage]
                    remote(box, box, sem, sem, self.chip.partner()).wait_send()
                box, sem = full.at[:, :, :, A], self.pass_send.at[layer, k]
                remote(box, box, sem, sem, self.chip.partner()).wait_send()


def pick_lanes(sel_lane, cols):
    return (iota((PAIR, WIDTH), 0) == sel_lane[:, cols]).astype(F32).astype(BF16)


def vector_blocks():
    return [slice(k * WIDTH, (k + 1) * WIDTH) for k in range(N_VEC // WIDTH)]


def unpack_vectors(small_v, layer, sel_shard, sel_lane, vec_ref):
    tiles = small_v[...].astype(F32).reshape((SHARDS, ROWS, PAIR))
    held = jnp.sum(jnp.where(iota(tiles.shape, 1) == layer, tiles, 0.0), axis=1).astype(BF16)
    for cols in vector_blocks():
        spread = dot(held, pick_lanes(sel_lane, cols))
        spread = jnp.where(iota((SHARDS, WIDTH), 0) == sel_shard[:, cols], spread, 0.0)
        vec_ref[layer:layer + 1, cols] = column_sum(spread)


def forward_kernel(x_hbm, ycot_hbm, tables_hbm, places_hbm, up_s, down_s, mix_s, small_ref, up_f, down_f, mix_f, small_full, vec_ref,
                   dout_cols, y_hbm, h_hbm, n1_hbm, n2_hbm, ctx_hbm, act_hbm, qkv_hbm, pre_hbm, up_v, down_v, mix_v, small_v, acc, pre_v,
                   n1_v, n2_v, qkv_v, ctx_v, y_v, n1_t, n2_t, ctx_t, act_t, send_sem, recv_sem, pass_send, pass_recv,
                   small_send, small_recv, own_sems, load_sem, save_sem, share_send, share_recv, act_save, act_send, act_recv, tables,
                   places):
    shards, fulls, own_sem = (up_s, down_s, mix_s), (up_f, down_f, mix_f), pool(own_sems)
    chip = Chip()
    with jax.named_scope('enter'):
        enter(chip)
    gather = Gather(chip, shards, fulls, (send_sem, recv_sem, pass_send, pass_recv))

    def small_copy(slot, where, device):
        place = small_full.at[(*where, chip.core)]
        return remote(place, place, small_send.at[slot], small_recv.at[slot], device)

    def small_reach(stage, step):
        where = list(chip.where)
        for axis in range(stage):
            where[axis] = pl.ds(0, SIDE)
        return small_copy(AXES * stage + step, where, chip.device(stage, ROLES[step], A))

    def small_begin(stage):
        start([small_reach(stage, step) for step in range(AXES)])

    def small_end(stage):
        for step in range(AXES):
            small_reach(stage, step).wait_recv()

    small_pass = small_copy(AXES * AXES, [pl.ds(0, SIDE)] * AXES, chip.partner())
    here = (*chip.where, chip.core)
    own = [pltpu.make_async_copy(small_ref, small_full.at[here], next(own_sem))]
    for shard, full in zip(shards, fulls):
        for layer in range(LAYERS):
            own.append(pltpu.make_async_copy(shard.at[layer], full.at[(layer, *here)], next(own_sem)))
    loads = [
        pltpu.make_async_copy(src, dst, next(own_sem)) for src, dst in ((x_hbm, y_v), (ycot_hbm, n1_v), (tables_hbm, tables), (places_hbm, places))]
    cot_copies = half_copies(chip, n1_v, dout_cols.at[LAYERS - 1], next(own_sem), next(own_sem), next(own_sem))
    with jax.named_scope('ag0'):
        gather.begin(A, A)
        start(own)
        gather.begin(B, A)
        wait(own)
        small_begin(A)
        gather.own(A)
        gather.own(B)
        start(loads)
        gather.end(A, A)
    with jax.named_scope('ag1'):
        gather.begin(A, B)
        small_end(A)
        small_begin(B)
        gather.end(B, A)
        gather.begin(B, B)
        gather.middle(A, B)
        small_end(B)
        small_begin(C)
        gather.middle(B, B)
        gather.end(A, B, (B, C))
    with jax.named_scope('ag2_start'):
        gather.begin(A, C)
        small_end(C)
        small_pass.start()
        gather.end(B, B, (B, C))
    with jax.named_scope('ag2_middle'):
        gather.middle(A, C)
        gather.begin(B, C)
    with jax.named_scope('unpack'):
        small_pass.wait_recv()
        fetch = pltpu.make_async_copy(small_full, small_v, next(own_sem))
        fetch.start()
        fetch.wait()
        wait(loads)
        start(cot_copies)
        for layer in range(LAYERS):
            unpack_vectors(small_v, layer, places[A:B], places[B:C], vec_ref)
    with jax.named_scope('ag2_late'):
        gather.end(A, C, (B,))
    with jax.named_scope('ag2_end'):
        gather.end(A, C, (C,))
        wait(cot_copies)

    def saves(layer):
        pairs = [(y_v, h_hbm.at[layer]), (qkv_v, qkv_hbm.at[layer])]
        kept = [pltpu.make_async_copy(src, dst, save_sem.at[n]) for n, (src, dst) in enumerate(pairs)]
        for n, (src, dst) in enumerate(((n1_t, n1_hbm), (n2_t, n2_hbm), (ctx_t, ctx_hbm))):
            dst = dst.at[layer, chip.core]
            kept.append((pltpu.make_async_copy(src, dst, save_sem.at[CORES + n]),
                         remote(src, dst, share_send.at[layer, n], share_recv.at[layer, n], chip.partner())))
        return kept

    def quarter(layer, t):
        rows, tiles = pl.ds(t * WIDTH, WIDTH), pl.ds(CORES * t, CORES)
        src, dst = act_t.at[rows], act_hbm.at[layer, chip.core, rows]
        return [pltpu.make_async_copy(pre_v.at[tiles], pre_hbm.at[layer, tiles], act_save.at[A, t]),
                pltpu.make_async_copy(src, dst, act_save.at[B, t]),
                remote(src, dst, act_send.at[layer, t], act_recv.at[layer, t], chip.partner())]

    def settle(layer):
        _, qkv_save, *shares = saves(layer)
        qkv_save.wait()
        for share in shares:
            wait(share)

        @loop(SIDE)
        def _(t):
            wait(quarter(layer, t))

    @loop(LAYERS)
    def _(layer):
        def vector(k, first=0, width=None):
            return vec_ref[pl.ds(layer, 1), lanes(OFFSETS[k] + first, width or SIZES[k])]

        def load(k, piece):
            if k == DOWN:
                return pltpu.make_async_copy(fulls[k].at[layer, piece], down_v.at[piece], load_sem.at[k, piece])
            cols = lanes(piece * WIDTH, WIDTH)
            return pltpu.make_async_copy(fulls[k].at[layer, :, :, :, :, :, cols], (up_v, None, mix_v)[k].at[:, :, :, :, :, cols],
                                         load_sem.at[k, piece])

        def matrix(held, piece):
            return held[:, :, :, :, :, lanes(piece * WIDTH, WIDTH)].reshape((WIDTH, WIDTH))

        def have(k):
            gather.arrived(layer, k)

        def meanwhile(action):
            @pl.when(layer == A)
            def _():
                action()

        h_save, qkv_save, n1_share, n2_share, ctx_share = saves(layer)
        with jax.named_scope('have_mix'):
            have(MIX)
            start([load(MIX, k) for k in range(SIDE)])

        h_save.start()

        @pl.when(layer == B)
        def _():
            settle(A)

        with jax.named_scope('ln'):
            @loop(SEQ // LN_ROWS)
            def _(r):
                rows = pl.ds(pl.multiple_of(r * LN_ROWS, LN_ROWS), LN_ROWS)
                scaled, _ = normalised(y_v[rows, :].astype(F32))
                n1_v[rows, :] = (scaled * vector(GAIN1) + vector(BIAS1)).astype(BF16)
                n2_v[rows, :] = (scaled * vector(GAIN2) + vector(BIAS2)).astype(BF16)

        for src, dst, share in ((n1_v, n1_t, n1_share), (n2_v, n2_t, n2_share)):
            dst[...] = src[...].T
            start(share)

        with jax.named_scope('qkv'):
            for k in range(PARTS):
                load(MIX, k).wait()
                x = dot(n1_v[...], matrix(mix_v, k)) + vector(QKV_BIAS, k * WIDTH, WIDTH)
                for c in range(N_PAIRS):
                    block = x[:, block_rows(c)]
                    if k < C:
                        block = turn(block, *[tables[n] for n in range(PARTS)])
                    qkv_v[:, lanes(k * WIDTH + c * PAIR)] = block.astype(BF16)

        qkv_save.start()
        with jax.named_scope('have_up'):
            have(UP)
            have(DOWN)

        start([load(UP, k) for k in range(SIDE)] + [load(DOWN, k) for k in range(SIDE)])
        with jax.named_scope('fattn'):
            def one_pair(pair):
                keys = split_heads(qkv_v[:, lanes(WIDTH + pair * PAIR)])
                values = split_heads(qkv_v[:, lanes(C * WIDTH + pair * PAIR)])
                for i in range(N_BLOCKS):
                    n = (i + 1) * CORES * PAIR
                    probs = probabilities(qkv_v[block_rows(i), lanes(pair * PAIR)], keys[:n], i)
                    ctx_v[block_rows(i), lanes(pair * PAIR)] = dot(side_by_side(probs), values[:n]).astype(BF16)

            @loop(N_PAIRS // CORES)
            def _(two):
                for k in HALVES:
                    one_pair(CORES * two + k)

                @pl.when((layer == A) & (two == A))
                def _():
                    gather.middle(B, C)

        ctx_t[...] = ctx_v[...].T
        start(ctx_share)
        with jax.named_scope('fout'):
            load(MIX, PARTS).wait()
            acc[...] = y_v[...].astype(F32) + dot(ctx_v[...], matrix(mix_v, PARTS)) + (vector(OUT_BIAS) + vector(DOWN_BIAS))

        with jax.named_scope('fmlp'):
            @loop(SIDE)
            def _(t):
                cols = lanes(t * WIDTH, WIDTH)
                load(UP, t).wait()
                pre = dot(n2_v[...], matrix(up_v, t)) + vector(UP_BIAS, t * WIDTH, WIDTH)
                for k in HALVES:
                    pre_v[CORES * t + k] = pre[:, k * TILE:(k + 1) * TILE]
                act = (0.5 * pre * (1.0 + lax.erf(pre * INV_SQRT2))).astype(BF16)
                act_t[cols, :] = act.T
                start(quarter(layer, t))
                load(DOWN, t).wait()
                acc[...] += dot(act, down_v[t].reshape((WIDTH, WIDTH)))

                @pl.when((layer == A) & (t == B))
                def _():
                    gather.end(B, C, (B,))

        h_save.wait()
        y_v[...] = acc[...].astype(BF16)
        with jax.named_scope('fend'):
            meanwhile(lambda: gather.end(B, C, (C,)))

    with jax.named_scope('ftail'):
        last = pltpu.make_async_copy(y_v, y_hbm, next(own_sem))
        last.start()
        for stage in range(AXES):
            for step in range(AXES):
                small_reach(stage, step).wait_send()
        small_pass.wait_send()
        gather.left()
        settle(LAYERS - 1)
        last.wait()


def forward(x, y_cot, shards, small_tile, tables, places):
    grid = CHIPS + (CORES,)
    full = [(LAYERS,) + grid + tensor.shape[1:] for tensor in shards]
    shapes = [(shape, BF16) for shape in full] + [(grid + small_tile.shape, BF16), ((LAYERS, N_VEC), F32), ((LAYERS, CORES, SEQ, TILE), BF16), ((SEQ, WIDTH), BF16),
                                                  ((LAYERS, SEQ, WIDTH), BF16)]
    shapes += [((LAYERS, CORES, width, SEQ), BF16) for width in (WIDTH, WIDTH, WIDTH, HIDDEN)]
    shapes += [((LAYERS, SEQ, QKV), BF16), ((LAYERS, N_TILES, SEQ, TILE), F32)]
    dma = pltpu.SemaphoreType.DMA
    slots = AXES * AXES
    scratch = [pltpu.VMEM(shape[1:], BF16) for shape in full] + [pltpu.VMEM(grid + small_tile.shape, BF16)]
    scratch += [pltpu.VMEM((SEQ, WIDTH), F32), pltpu.VMEM((N_TILES, SEQ, TILE), F32)]
    scratch += [pltpu.VMEM((SEQ, width), BF16) for width in (WIDTH, WIDTH, QKV, WIDTH, WIDTH)]
    scratch += [pltpu.VMEM((width, SEQ), BF16) for width in (WIDTH, WIDTH, WIDTH, HIDDEN)]
    scratch += [dma(shape) for shape in ((LAYERS, AXES, AXES), (LAYERS, AXES, len(HALVES), slots), (LAYERS, AXES), (LAYERS, AXES))]
    scratch += [dma(shape) for shape in ((slots + 1,), (slots + 1,), (slots + SIDE + SIDE + AXES,), (AXES, SIDE), (SIDE + 1,), (LAYERS, AXES), (LAYERS, AXES), (CORES, SIDE), (LAYERS, SIDE), (LAYERS, SIDE))]
    scratch += [pltpu.VMEM(tables.shape, F32), pltpu.VMEM(places.shape, jnp.int32)]
    out_specs = [IN_VMEM if dtype == F32 and len(shape) == LAYERS else ANY for shape, dtype in shapes]
    return pl.pallas_call(
        forward_kernel,
        out_shape=[jax.ShapeDtypeStruct(*s) for s in shapes],
        in_specs=[ANY] * SIDE + [IN_VMEM] * SIDE,
        out_specs=out_specs,
        scratch_shapes=scratch,
        compiler_params=pltpu.CompilerParams(collective_id=0, has_side_effects=True, vmem_limit_bytes=VMEM_LIMIT),
        name='forward_layers',
    )(x, y_cot, tables, places, *shards, small_tile)


WAVES = ((384, 384, 512), (384, 384, 256), (256, 256, 256))
LEADS = ((2,) + CHIPS[1:], CHIPS[1:], (2, SIDE), (SIDE,), (AXES,))
W_UP, W_DOWN, W_QKV, W_OUT = range(4)
STEPS = ((1, (2,)), (0, ()), (2, (4, 3)), (4, (5,)), (3, ()), (5, (6, 7, 8)), (8, (9,)), (9, ()))
LAST = AXES * AXES
CARRIED = ((0, 3, 2), (1, 1, 14), (2, 0, 0))
US_COLUMN, US_HOP, US_ADD, US_STEP = 0.022, 2.5, 0.0007, 0.2
US_FIRST, US_OUT, US_TILE, US_GRADIENT, US_PAIR, US_NORM = 2, 1.4, 1.6, 0.0025, 3.6, 2.7


class Schedule:
    def __init__(self):
        self.now, self.free, self.lines = 0.0, {}, []

    def send(self, link, columns):
        self.free[link] = max(self.free.get(link, 0.0), self.now) + columns * US_COLUMN
        return self.free[link] + US_HOP

    def due(self, limit):
        found = []
        while self.lines:
            line = min(self.lines, key=lambda one: one[A][A]())
            ready = line[A][A]()
            if limit is not None and ready > limit:
                break
            _, run, sends, cost = line.pop(A)
            self.lines = [one for one in self.lines if one]
            self.now = max(self.now, ready) + cost
            sends()
            found.append(run)
        return found

    def finish(self, line):
        while line:
            ready, run, sends, cost = line.pop(A)
            self.now = max(self.now, ready()) + cost
            sends()
            run()
        self.lines = [one for one in self.lines if one]

    def run(self, limit):
        for step in self.due(limit):
            step()

    def passed(self, cost):
        self.now += cost
        self.run(self.now)

    def hooks(self, count, cost):
        planned = []
        for _ in range(count):
            self.now += cost
            planned.append(self.due(self.now))
        return planned


def at_hooks(n, planned):
    for when, steps in enumerate(planned):
        if steps:
            @pl.when(n == when)
            def _():
                for step in steps:
                    step()


def add_into(dst, src, n_axes):
    if n_axes < 2:
        dst[...] += src[...]
        return

    @loop(SIDE)
    def _(k):
        dst[k] += src[k]


def at_axis(ref, axis, value, n_axes):
    every = [pl.ds(0, SIDE)] * n_axes
    every[axis] = value
    return ref.at[tuple(every)]


class Reduce:
    def __init__(self, chip, schedule, wave, grads, came, fin, sems, spare, write, done, when=None):
        self.wave, self.chip, self.schedule, self.widths, self.grads = wave, chip, schedule, WAVES[wave], grads
        self.came, self.fin, (self.send_sem, self.recv_sem), (self.spare, self.spare_sem) = came, fin, sems, spare
        self.write, self.done, self.when, self.times = write, done, when, {}

    def box(self, a, half, stage):
        order = ORDERS[a]
        ref = self.came[a][A].at[half, A]
        spot = [axis for axis in range(AXES) if axis != order[A]].index(order[B])
        if stage == B:
            return ref, spot, C
        return at_axis(ref, spot, self.chip.where[order[B]], C), A, B

    def copy(self, a, half, slot):
        stage, turn = divmod(slot, AXES)
        sems = self.send_sem.at[a, stage], self.recv_sem.at[a, half, slot]
        if slot == LAST:
            return remote(self.total(a, half).at[self.chip.other], self.fin[a].at[half], *sems, self.chip.partner())
        axis = ORDERS[a][stage]
        if stage == C:
            role = value = ROLES[turn]
            dst = self.came[a][SIDE].at[half, turn]
        else:
            role, value = TWO if turn == C else ONE, (ONE, CROSS, TWO)[turn]
            dst = self.came[a][CORES * stage + turn // C].at[half]
            dst = dst if turn == C else dst.at[turn]
        value = self.chip.at(axis, value, half)
        if stage:
            ref, spot, n_axes = self.box(a, half, stage)
            src = at_axis(ref, spot, value, n_axes)
        else:
            src = self.came[a][A].at[half, B] if turn == C else at_axis(self.grads[a].at[half], axis, value, AXES)
        return remote(src, dst, *sems, self.chip.device(axis, role, half))

    def each(self, action):
        for a in range(AXES):
            halves(lambda half: action(a, half))

    def sending(self, slot):
        stage = slot // AXES
        share = SIDE ** (CORES * stage)
        self.times[slot] = self.schedule.now + US_HOP if slot == LAST else max(
            self.schedule.send(ORDERS[a][stage], self.widths[a] / share) for a in range(AXES))

    def begin(self):
        for slot in (B, A):
            self.each(lambda a, half: self.copy(a, half, slot).start())

    def plan(self, first=0, last=None, late=0):
        for slot in (B, A):
            self.times[slot] = self.schedule.now + late
            if not first:
                self.sending(slot)
        for _, sent in STEPS[:first]:
            self.times.update((slot, self.schedule.now + late + US_HOP) for slot in sent)
        line = [
            (lambda slot=slot: self.times[slot], lambda k=k: self.step(k), lambda sent=sent: [self.sending(n) for n in sent],
             CORES * US_ADD * sum(self.widths) if k < C else US_STEP) for k, (slot, sent) in enumerate(STEPS)][first:last]
        self.schedule.lines.append(line)
        return line

    def step(self, k):
        def work():
            with jax.named_scope(f'w{self.wave}s{k}'):
                (self.first, self.first, self.halve, self.settle, self.settle, self.spread, self.cross, self.finish)[k](STEPS[k][A])
        if self.when is None:
            work()
        else:
            pl.when(self.when)(work)

    def held(self, a, half):
        ref = self.spare[A].at[a] if a < C else self.spare[B]
        return ref.at[half, :, :, :, :, pl.ds(0, self.widths[a])]

    def first(self, slot):
        def local(a, half):
            axis = ORDERS[a][A]
            return pltpu.make_async_copy(at_axis(self.grads[a].at[half], axis, self.chip.at(axis, TWO if slot else OWN, half), AXES),
                                         self.held(a, half), self.spare_sem.at[a, half])

        def action(a, half):
            local(a, half).wait()
            self.copy(a, half, slot).wait_recv()
            add_into(self.came[a][A].at[half, slot], self.held(a, half), C)
            if slot:
                self.copy(a, half, C).start()

        self.each(lambda a, half: local(a, half).start())
        self.each(action)

    def halve(self, slot):
        def action(a, half):
            ref, spot, n_axes = self.box(a, half, B)
            self.copy(a, half, slot).wait_recv()
            for turn, role in ((B, CROSS), (A, ONE), (C, TWO), (C, OWN)):
                value = self.chip.at(ORDERS[a][B], role, half)
                add_into(at_axis(ref, spot, value, n_axes), at_axis(self.came[a][B].at[half], spot, value, n_axes), B)
                if turn < C:
                    self.copy(a, half, AXES + turn).start()
        self.each(action)

    def settle(self, slot):
        def action(a, half):
            ref, spot, n_axes = self.box(a, half, B)
            self.copy(a, half, slot).wait_recv()
            value = self.chip.at(ORDERS[a][B], TWO if slot > AXES else OWN, half)
            add_into(at_axis(ref, spot, value, n_axes), self.came[a][C].at[half, slot - AXES], B)
            if slot > AXES:
                self.copy(a, half, AXES + C).start()
        self.each(action)

    def spread(self, slot):
        def action(a, half):
            ref, *_ = self.box(a, half, C)
            self.copy(a, half, slot).wait_recv()
            add_into(ref, self.came[a][AXES].at[half], B)
            for turn in range(AXES):
                self.copy(a, half, CORES * AXES + turn).start()
        self.each(action)

    def total(self, a, half):
        ref, *_ = self.box(a, half, C)
        return ref.at[self.chip.where[ORDERS[a][C]]]

    def cross(self, _):
        def action(a, half):
            for turn in range(AXES):
                self.copy(a, half, CORES * AXES + turn).wait_recv()
            self.total(a, half)[...] += total_of([self.came[a][SIDE][half, turn] for turn in range(AXES)])
            self.copy(a, half, LAST).start()
        self.each(action)

    def finish(self, _):
        def action(a, half):
            self.write(a, half, self.chip.core, self.total(a, half)[self.chip.core])
            self.copy(a, half, LAST).wait_recv()
            self.write(a, half, self.chip.other, self.fin[a][half])
        self.each(action)
        three = pl.ds(0, AXES)
        for a, (grad, fin) in enumerate(zip(self.grads, self.fin)):
            for stage, block in enumerate((grad.at[:, :, :, three], grad.at[:, :, three, A], grad.at[:, three, A, A], fin)):
                sem = self.send_sem.at[a, stage]
                remote(block, block, sem, sem, self.chip.partner()).wait_send()
        self.done()


class VectorSum:
    def __init__(self, chip, schedule, total, came, sems, finish, when=None):
        self.schedule, self.total, self.came, self.sems, self.finish, self.when, self.ready = schedule, total, came, sems, finish, when, 0.0
        self.devices = [[chip.device(axis, role, A) for role in ROLES] for axis in range(AXES)] + [[chip.partner()]]

    def copies(self, k):
        return [remote(self.total, self.came.at[AXES * k + n], self.sems.at[A, AXES * k + n], self.sems.at[B, AXES * k + n], device)
                for n, device in enumerate(self.devices[k])]

    def sending(self, k):
        if k < SIDE:
            self.ready = self.schedule.send(k, N_VEC / (SIDE * SIDE * ROWS))

    def step(self, k):
        def work():
            with jax.named_scope(f'vec{k}'):
                wait(self.copies(k - 1))
                for n in range(len(self.devices[k - 1])):
                    self.total[...] += self.came[AXES * (k - 1) + n]
            if k < SIDE:
                start(self.copies(k))
            else:
                self.finish()
        if self.when is None:
            work()
        else:
            pl.when(self.when)(work)

    def begin(self):
        start(self.copies(A))

    def plan(self):
        self.sending(A)
        self.schedule.lines.append([
            (lambda: self.ready, lambda k=k: self.step(k), lambda k=k: self.sending(k), US_STEP) for k in range(1, SIDE + 1)])


def backward_kernel(ycot_hbm, tables, vec_ref, places, up_hbm, down_hbm, mix_hbm, h_hbm, n1_hbm, n2_hbm, ctx_hbm,
                    act_hbm, qkv_hbm, pre_hbm, _, dx_hbm, small_ref, up_sum, down_sum, qkv_sum, out_sum, dout_cols, dpre_cols,
                    dqkv_cols, *refs):
    n_arrays, sums = AXES * len(WAVES), (up_sum, down_sum, qkv_sum, out_sum)
    grads, refs = refs[:n_arrays], refs[n_arrays:]
    (spare, spare_wide, tile_v, big_v, rhs_v, wup_v, wdown_v, pre_v, dn1, dn2, dctx, dk_acc, dv_acc, qkv_v, dpre_v, dqkv_v, dh_v, h_v,
     totals, came_vec, send_sem, recv_sem, spare_sem, tile_sem, big_sem, rhs_sem, mlp_sem, io_sem, own_sem, share_send,
     share_recv, pre_sem, vec_sem, credit, *refs) = refs
    fins, came = refs[:n_arrays], refs[n_arrays:]
    first_in = pltpu.make_async_copy(ycot_hbm, dh_v, io_sem.at[A])
    first_in.start()
    chip = Chip()
    core, other = chip.core, chip.other

    def exchange(layer, k, src, dst):
        return half_copies(chip, src, dst.at[layer], own_sem.at[k], share_send.at[k], share_recv.at[k])

    def tokens_load(layer, src, part, slot):
        return [pltpu.make_async_copy(src.at[layer, k, pl.ds(part * WIDTH, WIDTH)], big_v.at[slot, :, pl.ds(k * SEQ, SEQ)],
                                      big_sem.at[slot, k]) for k in range(CORES)]

    def weight_load(layer, k, slot):
        return pltpu.make_async_copy(mix_hbm.at[layer, :, lanes(k * WIDTH, WIDTH)], big_v.at[slot], big_sem.at[slot, CORES])

    def tile_loads(layer, t, slot):
        rows = lanes(t * TILE, TILE)
        pairs = ((down_hbm.at[layer, rows], wdown_v), (pre_hbm.at[layer, t], pre_v), (up_hbm.at[layer, :, rows], wup_v))
        return [pltpu.make_async_copy(src, dst.at[slot], mlp_sem.at[slot, n]) for n, (src, dst) in enumerate(pairs)]

    def input_loads(layer):
        return [pltpu.make_async_copy(qkv_hbm.at[layer], qkv_v, io_sem.at[B]), pltpu.make_async_copy(h_hbm.at[layer], h_v, io_sem.at[C])]

    def rhs_load(layer, src, first, width, k):
        cols = lanes(first, width)
        return [pltpu.make_async_copy(src.at[layer, n, :, cols], rhs_v.at[pl.ds(n * SEQ, SEQ), cols], rhs_sem.at[k, n])
                for n in range(CORES)]

    def prefetch(layer):
        start(tokens_load(layer, ctx_hbm, A, AXES) + tokens_load(layer, act_hbm, A, A))

    def prefetch_more(layer):
        start(tokens_load(layer, act_hbm, B, B) + tokens_load(layer, act_hbm, C, C) + input_loads(layer))
        for t in HALVES:
            start(tile_loads(layer, t, t))

    prefetch(LAYERS - 1)
    start(rhs_load(LAYERS - 1, dout_cols, A, TILE, A))
    with jax.named_scope('enter'):
        enter(chip)
    with jax.named_scope('first_in'):
        first_in.wait()
    dx_copy = pltpu.make_async_copy(dh_v, dx_hbm, io_sem.at[A])
    prefetch_more(LAYERS - 1)

    def vector_at(k, first=0, width=None):
        return lanes(OFFSETS[k] + first, width or SIZES[k])

    def reduction(schedule, layer, wave, when):
        def write(a, half, side, block):
            def put(arr, group, col, first, width):
                size = sums[arr].shape[-1] // CORES
                sums[arr][layer, group, :, lanes(side * size + col, width)] = block[:, first:first + width].astype(BF16)
            width, colour = WAVES[wave][a], CORES * a + half
            if wave:
                first = colour * width if wave == C or a < C else SIDE * WAVES[wave][A] + half * width
                put(W_QKV if wave == C else W_UP, A, first, A, width)
            elif a < C:
                put(W_DOWN, colour, A, A, width)
            else:
                for k in HALVES:
                    put(W_DOWN, CORES * half + k, WAVES[A][A], k * PAIR, PAIR)
                put(W_OUT, A, half * TWICE, TWICE, TWICE)

        def done():
            @pl.when(layer == LAYERS - 1)
            def _():
                chip.signal_partners(credit.at[wave])

        where = slice(AXES * wave, AXES * (wave + 1))
        count = len(LEADS)
        return Reduce(chip, schedule, wave, [grad.at[layer] for grad in grads[where]],
                      [came[count * (AXES * wave + a):count * (AXES * wave + a + 1)] for a in range(AXES)],
                      fins[where], (send_sem.at[wave], recv_sem.at[wave]), ((spare, spare_wide), spare_sem), write, done, when)

    def vector_sum(schedule, layer, when):
        def own_part():
            with jax.named_scope('own'):
                node, local = chip.base
                me = node * (SIDE * CORES) + local + core
                row = jnp.zeros((ROWS, PAIR), F32)
                for k, share in enumerate(SHARES):
                    if k == QKV_BIAS:
                        firsts = [part * WIDTH + lax.div(me, CORES * ROWS) * PAIR for part in range(PARTS)]
                    else:
                        firsts = [lax.div(me * share, PAIR) * PAIR]
                    for first in firsts:
                        cols = lanes(OFFSETS[k] + first)
                        left = jnp.zeros((ROWS, PAIR), F32) + totals[layer, :, cols] * (places[A:B, cols] == me).astype(F32)
                        pick = (iota((PAIR, PAIR), 0) == places[B:C, cols]).astype(F32).astype(BF16)
                        for _ in range(PARTS):
                            row = row + dot_t(left.astype(BF16), pick)
                            left = left - rounded(left)
                small_ref[layer] = row.astype(BF16)

            @pl.when(layer == LAYERS - 1)
            def _():
                chip.signal_partners(credit.at[AXES])

        return VectorSum(chip, schedule, totals.at[layer], came_vec, vec_sem, own_part, when)

    def run_on(schedule, layer, when):
        lines = [reduction(schedule, layer, wave, when).plan(step, late=late) for wave, step, late in CARRIED]
        vector_sum(schedule, layer, when).plan()
        return lines

    @loop(LAYERS + 1)
    def _(turn_no):
        layer = LAYERS - 1 - turn_no
        working = pl.when(turn_no < LAYERS)
        total = totals.at[layer]
        schedule = Schedule()

        carried = run_on(schedule, layer + 1, turn_no > A)

        def product(lhs_slot, first, width, out_slot):
            value = dot(big_v[lhs_slot, :, 0:CORES * SEQ], rhs_v[:, lanes(first, width)])
            tile_v[out_slot, :, :, :, :, :, 0:width] = value.reshape(CHIPS + (CORES, ROWS, width))

        def tile_out(slot, src, dst):
            return pltpu.make_async_copy(src, dst, tile_sem.at[slot])

        def tile_done(slot, width):
            block = tile_v.at[slot, :, :, :, :, :, pl.ds(0, width)]
            tile_out(slot, block, block).wait()

        def columns(wave, a, half, first, width):
            return grads[AXES * wave + a].at[layer, half, :, :, :, :, :, pl.ds(first, width)]

        def launch(wave):
            schedule.finish(carried[wave])

            @pl.when(turn_no == B)
            def _():
                pl.semaphore_wait(credit.at[wave], PARTNERS)

            current = reduction(schedule, layer, wave, turn_no < LAYERS)
            if wave == C:
                @pl.when(turn_no == B)
                def _():
                    pl.semaphore_wait(credit.at[AXES], PARTNERS)

                @working
                def _():
                    vector_sum(schedule, layer, None).begin()

            working(current.begin)
            if wave < C:
                current.plan(last=CARRIED[wave][B])

        @working
        def _():
            with jax.named_scope('dw_out'):
                @pl.when(turn_no == B)
                def _():
                    wait(exchange(layer, A, dh_v, dout_cols))
                    start(rhs_load(layer, dout_cols, A, TILE, A))

                wait(rhs_load(layer, dout_cols, A, TILE, A))
                wait(tokens_load(layer, ctx_hbm, A, AXES))
                product(AXES, A, TILE, B)
                start(tokens_load(layer, act_hbm, AXES, AXES))
                for k in HALVES:
                    tile_out(B, tile_v.at[B, :, :, :, :, :, pl.ds(k * TWICE, TWICE)], columns(A, C, k, TWICE, TWICE)).start()

        schedule.passed(US_FIRST)
        out_hooks = schedule.hooks(SIDE, US_OUT)

        @loop(SIDE)
        def _(z):
            @working
            def _():
                slot = parity(z)
                wait(tokens_load(layer, act_hbm, z, z))

                @pl.when(z > A)
                def _():
                    tile_done(slot, TILE)

                product(z, A, TILE, slot)
                split = WAVES[A][A]
                for k in range(SIDE):
                    a, half = divmod(k, CORES)
                    for c in range(CORES):
                        block = tile_v.at[slot, :, :, CORES * c + a, half]
                        tile_out(slot, block.at[:, :, :, pl.ds(0, split)], grads[a].at[layer, half, z, :, :, c]).start()
                        tile_out(slot, block.at[:, :, :, pl.ds(split, PAIR)],
                                 grads[C].at[layer, a, z, :, :, c, :, pl.ds(half * PAIR, PAIR)]).start()

            at_hooks(z, out_hooks)

        @working
        def _():
            start(tokens_load(layer, n2_hbm, A, A) + [weight_load(layer, k, k + 1) for k in range(PARTS)])
            for slot in HALVES:
                tile_done(slot, TILE)

        schedule.passed(US_STEP)
        launch(A)

        @working
        def _():
            dn2[...] = jnp.zeros_like(dn2)

        def pre_copy(t, slot, away):
            place = dpre_cols.at[layer, core, :, lanes(lax.rem(t, SIDE) * TILE, TILE)]
            if away:
                return remote(dpre_v.at[slot], place, pre_sem.at[A, t], pre_sem.at[B, t], chip.partner())
            return pltpu.make_async_copy(dpre_v.at[slot], place, own_sem.at[CORES + slot])

        def pre_act(t, leave):
            for away, whose in ((False, core), (True, other)):
                @pl.when(lax.div(t, SIDE) == whose)
                def _():
                    copy = pre_copy(t, parity(t), away)
                    if leave:
                        copy.start()
                    elif away:
                        copy.wait_send()
                    else:
                        copy.wait()

        tile_hooks = schedule.hooks(N_TILES, US_TILE)

        with jax.named_scope('mlp'):
            @loop(N_TILES)
            def _(t):
                @working
                def _():
                    slot = parity(t)
                    wait(tile_loads(layer, t, slot))
                    d_act = rounded(dot_t(dh_v[...], wdown_v[slot]))
                    pre = pre_v[slot]
                    slope = 0.5 * (1.0 + lax.erf(pre * INV_SQRT2)) + pre * (INV_SQRT2PI * jnp.exp(-0.5 * pre * pre))
                    d_pre = d_act * slope
                    total[:, vector_at(UP_BIAS, t * TILE, TILE)] = column_sum(d_pre)

                    @pl.when(t > B)
                    def _():
                        pre_act(t - CORES, False)

                    dpre_v[slot] = d_pre.astype(BF16)
                    pre_act(t, True)
                    dn2[...] += dot_t(dpre_v[slot], wup_v[slot])

                    @pl.when(t + CORES < N_TILES)
                    def _():
                        start(tile_loads(layer, t + CORES, slot))

                at_hooks(t, tile_hooks)

        @working
        def _():
            for t in HALVES:
                pre_act(N_TILES - CORES + t, False)
            for t in range(SIDE):
                pre_copy(SIDE * core + t, A, True).wait_recv()

        def gradient_loads(wave, source):
            first = 0
            for a in range(AXES):
                width = CORES * WAVES[wave][a]
                start(rhs_load(layer, source, first, width, a))
                first += width

        def gradient_wave(wave, source, lhs_slot, first, orders):
            split, count = WAVES[wave][orders[A]], len(orders)
            width = CORES * split
            planned = schedule.hooks(count, width * US_GRADIENT)

            @loop(count)
            def _(n):
                @working
                def _():
                    slot = parity(n)
                    wait(rhs_load(layer, source, first + n * width, width, orders[A] + n))

                    @pl.when(n > B)
                    def _():
                        tile_done(slot, width)

                    product(lhs_slot, first + n * width, width, slot)
                    for k, a in enumerate(orders):
                        @pl.when(n == k)
                        def _():
                            for half in HALVES:
                                block = tile_v.at[slot, :, :, :, :, :, pl.ds(half * split, split)]
                                tile_out(slot, block, columns(wave, a, half, 0, split)).start()

                at_hooks(n, planned)

            @working
            def _():
                for slot in range(min(count, CORES)):
                    tile_done(slot, width)

        @working
        def _():
            gradient_loads(B, dpre_cols)
            wait(tokens_load(layer, n2_hbm, A, A))

        with jax.named_scope('dw1'):
            gradient_wave(B, dpre_cols, A, A, (A, B))
            gradient_wave(B, dpre_cols, A, SIDE * WAVES[B][A], (C,))
        launch(B)
        @working
        def _():
            weight_load(layer, AXES, A).start()
            d_sum = column_sum(dh_v[...].astype(F32))
            total[:, vector_at(OUT_BIAS)] = d_sum
            total[:, vector_at(DOWN_BIAS)] = d_sum
            wait(input_loads(layer))
            weight_load(layer, AXES, A).wait()
            dctx[...] = dot_t(dh_v[...], big_v[A]).astype(BF16)

        pair_hooks = schedule.hooks(N_PAIRS // CORES, US_PAIR)

        with jax.named_scope('attn'):
            def one_pair(pair, dk_sum, dv_sum):
                at = lanes(pair * PAIR)
                keys = split_heads(qkv_v[:, lanes(WIDTH + pair * PAIR)])
                values = split_heads(qkv_v[:, lanes(C * WIDTH + pair * PAIR)])
                q_t = qkv_v[:, at].T
                dc_t = dctx[:, at].T
                bias_sums = [jnp.zeros((1, PAIR), F32)] * PARTS

                def turned_back(n, d, rows, to):
                    d = turn_back(rounded(d), *[tables[k, rows, :] for k in range(PARTS)])
                    bias_sums[n] = bias_sums[n] + column_sum(d)
                    dqkv_v[rows, to] = d.astype(BF16)

                for i in range(N_BLOCKS):
                    old, n = i * TWICE, (i + 1) * TWICE
                    rows = block_rows(i)
                    probs = probabilities(qkv_v[rows, at], keys[:n], i)
                    d_all = rounded(dot_t(dctx[rows, at], values[:n]))
                    d_scores = [d_all[:, block_rows(j)] for j in range(CORES * (i + 1))]
                    for head in HALVES:
                        mine = slice(head, None, CORES)
                        mean = row_sum(total_of([p * d for p, d in zip(probs[mine], d_scores[mine])]))
                        d_scores[mine] = [p * (d - mean) * SCALE for p, d in zip(probs[mine], d_scores[mine])]
                    d_scores, probs = side_by_side(d_scores), side_by_side(probs)
                    turned_back(A, dot(d_scores, keys[:n]), rows, at)
                    for acc, left, right in ((dk_sum, q_t, d_scores), (dv_sum, dc_t, probs)):
                        part = dot(left[:, rows], right)
                        if i:
                            acc[:, :old] += part[:, :old]
                        acc[:, old:n] = part[:, old:]
                first = iota((PAIR, PAIR), 0) < HEAD
                for j in range(N_BLOCKS):
                    rows = block_rows(j)
                    d_key, d_value = [jnp.where(first, acc[:, block_rows(CORES * j)], acc[:, block_rows(CORES * j + 1)]).T
                                      for acc in (dk_sum, dv_sum)]
                    turned_back(B, d_key, rows, lanes(WIDTH + pair * PAIR))
                    d_value = d_value.astype(BF16)
                    bias_sums[C] = bias_sums[C] + column_sum(d_value.astype(F32))
                    dqkv_v[rows, lanes(C * WIDTH + pair * PAIR)] = d_value
                for k, bias_sum in enumerate(bias_sums):
                    total[:, vector_at(QKV_BIAS, k * WIDTH + pair * PAIR, PAIR)] = bias_sum

            @loop(N_PAIRS // CORES)
            def _(two):
                @working
                def _():
                    for k in HALVES:
                        one_pair(CORES * two + k, dk_acc.at[k], dv_acc.at[k])

                at_hooks(two, pair_hooks)

        @working
        def _():
            start(exchange(layer, B, dqkv_v, dqkv_cols))
            dn1[...] = jnp.zeros_like(dn1)

            with jax.named_scope('dn1'):
                @loop(PARTS)
                def _(k):
                    weight_load(layer, k, k + 1).wait()
                    dn1[...] += dot_t(dqkv_v[:, lanes(k * WIDTH, WIDTH)], big_v[k + 1])

            start(tokens_load(layer, n1_hbm, A, B))

        schedule.passed(US_NORM)

        @working
        def _():
            for k in (GAIN1, BIAS1, GAIN2, BIAS2):
                total[:, vector_at(k)] = jnp.zeros((1, WIDTH), F32)

            with jax.named_scope('lnb'):
                @loop(SEQ // LN_ROWS)
                def _(r):
                    rows = pl.ds(pl.multiple_of(r * LN_ROWS, LN_ROWS), LN_ROWS)
                    scaled, inverse = normalised(h_v[rows, :].astype(F32))
                    d1, d2 = rounded(dn1[rows, :]), rounded(dn2[rows, :])
                    for k, value in ((GAIN1, d1 * scaled), (BIAS1, d1), (GAIN2, d2 * scaled), (BIAS2, d2)):
                        total[:, vector_at(k)] += column_sum(value)
                    g1, g2 = [vec_ref[pl.ds(layer, 1), lanes(OFFSETS[k], WIDTH)] for k in (GAIN1, GAIN2)]
                    d_scaled = d1 * g1 + d2 * g2
                    d_h = inverse * (d_scaled - row_mean(d_scaled) - scaled * row_mean(d_scaled * scaled))
                    dh_v[rows, :] = (dh_v[rows, :].astype(F32) + d_h).astype(BF16)

        schedule.passed(US_NORM)
        @working
        def _():
            wait(exchange(layer, B, dqkv_v, dqkv_cols))
            gradient_loads(C, dqkv_cols)
            wait(tokens_load(layer, n1_hbm, A, B))

        @pl.when(turn_no == A)
        def _():
            start(exchange(layer - 1, A, dh_v, dout_cols))

        @pl.when(turn_no == B)
        def _():
            dx_copy.start()

        with jax.named_scope('dw2'):
            gradient_wave(C, dqkv_cols, B, A, (A, B, C))

        @pl.when(turn_no == A)
        def _():
            prefetch(layer - 1)
            prefetch_more(layer - 1)

        schedule.run(None)
        launch(C)

    dx_copy.wait()


def backward(y_cot, tables, vectors, places, weights, saved):
    dma, one = pltpu.SemaphoreType.DMA, (1,)
    pair, wide, row = (len(HALVES),), (SEQ, WIDTH), one + (N_VEC,)
    shapes = [(wide, BF16), ((LAYERS, ROWS, PAIR), BF16)]
    shapes += [((LAYERS, groups, ROWS, width), BF16) for groups, width in ((*one, HIDDEN), (SIDE, WIDTH), (*one, QKV), (*one, WIDTH))]
    in_vmem = len(shapes)
    shapes += [((LAYERS, CORES, SEQ, width), BF16) for width in (TILE, SIDE * TILE, PARTS * TILE)]
    blocks = [(CORES, ROWS, width) for wave in WAVES for width in wave]
    shapes += [((LAYERS,) + pair + CHIPS + block, F32) for block in blocks]
    tile = (CORES, ROWS)
    scratch = [(pair + pair + CHIPS[1:] + tile + (WAVES[0][0],), F32), (pair + CHIPS[1:] + tile + (TILE,), F32), (pair + CHIPS + tile + (CORES * WAVES[0][0],), F32), ((SIDE, WIDTH, WIDTH), BF16), ((CORES * SEQ, SIDE * TILE), BF16)]
    scratch += [(pair + shape, BF16) for shape in ((WIDTH, TILE), (TILE, WIDTH))]
    scratch += [(pair + (SEQ, TILE), F32), (wide, F32), (wide, F32), (wide, BF16)] + [(pair + (PAIR, CORES * SEQ), F32)] * CORES
    scratch += [((SEQ, QKV), BF16), (pair + (SEQ, TILE), BF16), ((SEQ, QKV), BF16), (wide, BF16), (wide, BF16), ((LAYERS,) + row, F32),
                ((PARTNERS,) + row, F32)]
    slots = (len(WAVES), AXES) + pair + (LAST + 1,)
    sems = [dma(shape) for shape in ((len(WAVES), AXES, SIDE), slots, (AXES,) + pair, pair, (SIDE, AXES), (AXES, CORES), pair + (PARTS,), (AXES,),
                                     (SIDE,), pair, pair, pair + (N_TILES,), pair + (PARTNERS,))]
    late = [(pair + block[1:], F32) for block in blocks] + [(pair + lead + block, F32) for block in blocks for lead in LEADS]
    outs = pl.pallas_call(
        backward_kernel,
        out_shape=[jax.ShapeDtypeStruct(*s) for s in shapes],
        in_specs=[ANY] + [IN_VMEM] * AXES + [ANY] * (PARTNERS + 1),
        input_output_aliases={SIDE + PARTNERS: in_vmem},
        out_specs=[ANY] + [IN_VMEM] * (in_vmem - 1) + [ANY] * (len(shapes) - in_vmem),
        scratch_shapes=[pltpu.VMEM(*s) for s in scratch] + sems + [pltpu.SemaphoreType.REGULAR((SIDE,))]
        + [pltpu.VMEM(*s) for s in late],
        compiler_params=pltpu.CompilerParams(collective_id=1, has_side_effects=True, vmem_limit_bytes=VMEM_LIMIT),
        name='backward_layers',
    )(y_cot, tables, vectors, places, *weights, *saved)
    d_x, small, *sums = outs[:in_vmem]
    return d_x, small[:, 0], [s.reshape((LAYERS, -1, s.shape[-1])) for s in sums]


def finish_kernel(*refs):
    n_large = CORES + AXES
    large, small_ref, refs = refs[:n_large], refs[n_large], refs[n_large + 1:]
    outs, small_outs, refs = refs[:n_large], refs[n_large:n_large + len(SHARES)], refs[n_large + len(SHARES):]
    held, sems = refs[:n_large], refs[n_large]
    loads = start([pltpu.make_async_copy(src, dst, sems.at[n]) for n, (src, dst) in enumerate(zip(large, held))])
    first = 0
    for share, out in zip(SHARES, small_outs):
        out[...] = small_ref[:, first:first + share]
        first += share
    stores = []
    for load, src, dst in zip(loads, held, outs):
        load.wait()
        stores += start([pltpu.make_async_copy(src, dst, sems.at[n_large + len(stores)])])
    wait(stores)


def finish(large, small):
    shapes = [jax.ShapeDtypeStruct(t.shape, BF16) for t in large] + [jax.ShapeDtypeStruct((LAYERS, share), BF16) for share in SHARES]
    outs = pl.pallas_call(
        finish_kernel,
        out_shape=shapes,
        in_specs=[ANY] * len(large) + [IN_VMEM],
        out_specs=[ANY] * len(large) + [IN_VMEM] * len(SHARES),
        scratch_shapes=[pltpu.VMEM(t.shape, BF16) for t in large] + [pltpu.SemaphoreType.DMA((CORES * len(large),))],
        name='finish',
    )(*large, small)
    return outs[:len(large)], outs[len(large):]


def rope_tables():
    rot_dim, f32 = HEAD // SIDE, np.float32
    inv_freq = f32(1.0) / f32(10000.0) ** (np.arange(0, rot_dim, 2, dtype=f32) / f32(rot_dim))
    angles = np.arange(SEQ, dtype=f32)[:, None] * inv_freq[None, :]
    cos, sin = np.cos(angles), np.sin(angles)
    zero = np.zeros_like(sin)
    rest = np.zeros((SEQ, HEAD - rot_dim), f32)
    tables = ([cos, cos, rest + f32(1.0)], [-sin, zero, rest], [zero, sin, rest])
    return jnp.asarray(np.stack([np.tile(np.concatenate(table, axis=1), (1, 2)) for table in tables]).astype(f32))


def heads_last(tensor):
    lead = tensor.shape[:-2]
    return tensor.reshape(lead + (HEADS, PARTS, HEAD)).swapaxes(-3, -2).reshape(lead + (QKV,))


def heads_first(tensor):
    lead = tensor.shape[:-1]
    return tensor.reshape(lead + (PARTS, HEADS, HEAD)).swapaxes(-3, -2).reshape(lead + (HEADS, PARTS * HEAD))


def vector_places():
    shard, lane, first = [], [], 0
    for k, (share, size) in enumerate(zip(SHARES, SIZES)):
        place = np.arange(size)
        if k == QKV_BIAS:
            place = heads_last(place.reshape(HEADS, -1))
        shard.append(place // share)
        lane.append(first + place % share)
        first += share
    return jnp.asarray(np.stack([np.concatenate(shard), np.concatenate(lane)]).astype(np.int32))


def solution(mesh):
    shard_axes = ('node', 'local')
    act_spec = P(shard_axes)
    param_spec = P(None, shard_axes)

    def device_step(x, y_cot, ln1_gain, ln1_bias, qkv_weight, qkv_bias, out_weight, out_bias,
                    ln2_gain, ln2_bias, up_weight, up_bias, down_weight, down_bias):
        tables, places = rope_tables(), vector_places()
        small = (ln1_gain, ln1_bias, ln2_gain, ln2_bias, qkv_bias, out_bias, up_bias, down_bias)
        small_tile = jnp.pad(jnp.concatenate(small, axis=1), ((0, ROWS - LAYERS), (0, PAIR - sum(SHARES))))
        mix = jnp.concatenate([heads_last(qkv_weight), out_weight], axis=-1)
        *weights, _, vectors, dout_cols, y_out, hidden, n1, n2, ctx, act, qkv, pre = forward(
            x[0], y_cot[0], (up_weight, down_weight, mix), small_tile, tables, places)
        weights = [tensor.reshape((LAYERS, -1, tensor.shape[-1])) for tensor in weights]
        d_x, small_sums, (up, down, qkv, out) = backward(
            y_cot[0], tables, vectors, places, weights, (hidden, n1, n2, ctx, act, qkv, pre, dout_cols))
        (y_out, d_x, up, down, out), (g1, b1, g2, b2, qb, ob, ub, db) = finish((y_out, d_x, up, down, out), small_sums)
        return (y_out[None], d_x[None], g1, b1, heads_first(qkv), qb, out, ob, g2, b2, up, ub, down, db)

    return jax.shard_map(device_step, mesh=mesh,
                         in_specs=(act_spec, act_spec) + (param_spec,) * 12,
                         out_specs=(act_spec, act_spec) + (param_spec,) * 12,
                         check_vma=False)
```

```python
import functools
import jax
import jax.numpy as jnp
import numpy as np
from jax import lax
from jax.experimental import pallas as pl
from jax.experimental.pallas import tpu as pltpu
from jax.sharding import PartitionSpec as P

BF16, F32 = jnp.bfloat16, jnp.float32
EPSILON = 1e-5
MESH = pl.DeviceIdType.MESH
ANY = pl.BlockSpec(memory_space=pl.ANY)
IN_VMEM = pl.BlockSpec(memory_space=pltpu.VMEM)
VMEM_LIMIT = 67 * 10**6
LAYERS, AXES, SIDE, CORES, ROWS, PARTNERS = 2, 3, 4, 2, 8, 10
CHIPS = (SIDE, SIDE, SIDE)
SHARDS = SIDE * SIDE * SIDE * CORES
SEQ, WIDTH, HIDDEN, TILE, PAIR, LN_ROWS = 384, 1024, 4096, 512, 128, 64
HEADS, HEAD, PARTS = 16, 64, 3
QKV = PARTS * WIDTH
N_TILES, N_PAIRS, N_BLOCKS = HIDDEN // TILE, WIDTH // PAIR, SEQ // PAIR
TWICE = 2 * PAIR
INV_SQRT2, INV_SQRT2PI, SCALE = 0.7071067811865476, 0.3989422804014327, 0.125
SHARES = (8, 8, 8, 8, 24, 8, 32, 8)
SIZES = tuple(SHARDS * share for share in SHARES)
OFFSETS = tuple(sum(SIZES[:k]) for k in range(len(SIZES)))
N_VEC = sum(SIZES)
GAIN1, BIAS1, GAIN2, BIAS2, QKV_BIAS, OUT_BIAS, UP_BIAS, DOWN_BIAS = range(len(SHARES))
ORDERS = ((2, 1, 0), (1, 0, 2), (0, 2, 1))
HALVES = range(2)
OWN, ONE, CROSS, TWO = range(SIDE)
ROLES = (ONE, TWO, CROSS)
A, B, C = range(AXES)
UP, DOWN, MIX = range(3)
SELF = 3


class Chip:
    def __init__(self):
        node, local = lax.axis_index('node'), lax.axis_index('local')
        self.core, self.other = lax.rem(local, CORES), 1 - lax.rem(local, CORES)
        self.where = (lax.div(node, SIDE), lax.rem(node, SIDE), lax.div(local, CORES))
        self.base = (node, local - self.core)
        self.strides = ((SIDE, 0), (1, 0), (0, CORES))
        self.near = [(v, v + 1 - 2 * parity(v), lax.rem(v + 2, SIDE), SIDE - 1 - v) for v in self.where]

        self.gaps = [near[3] - near[1] for near in self.near]

    def at(self, axis, role, half):
        near = self.near[axis]
        if role in (OWN, CROSS):
            return near[role]
        return near[role] + half * self.gaps[axis] if role == ONE else near[role] - half * self.gaps[axis]

    def device(self, axis, role, half):
        shift = self.at(axis, role, half) - self.where[axis]
        node, local = [b + shift * s if s else b for b, s in zip(self.base, self.strides[axis])]
        return (node, local + self.core)

    def partner(self):
        node, local = self.base
        return (node, local + self.other)

    def signal_partners(self, semaphore):
        for axis in range(AXES):
            for role in ROLES:
                pl.semaphore_signal(semaphore, inc=1, device_id=self.device(axis, role, A), device_id_type=MESH)
        pl.semaphore_signal(semaphore, inc=1, device_id=self.partner(), device_id_type=MESH)


def enter(chip):
    barrier = pltpu.get_barrier_semaphore()
    chip.signal_partners(barrier)
    pl.semaphore_wait(barrier, PARTNERS)


def remote(src, dst, send_sem, recv_sem, device):
    return pltpu.make_async_remote_copy(src_ref=src, dst_ref=dst, send_sem=send_sem, recv_sem=recv_sem, device_id=device,
                                        device_id_type=MESH)


def start(copies):
    for copy in copies:
        copy.start()
    return copies


def wait(copies):
    for copy in copies:
        copy.wait()


def loop(count):
    return pl.loop(0, count)


def halves(body):
    loop(len(HALVES))(body)


def parity(n):
    return lax.rem(n, 2)


def pool(sems):
    return (sems.at[n] for n in range(sems.shape[0]))


def contract(a, b, a_axis, b_axis):
    return lax.dot_general(a, b, (((a_axis,), (b_axis,)), ((), ())), preferred_element_type=F32)


def dot(a, b):
    return contract(a, b, 1, 0)


def dot_t(a, b):
    return contract(a, b, 1, 1)


def row_sum(x):
    return jnp.sum(x, axis=1, keepdims=True)


def column_sum(x):
    return jnp.sum(x, axis=0, keepdims=True)


def rounded(x):
    return x.astype(BF16).astype(F32)


def lanes(first, width=PAIR):
    return pl.ds(pl.multiple_of(first, PAIR), width)


def turn(x, cos, sin_a, sin_b):
    return x * cos + pltpu.roll(x, PAIR - ROWS, 1) * sin_a + pltpu.roll(x, ROWS, 1) * sin_b


def turn_back(d, cos, sin_a, sin_b):
    return d * cos + pltpu.roll(d * sin_a, ROWS, 1) + pltpu.roll(d * sin_b, PAIR - ROWS, 1)


def iota(shape, axis):
    return lax.broadcasted_iota(jnp.int32, shape, axis)


def block_rows(j):
    return slice(j * PAIR, (j + 1) * PAIR)


def split_heads(x):
    first = iota((PAIR, PAIR), 1) < HEAD
    rows = []
    for j in range(N_BLOCKS):
        block = x[block_rows(j)]
        rows += [jnp.where(first, block, jnp.zeros_like(block)), jnp.where(first, jnp.zeros_like(block), block)]
    return jnp.concatenate(rows, axis=0)


def total_of(chunks, join=jnp.add):
    return functools.reduce(join, chunks)


def probabilities(q_block, keys, i):
    scores = dot_t(q_block, keys)
    causal = iota((PAIR, PAIR), 0) >= iota((PAIR, PAIR), 1)
    chunks = [scores[:, block_rows(j)] * SCALE for j in range(CORES * (i + 1))]
    for head in HALVES:
        mine = slice(head, None, CORES)
        *ahead, last = chunks[mine]
        held = ahead + [jnp.where(causal, last, -1e30)]
        top = jnp.max(total_of(held, jnp.maximum), axis=1, keepdims=True)
        held = [jnp.exp(chunk - top) for chunk in held]
        inverse = 1.0 / row_sum(total_of(held))
        chunks[mine] = [chunk * inverse for chunk in held]
    return chunks


def side_by_side(chunks):
    return jnp.concatenate([chunk.astype(BF16) for chunk in chunks], axis=1)


def row_mean(x):
    return jnp.mean(x, axis=1, keepdims=True)


def normalised(h):
    center = h - row_mean(h)
    inverse = lax.rsqrt(row_mean(center * center) + EPSILON)
    return center * inverse, inverse


def half_copies(chip, src, dst, own_sem, send_sem, recv_sem):
    width = dst.shape[-1]
    mine, away = [src.at[:, lanes(which * width, width)] for which in (chip.core, chip.other)]
    place = dst.at[chip.core]
    return [pltpu.make_async_copy(mine, place, own_sem), remote(away, place, send_sem, recv_sem, chip.partner())]


class Gather:
    def __init__(self, chip, shards, fulls, sems):
        self.chip, self.shards, self.fulls = chip, shards, fulls
        self.send_sem, self.recv_sem, self.pass_send, self.pass_recv = sems

    def box(self, layer, k, half, stage, role, own=False):
        width = self.fulls[k].shape[-1] // len(HALVES)
        cols = lanes(half * width, width)
        if own:
            return self.shards[k].at[layer, :, cols]
        where = list(self.chip.where)
        for axis in ORDERS[k][:stage]:
            where[axis] = pl.ds(0, SIDE)
        axis = ORDERS[k][stage]
        where[axis] = self.chip.at(axis, role, half)
        return self.fulls[k].at[layer, where[0], where[1], where[2], self.chip.core, :, cols]

    def reach(self, layer, k, half, stage, step):
        slot, on = AXES * stage + step, stage > A and step == C
        src = self.box(layer, k, half, stage, ONE if on else OWN, stage == A)
        return remote(src, self.box(layer, k, half, stage, ONE if on else OWN), self.send_sem.at[layer, k, stage],
                      self.recv_sem.at[layer, k, half, slot], self.chip.device(ORDERS[k][stage], TWO if on else ROLES[step], half))

    def passing(self, layer, k, half, stage, step):
        role = (*ROLES, OWN)[step]
        return remote(self.box(layer, k, half, stage, role, step == SELF), self.box(layer, k, half, stage, role),
                      self.pass_send.at[layer, k], self.pass_recv.at[layer, k], self.chip.partner())

    def each(self, action):
        for k in (MIX, UP, DOWN):
            @halves
            def _(half):
                action(k, half)

    def begin(self, layer, stage):
        for step in range(C if stage else AXES):
            self.each(lambda k, half: self.reach(layer, k, half, stage, step).start())

    def own(self, layer):
        self.each(lambda k, half: self.passing(layer, k, half, A, SELF).start())

    def middle(self, layer, stage):
        def action(k, half):
            self.reach(layer, k, half, stage, A).wait_recv()
            self.reach(layer, k, half, stage, C).start()
            self.passing(layer, k, half, stage, A).start()
        self.each(action)

    def end(self, layer, stage, steps=range(AXES)):
        def action(k, half):
            for step in steps:
                self.reach(layer, k, half, stage, step).wait_recv()
                self.passing(layer, k, half, stage, step).start()
        self.each(action)

    def arrived(self, layer, k):
        box = self.fulls[k].at[layer, :, :, :, self.chip.other]
        remote(box, box, self.pass_send.at[layer, k], self.pass_recv.at[layer, k], self.chip.partner()).wait_recv()

    def left(self):
        three, full = pl.ds(0, AXES), self.fulls[UP].at[A]
        boxes = (full.at[three, A, A, A], full.at[:, three, A, A], full.at[:, :, three, A])

        @loop(LAYERS)
        def _(layer):
            @loop(AXES)
            def _(k):
                for stage, box in enumerate(boxes):
                    sem = self.send_sem.at[layer, k, stage]
                    remote(box, box, sem, sem, self.chip.partner()).wait_send()
                box, sem = full.at[:, :, :, A], self.pass_send.at[layer, k]
                remote(box, box, sem, sem, self.chip.partner()).wait_send()


def pick_lanes(sel_lane, cols):
    return (iota((PAIR, WIDTH), 0) == sel_lane[:, cols]).astype(F32).astype(BF16)


def vector_blocks():
    return [slice(k * WIDTH, (k + 1) * WIDTH) for k in range(N_VEC // WIDTH)]


def unpack_vectors(small_v, layer, sel_shard, sel_lane, vec_ref):
    tiles = small_v[...].astype(F32).reshape((SHARDS, ROWS, PAIR))
    held = jnp.sum(jnp.where(iota(tiles.shape, 1) == layer, tiles, 0.0), axis=1).astype(BF16)
    for cols in vector_blocks():
        spread = dot(held, pick_lanes(sel_lane, cols))
        spread = jnp.where(iota((SHARDS, WIDTH), 0) == sel_shard[:, cols], spread, 0.0)
        vec_ref[layer:layer + 1, cols] = column_sum(spread)


def forward_kernel(x_hbm, ycot_hbm, tables_hbm, places_hbm, up_s, down_s, mix_s, small_ref, up_f, down_f, mix_f, small_full, vec_ref,
                   dout_cols, y_hbm, h_hbm, n1_hbm, n2_hbm, ctx_hbm, act_hbm, qkv_hbm, pre_hbm, up_v, down_v, mix_v, small_v, acc, pre_v,
                   n1_v, n2_v, qkv_v, ctx_v, y_v, n1_t, n2_t, ctx_t, act_t, send_sem, recv_sem, pass_send, pass_recv,
                   small_send, small_recv, own_sems, load_sem, save_sem, share_send, share_recv, act_save, act_send, act_recv, tables,
                   places):
    shards, fulls, own_sem = (up_s, down_s, mix_s), (up_f, down_f, mix_f), pool(own_sems)
    chip = Chip()
    with jax.named_scope('enter'):
        enter(chip)
    gather = Gather(chip, shards, fulls, (send_sem, recv_sem, pass_send, pass_recv))

    def small_copy(slot, where, device):
        place = small_full.at[(*where, chip.core)]
        return remote(place, place, small_send.at[slot], small_recv.at[slot], device)

    def small_reach(stage, step):
        where = list(chip.where)
        for axis in range(stage):
            where[axis] = pl.ds(0, SIDE)
        return small_copy(AXES * stage + step, where, chip.device(stage, ROLES[step], A))

    def small_begin(stage):
        start([small_reach(stage, step) for step in range(AXES)])

    def small_end(stage):
        for step in range(AXES):
            small_reach(stage, step).wait_recv()

    small_pass = small_copy(AXES * AXES, [pl.ds(0, SIDE)] * AXES, chip.partner())
    here = (*chip.where, chip.core)
    own = [pltpu.make_async_copy(small_ref, small_full.at[here], next(own_sem))]
    for shard, full in zip(shards, fulls):
        for layer in range(LAYERS):
            own.append(pltpu.make_async_copy(shard.at[layer], full.at[(layer, *here)], next(own_sem)))
    loads = [
        pltpu.make_async_copy(src, dst, next(own_sem)) for src, dst in ((x_hbm, y_v), (ycot_hbm, n1_v), (tables_hbm, tables), (places_hbm, places))]
    cot_copies = half_copies(chip, n1_v, dout_cols.at[LAYERS - 1], next(own_sem), next(own_sem), next(own_sem))
    with jax.named_scope('ag0'):
        gather.begin(A, A)
        start(own)
        gather.begin(B, A)
        wait(own)
        small_begin(A)
        gather.own(A)
        gather.own(B)
        start(loads)
        gather.end(A, A)
    with jax.named_scope('ag1'):
        gather.begin(A, B)
        small_end(A)
        small_begin(B)
        gather.end(B, A)
        gather.begin(B, B)
        gather.middle(A, B)
        small_end(B)
        small_begin(C)
        gather.middle(B, B)
        gather.end(A, B, (B, C))
    with jax.named_scope('ag2_start'):
        gather.begin(A, C)
        small_end(C)
        small_pass.start()
        gather.end(B, B, (B, C))
    with jax.named_scope('ag2_middle'):
        gather.middle(A, C)
        gather.begin(B, C)
    with jax.named_scope('unpack'):
        small_pass.wait_recv()
        fetch = pltpu.make_async_copy(small_full, small_v, next(own_sem))
        fetch.start()
        fetch.wait()
        wait(loads)
        start(cot_copies)
        for layer in range(LAYERS):
            unpack_vectors(small_v, layer, places[A:B], places[B:C], vec_ref)
    with jax.named_scope('ag2_late'):
        gather.end(A, C, (B,))
    with jax.named_scope('ag2_end'):
        gather.end(A, C, (C,))
        wait(cot_copies)

    def saves(layer):
        pairs = [(y_v, h_hbm.at[layer]), (qkv_v, qkv_hbm.at[layer])]
        kept = [pltpu.make_async_copy(src, dst, save_sem.at[n]) for n, (src, dst) in enumerate(pairs)]
        for n, (src, dst) in enumerate(((n1_t, n1_hbm), (n2_t, n2_hbm), (ctx_t, ctx_hbm))):
            dst = dst.at[layer, chip.core]
            kept.append((pltpu.make_async_copy(src, dst, save_sem.at[CORES + n]),
                         remote(src, dst, share_send.at[layer, n], share_recv.at[layer, n], chip.partner())))
        return kept

    def quarter(layer, t):
        rows, tiles = pl.ds(t * WIDTH, WIDTH), pl.ds(CORES * t, CORES)
        src, dst = act_t.at[rows], act_hbm.at[layer, chip.core, rows]
        return [pltpu.make_async_copy(pre_v.at[tiles], pre_hbm.at[layer, tiles], act_save.at[A, t]),
                pltpu.make_async_copy(src, dst, act_save.at[B, t]),
                remote(src, dst, act_send.at[layer, t], act_recv.at[layer, t], chip.partner())]

    def settle(layer):
        _, qkv_save, *shares = saves(layer)
        qkv_save.wait()
        for share in shares:
            wait(share)

        @loop(SIDE)
        def _(t):
            wait(quarter(layer, t))

    @loop(LAYERS)
    def _(layer):
        def vector(k, first=0, width=None):
            return vec_ref[pl.ds(layer, 1), lanes(OFFSETS[k] + first, width or SIZES[k])]

        def load(k, piece):
            if k == DOWN:
                return pltpu.make_async_copy(fulls[k].at[layer, piece], down_v.at[piece], load_sem.at[k, piece])
            cols = lanes(piece * WIDTH, WIDTH)
            return pltpu.make_async_copy(fulls[k].at[layer, :, :, :, :, :, cols], (up_v, None, mix_v)[k].at[:, :, :, :, :, cols],
                                         load_sem.at[k, piece])

        def matrix(held, piece):
            return held[:, :, :, :, :, lanes(piece * WIDTH, WIDTH)].reshape((WIDTH, WIDTH))

        def have(k):
            gather.arrived(layer, k)

        def meanwhile(action):
            @pl.when(layer == A)
            def _():
                action()

        h_save, qkv_save, n1_share, n2_share, ctx_share = saves(layer)
        with jax.named_scope('have_mix'):
            have(MIX)
            start([load(MIX, k) for k in range(SIDE)])

        h_save.start()

        @pl.when(layer == B)
        def _():
            settle(A)

        with jax.named_scope('ln'):
            @loop(SEQ // LN_ROWS)
            def _(r):
                rows = pl.ds(pl.multiple_of(r * LN_ROWS, LN_ROWS), LN_ROWS)
                scaled, _ = normalised(y_v[rows, :].astype(F32))
                n1_v[rows, :] = (scaled * vector(GAIN1) + vector(BIAS1)).astype(BF16)
                n2_v[rows, :] = (scaled * vector(GAIN2) + vector(BIAS2)).astype(BF16)

        for src, dst, share in ((n1_v, n1_t, n1_share), (n2_v, n2_t, n2_share)):
            dst[...] = src[...].T
            start(share)

        with jax.named_scope('qkv'):
            for k in range(PARTS):
                load(MIX, k).wait()
                x = dot(n1_v[...], matrix(mix_v, k)) + vector(QKV_BIAS, k * WIDTH, WIDTH)
                for c in range(N_PAIRS):
                    block = x[:, block_rows(c)]
                    if k < C:
                        block = turn(block, *[tables[n] for n in range(PARTS)])
                    qkv_v[:, lanes(k * WIDTH + c * PAIR)] = block.astype(BF16)

        qkv_save.start()
        with jax.named_scope('have_up'):
            have(UP)
            have(DOWN)

        start([load(UP, k) for k in range(SIDE)] + [load(DOWN, k) for k in range(SIDE)])
        with jax.named_scope('fattn'):
            def one_pair(pair):
                keys = split_heads(qkv_v[:, lanes(WIDTH + pair * PAIR)])
                values = split_heads(qkv_v[:, lanes(C * WIDTH + pair * PAIR)])
                for i in range(N_BLOCKS):
                    n = (i + 1) * CORES * PAIR
                    probs = probabilities(qkv_v[block_rows(i), lanes(pair * PAIR)], keys[:n], i)
                    ctx_v[block_rows(i), lanes(pair * PAIR)] = dot(side_by_side(probs), values[:n]).astype(BF16)

            @loop(N_PAIRS // CORES)
            def _(two):
                for k in HALVES:
                    one_pair(CORES * two + k)

                @pl.when((layer == A) & (two == A))
                def _():
                    gather.middle(B, C)

        ctx_t[...] = ctx_v[...].T
        start(ctx_share)
        with jax.named_scope('fout'):
            load(MIX, PARTS).wait()
            acc[...] = y_v[...].astype(F32) + dot(ctx_v[...], matrix(mix_v, PARTS)) + (vector(OUT_BIAS) + vector(DOWN_BIAS))

        with jax.named_scope('fmlp'):
            @loop(SIDE)
            def _(t):
                cols = lanes(t * WIDTH, WIDTH)
                load(UP, t).wait()
                pre = dot(n2_v[...], matrix(up_v, t)) + vector(UP_BIAS, t * WIDTH, WIDTH)
                for k in HALVES:
                    pre_v[CORES * t + k] = pre[:, k * TILE:(k + 1) * TILE]
                act = (0.5 * pre * (1.0 + lax.erf(pre * INV_SQRT2))).astype(BF16)
                act_t[cols, :] = act.T
                start(quarter(layer, t))
                load(DOWN, t).wait()
                acc[...] += dot(act, down_v[t].reshape((WIDTH, WIDTH)))

                @pl.when((layer == A) & (t == B))
                def _():
                    gather.end(B, C, (B,))

        h_save.wait()
        y_v[...] = acc[...].astype(BF16)
        with jax.named_scope('fend'):
            meanwhile(lambda: gather.end(B, C, (C,)))

    with jax.named_scope('ftail'):
        last = pltpu.make_async_copy(y_v, y_hbm, next(own_sem))
        last.start()
        for stage in range(AXES):
            for step in range(AXES):
                small_reach(stage, step).wait_send()
        small_pass.wait_send()
        gather.left()
        settle(LAYERS - 1)
        last.wait()


def forward(x, y_cot, shards, small_tile, tables, places):
    grid = CHIPS + (CORES,)
    full = [(LAYERS,) + grid + tensor.shape[1:] for tensor in shards]
    shapes = [(shape, BF16) for shape in full] + [(grid + small_tile.shape, BF16), ((LAYERS, N_VEC), F32), ((LAYERS, CORES, SEQ, TILE), BF16), ((SEQ, WIDTH), BF16),
                                                  ((LAYERS, SEQ, WIDTH), BF16)]
    shapes += [((LAYERS, CORES, width, SEQ), BF16) for width in (WIDTH, WIDTH, WIDTH, HIDDEN)]
    shapes += [((LAYERS, SEQ, QKV), BF16), ((LAYERS, N_TILES, SEQ, TILE), F32)]
    dma = pltpu.SemaphoreType.DMA
    slots = AXES * AXES
    scratch = [pltpu.VMEM(shape[1:], BF16) for shape in full] + [pltpu.VMEM(grid + small_tile.shape, BF16)]
    scratch += [pltpu.VMEM((SEQ, WIDTH), F32), pltpu.VMEM((N_TILES, SEQ, TILE), F32)]
    scratch += [pltpu.VMEM((SEQ, width), BF16) for width in (WIDTH, WIDTH, QKV, WIDTH, WIDTH)]
    scratch += [pltpu.VMEM((width, SEQ), BF16) for width in (WIDTH, WIDTH, WIDTH, HIDDEN)]
    scratch += [dma(shape) for shape in ((LAYERS, AXES, AXES), (LAYERS, AXES, len(HALVES), slots), (LAYERS, AXES), (LAYERS, AXES))]
    scratch += [dma(shape) for shape in ((slots + 1,), (slots + 1,), (slots + SIDE + SIDE + AXES,), (AXES, SIDE), (SIDE + 1,), (LAYERS, AXES), (LAYERS, AXES), (CORES, SIDE), (LAYERS, SIDE), (LAYERS, SIDE))]
    scratch += [pltpu.VMEM(tables.shape, F32), pltpu.VMEM(places.shape, jnp.int32)]
    out_specs = [IN_VMEM if dtype == F32 and len(shape) == LAYERS else ANY for shape, dtype in shapes]
    return pl.pallas_call(
        forward_kernel,
        out_shape=[jax.ShapeDtypeStruct(*s) for s in shapes],
        in_specs=[ANY] * SIDE + [IN_VMEM] * SIDE,
        out_specs=out_specs,
        scratch_shapes=scratch,
        compiler_params=pltpu.CompilerParams(collective_id=0, has_side_effects=True, vmem_limit_bytes=VMEM_LIMIT),
        name='forward_layers',
    )(x, y_cot, tables, places, *shards, small_tile)


WAVES = ((384, 384, 512), (384, 384, 256), (256, 256, 256))
LEADS = ((2,) + CHIPS[1:], CHIPS[1:], (2, SIDE), (SIDE,), (AXES,))
W_UP, W_DOWN, W_QKV, W_OUT = range(4)
STEPS = ((1, (2,)), (0, ()), (2, (4, 3)), (4, (5,)), (3, ()), (5, (6, 7, 8)), (8, (9,)), (9, ()))
LAST = AXES * AXES
CARRIED = ((0, 6, 0), (1, 4, 0), (2, 0, 0))
US_COLUMN, US_HOP, US_ADD, US_STEP = 0.022, 2.5, 0.0013, 0.2
US_FIRST, US_OUT, US_TILE, US_GRADIENT, US_PAIR, US_NORM = 2, 1.4, 1.6, 0.0035, 3.6, 2.7


class Schedule:
    def __init__(self):
        self.now, self.free, self.lines = 0.0, {}, []

    def send(self, link, columns):
        self.free[link] = max(self.free.get(link, 0.0), self.now) + columns * US_COLUMN
        return self.free[link] + US_HOP

    def due(self, limit):
        found = []
        while self.lines:
            line = min(self.lines, key=lambda one: one[A][A]())
            ready = line[A][A]()
            if limit is not None and ready > limit:
                break
            _, run, sends, cost = line.pop(A)
            self.lines = [one for one in self.lines if one]
            self.now = max(self.now, ready) + cost
            sends()
            found.append(run)
        return found

    def finish(self, line):
        while line:
            ready, run, sends, cost = line.pop(A)
            self.now = max(self.now, ready()) + cost
            sends()
            run()
        self.lines = [one for one in self.lines if one]

    def run(self, limit):
        for step in self.due(limit):
            step()

    def passed(self, cost):
        self.now += cost
        self.run(self.now)

    def hooks(self, count, cost):
        planned = []
        for _ in range(count):
            self.now += cost
            planned.append(self.due(self.now))
        return planned


def at_hooks(n, planned):
    for when, steps in enumerate(planned):
        if steps:
            @pl.when(n == when)
            def _():
                for step in steps:
                    step()


def add_into(dst, src, n_axes):
    if n_axes < 2:
        dst[...] += src[...]
        return

    @loop(SIDE)
    def _(k):
        dst[k] += src[k]


def at_axis(ref, axis, value, n_axes):
    every = [pl.ds(0, SIDE)] * n_axes
    every[axis] = value
    return ref.at[tuple(every)]


class Reduce:
    def __init__(self, chip, schedule, wave, grads, came, fin, sems, spare, write, done, when=None):
        self.wave, self.chip, self.schedule, self.widths, self.grads = wave, chip, schedule, WAVES[wave], grads
        self.came, self.fin, (self.send_sem, self.recv_sem), (self.spare, self.spare_sem) = came, fin, sems, spare
        self.write, self.done, self.when, self.times = write, done, when, {}

    def box(self, a, half, stage):
        order = ORDERS[a]
        ref = self.came[a][A].at[half, A]
        spot = [axis for axis in range(AXES) if axis != order[A]].index(order[B])
        if stage == B:
            return ref, spot, C
        return at_axis(ref, spot, self.chip.where[order[B]], C), A, B

    def copy(self, a, half, slot):
        stage, turn = divmod(slot, AXES)
        sems = self.send_sem.at[a, stage], self.recv_sem.at[a, half, slot]
        if slot == LAST:
            return remote(self.total(a, half).at[self.chip.other], self.fin[a].at[half], *sems, self.chip.partner())
        axis = ORDERS[a][stage]
        if stage == C:
            role = value = ROLES[turn]
            dst = self.came[a][SIDE].at[half, turn]
        else:
            role, value = TWO if turn == C else ONE, (ONE, CROSS, TWO)[turn]
            dst = self.came[a][CORES * stage + turn // C].at[half]
            dst = dst if turn == C else dst.at[turn]
        value = self.chip.at(axis, value, half)
        if stage:
            ref, spot, n_axes = self.box(a, half, stage)
            src = at_axis(ref, spot, value, n_axes)
        else:
            src = self.came[a][A].at[half, B] if turn == C else at_axis(self.grads[a].at[half], axis, value, AXES)
        return remote(src, dst, *sems, self.chip.device(axis, role, half))

    def each(self, action):
        for a in range(AXES):
            halves(lambda half: action(a, half))

    def sending(self, slot):
        stage = slot // AXES
        share = SIDE ** (CORES * stage)
        self.times[slot] = self.schedule.now + US_HOP if slot == LAST else max(
            self.schedule.send(ORDERS[a][stage], self.widths[a] / share) for a in range(AXES))

    def begin(self):
        for slot in (B, A):
            self.each(lambda a, half: self.copy(a, half, slot).start())

    def plan(self, first=0, last=None, late=0):
        for slot in (B, A):
            self.times[slot] = self.schedule.now + late
            if not first:
                self.sending(slot)
        for _, sent in STEPS[:first]:
            self.times.update((slot, self.schedule.now + late + US_HOP) for slot in sent)
        line = [
            (lambda slot=slot: self.times[slot], lambda k=k: self.step(k), lambda sent=sent: [self.sending(n) for n in sent],
             CORES * US_ADD * sum(self.widths) if k < C else US_STEP) for k, (slot, sent) in enumerate(STEPS)][first:last]
        self.schedule.lines.append(line)
        return line

    def step(self, k):
        def work():
            with jax.named_scope(f'w{self.wave}s{k}'):
                (self.first, self.first, self.halve, self.settle, self.settle, self.spread, self.cross, self.finish)[k](STEPS[k][A])
        if self.when is None:
            work()
        else:
            pl.when(self.when)(work)

    def held(self, a, half):
        ref = self.spare[A].at[a] if a < C else self.spare[B]
        return ref.at[half, :, :, :, :, pl.ds(0, self.widths[a])]

    def first(self, slot):
        def local(a, half):
            axis = ORDERS[a][A]
            return pltpu.make_async_copy(at_axis(self.grads[a].at[half], axis, self.chip.at(axis, TWO if slot else OWN, half), AXES),
                                         self.held(a, half), self.spare_sem.at[a, half])

        def action(a, half):
            local(a, half).wait()
            self.copy(a, half, slot).wait_recv()
            add_into(self.came[a][A].at[half, slot], self.held(a, half), C)
            if slot:
                self.copy(a, half, C).start()

        self.each(lambda a, half: local(a, half).start())
        self.each(action)

    def halve(self, slot):
        def action(a, half):
            ref, spot, n_axes = self.box(a, half, B)
            self.copy(a, half, slot).wait_recv()
            for turn, role in ((B, CROSS), (A, ONE), (C, TWO), (C, OWN)):
                value = self.chip.at(ORDERS[a][B], role, half)
                add_into(at_axis(ref, spot, value, n_axes), at_axis(self.came[a][B].at[half], spot, value, n_axes), B)
                if turn < C:
                    self.copy(a, half, AXES + turn).start()
        self.each(action)

    def settle(self, slot):
        def action(a, half):
            ref, spot, n_axes = self.box(a, half, B)
            self.copy(a, half, slot).wait_recv()
            value = self.chip.at(ORDERS[a][B], TWO if slot > AXES else OWN, half)
            add_into(at_axis(ref, spot, value, n_axes), self.came[a][C].at[half, slot - AXES], B)
            if slot > AXES:
                self.copy(a, half, AXES + C).start()
        self.each(action)

    def spread(self, slot):
        def action(a, half):
            ref, *_ = self.box(a, half, C)
            self.copy(a, half, slot).wait_recv()
            add_into(ref, self.came[a][AXES].at[half], B)
            for turn in range(AXES):
                self.copy(a, half, CORES * AXES + turn).start()
        self.each(action)

    def total(self, a, half):
        ref, *_ = self.box(a, half, C)
        return ref.at[self.chip.where[ORDERS[a][C]]]

    def cross(self, _):
        def action(a, half):
            for turn in range(AXES):
                self.copy(a, half, CORES * AXES + turn).wait_recv()
            self.total(a, half)[...] += total_of([self.came[a][SIDE][half, turn] for turn in range(AXES)])
            self.copy(a, half, LAST).start()
        self.each(action)

    def finish(self, _):
        def action(a, half):
            self.write(a, half, self.chip.core, self.total(a, half)[self.chip.core])
            self.copy(a, half, LAST).wait_recv()
            self.write(a, half, self.chip.other, self.fin[a][half])
        self.each(action)
        three = pl.ds(0, AXES)
        for a, (grad, fin) in enumerate(zip(self.grads, self.fin)):
            for stage, block in enumerate((grad.at[:, :, :, three], grad.at[:, :, three, A], grad.at[:, three, A, A], fin)):
                sem = self.send_sem.at[a, stage]
                remote(block, block, sem, sem, self.chip.partner()).wait_send()
        self.done()


class VectorSum:
    def __init__(self, chip, schedule, total, came, sems, finish, when=None):
        self.schedule, self.total, self.came, self.sems, self.finish, self.when, self.ready = schedule, total, came, sems, finish, when, 0.0
        self.devices = [[chip.device(axis, role, A) for role in ROLES] for axis in range(AXES)] + [[chip.partner()]]

    def copies(self, k):
        return [remote(self.total, self.came.at[AXES * k + n], self.sems.at[A, AXES * k + n], self.sems.at[B, AXES * k + n], device)
                for n, device in enumerate(self.devices[k])]

    def sending(self, k):
        if k < SIDE:
            self.ready = self.schedule.send(k, N_VEC / (SIDE * SIDE * ROWS))

    def step(self, k):
        def work():
            with jax.named_scope(f'vec{k}'):
                wait(self.copies(k - 1))
                for n in range(len(self.devices[k - 1])):
                    self.total[...] += self.came[AXES * (k - 1) + n]
            if k < SIDE:
                start(self.copies(k))
            else:
                self.finish()
        if self.when is None:
            work()
        else:
            pl.when(self.when)(work)

    def begin(self):
        start(self.copies(A))

    def plan(self):
        self.sending(A)
        self.schedule.lines.append([
            (lambda: self.ready, lambda k=k: self.step(k), lambda k=k: self.sending(k), US_STEP) for k in range(1, SIDE + 1)])


def backward_kernel(ycot_hbm, tables, vec_ref, places, up_hbm, down_hbm, mix_hbm, h_hbm, n1_hbm, n2_hbm, ctx_hbm,
                    act_hbm, qkv_hbm, pre_hbm, _, dx_hbm, small_ref, up_sum, down_sum, qkv_sum, out_sum, dout_cols, dpre_cols,
                    dqkv_cols, *refs):
    n_arrays, sums = AXES * len(WAVES), (up_sum, down_sum, qkv_sum, out_sum)
    grads, refs = refs[:n_arrays], refs[n_arrays:]
    (spare, spare_wide, tile_v, big_v, rhs_v, wup_v, wdown_v, pre_v, dn1, dn2, dctx, dk_acc, dv_acc, qkv_v, dpre_v, dqkv_v, dh_v, h_v,
     totals, came_vec, send_sem, recv_sem, spare_sem, tile_sem, big_sem, rhs_sem, mlp_sem, io_sem, own_sem, share_send,
     share_recv, pre_sem, vec_sem, credit, *refs) = refs
    fins, came = refs[:n_arrays], refs[n_arrays:]
    first_in = pltpu.make_async_copy(ycot_hbm, dh_v, io_sem.at[A])
    first_in.start()
    chip = Chip()
    core, other = chip.core, chip.other

    def exchange(layer, k, src, dst):
        return half_copies(chip, src, dst.at[layer], own_sem.at[k], share_send.at[k], share_recv.at[k])

    def tokens_load(layer, src, part, slot):
        return [pltpu.make_async_copy(src.at[layer, k, pl.ds(part * WIDTH, WIDTH)], big_v.at[slot, :, pl.ds(k * SEQ, SEQ)],
                                      big_sem.at[slot, k]) for k in range(CORES)]

    def weight_load(layer, k, slot):
        return pltpu.make_async_copy(mix_hbm.at[layer, :, lanes(k * WIDTH, WIDTH)], big_v.at[slot], big_sem.at[slot, CORES])

    def tile_loads(layer, t, slot):
        rows = lanes(t * TILE, TILE)
        pairs = ((down_hbm.at[layer, rows], wdown_v), (pre_hbm.at[layer, t], pre_v), (up_hbm.at[layer, :, rows], wup_v))
        return [pltpu.make_async_copy(src, dst.at[slot], mlp_sem.at[slot, n]) for n, (src, dst) in enumerate(pairs)]

    def input_loads(layer):
        return [pltpu.make_async_copy(qkv_hbm.at[layer], qkv_v, io_sem.at[B]), pltpu.make_async_copy(h_hbm.at[layer], h_v, io_sem.at[C])]

    def rhs_load(layer, src, first, width, k):
        cols = lanes(first, width)
        return [pltpu.make_async_copy(src.at[layer, n, :, cols], rhs_v.at[pl.ds(n * SEQ, SEQ), cols], rhs_sem.at[k, n])
                for n in range(CORES)]

    def prefetch(layer):
        start(tokens_load(layer, ctx_hbm, A, AXES) + tokens_load(layer, act_hbm, A, A))

    def prefetch_more(layer):
        start(tokens_load(layer, act_hbm, B, B) + tokens_load(layer, act_hbm, C, C) + input_loads(layer))
        for t in HALVES:
            start(tile_loads(layer, t, t))

    prefetch(LAYERS - 1)
    start(rhs_load(LAYERS - 1, dout_cols, A, TILE, A))
    with jax.named_scope('enter'):
        enter(chip)
    with jax.named_scope('first_in'):
        first_in.wait()
    dx_copy = pltpu.make_async_copy(dh_v, dx_hbm, io_sem.at[A])
    prefetch_more(LAYERS - 1)

    def vector_at(k, first=0, width=None):
        return lanes(OFFSETS[k] + first, width or SIZES[k])

    def reduction(schedule, layer, wave, when):
        def write(a, half, side, block):
            def put(arr, group, col, first, width):
                size = sums[arr].shape[-1] // CORES
                sums[arr][layer, group, :, lanes(side * size + col, width)] = block[:, first:first + width].astype(BF16)
            width, colour = WAVES[wave][a], CORES * a + half
            if wave:
                first = colour * width if wave == C or a < C else SIDE * WAVES[wave][A] + half * width
                put(W_QKV if wave == C else W_UP, A, first, A, width)
            elif a < C:
                put(W_DOWN, colour, A, A, width)
            else:
                for k in HALVES:
                    put(W_DOWN, CORES * half + k, WAVES[A][A], k * PAIR, PAIR)
                put(W_OUT, A, half * TWICE, TWICE, TWICE)

        def done():
            @pl.when(layer == LAYERS - 1)
            def _():
                chip.signal_partners(credit.at[wave])

        where = slice(AXES * wave, AXES * (wave + 1))
        count = len(LEADS)
        return Reduce(chip, schedule, wave, [grad.at[layer] for grad in grads[where]],
                      [came[count * (AXES * wave + a):count * (AXES * wave + a + 1)] for a in range(AXES)],
                      fins[where], (send_sem.at[wave], recv_sem.at[wave]), ((spare, spare_wide), spare_sem), write, done, when)

    def vector_sum(schedule, layer, when):
        def own_part():
            with jax.named_scope('own'):
                node, local = chip.base
                me = node * (SIDE * CORES) + local + core
                row = jnp.zeros((ROWS, PAIR), F32)
                for k, share in enumerate(SHARES):
                    if k == QKV_BIAS:
                        firsts = [part * WIDTH + lax.div(me, CORES * ROWS) * PAIR for part in range(PARTS)]
                    else:
                        firsts = [lax.div(me * share, PAIR) * PAIR]
                    for first in firsts:
                        cols = lanes(OFFSETS[k] + first)
                        left = jnp.zeros((ROWS, PAIR), F32) + totals[layer, :, cols] * (places[A:B, cols] == me).astype(F32)
                        pick = (iota((PAIR, PAIR), 0) == places[B:C, cols]).astype(F32).astype(BF16)
                        for _ in range(PARTS):
                            row = row + dot_t(left.astype(BF16), pick)
                            left = left - rounded(left)
                small_ref[layer] = row.astype(BF16)

            @pl.when(layer == LAYERS - 1)
            def _():
                chip.signal_partners(credit.at[AXES])

        return VectorSum(chip, schedule, totals.at[layer], came_vec, vec_sem, own_part, when)

    def run_on(schedule, layer, when):
        lines = [reduction(schedule, layer, wave, when).plan(step, late=late) for wave, step, late in CARRIED]
        vector_sum(schedule, layer, when).plan()
        return lines

    @loop(LAYERS + 1)
    def _(turn_no):
        layer = LAYERS - 1 - turn_no
        working = pl.when(turn_no < LAYERS)
        total = totals.at[layer]
        schedule = Schedule()

        carried = run_on(schedule, layer + 1, turn_no > A)

        def product(lhs_slot, first, width, out_slot):
            value = dot(big_v[lhs_slot, :, 0:CORES * SEQ], rhs_v[:, lanes(first, width)])
            tile_v[out_slot, :, :, :, :, :, 0:width] = value.reshape(CHIPS + (CORES, ROWS, width))

        def tile_out(slot, src, dst):
            return pltpu.make_async_copy(src, dst, tile_sem.at[slot])

        def tile_done(slot, width):
            block = tile_v.at[slot, :, :, :, :, :, pl.ds(0, width)]
            tile_out(slot, block, block).wait()

        def columns(wave, a, half, first, width):
            return grads[AXES * wave + a].at[layer, half, :, :, :, :, :, pl.ds(first, width)]

        def launch(wave):
            schedule.finish(carried[wave])

            @pl.when(turn_no == B)
            def _():
                pl.semaphore_wait(credit.at[wave], PARTNERS)

            current = reduction(schedule, layer, wave, turn_no < LAYERS)
            if wave == C:
                @pl.when(turn_no == B)
                def _():
                    pl.semaphore_wait(credit.at[AXES], PARTNERS)

                @working
                def _():
                    vector_sum(schedule, layer, None).begin()

            working(current.begin)
            if wave < C:
                current.plan(last=CARRIED[wave][B])

        @working
        def _():
            with jax.named_scope('dw_out'):
                @pl.when(turn_no == B)
                def _():
                    wait(exchange(layer, A, dh_v, dout_cols))
                    start(rhs_load(layer, dout_cols, A, TILE, A))

                wait(rhs_load(layer, dout_cols, A, TILE, A))
                wait(tokens_load(layer, ctx_hbm, A, AXES))
                product(AXES, A, TILE, B)
                start(tokens_load(layer, act_hbm, AXES, AXES))
                for k in HALVES:
                    tile_out(B, tile_v.at[B, :, :, :, :, :, pl.ds(k * TWICE, TWICE)], columns(A, C, k, TWICE, TWICE)).start()

        schedule.passed(US_FIRST)
        out_hooks = schedule.hooks(SIDE, US_OUT)

        @loop(SIDE)
        def _(z):
            @working
            def _():
                slot = parity(z)
                wait(tokens_load(layer, act_hbm, z, z))

                @pl.when(z > A)
                def _():
                    tile_done(slot, TILE)

                product(z, A, TILE, slot)
                split = WAVES[A][A]
                for k in range(SIDE):
                    a, half = divmod(k, CORES)
                    for c in range(CORES):
                        block = tile_v.at[slot, :, :, CORES * c + a, half]
                        tile_out(slot, block.at[:, :, :, pl.ds(0, split)], grads[a].at[layer, half, z, :, :, c]).start()
                        tile_out(slot, block.at[:, :, :, pl.ds(split, PAIR)],
                                 grads[C].at[layer, a, z, :, :, c, :, pl.ds(half * PAIR, PAIR)]).start()

            at_hooks(z, out_hooks)

        @working
        def _():
            start(tokens_load(layer, n2_hbm, A, A) + [weight_load(layer, k, k + 1) for k in range(PARTS)])
            for slot in HALVES:
                tile_done(slot, TILE)

        schedule.passed(US_STEP)
        launch(A)

        @working
        def _():
            dn2[...] = jnp.zeros_like(dn2)

        def pre_copy(t, slot, away):
            place = dpre_cols.at[layer, core, :, lanes(lax.rem(t, SIDE) * TILE, TILE)]
            if away:
                return remote(dpre_v.at[slot], place, pre_sem.at[A, t], pre_sem.at[B, t], chip.partner())
            return pltpu.make_async_copy(dpre_v.at[slot], place, own_sem.at[CORES + slot])

        def pre_act(t, leave):
            for away, whose in ((False, core), (True, other)):
                @pl.when(lax.div(t, SIDE) == whose)
                def _():
                    copy = pre_copy(t, parity(t), away)
                    if leave:
                        copy.start()
                    elif away:
                        copy.wait_send()
                    else:
                        copy.wait()

        tile_hooks = schedule.hooks(N_TILES, US_TILE)

        with jax.named_scope('mlp'):
            @loop(N_TILES)
            def _(t):
                @working
                def _():
                    slot = parity(t)
                    wait(tile_loads(layer, t, slot))
                    d_act = rounded(dot_t(dh_v[...], wdown_v[slot]))
                    pre = pre_v[slot]
                    slope = 0.5 * (1.0 + lax.erf(pre * INV_SQRT2)) + pre * (INV_SQRT2PI * jnp.exp(-0.5 * pre * pre))
                    d_pre = d_act * slope
                    total[:, vector_at(UP_BIAS, t * TILE, TILE)] = column_sum(d_pre)

                    @pl.when(t > B)
                    def _():
                        pre_act(t - CORES, False)

                    dpre_v[slot] = d_pre.astype(BF16)
                    pre_act(t, True)
                    dn2[...] += dot_t(dpre_v[slot], wup_v[slot])

                    @pl.when(t + CORES < N_TILES)
                    def _():
                        start(tile_loads(layer, t + CORES, slot))

                at_hooks(t, tile_hooks)

        @working
        def _():
            for t in HALVES:
                pre_act(N_TILES - CORES + t, False)
            for t in range(SIDE):
                pre_copy(SIDE * core + t, A, True).wait_recv()

        def gradient_loads(wave, source):
            first = 0
            for a in range(AXES):
                width = CORES * WAVES[wave][a]
                start(rhs_load(layer, source, first, width, a))
                first += width

        def gradient_wave(wave, source, lhs_slot, first, orders):
            split, count = WAVES[wave][orders[A]], len(orders)
            width = CORES * split
            planned = schedule.hooks(count, width * US_GRADIENT)

            @loop(count)
            def _(n):
                @working
                def _():
                    slot = parity(n)
                    wait(rhs_load(layer, source, first + n * width, width, orders[A] + n))

                    @pl.when(n > B)
                    def _():
                        tile_done(slot, width)

                    product(lhs_slot, first + n * width, width, slot)
                    for k, a in enumerate(orders):
                        @pl.when(n == k)
                        def _():
                            for half in HALVES:
                                block = tile_v.at[slot, :, :, :, :, :, pl.ds(half * split, split)]
                                tile_out(slot, block, columns(wave, a, half, 0, split)).start()

                at_hooks(n, planned)

            @working
            def _():
                for slot in range(min(count, CORES)):
                    tile_done(slot, width)

        @working
        def _():
            gradient_loads(B, dpre_cols)
            wait(tokens_load(layer, n2_hbm, A, A))

        with jax.named_scope('dw1'):
            gradient_wave(B, dpre_cols, A, A, (A, B))
            gradient_wave(B, dpre_cols, A, SIDE * WAVES[B][A], (C,))
        launch(B)
        @working
        def _():
            weight_load(layer, AXES, A).start()
            d_sum = column_sum(dh_v[...].astype(F32))
            total[:, vector_at(OUT_BIAS)] = d_sum
            total[:, vector_at(DOWN_BIAS)] = d_sum
            wait(input_loads(layer))
            weight_load(layer, AXES, A).wait()
            dctx[...] = dot_t(dh_v[...], big_v[A]).astype(BF16)

        pair_hooks = schedule.hooks(N_PAIRS // CORES, US_PAIR)

        with jax.named_scope('attn'):
            def one_pair(pair, dk_sum, dv_sum):
                at = lanes(pair * PAIR)
                keys = split_heads(qkv_v[:, lanes(WIDTH + pair * PAIR)])
                values = split_heads(qkv_v[:, lanes(C * WIDTH + pair * PAIR)])
                q_t = qkv_v[:, at].T
                dc_t = dctx[:, at].T
                bias_sums = [jnp.zeros((1, PAIR), F32)] * PARTS

                def turned_back(n, d, rows, to):
                    d = turn_back(rounded(d), *[tables[k, rows, :] for k in range(PARTS)])
                    bias_sums[n] = bias_sums[n] + column_sum(d)
                    dqkv_v[rows, to] = d.astype(BF16)

                for i in range(N_BLOCKS):
                    old, n = i * TWICE, (i + 1) * TWICE
                    rows = block_rows(i)
                    probs = probabilities(qkv_v[rows, at], keys[:n], i)
                    d_all = rounded(dot_t(dctx[rows, at], values[:n]))
                    d_scores = [d_all[:, block_rows(j)] for j in range(CORES * (i + 1))]
                    for head in HALVES:
                        mine = slice(head, None, CORES)
                        mean = row_sum(total_of([p * d for p, d in zip(probs[mine], d_scores[mine])]))
                        d_scores[mine] = [p * (d - mean) * SCALE for p, d in zip(probs[mine], d_scores[mine])]
                    d_scores, probs = side_by_side(d_scores), side_by_side(probs)
                    turned_back(A, dot(d_scores, keys[:n]), rows, at)
                    for acc, left, right in ((dk_sum, q_t, d_scores), (dv_sum, dc_t, probs)):
                        part = dot(left[:, rows], right)
                        if i:
                            acc[:, :old] += part[:, :old]
                        acc[:, old:n] = part[:, old:]
                first = iota((PAIR, PAIR), 0) < HEAD
                for j in range(N_BLOCKS):
                    rows = block_rows(j)
                    d_key, d_value = [jnp.where(first, acc[:, block_rows(CORES * j)], acc[:, block_rows(CORES * j + 1)]).T
                                      for acc in (dk_sum, dv_sum)]
                    turned_back(B, d_key, rows, lanes(WIDTH + pair * PAIR))
                    d_value = d_value.astype(BF16)
                    bias_sums[C] = bias_sums[C] + column_sum(d_value.astype(F32))
                    dqkv_v[rows, lanes(C * WIDTH + pair * PAIR)] = d_value
                for k, bias_sum in enumerate(bias_sums):
                    total[:, vector_at(QKV_BIAS, k * WIDTH + pair * PAIR, PAIR)] = bias_sum

            @loop(N_PAIRS // CORES)
            def _(two):
                @working
                def _():
                    for k in HALVES:
                        one_pair(CORES * two + k, dk_acc.at[k], dv_acc.at[k])

                at_hooks(two, pair_hooks)

        @working
        def _():
            start(exchange(layer, B, dqkv_v, dqkv_cols))
            dn1[...] = jnp.zeros_like(dn1)

            with jax.named_scope('dn1'):
                @loop(PARTS)
                def _(k):
                    weight_load(layer, k, k + 1).wait()
                    dn1[...] += dot_t(dqkv_v[:, lanes(k * WIDTH, WIDTH)], big_v[k + 1])

            start(tokens_load(layer, n1_hbm, A, B))

        schedule.passed(US_NORM)

        @working
        def _():
            for k in (GAIN1, BIAS1, GAIN2, BIAS2):
                total[:, vector_at(k)] = jnp.zeros((1, WIDTH), F32)

            with jax.named_scope('lnb'):
                @loop(SEQ // LN_ROWS)
                def _(r):
                    rows = pl.ds(pl.multiple_of(r * LN_ROWS, LN_ROWS), LN_ROWS)
                    scaled, inverse = normalised(h_v[rows, :].astype(F32))
                    d1, d2 = rounded(dn1[rows, :]), rounded(dn2[rows, :])
                    for k, value in ((GAIN1, d1 * scaled), (BIAS1, d1), (GAIN2, d2 * scaled), (BIAS2, d2)):
                        total[:, vector_at(k)] += column_sum(value)
                    g1, g2 = [vec_ref[pl.ds(layer, 1), lanes(OFFSETS[k], WIDTH)] for k in (GAIN1, GAIN2)]
                    d_scaled = d1 * g1 + d2 * g2
                    d_h = inverse * (d_scaled - row_mean(d_scaled) - scaled * row_mean(d_scaled * scaled))
                    dh_v[rows, :] = (dh_v[rows, :].astype(F32) + d_h).astype(BF16)

        schedule.passed(US_NORM)
        @working
        def _():
            wait(exchange(layer, B, dqkv_v, dqkv_cols))
            gradient_loads(C, dqkv_cols)
            wait(tokens_load(layer, n1_hbm, A, B))

        @pl.when(turn_no == A)
        def _():
            start(exchange(layer - 1, A, dh_v, dout_cols))

        @pl.when(turn_no == B)
        def _():
            dx_copy.start()

        with jax.named_scope('dw2'):
            gradient_wave(C, dqkv_cols, B, A, (A, B, C))

        @pl.when(turn_no == A)
        def _():
            prefetch(layer - 1)
            prefetch_more(layer - 1)

        schedule.run(None)
        launch(C)

    dx_copy.wait()


def backward(y_cot, tables, vectors, places, weights, saved):
    dma, one = pltpu.SemaphoreType.DMA, (1,)
    pair, wide, row = (len(HALVES),), (SEQ, WIDTH), one + (N_VEC,)
    shapes = [(wide, BF16), ((LAYERS, ROWS, PAIR), BF16)]
    shapes += [((LAYERS, groups, ROWS, width), BF16) for groups, width in ((*one, HIDDEN), (SIDE, WIDTH), (*one, QKV), (*one, WIDTH))]
    in_vmem = len(shapes)
    shapes += [((LAYERS, CORES, SEQ, width), BF16) for width in (TILE, SIDE * TILE, PARTS * TILE)]
    blocks = [(CORES, ROWS, width) for wave in WAVES for width in wave]
    shapes += [((LAYERS,) + pair + CHIPS + block, F32) for block in blocks]
    tile = (CORES, ROWS)
    scratch = [(pair + pair + CHIPS[1:] + tile + (WAVES[0][0],), F32), (pair + CHIPS[1:] + tile + (TILE,), F32), (pair + CHIPS + tile + (CORES * WAVES[0][0],), F32), ((SIDE, WIDTH, WIDTH), BF16), ((CORES * SEQ, SIDE * TILE), BF16)]
    scratch += [(pair + shape, BF16) for shape in ((WIDTH, TILE), (TILE, WIDTH))]
    scratch += [(pair + (SEQ, TILE), F32), (wide, F32), (wide, F32), (wide, BF16)] + [(pair + (PAIR, CORES * SEQ), F32)] * CORES
    scratch += [((SEQ, QKV), BF16), (pair + (SEQ, TILE), BF16), ((SEQ, QKV), BF16), (wide, BF16), (wide, BF16), ((LAYERS,) + row, F32),
                ((PARTNERS,) + row, F32)]
    slots = (len(WAVES), AXES) + pair + (LAST + 1,)
    sems = [dma(shape) for shape in ((len(WAVES), AXES, SIDE), slots, (AXES,) + pair, pair, (SIDE, AXES), (AXES, CORES), pair + (PARTS,), (AXES,),
                                     (SIDE,), pair, pair, pair + (N_TILES,), pair + (PARTNERS,))]
    late = [(pair + block[1:], F32) for block in blocks] + [(pair + lead + block, F32) for block in blocks for lead in LEADS]
    outs = pl.pallas_call(
        backward_kernel,
        out_shape=[jax.ShapeDtypeStruct(*s) for s in shapes],
        in_specs=[ANY] + [IN_VMEM] * AXES + [ANY] * (PARTNERS + 1),
        input_output_aliases={SIDE + PARTNERS: in_vmem},
        out_specs=[ANY] + [IN_VMEM] * (in_vmem - 1) + [ANY] * (len(shapes) - in_vmem),
        scratch_shapes=[pltpu.VMEM(*s) for s in scratch] + sems + [pltpu.SemaphoreType.REGULAR((SIDE,))]
        + [pltpu.VMEM(*s) for s in late],
        compiler_params=pltpu.CompilerParams(collective_id=1, has_side_effects=True, vmem_limit_bytes=VMEM_LIMIT),
        name='backward_layers',
    )(y_cot, tables, vectors, places, *weights, *saved)
    d_x, small, *sums = outs[:in_vmem]
    return d_x, small[:, 0], [s.reshape((LAYERS, -1, s.shape[-1])) for s in sums]


def finish_kernel(*refs):
    n_large = CORES + AXES
    large, small_ref, refs = refs[:n_large], refs[n_large], refs[n_large + 1:]
    outs, small_outs, refs = refs[:n_large], refs[n_large:n_large + len(SHARES)], refs[n_large + len(SHARES):]
    held, sems = refs[:n_large], refs[n_large]
    loads = start([pltpu.make_async_copy(src, dst, sems.at[n]) for n, (src, dst) in enumerate(zip(large, held))])
    first = 0
    for share, out in zip(SHARES, small_outs):
        out[...] = small_ref[:, first:first + share]
        first += share
    stores = []
    for load, src, dst in zip(loads, held, outs):
        load.wait()
        stores += start([pltpu.make_async_copy(src, dst, sems.at[n_large + len(stores)])])
    wait(stores)


def finish(large, small):
    shapes = [jax.ShapeDtypeStruct(t.shape, BF16) for t in large] + [jax.ShapeDtypeStruct((LAYERS, share), BF16) for share in SHARES]
    outs = pl.pallas_call(
        finish_kernel,
        out_shape=shapes,
        in_specs=[ANY] * len(large) + [IN_VMEM],
        out_specs=[ANY] * len(large) + [IN_VMEM] * len(SHARES),
        scratch_shapes=[pltpu.VMEM(t.shape, BF16) for t in large] + [pltpu.SemaphoreType.DMA((CORES * len(large),))],
        name='finish',
    )(*large, small)
    return outs[:len(large)], outs[len(large):]


def rope_tables():
    rot_dim, f32 = HEAD // SIDE, np.float32
    inv_freq = f32(1.0) / f32(10000.0) ** (np.arange(0, rot_dim, 2, dtype=f32) / f32(rot_dim))
    angles = np.arange(SEQ, dtype=f32)[:, None] * inv_freq[None, :]
    cos, sin = np.cos(angles), np.sin(angles)
    zero = np.zeros_like(sin)
    rest = np.zeros((SEQ, HEAD - rot_dim), f32)
    tables = ([cos, cos, rest + f32(1.0)], [-sin, zero, rest], [zero, sin, rest])
    return jnp.asarray(np.stack([np.tile(np.concatenate(table, axis=1), (1, 2)) for table in tables]).astype(f32))


def heads_last(tensor):
    lead = tensor.shape[:-2]
    return tensor.reshape(lead + (HEADS, PARTS, HEAD)).swapaxes(-3, -2).reshape(lead + (QKV,))


def heads_first(tensor):
    lead = tensor.shape[:-1]
    return tensor.reshape(lead + (PARTS, HEADS, HEAD)).swapaxes(-3, -2).reshape(lead + (HEADS, PARTS * HEAD))


def vector_places():
    shard, lane, first = [], [], 0
    for k, (share, size) in enumerate(zip(SHARES, SIZES)):
        place = np.arange(size)
        if k == QKV_BIAS:
            place = heads_last(place.reshape(HEADS, -1))
        shard.append(place // share)
        lane.append(first + place % share)
        first += share
    return jnp.asarray(np.stack([np.concatenate(shard), np.concatenate(lane)]).astype(np.int32))


def solution(mesh):
    shard_axes = ('node', 'local')
    act_spec = P(shard_axes)
    param_spec = P(None, shard_axes)

    def device_step(x, y_cot, ln1_gain, ln1_bias, qkv_weight, qkv_bias, out_weight, out_bias,
                    ln2_gain, ln2_bias, up_weight, up_bias, down_weight, down_bias):
        tables, places = rope_tables(), vector_places()
        small = (ln1_gain, ln1_bias, ln2_gain, ln2_bias, qkv_bias, out_bias, up_bias, down_bias)
        small_tile = jnp.pad(jnp.concatenate(small, axis=1), ((0, ROWS - LAYERS), (0, PAIR - sum(SHARES))))
        mix = jnp.concatenate([heads_last(qkv_weight), out_weight], axis=-1)
        *weights, _, vectors, dout_cols, y_out, hidden, n1, n2, ctx, act, qkv, pre = forward(
            x[0], y_cot[0], (up_weight, down_weight, mix), small_tile, tables, places)
        weights = [tensor.reshape((LAYERS, -1, tensor.shape[-1])) for tensor in weights]
        d_x, small_sums, (up, down, qkv, out) = backward(
            y_cot[0], tables, vectors, places, weights, (hidden, n1, n2, ctx, act, qkv, pre, dout_cols))
        (y_out, d_x, up, down, out), (g1, b1, g2, b2, qb, ob, ub, db) = finish((y_out, d_x, up, down, out), small_sums)
        return (y_out[None], d_x[None], g1, b1, heads_first(qkv), qb, out, ob, g2, b2, up, ub, down, db)

    return jax.shard_map(device_step, mesh=mesh,
                         in_specs=(act_spec, act_spec) + (param_spec,) * 12,
                         out_specs=(act_spec, act_spec) + (param_spec,) * 12,
                         check_vma=False)
```

```python
import functools
import jax
import jax.numpy as jnp
import numpy as np
from jax import lax
from jax.experimental import pallas as pl
from jax.experimental.pallas import tpu as pltpu
from jax.sharding import PartitionSpec as P

BF16, F32 = jnp.bfloat16, jnp.float32
EPSILON = 1e-5
MESH = pl.DeviceIdType.MESH
ANY = pl.BlockSpec(memory_space=pl.ANY)
IN_VMEM = pl.BlockSpec(memory_space=pltpu.VMEM)
VMEM_LIMIT = 67 * 10**6
LAYERS, AXES, SIDE, CORES, ROWS, PARTNERS = 2, 3, 4, 2, 8, 10
CHIPS = (SIDE, SIDE, SIDE)
SHARDS = SIDE * SIDE * SIDE * CORES
SEQ, WIDTH, HIDDEN, TILE, PAIR, LN_ROWS = 384, 1024, 4096, 512, 128, 64
HEADS, HEAD, PARTS = 16, 64, 3
QKV = PARTS * WIDTH
N_TILES, N_PAIRS, N_BLOCKS = HIDDEN // TILE, WIDTH // PAIR, SEQ // PAIR
TWICE = 2 * PAIR
INV_SQRT2, INV_SQRT2PI, SCALE = 0.7071067811865476, 0.3989422804014327, 0.125
SHARES = (8, 8, 8, 8, 24, 8, 32, 8)
SIZES = tuple(SHARDS * share for share in SHARES)
OFFSETS = tuple(sum(SIZES[:k]) for k in range(len(SIZES)))
N_VEC = sum(SIZES)
GAIN1, BIAS1, GAIN2, BIAS2, QKV_BIAS, OUT_BIAS, UP_BIAS, DOWN_BIAS = range(len(SHARES))
ORDERS = ((2, 1, 0), (1, 0, 2), (0, 2, 1))
HALVES = range(2)
OWN, ONE, CROSS, TWO = range(SIDE)
ROLES = (ONE, TWO, CROSS)
A, B, C = range(AXES)
UP, DOWN, MIX = range(3)
SELF = 3


class Chip:
    def __init__(self):
        node, local = lax.axis_index('node'), lax.axis_index('local')
        self.core, self.other = lax.rem(local, CORES), 1 - lax.rem(local, CORES)
        self.where = (lax.div(node, SIDE), lax.rem(node, SIDE), lax.div(local, CORES))
        self.base = (node, local - self.core)
        self.strides = ((SIDE, 0), (1, 0), (0, CORES))
        self.near = [(v, v + 1 - 2 * parity(v), lax.rem(v + 2, SIDE), SIDE - 1 - v) for v in self.where]

        self.gaps = [near[3] - near[1] for near in self.near]

    def at(self, axis, role, half):
        near = self.near[axis]
        if role in (OWN, CROSS):
            return near[role]
        return near[role] + half * self.gaps[axis] if role == ONE else near[role] - half * self.gaps[axis]

    def device(self, axis, role, half):
        shift = self.at(axis, role, half) - self.where[axis]
        node, local = [b + shift * s if s else b for b, s in zip(self.base, self.strides[axis])]
        return (node, local + self.core)

    def partner(self):
        node, local = self.base
        return (node, local + self.other)

    def signal_partners(self, semaphore):
        for axis in range(AXES):
            for role in ROLES:
                pl.semaphore_signal(semaphore, inc=1, device_id=self.device(axis, role, A), device_id_type=MESH)
        pl.semaphore_signal(semaphore, inc=1, device_id=self.partner(), device_id_type=MESH)


def enter(chip):
    barrier = pltpu.get_barrier_semaphore()
    chip.signal_partners(barrier)
    pl.semaphore_wait(barrier, PARTNERS)


def remote(src, dst, send_sem, recv_sem, device):
    return pltpu.make_async_remote_copy(src_ref=src, dst_ref=dst, send_sem=send_sem, recv_sem=recv_sem, device_id=device,
                                        device_id_type=MESH)


def start(copies):
    for copy in copies:
        copy.start()
    return copies


def wait(copies):
    for copy in copies:
        copy.wait()


def loop(count):
    return pl.loop(0, count)


def halves(body):
    loop(len(HALVES))(body)


def parity(n):
    return lax.rem(n, 2)


def pool(sems):
    return (sems.at[n] for n in range(sems.shape[0]))


def contract(a, b, a_axis, b_axis):
    return lax.dot_general(a, b, (((a_axis,), (b_axis,)), ((), ())), preferred_element_type=F32)


def dot(a, b):
    return contract(a, b, 1, 0)


def dot_t(a, b):
    return contract(a, b, 1, 1)


def row_sum(x):
    return jnp.sum(x, axis=1, keepdims=True)


def column_sum(x):
    return jnp.sum(x, axis=0, keepdims=True)


def rounded(x):
    return x.astype(BF16).astype(F32)


def lanes(first, width=PAIR):
    return pl.ds(pl.multiple_of(first, PAIR), width)


def turn(x, cos, sin_a, sin_b):
    return x * cos + pltpu.roll(x, PAIR - ROWS, 1) * sin_a + pltpu.roll(x, ROWS, 1) * sin_b


def turn_back(d, cos, sin_a, sin_b):
    return d * cos + pltpu.roll(d * sin_a, ROWS, 1) + pltpu.roll(d * sin_b, PAIR - ROWS, 1)


def iota(shape, axis):
    return lax.broadcasted_iota(jnp.int32, shape, axis)


def block_rows(j):
    return slice(j * PAIR, (j + 1) * PAIR)


def split_heads(x):
    first = iota((PAIR, PAIR), 1) < HEAD
    rows = []
    for j in range(N_BLOCKS):
        block = x[block_rows(j)]
        rows += [jnp.where(first, block, jnp.zeros_like(block)), jnp.where(first, jnp.zeros_like(block), block)]
    return jnp.concatenate(rows, axis=0)


def total_of(chunks, join=jnp.add):
    return functools.reduce(join, chunks)


def probabilities(q_block, keys, i):
    scores = dot_t(q_block, keys)
    causal = iota((PAIR, PAIR), 0) >= iota((PAIR, PAIR), 1)
    chunks = [scores[:, block_rows(j)] * SCALE for j in range(CORES * (i + 1))]
    for head in HALVES:
        mine = slice(head, None, CORES)
        *ahead, last = chunks[mine]
        held = ahead + [jnp.where(causal, last, -1e30)]
        top = jnp.max(total_of(held, jnp.maximum), axis=1, keepdims=True)
        held = [jnp.exp(chunk - top) for chunk in held]
        inverse = 1.0 / row_sum(total_of(held))
        chunks[mine] = [chunk * inverse for chunk in held]
    return chunks


def side_by_side(chunks):
    return jnp.concatenate([chunk.astype(BF16) for chunk in chunks], axis=1)


def row_mean(x):
    return jnp.mean(x, axis=1, keepdims=True)


def normalised(h):
    center = h - row_mean(h)
    inverse = lax.rsqrt(row_mean(center * center) + EPSILON)
    return center * inverse, inverse


def half_copies(chip, src, dst, own_sem, send_sem, recv_sem):
    width = dst.shape[-1]
    mine, away = [src.at[:, lanes(which * width, width)] for which in (chip.core, chip.other)]
    place = dst.at[chip.core]
    return [pltpu.make_async_copy(mine, place, own_sem), remote(away, place, send_sem, recv_sem, chip.partner())]


class Gather:
    def __init__(self, chip, shards, fulls, sems):
        self.chip, self.shards, self.fulls = chip, shards, fulls
        self.send_sem, self.recv_sem, self.pass_send, self.pass_recv = sems

    def box(self, layer, k, half, stage, role, own=False):
        width = self.fulls[k].shape[-1] // len(HALVES)
        cols = lanes(half * width, width)
        if own:
            return self.shards[k].at[layer, :, cols]
        where = list(self.chip.where)
        for axis in ORDERS[k][:stage]:
            where[axis] = pl.ds(0, SIDE)
        axis = ORDERS[k][stage]
        where[axis] = self.chip.at(axis, role, half)
        return self.fulls[k].at[layer, where[0], where[1], where[2], self.chip.core, :, cols]

    def reach(self, layer, k, half, stage, step):
        slot, on = AXES * stage + step, stage > A and step == C
        src = self.box(layer, k, half, stage, ONE if on else OWN, stage == A)
        return remote(src, self.box(layer, k, half, stage, ONE if on else OWN), self.send_sem.at[layer, k, stage],
                      self.recv_sem.at[layer, k, half, slot], self.chip.device(ORDERS[k][stage], TWO if on else ROLES[step], half))

    def passing(self, layer, k, half, stage, step):
        role = (*ROLES, OWN)[step]
        return remote(self.box(layer, k, half, stage, role, step == SELF), self.box(layer, k, half, stage, role),
                      self.pass_send.at[layer, k], self.pass_recv.at[layer, k], self.chip.partner())

    def each(self, action):
        for k in (MIX, UP, DOWN):
            @halves
            def _(half):
                action(k, half)

    def begin(self, layer, stage):
        for step in range(C if stage else AXES):
            self.each(lambda k, half: self.reach(layer, k, half, stage, step).start())

    def own(self, layer):
        self.each(lambda k, half: self.passing(layer, k, half, A, SELF).start())

    def middle(self, layer, stage):
        def action(k, half):
            self.reach(layer, k, half, stage, A).wait_recv()
            self.reach(layer, k, half, stage, C).start()
            self.passing(layer, k, half, stage, A).start()
        self.each(action)

    def end(self, layer, stage, steps=range(AXES)):
        def action(k, half):
            for step in steps:
                self.reach(layer, k, half, stage, step).wait_recv()
                self.passing(layer, k, half, stage, step).start()
        self.each(action)

    def arrived(self, layer, k):
        box = self.fulls[k].at[layer, :, :, :, self.chip.other]
        remote(box, box, self.pass_send.at[layer, k], self.pass_recv.at[layer, k], self.chip.partner()).wait_recv()

    def left(self):
        three, full = pl.ds(0, AXES), self.fulls[UP].at[A]
        boxes = (full.at[three, A, A, A], full.at[:, three, A, A], full.at[:, :, three, A])

        @loop(LAYERS)
        def _(layer):
            @loop(AXES)
            def _(k):
                for stage, box in enumerate(boxes):
                    sem = self.send_sem.at[layer, k, stage]
                    remote(box, box, sem, sem, self.chip.partner()).wait_send()
                box, sem = full.at[:, :, :, A], self.pass_send.at[layer, k]
                remote(box, box, sem, sem, self.chip.partner()).wait_send()


def pick_lanes(sel_lane, cols):
    return (iota((PAIR, WIDTH), 0) == sel_lane[:, cols]).astype(F32).astype(BF16)


def vector_blocks():
    return [slice(k * WIDTH, (k + 1) * WIDTH) for k in range(N_VEC // WIDTH)]


def unpack_vectors(small_v, layer, sel_shard, sel_lane, vec_ref):
    tiles = small_v[...].astype(F32).reshape((SHARDS, ROWS, PAIR))
    held = jnp.sum(jnp.where(iota(tiles.shape, 1) == layer, tiles, 0.0), axis=1).astype(BF16)
    for cols in vector_blocks():
        spread = dot(held, pick_lanes(sel_lane, cols))
        spread = jnp.where(iota((SHARDS, WIDTH), 0) == sel_shard[:, cols], spread, 0.0)
        vec_ref[layer:layer + 1, cols] = column_sum(spread)


def forward_kernel(x_hbm, ycot_hbm, tables_hbm, places_hbm, up_s, down_s, mix_s, small_ref, up_f, down_f, mix_f, small_full, vec_ref,
                   dout_cols, y_hbm, h_hbm, n1_hbm, n2_hbm, ctx_hbm, act_hbm, qkv_hbm, pre_hbm, up_v, down_v, mix_v, small_v, acc, pre_v,
                   n1_v, n2_v, qkv_v, ctx_v, y_v, n1_t, n2_t, ctx_t, act_t, send_sem, recv_sem, pass_send, pass_recv,
                   small_send, small_recv, own_sems, load_sem, save_sem, share_send, share_recv, act_save, act_send, act_recv, tables,
                   places):
    shards, fulls, own_sem = (up_s, down_s, mix_s), (up_f, down_f, mix_f), pool(own_sems)
    chip = Chip()
    gather = Gather(chip, shards, fulls, (send_sem, recv_sem, pass_send, pass_recv))

    def small_copy(slot, where, device):
        place = small_full.at[(*where, chip.core)]
        return remote(place, place, small_send.at[slot], small_recv.at[slot], device)

    def small_reach(stage, step):
        where = list(chip.where)
        for axis in range(stage):
            where[axis] = pl.ds(0, SIDE)
        return small_copy(AXES * stage + step, where, chip.device(stage, ROLES[step], A))

    def small_begin(stage):
        start([small_reach(stage, step) for step in range(AXES)])

    def small_end(stage):
        for step in range(AXES):
            small_reach(stage, step).wait_recv()

    small_pass = small_copy(AXES * AXES, [pl.ds(0, SIDE)] * AXES, chip.partner())
    here = (*chip.where, chip.core)
    own = [pltpu.make_async_copy(small_ref, small_full.at[here], next(own_sem))]
    for shard, full in zip(shards, fulls):
        for layer in range(LAYERS):
            own.append(pltpu.make_async_copy(shard.at[layer], full.at[(layer, *here)], next(own_sem)))
    loads = [
        pltpu.make_async_copy(src, dst, next(own_sem)) for src, dst in ((x_hbm, y_v), (ycot_hbm, n1_v), (tables_hbm, tables), (places_hbm, places))]
    cot_copies = half_copies(chip, n1_v, dout_cols.at[LAYERS - 1], next(own_sem), next(own_sem), next(own_sem))
    start(own)
    start(loads)
    with jax.named_scope('enter'):
        enter(chip)
    with jax.named_scope('ag0'):
        gather.begin(A, A)
        gather.begin(B, A)
        wait(own)
        small_begin(A)
        gather.own(A)
        gather.own(B)
        gather.end(A, A)
    with jax.named_scope('ag1'):
        gather.begin(A, B)
        small_end(A)
        small_begin(B)
        gather.end(B, A)
        gather.begin(B, B)
        gather.middle(A, B)
        small_end(B)
        small_begin(C)
        gather.middle(B, B)
        gather.end(A, B, (B, C))
    with jax.named_scope('ag2_start'):
        gather.begin(A, C)
        small_end(C)
        small_pass.start()
        gather.end(B, B, (B, C))
    with jax.named_scope('ag2_middle'):
        gather.middle(A, C)
        gather.begin(B, C)
    with jax.named_scope('unpack'):
        small_pass.wait_recv()
        fetch = pltpu.make_async_copy(small_full, small_v, next(own_sem))
        fetch.start()
        fetch.wait()
        wait(loads)
        start(cot_copies)
        for layer in range(LAYERS):
            unpack_vectors(small_v, layer, places[A:B], places[B:C], vec_ref)
    with jax.named_scope('ag2_late'):
        gather.end(A, C, (B,))
    with jax.named_scope('ag2_end'):
        gather.end(A, C, (C,))
        wait(cot_copies)

    def saves(layer):
        pairs = [(y_v, h_hbm.at[layer]), (qkv_v, qkv_hbm.at[layer])]
        kept = [pltpu.make_async_copy(src, dst, save_sem.at[n]) for n, (src, dst) in enumerate(pairs)]
        for n, (src, dst) in enumerate(((n1_t, n1_hbm), (n2_t, n2_hbm), (ctx_t, ctx_hbm))):
            dst = dst.at[layer, chip.core]
            kept.append((pltpu.make_async_copy(src, dst, save_sem.at[CORES + n]),
                         remote(src, dst, share_send.at[layer, n], share_recv.at[layer, n], chip.partner())))
        return kept

    def quarter(layer, t):
        rows, tiles = pl.ds(t * WIDTH, WIDTH), pl.ds(CORES * t, CORES)
        src, dst = act_t.at[rows], act_hbm.at[layer, chip.core, rows]
        return [pltpu.make_async_copy(pre_v.at[tiles], pre_hbm.at[layer, tiles], act_save.at[A, t]),
                pltpu.make_async_copy(src, dst, act_save.at[B, t]),
                remote(src, dst, act_send.at[layer, t], act_recv.at[layer, t], chip.partner())]

    def settle(layer):
        _, qkv_save, *shares = saves(layer)
        qkv_save.wait()
        for share in shares:
            wait(share)

        @loop(SIDE)
        def _(t):
            wait(quarter(layer, t))

    @loop(LAYERS)
    def _(layer):
        def vector(k, first=0, width=None):
            return vec_ref[pl.ds(layer, 1), lanes(OFFSETS[k] + first, width or SIZES[k])]

        def load(k, piece):
            if k == DOWN:
                return pltpu.make_async_copy(fulls[k].at[layer, piece], down_v.at[piece], load_sem.at[k, piece])
            cols = lanes(piece * WIDTH, WIDTH)
            return pltpu.make_async_copy(fulls[k].at[layer, :, :, :, :, :, cols], (up_v, None, mix_v)[k].at[:, :, :, :, :, cols],
                                         load_sem.at[k, piece])

        def matrix(held, piece):
            return held[:, :, :, :, :, lanes(piece * WIDTH, WIDTH)].reshape((WIDTH, WIDTH))

        def have(k):
            gather.arrived(layer, k)

        def meanwhile(action):
            @pl.when(layer == A)
            def _():
                action()

        h_save, qkv_save, n1_share, n2_share, ctx_share = saves(layer)
        with jax.named_scope('have_mix'):
            have(MIX)
            start([load(MIX, k) for k in range(SIDE)])

        h_save.start()

        @pl.when(layer == B)
        def _():
            settle(A)

        with jax.named_scope('ln'):
            @loop(SEQ // LN_ROWS)
            def _(r):
                rows = pl.ds(pl.multiple_of(r * LN_ROWS, LN_ROWS), LN_ROWS)
                scaled, _ = normalised(y_v[rows, :].astype(F32))
                n1_v[rows, :] = (scaled * vector(GAIN1) + vector(BIAS1)).astype(BF16)
                n2_v[rows, :] = (scaled * vector(GAIN2) + vector(BIAS2)).astype(BF16)

        for src, dst, share in ((n1_v, n1_t, n1_share), (n2_v, n2_t, n2_share)):
            dst[...] = src[...].T
            start(share)

        with jax.named_scope('qkv'):
            for k in range(PARTS):
                load(MIX, k).wait()
                x = dot(n1_v[...], matrix(mix_v, k)) + vector(QKV_BIAS, k * WIDTH, WIDTH)
                for c in range(N_PAIRS):
                    block = x[:, block_rows(c)]
                    if k < C:
                        block = turn(block, *[tables[n] for n in range(PARTS)])
                    qkv_v[:, lanes(k * WIDTH + c * PAIR)] = block.astype(BF16)

        qkv_save.start()
        with jax.named_scope('have_up'):
            have(UP)
            have(DOWN)

        start([load(UP, k) for k in range(SIDE)] + [load(DOWN, k) for k in range(SIDE)])
        with jax.named_scope('fattn'):
            def one_pair(pair):
                keys = split_heads(qkv_v[:, lanes(WIDTH + pair * PAIR)])
                values = split_heads(qkv_v[:, lanes(C * WIDTH + pair * PAIR)])
                for i in range(N_BLOCKS):
                    n = (i + 1) * CORES * PAIR
                    probs = probabilities(qkv_v[block_rows(i), lanes(pair * PAIR)], keys[:n], i)
                    ctx_v[block_rows(i), lanes(pair * PAIR)] = dot(side_by_side(probs), values[:n]).astype(BF16)

            @loop(N_PAIRS // CORES)
            def _(two):
                for k in HALVES:
                    one_pair(CORES * two + k)

                @pl.when((layer == A) & (two == A))
                def _():
                    gather.middle(B, C)

        ctx_t[...] = ctx_v[...].T
        start(ctx_share)
        with jax.named_scope('fout'):
            load(MIX, PARTS).wait()
            acc[...] = y_v[...].astype(F32) + dot(ctx_v[...], matrix(mix_v, PARTS)) + (vector(OUT_BIAS) + vector(DOWN_BIAS))

        with jax.named_scope('fmlp'):
            @loop(SIDE)
            def _(t):
                cols = lanes(t * WIDTH, WIDTH)
                load(UP, t).wait()
                pre = dot(n2_v[...], matrix(up_v, t)) + vector(UP_BIAS, t * WIDTH, WIDTH)
                for k in HALVES:
                    pre_v[CORES * t + k] = pre[:, k * TILE:(k + 1) * TILE]
                act = (0.5 * pre * (1.0 + lax.erf(pre * INV_SQRT2))).astype(BF16)
                act_t[cols, :] = act.T
                start(quarter(layer, t))
                load(DOWN, t).wait()
                acc[...] += dot(act, down_v[t].reshape((WIDTH, WIDTH)))

                @pl.when((layer == A) & (t == B))
                def _():
                    gather.end(B, C, (B,))

        h_save.wait()
        y_v[...] = acc[...].astype(BF16)
        with jax.named_scope('fend'):
            meanwhile(lambda: gather.end(B, C, (C,)))

    with jax.named_scope('ftail'):
        last = pltpu.make_async_copy(y_v, y_hbm, next(own_sem))
        last.start()
        for stage in range(AXES):
            for step in range(AXES):
                small_reach(stage, step).wait_send()
        small_pass.wait_send()
        gather.left()
        settle(LAYERS - 1)
        last.wait()


def forward(x, y_cot, shards, small_tile, tables, places):
    grid = CHIPS + (CORES,)
    full = [(LAYERS,) + grid + tensor.shape[1:] for tensor in shards]
    shapes = [(shape, BF16) for shape in full] + [(grid + small_tile.shape, BF16), ((LAYERS, N_VEC), F32), ((LAYERS, CORES, SEQ, TILE), BF16), ((SEQ, WIDTH), BF16),
                                                  ((LAYERS, SEQ, WIDTH), BF16)]
    shapes += [((LAYERS, CORES, width, SEQ), BF16) for width in (WIDTH, WIDTH, WIDTH, HIDDEN)]
    shapes += [((LAYERS, SEQ, QKV), BF16), ((LAYERS, N_TILES, SEQ, TILE), F32)]
    dma = pltpu.SemaphoreType.DMA
    slots = AXES * AXES
    scratch = [pltpu.VMEM(shape[1:], BF16) for shape in full] + [pltpu.VMEM(grid + small_tile.shape, BF16)]
    scratch += [pltpu.VMEM((SEQ, WIDTH), F32), pltpu.VMEM((N_TILES, SEQ, TILE), F32)]
    scratch += [pltpu.VMEM((SEQ, width), BF16) for width in (WIDTH, WIDTH, QKV, WIDTH, WIDTH)]
    scratch += [pltpu.VMEM((width, SEQ), BF16) for width in (WIDTH, WIDTH, WIDTH, HIDDEN)]
    scratch += [dma(shape) for shape in ((LAYERS, AXES, AXES), (LAYERS, AXES, len(HALVES), slots), (LAYERS, AXES), (LAYERS, AXES))]
    scratch += [dma(shape) for shape in ((slots + 1,), (slots + 1,), (slots + SIDE + SIDE + AXES,), (AXES, SIDE), (SIDE + 1,), (LAYERS, AXES), (LAYERS, AXES), (CORES, SIDE), (LAYERS, SIDE), (LAYERS, SIDE))]
    scratch += [pltpu.VMEM(tables.shape, F32), pltpu.VMEM(places.shape, jnp.int32)]
    out_specs = [IN_VMEM if dtype == F32 and len(shape) == LAYERS else ANY for shape, dtype in shapes]
    return pl.pallas_call(
        forward_kernel,
        out_shape=[jax.ShapeDtypeStruct(*s) for s in shapes],
        in_specs=[ANY] * SIDE + [IN_VMEM] * SIDE,
        out_specs=out_specs,
        scratch_shapes=scratch,
        compiler_params=pltpu.CompilerParams(collective_id=0, has_side_effects=True, vmem_limit_bytes=VMEM_LIMIT),
        name='forward_layers',
    )(x, y_cot, tables, places, *shards, small_tile)


WAVES = ((384, 384, 512), (384, 384, 256), (256, 256, 256))
LEADS = ((2,) + CHIPS[1:], CHIPS[1:], (2, SIDE), (SIDE,), (AXES,))
W_UP, W_DOWN, W_QKV, W_OUT = range(4)
STEPS = ((1, (2,)), (0, ()), (2, (4, 3)), (4, (5,)), (3, ()), (5, (6, 7, 8)), (8, (9,)), (9, ()))
LAST = AXES * AXES
CARRIED = ((0, 6, 0), (1, 4, 0), (2, 0, 0))
US_COLUMN, US_HOP, US_ADD, US_STEP = 0.022, 2.5, 0.0013, 0.2
US_FIRST, US_OUT, US_TILE, US_GRADIENT, US_PAIR, US_NORM = 2, 1.4, 1.6, 0.0035, 3.6, 2.7


class Schedule:
    def __init__(self):
        self.now, self.free, self.lines = 0.0, {}, []

    def send(self, link, columns):
        self.free[link] = max(self.free.get(link, 0.0), self.now) + columns * US_COLUMN
        return self.free[link] + US_HOP

    def due(self, limit):
        found = []
        while self.lines:
            line = min(self.lines, key=lambda one: one[A][A]())
            ready = line[A][A]()
            if limit is not None and ready > limit:
                break
            _, run, sends, cost = line.pop(A)
            self.lines = [one for one in self.lines if one]
            self.now = max(self.now, ready) + cost
            sends()
            found.append(run)
        return found

    def finish(self, line):
        while line:
            ready, run, sends, cost = line.pop(A)
            self.now = max(self.now, ready()) + cost
            sends()
            run()
        self.lines = [one for one in self.lines if one]

    def run(self, limit):
        for step in self.due(limit):
            step()

    def passed(self, cost):
        self.now += cost
        self.run(self.now)

    def hooks(self, count, cost):
        planned = []
        for _ in range(count):
            self.now += cost
            planned.append(self.due(self.now))
        return planned


def at_hooks(n, planned):
    for when, steps in enumerate(planned):
        if steps:
            @pl.when(n == when)
            def _():
                for step in steps:
                    step()


def add_into(dst, src, n_axes):
    if n_axes < 2:
        dst[...] += src[...]
        return

    @loop(SIDE)
    def _(k):
        dst[k] += src[k]


def at_axis(ref, axis, value, n_axes):
    every = [pl.ds(0, SIDE)] * n_axes
    every[axis] = value
    return ref.at[tuple(every)]


class Reduce:
    def __init__(self, chip, schedule, wave, grads, came, fin, sems, spare, write, done, when=None):
        self.wave, self.chip, self.schedule, self.widths, self.grads = wave, chip, schedule, WAVES[wave], grads
        self.came, self.fin, (self.send_sem, self.recv_sem), (self.spare, self.spare_sem) = came, fin, sems, spare
        self.write, self.done, self.when, self.times = write, done, when, {}

    def box(self, a, half, stage):
        order = ORDERS[a]
        ref = self.came[a][A].at[half, A]
        spot = [axis for axis in range(AXES) if axis != order[A]].index(order[B])
        if stage == B:
            return ref, spot, C
        return at_axis(ref, spot, self.chip.where[order[B]], C), A, B

    def copy(self, a, half, slot):
        stage, turn = divmod(slot, AXES)
        sems = self.send_sem.at[a, stage], self.recv_sem.at[a, half, slot]
        if slot == LAST:
            return remote(self.total(a, half).at[self.chip.other], self.fin[a].at[half], *sems, self.chip.partner())
        axis = ORDERS[a][stage]
        if stage == C:
            role = value = ROLES[turn]
            dst = self.came[a][SIDE].at[half, turn]
        else:
            role, value = TWO if turn == C else ONE, (ONE, CROSS, TWO)[turn]
            dst = self.came[a][CORES * stage + turn // C].at[half]
            dst = dst if turn == C else dst.at[turn]
        value = self.chip.at(axis, value, half)
        if stage:
            ref, spot, n_axes = self.box(a, half, stage)
            src = at_axis(ref, spot, value, n_axes)
        else:
            src = self.came[a][A].at[half, B] if turn == C else at_axis(self.grads[a].at[half], axis, value, AXES)
        return remote(src, dst, *sems, self.chip.device(axis, role, half))

    def each(self, action):
        for a in range(AXES):
            halves(lambda half: action(a, half))

    def sending(self, slot):
        stage = slot // AXES
        share = SIDE ** (CORES * stage)
        self.times[slot] = self.schedule.now + US_HOP if slot == LAST else max(
            self.schedule.send(ORDERS[a][stage], self.widths[a] / share) for a in range(AXES))

    def begin(self):
        for slot in (B, A):
            self.each(lambda a, half: self.copy(a, half, slot).start())

    def plan(self, first=0, last=None, late=0):
        for slot in (B, A):
            self.times[slot] = self.schedule.now + late
            if not first:
                self.sending(slot)
        for _, sent in STEPS[:first]:
            self.times.update((slot, self.schedule.now + late + US_HOP) for slot in sent)
        line = [
            (lambda slot=slot: self.times[slot], lambda k=k: self.step(k), lambda sent=sent: [self.sending(n) for n in sent],
             CORES * US_ADD * sum(self.widths) if k < C else US_STEP) for k, (slot, sent) in enumerate(STEPS)][first:last]
        self.schedule.lines.append(line)
        return line

    def step(self, k):
        def work():
            with jax.named_scope(f'w{self.wave}s{k}'):
                (self.first, self.first, self.halve, self.settle, self.settle, self.spread, self.cross, self.finish)[k](STEPS[k][A])
        if self.when is None:
            work()
        else:
            pl.when(self.when)(work)

    def held(self, a, half):
        ref = self.spare[A].at[a] if a < C else self.spare[B]
        return ref.at[half, :, :, :, :, pl.ds(0, self.widths[a])]

    def first(self, slot):
        def local(a, half):
            axis = ORDERS[a][A]
            return pltpu.make_async_copy(at_axis(self.grads[a].at[half], axis, self.chip.at(axis, TWO if slot else OWN, half), AXES),
                                         self.held(a, half), self.spare_sem.at[a, half])

        def action(a, half):
            local(a, half).wait()
            self.copy(a, half, slot).wait_recv()
            add_into(self.came[a][A].at[half, slot], self.held(a, half), C)
            if slot:
                self.copy(a, half, C).start()

        self.each(lambda a, half: local(a, half).start())
        self.each(action)

    def halve(self, slot):
        def action(a, half):
            ref, spot, n_axes = self.box(a, half, B)
            self.copy(a, half, slot).wait_recv()
            for turn, role in ((B, CROSS), (A, ONE), (C, TWO), (C, OWN)):
                value = self.chip.at(ORDERS[a][B], role, half)
                add_into(at_axis(ref, spot, value, n_axes), at_axis(self.came[a][B].at[half], spot, value, n_axes), B)
                if turn < C:
                    self.copy(a, half, AXES + turn).start()
        self.each(action)

    def settle(self, slot):
        def action(a, half):
            ref, spot, n_axes = self.box(a, half, B)
            self.copy(a, half, slot).wait_recv()
            value = self.chip.at(ORDERS[a][B], TWO if slot > AXES else OWN, half)
            add_into(at_axis(ref, spot, value, n_axes), self.came[a][C].at[half, slot - AXES], B)
            if slot > AXES:
                self.copy(a, half, AXES + C).start()
        self.each(action)

    def spread(self, slot):
        def action(a, half):
            ref, *_ = self.box(a, half, C)
            self.copy(a, half, slot).wait_recv()
            add_into(ref, self.came[a][AXES].at[half], B)
            for turn in range(AXES):
                self.copy(a, half, CORES * AXES + turn).start()
        self.each(action)

    def total(self, a, half):
        ref, *_ = self.box(a, half, C)
        return ref.at[self.chip.where[ORDERS[a][C]]]

    def cross(self, _):
        def action(a, half):
            for turn in range(AXES):
                self.copy(a, half, CORES * AXES + turn).wait_recv()
            self.total(a, half)[...] += total_of([self.came[a][SIDE][half, turn] for turn in range(AXES)])
            self.copy(a, half, LAST).start()
        self.each(action)

    def finish(self, _):
        def action(a, half):
            self.write(a, half, self.chip.core, self.total(a, half)[self.chip.core])
            self.copy(a, half, LAST).wait_recv()
            self.write(a, half, self.chip.other, self.fin[a][half])
        self.each(action)
        three = pl.ds(0, AXES)
        for a, (grad, fin) in enumerate(zip(self.grads, self.fin)):
            for stage, block in enumerate((grad.at[:, :, :, three], grad.at[:, :, three, A], grad.at[:, three, A, A], fin)):
                sem = self.send_sem.at[a, stage]
                remote(block, block, sem, sem, self.chip.partner()).wait_send()
        self.done()


class VectorSum:
    def __init__(self, chip, schedule, total, came, sems, finish, when=None):
        self.schedule, self.total, self.came, self.sems, self.finish, self.when, self.ready = schedule, total, came, sems, finish, when, 0.0
        self.devices = [[chip.device(axis, role, A) for role in ROLES] for axis in range(AXES)] + [[chip.partner()]]

    def copies(self, k):
        return [remote(self.total, self.came.at[AXES * k + n], self.sems.at[A, AXES * k + n], self.sems.at[B, AXES * k + n], device)
                for n, device in enumerate(self.devices[k])]

    def sending(self, k):
        if k < SIDE:
            self.ready = self.schedule.send(k, N_VEC / (SIDE * SIDE * ROWS))

    def step(self, k):
        def work():
            with jax.named_scope(f'vec{k}'):
                wait(self.copies(k - 1))
                for n in range(len(self.devices[k - 1])):
                    self.total[...] += self.came[AXES * (k - 1) + n]
            if k < SIDE:
                start(self.copies(k))
            else:
                self.finish()
        if self.when is None:
            work()
        else:
            pl.when(self.when)(work)

    def begin(self):
        start(self.copies(A))

    def plan(self):
        self.sending(A)
        self.schedule.lines.append([
            (lambda: self.ready, lambda k=k: self.step(k), lambda k=k: self.sending(k), US_STEP) for k in range(1, SIDE + 1)])


def backward_kernel(ycot_hbm, tables, vec_ref, places, up_hbm, down_hbm, mix_hbm, h_hbm, n1_hbm, n2_hbm, ctx_hbm,
                    act_hbm, qkv_hbm, pre_hbm, _, dx_hbm, small_ref, up_sum, down_sum, qkv_sum, out_sum, dout_cols, dpre_cols,
                    dqkv_cols, *refs):
    n_arrays, sums = AXES * len(WAVES), (up_sum, down_sum, qkv_sum, out_sum)
    grads, refs = refs[:n_arrays], refs[n_arrays:]
    (spare, spare_wide, tile_v, big_v, rhs_v, wup_v, wdown_v, pre_v, dn1, dn2, dctx, dk_acc, dv_acc, qkv_v, dpre_v, dqkv_v, dh_v, h_v,
     totals, came_vec, send_sem, recv_sem, spare_sem, tile_sem, big_sem, rhs_sem, mlp_sem, io_sem, own_sem, share_send,
     share_recv, pre_sem, vec_sem, credit, *refs) = refs
    fins, came = refs[:n_arrays], refs[n_arrays:]
    first_in = pltpu.make_async_copy(ycot_hbm, dh_v, io_sem.at[A])
    first_in.start()
    chip = Chip()
    core, other = chip.core, chip.other

    def exchange(layer, k, src, dst):
        return half_copies(chip, src, dst.at[layer], own_sem.at[k], share_send.at[k], share_recv.at[k])

    def tokens_load(layer, src, part, slot):
        return [pltpu.make_async_copy(src.at[layer, k, pl.ds(part * WIDTH, WIDTH)], big_v.at[slot, :, pl.ds(k * SEQ, SEQ)],
                                      big_sem.at[slot, k]) for k in range(CORES)]

    def weight_load(layer, k, slot):
        return pltpu.make_async_copy(mix_hbm.at[layer, :, lanes(k * WIDTH, WIDTH)], big_v.at[slot], big_sem.at[slot, CORES])

    def tile_loads(layer, t, slot):
        rows = lanes(t * TILE, TILE)
        pairs = ((down_hbm.at[layer, rows], wdown_v), (pre_hbm.at[layer, t], pre_v), (up_hbm.at[layer, :, rows], wup_v))
        return [pltpu.make_async_copy(src, dst.at[slot], mlp_sem.at[slot, n]) for n, (src, dst) in enumerate(pairs)]

    def input_loads(layer):
        return [pltpu.make_async_copy(qkv_hbm.at[layer], qkv_v, io_sem.at[B]), pltpu.make_async_copy(h_hbm.at[layer], h_v, io_sem.at[C])]

    def rhs_load(layer, src, first, width, k):
        cols = lanes(first, width)
        return [pltpu.make_async_copy(src.at[layer, n, :, cols], rhs_v.at[pl.ds(n * SEQ, SEQ), cols], rhs_sem.at[k, n])
                for n in range(CORES)]

    def prefetch(layer):
        start(tokens_load(layer, ctx_hbm, A, AXES) + tokens_load(layer, act_hbm, A, A))

    def prefetch_more(layer):
        start(tokens_load(layer, act_hbm, B, B) + tokens_load(layer, act_hbm, C, C) + input_loads(layer))
        for t in HALVES:
            start(tile_loads(layer, t, t))

    prefetch(LAYERS - 1)
    start(rhs_load(LAYERS - 1, dout_cols, A, TILE, A))
    prefetch_more(LAYERS - 1)
    with jax.named_scope('enter'):
        enter(chip)
    with jax.named_scope('first_in'):
        first_in.wait()
    dx_copy = pltpu.make_async_copy(dh_v, dx_hbm, io_sem.at[A])

    def vector_at(k, first=0, width=None):
        return lanes(OFFSETS[k] + first, width or SIZES[k])

    def reduction(schedule, layer, wave, when):
        def write(a, half, side, block):
            def put(arr, group, col, first, width):
                size = sums[arr].shape[-1] // CORES
                sums[arr][layer, group, :, lanes(side * size + col, width)] = block[:, first:first + width].astype(BF16)
            width, colour = WAVES[wave][a], CORES * a + half
            if wave:
                first = colour * width if wave == C or a < C else SIDE * WAVES[wave][A] + half * width
                put(W_QKV if wave == C else W_UP, A, first, A, width)
            elif a < C:
                put(W_DOWN, colour, A, A, width)
            else:
                for k in HALVES:
                    put(W_DOWN, CORES * half + k, WAVES[A][A], k * PAIR, PAIR)
                put(W_OUT, A, half * TWICE, TWICE, TWICE)

        def done():
            @pl.when(layer == LAYERS - 1)
            def _():
                chip.signal_partners(credit.at[wave])

        where = slice(AXES * wave, AXES * (wave + 1))
        count = len(LEADS)
        return Reduce(chip, schedule, wave, [grad.at[layer] for grad in grads[where]],
                      [came[count * (AXES * wave + a):count * (AXES * wave + a + 1)] for a in range(AXES)],
                      fins[where], (send_sem.at[wave], recv_sem.at[wave]), ((spare, spare_wide), spare_sem), write, done, when)

    def vector_sum(schedule, layer, when):
        def own_part():
            with jax.named_scope('own'):
                node, local = chip.base
                me = node * (SIDE * CORES) + local + core
                row = jnp.zeros((ROWS, PAIR), F32)
                for k, share in enumerate(SHARES):
                    if k == QKV_BIAS:
                        firsts = [part * WIDTH + lax.div(me, CORES * ROWS) * PAIR for part in range(PARTS)]
                    else:
                        firsts = [lax.div(me * share, PAIR) * PAIR]
                    for first in firsts:
                        cols = lanes(OFFSETS[k] + first)
                        left = jnp.zeros((ROWS, PAIR), F32) + totals[layer, :, cols] * (places[A:B, cols] == me).astype(F32)
                        pick = (iota((PAIR, PAIR), 0) == places[B:C, cols]).astype(F32).astype(BF16)
                        for _ in range(PARTS):
                            row = row + dot_t(left.astype(BF16), pick)
                            left = left - rounded(left)
                small_ref[layer] = row.astype(BF16)

            @pl.when(layer == LAYERS - 1)
            def _():
                chip.signal_partners(credit.at[AXES])

        return VectorSum(chip, schedule, totals.at[layer], came_vec, vec_sem, own_part, when)

    def run_on(schedule, layer, when):
        lines = [reduction(schedule, layer, wave, when).plan(step, late=late) for wave, step, late in CARRIED]
        vector_sum(schedule, layer, when).plan()
        return lines

    @loop(LAYERS + 1)
    def _(turn_no):
        layer = LAYERS - 1 - turn_no
        working = pl.when(turn_no < LAYERS)
        total = totals.at[layer]
        schedule = Schedule()

        carried = run_on(schedule, layer + 1, turn_no > A)

        def product(lhs_slot, first, width, out_slot):
            value = dot(big_v[lhs_slot, :, 0:CORES * SEQ], rhs_v[:, lanes(first, width)])
            tile_v[out_slot, :, :, :, :, :, 0:width] = value.reshape(CHIPS + (CORES, ROWS, width))

        def tile_out(slot, src, dst):
            return pltpu.make_async_copy(src, dst, tile_sem.at[slot])

        def tile_done(slot, width):
            block = tile_v.at[slot, :, :, :, :, :, pl.ds(0, width)]
            tile_out(slot, block, block).wait()

        def columns(wave, a, half, first, width):
            return grads[AXES * wave + a].at[layer, half, :, :, :, :, :, pl.ds(first, width)]

        def launch(wave):
            schedule.finish(carried[wave])

            @pl.when(turn_no == B)
            def _():
                pl.semaphore_wait(credit.at[wave], PARTNERS)

            current = reduction(schedule, layer, wave, turn_no < LAYERS)
            if wave == C:
                @pl.when(turn_no == B)
                def _():
                    pl.semaphore_wait(credit.at[AXES], PARTNERS)

                @working
                def _():
                    vector_sum(schedule, layer, None).begin()

            working(current.begin)
            if wave < C:
                current.plan(last=CARRIED[wave][B])

        @working
        def _():
            with jax.named_scope('dw_out'):
                @pl.when(turn_no == B)
                def _():
                    wait(exchange(layer, A, dh_v, dout_cols))
                    start(rhs_load(layer, dout_cols, A, TILE, A))

                wait(rhs_load(layer, dout_cols, A, TILE, A))
                wait(tokens_load(layer, ctx_hbm, A, AXES))
                product(AXES, A, TILE, B)
                start(tokens_load(layer, act_hbm, AXES, AXES))
                for k in HALVES:
                    tile_out(B, tile_v.at[B, :, :, :, :, :, pl.ds(k * TWICE, TWICE)], columns(A, C, k, TWICE, TWICE)).start()

        schedule.passed(US_FIRST)
        out_hooks = schedule.hooks(SIDE, US_OUT)

        @loop(SIDE)
        def _(z):
            @working
            def _():
                slot = parity(z)
                wait(tokens_load(layer, act_hbm, z, z))

                @pl.when(z > A)
                def _():
                    tile_done(slot, TILE)

                product(z, A, TILE, slot)
                split = WAVES[A][A]
                for k in range(SIDE):
                    a, half = divmod(k, CORES)
                    for c in range(CORES):
                        block = tile_v.at[slot, :, :, CORES * c + a, half]
                        tile_out(slot, block.at[:, :, :, pl.ds(0, split)], grads[a].at[layer, half, z, :, :, c]).start()
                        tile_out(slot, block.at[:, :, :, pl.ds(split, PAIR)],
                                 grads[C].at[layer, a, z, :, :, c, :, pl.ds(half * PAIR, PAIR)]).start()

            at_hooks(z, out_hooks)

        @working
        def _():
            start(tokens_load(layer, n2_hbm, A, A) + [weight_load(layer, k, k + 1) for k in range(PARTS)])
            for slot in HALVES:
                tile_done(slot, TILE)

        schedule.passed(US_STEP)
        launch(A)

        @working
        def _():
            dn2[...] = jnp.zeros_like(dn2)

        def pre_copy(t, slot, away):
            place = dpre_cols.at[layer, core, :, lanes(lax.rem(t, SIDE) * TILE, TILE)]
            if away:
                return remote(dpre_v.at[slot], place, pre_sem.at[A, t], pre_sem.at[B, t], chip.partner())
            return pltpu.make_async_copy(dpre_v.at[slot], place, own_sem.at[CORES + slot])

        def pre_act(t, leave):
            for away, whose in ((False, core), (True, other)):
                @pl.when(lax.div(t, SIDE) == whose)
                def _():
                    copy = pre_copy(t, parity(t), away)
                    if leave:
                        copy.start()
                    elif away:
                        copy.wait_send()
                    else:
                        copy.wait()

        tile_hooks = schedule.hooks(N_TILES, US_TILE)

        with jax.named_scope('mlp'):
            @loop(N_TILES)
            def _(t):
                @working
                def _():
                    slot = parity(t)
                    wait(tile_loads(layer, t, slot))
                    d_act = rounded(dot_t(dh_v[...], wdown_v[slot]))
                    pre = pre_v[slot]
                    slope = 0.5 * (1.0 + lax.erf(pre * INV_SQRT2)) + pre * (INV_SQRT2PI * jnp.exp(-0.5 * pre * pre))
                    d_pre = d_act * slope
                    total[:, vector_at(UP_BIAS, t * TILE, TILE)] = column_sum(d_pre)

                    @pl.when(t > B)
                    def _():
                        pre_act(t - CORES, False)

                    dpre_v[slot] = d_pre.astype(BF16)
                    pre_act(t, True)
                    dn2[...] += dot_t(dpre_v[slot], wup_v[slot])

                    @pl.when(t + CORES < N_TILES)
                    def _():
                        start(tile_loads(layer, t + CORES, slot))

                at_hooks(t, tile_hooks)

        @working
        def _():
            for t in HALVES:
                pre_act(N_TILES - CORES + t, False)
            for t in range(SIDE):
                pre_copy(SIDE * core + t, A, True).wait_recv()

        def gradient_loads(wave, source):
            first = 0
            for a in range(AXES):
                width = CORES * WAVES[wave][a]
                start(rhs_load(layer, source, first, width, a))
                first += width

        def gradient_wave(wave, source, lhs_slot, first, orders):
            split, count = WAVES[wave][orders[A]], len(orders)
            width = CORES * split
            planned = schedule.hooks(count, width * US_GRADIENT)

            @loop(count)
            def _(n):
                @working
                def _():
                    slot = parity(n)
                    wait(rhs_load(layer, source, first + n * width, width, orders[A] + n))

                    @pl.when(n > B)
                    def _():
                        tile_done(slot, width)

                    product(lhs_slot, first + n * width, width, slot)
                    for k, a in enumerate(orders):
                        @pl.when(n == k)
                        def _():
                            for half in HALVES:
                                block = tile_v.at[slot, :, :, :, :, :, pl.ds(half * split, split)]
                                tile_out(slot, block, columns(wave, a, half, 0, split)).start()

                at_hooks(n, planned)

            @working
            def _():
                for slot in range(min(count, CORES)):
                    tile_done(slot, width)

        @working
        def _():
            gradient_loads(B, dpre_cols)
            wait(tokens_load(layer, n2_hbm, A, A))

        with jax.named_scope('dw1'):
            gradient_wave(B, dpre_cols, A, A, (A, B))
            gradient_wave(B, dpre_cols, A, SIDE * WAVES[B][A], (C,))
        launch(B)
        @working
        def _():
            weight_load(layer, AXES, A).start()
            d_sum = column_sum(dh_v[...].astype(F32))
            total[:, vector_at(OUT_BIAS)] = d_sum
            total[:, vector_at(DOWN_BIAS)] = d_sum
            wait(input_loads(layer))
            weight_load(layer, AXES, A).wait()
            dctx[...] = dot_t(dh_v[...], big_v[A]).astype(BF16)

        pair_hooks = schedule.hooks(N_PAIRS // CORES, US_PAIR)

        with jax.named_scope('attn'):
            def one_pair(pair, dk_sum, dv_sum):
                at = lanes(pair * PAIR)
                keys = split_heads(qkv_v[:, lanes(WIDTH + pair * PAIR)])
                values = split_heads(qkv_v[:, lanes(C * WIDTH + pair * PAIR)])
                q_t = qkv_v[:, at].T
                dc_t = dctx[:, at].T
                bias_sums = [jnp.zeros((1, PAIR), F32)] * PARTS

                def turned_back(n, d, rows, to):
                    d = turn_back(rounded(d), *[tables[k, rows, :] for k in range(PARTS)])
                    bias_sums[n] = bias_sums[n] + column_sum(d)
                    dqkv_v[rows, to] = d.astype(BF16)

                for i in range(N_BLOCKS):
                    old, n = i * TWICE, (i + 1) * TWICE
                    rows = block_rows(i)
                    probs = probabilities(qkv_v[rows, at], keys[:n], i)
                    d_all = rounded(dot_t(dctx[rows, at], values[:n]))
                    d_scores = [d_all[:, block_rows(j)] for j in range(CORES * (i + 1))]
                    for head in HALVES:
                        mine = slice(head, None, CORES)
                        mean = row_sum(total_of([p * d for p, d in zip(probs[mine], d_scores[mine])]))
                        d_scores[mine] = [p * (d - mean) * SCALE for p, d in zip(probs[mine], d_scores[mine])]
                    d_scores, probs = side_by_side(d_scores), side_by_side(probs)
                    turned_back(A, dot(d_scores, keys[:n]), rows, at)
                    for acc, left, right in ((dk_sum, q_t, d_scores), (dv_sum, dc_t, probs)):
                        part = dot(left[:, rows], right)
                        if i:
                            acc[:, :old] += part[:, :old]
                        acc[:, old:n] = part[:, old:]
                first = iota((PAIR, PAIR), 0) < HEAD
                for j in range(N_BLOCKS):
                    rows = block_rows(j)
                    d_key, d_value = [jnp.where(first, acc[:, block_rows(CORES * j)], acc[:, block_rows(CORES * j + 1)]).T
                                      for acc in (dk_sum, dv_sum)]
                    turned_back(B, d_key, rows, lanes(WIDTH + pair * PAIR))
                    d_value = d_value.astype(BF16)
                    bias_sums[C] = bias_sums[C] + column_sum(d_value.astype(F32))
                    dqkv_v[rows, lanes(C * WIDTH + pair * PAIR)] = d_value
                for k, bias_sum in enumerate(bias_sums):
                    total[:, vector_at(QKV_BIAS, k * WIDTH + pair * PAIR, PAIR)] = bias_sum

            @loop(N_PAIRS // CORES)
            def _(two):
                @working
                def _():
                    for k in HALVES:
                        one_pair(CORES * two + k, dk_acc.at[k], dv_acc.at[k])

                at_hooks(two, pair_hooks)

        @working
        def _():
            start(exchange(layer, B, dqkv_v, dqkv_cols))
            dn1[...] = jnp.zeros_like(dn1)

            with jax.named_scope('dn1'):
                @loop(PARTS)
                def _(k):
                    weight_load(layer, k, k + 1).wait()
                    dn1[...] += dot_t(dqkv_v[:, lanes(k * WIDTH, WIDTH)], big_v[k + 1])

            start(tokens_load(layer, n1_hbm, A, B))

        schedule.passed(US_NORM)

        @working
        def _():
            for k in (GAIN1, BIAS1, GAIN2, BIAS2):
                total[:, vector_at(k)] = jnp.zeros((1, WIDTH), F32)

            with jax.named_scope('lnb'):
                @loop(SEQ // LN_ROWS)
                def _(r):
                    rows = pl.ds(pl.multiple_of(r * LN_ROWS, LN_ROWS), LN_ROWS)
                    scaled, inverse = normalised(h_v[rows, :].astype(F32))
                    d1, d2 = rounded(dn1[rows, :]), rounded(dn2[rows, :])
                    for k, value in ((GAIN1, d1 * scaled), (BIAS1, d1), (GAIN2, d2 * scaled), (BIAS2, d2)):
                        total[:, vector_at(k)] += column_sum(value)
                    g1, g2 = [vec_ref[pl.ds(layer, 1), lanes(OFFSETS[k], WIDTH)] for k in (GAIN1, GAIN2)]
                    d_scaled = d1 * g1 + d2 * g2
                    d_h = inverse * (d_scaled - row_mean(d_scaled) - scaled * row_mean(d_scaled * scaled))
                    dh_v[rows, :] = (dh_v[rows, :].astype(F32) + d_h).astype(BF16)

        schedule.passed(US_NORM)
        @working
        def _():
            wait(exchange(layer, B, dqkv_v, dqkv_cols))
            gradient_loads(C, dqkv_cols)
            wait(tokens_load(layer, n1_hbm, A, B))

        @pl.when(turn_no == A)
        def _():
            start(exchange(layer - 1, A, dh_v, dout_cols))

        @pl.when(turn_no == B)
        def _():
            dx_copy.start()

        with jax.named_scope('dw2'):
            gradient_wave(C, dqkv_cols, B, A, (A, B, C))

        @pl.when(turn_no == A)
        def _():
            prefetch(layer - 1)
            prefetch_more(layer - 1)

        schedule.run(None)
        launch(C)

    dx_copy.wait()


def backward(y_cot, tables, vectors, places, weights, saved):
    dma, one = pltpu.SemaphoreType.DMA, (1,)
    pair, wide, row = (len(HALVES),), (SEQ, WIDTH), one + (N_VEC,)
    shapes = [(wide, BF16), ((LAYERS, ROWS, PAIR), BF16)]
    shapes += [((LAYERS, groups, ROWS, width), BF16) for groups, width in ((*one, HIDDEN), (SIDE, WIDTH), (*one, QKV), (*one, WIDTH))]
    in_vmem = len(shapes)
    shapes += [((LAYERS, CORES, SEQ, width), BF16) for width in (TILE, SIDE * TILE, PARTS * TILE)]
    blocks = [(CORES, ROWS, width) for wave in WAVES for width in wave]
    shapes += [((LAYERS,) + pair + CHIPS + block, F32) for block in blocks]
    tile = (CORES, ROWS)
    scratch = [(pair + pair + CHIPS[1:] + tile + (WAVES[0][0],), F32), (pair + CHIPS[1:] + tile + (TILE,), F32), (pair + CHIPS + tile + (CORES * WAVES[0][0],), F32), ((SIDE, WIDTH, WIDTH), BF16), ((CORES * SEQ, SIDE * TILE), BF16)]
    scratch += [(pair + shape, BF16) for shape in ((WIDTH, TILE), (TILE, WIDTH))]
    scratch += [(pair + (SEQ, TILE), F32), (wide, F32), (wide, F32), (wide, BF16)] + [(pair + (PAIR, CORES * SEQ), F32)] * CORES
    scratch += [((SEQ, QKV), BF16), (pair + (SEQ, TILE), BF16), ((SEQ, QKV), BF16), (wide, BF16), (wide, BF16), ((LAYERS,) + row, F32),
                ((PARTNERS,) + row, F32)]
    slots = (len(WAVES), AXES) + pair + (LAST + 1,)
    sems = [dma(shape) for shape in ((len(WAVES), AXES, SIDE), slots, (AXES,) + pair, pair, (SIDE, AXES), (AXES, CORES), pair + (PARTS,), (AXES,),
                                     (SIDE,), pair, pair, pair + (N_TILES,), pair + (PARTNERS,))]
    late = [(pair + block[1:], F32) for block in blocks] + [(pair + lead + block, F32) for block in blocks for lead in LEADS]
    outs = pl.pallas_call(
        backward_kernel,
        out_shape=[jax.ShapeDtypeStruct(*s) for s in shapes],
        in_specs=[ANY] + [IN_VMEM] * AXES + [ANY] * (PARTNERS + 1),
        input_output_aliases={SIDE + PARTNERS: in_vmem},
        out_specs=[ANY] + [IN_VMEM] * (in_vmem - 1) + [ANY] * (len(shapes) - in_vmem),
        scratch_shapes=[pltpu.VMEM(*s) for s in scratch] + sems + [pltpu.SemaphoreType.REGULAR((SIDE,))]
        + [pltpu.VMEM(*s) for s in late],
        compiler_params=pltpu.CompilerParams(collective_id=1, has_side_effects=True, vmem_limit_bytes=VMEM_LIMIT),
        name='backward_layers',
    )(y_cot, tables, vectors, places, *weights, *saved)
    d_x, small, *sums = outs[:in_vmem]
    return d_x, small[:, 0], [s.reshape((LAYERS, -1, s.shape[-1])) for s in sums]


def finish_kernel(*refs):
    n_large = CORES + AXES
    large, small_ref, refs = refs[:n_large], refs[n_large], refs[n_large + 1:]
    outs, small_outs, refs = refs[:n_large], refs[n_large:n_large + len(SHARES)], refs[n_large + len(SHARES):]
    held, sems = refs[:n_large], refs[n_large]
    loads = start([pltpu.make_async_copy(src, dst, sems.at[n]) for n, (src, dst) in enumerate(zip(large, held))])
    first = 0
    for share, out in zip(SHARES, small_outs):
        out[...] = small_ref[:, first:first + share]
        first += share
    stores = []
    for load, src, dst in zip(loads, held, outs):
        load.wait()
        stores += start([pltpu.make_async_copy(src, dst, sems.at[n_large + len(stores)])])
    wait(stores)


def finish(large, small):
    shapes = [jax.ShapeDtypeStruct(t.shape, BF16) for t in large] + [jax.ShapeDtypeStruct((LAYERS, share), BF16) for share in SHARES]
    outs = pl.pallas_call(
        finish_kernel,
        out_shape=shapes,
        in_specs=[ANY] * len(large) + [IN_VMEM],
        out_specs=[ANY] * len(large) + [IN_VMEM] * len(SHARES),
        scratch_shapes=[pltpu.VMEM(t.shape, BF16) for t in large] + [pltpu.SemaphoreType.DMA((CORES * len(large),))],
        name='finish',
    )(*large, small)
    return outs[:len(large)], outs[len(large):]


def rope_tables():
    rot_dim, f32 = HEAD // SIDE, np.float32
    inv_freq = f32(1.0) / f32(10000.0) ** (np.arange(0, rot_dim, 2, dtype=f32) / f32(rot_dim))
    angles = np.arange(SEQ, dtype=f32)[:, None] * inv_freq[None, :]
    cos, sin = np.cos(angles), np.sin(angles)
    zero = np.zeros_like(sin)
    rest = np.zeros((SEQ, HEAD - rot_dim), f32)
    tables = ([cos, cos, rest + f32(1.0)], [-sin, zero, rest], [zero, sin, rest])
    return jnp.asarray(np.stack([np.tile(np.concatenate(table, axis=1), (1, 2)) for table in tables]).astype(f32))


def heads_last(tensor):
    lead = tensor.shape[:-2]
    return tensor.reshape(lead + (HEADS, PARTS, HEAD)).swapaxes(-3, -2).reshape(lead + (QKV,))


def heads_first(tensor):
    lead = tensor.shape[:-1]
    return tensor.reshape(lead + (PARTS, HEADS, HEAD)).swapaxes(-3, -2).reshape(lead + (HEADS, PARTS * HEAD))


def vector_places():
    shard, lane, first = [], [], 0
    for k, (share, size) in enumerate(zip(SHARES, SIZES)):
        place = np.arange(size)
        if k == QKV_BIAS:
            place = heads_last(place.reshape(HEADS, -1))
        shard.append(place // share)
        lane.append(first + place % share)
        first += share
    return jnp.asarray(np.stack([np.concatenate(shard), np.concatenate(lane)]).astype(np.int32))


def solution(mesh):
    shard_axes = ('node', 'local')
    act_spec = P(shard_axes)
    param_spec = P(None, shard_axes)

    def device_step(x, y_cot, ln1_gain, ln1_bias, qkv_weight, qkv_bias, out_weight, out_bias,
                    ln2_gain, ln2_bias, up_weight, up_bias, down_weight, down_bias):
        tables, places = rope_tables(), vector_places()
        small = (ln1_gain, ln1_bias, ln2_gain, ln2_bias, qkv_bias, out_bias, up_bias, down_bias)
        small_tile = jnp.pad(jnp.concatenate(small, axis=1), ((0, ROWS - LAYERS), (0, PAIR - sum(SHARES))))
        mix = jnp.concatenate([heads_last(qkv_weight), out_weight], axis=-1)
        *weights, _, vectors, dout_cols, y_out, hidden, n1, n2, ctx, act, qkv, pre = forward(
            x[0], y_cot[0], (up_weight, down_weight, mix), small_tile, tables, places)
        weights = [tensor.reshape((LAYERS, -1, tensor.shape[-1])) for tensor in weights]
        d_x, small_sums, (up, down, qkv, out) = backward(
            y_cot[0], tables, vectors, places, weights, (hidden, n1, n2, ctx, act, qkv, pre, dout_cols))
        (y_out, d_x, up, down, out), (g1, b1, g2, b2, qb, ob, ub, db) = finish((y_out, d_x, up, down, out), small_sums)
        return (y_out[None], d_x[None], g1, b1, heads_first(qkv), qb, out, ob, g2, b2, up, ub, down, db)

    return jax.shard_map(device_step, mesh=mesh,
                         in_specs=(act_spec, act_spec) + (param_spec,) * 12,
                         out_specs=(act_spec, act_spec) + (param_spec,) * 12,
                         check_vma=False)
```

```python
import functools
import jax
import jax.numpy as jnp
import numpy as np
from jax import lax
from jax.experimental import pallas as pl
from jax.experimental.pallas import tpu as pltpu
from jax.sharding import PartitionSpec as P

BF16, F32 = jnp.bfloat16, jnp.float32
EPSILON = 1e-5
MESH = pl.DeviceIdType.MESH
ANY = pl.BlockSpec(memory_space=pl.ANY)
IN_VMEM = pl.BlockSpec(memory_space=pltpu.VMEM)
VMEM_LIMIT = 67 * 10**6
LAYERS, AXES, SIDE, CORES, ROWS, PARTNERS = 2, 3, 4, 2, 8, 10
CHIPS = (SIDE, SIDE, SIDE)
SHARDS = SIDE * SIDE * SIDE * CORES
SEQ, WIDTH, HIDDEN, TILE, PAIR, LN_ROWS = 384, 1024, 4096, 512, 128, 64
HEADS, HEAD, PARTS = 16, 64, 3
QKV = PARTS * WIDTH
N_TILES, N_PAIRS, N_BLOCKS = HIDDEN // TILE, WIDTH // PAIR, SEQ // PAIR
TWICE = 2 * PAIR
INV_SQRT2, INV_SQRT2PI, SCALE = 0.7071067811865476, 0.3989422804014327, 0.125
SHARES = (8, 8, 8, 8, 24, 8, 32, 8)
SIZES = tuple(SHARDS * share for share in SHARES)
OFFSETS = tuple(sum(SIZES[:k]) for k in range(len(SIZES)))
N_VEC = sum(SIZES)
GAIN1, BIAS1, GAIN2, BIAS2, QKV_BIAS, OUT_BIAS, UP_BIAS, DOWN_BIAS = range(len(SHARES))
ORDERS = ((2, 1, 0), (1, 0, 2), (0, 2, 1))
HALVES = range(2)
OWN, ONE, CROSS, TWO = range(SIDE)
ROLES = (ONE, TWO, CROSS)
A, B, C = range(AXES)
UP, DOWN, MIX = range(3)
SELF = 3


class Chip:
    def __init__(self):
        node, local = lax.axis_index('node'), lax.axis_index('local')
        self.core, self.other = lax.rem(local, CORES), 1 - lax.rem(local, CORES)
        self.where = (lax.div(node, SIDE), lax.rem(node, SIDE), lax.div(local, CORES))
        self.base = (node, local - self.core)
        self.strides = ((SIDE, 0), (1, 0), (0, CORES))
        self.near = [(v, v + 1 - 2 * parity(v), lax.rem(v + 2, SIDE), SIDE - 1 - v) for v in self.where]

        self.gaps = [near[3] - near[1] for near in self.near]

    def at(self, axis, role, half):
        near = self.near[axis]
        if role in (OWN, CROSS):
            return near[role]
        return near[role] + half * self.gaps[axis] if role == ONE else near[role] - half * self.gaps[axis]

    def device(self, axis, role, half):
        shift = self.at(axis, role, half) - self.where[axis]
        node, local = [b + shift * s if s else b for b, s in zip(self.base, self.strides[axis])]
        return (node, local + self.core)

    def partner(self):
        node, local = self.base
        return (node, local + self.other)

    def signal_partners(self, semaphore):
        for axis in range(AXES):
            for role in ROLES:
                pl.semaphore_signal(semaphore, inc=1, device_id=self.device(axis, role, A), device_id_type=MESH)
        pl.semaphore_signal(semaphore, inc=1, device_id=self.partner(), device_id_type=MESH)


def enter(chip):
    barrier = pltpu.get_barrier_semaphore()
    chip.signal_partners(barrier)
    pl.semaphore_wait(barrier, PARTNERS)


def remote(src, dst, send_sem, recv_sem, device):
    return pltpu.make_async_remote_copy(src_ref=src, dst_ref=dst, send_sem=send_sem, recv_sem=recv_sem, device_id=device,
                                        device_id_type=MESH)


def start(copies):
    for copy in copies:
        copy.start()
    return copies


def wait(copies):
    for copy in copies:
        copy.wait()


def loop(count):
    return pl.loop(0, count)


def halves(body):
    loop(len(HALVES))(body)


def parity(n):
    return lax.rem(n, 2)


def pool(sems):
    return (sems.at[n] for n in range(sems.shape[0]))


def contract(a, b, a_axis, b_axis):
    return lax.dot_general(a, b, (((a_axis,), (b_axis,)), ((), ())), preferred_element_type=F32)


def dot(a, b):
    return contract(a, b, 1, 0)


def dot_t(a, b):
    return contract(a, b, 1, 1)


def row_sum(x):
    return jnp.sum(x, axis=1, keepdims=True)


def column_sum(x):
    return jnp.sum(x, axis=0, keepdims=True)


def rounded(x):
    return x.astype(BF16).astype(F32)


def lanes(first, width=PAIR):
    return pl.ds(pl.multiple_of(first, PAIR), width)


def turn(x, cos, sin_a, sin_b):
    return x * cos + pltpu.roll(x, PAIR - ROWS, 1) * sin_a + pltpu.roll(x, ROWS, 1) * sin_b


def turn_back(d, cos, sin_a, sin_b):
    return d * cos + pltpu.roll(d * sin_a, ROWS, 1) + pltpu.roll(d * sin_b, PAIR - ROWS, 1)


def iota(shape, axis):
    return lax.broadcasted_iota(jnp.int32, shape, axis)


def block_rows(j):
    return slice(j * PAIR, (j + 1) * PAIR)


def split_heads(x):
    first = iota((PAIR, PAIR), 1) < HEAD
    rows = []
    for j in range(N_BLOCKS):
        block = x[block_rows(j)]
        rows += [jnp.where(first, block, jnp.zeros_like(block)), jnp.where(first, jnp.zeros_like(block), block)]
    return jnp.concatenate(rows, axis=0)


def total_of(chunks, join=jnp.add):
    return functools.reduce(join, chunks)


def probabilities(q_block, keys, i):
    scores = dot_t(q_block, keys)
    causal = iota((PAIR, PAIR), 0) >= iota((PAIR, PAIR), 1)
    chunks = [scores[:, block_rows(j)] * SCALE for j in range(CORES * (i + 1))]
    for head in HALVES:
        mine = slice(head, None, CORES)
        *ahead, last = chunks[mine]
        held = ahead + [jnp.where(causal, last, -1e30)]
        top = jnp.max(total_of(held, jnp.maximum), axis=1, keepdims=True)
        held = [jnp.exp(chunk - top) for chunk in held]
        inverse = 1.0 / row_sum(total_of(held))
        chunks[mine] = [chunk * inverse for chunk in held]
    return chunks


def side_by_side(chunks):
    return jnp.concatenate([chunk.astype(BF16) for chunk in chunks], axis=1)


def row_mean(x):
    return jnp.mean(x, axis=1, keepdims=True)


def normalised(h):
    center = h - row_mean(h)
    inverse = lax.rsqrt(row_mean(center * center) + EPSILON)
    return center * inverse, inverse


def half_copies(chip, src, dst, own_sem, send_sem, recv_sem):
    width = dst.shape[-1]
    mine, away = [src.at[:, lanes(which * width, width)] for which in (chip.core, chip.other)]
    place = dst.at[chip.core]
    return [pltpu.make_async_copy(mine, place, own_sem), remote(away, place, send_sem, recv_sem, chip.partner())]


class Gather:
    def __init__(self, chip, shards, fulls, sems):
        self.chip, self.shards, self.fulls = chip, shards, fulls
        self.send_sem, self.recv_sem, self.pass_send, self.pass_recv = sems

    def box(self, layer, k, half, stage, role, own=False):
        width = self.fulls[k].shape[-1] // len(HALVES)
        cols = lanes(half * width, width)
        if own:
            return self.shards[k].at[layer, :, cols]
        where = list(self.chip.where)
        for axis in ORDERS[k][:stage]:
            where[axis] = pl.ds(0, SIDE)
        axis = ORDERS[k][stage]
        where[axis] = self.chip.at(axis, role, half)
        return self.fulls[k].at[layer, where[0], where[1], where[2], self.chip.core, :, cols]

    def reach(self, layer, k, half, stage, step):
        slot, on = AXES * stage + step, stage > A and step == C
        src = self.box(layer, k, half, stage, ONE if on else OWN, stage == A)
        return remote(src, self.box(layer, k, half, stage, ONE if on else OWN), self.send_sem.at[layer, k, stage],
                      self.recv_sem.at[layer, k, half, slot], self.chip.device(ORDERS[k][stage], TWO if on else ROLES[step], half))

    def passing(self, layer, k, half, stage, step):
        role = (*ROLES, OWN)[step]
        return remote(self.box(layer, k, half, stage, role, step == SELF), self.box(layer, k, half, stage, role),
                      self.pass_send.at[layer, k], self.pass_recv.at[layer, k], self.chip.partner())

    def each(self, action):
        for k in (MIX, UP, DOWN):
            @halves
            def _(half):
                action(k, half)

    def begin(self, layer, stage):
        for step in range(C if stage else AXES):
            self.each(lambda k, half: self.reach(layer, k, half, stage, step).start())

    def own(self, layer):
        self.each(lambda k, half: self.passing(layer, k, half, A, SELF).start())

    def middle(self, layer, stage):
        def action(k, half):
            self.reach(layer, k, half, stage, A).wait_recv()
            self.reach(layer, k, half, stage, C).start()
            self.passing(layer, k, half, stage, A).start()
        self.each(action)

    def end(self, layer, stage, steps=range(AXES)):
        def action(k, half):
            for step in steps:
                self.reach(layer, k, half, stage, step).wait_recv()
                self.passing(layer, k, half, stage, step).start()
        self.each(action)

    def arrived(self, layer, k):
        box = self.fulls[k].at[layer, :, :, :, self.chip.other]
        remote(box, box, self.pass_send.at[layer, k], self.pass_recv.at[layer, k], self.chip.partner()).wait_recv()

    def left(self):
        three, full = pl.ds(0, AXES), self.fulls[UP].at[A]
        boxes = (full.at[three, A, A, A], full.at[:, three, A, A], full.at[:, :, three, A])

        @loop(LAYERS)
        def _(layer):
            @loop(AXES)
            def _(k):
                for stage, box in enumerate(boxes):
                    sem = self.send_sem.at[layer, k, stage]
                    remote(box, box, sem, sem, self.chip.partner()).wait_send()
                box, sem = full.at[:, :, :, A], self.pass_send.at[layer, k]
                remote(box, box, sem, sem, self.chip.partner()).wait_send()


def pick_lanes(sel_lane, cols):
    return (iota((PAIR, WIDTH), 0) == sel_lane[:, cols]).astype(F32).astype(BF16)


def vector_blocks():
    return [slice(k * WIDTH, (k + 1) * WIDTH) for k in range(N_VEC // WIDTH)]


def unpack_vectors(small_v, layer, sel_shard, sel_lane, vec_ref):
    tiles = small_v[...].astype(F32).reshape((SHARDS, ROWS, PAIR))
    held = jnp.sum(jnp.where(iota(tiles.shape, 1) == layer, tiles, 0.0), axis=1).astype(BF16)
    for cols in vector_blocks():
        spread = dot(held, pick_lanes(sel_lane, cols))
        spread = jnp.where(iota((SHARDS, WIDTH), 0) == sel_shard[:, cols], spread, 0.0)
        vec_ref[layer:layer + 1, cols] = column_sum(spread)


def forward_kernel(x_hbm, ycot_hbm, tables_hbm, places_hbm, up_s, down_s, mix_s, small_ref, up_f, down_f, mix_f, small_full, vec_ref,
                   dout_cols, y_hbm, h_hbm, n1_hbm, n2_hbm, ctx_hbm, act_hbm, qkv_hbm, pre_hbm, up_v, down_v, mix_v, small_v, acc, pre_v,
                   n1_v, n2_v, qkv_v, ctx_v, y_v, n1_t, n2_t, ctx_t, act_t, send_sem, recv_sem, pass_send, pass_recv,
                   small_send, small_recv, own_sems, load_sem, save_sem, share_send, share_recv, act_save, act_send, act_recv, tables,
                   places):
    shards, fulls, own_sem = (up_s, down_s, mix_s), (up_f, down_f, mix_f), pool(own_sems)
    chip = Chip()
    gather = Gather(chip, shards, fulls, (send_sem, recv_sem, pass_send, pass_recv))

    def small_copy(slot, where, device):
        place = small_full.at[(*where, chip.core)]
        return remote(place, place, small_send.at[slot], small_recv.at[slot], device)

    def small_reach(stage, step):
        where = list(chip.where)
        for axis in range(stage):
            where[axis] = pl.ds(0, SIDE)
        return small_copy(AXES * stage + step, where, chip.device(stage, ROLES[step], A))

    def small_begin(stage):
        start([small_reach(stage, step) for step in range(AXES)])

    def small_end(stage):
        for step in range(AXES):
            small_reach(stage, step).wait_recv()

    small_pass = small_copy(AXES * AXES, [pl.ds(0, SIDE)] * AXES, chip.partner())
    here = (*chip.where, chip.core)
    own = [pltpu.make_async_copy(small_ref, small_full.at[here], next(own_sem))]
    for shard, full in zip(shards, fulls):
        for layer in range(LAYERS):
            own.append(pltpu.make_async_copy(shard.at[layer], full.at[(layer, *here)], next(own_sem)))
    loads = [
        pltpu.make_async_copy(src, dst, next(own_sem)) for src, dst in ((x_hbm, y_v), (ycot_hbm, n1_v), (tables_hbm, tables), (places_hbm, places))]
    cot_copies = half_copies(chip, n1_v, dout_cols.at[LAYERS - 1], next(own_sem), next(own_sem), next(own_sem))
    start(own)
    start(loads)
    with jax.named_scope('enter'):
        enter(chip)
    with jax.named_scope('ag0'):
        gather.begin(A, A)
        gather.begin(B, A)
        wait(own)
        small_begin(A)
        gather.own(A)
        gather.own(B)
        gather.end(A, A)
    with jax.named_scope('ag1'):
        gather.begin(A, B)
        small_end(A)
        small_begin(B)
        gather.end(B, A)
        gather.begin(B, B)
        gather.middle(A, B)
        small_end(B)
        small_begin(C)
        gather.middle(B, B)
        gather.end(A, B, (B, C))
    with jax.named_scope('ag2_start'):
        gather.begin(A, C)
        small_end(C)
        small_pass.start()
        gather.end(B, B, (B, C))
    with jax.named_scope('ag2_middle'):
        gather.middle(A, C)
        gather.begin(B, C)
    with jax.named_scope('unpack'):
        small_pass.wait_recv()
        fetch = pltpu.make_async_copy(small_full, small_v, next(own_sem))
        fetch.start()
        fetch.wait()
        wait(loads)
        start(cot_copies)
        for layer in range(LAYERS):
            unpack_vectors(small_v, layer, places[A:B], places[B:C], vec_ref)
    with jax.named_scope('ag2_late'):
        gather.end(A, C, (B,))
    with jax.named_scope('ag2_end'):
        gather.end(A, C, (C,))
        wait(cot_copies)

    def saves(layer):
        pairs = [(y_v, h_hbm.at[layer]), (qkv_v, qkv_hbm.at[layer])]
        kept = [pltpu.make_async_copy(src, dst, save_sem.at[n]) for n, (src, dst) in enumerate(pairs)]
        for n, (src, dst) in enumerate(((n1_t, n1_hbm), (n2_t, n2_hbm), (ctx_t, ctx_hbm))):
            dst = dst.at[layer, chip.core]
            kept.append((pltpu.make_async_copy(src, dst, save_sem.at[CORES + n]),
                         remote(src, dst, share_send.at[layer, n], share_recv.at[layer, n], chip.partner())))
        return kept

    def quarter(layer, t):
        rows, tiles = pl.ds(t * WIDTH, WIDTH), pl.ds(CORES * t, CORES)
        src, dst = act_t.at[rows], act_hbm.at[layer, chip.core, rows]
        return [pltpu.make_async_copy(pre_v.at[tiles], pre_hbm.at[layer, tiles], act_save.at[A, t]),
                pltpu.make_async_copy(src, dst, act_save.at[B, t]),
                remote(src, dst, act_send.at[layer, t], act_recv.at[layer, t], chip.partner())]

    def settle(layer):
        _, qkv_save, *shares = saves(layer)
        qkv_save.wait()
        for share in shares:
            wait(share)

        @loop(SIDE)
        def _(t):
            wait(quarter(layer, t))

    @loop(LAYERS)
    def _(layer):
        def vector(k, first=0, width=None):
            return vec_ref[pl.ds(layer, 1), lanes(OFFSETS[k] + first, width or SIZES[k])]

        def load(k, piece):
            if k == DOWN:
                return pltpu.make_async_copy(fulls[k].at[layer, piece], down_v.at[piece], load_sem.at[k, piece])
            cols = lanes(piece * WIDTH, WIDTH)
            return pltpu.make_async_copy(fulls[k].at[layer, :, :, :, :, :, cols], (up_v, None, mix_v)[k].at[:, :, :, :, :, cols],
                                         load_sem.at[k, piece])

        def matrix(held, piece):
            return held[:, :, :, :, :, lanes(piece * WIDTH, WIDTH)].reshape((WIDTH, WIDTH))

        def have(k):
            gather.arrived(layer, k)

        def meanwhile(action):
            @pl.when(layer == A)
            def _():
                action()

        h_save, qkv_save, n1_share, n2_share, ctx_share = saves(layer)
        with jax.named_scope('have_mix'):
            have(MIX)
            start([load(MIX, k) for k in range(SIDE)])

        h_save.start()

        @pl.when(layer == B)
        def _():
            settle(A)

        with jax.named_scope('ln'):
            @loop(SEQ // LN_ROWS)
            def _(r):
                rows = pl.ds(pl.multiple_of(r * LN_ROWS, LN_ROWS), LN_ROWS)
                scaled, _ = normalised(y_v[rows, :].astype(F32))
                n1_v[rows, :] = (scaled * vector(GAIN1) + vector(BIAS1)).astype(BF16)
                n2_v[rows, :] = (scaled * vector(GAIN2) + vector(BIAS2)).astype(BF16)

        for src, dst, share in ((n1_v, n1_t, n1_share), (n2_v, n2_t, n2_share)):
            dst[...] = src[...].T
            start(share)

        with jax.named_scope('qkv'):
            for k in range(PARTS):
                load(MIX, k).wait()
                x = dot(n1_v[...], matrix(mix_v, k)) + vector(QKV_BIAS, k * WIDTH, WIDTH)
                for c in range(N_PAIRS):
                    block = x[:, block_rows(c)]
                    if k < C:
                        block = turn(block, *[tables[n] for n in range(PARTS)])
                    qkv_v[:, lanes(k * WIDTH + c * PAIR)] = block.astype(BF16)

        qkv_save.start()
        with jax.named_scope('have_up'):
            have(UP)
            have(DOWN)

        start([load(UP, k) for k in range(SIDE)] + [load(DOWN, k) for k in range(SIDE)])
        with jax.named_scope('fattn'):
            def one_pair(pair):
                keys = split_heads(qkv_v[:, lanes(WIDTH + pair * PAIR)])
                values = split_heads(qkv_v[:, lanes(C * WIDTH + pair * PAIR)])
                for i in range(N_BLOCKS):
                    n = (i + 1) * CORES * PAIR
                    probs = probabilities(qkv_v[block_rows(i), lanes(pair * PAIR)], keys[:n], i)
                    ctx_v[block_rows(i), lanes(pair * PAIR)] = dot(side_by_side(probs), values[:n]).astype(BF16)

            @loop(N_PAIRS // CORES)
            def _(two):
                for k in HALVES:
                    one_pair(CORES * two + k)

                @pl.when((layer == A) & (two == A))
                def _():
                    gather.middle(B, C)

        ctx_t[...] = ctx_v[...].T
        start(ctx_share)
        with jax.named_scope('fout'):
            load(MIX, PARTS).wait()
            acc[...] = y_v[...].astype(F32) + dot(ctx_v[...], matrix(mix_v, PARTS)) + (vector(OUT_BIAS) + vector(DOWN_BIAS))

        with jax.named_scope('fmlp'):
            @loop(SIDE)
            def _(t):
                cols = lanes(t * WIDTH, WIDTH)
                load(UP, t).wait()
                pre = dot(n2_v[...], matrix(up_v, t)) + vector(UP_BIAS, t * WIDTH, WIDTH)
                for k in HALVES:
                    pre_v[CORES * t + k] = pre[:, k * TILE:(k + 1) * TILE]
                act = (0.5 * pre * (1.0 + lax.erf(pre * INV_SQRT2))).astype(BF16)
                act_t[cols, :] = act.T
                start(quarter(layer, t))
                load(DOWN, t).wait()
                acc[...] += dot(act, down_v[t].reshape((WIDTH, WIDTH)))

                @pl.when((layer == A) & (t == B))
                def _():
                    gather.end(B, C, (B,))

        h_save.wait()
        y_v[...] = acc[...].astype(BF16)
        with jax.named_scope('fend'):
            meanwhile(lambda: gather.end(B, C, (C,)))

    with jax.named_scope('ftail'):
        last = pltpu.make_async_copy(y_v, y_hbm, next(own_sem))
        last.start()
        for stage in range(AXES):
            for step in range(AXES):
                small_reach(stage, step).wait_send()
        small_pass.wait_send()
        gather.left()
        settle(LAYERS - 1)
        last.wait()


def forward(x, y_cot, shards, small_tile, tables, places):
    grid = CHIPS + (CORES,)
    full = [(LAYERS,) + grid + tensor.shape[1:] for tensor in shards]
    shapes = [(shape, BF16) for shape in full] + [(grid + small_tile.shape, BF16), ((LAYERS, N_VEC), F32), ((LAYERS, CORES, SEQ, TILE), BF16), ((SEQ, WIDTH), BF16),
                                                  ((LAYERS, SEQ, WIDTH), BF16)]
    shapes += [((LAYERS, CORES, width, SEQ), BF16) for width in (WIDTH, WIDTH, WIDTH, HIDDEN)]
    shapes += [((LAYERS, SEQ, QKV), BF16), ((LAYERS, N_TILES, SEQ, TILE), F32)]
    dma = pltpu.SemaphoreType.DMA
    slots = AXES * AXES
    scratch = [pltpu.VMEM(shape[1:], BF16) for shape in full] + [pltpu.VMEM(grid + small_tile.shape, BF16)]
    scratch += [pltpu.VMEM((SEQ, WIDTH), F32), pltpu.VMEM((N_TILES, SEQ, TILE), F32)]
    scratch += [pltpu.VMEM((SEQ, width), BF16) for width in (WIDTH, WIDTH, QKV, WIDTH, WIDTH)]
    scratch += [pltpu.VMEM((width, SEQ), BF16) for width in (WIDTH, WIDTH, WIDTH, HIDDEN)]
    scratch += [dma(shape) for shape in ((LAYERS, AXES, AXES), (LAYERS, AXES, len(HALVES), slots), (LAYERS, AXES), (LAYERS, AXES))]
    scratch += [dma(shape) for shape in ((slots + 1,), (slots + 1,), (slots + SIDE + SIDE + AXES,), (AXES, SIDE), (SIDE + 1,), (LAYERS, AXES), (LAYERS, AXES), (CORES, SIDE), (LAYERS, SIDE), (LAYERS, SIDE))]
    scratch += [pltpu.VMEM(tables.shape, F32), pltpu.VMEM(places.shape, jnp.int32)]
    out_specs = [IN_VMEM if dtype == F32 and len(shape) == LAYERS else ANY for shape, dtype in shapes]
    return pl.pallas_call(
        forward_kernel,
        out_shape=[jax.ShapeDtypeStruct(*s) for s in shapes],
        in_specs=[ANY] * SIDE + [IN_VMEM] * SIDE,
        out_specs=out_specs,
        scratch_shapes=scratch,
        compiler_params=pltpu.CompilerParams(collective_id=0, has_side_effects=True, vmem_limit_bytes=VMEM_LIMIT),
        name='forward_layers',
    )(x, y_cot, tables, places, *shards, small_tile)


WAVES = ((384, 384, 512), (384, 384, 256), (256, 256, 256))
LEADS = ((2,) + CHIPS[1:], CHIPS[1:], (2, SIDE), (SIDE,), (AXES,))
W_UP, W_DOWN, W_QKV, W_OUT = range(4)
STEPS = ((1, (2,)), (0, ()), (2, (4, 3)), (4, (5,)), (3, ()), (5, (6, 7, 8)), (8, (9,)), (9, ()))
LAST = AXES * AXES
CARRIED = ((0, 6, 0), (1, 4, 0), (2, 0, 0))
US_COLUMN, US_HOP, US_ADD, US_STEP = 0.022, 2.5, 0.0013, 0.2
US_FIRST, US_OUT, US_TILE, US_GRADIENT, US_PAIR, US_NORM = 2, 1.4, 1.6, 0.0035, 3.6, 2.7


class Schedule:
    def __init__(self):
        self.now, self.free, self.lines = 0.0, {}, []

    def send(self, link, columns):
        self.free[link] = max(self.free.get(link, 0.0), self.now) + columns * US_COLUMN
        return self.free[link] + US_HOP

    def due(self, limit):
        found = []
        while self.lines:
            line = min(self.lines, key=lambda one: one[A][A]())
            ready = line[A][A]()
            if limit is not None and ready > limit:
                break
            _, run, sends, cost = line.pop(A)
            self.lines = [one for one in self.lines if one]
            self.now = max(self.now, ready) + cost
            sends()
            found.append(run)
        return found

    def finish(self, line):
        while line:
            ready, run, sends, cost = line.pop(A)
            self.now = max(self.now, ready()) + cost
            sends()
            run()
        self.lines = [one for one in self.lines if one]

    def run(self, limit):
        for step in self.due(limit):
            step()

    def passed(self, cost):
        self.now += cost
        self.run(self.now)

    def hooks(self, count, cost):
        planned = []
        for _ in range(count):
            self.now += cost
            planned.append(self.due(self.now))
        return planned


def at_hooks(n, planned):
    for when, steps in enumerate(planned):
        if steps:
            @pl.when(n == when)
            def _():
                for step in steps:
                    step()


def add_into(dst, src, n_axes):
    if n_axes < 2:
        dst[...] += src[...]
        return

    @loop(SIDE)
    def _(k):
        dst[k] += src[k]


def at_axis(ref, axis, value, n_axes):
    every = [pl.ds(0, SIDE)] * n_axes
    every[axis] = value
    return ref.at[tuple(every)]


class Reduce:
    def __init__(self, chip, schedule, wave, grads, came, fin, sems, spare, write, done, when=None):
        self.wave, self.chip, self.schedule, self.widths, self.grads = wave, chip, schedule, WAVES[wave], grads
        self.came, self.fin, (self.send_sem, self.recv_sem), (self.spare, self.spare_sem) = came, fin, sems, spare
        self.write, self.done, self.when, self.times = write, done, when, {}

    def box(self, a, half, stage):
        order = ORDERS[a]
        ref = self.came[a][A].at[half, A]
        spot = [axis for axis in range(AXES) if axis != order[A]].index(order[B])
        if stage == B:
            return ref, spot, C
        return at_axis(ref, spot, self.chip.where[order[B]], C), A, B

    def copy(self, a, half, slot):
        stage, turn = divmod(slot, AXES)
        sems = self.send_sem.at[a, stage], self.recv_sem.at[a, half, slot]
        if slot == LAST:
            return remote(self.total(a, half).at[self.chip.other], self.fin[a].at[half], *sems, self.chip.partner())
        axis = ORDERS[a][stage]
        if stage == C:
            role = value = ROLES[turn]
            dst = self.came[a][SIDE].at[half, turn]
        else:
            role, value = TWO if turn == C else ONE, (ONE, CROSS, TWO)[turn]
            dst = self.came[a][CORES * stage + turn // C].at[half]
            dst = dst if turn == C else dst.at[turn]
        value = self.chip.at(axis, value, half)
        if stage:
            ref, spot, n_axes = self.box(a, half, stage)
            src = at_axis(ref, spot, value, n_axes)
        else:
            src = self.came[a][A].at[half, B] if turn == C else at_axis(self.grads[a].at[half], axis, value, AXES)
        return remote(src, dst, *sems, self.chip.device(axis, role, half))

    def each(self, action):
        for a in range(AXES):
            halves(lambda half: action(a, half))

    def sending(self, slot):
        stage = slot // AXES
        share = SIDE ** (CORES * stage)
        self.times[slot] = self.schedule.now + US_HOP if slot == LAST else max(
            self.schedule.send(ORDERS[a][stage], self.widths[a] / share) for a in range(AXES))

    def begin(self):
        for slot in (B, A):
            self.each(lambda a, half: self.copy(a, half, slot).start())

    def plan(self, first=0, last=None, late=0):
        for slot in (B, A):
            self.times[slot] = self.schedule.now + late
            if not first:
                self.sending(slot)
        for _, sent in STEPS[:first]:
            self.times.update((slot, self.schedule.now + late + US_HOP) for slot in sent)
        line = [
            (lambda slot=slot: self.times[slot], lambda k=k: self.step(k), lambda sent=sent: [self.sending(n) for n in sent],
             CORES * US_ADD * sum(self.widths) if k < C else US_STEP) for k, (slot, sent) in enumerate(STEPS)][first:last]
        self.schedule.lines.append(line)
        return line

    def step(self, k):
        def work():
            with jax.named_scope(f'w{self.wave}s{k}'):
                (self.first, self.first, self.halve, self.settle, self.settle, self.spread, self.cross, self.finish)[k](STEPS[k][A])
        if self.when is None:
            work()
        else:
            pl.when(self.when)(work)

    def held(self, a, half):
        ref = self.spare[A].at[a] if a < C else self.spare[B]
        return ref.at[half, :, :, :, :, pl.ds(0, self.widths[a])]

    def first(self, slot):
        def local(a, half):
            axis = ORDERS[a][A]
            return pltpu.make_async_copy(at_axis(self.grads[a].at[half], axis, self.chip.at(axis, TWO if slot else OWN, half), AXES),
                                         self.held(a, half), self.spare_sem.at[a, half])

        def action(a, half):
            local(a, half).wait()
            self.copy(a, half, slot).wait_recv()
            add_into(self.came[a][A].at[half, slot], self.held(a, half), C)
            if slot:
                self.copy(a, half, C).start()

        self.each(lambda a, half: local(a, half).start())
        self.each(action)

    def halve(self, slot):
        def action(a, half):
            ref, spot, n_axes = self.box(a, half, B)
            self.copy(a, half, slot).wait_recv()
            for turn, role in ((B, CROSS), (A, ONE), (C, TWO), (C, OWN)):
                value = self.chip.at(ORDERS[a][B], role, half)
                add_into(at_axis(ref, spot, value, n_axes), at_axis(self.came[a][B].at[half], spot, value, n_axes), B)
                if turn < C:
                    self.copy(a, half, AXES + turn).start()
        self.each(action)

    def settle(self, slot):
        def action(a, half):
            ref, spot, n_axes = self.box(a, half, B)
            self.copy(a, half, slot).wait_recv()
            value = self.chip.at(ORDERS[a][B], TWO if slot > AXES else OWN, half)
            add_into(at_axis(ref, spot, value, n_axes), self.came[a][C].at[half, slot - AXES], B)
            if slot > AXES:
                self.copy(a, half, AXES + C).start()
        self.each(action)

    def spread(self, slot):
        def action(a, half):
            ref, *_ = self.box(a, half, C)
            self.copy(a, half, slot).wait_recv()
            add_into(ref, self.came[a][AXES].at[half], B)
            for turn in range(AXES):
                self.copy(a, half, CORES * AXES + turn).start()
        self.each(action)

    def total(self, a, half):
        ref, *_ = self.box(a, half, C)
        return ref.at[self.chip.where[ORDERS[a][C]]]

    def cross(self, _):
        def action(a, half):
            for turn in range(AXES):
                self.copy(a, half, CORES * AXES + turn).wait_recv()
            self.total(a, half)[...] += total_of([self.came[a][SIDE][half, turn] for turn in range(AXES)])
            self.copy(a, half, LAST).start()
        self.each(action)

    def finish(self, _):
        def action(a, half):
            self.write(a, half, self.chip.core, self.total(a, half)[self.chip.core])
            self.copy(a, half, LAST).wait_recv()
            self.write(a, half, self.chip.other, self.fin[a][half])
        self.each(action)
        three = pl.ds(0, AXES)
        for a, (grad, fin) in enumerate(zip(self.grads, self.fin)):
            for stage, block in enumerate((grad.at[:, :, :, three], grad.at[:, :, three, A], grad.at[:, three, A, A], fin)):
                sem = self.send_sem.at[a, stage]
                remote(block, block, sem, sem, self.chip.partner()).wait_send()
        self.done()


class VectorSum:
    def __init__(self, chip, schedule, total, came, sems, finish, when=None):
        self.schedule, self.total, self.came, self.sems, self.finish, self.when, self.ready = schedule, total, came, sems, finish, when, 0.0
        self.devices = [[chip.device(axis, role, A) for role in ROLES] for axis in range(AXES)] + [[chip.partner()]]

    def copies(self, k):
        return [remote(self.total, self.came.at[AXES * k + n], self.sems.at[A, AXES * k + n], self.sems.at[B, AXES * k + n], device)
                for n, device in enumerate(self.devices[k])]

    def sending(self, k):
        if k < SIDE:
            self.ready = self.schedule.send(k, N_VEC / (SIDE * SIDE * ROWS))

    def step(self, k):
        def work():
            with jax.named_scope(f'vec{k}'):
                wait(self.copies(k - 1))
                for n in range(len(self.devices[k - 1])):
                    self.total[...] += self.came[AXES * (k - 1) + n]
            if k < SIDE:
                start(self.copies(k))
            else:
                self.finish()
        if self.when is None:
            work()
        else:
            pl.when(self.when)(work)

    def begin(self):
        start(self.copies(A))

    def plan(self):
        self.sending(A)
        self.schedule.lines.append([
            (lambda: self.ready, lambda k=k: self.step(k), lambda k=k: self.sending(k), US_STEP) for k in range(1, SIDE + 1)])


def backward_kernel(ycot_hbm, tables, vec_ref, places, up_hbm, down_hbm, mix_hbm, h_hbm, n1_hbm, n2_hbm, ctx_hbm,
                    act_hbm, qkv_hbm, pre_hbm, _, dx_hbm, small_ref, up_sum, down_sum, qkv_sum, out_sum, dout_cols, dpre_cols,
                    dqkv_cols, *refs):
    n_arrays, sums = AXES * len(WAVES), (up_sum, down_sum, qkv_sum, out_sum)
    grads, refs = refs[:n_arrays], refs[n_arrays:]
    (spare, spare_wide, tile_v, big_v, rhs_v, wup_v, wdown_v, pre_v, dn1, dn2, dctx, dk_acc, dv_acc, qkv_v, dpre_v, dqkv_v, dh_v, h_v,
     totals, came_vec, send_sem, recv_sem, spare_sem, tile_sem, big_sem, rhs_sem, mlp_sem, io_sem, own_sem, share_send,
     share_recv, pre_sem, vec_sem, credit, *refs) = refs
    fins, came = refs[:n_arrays], refs[n_arrays:]
    first_in = pltpu.make_async_copy(ycot_hbm, dh_v, io_sem.at[A])
    first_in.start()
    chip = Chip()
    core, other = chip.core, chip.other

    def exchange(layer, k, src, dst):
        return half_copies(chip, src, dst.at[layer], own_sem.at[k], share_send.at[k], share_recv.at[k])

    def tokens_load(layer, src, part, slot):
        return [pltpu.make_async_copy(src.at[layer, k, pl.ds(part * WIDTH, WIDTH)], big_v.at[slot, :, pl.ds(k * SEQ, SEQ)],
                                      big_sem.at[slot, k]) for k in range(CORES)]

    def weight_load(layer, k, slot):
        return pltpu.make_async_copy(mix_hbm.at[layer, :, lanes(k * WIDTH, WIDTH)], big_v.at[slot], big_sem.at[slot, CORES])

    def tile_loads(layer, t, slot):
        rows = lanes(t * TILE, TILE)
        pairs = ((down_hbm.at[layer, rows], wdown_v), (pre_hbm.at[layer, t], pre_v), (up_hbm.at[layer, :, rows], wup_v))
        return [pltpu.make_async_copy(src, dst.at[slot], mlp_sem.at[slot, n]) for n, (src, dst) in enumerate(pairs)]

    def input_loads(layer):
        return [pltpu.make_async_copy(qkv_hbm.at[layer], qkv_v, io_sem.at[B]), pltpu.make_async_copy(h_hbm.at[layer], h_v, io_sem.at[C])]

    def rhs_load(layer, src, first, width, k):
        cols = lanes(first, width)
        return [pltpu.make_async_copy(src.at[layer, n, :, cols], rhs_v.at[pl.ds(n * SEQ, SEQ), cols], rhs_sem.at[k, n])
                for n in range(CORES)]

    def prefetch(layer):
        start(tokens_load(layer, ctx_hbm, A, AXES) + tokens_load(layer, act_hbm, A, A))

    def prefetch_more(layer):
        start(tokens_load(layer, act_hbm, B, B) + tokens_load(layer, act_hbm, C, C) + input_loads(layer))
        for t in HALVES:
            start(tile_loads(layer, t, t))

    prefetch(LAYERS - 1)
    start(rhs_load(LAYERS - 1, dout_cols, A, TILE, A))
    prefetch_more(LAYERS - 1)
    with jax.named_scope('enter'):
        enter(chip)
    with jax.named_scope('first_in'):
        first_in.wait()
    dx_copy = pltpu.make_async_copy(dh_v, dx_hbm, io_sem.at[A])

    def vector_at(k, first=0, width=None):
        return lanes(OFFSETS[k] + first, width or SIZES[k])

    def reduction(schedule, layer, wave, when):
        def write(a, half, side, block):
            def put(arr, group, col, first, width):
                size = sums[arr].shape[-1] // CORES
                sums[arr][layer, group, :, lanes(side * size + col, width)] = block[:, first:first + width].astype(BF16)
            width, colour = WAVES[wave][a], CORES * a + half
            if wave:
                first = colour * width if wave == C or a < C else SIDE * WAVES[wave][A] + half * width
                put(W_QKV if wave == C else W_UP, A, first, A, width)
            elif a < C:
                put(W_DOWN, colour, A, A, width)
            else:
                for k in HALVES:
                    put(W_DOWN, CORES * half + k, WAVES[A][A], k * PAIR, PAIR)
                put(W_OUT, A, half * TWICE, TWICE, TWICE)

        def done():
            @pl.when(layer == LAYERS - 1)
            def _():
                chip.signal_partners(credit.at[wave])

        where = slice(AXES * wave, AXES * (wave + 1))
        count = len(LEADS)
        return Reduce(chip, schedule, wave, [grad.at[layer] for grad in grads[where]],
                      [came[count * (AXES * wave + a):count * (AXES * wave + a + 1)] for a in range(AXES)],
                      fins[where], (send_sem.at[wave], recv_sem.at[wave]), ((spare, spare_wide), spare_sem), write, done, when)

    def vector_sum(schedule, layer, when):
        def own_part():
            with jax.named_scope('own'):
                node, local = chip.base
                me = node * (SIDE * CORES) + local + core
                row = jnp.zeros((ROWS, PAIR), F32)
                for k, share in enumerate(SHARES):
                    if k == QKV_BIAS:
                        firsts = [part * WIDTH + lax.div(me, CORES * ROWS) * PAIR for part in range(PARTS)]
                    else:
                        firsts = [lax.div(me * share, PAIR) * PAIR]
                    for first in firsts:
                        cols = lanes(OFFSETS[k] + first)
                        left = jnp.zeros((ROWS, PAIR), F32) + totals[layer, :, cols] * (places[A:B, cols] == me).astype(F32)
                        pick = (iota((PAIR, PAIR), 0) == places[B:C, cols]).astype(F32).astype(BF16)
                        for _ in range(PARTS):
                            row = row + dot_t(left.astype(BF16), pick)
                            left = left - rounded(left)
                small_ref[layer] = row.astype(BF16)

            @pl.when(layer == LAYERS - 1)
            def _():
                chip.signal_partners(credit.at[AXES])

        return VectorSum(chip, schedule, totals.at[layer], came_vec, vec_sem, own_part, when)

    def run_on(schedule, layer, when):
        lines = [reduction(schedule, layer, wave, when).plan(step, late=late) for wave, step, late in CARRIED]
        vector_sum(schedule, layer, when).plan()
        return lines

    @loop(LAYERS + 1)
    def _(turn_no):
        layer = LAYERS - 1 - turn_no
        working = pl.when(turn_no < LAYERS)
        total = totals.at[layer]
        schedule = Schedule()

        carried = run_on(schedule, layer + 1, turn_no > A)

        def product(lhs_slot, first, width, out_slot):
            value = dot(big_v[lhs_slot, :, 0:CORES * SEQ], rhs_v[:, lanes(first, width)])
            tile_v[out_slot, :, :, :, :, :, 0:width] = value.reshape(CHIPS + (CORES, ROWS, width))

        def tile_out(slot, src, dst):
            return pltpu.make_async_copy(src, dst, tile_sem.at[slot])

        def tile_done(slot, width):
            block = tile_v.at[slot, :, :, :, :, :, pl.ds(0, width)]
            tile_out(slot, block, block).wait()

        def columns(wave, a, half, first, width):
            return grads[AXES * wave + a].at[layer, half, :, :, :, :, :, pl.ds(first, width)]

        def launch(wave):
            schedule.finish(carried[wave])

            @pl.when(turn_no == B)
            def _():
                pl.semaphore_wait(credit.at[wave], PARTNERS)

            current = reduction(schedule, layer, wave, turn_no < LAYERS)
            if wave == C:
                @pl.when(turn_no == B)
                def _():
                    pl.semaphore_wait(credit.at[AXES], PARTNERS)

                @working
                def _():
                    vector_sum(schedule, layer, None).begin()

            working(current.begin)
            if wave < C:
                current.plan(last=CARRIED[wave][B])

        @working
        def _():
            with jax.named_scope('dw_out'):
                @pl.when(turn_no == B)
                def _():
                    wait(exchange(layer, A, dh_v, dout_cols))
                    start(rhs_load(layer, dout_cols, A, TILE, A))

                wait(rhs_load(layer, dout_cols, A, TILE, A))
                wait(tokens_load(layer, ctx_hbm, A, AXES))
                product(AXES, A, TILE, B)
                start(tokens_load(layer, act_hbm, AXES, AXES))
                for k in HALVES:
                    tile_out(B, tile_v.at[B, :, :, :, :, :, pl.ds(k * TWICE, TWICE)], columns(A, C, k, TWICE, TWICE)).start()

        schedule.passed(US_FIRST)
        out_hooks = schedule.hooks(SIDE, US_OUT)

        @loop(SIDE)
        def _(z):
            @working
            def _():
                slot = parity(z)
                wait(tokens_load(layer, act_hbm, z, z))

                @pl.when(z > A)
                def _():
                    tile_done(slot, TILE)

                product(z, A, TILE, slot)
                split = WAVES[A][A]
                for k in range(SIDE):
                    a, half = divmod(k, CORES)
                    for c in range(CORES):
                        block = tile_v.at[slot, :, :, CORES * c + a, half]
                        tile_out(slot, block.at[:, :, :, pl.ds(0, split)], grads[a].at[layer, half, z, :, :, c]).start()
                        tile_out(slot, block.at[:, :, :, pl.ds(split, PAIR)],
                                 grads[C].at[layer, a, z, :, :, c, :, pl.ds(half * PAIR, PAIR)]).start()

            at_hooks(z, out_hooks)

        @working
        def _():
            start(tokens_load(layer, n2_hbm, A, A) + [weight_load(layer, k, k + 1) for k in range(PARTS)])
            for slot in HALVES:
                tile_done(slot, TILE)

        schedule.passed(US_STEP)
        launch(A)

        @working
        def _():
            dn2[...] = jnp.zeros_like(dn2)

        def pre_copy(t, slot, away):
            place = dpre_cols.at[layer, core, :, lanes(lax.rem(t, SIDE) * TILE, TILE)]
            if away:
                return remote(dpre_v.at[slot], place, pre_sem.at[A, t], pre_sem.at[B, t], chip.partner())
            return pltpu.make_async_copy(dpre_v.at[slot], place, own_sem.at[CORES + slot])

        def pre_act(t, leave):
            for away, whose in ((False, core), (True, other)):
                @pl.when(lax.div(t, SIDE) == whose)
                def _():
                    copy = pre_copy(t, parity(t), away)
                    if leave:
                        copy.start()
                    elif away:
                        copy.wait_send()
                    else:
                        copy.wait()

        tile_hooks = schedule.hooks(N_TILES, US_TILE)

        with jax.named_scope('mlp'):
            @loop(N_TILES)
            def _(t):
                @working
                def _():
                    slot = parity(t)
                    wait(tile_loads(layer, t, slot))
                    d_act = rounded(dot_t(dh_v[...], wdown_v[slot]))
                    pre = pre_v[slot]
                    slope = 0.5 * (1.0 + lax.erf(pre * INV_SQRT2)) + pre * (INV_SQRT2PI * jnp.exp(-0.5 * pre * pre))
                    d_pre = d_act * slope
                    total[:, vector_at(UP_BIAS, t * TILE, TILE)] = column_sum(d_pre)

                    @pl.when(t > B)
                    def _():
                        pre_act(t - CORES, False)

                    dpre_v[slot] = d_pre.astype(BF16)
                    pre_act(t, True)
                    dn2[...] += dot_t(dpre_v[slot], wup_v[slot])

                    @pl.when(t + CORES < N_TILES)
                    def _():
                        start(tile_loads(layer, t + CORES, slot))

                at_hooks(t, tile_hooks)

        @working
        def _():
            for t in HALVES:
                pre_act(N_TILES - CORES + t, False)
            for t in range(SIDE):
                pre_copy(SIDE * core + t, A, True).wait_recv()

        def gradient_loads(wave, source):
            first = 0
            for a in range(AXES):
                width = CORES * WAVES[wave][a]
                start(rhs_load(layer, source, first, width, a))
                first += width

        def gradient_wave(wave, source, lhs_slot, first, orders):
            split, count = WAVES[wave][orders[A]], len(orders)
            width = CORES * split
            planned = schedule.hooks(count, width * US_GRADIENT)

            @loop(count)
            def _(n):
                @working
                def _():
                    slot = parity(n)
                    wait(rhs_load(layer, source, first + n * width, width, orders[A] + n))

                    @pl.when(n > B)
                    def _():
                        tile_done(slot, width)

                    product(lhs_slot, first + n * width, width, slot)
                    for k, a in enumerate(orders):
                        @pl.when(n == k)
                        def _():
                            for half in HALVES:
                                block = tile_v.at[slot, :, :, :, :, :, pl.ds(half * split, split)]
                                tile_out(slot, block, columns(wave, a, half, 0, split)).start()

                at_hooks(n, planned)

            @working
            def _():
                for slot in range(min(count, CORES)):
                    tile_done(slot, width)

        @working
        def _():
            gradient_loads(B, dpre_cols)
            wait(tokens_load(layer, n2_hbm, A, A))

        with jax.named_scope('dw1'):
            gradient_wave(B, dpre_cols, A, A, (A, B))
            gradient_wave(B, dpre_cols, A, SIDE * WAVES[B][A], (C,))
        launch(B)
        @working
        def _():
            weight_load(layer, AXES, A).start()
            d_sum = column_sum(dh_v[...].astype(F32))
            total[:, vector_at(OUT_BIAS)] = d_sum
            total[:, vector_at(DOWN_BIAS)] = d_sum
            wait(input_loads(layer))
            weight_load(layer, AXES, A).wait()
            dctx[...] = dot_t(dh_v[...], big_v[A]).astype(BF16)

        pair_hooks = schedule.hooks(N_PAIRS // CORES, US_PAIR)

        with jax.named_scope('attn'):
            def one_pair(pair, dk_sum, dv_sum):
                at = lanes(pair * PAIR)
                keys = split_heads(qkv_v[:, lanes(WIDTH + pair * PAIR)])
                values = split_heads(qkv_v[:, lanes(C * WIDTH + pair * PAIR)])
                q_t = qkv_v[:, at].T
                dc_t = dctx[:, at].T
                bias_sums = [jnp.zeros((1, PAIR), F32)] * PARTS

                def turned_back(n, d, rows, to):
                    d = turn_back(rounded(d), *[tables[k, rows, :] for k in range(PARTS)])
                    bias_sums[n] = bias_sums[n] + column_sum(d)
                    dqkv_v[rows, to] = d.astype(BF16)

                for i in range(N_BLOCKS):
                    old, n = i * TWICE, (i + 1) * TWICE
                    rows = block_rows(i)
                    probs = probabilities(qkv_v[rows, at], keys[:n], i)
                    d_all = rounded(dot_t(dctx[rows, at], values[:n]))
                    d_scores = [d_all[:, block_rows(j)] for j in range(CORES * (i + 1))]
                    for head in HALVES:
                        mine = slice(head, None, CORES)
                        mean = row_sum(total_of([p * d for p, d in zip(probs[mine], d_scores[mine])]))
                        d_scores[mine] = [p * (d - mean) * SCALE for p, d in zip(probs[mine], d_scores[mine])]
                    d_scores, probs = side_by_side(d_scores), side_by_side(probs)
                    turned_back(A, dot(d_scores, keys[:n]), rows, at)
                    for acc, left, right in ((dk_sum, q_t, d_scores), (dv_sum, dc_t, probs)):
                        part = dot(left[:, rows], right)
                        if i:
                            acc[:, :old] += part[:, :old]
                        acc[:, old:n] = part[:, old:]
                first = iota((PAIR, PAIR), 0) < HEAD
                for j in range(N_BLOCKS):
                    rows = block_rows(j)
                    d_key, d_value = [jnp.where(first, acc[:, block_rows(CORES * j)], acc[:, block_rows(CORES * j + 1)]).T
                                      for acc in (dk_sum, dv_sum)]
                    turned_back(B, d_key, rows, lanes(WIDTH + pair * PAIR))
                    d_value = d_value.astype(BF16)
                    bias_sums[C] = bias_sums[C] + column_sum(d_value.astype(F32))
                    dqkv_v[rows, lanes(C * WIDTH + pair * PAIR)] = d_value
                for k, bias_sum in enumerate(bias_sums):
                    total[:, vector_at(QKV_BIAS, k * WIDTH + pair * PAIR, PAIR)] = bias_sum

            @loop(N_PAIRS // CORES)
            def _(two):
                @working
                def _():
                    for k in HALVES:
                        one_pair(CORES * two + k, dk_acc.at[k], dv_acc.at[k])

                at_hooks(two, pair_hooks)

        @working
        def _():
            start(exchange(layer, B, dqkv_v, dqkv_cols))
            dn1[...] = jnp.zeros_like(dn1)

            with jax.named_scope('dn1'):
                @loop(PARTS)
                def _(k):
                    weight_load(layer, k, k + 1).wait()
                    dn1[...] += dot_t(dqkv_v[:, lanes(k * WIDTH, WIDTH)], big_v[k + 1])

                    @pl.when(k == A)
                    def _():
                        start(tokens_load(layer, n1_hbm, A, B))

        schedule.passed(US_NORM)

        @working
        def _():
            wait(exchange(layer, B, dqkv_v, dqkv_cols))
            gradient_loads(C, dqkv_cols)
            wait(tokens_load(layer, n1_hbm, A, B))

        with jax.named_scope('dw2'):
            gradient_wave(C, dqkv_cols, B, A, (A, B, C))

        @working
        def _():
            for k in (GAIN1, BIAS1, GAIN2, BIAS2):
                total[:, vector_at(k)] = jnp.zeros((1, WIDTH), F32)

            with jax.named_scope('lnb'):
                @loop(SEQ // LN_ROWS)
                def _(r):
                    rows = pl.ds(pl.multiple_of(r * LN_ROWS, LN_ROWS), LN_ROWS)
                    scaled, inverse = normalised(h_v[rows, :].astype(F32))
                    d1, d2 = rounded(dn1[rows, :]), rounded(dn2[rows, :])
                    for k, value in ((GAIN1, d1 * scaled), (BIAS1, d1), (GAIN2, d2 * scaled), (BIAS2, d2)):
                        total[:, vector_at(k)] += column_sum(value)
                    g1, g2 = [vec_ref[pl.ds(layer, 1), lanes(OFFSETS[k], WIDTH)] for k in (GAIN1, GAIN2)]
                    d_scaled = d1 * g1 + d2 * g2
                    d_h = inverse * (d_scaled - row_mean(d_scaled) - scaled * row_mean(d_scaled * scaled))
                    dh_v[rows, :] = (dh_v[rows, :].astype(F32) + d_h).astype(BF16)

        @pl.when(turn_no == A)
        def _():
            start(exchange(layer - 1, A, dh_v, dout_cols))

        @pl.when(turn_no == B)
        def _():
            dx_copy.start()

        @pl.when(turn_no == A)
        def _():
            prefetch(layer - 1)
            prefetch_more(layer - 1)

        schedule.now += US_NORM
        schedule.run(None)
        launch(C)

    dx_copy.wait()


def backward(y_cot, tables, vectors, places, weights, saved):
    dma, one = pltpu.SemaphoreType.DMA, (1,)
    pair, wide, row = (len(HALVES),), (SEQ, WIDTH), one + (N_VEC,)
    shapes = [(wide, BF16), ((LAYERS, ROWS, PAIR), BF16)]
    shapes += [((LAYERS, groups, ROWS, width), BF16) for groups, width in ((*one, HIDDEN), (SIDE, WIDTH), (*one, QKV), (*one, WIDTH))]
    in_vmem = len(shapes)
    shapes += [((LAYERS, CORES, SEQ, width), BF16) for width in (TILE, SIDE * TILE, PARTS * TILE)]
    blocks = [(CORES, ROWS, width) for wave in WAVES for width in wave]
    shapes += [((LAYERS,) + pair + CHIPS + block, F32) for block in blocks]
    tile = (CORES, ROWS)
    scratch = [(pair + pair + CHIPS[1:] + tile + (WAVES[0][0],), F32), (pair + CHIPS[1:] + tile + (TILE,), F32), (pair + CHIPS + tile + (CORES * WAVES[0][0],), F32), ((SIDE, WIDTH, WIDTH), BF16), ((CORES * SEQ, SIDE * TILE), BF16)]
    scratch += [(pair + shape, BF16) for shape in ((WIDTH, TILE), (TILE, WIDTH))]
    scratch += [(pair + (SEQ, TILE), F32), (wide, F32), (wide, F32), (wide, BF16)] + [(pair + (PAIR, CORES * SEQ), F32)] * CORES
    scratch += [((SEQ, QKV), BF16), (pair + (SEQ, TILE), BF16), ((SEQ, QKV), BF16), (wide, BF16), (wide, BF16), ((LAYERS,) + row, F32),
                ((PARTNERS,) + row, F32)]
    slots = (len(WAVES), AXES) + pair + (LAST + 1,)
    sems = [dma(shape) for shape in ((len(WAVES), AXES, SIDE), slots, (AXES,) + pair, pair, (SIDE, AXES), (AXES, CORES), pair + (PARTS,), (AXES,),
                                     (SIDE,), pair, pair, pair + (N_TILES,), pair + (PARTNERS,))]
    late = [(pair + block[1:], F32) for block in blocks] + [(pair + lead + block, F32) for block in blocks for lead in LEADS]
    outs = pl.pallas_call(
        backward_kernel,
        out_shape=[jax.ShapeDtypeStruct(*s) for s in shapes],
        in_specs=[ANY] + [IN_VMEM] * AXES + [ANY] * (PARTNERS + 1),
        input_output_aliases={SIDE + PARTNERS: in_vmem},
        out_specs=[ANY] + [IN_VMEM] * (in_vmem - 1) + [ANY] * (len(shapes) - in_vmem),
        scratch_shapes=[pltpu.VMEM(*s) for s in scratch] + sems + [pltpu.SemaphoreType.REGULAR((SIDE,))]
        + [pltpu.VMEM(*s) for s in late],
        compiler_params=pltpu.CompilerParams(collective_id=1, has_side_effects=True, vmem_limit_bytes=VMEM_LIMIT),
        name='backward_layers',
    )(y_cot, tables, vectors, places, *weights, *saved)
    d_x, small, *sums = outs[:in_vmem]
    return d_x, small[:, 0], [s.reshape((LAYERS, -1, s.shape[-1])) for s in sums]


def finish_kernel(*refs):
    n_large = CORES + AXES
    large, small_ref, refs = refs[:n_large], refs[n_large], refs[n_large + 1:]
    outs, small_outs, refs = refs[:n_large], refs[n_large:n_large + len(SHARES)], refs[n_large + len(SHARES):]
    held, sems = refs[:n_large], refs[n_large]
    loads = start([pltpu.make_async_copy(src, dst, sems.at[n]) for n, (src, dst) in enumerate(zip(large, held))])
    first = 0
    for share, out in zip(SHARES, small_outs):
        out[...] = small_ref[:, first:first + share]
        first += share
    stores = []
    for load, src, dst in zip(loads, held, outs):
        load.wait()
        stores += start([pltpu.make_async_copy(src, dst, sems.at[n_large + len(stores)])])
    wait(stores)


def finish(large, small):
    shapes = [jax.ShapeDtypeStruct(t.shape, BF16) for t in large] + [jax.ShapeDtypeStruct((LAYERS, share), BF16) for share in SHARES]
    outs = pl.pallas_call(
        finish_kernel,
        out_shape=shapes,
        in_specs=[ANY] * len(large) + [IN_VMEM],
        out_specs=[ANY] * len(large) + [IN_VMEM] * len(SHARES),
        scratch_shapes=[pltpu.VMEM(t.shape, BF16) for t in large] + [pltpu.SemaphoreType.DMA((CORES * len(large),))],
        name='finish',
    )(*large, small)
    return outs[:len(large)], outs[len(large):]


def rope_tables():
    rot_dim, f32 = HEAD // SIDE, np.float32
    inv_freq = f32(1.0) / f32(10000.0) ** (np.arange(0, rot_dim, 2, dtype=f32) / f32(rot_dim))
    angles = np.arange(SEQ, dtype=f32)[:, None] * inv_freq[None, :]
    cos, sin = np.cos(angles), np.sin(angles)
    zero = np.zeros_like(sin)
    rest = np.zeros((SEQ, HEAD - rot_dim), f32)
    tables = ([cos, cos, rest + f32(1.0)], [-sin, zero, rest], [zero, sin, rest])
    return jnp.asarray(np.stack([np.tile(np.concatenate(table, axis=1), (1, 2)) for table in tables]).astype(f32))


def heads_last(tensor):
    lead = tensor.shape[:-2]
    return tensor.reshape(lead + (HEADS, PARTS, HEAD)).swapaxes(-3, -2).reshape(lead + (QKV,))


def heads_first(tensor):
    lead = tensor.shape[:-1]
    return tensor.reshape(lead + (PARTS, HEADS, HEAD)).swapaxes(-3, -2).reshape(lead + (HEADS, PARTS * HEAD))


def vector_places():
    shard, lane, first = [], [], 0
    for k, (share, size) in enumerate(zip(SHARES, SIZES)):
        place = np.arange(size)
        if k == QKV_BIAS:
            place = heads_last(place.reshape(HEADS, -1))
        shard.append(place // share)
        lane.append(first + place % share)
        first += share
    return jnp.asarray(np.stack([np.concatenate(shard), np.concatenate(lane)]).astype(np.int32))


def solution(mesh):
    shard_axes = ('node', 'local')
    act_spec = P(shard_axes)
    param_spec = P(None, shard_axes)

    def device_step(x, y_cot, ln1_gain, ln1_bias, qkv_weight, qkv_bias, out_weight, out_bias,
                    ln2_gain, ln2_bias, up_weight, up_bias, down_weight, down_bias):
        tables, places = rope_tables(), vector_places()
        small = (ln1_gain, ln1_bias, ln2_gain, ln2_bias, qkv_bias, out_bias, up_bias, down_bias)
        small_tile = jnp.pad(jnp.concatenate(small, axis=1), ((0, ROWS - LAYERS), (0, PAIR - sum(SHARES))))
        mix = jnp.concatenate([heads_last(qkv_weight), out_weight], axis=-1)
        *weights, _, vectors, dout_cols, y_out, hidden, n1, n2, ctx, act, qkv, pre = forward(
            x[0], y_cot[0], (up_weight, down_weight, mix), small_tile, tables, places)
        weights = [tensor.reshape((LAYERS, -1, tensor.shape[-1])) for tensor in weights]
        d_x, small_sums, (up, down, qkv, out) = backward(
            y_cot[0], tables, vectors, places, weights, (hidden, n1, n2, ctx, act, qkv, pre, dout_cols))
        (y_out, d_x, up, down, out), (g1, b1, g2, b2, qb, ob, ub, db) = finish((y_out, d_x, up, down, out), small_sums)
        return (y_out[None], d_x[None], g1, b1, heads_first(qkv), qb, out, ob, g2, b2, up, ub, down, db)

    return jax.shard_map(device_step, mesh=mesh,
                         in_specs=(act_spec, act_spec) + (param_spec,) * 12,
                         out_specs=(act_spec, act_spec) + (param_spec,) * 12,
                         check_vma=False)
```

```python
import functools
import jax
import jax.numpy as jnp
import numpy as np
from jax import lax
from jax.experimental import pallas as pl
from jax.experimental.pallas import tpu as pltpu
from jax.sharding import PartitionSpec as P

BF16, F32 = jnp.bfloat16, jnp.float32
EPSILON = 1e-5
MESH = pl.DeviceIdType.MESH
ANY = pl.BlockSpec(memory_space=pl.ANY)
IN_VMEM = pl.BlockSpec(memory_space=pltpu.VMEM)
VMEM_LIMIT = 67 * 10**6
LAYERS, AXES, SIDE, CORES, ROWS, PARTNERS = 2, 3, 4, 2, 8, 10
CHIPS = (SIDE, SIDE, SIDE)
SHARDS = SIDE * SIDE * SIDE * CORES
SEQ, WIDTH, HIDDEN, TILE, PAIR, LN_ROWS = 384, 1024, 4096, 512, 128, 64
HEADS, HEAD, PARTS = 16, 64, 3
QKV = PARTS * WIDTH
N_TILES, N_PAIRS, N_BLOCKS = HIDDEN // TILE, WIDTH // PAIR, SEQ // PAIR
TWICE = 2 * PAIR
INV_SQRT2, INV_SQRT2PI, SCALE = 0.7071067811865476, 0.3989422804014327, 0.125
SHARES = (8, 8, 8, 8, 24, 8, 32, 8)
SIZES = tuple(SHARDS * share for share in SHARES)
OFFSETS = tuple(sum(SIZES[:k]) for k in range(len(SIZES)))
N_VEC = sum(SIZES)
GAIN1, BIAS1, GAIN2, BIAS2, QKV_BIAS, OUT_BIAS, UP_BIAS, DOWN_BIAS = range(len(SHARES))
ORDERS = ((2, 1, 0), (1, 0, 2), (0, 2, 1))
HALVES = range(2)
OWN, ONE, CROSS, TWO = range(SIDE)
ROLES = (ONE, TWO, CROSS)
A, B, C = range(AXES)
UP, DOWN, MIX = range(3)
SELF = 3


class Chip:
    def __init__(self):
        node, local = lax.axis_index('node'), lax.axis_index('local')
        self.core, self.other = lax.rem(local, CORES), 1 - lax.rem(local, CORES)
        self.where = (lax.div(node, SIDE), lax.rem(node, SIDE), lax.div(local, CORES))
        self.base = (node, local - self.core)
        self.strides = ((SIDE, 0), (1, 0), (0, CORES))
        self.near = [(v, v + 1 - 2 * parity(v), lax.rem(v + 2, SIDE), SIDE - 1 - v) for v in self.where]

        self.gaps = [near[3] - near[1] for near in self.near]

    def at(self, axis, role, half):
        near = self.near[axis]
        if role in (OWN, CROSS):
            return near[role]
        return near[role] + half * self.gaps[axis] if role == ONE else near[role] - half * self.gaps[axis]

    def device(self, axis, role, half):
        shift = self.at(axis, role, half) - self.where[axis]
        node, local = [b + shift * s if s else b for b, s in zip(self.base, self.strides[axis])]
        return (node, local + self.core)

    def partner(self):
        node, local = self.base
        return (node, local + self.other)

    def signal_partners(self, semaphore):
        for axis in range(AXES):
            for role in ROLES:
                pl.semaphore_signal(semaphore, inc=1, device_id=self.device(axis, role, A), device_id_type=MESH)
        pl.semaphore_signal(semaphore, inc=1, device_id=self.partner(), device_id_type=MESH)


def enter(chip):
    barrier = pltpu.get_barrier_semaphore()
    chip.signal_partners(barrier)
    pl.semaphore_wait(barrier, PARTNERS)


def remote(src, dst, send_sem, recv_sem, device):
    return pltpu.make_async_remote_copy(src_ref=src, dst_ref=dst, send_sem=send_sem, recv_sem=recv_sem, device_id=device,
                                        device_id_type=MESH)


def start(copies):
    for copy in copies:
        copy.start()
    return copies


def wait(copies):
    for copy in copies:
        copy.wait()


def loop(count):
    return pl.loop(0, count)


def halves(body):
    loop(len(HALVES))(body)


def parity(n):
    return lax.rem(n, 2)


def pool(sems):
    return (sems.at[n] for n in range(sems.shape[0]))


def contract(a, b, a_axis, b_axis):
    return lax.dot_general(a, b, (((a_axis,), (b_axis,)), ((), ())), preferred_element_type=F32)


def dot(a, b):
    return contract(a, b, 1, 0)


def dot_t(a, b):
    return contract(a, b, 1, 1)


def row_sum(x):
    return jnp.sum(x, axis=1, keepdims=True)


def column_sum(x):
    return jnp.sum(x, axis=0, keepdims=True)


def rounded(x):
    return x.astype(BF16).astype(F32)


def lanes(first, width=PAIR):
    return pl.ds(pl.multiple_of(first, PAIR), width)


def turn(x, cos, sin_a, sin_b):
    return x * cos + pltpu.roll(x, PAIR - ROWS, 1) * sin_a + pltpu.roll(x, ROWS, 1) * sin_b


def turn_back(d, cos, sin_a, sin_b):
    return d * cos + pltpu.roll(d * sin_a, ROWS, 1) + pltpu.roll(d * sin_b, PAIR - ROWS, 1)


def iota(shape, axis):
    return lax.broadcasted_iota(jnp.int32, shape, axis)


def block_rows(j):
    return slice(j * PAIR, (j + 1) * PAIR)


def split_heads(x):
    first = iota((PAIR, PAIR), 1) < HEAD
    rows = []
    for j in range(N_BLOCKS):
        block = x[block_rows(j)]
        rows += [jnp.where(first, block, jnp.zeros_like(block)), jnp.where(first, jnp.zeros_like(block), block)]
    return jnp.concatenate(rows, axis=0)


def total_of(chunks, join=jnp.add):
    return functools.reduce(join, chunks)


def probabilities(q_block, keys, i):
    scores = dot_t(q_block, keys)
    causal = iota((PAIR, PAIR), 0) >= iota((PAIR, PAIR), 1)
    chunks = [scores[:, block_rows(j)] * SCALE for j in range(CORES * (i + 1))]
    for head in HALVES:
        mine = slice(head, None, CORES)
        *ahead, last = chunks[mine]
        held = ahead + [jnp.where(causal, last, -1e30)]
        top = jnp.max(total_of(held, jnp.maximum), axis=1, keepdims=True)
        held = [jnp.exp(chunk - top) for chunk in held]
        inverse = 1.0 / row_sum(total_of(held))
        chunks[mine] = [chunk * inverse for chunk in held]
    return chunks


def side_by_side(chunks):
    return jnp.concatenate([chunk.astype(BF16) for chunk in chunks], axis=1)


def row_mean(x):
    return jnp.mean(x, axis=1, keepdims=True)


def normalised(h):
    center = h - row_mean(h)
    inverse = lax.rsqrt(row_mean(center * center) + EPSILON)
    return center * inverse, inverse


def half_copies(chip, src, dst, own_sem, send_sem, recv_sem):
    width = dst.shape[-1]
    mine, away = [src.at[:, lanes(which * width, width)] for which in (chip.core, chip.other)]
    place = dst.at[chip.core]
    return [pltpu.make_async_copy(mine, place, own_sem), remote(away, place, send_sem, recv_sem, chip.partner())]


class Gather:
    def __init__(self, chip, shards, fulls, sems):
        self.chip, self.shards, self.fulls = chip, shards, fulls
        self.send_sem, self.recv_sem, self.pass_send, self.pass_recv = sems

    def box(self, layer, k, half, stage, role, own=False):
        width = self.fulls[k].shape[-1] // len(HALVES)
        cols = lanes(half * width, width)
        if own:
            return self.shards[k].at[layer, :, cols]
        where = list(self.chip.where)
        for axis in ORDERS[k][:stage]:
            where[axis] = pl.ds(0, SIDE)
        axis = ORDERS[k][stage]
        where[axis] = self.chip.at(axis, role, half)
        return self.fulls[k].at[layer, where[0], where[1], where[2], self.chip.core, :, cols]

    def reach(self, layer, k, half, stage, step):
        slot, on = AXES * stage + step, stage > A and step == C
        src = self.box(layer, k, half, stage, ONE if on else OWN, stage == A)
        return remote(src, self.box(layer, k, half, stage, ONE if on else OWN), self.send_sem.at[layer, k, stage],
                      self.recv_sem.at[layer, k, half, slot], self.chip.device(ORDERS[k][stage], TWO if on else ROLES[step], half))

    def passing(self, layer, k, half, stage, step):
        role = (*ROLES, OWN)[step]
        return remote(self.box(layer, k, half, stage, role, step == SELF), self.box(layer, k, half, stage, role),
                      self.pass_send.at[layer, k], self.pass_recv.at[layer, k], self.chip.partner())

    def each(self, action):
        for k in (MIX, UP, DOWN):
            @halves
            def _(half):
                action(k, half)

    def begin(self, layer, stage):
        for step in range(C if stage else AXES):
            self.each(lambda k, half: self.reach(layer, k, half, stage, step).start())

    def own(self, layer):
        self.each(lambda k, half: self.passing(layer, k, half, A, SELF).start())

    def middle(self, layer, stage):
        def action(k, half):
            self.reach(layer, k, half, stage, A).wait_recv()
            self.reach(layer, k, half, stage, C).start()
            self.passing(layer, k, half, stage, A).start()
        self.each(action)

    def end(self, layer, stage, steps=range(AXES)):
        def action(k, half):
            for step in steps:
                self.reach(layer, k, half, stage, step).wait_recv()
                self.passing(layer, k, half, stage, step).start()
        self.each(action)

    def arrived(self, layer, k):
        box = self.fulls[k].at[layer, :, :, :, self.chip.other]
        remote(box, box, self.pass_send.at[layer, k], self.pass_recv.at[layer, k], self.chip.partner()).wait_recv()

    def left(self):
        three, full = pl.ds(0, AXES), self.fulls[UP].at[A]
        boxes = (full.at[three, A, A, A], full.at[:, three, A, A], full.at[:, :, three, A])

        @loop(LAYERS)
        def _(layer):
            @loop(AXES)
            def _(k):
                for stage, box in enumerate(boxes):
                    sem = self.send_sem.at[layer, k, stage]
                    remote(box, box, sem, sem, self.chip.partner()).wait_send()
                box, sem = full.at[:, :, :, A], self.pass_send.at[layer, k]
                remote(box, box, sem, sem, self.chip.partner()).wait_send()


def pick_lanes(sel_lane, cols):
    return (iota((PAIR, WIDTH), 0) == sel_lane[:, cols]).astype(F32).astype(BF16)


def vector_blocks():
    return [slice(k * WIDTH, (k + 1) * WIDTH) for k in range(N_VEC // WIDTH)]


def unpack_vectors(small_v, layer, sel_shard, sel_lane, vec_ref):
    tiles = small_v[...].astype(F32).reshape((SHARDS, ROWS, PAIR))
    held = jnp.sum(jnp.where(iota(tiles.shape, 1) == layer, tiles, 0.0), axis=1).astype(BF16)
    for cols in vector_blocks():
        spread = dot(held, pick_lanes(sel_lane, cols))
        spread = jnp.where(iota((SHARDS, WIDTH), 0) == sel_shard[:, cols], spread, 0.0)
        vec_ref[layer:layer + 1, cols] = column_sum(spread)


def forward_kernel(x_hbm, ycot_hbm, tables_hbm, places_hbm, up_s, down_s, mix_s, small_ref, up_f, down_f, mix_f, small_full, vec_ref,
                   dout_cols, y_hbm, h_hbm, n1_hbm, n2_hbm, ctx_hbm, act_hbm, qkv_hbm, pre_hbm, up_v, down_v, mix_v, small_v, acc, pre_v,
                   n1_v, n2_v, qkv_v, ctx_v, y_v, n1_t, n2_t, ctx_t, act_t, send_sem, recv_sem, pass_send, pass_recv,
                   small_send, small_recv, own_sems, load_sem, save_sem, share_send, share_recv, act_save, act_send, act_recv, tables,
                   places):
    shards, fulls, own_sem = (up_s, down_s, mix_s), (up_f, down_f, mix_f), pool(own_sems)
    chip = Chip()
    gather = Gather(chip, shards, fulls, (send_sem, recv_sem, pass_send, pass_recv))

    def small_copy(slot, where, device):
        place = small_full.at[(*where, chip.core)]
        return remote(place, place, small_send.at[slot], small_recv.at[slot], device)

    def small_reach(stage, step):
        where = list(chip.where)
        for axis in range(stage):
            where[axis] = pl.ds(0, SIDE)
        return small_copy(AXES * stage + step, where, chip.device(stage, ROLES[step], A))

    def small_begin(stage):
        start([small_reach(stage, step) for step in range(AXES)])

    def small_end(stage):
        for step in range(AXES):
            small_reach(stage, step).wait_recv()

    small_pass = small_copy(AXES * AXES, [pl.ds(0, SIDE)] * AXES, chip.partner())
    here = (*chip.where, chip.core)
    own = [pltpu.make_async_copy(small_ref, small_full.at[here], next(own_sem))]
    for shard, full in zip(shards, fulls):
        for layer in range(LAYERS):
            own.append(pltpu.make_async_copy(shard.at[layer], full.at[(layer, *here)], next(own_sem)))
    loads = [
        pltpu.make_async_copy(src, dst, next(own_sem)) for src, dst in ((x_hbm, y_v), (ycot_hbm, n1_v), (tables_hbm, tables), (places_hbm, places))]
    cot_copies = half_copies(chip, n1_v, dout_cols.at[LAYERS - 1], next(own_sem), next(own_sem), next(own_sem))
    start(own)
    start(loads)
    with jax.named_scope('enter'):
        enter(chip)
    with jax.named_scope('ag0'):
        gather.begin(A, A)
        gather.begin(B, A)
        wait(own)
        small_begin(A)
        gather.own(A)
        gather.own(B)
        gather.end(A, A)
    with jax.named_scope('ag1'):
        gather.begin(A, B)
        small_end(A)
        small_begin(B)
        gather.end(B, A)
        gather.begin(B, B)
        gather.middle(A, B)
        small_end(B)
        small_begin(C)
        gather.middle(B, B)
        gather.end(A, B, (B, C))
    with jax.named_scope('ag2_start'):
        gather.begin(A, C)
        small_end(C)
        small_pass.start()
        gather.end(B, B, (B, C))
    with jax.named_scope('ag2_middle'):
        gather.middle(A, C)
        gather.begin(B, C)
    with jax.named_scope('unpack'):
        small_pass.wait_recv()
        fetch = pltpu.make_async_copy(small_full, small_v, next(own_sem))
        fetch.start()
        fetch.wait()
        wait(loads)
        start(cot_copies)
        for layer in range(LAYERS):
            unpack_vectors(small_v, layer, places[A:B], places[B:C], vec_ref)
    with jax.named_scope('ag2_late'):
        gather.end(A, C, (B,))
    with jax.named_scope('ag2_end'):
        gather.end(A, C, (C,))
        wait(cot_copies)

    def saves(layer):
        pairs = [(y_v, h_hbm.at[layer]), (qkv_v, qkv_hbm.at[layer])]
        kept = [pltpu.make_async_copy(src, dst, save_sem.at[n]) for n, (src, dst) in enumerate(pairs)]
        for n, (src, dst) in enumerate(((n1_t, n1_hbm), (n2_t, n2_hbm), (ctx_t, ctx_hbm))):
            dst = dst.at[layer, chip.core]
            kept.append((pltpu.make_async_copy(src, dst, save_sem.at[CORES + n]),
                         remote(src, dst, share_send.at[layer, n], share_recv.at[layer, n], chip.partner())))
        return kept

    def quarter(layer, t):
        rows, tiles = pl.ds(t * WIDTH, WIDTH), pl.ds(CORES * t, CORES)
        src, dst = act_t.at[rows], act_hbm.at[layer, chip.core, rows]
        return [pltpu.make_async_copy(pre_v.at[tiles], pre_hbm.at[layer, tiles], act_save.at[A, t]),
                pltpu.make_async_copy(src, dst, act_save.at[B, t]),
                remote(src, dst, act_send.at[layer, t], act_recv.at[layer, t], chip.partner())]

    def settle(layer):
        _, qkv_save, *shares = saves(layer)
        qkv_save.wait()
        for share in shares:
            wait(share)

        @loop(SIDE)
        def _(t):
            wait(quarter(layer, t))

    @loop(LAYERS)
    def _(layer):
        def vector(k, first=0, width=None):
            return vec_ref[pl.ds(layer, 1), lanes(OFFSETS[k] + first, width or SIZES[k])]

        def load(k, piece):
            if k == DOWN:
                return pltpu.make_async_copy(fulls[k].at[layer, piece], down_v.at[piece], load_sem.at[k, piece])
            cols = lanes(piece * WIDTH, WIDTH)
            return pltpu.make_async_copy(fulls[k].at[layer, :, :, :, :, :, cols], (up_v, None, mix_v)[k].at[:, :, :, :, :, cols],
                                         load_sem.at[k, piece])

        def matrix(held, piece):
            return held[:, :, :, :, :, lanes(piece * WIDTH, WIDTH)].reshape((WIDTH, WIDTH))

        def have(k):
            gather.arrived(layer, k)

        def meanwhile(action):
            @pl.when(layer == A)
            def _():
                action()

        h_save, qkv_save, n1_share, n2_share, ctx_share = saves(layer)
        with jax.named_scope('have_mix'):
            have(MIX)
            start([load(MIX, k) for k in range(SIDE)])

        h_save.start()

        @pl.when(layer == B)
        def _():
            settle(A)

        with jax.named_scope('ln'):
            @loop(SEQ // LN_ROWS)
            def _(r):
                rows = pl.ds(pl.multiple_of(r * LN_ROWS, LN_ROWS), LN_ROWS)
                scaled, _ = normalised(y_v[rows, :].astype(F32))
                n1_v[rows, :] = (scaled * vector(GAIN1) + vector(BIAS1)).astype(BF16)
                n2_v[rows, :] = (scaled * vector(GAIN2) + vector(BIAS2)).astype(BF16)

        for src, dst, share in ((n1_v, n1_t, n1_share), (n2_v, n2_t, n2_share)):
            dst[...] = src[...].T
            start(share)

        with jax.named_scope('qkv'):
            for k in range(PARTS):
                load(MIX, k).wait()
                x = dot(n1_v[...], matrix(mix_v, k)) + vector(QKV_BIAS, k * WIDTH, WIDTH)
                for c in range(N_PAIRS):
                    block = x[:, block_rows(c)]
                    if k < C:
                        block = turn(block, *[tables[n] for n in range(PARTS)])
                    qkv_v[:, lanes(k * WIDTH + c * PAIR)] = block.astype(BF16)

        qkv_save.start()
        with jax.named_scope('have_up'):
            have(UP)
            have(DOWN)

        start([load(UP, k) for k in range(SIDE)] + [load(DOWN, k) for k in range(SIDE)])
        with jax.named_scope('fattn'):
            def one_pair(pair):
                keys = split_heads(qkv_v[:, lanes(WIDTH + pair * PAIR)])
                values = split_heads(qkv_v[:, lanes(C * WIDTH + pair * PAIR)])
                for i in range(N_BLOCKS):
                    n = (i + 1) * CORES * PAIR
                    probs = probabilities(qkv_v[block_rows(i), lanes(pair * PAIR)], keys[:n], i)
                    ctx_v[block_rows(i), lanes(pair * PAIR)] = dot(side_by_side(probs), values[:n]).astype(BF16)

            @loop(N_PAIRS // CORES)
            def _(two):
                for k in HALVES:
                    one_pair(CORES * two + k)

                @pl.when((layer == A) & (two == A))
                def _():
                    gather.middle(B, C)

        ctx_t[...] = ctx_v[...].T
        start(ctx_share)
        with jax.named_scope('fout'):
            load(MIX, PARTS).wait()
            acc[...] = y_v[...].astype(F32) + dot(ctx_v[...], matrix(mix_v, PARTS)) + (vector(OUT_BIAS) + vector(DOWN_BIAS))

        with jax.named_scope('fmlp'):
            @loop(SIDE)
            def _(t):
                cols = lanes(t * WIDTH, WIDTH)
                load(UP, t).wait()
                pre = dot(n2_v[...], matrix(up_v, t)) + vector(UP_BIAS, t * WIDTH, WIDTH)
                for k in HALVES:
                    pre_v[CORES * t + k] = pre[:, k * TILE:(k + 1) * TILE]
                act = (0.5 * pre * (1.0 + lax.erf(pre * INV_SQRT2))).astype(BF16)
                act_t[cols, :] = act.T
                start(quarter(layer, t))
                load(DOWN, t).wait()
                acc[...] += dot(act, down_v[t].reshape((WIDTH, WIDTH)))

                @pl.when((layer == A) & (t == B))
                def _():
                    gather.end(B, C, (B,))

        h_save.wait()
        y_v[...] = acc[...].astype(BF16)
        with jax.named_scope('fend'):
            meanwhile(lambda: gather.end(B, C, (C,)))

    with jax.named_scope('ftail'):
        last = pltpu.make_async_copy(y_v, y_hbm, next(own_sem))
        last.start()
        for stage in range(AXES):
            for step in range(AXES):
                small_reach(stage, step).wait_send()
        small_pass.wait_send()
        gather.left()
        settle(LAYERS - 1)
        last.wait()


def forward(x, y_cot, shards, small_tile, tables, places):
    grid = CHIPS + (CORES,)
    full = [(LAYERS,) + grid + tensor.shape[1:] for tensor in shards]
    shapes = [(shape, BF16) for shape in full] + [(grid + small_tile.shape, BF16), ((LAYERS, N_VEC), F32), ((LAYERS, CORES, SEQ, TILE), BF16), ((SEQ, WIDTH), BF16),
                                                  ((LAYERS, SEQ, WIDTH), BF16)]
    shapes += [((LAYERS, CORES, width, SEQ), BF16) for width in (WIDTH, WIDTH, WIDTH, HIDDEN)]
    shapes += [((LAYERS, SEQ, QKV), BF16), ((LAYERS, N_TILES, SEQ, TILE), F32)]
    dma = pltpu.SemaphoreType.DMA
    slots = AXES * AXES
    scratch = [pltpu.VMEM(shape[1:], BF16) for shape in full] + [pltpu.VMEM(grid + small_tile.shape, BF16)]
    scratch += [pltpu.VMEM((SEQ, WIDTH), F32), pltpu.VMEM((N_TILES, SEQ, TILE), F32)]
    scratch += [pltpu.VMEM((SEQ, width), BF16) for width in (WIDTH, WIDTH, QKV, WIDTH, WIDTH)]
    scratch += [pltpu.VMEM((width, SEQ), BF16) for width in (WIDTH, WIDTH, WIDTH, HIDDEN)]
    scratch += [dma(shape) for shape in ((LAYERS, AXES, AXES), (LAYERS, AXES, len(HALVES), slots), (LAYERS, AXES), (LAYERS, AXES))]
    scratch += [dma(shape) for shape in ((slots + 1,), (slots + 1,), (slots + SIDE + SIDE + AXES,), (AXES, SIDE), (SIDE + 1,), (LAYERS, AXES), (LAYERS, AXES), (CORES, SIDE), (LAYERS, SIDE), (LAYERS, SIDE))]
    scratch += [pltpu.VMEM(tables.shape, F32), pltpu.VMEM(places.shape, jnp.int32)]
    out_specs = [IN_VMEM if dtype == F32 and len(shape) == LAYERS else ANY for shape, dtype in shapes]
    return pl.pallas_call(
        forward_kernel,
        out_shape=[jax.ShapeDtypeStruct(*s) for s in shapes],
        in_specs=[ANY] * SIDE + [IN_VMEM] * SIDE,
        out_specs=out_specs,
        scratch_shapes=scratch,
        compiler_params=pltpu.CompilerParams(collective_id=0, has_side_effects=True, vmem_limit_bytes=VMEM_LIMIT),
        name='forward_layers',
    )(x, y_cot, tables, places, *shards, small_tile)


WAVES = ((384, 384, 512), (384, 384, 256), (256, 256, 256))
LEADS = ((2,) + CHIPS[1:], CHIPS[1:], (2, SIDE), (SIDE,), (AXES,))
W_UP, W_DOWN, W_QKV, W_OUT = range(4)
STEPS = ((1, (2,)), (0, ()), (2, (4, 3)), (4, (5,)), (3, ()), (5, (6, 7, 8)), (8, (9,)), (9, ()))
LAST = AXES * AXES
CARRIED = ((0, 6, 0), (1, 4, 0), (2, 0, 0))
US_COLUMN, US_HOP, US_ADD, US_STEP = 0.021, 2.5, 0.0013, 0.2
US_FIRST, US_OUT, US_TILE, US_GRADIENT, US_PAIR, US_NORM = 2, 1.4, 1.6, 0.0035, 3.6, 2.7


class Schedule:
    def __init__(self):
        self.now, self.free, self.lines = 0.0, {}, []

    def send(self, link, columns):
        self.free[link] = max(self.free.get(link, 0.0), self.now) + columns * US_COLUMN
        return self.free[link] + US_HOP

    def due(self, limit):
        found = []
        while self.lines:
            line = min(self.lines, key=lambda one: one[A][A]())
            ready = line[A][A]()
            if limit is not None and ready > limit:
                break
            _, run, sends, cost = line.pop(A)
            self.lines = [one for one in self.lines if one]
            self.now = max(self.now, ready) + cost
            sends()
            found.append(run)
        return found

    def finish(self, line):
        while line:
            ready, run, sends, cost = line.pop(A)
            self.now = max(self.now, ready()) + cost
            sends()
            run()
        self.lines = [one for one in self.lines if one]

    def run(self, limit):
        for step in self.due(limit):
            step()

    def passed(self, cost):
        self.now += cost
        self.run(self.now)

    def hooks(self, count, cost):
        planned = []
        for _ in range(count):
            self.now += cost
            planned.append(self.due(self.now))
        return planned


def at_hooks(n, planned):
    for when, steps in enumerate(planned):
        if steps:
            @pl.when(n == when)
            def _():
                for step in steps:
                    step()


def add_into(dst, src, n_axes):
    if n_axes < 2:
        dst[...] += src[...]
        return

    @loop(SIDE)
    def _(k):
        dst[k] += src[k]


def at_axis(ref, axis, value, n_axes):
    every = [pl.ds(0, SIDE)] * n_axes
    every[axis] = value
    return ref.at[tuple(every)]


class Reduce:
    def __init__(self, chip, schedule, wave, grads, came, fin, sems, spare, write, done, when=None):
        self.wave, self.chip, self.schedule, self.widths, self.grads = wave, chip, schedule, WAVES[wave], grads
        self.came, self.fin, (self.send_sem, self.recv_sem), (self.spare, self.spare_sem) = came, fin, sems, spare
        self.write, self.done, self.when, self.times = write, done, when, {}

    def box(self, a, half, stage):
        order = ORDERS[a]
        ref = self.came[a][A].at[half, A]
        spot = [axis for axis in range(AXES) if axis != order[A]].index(order[B])
        if stage == B:
            return ref, spot, C
        return at_axis(ref, spot, self.chip.where[order[B]], C), A, B

    def copy(self, a, half, slot):
        stage, turn = divmod(slot, AXES)
        sems = self.send_sem.at[a, stage], self.recv_sem.at[a, half, slot]
        if slot == LAST:
            return remote(self.total(a, half).at[self.chip.other], self.fin[a].at[half], *sems, self.chip.partner())
        axis = ORDERS[a][stage]
        if stage == C:
            role = value = ROLES[turn]
            dst = self.came[a][SIDE].at[half, turn]
        else:
            role, value = TWO if turn == C else ONE, (ONE, CROSS, TWO)[turn]
            dst = self.came[a][CORES * stage + turn // C].at[half]
            dst = dst if turn == C else dst.at[turn]
        value = self.chip.at(axis, value, half)
        if stage:
            ref, spot, n_axes = self.box(a, half, stage)
            src = at_axis(ref, spot, value, n_axes)
        else:
            src = self.came[a][A].at[half, B] if turn == C else at_axis(self.grads[a].at[half], axis, value, AXES)
        return remote(src, dst, *sems, self.chip.device(axis, role, half))

    def each(self, action):
        for a in range(AXES):
            halves(lambda half: action(a, half))

    def sending(self, slot):
        stage = slot // AXES
        share = SIDE ** (CORES * stage)
        self.times[slot] = self.schedule.now + US_HOP if slot == LAST else max(
            self.schedule.send(ORDERS[a][stage], self.widths[a] / share) for a in range(AXES))

    def begin(self):
        for slot in (B, A):
            self.each(lambda a, half: self.copy(a, half, slot).start())

    def plan(self, first=0, last=None, late=0):
        for slot in (B, A):
            self.times[slot] = self.schedule.now + late
            if not first:
                self.sending(slot)
        for _, sent in STEPS[:first]:
            self.times.update((slot, self.schedule.now + late + US_HOP) for slot in sent)
        line = [
            (lambda slot=slot: self.times[slot], lambda k=k: self.step(k), lambda sent=sent: [self.sending(n) for n in sent],
             CORES * US_ADD * sum(self.widths) if k < C else US_STEP) for k, (slot, sent) in enumerate(STEPS)][first:last]
        self.schedule.lines.append(line)
        return line

    def step(self, k):
        def work():
            with jax.named_scope(f'w{self.wave}s{k}'):
                (self.first, self.first, self.halve, self.settle, self.settle, self.spread, self.cross, self.finish)[k](STEPS[k][A])
        if self.when is None:
            work()
        else:
            pl.when(self.when)(work)

    def held(self, a, half):
        ref = self.spare[A].at[a] if a < C else self.spare[B]
        return ref.at[half, :, :, :, :, pl.ds(0, self.widths[a])]

    def first(self, slot):
        def local(a, half):
            axis = ORDERS[a][A]
            return pltpu.make_async_copy(at_axis(self.grads[a].at[half], axis, self.chip.at(axis, TWO if slot else OWN, half), AXES),
                                         self.held(a, half), self.spare_sem.at[a, half])

        def action(a, half):
            local(a, half).wait()
            self.copy(a, half, slot).wait_recv()
            add_into(self.came[a][A].at[half, slot], self.held(a, half), C)
            if slot:
                self.copy(a, half, C).start()

        self.each(lambda a, half: local(a, half).start())
        self.each(action)

    def halve(self, slot):
        def action(a, half):
            ref, spot, n_axes = self.box(a, half, B)
            self.copy(a, half, slot).wait_recv()
            for turn, role in ((B, CROSS), (A, ONE), (C, TWO), (C, OWN)):
                value = self.chip.at(ORDERS[a][B], role, half)
                add_into(at_axis(ref, spot, value, n_axes), at_axis(self.came[a][B].at[half], spot, value, n_axes), B)
                if turn < C:
                    self.copy(a, half, AXES + turn).start()
        self.each(action)

    def settle(self, slot):
        def action(a, half):
            ref, spot, n_axes = self.box(a, half, B)
            self.copy(a, half, slot).wait_recv()
            value = self.chip.at(ORDERS[a][B], TWO if slot > AXES else OWN, half)
            add_into(at_axis(ref, spot, value, n_axes), self.came[a][C].at[half, slot - AXES], B)
            if slot > AXES:
                self.copy(a, half, AXES + C).start()
        self.each(action)

    def spread(self, slot):
        def action(a, half):
            ref, *_ = self.box(a, half, C)
            self.copy(a, half, slot).wait_recv()
            add_into(ref, self.came[a][AXES].at[half], B)
            for turn in range(AXES):
                self.copy(a, half, CORES * AXES + turn).start()
        self.each(action)

    def total(self, a, half):
        ref, *_ = self.box(a, half, C)
        return ref.at[self.chip.where[ORDERS[a][C]]]

    def cross(self, _):
        def action(a, half):
            for turn in range(AXES):
                self.copy(a, half, CORES * AXES + turn).wait_recv()
            self.total(a, half)[...] += total_of([self.came[a][SIDE][half, turn] for turn in range(AXES)])
            self.copy(a, half, LAST).start()
        self.each(action)

    def finish(self, _):
        def action(a, half):
            self.write(a, half, self.chip.core, self.total(a, half)[self.chip.core])
            self.copy(a, half, LAST).wait_recv()
            self.write(a, half, self.chip.other, self.fin[a][half])
        self.each(action)
        three = pl.ds(0, AXES)
        for a, (grad, fin) in enumerate(zip(self.grads, self.fin)):
            for stage, block in enumerate((grad.at[:, :, :, three], grad.at[:, :, three, A], grad.at[:, three, A, A], fin)):
                sem = self.send_sem.at[a, stage]
                remote(block, block, sem, sem, self.chip.partner()).wait_send()
        self.done()


class VectorSum:
    def __init__(self, chip, schedule, total, came, sems, finish, when=None):
        self.schedule, self.total, self.came, self.sems, self.finish, self.when, self.ready = schedule, total, came, sems, finish, when, 0.0
        self.devices = [[chip.device(axis, role, A) for role in ROLES] for axis in range(AXES)] + [[chip.partner()]]

    def copies(self, k):
        return [remote(self.total, self.came.at[AXES * k + n], self.sems.at[A, AXES * k + n], self.sems.at[B, AXES * k + n], device)
                for n, device in enumerate(self.devices[k])]

    def sending(self, k):
        if k < SIDE:
            self.ready = self.schedule.send(k, N_VEC / (SIDE * SIDE * ROWS))

    def step(self, k):
        def work():
            with jax.named_scope(f'vec{k}'):
                wait(self.copies(k - 1))
                for n in range(len(self.devices[k - 1])):
                    self.total[...] += self.came[AXES * (k - 1) + n]
            if k < SIDE:
                start(self.copies(k))
            else:
                self.finish()
        if self.when is None:
            work()
        else:
            pl.when(self.when)(work)

    def begin(self):
        start(self.copies(A))

    def plan(self):
        self.sending(A)
        self.schedule.lines.append([
            (lambda: self.ready, lambda k=k: self.step(k), lambda k=k: self.sending(k), US_STEP) for k in range(1, SIDE + 1)])


def backward_kernel(ycot_hbm, tables, vec_ref, places, up_hbm, down_hbm, mix_hbm, h_hbm, n1_hbm, n2_hbm, ctx_hbm,
                    act_hbm, qkv_hbm, pre_hbm, _, dx_hbm, small_ref, up_sum, down_sum, qkv_sum, out_sum, dout_cols, dpre_cols,
                    dqkv_cols, *refs):
    n_arrays, sums = AXES * len(WAVES), (up_sum, down_sum, qkv_sum, out_sum)
    grads, refs = refs[:n_arrays], refs[n_arrays:]
    (spare, spare_wide, tile_v, big_v, rhs_v, wup_v, wdown_v, pre_v, dn1, dn2, dctx, dk_acc, dv_acc, qkv_v, dpre_v, dqkv_v, dh_v, h_v,
     totals, came_vec, send_sem, recv_sem, spare_sem, tile_sem, big_sem, rhs_sem, mlp_sem, io_sem, own_sem, share_send,
     share_recv, pre_sem, vec_sem, credit, *refs) = refs
    fins, came = refs[:n_arrays], refs[n_arrays:]
    first_in = pltpu.make_async_copy(ycot_hbm, dh_v, io_sem.at[A])
    first_in.start()
    chip = Chip()
    core, other = chip.core, chip.other

    def exchange(layer, k, src, dst):
        return half_copies(chip, src, dst.at[layer], own_sem.at[k], share_send.at[k], share_recv.at[k])

    def tokens_load(layer, src, part, slot):
        return [pltpu.make_async_copy(src.at[layer, k, pl.ds(part * WIDTH, WIDTH)], big_v.at[slot, :, pl.ds(k * SEQ, SEQ)],
                                      big_sem.at[slot, k]) for k in range(CORES)]

    def weight_load(layer, k, slot):
        return pltpu.make_async_copy(mix_hbm.at[layer, :, lanes(k * WIDTH, WIDTH)], big_v.at[slot], big_sem.at[slot, CORES])

    def tile_loads(layer, t, slot):
        rows = lanes(t * TILE, TILE)
        pairs = ((down_hbm.at[layer, rows], wdown_v), (pre_hbm.at[layer, t], pre_v), (up_hbm.at[layer, :, rows], wup_v))
        return [pltpu.make_async_copy(src, dst.at[slot], mlp_sem.at[slot, n]) for n, (src, dst) in enumerate(pairs)]

    def input_loads(layer):
        return [pltpu.make_async_copy(qkv_hbm.at[layer], qkv_v, io_sem.at[B]), pltpu.make_async_copy(h_hbm.at[layer], h_v, io_sem.at[C])]

    def rhs_load(layer, src, first, width, k):
        cols = lanes(first, width)
        return [pltpu.make_async_copy(src.at[layer, n, :, cols], rhs_v.at[pl.ds(n * SEQ, SEQ), cols], rhs_sem.at[k, n])
                for n in range(CORES)]

    def prefetch(layer):
        start(tokens_load(layer, ctx_hbm, A, AXES) + tokens_load(layer, act_hbm, A, A))

    def prefetch_more(layer):
        start(tokens_load(layer, act_hbm, B, B) + tokens_load(layer, act_hbm, C, C) + input_loads(layer))
        for t in HALVES:
            start(tile_loads(layer, t, t))

    prefetch(LAYERS - 1)
    start(rhs_load(LAYERS - 1, dout_cols, A, TILE, A))
    prefetch_more(LAYERS - 1)
    with jax.named_scope('enter'):
        enter(chip)
    with jax.named_scope('first_in'):
        first_in.wait()
    dx_copy = pltpu.make_async_copy(dh_v, dx_hbm, io_sem.at[A])

    def vector_at(k, first=0, width=None):
        return lanes(OFFSETS[k] + first, width or SIZES[k])

    def reduction(schedule, layer, wave, when):
        def write(a, half, side, block):
            def put(arr, group, col, first, width):
                size = sums[arr].shape[-1] // CORES
                sums[arr][layer, group, :, lanes(side * size + col, width)] = block[:, first:first + width].astype(BF16)
            width, colour = WAVES[wave][a], CORES * a + half
            if wave:
                first = colour * width if wave == C or a < C else SIDE * WAVES[wave][A] + half * width
                put(W_QKV if wave == C else W_UP, A, first, A, width)
            elif a < C:
                put(W_DOWN, colour, A, A, width)
            else:
                for k in HALVES:
                    put(W_DOWN, CORES * half + k, WAVES[A][A], k * PAIR, PAIR)
                put(W_OUT, A, half * TWICE, TWICE, TWICE)

        def done():
            @pl.when(layer == LAYERS - 1)
            def _():
                chip.signal_partners(credit.at[wave])

        where = slice(AXES * wave, AXES * (wave + 1))
        count = len(LEADS)
        return Reduce(chip, schedule, wave, [grad.at[layer] for grad in grads[where]],
                      [came[count * (AXES * wave + a):count * (AXES * wave + a + 1)] for a in range(AXES)],
                      fins[where], (send_sem.at[wave], recv_sem.at[wave]), ((spare, spare_wide), spare_sem), write, done, when)

    def vector_sum(schedule, layer, when):
        def own_part():
            with jax.named_scope('own'):
                node, local = chip.base
                me = node * (SIDE * CORES) + local + core
                row = jnp.zeros((ROWS, PAIR), F32)
                for k, share in enumerate(SHARES):
                    if k == QKV_BIAS:
                        firsts = [part * WIDTH + lax.div(me, CORES * ROWS) * PAIR for part in range(PARTS)]
                    else:
                        firsts = [lax.div(me * share, PAIR) * PAIR]
                    for first in firsts:
                        cols = lanes(OFFSETS[k] + first)
                        left = jnp.zeros((ROWS, PAIR), F32) + totals[layer, :, cols] * (places[A:B, cols] == me).astype(F32)
                        pick = (iota((PAIR, PAIR), 0) == places[B:C, cols]).astype(F32).astype(BF16)
                        for _ in range(PARTS):
                            row = row + dot_t(left.astype(BF16), pick)
                            left = left - rounded(left)
                small_ref[layer] = row.astype(BF16)

            @pl.when(layer == LAYERS - 1)
            def _():
                chip.signal_partners(credit.at[AXES])

        return VectorSum(chip, schedule, totals.at[layer], came_vec, vec_sem, own_part, when)

    def run_on(schedule, layer, when):
        lines = [reduction(schedule, layer, wave, when).plan(step, late=late) for wave, step, late in CARRIED]
        vector_sum(schedule, layer, when).plan()
        return lines

    @loop(LAYERS + 1)
    def _(turn_no):
        layer = LAYERS - 1 - turn_no
        working = pl.when(turn_no < LAYERS)
        total = totals.at[layer]
        schedule = Schedule()

        carried = run_on(schedule, layer + 1, turn_no > A)

        def product(lhs_slot, first, width, out_slot):
            value = dot(big_v[lhs_slot, :, 0:CORES * SEQ], rhs_v[:, lanes(first, width)])
            tile_v[out_slot, :, :, :, :, :, 0:width] = value.reshape(CHIPS + (CORES, ROWS, width))

        def tile_out(slot, src, dst):
            return pltpu.make_async_copy(src, dst, tile_sem.at[slot])

        def tile_done(slot, width):
            block = tile_v.at[slot, :, :, :, :, :, pl.ds(0, width)]
            tile_out(slot, block, block).wait()

        def columns(wave, a, half, first, width):
            return grads[AXES * wave + a].at[layer, half, :, :, :, :, :, pl.ds(first, width)]

        def launch(wave):
            schedule.finish(carried[wave])

            @pl.when(turn_no == B)
            def _():
                pl.semaphore_wait(credit.at[wave], PARTNERS)

            current = reduction(schedule, layer, wave, turn_no < LAYERS)
            if wave == C:
                @pl.when(turn_no == B)
                def _():
                    pl.semaphore_wait(credit.at[AXES], PARTNERS)

                @working
                def _():
                    vector_sum(schedule, layer, None).begin()

            working(current.begin)
            if wave < C:
                current.plan(last=CARRIED[wave][B])

        @working
        def _():
            with jax.named_scope('dw_out'):
                @pl.when(turn_no == B)
                def _():
                    wait(exchange(layer, A, dh_v, dout_cols))
                    start(rhs_load(layer, dout_cols, A, TILE, A))

                wait(rhs_load(layer, dout_cols, A, TILE, A))
                wait(tokens_load(layer, ctx_hbm, A, AXES))
                product(AXES, A, TILE, B)
                start(tokens_load(layer, act_hbm, AXES, AXES))
                for k in HALVES:
                    tile_out(B, tile_v.at[B, :, :, :, :, :, pl.ds(k * TWICE, TWICE)], columns(A, C, k, TWICE, TWICE)).start()

        schedule.passed(US_FIRST)
        out_hooks = schedule.hooks(SIDE, US_OUT)

        @loop(SIDE)
        def _(z):
            @working
            def _():
                slot = parity(z)
                wait(tokens_load(layer, act_hbm, z, z))

                @pl.when(z > A)
                def _():
                    tile_done(slot, TILE)

                product(z, A, TILE, slot)
                split = WAVES[A][A]
                for k in range(SIDE):
                    a, half = divmod(k, CORES)
                    for c in range(CORES):
                        block = tile_v.at[slot, :, :, CORES * c + a, half]
                        tile_out(slot, block.at[:, :, :, pl.ds(0, split)], grads[a].at[layer, half, z, :, :, c]).start()
                        tile_out(slot, block.at[:, :, :, pl.ds(split, PAIR)],
                                 grads[C].at[layer, a, z, :, :, c, :, pl.ds(half * PAIR, PAIR)]).start()

            at_hooks(z, out_hooks)

        @working
        def _():
            start(tokens_load(layer, n2_hbm, A, A) + [weight_load(layer, k, k + 1) for k in range(PARTS)])
            for slot in HALVES:
                tile_done(slot, TILE)

        schedule.passed(US_STEP)
        launch(A)

        @working
        def _():
            dn2[...] = jnp.zeros_like(dn2)

        def pre_copy(t, slot, away):
            place = dpre_cols.at[layer, core, :, lanes(lax.rem(t, SIDE) * TILE, TILE)]
            if away:
                return remote(dpre_v.at[slot], place, pre_sem.at[A, t], pre_sem.at[B, t], chip.partner())
            return pltpu.make_async_copy(dpre_v.at[slot], place, own_sem.at[CORES + slot])

        def pre_act(t, leave):
            for away, whose in ((False, core), (True, other)):
                @pl.when(lax.div(t, SIDE) == whose)
                def _():
                    copy = pre_copy(t, parity(t), away)
                    if leave:
                        copy.start()
                    elif away:
                        copy.wait_send()
                    else:
                        copy.wait()

        tile_hooks = schedule.hooks(N_TILES, US_TILE)

        with jax.named_scope('mlp'):
            @loop(N_TILES)
            def _(t):
                @working
                def _():
                    slot = parity(t)
                    wait(tile_loads(layer, t, slot))
                    d_act = rounded(dot_t(dh_v[...], wdown_v[slot]))
                    pre = pre_v[slot]
                    slope = 0.5 * (1.0 + lax.erf(pre * INV_SQRT2)) + pre * (INV_SQRT2PI * jnp.exp(-0.5 * pre * pre))
                    d_pre = d_act * slope
                    total[:, vector_at(UP_BIAS, t * TILE, TILE)] = column_sum(d_pre)

                    @pl.when(t > B)
                    def _():
                        pre_act(t - CORES, False)

                    dpre_v[slot] = d_pre.astype(BF16)
                    pre_act(t, True)
                    dn2[...] += dot_t(dpre_v[slot], wup_v[slot])

                    @pl.when(t + CORES < N_TILES)
                    def _():
                        start(tile_loads(layer, t + CORES, slot))

                at_hooks(t, tile_hooks)

        @working
        def _():
            for t in HALVES:
                pre_act(N_TILES - CORES + t, False)
            for t in range(SIDE):
                pre_copy(SIDE * core + t, A, True).wait_recv()

        def gradient_loads(wave, source):
            first = 0
            for a in range(AXES):
                width = CORES * WAVES[wave][a]
                start(rhs_load(layer, source, first, width, a))
                first += width

        def gradient_wave(wave, source, lhs_slot, first, orders):
            split, count = WAVES[wave][orders[A]], len(orders)
            width = CORES * split
            planned = schedule.hooks(count, width * US_GRADIENT)

            @loop(count)
            def _(n):
                @working
                def _():
                    slot = parity(n)
                    wait(rhs_load(layer, source, first + n * width, width, orders[A] + n))

                    @pl.when(n > B)
                    def _():
                        tile_done(slot, width)

                    product(lhs_slot, first + n * width, width, slot)
                    for k, a in enumerate(orders):
                        @pl.when(n == k)
                        def _():
                            for half in HALVES:
                                block = tile_v.at[slot, :, :, :, :, :, pl.ds(half * split, split)]
                                tile_out(slot, block, columns(wave, a, half, 0, split)).start()

                at_hooks(n, planned)

            @working
            def _():
                for slot in range(min(count, CORES)):
                    tile_done(slot, width)

        @working
        def _():
            gradient_loads(B, dpre_cols)
            wait(tokens_load(layer, n2_hbm, A, A))

        with jax.named_scope('dw1'):
            gradient_wave(B, dpre_cols, A, A, (A, B))
            gradient_wave(B, dpre_cols, A, SIDE * WAVES[B][A], (C,))
        launch(B)
        @working
        def _():
            weight_load(layer, AXES, A).start()
            d_sum = column_sum(dh_v[...].astype(F32))
            total[:, vector_at(OUT_BIAS)] = d_sum
            total[:, vector_at(DOWN_BIAS)] = d_sum
            wait(input_loads(layer))
            weight_load(layer, AXES, A).wait()
            dctx[...] = dot_t(dh_v[...], big_v[A]).astype(BF16)

        pair_hooks = schedule.hooks(N_PAIRS // CORES, US_PAIR)

        with jax.named_scope('attn'):
            def one_pair(pair, dk_sum, dv_sum):
                at = lanes(pair * PAIR)
                keys = split_heads(qkv_v[:, lanes(WIDTH + pair * PAIR)])
                values = split_heads(qkv_v[:, lanes(C * WIDTH + pair * PAIR)])
                q_t = qkv_v[:, at].T
                dc_t = dctx[:, at].T
                bias_sums = [jnp.zeros((1, PAIR), F32)] * PARTS

                def turned_back(n, d, rows, to):
                    d = turn_back(rounded(d), *[tables[k, rows, :] for k in range(PARTS)])
                    bias_sums[n] = bias_sums[n] + column_sum(d)
                    dqkv_v[rows, to] = d.astype(BF16)

                for i in range(N_BLOCKS):
                    old, n = i * TWICE, (i + 1) * TWICE
                    rows = block_rows(i)
                    probs = probabilities(qkv_v[rows, at], keys[:n], i)
                    d_all = rounded(dot_t(dctx[rows, at], values[:n]))
                    d_scores = [d_all[:, block_rows(j)] for j in range(CORES * (i + 1))]
                    for head in HALVES:
                        mine = slice(head, None, CORES)
                        mean = row_sum(total_of([p * d for p, d in zip(probs[mine], d_scores[mine])]))
                        d_scores[mine] = [p * (d - mean) * SCALE for p, d in zip(probs[mine], d_scores[mine])]
                    d_scores, probs = side_by_side(d_scores), side_by_side(probs)
                    turned_back(A, dot(d_scores, keys[:n]), rows, at)
                    for acc, left, right in ((dk_sum, q_t, d_scores), (dv_sum, dc_t, probs)):
                        part = dot(left[:, rows], right)
                        if i:
                            acc[:, :old] += part[:, :old]
                        acc[:, old:n] = part[:, old:]
                first = iota((PAIR, PAIR), 0) < HEAD
                for j in range(N_BLOCKS):
                    rows = block_rows(j)
                    d_key, d_value = [jnp.where(first, acc[:, block_rows(CORES * j)], acc[:, block_rows(CORES * j + 1)]).T
                                      for acc in (dk_sum, dv_sum)]
                    turned_back(B, d_key, rows, lanes(WIDTH + pair * PAIR))
                    d_value = d_value.astype(BF16)
                    bias_sums[C] = bias_sums[C] + column_sum(d_value.astype(F32))
                    dqkv_v[rows, lanes(C * WIDTH + pair * PAIR)] = d_value
                for k, bias_sum in enumerate(bias_sums):
                    total[:, vector_at(QKV_BIAS, k * WIDTH + pair * PAIR, PAIR)] = bias_sum

            @loop(N_PAIRS // CORES)
            def _(two):
                @working
                def _():
                    for k in HALVES:
                        one_pair(CORES * two + k, dk_acc.at[k], dv_acc.at[k])

                at_hooks(two, pair_hooks)

        @working
        def _():
            start(exchange(layer, B, dqkv_v, dqkv_cols))
            dn1[...] = jnp.zeros_like(dn1)

            with jax.named_scope('dn1'):
                @loop(PARTS)
                def _(k):
                    weight_load(layer, k, k + 1).wait()
                    dn1[...] += dot_t(dqkv_v[:, lanes(k * WIDTH, WIDTH)], big_v[k + 1])

                    @pl.when(k == A)
                    def _():
                        start(tokens_load(layer, n1_hbm, A, B))

        schedule.passed(US_NORM)

        @working
        def _():
            wait(exchange(layer, B, dqkv_v, dqkv_cols))
            gradient_loads(C, dqkv_cols)
            wait(tokens_load(layer, n1_hbm, A, B))

        with jax.named_scope('dw2'):
            gradient_wave(C, dqkv_cols, B, A, (A, B, C))

        @working
        def _():
            for k in (GAIN1, BIAS1, GAIN2, BIAS2):
                total[:, vector_at(k)] = jnp.zeros((1, WIDTH), F32)

            with jax.named_scope('lnb'):
                @loop(SEQ // LN_ROWS)
                def _(r):
                    rows = pl.ds(pl.multiple_of(r * LN_ROWS, LN_ROWS), LN_ROWS)
                    scaled, inverse = normalised(h_v[rows, :].astype(F32))
                    d1, d2 = rounded(dn1[rows, :]), rounded(dn2[rows, :])
                    for k, value in ((GAIN1, d1 * scaled), (BIAS1, d1), (GAIN2, d2 * scaled), (BIAS2, d2)):
                        total[:, vector_at(k)] += column_sum(value)
                    g1, g2 = [vec_ref[pl.ds(layer, 1), lanes(OFFSETS[k], WIDTH)] for k in (GAIN1, GAIN2)]
                    d_scaled = d1 * g1 + d2 * g2
                    d_h = inverse * (d_scaled - row_mean(d_scaled) - scaled * row_mean(d_scaled * scaled))
                    dh_v[rows, :] = (dh_v[rows, :].astype(F32) + d_h).astype(BF16)

        @pl.when(turn_no == A)
        def _():
            start(exchange(layer - 1, A, dh_v, dout_cols))

        @pl.when(turn_no == B)
        def _():
            dx_copy.start()

        @pl.when(turn_no == A)
        def _():
            prefetch(layer - 1)
            prefetch_more(layer - 1)

        schedule.now += US_NORM
        schedule.run(None)
        launch(C)

    dx_copy.wait()


def backward(y_cot, tables, vectors, places, weights, saved):
    dma, one = pltpu.SemaphoreType.DMA, (1,)
    pair, wide, row = (len(HALVES),), (SEQ, WIDTH), one + (N_VEC,)
    shapes = [(wide, BF16), ((LAYERS, ROWS, PAIR), BF16)]
    shapes += [((LAYERS, groups, ROWS, width), BF16) for groups, width in ((*one, HIDDEN), (SIDE, WIDTH), (*one, QKV), (*one, WIDTH))]
    in_vmem = len(shapes)
    shapes += [((LAYERS, CORES, SEQ, width), BF16) for width in (TILE, SIDE * TILE, PARTS * TILE)]
    blocks = [(CORES, ROWS, width) for wave in WAVES for width in wave]
    shapes += [((LAYERS,) + pair + CHIPS + block, F32) for block in blocks]
    tile = (CORES, ROWS)
    scratch = [(pair + pair + CHIPS[1:] + tile + (WAVES[0][0],), F32), (pair + CHIPS[1:] + tile + (TILE,), F32), (pair + CHIPS + tile + (CORES * WAVES[0][0],), F32), ((SIDE, WIDTH, WIDTH), BF16), ((CORES * SEQ, SIDE * TILE), BF16)]
    scratch += [(pair + shape, BF16) for shape in ((WIDTH, TILE), (TILE, WIDTH))]
    scratch += [(pair + (SEQ, TILE), F32), (wide, F32), (wide, F32), (wide, BF16)] + [(pair + (PAIR, CORES * SEQ), F32)] * CORES
    scratch += [((SEQ, QKV), BF16), (pair + (SEQ, TILE), BF16), ((SEQ, QKV), BF16), (wide, BF16), (wide, BF16), ((LAYERS,) + row, F32),
                ((PARTNERS,) + row, F32)]
    slots = (len(WAVES), AXES) + pair + (LAST + 1,)
    sems = [dma(shape) for shape in ((len(WAVES), AXES, SIDE), slots, (AXES,) + pair, pair, (SIDE, AXES), (AXES, CORES), pair + (PARTS,), (AXES,),
                                     (SIDE,), pair, pair, pair + (N_TILES,), pair + (PARTNERS,))]
    late = [(pair + block[1:], F32) for block in blocks] + [(pair + lead + block, F32) for block in blocks for lead in LEADS]
    outs = pl.pallas_call(
        backward_kernel,
        out_shape=[jax.ShapeDtypeStruct(*s) for s in shapes],
        in_specs=[ANY] + [IN_VMEM] * AXES + [ANY] * (PARTNERS + 1),
        input_output_aliases={SIDE + PARTNERS: in_vmem},
        out_specs=[ANY] + [IN_VMEM] * (in_vmem - 1) + [ANY] * (len(shapes) - in_vmem),
        scratch_shapes=[pltpu.VMEM(*s) for s in scratch] + sems + [pltpu.SemaphoreType.REGULAR((SIDE,))]
        + [pltpu.VMEM(*s) for s in late],
        compiler_params=pltpu.CompilerParams(collective_id=1, has_side_effects=True, vmem_limit_bytes=VMEM_LIMIT),
        name='backward_layers',
    )(y_cot, tables, vectors, places, *weights, *saved)
    d_x, small, *sums = outs[:in_vmem]
    return d_x, small[:, 0], [s.reshape((LAYERS, -1, s.shape[-1])) for s in sums]


def finish_kernel(*refs):
    n_large = CORES + AXES
    large, small_ref, refs = refs[:n_large], refs[n_large], refs[n_large + 1:]
    outs, small_outs, refs = refs[:n_large], refs[n_large:n_large + len(SHARES)], refs[n_large + len(SHARES):]
    held, sems = refs[:n_large], refs[n_large]
    loads = start([pltpu.make_async_copy(src, dst, sems.at[n]) for n, (src, dst) in enumerate(zip(large, held))])
    first = 0
    for share, out in zip(SHARES, small_outs):
        out[...] = small_ref[:, first:first + share]
        first += share
    stores = []
    for load, src, dst in zip(loads, held, outs):
        load.wait()
        stores += start([pltpu.make_async_copy(src, dst, sems.at[n_large + len(stores)])])
    wait(stores)


def finish(large, small):
    shapes = [jax.ShapeDtypeStruct(t.shape, BF16) for t in large] + [jax.ShapeDtypeStruct((LAYERS, share), BF16) for share in SHARES]
    outs = pl.pallas_call(
        finish_kernel,
        out_shape=shapes,
        in_specs=[ANY] * len(large) + [IN_VMEM],
        out_specs=[ANY] * len(large) + [IN_VMEM] * len(SHARES),
        scratch_shapes=[pltpu.VMEM(t.shape, BF16) for t in large] + [pltpu.SemaphoreType.DMA((CORES * len(large),))],
        name='finish',
    )(*large, small)
    return outs[:len(large)], outs[len(large):]


def rope_tables():
    rot_dim, f32 = HEAD // SIDE, np.float32
    inv_freq = f32(1.0) / f32(10000.0) ** (np.arange(0, rot_dim, 2, dtype=f32) / f32(rot_dim))
    angles = np.arange(SEQ, dtype=f32)[:, None] * inv_freq[None, :]
    cos, sin = np.cos(angles), np.sin(angles)
    zero = np.zeros_like(sin)
    rest = np.zeros((SEQ, HEAD - rot_dim), f32)
    tables = ([cos, cos, rest + f32(1.0)], [-sin, zero, rest], [zero, sin, rest])
    return jnp.asarray(np.stack([np.tile(np.concatenate(table, axis=1), (1, 2)) for table in tables]).astype(f32))


def heads_last(tensor):
    lead = tensor.shape[:-2]
    return tensor.reshape(lead + (HEADS, PARTS, HEAD)).swapaxes(-3, -2).reshape(lead + (QKV,))


def heads_first(tensor):
    lead = tensor.shape[:-1]
    return tensor.reshape(lead + (PARTS, HEADS, HEAD)).swapaxes(-3, -2).reshape(lead + (HEADS, PARTS * HEAD))


def vector_places():
    shard, lane, first = [], [], 0
    for k, (share, size) in enumerate(zip(SHARES, SIZES)):
        place = np.arange(size)
        if k == QKV_BIAS:
            place = heads_last(place.reshape(HEADS, -1))
        shard.append(place // share)
        lane.append(first + place % share)
        first += share
    return jnp.asarray(np.stack([np.concatenate(shard), np.concatenate(lane)]).astype(np.int32))


def solution(mesh):
    shard_axes = ('node', 'local')
    act_spec = P(shard_axes)
    param_spec = P(None, shard_axes)

    def device_step(x, y_cot, ln1_gain, ln1_bias, qkv_weight, qkv_bias, out_weight, out_bias,
                    ln2_gain, ln2_bias, up_weight, up_bias, down_weight, down_bias):
        tables, places = rope_tables(), vector_places()
        small = (ln1_gain, ln1_bias, ln2_gain, ln2_bias, qkv_bias, out_bias, up_bias, down_bias)
        small_tile = jnp.pad(jnp.concatenate(small, axis=1), ((0, ROWS - LAYERS), (0, PAIR - sum(SHARES))))
        mix = jnp.concatenate([heads_last(qkv_weight), out_weight], axis=-1)
        *weights, _, vectors, dout_cols, y_out, hidden, n1, n2, ctx, act, qkv, pre = forward(
            x[0], y_cot[0], (up_weight, down_weight, mix), small_tile, tables, places)
        weights = [tensor.reshape((LAYERS, -1, tensor.shape[-1])) for tensor in weights]
        d_x, small_sums, (up, down, qkv, out) = backward(
            y_cot[0], tables, vectors, places, weights, (hidden, n1, n2, ctx, act, qkv, pre, dout_cols))
        (y_out, d_x, up, down, out), (g1, b1, g2, b2, qb, ob, ub, db) = finish((y_out, d_x, up, down, out), small_sums)
        return (y_out[None], d_x[None], g1, b1, heads_first(qkv), qb, out, ob, g2, b2, up, ub, down, db)

    return jax.shard_map(device_step, mesh=mesh,
                         in_specs=(act_spec, act_spec) + (param_spec,) * 12,
                         out_specs=(act_spec, act_spec) + (param_spec,) * 12,
                         check_vma=False)
```
